128 devices in a mesh: batch: 1, head: 16 (over z, y), seq: 8 (over x, core).
Axes of the slice: x: 4, y: 4, z: 4, core: 2. Of those that a mesh axis runs over, the one named last changes fastest.
Arguments:
- x_embed: bfloat16 [8192, 4096], P(('batch', 'seq'))
- positions: int32 [8192], P(('batch', 'seq'))
- w_q: bfloat16 [2, 4096, 16, 256], P(None, None, 'head')
- w_k: bfloat16 [2, 4096, 16, 256], P(None, None, 'head')
- w_v: bfloat16 [2, 4096, 16, 256], P(None, None, 'head')
- w_o: bfloat16 [2, 16, 256, 4096], P(None, 'head')
- w_gate: bfloat16 [2, 4096, 16384], P(None, None, 'head')
- w_up: bfloat16 [2, 4096, 16384], P(None, None, 'head')
- w_down: bfloat16 [2, 16384, 4096], P(None, 'head')
- norm_gain: bfloat16 [2, 4096], replicated
Outputs:
- output 1: bfloat16 [8192, 4096], P(('batch', 'seq'))
- output 2: bfloat16 [2, 8192, 16, 256], P(None, ('batch', 'seq'), 'head')
- output 3: bfloat16 [2, 8192, 16, 256], P(None, ('batch', 'seq'), 'head')
All inputs are finite; a program needn't handle non-finite values.
Results may differ from the reference program's by a relative error of at most 0.02.
Values are sent between devices in bfloat16 or wider.
A program may use at most 1 GiB of HBM per device.

```python
import math
import jax
import jax.numpy as jnp
from jax import lax

SEQ_LEN = 8192
D_MODEL = 4096
NUM_HEADS = 16
KV_HEADS = 16
HEAD_DIM = 256
FF_DIM = 16384
LAYERS = 2
QUERY_BLOCK = 128
ROPE_BASE = 500000
EPS = 1e-5


def draw_normal(rng_key, arr_shape, std_scale):
    return (jax.random.normal(rng_key, arr_shape, jnp.float32) * std_scale).astype(jnp.bfloat16)


def setup_inputs(seed: int = 0, part: int = 0) -> dict:
    shared_root, part_root = jax.random.split(jax.random.key(seed))
    part_key = jax.random.fold_in(part_root, part)
    key_embed, key_gap, key_offset = jax.random.split(part_key, 3)
    weight_keys = jax.random.split(shared_root, 8)
    logit_std = math.sqrt(0.5 * math.log(SEQ_LEN))
    qk_scale = math.sqrt(logit_std / D_MODEL)
    out_scale = 0.5 * SEQ_LEN ** 0.25 / math.sqrt(NUM_HEADS * HEAD_DIM)
    x_embed = draw_normal(key_embed, (SEQ_LEN, D_MODEL), 1.0)
    pos_gaps = jax.random.randint(key_gap, (SEQ_LEN,), 1, 4)
    offset = jax.random.randint(key_offset, (), 0, 1024)
    positions = (offset + jnp.cumsum(pos_gaps) - pos_gaps[0]).astype(jnp.int32)
    gains = 1.0 + 0.3 * jax.random.normal(weight_keys[7], (LAYERS, D_MODEL), jnp.float32)
    return {
        'x_embed': x_embed,
        'positions': positions,
        'w_q': draw_normal(weight_keys[0], (LAYERS, D_MODEL, NUM_HEADS, HEAD_DIM), qk_scale),
        'w_k': draw_normal(weight_keys[1], (LAYERS, D_MODEL, KV_HEADS, HEAD_DIM), qk_scale),
        'w_v': draw_normal(weight_keys[2], (LAYERS, D_MODEL, KV_HEADS, HEAD_DIM), D_MODEL ** -0.5),
        'w_o': draw_normal(weight_keys[3], (LAYERS, NUM_HEADS, HEAD_DIM, D_MODEL), out_scale),
        'w_gate': draw_normal(weight_keys[4], (LAYERS, D_MODEL, FF_DIM), D_MODEL ** -0.5),
        'w_up': draw_normal(weight_keys[5], (LAYERS, D_MODEL, FF_DIM), D_MODEL ** -0.5),
        'w_down': draw_normal(weight_keys[6], (LAYERS, FF_DIM, D_MODEL), 1.5 * FF_DIM ** -0.5),
        'norm_gain': gains.astype(jnp.bfloat16),
    }


def rms_norm(x_in, gain_row):
    x_f32 = x_in.astype(jnp.float32)
    inv_rms = lax.rsqrt(jnp.mean(x_f32 * x_f32, axis=-1, keepdims=True) + EPS)
    return (x_f32 * inv_rms * gain_row.astype(jnp.float32)).astype(jnp.bfloat16)


def rope_tables(positions):
    half_dim = HEAD_DIM // 2
    inv_freq = float(ROPE_BASE) ** (-(jnp.arange(half_dim, dtype=jnp.float32) * 2.0 / HEAD_DIM))
    angles = positions.astype(jnp.float32)[..., None] * inv_freq
    return jnp.cos(angles), jnp.sin(angles)


def apply_rope(heads_in, cos_t, sin_t):
    half_dim = heads_in.shape[-1] // 2
    heads_f32 = heads_in.astype(jnp.float32)
    first_half = heads_f32[..., :half_dim]
    second_half = heads_f32[..., half_dim:]
    cos_b = cos_t[..., None, :]
    sin_b = sin_t[..., None, :]
    rotated = jnp.concatenate([first_half * cos_b - second_half * sin_b, second_half * cos_b + first_half * sin_b], axis=-1)
    return rotated.astype(jnp.bfloat16)


def causal_attention(q_rot, k_rot, v_heads):
    group_size = NUM_HEADS // KV_HEADS
    logit_scale = 1.0 / math.sqrt(HEAD_DIM)
    num_blocks = SEQ_LEN // QUERY_BLOCK
    q_blocks = q_rot.reshape(num_blocks, QUERY_BLOCK, KV_HEADS, group_size, HEAD_DIM).astype(jnp.float32)
    k_f32 = k_rot.astype(jnp.float32)
    v_f32 = v_heads.astype(jnp.float32)
    key_index = jnp.arange(SEQ_LEN)

    def one_block(block_args):
        block_id, q_blk = block_args
        logits = jnp.einsum('qkgd,skd->qkgs', q_blk, k_f32) * logit_scale
        query_index = block_id * QUERY_BLOCK + jnp.arange(QUERY_BLOCK)
        allowed = (query_index[:, None] >= key_index[None, :])[:, None, None, :]
        logits = jnp.where(allowed, logits, -jnp.inf)
        row_max = jnp.max(logits, axis=-1, keepdims=True)
        prob_f32 = jnp.exp(logits - row_max)
        row_sum = jnp.sum(prob_f32, axis=-1, keepdims=True)
        prob_low = prob_f32.astype(jnp.bfloat16).astype(jnp.float32)
        return jnp.einsum('qkgs,skd->qkgd', prob_low, v_f32) / row_sum

    block_out = lax.map(one_block, (jnp.arange(num_blocks), q_blocks))
    return block_out.reshape(SEQ_LEN, NUM_HEADS * HEAD_DIM).astype(jnp.bfloat16)


def reference(x_embed, positions, w_q, w_k, w_v, w_o, w_gate, w_up, w_down, norm_gain):
    cos_t, sin_t = rope_tables(positions)

    def layer_step(x_cur, layer_weights):
        wq_l, wk_l, wv_l, wo_l, wg_l, wu_l, wd_l, gain_row = layer_weights
        normed = rms_norm(x_cur, gain_row)
        q_proj = jnp.dot(normed, wq_l.reshape(D_MODEL, NUM_HEADS * HEAD_DIM), preferred_element_type=jnp.float32).astype(jnp.bfloat16)
        k_proj = jnp.dot(normed, wk_l.reshape(D_MODEL, KV_HEADS * HEAD_DIM), preferred_element_type=jnp.float32).astype(jnp.bfloat16)
        v_proj = jnp.dot(normed, wv_l.reshape(D_MODEL, KV_HEADS * HEAD_DIM), preferred_element_type=jnp.float32).astype(jnp.bfloat16)
        q_rot = apply_rope(q_proj.reshape(SEQ_LEN, NUM_HEADS, HEAD_DIM), cos_t, sin_t)
        k_rot = apply_rope(k_proj.reshape(SEQ_LEN, KV_HEADS, HEAD_DIM), cos_t, sin_t)
        v_heads = v_proj.reshape(SEQ_LEN, KV_HEADS, HEAD_DIM)
        attn_heads = causal_attention(q_rot, k_rot, v_heads)
        attn_part = jnp.dot(attn_heads, wo_l.reshape(NUM_HEADS * HEAD_DIM, D_MODEL), preferred_element_type=jnp.float32)
        gate_f32 = jnp.dot(normed, wg_l, preferred_element_type=jnp.float32)
        up_f32 = jnp.dot(normed, wu_l, preferred_element_type=jnp.float32)
        hidden = (jax.nn.silu(gate_f32) * up_f32).astype(jnp.bfloat16)
        mlp_part = jnp.dot(hidden, wd_l, preferred_element_type=jnp.float32)
        update = (attn_part + mlp_part).astype(jnp.bfloat16)
        x_next = (x_cur.astype(jnp.float32) + update.astype(jnp.float32)).astype(jnp.bfloat16)
        return x_next, (k_rot, v_heads)

    stacked = (w_q, w_k, w_v, w_o, w_gate, w_up, w_down, norm_gain)
    x_out, caches = lax.scan(layer_step, x_embed, stacked)
    return x_out, caches[0], caches[1]
```

```python
import math
import jax
import jax.numpy as jnp
from jax import lax
from jax.sharding import PartitionSpec as P

ROPE_BASE = 500000.0
EPS = 1e-5


def rms_norm(x_in, gain_row):
    x_f32 = x_in.astype(jnp.float32)
    inv_rms = lax.rsqrt(jnp.mean(x_f32 * x_f32, axis=-1, keepdims=True) + EPS)
    return (x_f32 * inv_rms * gain_row.astype(jnp.float32)).astype(jnp.bfloat16)


def rope_tables(positions, head_dim):
    half_dim = head_dim // 2
    inv_freq = ROPE_BASE ** (-(jnp.arange(half_dim, dtype=jnp.float32) * 2.0 / head_dim))
    angles = positions.astype(jnp.float32)[..., None] * inv_freq
    return jnp.cos(angles), jnp.sin(angles)


def apply_rope(heads_in, cos_t, sin_t):
    half_dim = heads_in.shape[-1] // 2
    heads_f32 = heads_in.astype(jnp.float32)
    first_half = heads_f32[..., :half_dim]
    second_half = heads_f32[..., half_dim:]
    cos_b = cos_t[..., None, :]
    sin_b = sin_t[..., None, :]
    rotated = jnp.concatenate([first_half * cos_b - second_half * sin_b, second_half * cos_b + first_half * sin_b], axis=-1)
    return rotated.astype(jnp.bfloat16)


def block_update(soft_state, q_rot, k_blk, v_blk, row_index, col_index, logit_scale):
    row_max, row_sum, accum_out = soft_state
    logits = jnp.einsum('qkgd,skd->qkgs', q_rot, k_blk, preferred_element_type=jnp.float32) * logit_scale
    allowed = (row_index[:, None] >= col_index[None, :])[:, None, None, :]
    logits = jnp.where(allowed, logits, -jnp.inf)
    new_max = jnp.maximum(row_max, jnp.max(logits, axis=-1))
    prob_f32 = jnp.exp(logits - new_max[..., None])
    rescale = jnp.exp(row_max - new_max)
    row_sum = row_sum * rescale + jnp.sum(prob_f32, axis=-1)
    pv_part = jnp.einsum('qkgs,skd->qkgd', prob_f32.astype(jnp.bfloat16), v_blk, preferred_element_type=jnp.float32)
    accum_out = accum_out * rescale[..., None] + pv_part
    return new_max, row_sum, accum_out


def passed_attention(q_rot, k_rot, v_heads, seq_count):
    tok_count, kv_local, group_size, head_dim = q_rot.shape
    my_index = lax.axis_index('seq')
    logit_scale = 1.0 / math.sqrt(head_dim)
    local_index = jnp.arange(tok_count)
    row_index = my_index * tok_count + local_index
    shift_pairs = [(sender, (sender + 1) % seq_count) for sender in range(seq_count)]
    stat_shape = (tok_count, kv_local, group_size)
    init_state = (jnp.full(stat_shape, -jnp.inf, jnp.float32), jnp.zeros(stat_shape, jnp.float32), jnp.zeros(stat_shape + (head_dim,), jnp.float32))
    first_state = block_update(init_state, q_rot, k_rot, v_heads, row_index, row_index, logit_scale)

    def pass_step(step_num, loop_carry):
        k_blk, v_blk, state_in = loop_carry
        k_blk = lax.ppermute(k_blk, 'seq', shift_pairs)
        v_blk = lax.ppermute(v_blk, 'seq', shift_pairs)
        src_index = (my_index - step_num) % seq_count
        col_index = src_index * tok_count + local_index
        return k_blk, v_blk, block_update(state_in, q_rot, k_blk, v_blk, row_index, col_index, logit_scale)

    final_carry = lax.fori_loop(1, seq_count, pass_step, (k_rot, v_heads, first_state))
    row_max, row_sum, accum_out = final_carry[2]
    attn_heads = (accum_out / row_sum[..., None]).astype(jnp.bfloat16)
    return attn_heads.reshape(tok_count, kv_local * group_size * head_dim)


def solution(mesh):
    seq_count = mesh.shape['seq']
    row_spec = P(('batch', 'seq'), None)
    pos_spec = P(('batch', 'seq'))
    head_spec = P(None, None, 'head', None)
    out_proj_spec = P(None, 'head', None, None)
    col_spec = P(None, None, 'head')
    down_spec = P(None, 'head', None)
    cache_spec = P(None, ('batch', 'seq'), 'head', None)

    def local_forward(x_loc, pos_loc, w_q, w_k, w_v, w_o, w_gate, w_up, w_down, norm_gain):
        tok_count, d_model = x_loc.shape
        layer_count = w_q.shape[0]
        q_local = w_q.shape[2]
        head_dim = w_q.shape[3]
        kv_local = w_k.shape[2]
        group_size = q_local // kv_local
        cos_t, sin_t = rope_tables(pos_loc, head_dim)
        x_cur = x_loc
        k_list = []
        v_list = []
        for layer in range(layer_count):
            normed = rms_norm(x_cur, norm_gain[layer])
            q_proj = jnp.dot(normed, w_q[layer].reshape(d_model, q_local * head_dim), preferred_element_type=jnp.float32).astype(jnp.bfloat16)
            k_proj = jnp.dot(normed, w_k[layer].reshape(d_model, kv_local * head_dim), preferred_element_type=jnp.float32).astype(jnp.bfloat16)
            v_proj = jnp.dot(normed, w_v[layer].reshape(d_model, kv_local * head_dim), preferred_element_type=jnp.float32).astype(jnp.bfloat16)
            q_rot = apply_rope(q_proj.reshape(tok_count, q_local, head_dim), cos_t, sin_t).reshape(tok_count, kv_local, group_size, head_dim)
            k_rot = apply_rope(k_proj.reshape(tok_count, kv_local, head_dim), cos_t, sin_t)
            v_heads = v_proj.reshape(tok_count, kv_local, head_dim)
            attn_heads = passed_attention(q_rot, k_rot, v_heads, seq_count)
            part_sum = jnp.dot(attn_heads, w_o[layer].reshape(q_local * head_dim, d_model), preferred_element_type=jnp.float32)
            gate_f32 = jnp.dot(normed, w_gate[layer], preferred_element_type=jnp.float32)
            up_f32 = jnp.dot(normed, w_up[layer], preferred_element_type=jnp.float32)
            hidden = (jax.nn.silu(gate_f32) * up_f32).astype(jnp.bfloat16)
            part_sum = part_sum + jnp.dot(hidden, w_down[layer], preferred_element_type=jnp.float32)
            head_count = lax.axis_size('head')
            own_rows = tok_count // head_count
            update = lax.psum_scatter(part_sum, 'head', scatter_dimension=0, tiled=True).astype(jnp.bfloat16)
            x_own = lax.dynamic_slice_in_dim(x_cur, lax.axis_index('head') * own_rows, own_rows, axis=0)
            x_own = (x_own.astype(jnp.float32) + update.astype(jnp.float32)).astype(jnp.bfloat16)
            x_cur = lax.all_gather(x_own, 'head', axis=0, tiled=True)
            k_list.append(k_rot)
            v_list.append(v_heads)
        return x_cur, jnp.stack(k_list), jnp.stack(v_list)

    return jax.shard_map(local_forward, mesh=mesh, in_specs=(row_spec, pos_spec, head_spec, head_spec, head_spec, out_proj_spec, col_spec, col_spec, down_spec, P(None, None)), out_specs=(row_spec, cache_spec, cache_spec), check_vma=False)
```

```python
import functools
import math
import jax
import jax.numpy as jnp
from jax import lax
from jax.experimental import pallas as pl
from jax.experimental.pallas import tpu as pltpu
from jax.sharding import PartitionSpec as P

ROPE_BASE = 500000.0
EPS = 1e-5


def rms_norm(x_in, gain_row):
    x_f32 = x_in.astype(jnp.float32)
    inv_rms = lax.rsqrt(jnp.mean(x_f32 * x_f32, axis=-1, keepdims=True) + EPS)
    return (x_f32 * inv_rms * gain_row.astype(jnp.float32)).astype(jnp.bfloat16)


def rope_tables(positions, head_dim):
    half_dim = head_dim // 2
    inv_freq = ROPE_BASE ** (-(jnp.arange(half_dim, dtype=jnp.float32) * 2.0 / head_dim))
    angles = positions.astype(jnp.float32)[..., None] * inv_freq
    return jnp.cos(angles), jnp.sin(angles)


def apply_rope(heads_in, cos_t, sin_t):
    half_dim = heads_in.shape[-1] // 2
    heads_f32 = heads_in.astype(jnp.float32)
    first_half = heads_f32[..., :half_dim]
    second_half = heads_f32[..., half_dim:]
    cos_b = cos_t[..., None, :]
    sin_b = sin_t[..., None, :]
    rotated = jnp.concatenate([first_half * cos_b - second_half * sin_b, second_half * cos_b + first_half * sin_b], axis=-1)
    return rotated.astype(jnp.bfloat16)


LOG2E = 1.4426950408889634
KEY_BLOCK = 1024
ROW_BLOCK = 256


def flash_kernel(seq_tokens, q_ref, kv_ref, out_ref):
    rows, head_dim = q_ref.shape
    my_seq = lax.axis_index('seq')
    row_block = pl.program_id(0)
    scale = LOG2E / math.sqrt(head_dim)
    q_val = q_ref[...]

    def visit(state, key_start, key_count, masked):
        row_max, row_sum, accum = state
        keys = kv_ref[pl.ds(key_start, key_count), :head_dim]
        vals = kv_ref[pl.ds(key_start, key_count), head_dim:]
        logits = lax.dot_general(q_val, keys, (((1,), (1,)), ((), ())), preferred_element_type=jnp.float32) * scale
        if masked:
            row_iota = lax.broadcasted_iota(jnp.int32, logits.shape, 0)
            col_iota = lax.broadcasted_iota(jnp.int32, logits.shape, 1)
            logits = jnp.where(row_iota >= col_iota, logits, -jnp.inf)
        new_max = jnp.maximum(row_max, jnp.max(logits, axis=-1, keepdims=True))
        prob = jnp.exp2(logits - new_max)
        rescale = jnp.exp2(row_max - new_max)
        row_sum = row_sum * rescale + jnp.sum(prob, axis=-1, keepdims=True)
        accum = accum * rescale + jnp.dot(prob.astype(jnp.bfloat16), vals, preferred_element_type=jnp.float32)
        return new_max, row_sum, accum

    own_start = my_seq * seq_tokens
    state = (jnp.full((rows, 1), -jnp.inf, jnp.float32), jnp.zeros((rows, 1), jnp.float32), jnp.zeros((rows, head_dim), jnp.float32))
    diag_start = pl.multiple_of(own_start + row_block * rows, rows)
    state = visit(state, diag_start, rows, True)
    state = lax.fori_loop(0, row_block, lambda i, st: visit(st, pl.multiple_of(own_start + i * rows, rows), rows, False), state)
    past_blocks = own_start // KEY_BLOCK
    state = lax.fori_loop(0, past_blocks, lambda i, st: visit(st, pl.multiple_of(i * KEY_BLOCK, KEY_BLOCK), KEY_BLOCK, False), state)
    out_ref[...] = (state[2] / state[1]).astype(jnp.bfloat16)


def flash_attention(q_rot, kv_full):
    tok_count, head_dim = q_rot.shape
    return pl.pallas_call(
        functools.partial(flash_kernel, tok_count),
        out_shape=jax.ShapeDtypeStruct((tok_count, head_dim), jnp.bfloat16),
        grid=(tok_count // ROW_BLOCK,),
        in_specs=[pl.BlockSpec((ROW_BLOCK, head_dim), lambda i: (i, 0)), pl.BlockSpec(kv_full.shape, lambda i: (0, 0))],
        out_specs=pl.BlockSpec((ROW_BLOCK, head_dim), lambda i: (i, 0)),
        compiler_params=pltpu.CompilerParams(dimension_semantics=('arbitrary',), vmem_limit_bytes=48 * 1024 * 1024),
        cost_estimate=pl.CostEstimate(flops=4 * tok_count * kv_full.shape[0] * head_dim, bytes_accessed=kv_full.size * 2, transcendentals=tok_count * kv_full.shape[0]),
        name='flash',
    )(q_rot, kv_full)


def solution(mesh):
    row_spec = P(('batch', 'seq'), None)
    pos_spec = P(('batch', 'seq'))
    head_spec = P(None, None, 'head', None)
    out_proj_spec = P(None, 'head', None, None)
    col_spec = P(None, None, 'head')
    down_spec = P(None, 'head', None)
    cache_spec = P(None, ('batch', 'seq'), 'head', None)

    def local_forward(x_loc, pos_loc, w_q, w_k, w_v, w_o, w_gate, w_up, w_down, norm_gain):
        tok_count, d_model = x_loc.shape
        layer_count = w_q.shape[0]
        q_local = w_q.shape[2]
        head_dim = w_q.shape[3]
        kv_local = w_k.shape[2]
        cos_t, sin_t = rope_tables(pos_loc, head_dim)
        x_cur = x_loc
        k_list = []
        v_list = []
        for layer in range(layer_count):
            normed = rms_norm(x_cur, norm_gain[layer])
            q_proj = jnp.dot(normed, w_q[layer].reshape(d_model, q_local * head_dim), preferred_element_type=jnp.float32).astype(jnp.bfloat16)
            k_proj = jnp.dot(normed, w_k[layer].reshape(d_model, kv_local * head_dim), preferred_element_type=jnp.float32).astype(jnp.bfloat16)
            v_proj = jnp.dot(normed, w_v[layer].reshape(d_model, kv_local * head_dim), preferred_element_type=jnp.float32).astype(jnp.bfloat16)
            q_rot = apply_rope(q_proj.reshape(tok_count, q_local, head_dim), cos_t, sin_t)
            k_rot = apply_rope(k_proj.reshape(tok_count, kv_local, head_dim), cos_t, sin_t)
            v_heads = v_proj.reshape(tok_count, kv_local, head_dim)
            kv_own = jnp.concatenate([k_rot.reshape(tok_count, head_dim), v_proj], axis=1)
            kv_full = lax.all_gather(kv_own, 'seq', axis=0, tiled=True)
            attn_heads = flash_attention(q_rot.reshape(tok_count, head_dim), kv_full)
            gate_f32 = jnp.dot(normed, w_gate[layer], preferred_element_type=jnp.float32)
            up_f32 = jnp.dot(normed, w_up[layer], preferred_element_type=jnp.float32)
            hidden = (jax.nn.silu(gate_f32) * up_f32).astype(jnp.bfloat16)
            part_sum = jnp.dot(hidden, w_down[layer], preferred_element_type=jnp.float32)
            part_sum = part_sum + jnp.dot(attn_heads, w_o[layer].reshape(q_local * head_dim, d_model), preferred_element_type=jnp.float32)
            head_count = lax.axis_size('head')
            own_rows = tok_count // head_count
            update = lax.psum_scatter(part_sum, 'head', scatter_dimension=0, tiled=True).astype(jnp.bfloat16)
            x_own = lax.dynamic_slice_in_dim(x_cur, lax.axis_index('head') * own_rows, own_rows, axis=0)
            x_own = (x_own.astype(jnp.float32) + update.astype(jnp.float32)).astype(jnp.bfloat16)
            x_cur = lax.all_gather(x_own, 'head', axis=0, tiled=True)
            k_list.append(k_rot)
            v_list.append(v_heads)
        return x_cur, jnp.stack(k_list), jnp.stack(v_list)

    return jax.shard_map(local_forward, mesh=mesh, in_specs=(row_spec, pos_spec, head_spec, head_spec, head_spec, out_proj_spec, col_spec, col_spec, down_spec, P(None, None)), out_specs=(row_spec, cache_spec, cache_spec), check_vma=False)
```

```python
import functools
import math
import jax
import jax.numpy as jnp
from jax import lax
from jax.experimental import pallas as pl
from jax.experimental.pallas import tpu as pltpu
from jax.sharding import PartitionSpec as P

ROPE_BASE = 500000.0
EPS = 1e-5


def rms_norm(x_in, gain_row):
    x_f32 = x_in.astype(jnp.float32)
    inv_rms = lax.rsqrt(jnp.mean(x_f32 * x_f32, axis=-1, keepdims=True) + EPS)
    return (x_f32 * inv_rms * gain_row.astype(jnp.float32)).astype(jnp.bfloat16)


def rope_tables(positions, head_dim):
    half_dim = head_dim // 2
    inv_freq = ROPE_BASE ** (-(jnp.arange(half_dim, dtype=jnp.float32) * 2.0 / head_dim))
    angles = positions.astype(jnp.float32)[..., None] * inv_freq
    return jnp.cos(angles), jnp.sin(angles)


def apply_rope(heads_in, cos_t, sin_t):
    half_dim = heads_in.shape[-1] // 2
    heads_f32 = heads_in.astype(jnp.float32)
    first_half = heads_f32[..., :half_dim]
    second_half = heads_f32[..., half_dim:]
    cos_b = cos_t[..., None, :]
    sin_b = sin_t[..., None, :]
    rotated = jnp.concatenate([first_half * cos_b - second_half * sin_b, second_half * cos_b + first_half * sin_b], axis=-1)
    return rotated.astype(jnp.bfloat16)


LOG2E = 1.4426950408889634
KEY_BLOCK = 1024
ROW_BLOCK = 256
CHUNK_ROWS = 128


def flash_kernel(seq_tokens, q_ref, kv_ref, out_ref):
    rows, head_dim = q_ref.shape
    my_seq = lax.axis_index('seq')
    row_block = pl.program_id(0)
    scale = LOG2E / math.sqrt(head_dim)
    q_val = q_ref[...]

    def visit(state, key_start, key_count, masked):
        row_max, row_sum, accum = state
        keys = kv_ref[pl.ds(key_start, key_count), :head_dim]
        vals = kv_ref[pl.ds(key_start, key_count), head_dim:]
        logits = lax.dot_general(q_val, keys, (((1,), (1,)), ((), ())), preferred_element_type=jnp.float32) * scale
        if masked:
            row_iota = lax.broadcasted_iota(jnp.int32, logits.shape, 0)
            col_iota = lax.broadcasted_iota(jnp.int32, logits.shape, 1)
            logits = jnp.where(row_iota >= col_iota, logits, -jnp.inf)
        new_max = jnp.maximum(row_max, jnp.max(logits, axis=-1, keepdims=True))
        prob = jnp.exp2(logits - new_max)
        rescale = jnp.exp2(row_max - new_max)
        row_sum = row_sum * rescale + jnp.sum(prob, axis=-1, keepdims=True)
        accum = accum * rescale + jnp.dot(prob.astype(jnp.bfloat16), vals, preferred_element_type=jnp.float32)
        return new_max, row_sum, accum

    own_start = my_seq * seq_tokens
    state = (jnp.full((rows, 1), -jnp.inf, jnp.float32), jnp.zeros((rows, 1), jnp.float32), jnp.zeros((rows, head_dim), jnp.float32))
    diag_start = pl.multiple_of(own_start + row_block * rows, rows)
    state = visit(state, diag_start, rows, True)
    state = lax.fori_loop(0, row_block, lambda i, st: visit(st, pl.multiple_of(own_start + i * rows, rows), rows, False), state)
    past_blocks = own_start // KEY_BLOCK
    state = lax.fori_loop(0, past_blocks, lambda i, st: visit(st, pl.multiple_of(i * KEY_BLOCK, KEY_BLOCK), KEY_BLOCK, False), state)
    out_ref[...] = (state[2] / state[1]).astype(jnp.bfloat16)


def flash_attention(q_rot, kv_full):
    tok_count, head_dim = q_rot.shape
    return pl.pallas_call(
        functools.partial(flash_kernel, tok_count),
        out_shape=jax.ShapeDtypeStruct((tok_count, head_dim), jnp.bfloat16),
        grid=(tok_count // ROW_BLOCK,),
        in_specs=[pl.BlockSpec((ROW_BLOCK, head_dim), lambda i: (i, 0)), pl.BlockSpec(kv_full.shape, lambda i: (0, 0))],
        out_specs=pl.BlockSpec((ROW_BLOCK, head_dim), lambda i: (i, 0)),
        compiler_params=pltpu.CompilerParams(dimension_semantics=('arbitrary',), vmem_limit_bytes=48 * 1024 * 1024),
        cost_estimate=pl.CostEstimate(flops=4 * tok_count * kv_full.shape[0] * head_dim, bytes_accessed=kv_full.size * 2, transcendentals=tok_count * kv_full.shape[0]),
        name='flash',
    )(q_rot, kv_full)


RING = 4
HALVES = 2
DIRS = 2
STEPS = 8


def tail_kernel(layer, chunk_rows, hid_ref, att_ref, x_ref, wd_ref, wo_ref, out_ref, part, xbuf, wbuf, recv_a, recv_b, load_sem, store_sem, send_sem, recv_sem):
    tok_count, d_model = xbuf.shape
    ff_local = hid_ref.shape[1]
    chunk_count = tok_count // chunk_rows
    quarter, eighth = chunk_rows // RING, chunk_rows // (2 * RING)
    half_cols = d_model // HALVES
    piece_cols = half_cols // RING
    my_head = lax.axis_index('head')
    pos_z, pos_y = my_head // RING, my_head % RING
    sign = (1, -1)

    def y_peer(d):
        return pos_z * RING + (pos_y + sign[d] + RING) % RING

    def z_peer(d):
        return ((pos_z + sign[d] + RING) % RING) * RING + pos_y

    first_pos, second_pos = (pos_y, pos_z), (pos_z, pos_y)
    first_peer, second_peer = (y_peer, z_peer), (z_peer, y_peer)

    loads = [
        pltpu.make_async_copy(wd_ref.at[layer], wbuf.at[pl.ds(0, ff_local), :], load_sem.at[0]),
        pltpu.make_async_copy(wo_ref.at[layer, 0], wbuf.at[pl.ds(ff_local, wo_ref.shape[2]), :], load_sem.at[1]),
        pltpu.make_async_copy(x_ref, xbuf, load_sem.at[2]),
    ]
    for load in loads:
        load.start()
    barrier = pltpu.get_barrier_semaphore()
    for peer in (y_peer, z_peer):
        for d in range(DIRS):
            pl.semaphore_signal(barrier, inc=1, device_id={'head': peer(d)}, device_id_type=pl.DeviceIdType.MESH)
    pl.semaphore_wait(barrier, 2 * DIRS)
    for load in loads:
        load.wait()

    def rows_of(chunk, piece, offset, count):
        return pl.ds(pl.multiple_of(chunk * chunk_rows + piece * quarter + offset, eighth), count)

    def cols_of(h, piece):
        return pl.ds(pl.multiple_of(h * half_cols + piece * piece_cols, piece_cols), piece_cols)

    def half_of(h):
        return pl.ds(h * half_cols, half_cols)

    def message(step, chunk, h, d):
        p1, p2, s = first_pos[h], second_pos[h], sign[d]
        far1, near1, behind1 = (p1 + 2) % RING, (p1 + s + RING) % RING, (p1 - s + RING) % RING
        far2, near2, behind2 = (p2 + 2) % RING, (p2 + s + RING) % RING, (p2 - s + RING) % RING
        if step == 0:
            src, dst = part.at[rows_of(chunk, far1, d * eighth, eighth), half_of(h)], recv_a.at[chunk, h, d, pl.ds(quarter, eighth), :]
        elif step == 1:
            src, dst = part.at[rows_of(chunk, near1, 0, quarter), half_of(h)], recv_a.at[chunk, h, d, pl.ds(0, quarter), :]
        elif step == 2:
            src, dst = part.at[rows_of(chunk, p1, d * eighth, eighth), cols_of(h, far2)], recv_b.at[chunk, h, d, pl.ds(quarter, eighth), :]
        elif step == 3:
            src, dst = part.at[rows_of(chunk, p1, 0, quarter), cols_of(h, near2)], recv_b.at[chunk, h, d, pl.ds(0, quarter), :]
        elif step == 4:
            src = dst = xbuf.at[rows_of(chunk, p1, 0, quarter), cols_of(h, p2)]
        elif step == 5:
            src = dst = xbuf.at[rows_of(chunk, p1, d * eighth, eighth), cols_of(h, behind2)]
        elif step == 6:
            src = dst = xbuf.at[rows_of(chunk, p1, 0, quarter), half_of(h)]
        else:
            src = dst = xbuf.at[rows_of(chunk, behind1, d * eighth, eighth), half_of(h)]
        peer = (first_peer if step in (0, 1, 6, 7) else second_peer)[h](d)
        return pltpu.make_async_remote_copy(
            src_ref=src, dst_ref=dst, send_sem=send_sem.at[chunk, step, h * DIRS + d], recv_sem=recv_sem.at[chunk, step, h * DIRS + d],
            device_id={'head': peer}, device_id_type=pl.DeviceIdType.MESH)

    def project(chunk):
        rows = pl.ds(pl.multiple_of(chunk * chunk_rows, chunk_rows), chunk_rows)

        def one_tile(i, carry):
            cols = pl.ds(pl.multiple_of(i * piece_cols, piece_cols), piece_cols)
            total = jnp.dot(hid_ref[rows, :], wbuf[:ff_local, cols], preferred_element_type=jnp.float32)
            part[rows, cols] = total + jnp.dot(att_ref[rows, :], wbuf[ff_local:, cols], preferred_element_type=jnp.float32)
            return carry

        lax.fori_loop(0, d_model // piece_cols, one_tile, 0)

    def store(chunk):
        rows = pl.ds(pl.multiple_of(chunk * chunk_rows, chunk_rows), chunk_rows)
        return pltpu.make_async_copy(xbuf.at[rows, :], out_ref.at[rows, :], store_sem.at[chunk])

    def stage(number, chunk):
        if number == 0:
            project(chunk)
        for h in range(HALVES):
            p1, p2 = first_pos[h], second_pos[h]
            if number:
                for d in range(DIRS):
                    message(number - 1, chunk, h, d).wait_recv()
            if number in (1, 3):
                for d in range(DIRS):
                    if number == 1:
                        rows, cols, arrived = rows_of(chunk, (p1 + sign[d] + RING) % RING, d * eighth, eighth), half_of(h), recv_a
                    else:
                        rows, cols, arrived = rows_of(chunk, p1, d * eighth, eighth), cols_of(h, (p2 + sign[d] + RING) % RING), recv_b
                    part[rows, cols] = part[rows, cols] + arrived[chunk, h, d, pl.ds(quarter, eighth), :]
            if number == 2:
                rows = rows_of(chunk, p1, 0, quarter)
                part[rows, half_of(h)] = part[rows, half_of(h)] + recv_a[chunk, h, 0, pl.ds(0, quarter), :] + recv_a[chunk, h, 1, pl.ds(0, quarter), :]
            if number == 4:
                rows, cols = rows_of(chunk, p1, 0, quarter), cols_of(h, p2)
                total = part[rows, cols] + recv_b[chunk, h, 0, pl.ds(0, quarter), :] + recv_b[chunk, h, 1, pl.ds(0, quarter), :]
                update = total.astype(jnp.bfloat16).astype(jnp.float32)
                xbuf[rows, cols] = (xbuf[rows, cols].astype(jnp.float32) + update).astype(jnp.bfloat16)
            if number < STEPS:
                for d in range(DIRS):
                    message(number, chunk, h, d).start()
        if number == STEPS:
            store(chunk).start()

    def tick(t, carry):
        for number in range(STEPS, -1, -1):
            chunk = t - number

            @pl.when(jnp.logical_and(chunk >= 0, chunk < chunk_count))
            def _():
                stage(number, chunk)
        return carry

    lax.fori_loop(0, chunk_count + STEPS, tick, 0)

    def drain(chunk, carry):
        for step in range(STEPS):
            for h in range(HALVES):
                for d in range(DIRS):
                    message(step, chunk, h, d).wait_send()
        store(chunk).wait()
        return carry

    lax.fori_loop(0, chunk_count, drain, 0)


def layer_tail(layer, hidden, attn_heads, x_cur, w_down, w_o):
    tok_count, d_model = x_cur.shape
    chunk_rows = min(CHUNK_ROWS, tok_count)
    chunk_count = tok_count // chunk_rows
    depth = hidden.shape[1] + attn_heads.shape[1]
    landed = 3 * chunk_rows // (2 * RING)
    any_spec = pl.BlockSpec(memory_space=pl.ANY)
    vmem_spec = pl.BlockSpec(memory_space=pltpu.VMEM)
    return pl.pallas_call(
        functools.partial(tail_kernel, layer, chunk_rows),
        out_shape=jax.ShapeDtypeStruct((tok_count, d_model), jnp.bfloat16),
        in_specs=[vmem_spec, vmem_spec, any_spec, any_spec, any_spec],
        out_specs=any_spec,
        scratch_shapes=[
            pltpu.VMEM((tok_count, d_model), jnp.float32),
            pltpu.VMEM((tok_count, d_model), jnp.bfloat16),
            pltpu.VMEM((depth, d_model), jnp.bfloat16),
            pltpu.VMEM((chunk_count, HALVES, DIRS, landed, d_model // HALVES), jnp.float32),
            pltpu.VMEM((chunk_count, HALVES, DIRS, landed, d_model // HALVES // RING), jnp.float32),
            pltpu.SemaphoreType.DMA((3,)),
            pltpu.SemaphoreType.DMA((chunk_count,)),
            pltpu.SemaphoreType.DMA((chunk_count, STEPS, HALVES * DIRS)),
            pltpu.SemaphoreType.DMA((chunk_count, STEPS, HALVES * DIRS)),
        ],
        compiler_params=pltpu.CompilerParams(collective_id=layer, has_side_effects=True, vmem_limit_bytes=63 * 1024 * 1024),
        cost_estimate=pl.CostEstimate(flops=2 * tok_count * depth * d_model, bytes_accessed=depth * d_model * 2, transcendentals=0),
        name='tail',
    )(hidden, attn_heads, x_cur, w_down, w_o)


def solution(mesh):
    row_spec = P(('batch', 'seq'), None)
    pos_spec = P(('batch', 'seq'))
    head_spec = P(None, None, 'head', None)
    out_proj_spec = P(None, 'head', None, None)
    col_spec = P(None, None, 'head')
    down_spec = P(None, 'head', None)
    cache_spec = P(None, ('batch', 'seq'), 'head', None)

    def local_forward(x_loc, pos_loc, w_q, w_k, w_v, w_o, w_gate, w_up, w_down, norm_gain):
        tok_count, d_model = x_loc.shape
        layer_count = w_q.shape[0]
        q_local = w_q.shape[2]
        head_dim = w_q.shape[3]
        kv_local = w_k.shape[2]
        cos_t, sin_t = rope_tables(pos_loc, head_dim)
        x_cur = x_loc
        k_list = []
        v_list = []
        for layer in range(layer_count):
            normed = rms_norm(x_cur, norm_gain[layer])
            q_proj = jnp.dot(normed, w_q[layer].reshape(d_model, q_local * head_dim), preferred_element_type=jnp.float32).astype(jnp.bfloat16)
            k_proj = jnp.dot(normed, w_k[layer].reshape(d_model, kv_local * head_dim), preferred_element_type=jnp.float32).astype(jnp.bfloat16)
            v_proj = jnp.dot(normed, w_v[layer].reshape(d_model, kv_local * head_dim), preferred_element_type=jnp.float32).astype(jnp.bfloat16)
            q_rot = apply_rope(q_proj.reshape(tok_count, q_local, head_dim), cos_t, sin_t)
            k_rot = apply_rope(k_proj.reshape(tok_count, kv_local, head_dim), cos_t, sin_t)
            v_heads = v_proj.reshape(tok_count, kv_local, head_dim)
            kv_own = jnp.concatenate([k_rot.reshape(tok_count, head_dim), v_proj], axis=1)
            kv_full = lax.all_gather(kv_own, 'seq', axis=0, tiled=True)
            attn_heads = flash_attention(q_rot.reshape(tok_count, head_dim), kv_full)
            gate_f32 = jnp.dot(normed, w_gate[layer], preferred_element_type=jnp.float32)
            up_f32 = jnp.dot(normed, w_up[layer], preferred_element_type=jnp.float32)
            hidden = (jax.nn.silu(gate_f32) * up_f32).astype(jnp.bfloat16)
            x_cur = layer_tail(layer, hidden, attn_heads, x_cur, w_down, w_o)
            k_list.append(k_rot)
            v_list.append(v_heads)
        return x_cur, jnp.stack(k_list), jnp.stack(v_list)

    return jax.shard_map(local_forward, mesh=mesh, in_specs=(row_spec, pos_spec, head_spec, head_spec, head_spec, out_proj_spec, col_spec, col_spec, down_spec, P(None, None)), out_specs=(row_spec, cache_spec, cache_spec), check_vma=False)
```

```python
import functools
import math
import jax
import jax.numpy as jnp
from jax import lax
from jax.experimental import pallas as pl
from jax.experimental.pallas import tpu as pltpu
from jax.sharding import PartitionSpec as P

ROPE_BASE = 500000.0
EPS = 1e-5


def rope_tables(positions, head_dim):
    half_dim = head_dim // 2
    inv_freq = ROPE_BASE ** (-(jnp.arange(half_dim, dtype=jnp.float32) * 2.0 / head_dim))
    angles = positions.astype(jnp.float32)[..., None] * inv_freq
    return jnp.cos(angles), jnp.sin(angles)


LOG2E = 1.4426950408889634
CHUNK_ROWS = 128


CHIPS = 4
KV_CHUNKS = 4
W_TILE = 256
NORM_ROWS = 64


def head_kernel(layer, x_ref, cos_ref, sin_ref, gain_ref, wq_ref, wk_ref, wv_ref, wg_ref, wu_ref, hid_ref, att_ref, k_ref, v_ref,
                hbuf, xs, wqkv, wtile, kv, qbuf, acc, row_max, row_sum, x_sem, w_sem, t_sem, out_sem, own_send, pass_send, ici_recv, core_recv):
    tok_count, d_model = hbuf.shape
    head_dim = qbuf.shape[1]
    half_dim = head_dim // 2
    rows_per = tok_count // KV_CHUNKS
    half_rows = tok_count // 2
    my_seq = lax.axis_index('seq')
    chip, core = my_seq // 2, my_seq % 2
    other = chip * 2 + 1 - core
    right = ((chip + 1) % CHIPS) * 2 + core
    left = ((chip + CHIPS - 1) % CHIPS) * 2 + core

    def x_load(i):
        return pltpu.make_async_copy(x_ref.at[pl.ds(pl.multiple_of(i * rows_per, rows_per), rows_per), :], xs.at[i % 2], x_sem.at[i % 2])

    def tile_load(i, which):
        ref = (wg_ref, wu_ref)[which]
        return pltpu.make_async_copy(ref.at[layer, :, pl.ds(pl.multiple_of(i * W_TILE, W_TILE), W_TILE)], wtile.at[i % 2, which], t_sem.at[i % 2, which])

    x_load(0).start()
    w_loads = [pltpu.make_async_copy(ref.at[layer], wqkv.at[n], w_sem.at[n]) for n, ref in enumerate((wk_ref, wv_ref, wq_ref))]
    for load in w_loads:
        load.start()
    x_load(1).start()
    for which in range(2):
        tile_load(0, which).start()

    barrier = pltpu.get_barrier_semaphore()
    for peer in (left, right, other):
        pl.semaphore_signal(barrier, inc=1, device_id={'seq': peer}, device_id_type=pl.DeviceIdType.MESH)
    pl.semaphore_wait(barrier, 3)

    def kv_copy(origin_chip, origin_core, i, to, send, recv):
        rows = kv.at[pl.ds(pl.multiple_of((origin_chip * 2 + origin_core) * tok_count + i * rows_per, rows_per), rows_per), :]
        return pltpu.make_async_remote_copy(src_ref=rows, dst_ref=rows, send_sem=send, recv_sem=recv, device_id={'seq': to}, device_id_type=pl.DeviceIdType.MESH)

    def to_right(i):
        return kv_copy(chip, core, i, right, own_send.at[0, i], ici_recv.at[0, i])

    def to_wrap(i):
        return kv_copy(chip, core, i, left, own_send.at[1, i], ici_recv.at[2, i])

    def to_other(i):
        return kv_copy(chip, core, i, other, own_send.at[2, i], core_recv.at[0, i])

    def on_right(i):
        return kv_copy(chip - 1, core, i, right, pass_send.at[0, i], ici_recv.at[1, i])

    def on_other(back, i):
        return kv_copy(chip - back, core, i, other, pass_send.at[back, i], core_recv.at[back, i])

    def arrival(back, i):
        return kv_copy(chip - back, core, i, other, pass_send.at[back, i], ici_recv.at[back - 1, i])

    def serve(back, i):
        @pl.when(chip >= back)
        def _():
            arrival(back, i).wait_recv()
            on_other(back, i).start()
        if back == 1:
            @pl.when(jnp.logical_and(chip >= 1, chip < CHIPS - 1))
            def _():
                on_right(i).start()

    def rope(values, rows):
        cos_t, sin_t = cos_ref[rows, :], sin_ref[rows, :]
        wide = values.astype(jnp.bfloat16).astype(jnp.float32)
        first, second = wide[:, :half_dim], wide[:, half_dim:]
        return jnp.concatenate([first * cos_t - second * sin_t, second * cos_t + first * sin_t], axis=1).astype(jnp.bfloat16)

    gain = gain_ref[pl.ds(layer, 1), :].astype(jnp.float32)

    def prepare(i, carry):
        x_load(i).wait()
        rows = pl.ds(pl.multiple_of(i * rows_per, rows_per), rows_per)

        def norm(j, inner):
            few = pl.ds(pl.multiple_of(j * NORM_ROWS, NORM_ROWS), NORM_ROWS)
            x_f32 = xs[i % 2, few, :].astype(jnp.float32)
            inv_rms = lax.rsqrt(jnp.mean(x_f32 * x_f32, axis=-1, keepdims=True) + EPS)
            hbuf[pl.ds(pl.multiple_of(i * rows_per + j * NORM_ROWS, NORM_ROWS), NORM_ROWS), :] = (x_f32 * inv_rms * gain).astype(jnp.bfloat16)
            return inner

        lax.fori_loop(0, rows_per // NORM_ROWS, norm, 0)

        @pl.when(i + 2 < KV_CHUNKS)
        def _():
            x_load(i + 2).start()

        @pl.when(i == 0)
        def _():
            w_loads[0].wait()
            w_loads[1].wait()

        normed = hbuf[rows, :]
        own = pl.ds(pl.multiple_of(my_seq * tok_count + i * rows_per, rows_per), rows_per)
        kv[own, :head_dim] = rope(jnp.dot(normed, wqkv[0], preferred_element_type=jnp.float32), rows)
        kv[own, head_dim:] = jnp.dot(normed, wqkv[1], preferred_element_type=jnp.float32).astype(jnp.bfloat16)

        @pl.when(chip < CHIPS - 1)
        def _():
            to_right(i).start()

        @pl.when(chip == 0)
        def _():
            to_wrap(i).start()

        @pl.when(core == 0)
        def _():
            to_other(i).start()
        return carry

    lax.fori_loop(0, KV_CHUNKS, prepare, 0)
    w_loads[2].wait()
    own_rows = pl.ds(pl.multiple_of(my_seq * tok_count, tok_count), tok_count)
    k_store = pltpu.make_async_copy(kv.at[own_rows, pl.ds(0, head_dim)], k_ref, out_sem.at[0])
    v_store = pltpu.make_async_copy(kv.at[own_rows, pl.ds(head_dim, head_dim)], v_ref, out_sem.at[1])
    k_store.start()
    v_store.start()

    def query(i, carry):
        rows = pl.ds(pl.multiple_of(i * rows_per, rows_per), rows_per)
        qbuf[rows, :] = rope(jnp.dot(hbuf[rows, :], wqkv[2], preferred_element_type=jnp.float32), rows)
        return carry

    lax.fori_loop(0, KV_CHUNKS, query, 0)

    def gated(i, carry):
        for which in range(2):
            tile_load(i, which).wait()

        @pl.when(i + 1 < wg_ref.shape[2] // W_TILE)
        def _():
            for which in range(2):
                tile_load(i + 1, which).start()

        def rows_step(j, inner):
            rows = pl.ds(pl.multiple_of(j * rows_per, rows_per), rows_per)
            normed = hbuf[rows, :]
            gate = jnp.dot(normed, wtile[i % 2, 0], preferred_element_type=jnp.float32)
            up = jnp.dot(normed, wtile[i % 2, 1], preferred_element_type=jnp.float32)
            hid_ref[rows, pl.ds(pl.multiple_of(i * W_TILE, W_TILE), W_TILE)] = (gate * jax.nn.sigmoid(gate) * up).astype(jnp.bfloat16)
            return inner

        lax.fori_loop(0, KV_CHUNKS, rows_step, 0)
        serve(1, i)
        serve(3, i)
        return carry

    lax.fori_loop(0, KV_CHUNKS, gated, 0)

    scale = LOG2E / math.sqrt(head_dim)
    lanes = row_max.shape[1]

    def attend(key_start, q_half, masked, first):
        rows = pl.ds(q_half * half_rows, half_rows)
        some = pl.ds(key_start, half_rows)
        logits = lax.dot_general(qbuf[rows, :], kv[some, :head_dim], (((1,), (1,)), ((), ())), preferred_element_type=jnp.float32) * scale
        if masked:
            seen = lax.broadcasted_iota(jnp.int32, logits.shape, 0) >= lax.broadcasted_iota(jnp.int32, logits.shape, 1)
            logits = jnp.where(seen, logits, -jnp.inf)
        block_max = jnp.max(logits, axis=-1, keepdims=True)
        if first:
            new_max = jnp.broadcast_to(block_max, (half_rows, lanes))
        else:
            new_max = jnp.maximum(row_max[rows, :], block_max)
        prob = jnp.exp2(logits - jnp.concatenate([new_max] * (half_rows // lanes), axis=1))
        block_sum = jnp.sum(prob, axis=-1, keepdims=True)
        block_out = jnp.dot(prob.astype(jnp.bfloat16), kv[some, head_dim:], preferred_element_type=jnp.float32)
        if first:
            row_sum[rows, :] = jnp.broadcast_to(block_sum, (half_rows, lanes))
            acc[rows, :] = block_out
        else:
            rescale = jnp.exp2(row_max[rows, :] - new_max)
            row_sum[rows, :] = row_sum[rows, :] * rescale + block_sum
            acc[rows, :] = acc[rows, :] * jnp.concatenate([rescale] * (head_dim // lanes), axis=1) + block_out
        row_max[rows, :] = new_max

    own_start = pl.multiple_of(my_seq * tok_count, tok_count)
    attend(own_start, 0, True, True)
    attend(own_start, 1, False, True)
    attend(pl.multiple_of(own_start + half_rows, half_rows), 1, True, False)

    def past(block_chip, block_core):
        def one(n, carry):
            start = pl.multiple_of((block_chip * 2 + block_core) * tok_count + n * half_rows, half_rows)
            attend(start, 0, False, False)
            attend(start, 1, False, False)
            return carry
        lax.fori_loop(0, 2, one, 0)

    def taken(back):
        for i in range(KV_CHUNKS):
            kv_copy(chip - back, 1 - core, i, other, pass_send.at[0, i], core_recv.at[back, i]).wait_recv()

    @pl.when(core == 1)
    def _():
        taken(0)
        past(chip, 0)

    for back in (1, 3, 2):
        if back == 2:
            for i in range(KV_CHUNKS):
                serve(2, i)

        @pl.when(chip >= back)
        def _():
            past(chip - back, core)
            taken(back)
            past(chip - back, 1 - core)

    def finish(i, carry):
        rows = pl.ds(pl.multiple_of(i * rows_per, rows_per), rows_per)
        att_ref[rows, :] = (acc[rows, :] / jnp.concatenate([row_sum[rows, :]] * (head_dim // lanes), axis=1)).astype(jnp.bfloat16)
        return carry

    lax.fori_loop(0, KV_CHUNKS, finish, 0)
    k_store.wait()
    v_store.wait()
    for i in range(KV_CHUNKS):
        @pl.when(chip < CHIPS - 1)
        def _():
            to_right(i).wait_send()

        @pl.when(chip == 0)
        def _():
            to_wrap(i).wait_send()

        @pl.when(core == 0)
        def _():
            to_other(i).wait_send()

        @pl.when(jnp.logical_and(chip >= 1, chip < CHIPS - 1))
        def _():
            on_right(i).wait_send()

        for back in (1, 2, 3):
            @pl.when(chip >= back)
            def _():
                on_other(back, i).wait_send()


def layer_head(layer, x_cur, cos_t, sin_t, norm_gain, w_q, w_k, w_v, w_gate, w_up):
    tok_count, d_model = x_cur.shape
    head_dim = w_q.shape[2]
    ff_local = w_gate.shape[2]
    rows_per = tok_count // KV_CHUNKS
    any_spec = pl.BlockSpec(memory_space=pl.ANY)
    vmem_spec = pl.BlockSpec(memory_space=pltpu.VMEM)
    bf16 = jnp.bfloat16
    return pl.pallas_call(
        functools.partial(head_kernel, layer),
        out_shape=[
            jax.ShapeDtypeStruct((tok_count, ff_local), bf16),
            jax.ShapeDtypeStruct((tok_count, head_dim), bf16),
            jax.ShapeDtypeStruct((tok_count, head_dim), bf16),
            jax.ShapeDtypeStruct((tok_count, head_dim), bf16),
        ],
        in_specs=[any_spec, vmem_spec, vmem_spec, vmem_spec, any_spec, any_spec, any_spec, any_spec, any_spec],
        out_specs=[vmem_spec, vmem_spec, any_spec, any_spec],
        scratch_shapes=[
            pltpu.VMEM((tok_count, d_model), bf16),
            pltpu.VMEM((2, rows_per, d_model), bf16),
            pltpu.VMEM((3, d_model, head_dim), bf16),
            pltpu.VMEM((2, 2, d_model, W_TILE), bf16),
            pltpu.VMEM((2 * CHIPS * tok_count, 2 * head_dim), bf16),
            pltpu.VMEM((tok_count, head_dim), bf16),
            pltpu.VMEM((tok_count, head_dim), jnp.float32),
            pltpu.VMEM((tok_count, 128), jnp.float32),
            pltpu.VMEM((tok_count, 128), jnp.float32),
            pltpu.SemaphoreType.DMA((2,)),
            pltpu.SemaphoreType.DMA((3,)),
            pltpu.SemaphoreType.DMA((2, 2)),
            pltpu.SemaphoreType.DMA((2,)),
            pltpu.SemaphoreType.DMA((3, KV_CHUNKS)),
            pltpu.SemaphoreType.DMA((4, KV_CHUNKS)),
            pltpu.SemaphoreType.DMA((3, KV_CHUNKS)),
            pltpu.SemaphoreType.DMA((4, KV_CHUNKS)),
        ],
        compiler_params=pltpu.CompilerParams(collective_id=2 + layer, has_side_effects=True, vmem_limit_bytes=63 * 1024 * 1024),
        cost_estimate=pl.CostEstimate(flops=2 * tok_count * d_model * (3 * head_dim + 2 * ff_local), bytes_accessed=d_model * (3 * head_dim + 2 * ff_local) * 2, transcendentals=0),
        name='head',
    )(x_cur, cos_t, sin_t, norm_gain, w_q, w_k, w_v, w_gate, w_up)


RING = 4
HALVES = 2
DIRS = 2
STEPS = 8


def tail_kernel(layer, chunk_rows, hid_ref, att_ref, x_ref, wd_ref, wo_ref, out_ref, part, xbuf, wbuf, recv_a, recv_b, load_sem, store_sem, send_sem, recv_sem):
    tok_count, d_model = xbuf.shape
    ff_local = hid_ref.shape[1]
    chunk_count = tok_count // chunk_rows
    quarter, eighth = chunk_rows // RING, chunk_rows // (2 * RING)
    half_cols = d_model // HALVES
    piece_cols = half_cols // RING
    my_head = lax.axis_index('head')
    pos_z, pos_y = my_head // RING, my_head % RING
    sign = (1, -1)

    def y_peer(d):
        return pos_z * RING + (pos_y + sign[d] + RING) % RING

    def z_peer(d):
        return ((pos_z + sign[d] + RING) % RING) * RING + pos_y

    first_pos, second_pos = (pos_y, pos_z), (pos_z, pos_y)
    first_peer, second_peer = (y_peer, z_peer), (z_peer, y_peer)

    loads = [
        pltpu.make_async_copy(wd_ref.at[layer], wbuf.at[pl.ds(0, ff_local), :], load_sem.at[0]),
        pltpu.make_async_copy(wo_ref.at[layer, 0], wbuf.at[pl.ds(ff_local, wo_ref.shape[2]), :], load_sem.at[1]),
        pltpu.make_async_copy(x_ref, xbuf, load_sem.at[2]),
    ]
    for load in loads:
        load.start()
    barrier = pltpu.get_barrier_semaphore()
    for peer in (y_peer, z_peer):
        for d in range(DIRS):
            pl.semaphore_signal(barrier, inc=1, device_id={'head': peer(d)}, device_id_type=pl.DeviceIdType.MESH)
    pl.semaphore_wait(barrier, 2 * DIRS)
    for load in loads:
        load.wait()

    def rows_of(chunk, piece, offset, count):
        return pl.ds(pl.multiple_of(chunk * chunk_rows + piece * quarter + offset, eighth), count)

    def cols_of(h, piece):
        return pl.ds(pl.multiple_of(h * half_cols + piece * piece_cols, piece_cols), piece_cols)

    def half_of(h):
        return pl.ds(h * half_cols, half_cols)

    def message(step, chunk, h, d):
        p1, p2, s = first_pos[h], second_pos[h], sign[d]
        far1, near1, behind1 = (p1 + 2) % RING, (p1 + s + RING) % RING, (p1 - s + RING) % RING
        far2, near2, behind2 = (p2 + 2) % RING, (p2 + s + RING) % RING, (p2 - s + RING) % RING
        if step == 0:
            src, dst = part.at[rows_of(chunk, far1, d * eighth, eighth), half_of(h)], recv_a.at[chunk, h, d, pl.ds(quarter, eighth), :]
        elif step == 1:
            src, dst = part.at[rows_of(chunk, near1, 0, quarter), half_of(h)], recv_a.at[chunk, h, d, pl.ds(0, quarter), :]
        elif step == 2:
            src, dst = part.at[rows_of(chunk, p1, d * eighth, eighth), cols_of(h, far2)], recv_b.at[chunk, h, d, pl.ds(quarter, eighth), :]
        elif step == 3:
            src, dst = part.at[rows_of(chunk, p1, 0, quarter), cols_of(h, near2)], recv_b.at[chunk, h, d, pl.ds(0, quarter), :]
        elif step == 4:
            src = dst = xbuf.at[rows_of(chunk, p1, 0, quarter), cols_of(h, p2)]
        elif step == 5:
            src = dst = xbuf.at[rows_of(chunk, p1, d * eighth, eighth), cols_of(h, behind2)]
        elif step == 6:
            src = dst = xbuf.at[rows_of(chunk, p1, 0, quarter), half_of(h)]
        else:
            src = dst = xbuf.at[rows_of(chunk, behind1, d * eighth, eighth), half_of(h)]
        peer = (first_peer if step in (0, 1, 6, 7) else second_peer)[h](d)
        return pltpu.make_async_remote_copy(
            src_ref=src, dst_ref=dst, send_sem=send_sem.at[chunk, step, h * DIRS + d], recv_sem=recv_sem.at[chunk, step, h * DIRS + d],
            device_id={'head': peer}, device_id_type=pl.DeviceIdType.MESH)

    def project(chunk):
        rows = pl.ds(pl.multiple_of(chunk * chunk_rows, chunk_rows), chunk_rows)

        def one_tile(i, carry):
            cols = pl.ds(pl.multiple_of(i * piece_cols, piece_cols), piece_cols)
            total = jnp.dot(hid_ref[rows, :], wbuf[:ff_local, cols], preferred_element_type=jnp.float32)
            part[rows, cols] = total + jnp.dot(att_ref[rows, :], wbuf[ff_local:, cols], preferred_element_type=jnp.float32)
            return carry

        lax.fori_loop(0, d_model // piece_cols, one_tile, 0)

    def store(chunk):
        rows = pl.ds(pl.multiple_of(chunk * chunk_rows, chunk_rows), chunk_rows)
        return pltpu.make_async_copy(xbuf.at[rows, :], out_ref.at[rows, :], store_sem.at[chunk])

    def stage(number, chunk):
        if number == 0:
            project(chunk)
        for h in range(HALVES):
            p1, p2 = first_pos[h], second_pos[h]
            if number:
                for d in range(DIRS):
                    message(number - 1, chunk, h, d).wait_recv()
            if number in (1, 3):
                for d in range(DIRS):
                    if number == 1:
                        rows, cols, arrived = rows_of(chunk, (p1 + sign[d] + RING) % RING, d * eighth, eighth), half_of(h), recv_a
                    else:
                        rows, cols, arrived = rows_of(chunk, p1, d * eighth, eighth), cols_of(h, (p2 + sign[d] + RING) % RING), recv_b
                    part[rows, cols] = part[rows, cols] + arrived[chunk, h, d, pl.ds(quarter, eighth), :]
            if number == 2:
                rows = rows_of(chunk, p1, 0, quarter)
                part[rows, half_of(h)] = part[rows, half_of(h)] + recv_a[chunk, h, 0, pl.ds(0, quarter), :] + recv_a[chunk, h, 1, pl.ds(0, quarter), :]
            if number == 4:
                rows, cols = rows_of(chunk, p1, 0, quarter), cols_of(h, p2)
                total = part[rows, cols] + recv_b[chunk, h, 0, pl.ds(0, quarter), :] + recv_b[chunk, h, 1, pl.ds(0, quarter), :]
                update = total.astype(jnp.bfloat16).astype(jnp.float32)
                xbuf[rows, cols] = (xbuf[rows, cols].astype(jnp.float32) + update).astype(jnp.bfloat16)
            if number < STEPS:
                for d in range(DIRS):
                    message(number, chunk, h, d).start()
        if number == STEPS:
            store(chunk).start()

    def tick(t, carry):
        for number in range(STEPS, -1, -1):
            chunk = t - number

            @pl.when(jnp.logical_and(chunk >= 0, chunk < chunk_count))
            def _():
                stage(number, chunk)
        return carry

    lax.fori_loop(0, chunk_count + STEPS, tick, 0)

    def drain(chunk, carry):
        for step in range(STEPS):
            for h in range(HALVES):
                for d in range(DIRS):
                    message(step, chunk, h, d).wait_send()
        store(chunk).wait()
        return carry

    lax.fori_loop(0, chunk_count, drain, 0)


def layer_tail(layer, hidden, attn_heads, x_cur, w_down, w_o):
    tok_count, d_model = x_cur.shape
    chunk_rows = min(CHUNK_ROWS, tok_count)
    chunk_count = tok_count // chunk_rows
    depth = hidden.shape[1] + attn_heads.shape[1]
    landed = 3 * chunk_rows // (2 * RING)
    any_spec = pl.BlockSpec(memory_space=pl.ANY)
    vmem_spec = pl.BlockSpec(memory_space=pltpu.VMEM)
    return pl.pallas_call(
        functools.partial(tail_kernel, layer, chunk_rows),
        out_shape=jax.ShapeDtypeStruct((tok_count, d_model), jnp.bfloat16),
        in_specs=[vmem_spec, vmem_spec, any_spec, any_spec, any_spec],
        out_specs=any_spec,
        scratch_shapes=[
            pltpu.VMEM((tok_count, d_model), jnp.float32),
            pltpu.VMEM((tok_count, d_model), jnp.bfloat16),
            pltpu.VMEM((depth, d_model), jnp.bfloat16),
            pltpu.VMEM((chunk_count, HALVES, DIRS, landed, d_model // HALVES), jnp.float32),
            pltpu.VMEM((chunk_count, HALVES, DIRS, landed, d_model // HALVES // RING), jnp.float32),
            pltpu.SemaphoreType.DMA((3,)),
            pltpu.SemaphoreType.DMA((chunk_count,)),
            pltpu.SemaphoreType.DMA((chunk_count, STEPS, HALVES * DIRS)),
            pltpu.SemaphoreType.DMA((chunk_count, STEPS, HALVES * DIRS)),
        ],
        compiler_params=pltpu.CompilerParams(collective_id=layer, has_side_effects=True, vmem_limit_bytes=63 * 1024 * 1024),
        cost_estimate=pl.CostEstimate(flops=2 * tok_count * depth * d_model, bytes_accessed=depth * d_model * 2, transcendentals=0),
        name='tail',
    )(hidden, attn_heads, x_cur, w_down, w_o)


def solution(mesh):
    row_spec = P(('batch', 'seq'), None)
    pos_spec = P(('batch', 'seq'))
    head_spec = P(None, None, 'head', None)
    out_proj_spec = P(None, 'head', None, None)
    col_spec = P(None, None, 'head')
    down_spec = P(None, 'head', None)
    cache_spec = P(None, ('batch', 'seq'), 'head', None)

    def local_forward(x_loc, pos_loc, w_q, w_k, w_v, w_o, w_gate, w_up, w_down, norm_gain):
        tok_count, d_model = x_loc.shape
        layer_count = w_q.shape[0]
        head_dim = w_q.shape[3]
        flat_q, flat_k, flat_v = (w.reshape(layer_count, d_model, head_dim) for w in (w_q, w_k, w_v))
        cos_t, sin_t = rope_tables(pos_loc, head_dim)
        x_cur = x_loc
        k_list = []
        v_list = []
        for layer in range(layer_count):
            hidden, attn_heads, k_rot, v_heads = layer_head(layer, x_cur, cos_t, sin_t, norm_gain, flat_q, flat_k, flat_v, w_gate, w_up)
            x_cur = layer_tail(layer, hidden, attn_heads, x_cur, w_down, w_o)
            k_list.append(k_rot.reshape(tok_count, 1, head_dim))
            v_list.append(v_heads.reshape(tok_count, 1, head_dim))
        return x_cur, jnp.stack(k_list), jnp.stack(v_list)

    return jax.shard_map(local_forward, mesh=mesh, in_specs=(row_spec, pos_spec, head_spec, head_spec, head_spec, out_proj_spec, col_spec, col_spec, down_spec, P(None, None)), out_specs=(row_spec, cache_spec, cache_spec), check_vma=False)
```

```python
import functools
import math
import jax
import jax.numpy as jnp
from jax import lax
from jax.experimental import pallas as pl
from jax.experimental.pallas import tpu as pltpu
from jax.sharding import PartitionSpec as P

ROPE_BASE = 500000.0
EPS = 1e-5


def rope_tables(positions, head_dim):
    half_dim = head_dim // 2
    inv_freq = ROPE_BASE ** (-(jnp.arange(half_dim, dtype=jnp.float32) * 2.0 / head_dim))
    angles = positions.astype(jnp.float32)[..., None] * inv_freq
    return jnp.cos(angles), jnp.sin(angles)


LOG2E = 1.4426950408889634
CHUNK_ROWS = 128


CHIPS = 4
KV_CHUNKS = 4
W_TILE = 256
NORM_ROWS = 64


def head_kernel(layer, x_ref, cos_ref, sin_ref, gain_ref, wq_ref, wk_ref, wv_ref, wg_ref, wu_ref, hid_ref, att_ref, k_ref, v_ref,
                hbuf, xs, wqkv, wtile, kv, qbuf, acc, row_max, row_sum, x_sem, w_sem, t_sem, out_sem, own_send, pass_send, ici_recv, core_recv):
    tok_count, d_model = hbuf.shape
    head_dim = qbuf.shape[1]
    half_dim = head_dim // 2
    rows_per = tok_count // KV_CHUNKS
    half_rows = tok_count // 2
    my_seq = lax.axis_index('seq')
    chip, core = my_seq // 2, my_seq % 2
    other = chip * 2 + 1 - core
    right = ((chip + 1) % CHIPS) * 2 + core
    left = ((chip + CHIPS - 1) % CHIPS) * 2 + core

    def x_load(i):
        return pltpu.make_async_copy(x_ref.at[pl.ds(pl.multiple_of(i * rows_per, rows_per), rows_per), :], xs.at[i % 2], x_sem.at[i % 2])

    def tile_load(i, which):
        ref = (wg_ref, wu_ref)[which]
        return pltpu.make_async_copy(ref.at[layer, :, pl.ds(pl.multiple_of(i * W_TILE, W_TILE), W_TILE)], wtile.at[i % 2, which], t_sem.at[i % 2, which])

    x_load(0).start()
    w_loads = [pltpu.make_async_copy(ref.at[layer], wqkv.at[n], w_sem.at[n]) for n, ref in enumerate((wk_ref, wv_ref, wq_ref))]
    for load in w_loads:
        load.start()
    x_load(1).start()
    for which in range(2):
        tile_load(0, which).start()

    barrier = pltpu.get_barrier_semaphore()
    for peer in (left, right, other):
        pl.semaphore_signal(barrier, inc=1, device_id={'seq': peer}, device_id_type=pl.DeviceIdType.MESH)
    pl.semaphore_wait(barrier, 3)

    def kv_copy(origin_chip, origin_core, i, to, send, recv):
        rows = kv.at[pl.ds(pl.multiple_of((origin_chip * 2 + origin_core) * tok_count + i * rows_per, rows_per), rows_per), :]
        return pltpu.make_async_remote_copy(src_ref=rows, dst_ref=rows, send_sem=send, recv_sem=recv, device_id={'seq': to}, device_id_type=pl.DeviceIdType.MESH)

    def to_right(i):
        return kv_copy(chip, core, i, right, own_send.at[0, i], ici_recv.at[0, i])

    def to_wrap(i):
        return kv_copy(chip, core, i, left, own_send.at[1, i], ici_recv.at[2, i])

    def to_other(i):
        return kv_copy(chip, core, i, other, own_send.at[2, i], core_recv.at[0, i])

    def on_right(i):
        return kv_copy(chip - 1, core, i, right, pass_send.at[0, i], ici_recv.at[1, i])

    def on_other(back, i):
        return kv_copy(chip - back, core, i, other, pass_send.at[back, i], core_recv.at[back, i])

    def arrival(back, i):
        return kv_copy(chip - back, core, i, other, pass_send.at[back, i], ici_recv.at[back - 1, i])

    def serve(back, i):
        @pl.when(chip >= back)
        def _():
            arrival(back, i).wait_recv()
            on_other(back, i).start()
        if back == 1:
            @pl.when(jnp.logical_and(chip >= 1, chip < CHIPS - 1))
            def _():
                on_right(i).start()

    def rope(values, rows):
        cos_t, sin_t = cos_ref[rows, :], sin_ref[rows, :]
        wide = values.astype(jnp.bfloat16).astype(jnp.float32)
        first, second = wide[:, :half_dim], wide[:, half_dim:]
        return jnp.concatenate([first * cos_t - second * sin_t, second * cos_t + first * sin_t], axis=1).astype(jnp.bfloat16)

    gain = gain_ref[pl.ds(layer, 1), :].astype(jnp.float32)

    def prepare(i, carry):
        x_load(i).wait()
        rows = pl.ds(pl.multiple_of(i * rows_per, rows_per), rows_per)

        def norm(j, inner):
            few = pl.ds(pl.multiple_of(j * NORM_ROWS, NORM_ROWS), NORM_ROWS)
            x_f32 = xs[i % 2, few, :].astype(jnp.float32)
            inv_rms = lax.rsqrt(jnp.mean(x_f32 * x_f32, axis=-1, keepdims=True) + EPS)
            hbuf[pl.ds(pl.multiple_of(i * rows_per + j * NORM_ROWS, NORM_ROWS), NORM_ROWS), :] = (x_f32 * inv_rms * gain).astype(jnp.bfloat16)
            return inner

        lax.fori_loop(0, rows_per // NORM_ROWS, norm, 0)

        @pl.when(i + 2 < KV_CHUNKS)
        def _():
            x_load(i + 2).start()

        @pl.when(i == 0)
        def _():
            w_loads[0].wait()
            w_loads[1].wait()

        normed = hbuf[rows, :]
        own = pl.ds(pl.multiple_of(my_seq * tok_count + i * rows_per, rows_per), rows_per)
        kv[own, :head_dim] = rope(jnp.dot(normed, wqkv[0], preferred_element_type=jnp.float32), rows)
        kv[own, head_dim:] = jnp.dot(normed, wqkv[1], preferred_element_type=jnp.float32).astype(jnp.bfloat16)

        @pl.when(chip < CHIPS - 1)
        def _():
            to_right(i).start()

        @pl.when(chip == 0)
        def _():
            to_wrap(i).start()

        @pl.when(core == 0)
        def _():
            to_other(i).start()
        return carry

    lax.fori_loop(0, KV_CHUNKS, prepare, 0)
    w_loads[2].wait()
    own_rows = pl.ds(pl.multiple_of(my_seq * tok_count, tok_count), tok_count)
    k_store = pltpu.make_async_copy(kv.at[own_rows, pl.ds(0, head_dim)], k_ref, out_sem.at[0])
    v_store = pltpu.make_async_copy(kv.at[own_rows, pl.ds(head_dim, head_dim)], v_ref, out_sem.at[1])
    k_store.start()
    v_store.start()

    def query(i, carry):
        rows = pl.ds(pl.multiple_of(i * rows_per, rows_per), rows_per)
        qbuf[rows, :] = rope(jnp.dot(hbuf[rows, :], wqkv[2], preferred_element_type=jnp.float32), rows)
        return carry

    lax.fori_loop(0, KV_CHUNKS, query, 0)

    def gated(i, carry):
        for which in range(2):
            tile_load(i, which).wait()

        @pl.when(i + 1 < wg_ref.shape[2] // W_TILE)
        def _():
            for which in range(2):
                tile_load(i + 1, which).start()

        def rows_step(j, inner):
            rows = pl.ds(pl.multiple_of(j * rows_per, rows_per), rows_per)
            normed = hbuf[rows, :]
            gate = jnp.dot(normed, wtile[i % 2, 0], preferred_element_type=jnp.float32)
            up = jnp.dot(normed, wtile[i % 2, 1], preferred_element_type=jnp.float32)
            hid_ref[rows, pl.ds(pl.multiple_of(i * W_TILE, W_TILE), W_TILE)] = (gate * jax.nn.sigmoid(gate) * up).astype(jnp.bfloat16)
            return inner

        lax.fori_loop(0, KV_CHUNKS, rows_step, 0)
        serve(1, i)
        serve(3, i)
        return carry

    lax.fori_loop(0, KV_CHUNKS, gated, 0)

    scale = LOG2E / math.sqrt(head_dim)
    lanes = row_max.shape[1]

    def attend(key_start, q_half, masked, first):
        rows = pl.ds(q_half * half_rows, half_rows)
        some = pl.ds(key_start, half_rows)
        logits = lax.dot_general(qbuf[rows, :], kv[some, :head_dim], (((1,), (1,)), ((), ())), preferred_element_type=jnp.float32) * scale
        if masked:
            seen = lax.broadcasted_iota(jnp.int32, logits.shape, 0) >= lax.broadcasted_iota(jnp.int32, logits.shape, 1)
            logits = jnp.where(seen, logits, -jnp.inf)
        block_max = jnp.max(logits, axis=-1, keepdims=True)
        if first:
            new_max = jnp.broadcast_to(block_max, (half_rows, lanes))
        else:
            new_max = jnp.maximum(row_max[rows, :], block_max)
        prob = jnp.exp2(logits - jnp.concatenate([new_max] * (half_rows // lanes), axis=1))
        block_sum = jnp.sum(prob, axis=-1, keepdims=True)
        block_out = jnp.dot(prob.astype(jnp.bfloat16), kv[some, head_dim:], preferred_element_type=jnp.float32)
        if first:
            row_sum[rows, :] = jnp.broadcast_to(block_sum, (half_rows, lanes))
            acc[rows, :] = block_out
        else:
            rescale = jnp.exp2(row_max[rows, :] - new_max)
            row_sum[rows, :] = row_sum[rows, :] * rescale + block_sum
            acc[rows, :] = acc[rows, :] * jnp.concatenate([rescale] * (head_dim // lanes), axis=1) + block_out
        row_max[rows, :] = new_max

    own_start = pl.multiple_of(my_seq * tok_count, tok_count)
    attend(own_start, 0, True, True)
    attend(own_start, 1, False, True)
    attend(pl.multiple_of(own_start + half_rows, half_rows), 1, True, False)

    def past(block_chip, block_core):
        def one(n, carry):
            start = pl.multiple_of((block_chip * 2 + block_core) * tok_count + n * half_rows, half_rows)
            attend(start, 0, False, False)
            attend(start, 1, False, False)
            return carry
        lax.fori_loop(0, 2, one, 0)

    def taken(back):
        for i in range(KV_CHUNKS):
            kv_copy(chip - back, 1 - core, i, other, pass_send.at[0, i], core_recv.at[back, i]).wait_recv()

    @pl.when(core == 1)
    def _():
        taken(0)
        past(chip, 0)

    for back in (1, 3, 2):
        if back == 2:
            for i in range(KV_CHUNKS):
                serve(2, i)

        @pl.when(chip >= back)
        def _():
            past(chip - back, core)
            taken(back)
            past(chip - back, 1 - core)

    def finish(i, carry):
        rows = pl.ds(pl.multiple_of(i * rows_per, rows_per), rows_per)
        att_ref[rows, :] = (acc[rows, :] / jnp.concatenate([row_sum[rows, :]] * (head_dim // lanes), axis=1)).astype(jnp.bfloat16)
        return carry

    lax.fori_loop(0, KV_CHUNKS, finish, 0)
    k_store.wait()
    v_store.wait()
    for i in range(KV_CHUNKS):
        @pl.when(chip < CHIPS - 1)
        def _():
            to_right(i).wait_send()

        @pl.when(chip == 0)
        def _():
            to_wrap(i).wait_send()

        @pl.when(core == 0)
        def _():
            to_other(i).wait_send()

        @pl.when(jnp.logical_and(chip >= 1, chip < CHIPS - 1))
        def _():
            on_right(i).wait_send()

        for back in (1, 2, 3):
            @pl.when(chip >= back)
            def _():
                on_other(back, i).wait_send()


def layer_head(layer, x_cur, cos_t, sin_t, norm_gain, w_q, w_k, w_v, w_gate, w_up):
    tok_count, d_model = x_cur.shape
    head_dim = w_q.shape[2]
    ff_local = w_gate.shape[2]
    rows_per = tok_count // KV_CHUNKS
    any_spec = pl.BlockSpec(memory_space=pl.ANY)
    vmem_spec = pl.BlockSpec(memory_space=pltpu.VMEM)
    bf16 = jnp.bfloat16
    return pl.pallas_call(
        functools.partial(head_kernel, layer),
        out_shape=[
            jax.ShapeDtypeStruct((tok_count, ff_local), bf16),
            jax.ShapeDtypeStruct((tok_count, head_dim), bf16),
            jax.ShapeDtypeStruct((tok_count, head_dim), bf16),
            jax.ShapeDtypeStruct((tok_count, head_dim), bf16),
        ],
        in_specs=[any_spec, vmem_spec, vmem_spec, vmem_spec, any_spec, any_spec, any_spec, any_spec, any_spec],
        out_specs=[vmem_spec, vmem_spec, any_spec, any_spec],
        scratch_shapes=[
            pltpu.VMEM((tok_count, d_model), bf16),
            pltpu.VMEM((2, rows_per, d_model), bf16),
            pltpu.VMEM((3, d_model, head_dim), bf16),
            pltpu.VMEM((2, 2, d_model, W_TILE), bf16),
            pltpu.VMEM((2 * CHIPS * tok_count, 2 * head_dim), bf16),
            pltpu.VMEM((tok_count, head_dim), bf16),
            pltpu.VMEM((tok_count, head_dim), jnp.float32),
            pltpu.VMEM((tok_count, 128), jnp.float32),
            pltpu.VMEM((tok_count, 128), jnp.float32),
            pltpu.SemaphoreType.DMA((2,)),
            pltpu.SemaphoreType.DMA((3,)),
            pltpu.SemaphoreType.DMA((2, 2)),
            pltpu.SemaphoreType.DMA((2,)),
            pltpu.SemaphoreType.DMA((3, KV_CHUNKS)),
            pltpu.SemaphoreType.DMA((4, KV_CHUNKS)),
            pltpu.SemaphoreType.DMA((3, KV_CHUNKS)),
            pltpu.SemaphoreType.DMA((4, KV_CHUNKS)),
        ],
        compiler_params=pltpu.CompilerParams(collective_id=2 + layer, has_side_effects=True, vmem_limit_bytes=63 * 1024 * 1024),
        cost_estimate=pl.CostEstimate(flops=2 * tok_count * d_model * (3 * head_dim + 2 * ff_local), bytes_accessed=d_model * (3 * head_dim + 2 * ff_local) * 2, transcendentals=0),
        name='head',
    )(x_cur, cos_t, sin_t, norm_gain, w_q, w_k, w_v, w_gate, w_up)


RING = 4
HALVES = 2
DIRS = 2
STEPS = 8
SKEW = 2
W_GROUPS = 4


def tail_kernel(layer, chunk_rows, hid_ref, att_ref, x_ref, wd_ref, wo_ref, out_ref, part, xbuf, wbuf, recv_a, recv_b, load_sem, store_sem, send_sem, recv_sem):
    tok_count, d_model = xbuf.shape
    ff_local = hid_ref.shape[1]
    chunk_count = tok_count // chunk_rows
    quarter, eighth = chunk_rows // RING, chunk_rows // (2 * RING)
    half_cols = d_model // HALVES
    piece_cols = half_cols // RING
    my_head = lax.axis_index('head')
    pos_z, pos_y = my_head // RING, my_head % RING
    sign = (1, -1)

    def y_peer(d):
        return pos_z * RING + (pos_y + sign[d] + RING) % RING

    def z_peer(d):
        return ((pos_z + sign[d] + RING) % RING) * RING + pos_y

    first_pos, second_pos = (pos_y, pos_z), (pos_z, pos_y)
    first_peer, second_peer = (y_peer, z_peer), (z_peer, y_peer)

    group_cols = d_model // W_GROUPS

    def w_load(g):
        cols = pl.ds(pl.multiple_of(g * group_cols, group_cols), group_cols)
        return (pltpu.make_async_copy(wd_ref.at[layer, :, cols], wbuf.at[pl.ds(0, ff_local), cols], load_sem.at[g, 0]),
                pltpu.make_async_copy(wo_ref.at[layer, 0, :, cols], wbuf.at[pl.ds(ff_local, wo_ref.shape[2]), cols], load_sem.at[g, 1]))

    x_load = pltpu.make_async_copy(x_ref, xbuf, load_sem.at[W_GROUPS, 0])
    for g in range(W_GROUPS):
        for load in w_load(g):
            load.start()
    x_load.start()
    barrier = pltpu.get_barrier_semaphore()
    for peer in (y_peer, z_peer):
        for d in range(DIRS):
            pl.semaphore_signal(barrier, inc=1, device_id={'head': peer(d)}, device_id_type=pl.DeviceIdType.MESH)
    pl.semaphore_wait(barrier, 2 * DIRS)

    def rows_of(chunk, piece, offset, count):
        return pl.ds(pl.multiple_of(chunk * chunk_rows + piece * quarter + offset, eighth), count)

    def cols_of(h, piece):
        return pl.ds(pl.multiple_of(h * half_cols + piece * piece_cols, piece_cols), piece_cols)

    def half_of(h):
        return pl.ds(h * half_cols, half_cols)

    def message(step, chunk, h, d):
        p1, p2, s = first_pos[h], second_pos[h], sign[d]
        far1, near1, behind1 = (p1 + 2) % RING, (p1 + s + RING) % RING, (p1 - s + RING) % RING
        far2, near2, behind2 = (p2 + 2) % RING, (p2 + s + RING) % RING, (p2 - s + RING) % RING
        if step == 0:
            src, dst = part.at[rows_of(chunk, far1, d * eighth, eighth), half_of(h)], recv_a.at[chunk, h, d, pl.ds(quarter, eighth), :]
        elif step == 1:
            src, dst = part.at[rows_of(chunk, near1, 0, quarter), half_of(h)], recv_a.at[chunk, h, d, pl.ds(0, quarter), :]
        elif step == 2:
            src, dst = part.at[rows_of(chunk, p1, d * eighth, eighth), cols_of(h, far2)], recv_b.at[chunk, h, d, pl.ds(quarter, eighth), :]
        elif step == 3:
            src, dst = part.at[rows_of(chunk, p1, 0, quarter), cols_of(h, near2)], recv_b.at[chunk, h, d, pl.ds(0, quarter), :]
        elif step == 4:
            src = dst = xbuf.at[rows_of(chunk, p1, 0, quarter), cols_of(h, p2)]
        elif step == 5:
            src = dst = xbuf.at[rows_of(chunk, p1, d * eighth, eighth), cols_of(h, behind2)]
        elif step == 6:
            src = dst = xbuf.at[rows_of(chunk, p1, 0, quarter), half_of(h)]
        else:
            src = dst = xbuf.at[rows_of(chunk, behind1, d * eighth, eighth), half_of(h)]
        peer = (first_peer if step in (0, 1, 6, 7) else second_peer)[h](d)
        return pltpu.make_async_remote_copy(
            src_ref=src, dst_ref=dst, send_sem=send_sem.at[chunk, step, h * DIRS + d], recv_sem=recv_sem.at[chunk, step, h * DIRS + d],
            device_id={'head': peer}, device_id_type=pl.DeviceIdType.MESH)

    def project(chunk):
        rows = pl.ds(pl.multiple_of(chunk * chunk_rows, chunk_rows), chunk_rows)

        def one_tile(i, carry):
            cols = pl.ds(pl.multiple_of(i * piece_cols, piece_cols), piece_cols)
            per_group = group_cols // piece_cols

            @pl.when(jnp.logical_and(chunk == 0, i % per_group == 0))
            def _():
                for load in w_load(i // per_group):
                    load.wait()

            total = jnp.dot(hid_ref[rows, :], wbuf[:ff_local, cols], preferred_element_type=jnp.float32)
            part[rows, cols] = total + jnp.dot(att_ref[rows, :], wbuf[ff_local:, cols], preferred_element_type=jnp.float32)
            return carry

        lax.fori_loop(0, d_model // piece_cols, one_tile, 0)

    def store(chunk):
        rows = pl.ds(pl.multiple_of(chunk * chunk_rows, chunk_rows), chunk_rows)
        return pltpu.make_async_copy(xbuf.at[rows, :], out_ref.at[rows, :], store_sem.at[chunk])

    def stage(number, chunk):
        if number == 0:
            project(chunk)
        if number == 1:
            @pl.when(chunk == 0)
            def _():
                x_load.wait()
        for h in range(HALVES):
            p1, p2 = first_pos[h], second_pos[h]
            if number:
                for d in range(DIRS):
                    message(number - 1, chunk, h, d).wait_recv()
            if number in (1, 3):
                for d in range(DIRS):
                    if number == 1:
                        rows, cols, arrived = rows_of(chunk, (p1 + sign[d] + RING) % RING, d * eighth, eighth), half_of(h), recv_a
                    else:
                        rows, cols, arrived = rows_of(chunk, p1, d * eighth, eighth), cols_of(h, (p2 + sign[d] + RING) % RING), recv_b
                    part[rows, cols] = part[rows, cols] + arrived[chunk, h, d, pl.ds(quarter, eighth), :]
            if number == 2:
                rows = rows_of(chunk, p1, 0, quarter)
                part[rows, half_of(h)] = part[rows, half_of(h)] + recv_a[chunk, h, 0, pl.ds(0, quarter), :] + recv_a[chunk, h, 1, pl.ds(0, quarter), :]
            if number == 4:
                rows, cols = rows_of(chunk, p1, 0, quarter), cols_of(h, p2)
                total = part[rows, cols] + recv_b[chunk, h, 0, pl.ds(0, quarter), :] + recv_b[chunk, h, 1, pl.ds(0, quarter), :]
                update = total.astype(jnp.bfloat16).astype(jnp.float32)
                xbuf[rows, cols] = (xbuf[rows, cols].astype(jnp.float32) + update).astype(jnp.bfloat16)
            if number < STEPS:
                for d in range(DIRS):
                    message(number, chunk, h, d).start()
        if number == STEPS:
            store(chunk).start()

    def tick(t, carry):
        for number in range(STEPS, -1, -1):
            chunk = t - SKEW * number

            @pl.when(jnp.logical_and(chunk >= 0, chunk < chunk_count))
            def _():
                stage(number, chunk)
        return carry

    lax.fori_loop(0, chunk_count + SKEW * STEPS, tick, 0)

    def drain(chunk, carry):
        for step in range(STEPS):
            for h in range(HALVES):
                for d in range(DIRS):
                    message(step, chunk, h, d).wait_send()
        store(chunk).wait()
        return carry

    lax.fori_loop(0, chunk_count, drain, 0)


def layer_tail(layer, hidden, attn_heads, x_cur, w_down, w_o):
    tok_count, d_model = x_cur.shape
    chunk_rows = min(CHUNK_ROWS, tok_count)
    chunk_count = tok_count // chunk_rows
    depth = hidden.shape[1] + attn_heads.shape[1]
    landed = 3 * chunk_rows // (2 * RING)
    any_spec = pl.BlockSpec(memory_space=pl.ANY)
    vmem_spec = pl.BlockSpec(memory_space=pltpu.VMEM)
    return pl.pallas_call(
        functools.partial(tail_kernel, layer, chunk_rows),
        out_shape=jax.ShapeDtypeStruct((tok_count, d_model), jnp.bfloat16),
        in_specs=[vmem_spec, vmem_spec, any_spec, any_spec, any_spec],
        out_specs=any_spec,
        scratch_shapes=[
            pltpu.VMEM((tok_count, d_model), jnp.float32),
            pltpu.VMEM((tok_count, d_model), jnp.bfloat16),
            pltpu.VMEM((depth, d_model), jnp.bfloat16),
            pltpu.VMEM((chunk_count, HALVES, DIRS, landed, d_model // HALVES), jnp.float32),
            pltpu.VMEM((chunk_count, HALVES, DIRS, landed, d_model // HALVES // RING), jnp.float32),
            pltpu.SemaphoreType.DMA((W_GROUPS + 1, 2)),
            pltpu.SemaphoreType.DMA((chunk_count,)),
            pltpu.SemaphoreType.DMA((chunk_count, STEPS, HALVES * DIRS)),
            pltpu.SemaphoreType.DMA((chunk_count, STEPS, HALVES * DIRS)),
        ],
        compiler_params=pltpu.CompilerParams(collective_id=layer, has_side_effects=True, vmem_limit_bytes=63 * 1024 * 1024),
        cost_estimate=pl.CostEstimate(flops=2 * tok_count * depth * d_model, bytes_accessed=depth * d_model * 2, transcendentals=0),
        name='tail',
    )(hidden, attn_heads, x_cur, w_down, w_o)


def solution(mesh):
    row_spec = P(('batch', 'seq'), None)
    pos_spec = P(('batch', 'seq'))
    head_spec = P(None, None, 'head', None)
    out_proj_spec = P(None, 'head', None, None)
    col_spec = P(None, None, 'head')
    down_spec = P(None, 'head', None)
    cache_spec = P(None, ('batch', 'seq'), 'head', None)

    def local_forward(x_loc, pos_loc, w_q, w_k, w_v, w_o, w_gate, w_up, w_down, norm_gain):
        tok_count, d_model = x_loc.shape
        layer_count = w_q.shape[0]
        head_dim = w_q.shape[3]
        flat_q, flat_k, flat_v = (w.reshape(layer_count, d_model, head_dim) for w in (w_q, w_k, w_v))
        cos_t, sin_t = rope_tables(pos_loc, head_dim)
        x_cur = x_loc
        k_list = []
        v_list = []
        for layer in range(layer_count):
            hidden, attn_heads, k_rot, v_heads = layer_head(layer, x_cur, cos_t, sin_t, norm_gain, flat_q, flat_k, flat_v, w_gate, w_up)
            x_cur = layer_tail(layer, hidden, attn_heads, x_cur, w_down, w_o)
            k_list.append(k_rot.reshape(tok_count, 1, head_dim))
            v_list.append(v_heads.reshape(tok_count, 1, head_dim))
        return x_cur, jnp.stack(k_list), jnp.stack(v_list)

    return jax.shard_map(local_forward, mesh=mesh, in_specs=(row_spec, pos_spec, head_spec, head_spec, head_spec, out_proj_spec, col_spec, col_spec, down_spec, P(None, None)), out_specs=(row_spec, cache_spec, cache_spec), check_vma=False)
```

```python
import functools
import math
import jax
import jax.numpy as jnp
from jax import lax
from jax.experimental import pallas as pl
from jax.experimental.pallas import tpu as pltpu
from jax.sharding import PartitionSpec as P

ROPE_BASE = 500000.0
EPS = 1e-5


def rope_tables(positions, head_dim):
    half_dim = head_dim // 2
    inv_freq = ROPE_BASE ** (-(jnp.arange(half_dim, dtype=jnp.float32) * 2.0 / head_dim))
    angles = positions.astype(jnp.float32)[..., None] * inv_freq
    return jnp.cos(angles), jnp.sin(angles)


LOG2E = 1.4426950408889634
CHUNKS = 8
NEAR_TICKS = (6, 9, 13)
FAR_TICKS = (16, 19, 23)


CHIPS = 4
RING = 4
HALVES = 2
DIRS = 2
KV_CHUNKS = 4
W_TILE = 256
NORM_ROWS = 64


def head_kernel(layer, spread, *refs):
    x_ref, cos_ref, sin_ref, gain_ref, wq_ref, wk_ref, wv_ref, wg_ref, wu_ref = refs[:9]
    if spread:
        hid_all_ref, att_all_ref, k_ref, v_ref, hid_ref, att_ref, give_send, give_recv, keep_sem = refs[9:18]
    else:
        wd_ref, wo_ref, hid_ref, att_ref, k_ref, v_ref, gd_ref, go_ref, give_send, give_recv = refs[9:19]
    hbuf, xs, wqkv, wtile, kv, qbuf, acc, row_max, row_sum, x_sem, w_sem, t_sem, out_sem, own_send, pass_send, ici_recv, core_recv = refs[-17:]
    my_head = lax.axis_index('head')
    pos_z, pos_y = my_head // RING, my_head % RING
    sign = (1, -1)

    def z_device(z):
        return (z + RING) % RING * RING + pos_y

    tok_count, d_model = hbuf.shape
    head_dim = qbuf.shape[1]
    half_dim = head_dim // 2
    rows_per = tok_count // KV_CHUNKS
    half_rows = tok_count // 2
    my_seq = lax.axis_index('seq')
    chip, core = my_seq // 2, my_seq % 2
    other = chip * 2 + 1 - core
    right = ((chip + 1) % CHIPS) * 2 + core
    left = ((chip + CHIPS - 1) % CHIPS) * 2 + core

    def x_load(i):
        return pltpu.make_async_copy(x_ref.at[pl.ds(pl.multiple_of(i * rows_per, rows_per), rows_per), :], xs.at[i % 2], x_sem.at[i % 2])

    def tile_load(i, which):
        ref = (wg_ref, wu_ref)[which]
        return pltpu.make_async_copy(ref.at[layer, :, pl.ds(pl.multiple_of(i * W_TILE, W_TILE), W_TILE)], wtile.at[i % 2, which], t_sem.at[i % 2, which])

    x_load(0).start()
    w_loads = [pltpu.make_async_copy(ref.at[layer], wqkv.at[n], w_sem.at[n]) for n, ref in enumerate((wk_ref, wv_ref, wq_ref))]
    for load in w_loads:
        load.start()
    x_load(1).start()
    for which in range(2):
        tile_load(0, which).start()

    barrier = pltpu.get_barrier_semaphore()
    for peer in (left, right, other):
        pl.semaphore_signal(barrier, inc=1, device_id={'seq': peer}, device_id_type=pl.DeviceIdType.MESH)
    for j in range(1, RING):
        pl.semaphore_signal(barrier, inc=1, device_id={'head': z_device(pos_z + j)}, device_id_type=pl.DeviceIdType.MESH)
    pl.semaphore_wait(barrier, 6)

    def weight_part(step, d):
        copies = []
        for n, (own_ref, all_ref) in enumerate(((wd_ref, gd_ref), (wo_ref, go_ref))):
            size = all_ref.shape[1] // (2 * CHIPS)
            if step == 0:
                rows = pl.ds(pl.multiple_of(my_seq * size, size), size)
                src = own_ref.at[layer + 1, rows, :] if n == 0 else own_ref.at[layer + 1, 0, rows, :]
                dst = all_ref.at[pos_z, rows, :]
            else:
                rows = pl.ds(pl.multiple_of(my_seq * size + d * (size // 2), size // 2), size // 2)
                src = dst = all_ref.at[(pos_z - sign[d] + RING) % RING, rows, :]
            copies.append(pltpu.make_async_remote_copy(
                src_ref=src, dst_ref=dst, send_sem=give_send.at[step, d, n], recv_sem=give_recv.at[step, d, n],
                device_id={'head': z_device(pos_z + sign[d])}, device_id_type=pl.DeviceIdType.MESH))
        return copies

    def give(src, dst, send, recv, z):
        return pltpu.make_async_remote_copy(src_ref=src, dst_ref=dst, send_sem=send, recv_sem=recv, device_id={'head': z_device(z)}, device_id_type=pl.DeviceIdType.MESH)

    def give_hidden(z, i, source):
        rows = pl.ds(pl.multiple_of(z * rows_per, rows_per), rows_per)
        cols = pl.ds(pl.multiple_of(i * W_TILE, W_TILE), W_TILE)
        return give(hid_ref.at[rows, cols], hid_all_ref.at[source, :, cols], give_send.at[z, i], give_recv.at[source, i], z)

    def keep_hidden(i):
        rows = pl.ds(pl.multiple_of(pos_z * rows_per, rows_per), rows_per)
        cols = pl.ds(pl.multiple_of(i * W_TILE, W_TILE), W_TILE)
        return pltpu.make_async_copy(hid_ref.at[rows, cols], hid_all_ref.at[pos_z, :, cols], keep_sem.at[i])

    def give_rows(z, source):
        rows = pl.ds(pl.multiple_of(z * rows_per, rows_per), rows_per)
        return give(att_ref.at[rows, :], att_all_ref.at[source], give_send.at[z, KV_CHUNKS], give_recv.at[source, KV_CHUNKS], z)

    def keep_rows():
        rows = pl.ds(pl.multiple_of(pos_z * rows_per, rows_per), rows_per)
        return pltpu.make_async_copy(att_ref.at[rows, :], att_all_ref.at[pos_z], keep_sem.at[KV_CHUNKS])

    if not spread:
        for d in range(DIRS):
            for copy in weight_part(0, d):
                copy.start()

    def kv_copy(origin_chip, origin_core, i, to, send, recv):
        rows = kv.at[pl.ds(pl.multiple_of((origin_chip * 2 + origin_core) * tok_count + i * rows_per, rows_per), rows_per), :]
        return pltpu.make_async_remote_copy(src_ref=rows, dst_ref=rows, send_sem=send, recv_sem=recv, device_id={'seq': to}, device_id_type=pl.DeviceIdType.MESH)

    def to_right(i):
        return kv_copy(chip, core, i, right, own_send.at[0, i], ici_recv.at[0, i])

    def to_wrap(i):
        return kv_copy(chip, core, i, left, own_send.at[1, i], ici_recv.at[2, i])

    def to_other(i):
        return kv_copy(chip, core, i, other, own_send.at[2, i], core_recv.at[0, i])

    def on_right(i):
        return kv_copy(chip - 1, core, i, right, pass_send.at[0, i], ici_recv.at[1, i])

    def on_other(back, i):
        return kv_copy(chip - back, core, i, other, pass_send.at[back, i], core_recv.at[back, i])

    def arrival(back, i):
        return kv_copy(chip - back, core, i, other, pass_send.at[back, i], ici_recv.at[back - 1, i])

    def serve(back, i):
        @pl.when(chip >= back)
        def _():
            arrival(back, i).wait_recv()
            on_other(back, i).start()
        if back == 1:
            @pl.when(jnp.logical_and(chip >= 1, chip < CHIPS - 1))
            def _():
                on_right(i).start()

    def rope(values, rows):
        cos_t, sin_t = cos_ref[rows, :], sin_ref[rows, :]
        wide = values.astype(jnp.bfloat16).astype(jnp.float32)
        first, second = wide[:, :half_dim], wide[:, half_dim:]
        return jnp.concatenate([first * cos_t - second * sin_t, second * cos_t + first * sin_t], axis=1).astype(jnp.bfloat16)

    gain = gain_ref[pl.ds(layer, 1), :].astype(jnp.float32)

    def prepare(i, carry):
        x_load(i).wait()
        rows = pl.ds(pl.multiple_of(i * rows_per, rows_per), rows_per)

        def norm(j, inner):
            few = pl.ds(pl.multiple_of(j * NORM_ROWS, NORM_ROWS), NORM_ROWS)
            x_f32 = xs[i % 2, few, :].astype(jnp.float32)
            inv_rms = lax.rsqrt(jnp.mean(x_f32 * x_f32, axis=-1, keepdims=True) + EPS)
            hbuf[pl.ds(pl.multiple_of(i * rows_per + j * NORM_ROWS, NORM_ROWS), NORM_ROWS), :] = (x_f32 * inv_rms * gain).astype(jnp.bfloat16)
            return inner

        lax.fori_loop(0, rows_per // NORM_ROWS, norm, 0)

        @pl.when(i + 2 < KV_CHUNKS)
        def _():
            x_load(i + 2).start()

        @pl.when(i == 0)
        def _():
            w_loads[0].wait()
            w_loads[1].wait()

        normed = hbuf[rows, :]
        own = pl.ds(pl.multiple_of(my_seq * tok_count + i * rows_per, rows_per), rows_per)
        kv[own, :head_dim] = rope(jnp.dot(normed, wqkv[0], preferred_element_type=jnp.float32), rows)
        kv[own, head_dim:] = jnp.dot(normed, wqkv[1], preferred_element_type=jnp.float32).astype(jnp.bfloat16)

        @pl.when(chip < CHIPS - 1)
        def _():
            to_right(i).start()

        @pl.when(chip == 0)
        def _():
            to_wrap(i).start()

        @pl.when(core == 0)
        def _():
            to_other(i).start()
        return carry

    lax.fori_loop(0, KV_CHUNKS, prepare, 0)
    w_loads[2].wait()
    own_rows = pl.ds(pl.multiple_of(my_seq * tok_count, tok_count), tok_count)
    k_store = pltpu.make_async_copy(kv.at[own_rows, pl.ds(0, head_dim)], k_ref, out_sem.at[0])
    v_store = pltpu.make_async_copy(kv.at[own_rows, pl.ds(head_dim, head_dim)], v_ref, out_sem.at[1])
    k_store.start()
    v_store.start()

    def query(i, carry):
        rows = pl.ds(pl.multiple_of(i * rows_per, rows_per), rows_per)
        qbuf[rows, :] = rope(jnp.dot(hbuf[rows, :], wqkv[2], preferred_element_type=jnp.float32), rows)
        return carry

    lax.fori_loop(0, KV_CHUNKS, query, 0)

    def gated(i, carry):
        for which in range(2):
            tile_load(i, which).wait()

        @pl.when(i + 1 < wg_ref.shape[2] // W_TILE)
        def _():
            for which in range(2):
                tile_load(i + 1, which).start()

        def rows_step(j, inner):
            rows = pl.ds(pl.multiple_of(j * rows_per, rows_per), rows_per)
            normed = hbuf[rows, :]
            gate = jnp.dot(normed, wtile[i % 2, 0], preferred_element_type=jnp.float32)
            up = jnp.dot(normed, wtile[i % 2, 1], preferred_element_type=jnp.float32)
            hid_ref[rows, pl.ds(pl.multiple_of(i * W_TILE, W_TILE), W_TILE)] = (gate * jax.nn.sigmoid(gate) * up).astype(jnp.bfloat16)
            if spread:
                @pl.when(j == pos_z)
                def _():
                    keep_hidden(i).start()

                @pl.when(j != pos_z)
                def _():
                    give_hidden(j, i, pos_z).start()
            return inner

        lax.fori_loop(0, KV_CHUNKS, rows_step, 0)
        serve(1, i)
        serve(3, i)
        return carry

    lax.fori_loop(0, KV_CHUNKS, gated, 0)
    if not spread:
        for d in range(DIRS):
            for copy in weight_part(0, d):
                copy.wait_recv()
            for copy in weight_part(1, d):
                copy.start()

    scale = LOG2E / math.sqrt(head_dim)
    lanes = row_max.shape[1]

    def attend(key_start, q_half, masked, first):
        rows = pl.ds(q_half * half_rows, half_rows)
        some = pl.ds(key_start, half_rows)
        logits = lax.dot_general(qbuf[rows, :], kv[some, :head_dim], (((1,), (1,)), ((), ())), preferred_element_type=jnp.float32) * scale
        if masked:
            seen = lax.broadcasted_iota(jnp.int32, logits.shape, 0) >= lax.broadcasted_iota(jnp.int32, logits.shape, 1)
            logits = jnp.where(seen, logits, -jnp.inf)
        block_max = jnp.max(logits, axis=-1, keepdims=True)
        if first:
            new_max = jnp.broadcast_to(block_max, (half_rows, lanes))
        else:
            new_max = jnp.maximum(row_max[rows, :], block_max)
        prob = jnp.exp2(logits - jnp.concatenate([new_max] * (half_rows // lanes), axis=1))
        block_sum = jnp.sum(prob, axis=-1, keepdims=True)
        block_out = jnp.dot(prob.astype(jnp.bfloat16), kv[some, head_dim:], preferred_element_type=jnp.float32)
        if first:
            row_sum[rows, :] = jnp.broadcast_to(block_sum, (half_rows, lanes))
            acc[rows, :] = block_out
        else:
            rescale = jnp.exp2(row_max[rows, :] - new_max)
            row_sum[rows, :] = row_sum[rows, :] * rescale + block_sum
            acc[rows, :] = acc[rows, :] * jnp.concatenate([rescale] * (head_dim // lanes), axis=1) + block_out
        row_max[rows, :] = new_max

    own_start = pl.multiple_of(my_seq * tok_count, tok_count)
    attend(own_start, 0, True, True)
    attend(own_start, 1, False, True)
    attend(pl.multiple_of(own_start + half_rows, half_rows), 1, True, False)

    def past(block_chip, block_core):
        def one(n, carry):
            start = pl.multiple_of((block_chip * 2 + block_core) * tok_count + n * half_rows, half_rows)
            attend(start, 0, False, False)
            attend(start, 1, False, False)
            return carry
        lax.fori_loop(0, 2, one, 0)

    def taken(back):
        for i in range(KV_CHUNKS):
            kv_copy(chip - back, 1 - core, i, other, pass_send.at[0, i], core_recv.at[back, i]).wait_recv()

    @pl.when(core == 1)
    def _():
        taken(0)
        past(chip, 0)

    for back in (1, 3, 2):
        if back == 2:
            for i in range(KV_CHUNKS):
                serve(2, i)

        @pl.when(chip >= back)
        def _():
            past(chip - back, core)
            taken(back)
            past(chip - back, 1 - core)

    def finish(i, carry):
        rows = pl.ds(pl.multiple_of(i * rows_per, rows_per), rows_per)
        att_ref[rows, :] = (acc[rows, :] / jnp.concatenate([row_sum[rows, :]] * (head_dim // lanes), axis=1)).astype(jnp.bfloat16)
        if spread:
            @pl.when(i == pos_z)
            def _():
                keep_rows().start()

            @pl.when(i != pos_z)
            def _():
                give_rows(i, pos_z).start()
        return carry

    lax.fori_loop(0, KV_CHUNKS, finish, 0)
    if spread:
        for i in range(KV_CHUNKS):
            keep_hidden(i).wait()
        keep_rows().wait()
        for j in range(1, RING):
            z = (pos_z + j) % RING
            for i in range(KV_CHUNKS):
                give_hidden(z, i, z).wait_recv()
                give_hidden(z, i, pos_z).wait_send()
            give_rows(z, z).wait_recv()
            give_rows(z, pos_z).wait_send()
    else:
        for d in range(DIRS):
            for copy in weight_part(1, d):
                copy.wait_recv()
            for step in range(2):
                for copy in weight_part(step, d):
                    copy.wait_send()
    k_store.wait()
    v_store.wait()
    for i in range(KV_CHUNKS):
        @pl.when(chip < CHIPS - 1)
        def _():
            to_right(i).wait_send()

        @pl.when(chip == 0)
        def _():
            to_wrap(i).wait_send()

        @pl.when(core == 0)
        def _():
            to_other(i).wait_send()

        @pl.when(jnp.logical_and(chip >= 1, chip < CHIPS - 1))
        def _():
            on_right(i).wait_send()

        for back in (1, 2, 3):
            @pl.when(chip >= back)
            def _():
                on_other(back, i).wait_send()


def layer_head(layer, x_cur, cos_t, sin_t, norm_gain, w_q, w_k, w_v, w_gate, w_up, w_down, w_o, spread):
    tok_count, d_model = x_cur.shape
    head_dim = w_q.shape[2]
    ff_local = w_gate.shape[2]
    rows_per = tok_count // KV_CHUNKS
    any_spec = pl.BlockSpec(memory_space=pl.ANY)
    vmem_spec = pl.BlockSpec(memory_space=pltpu.VMEM)
    bf16 = jnp.bfloat16
    rows_shape = jax.ShapeDtypeStruct((tok_count, head_dim), bf16)
    args = (x_cur, cos_t, sin_t, norm_gain, w_q, w_k, w_v, w_gate, w_up)
    in_specs = [any_spec, vmem_spec, vmem_spec, vmem_spec, any_spec, any_spec, any_spec, any_spec, any_spec]
    if spread:
        out_shape = [jax.ShapeDtypeStruct((RING, rows_per, ff_local), bf16), jax.ShapeDtypeStruct((RING, rows_per, head_dim), bf16), rows_shape, rows_shape]
        out_specs = [any_spec] * 4
        extra = [pltpu.VMEM((tok_count, ff_local), bf16), pltpu.VMEM((tok_count, head_dim), bf16), pltpu.SemaphoreType.DMA((RING, KV_CHUNKS + 1)),
                 pltpu.SemaphoreType.DMA((RING, KV_CHUNKS + 1)), pltpu.SemaphoreType.DMA((KV_CHUNKS + 1,))]
    else:
        args += (w_down, w_o)
        in_specs += [any_spec, any_spec]
        out_shape = [jax.ShapeDtypeStruct((tok_count, ff_local), bf16), rows_shape, rows_shape, rows_shape,
                     jax.ShapeDtypeStruct((RING, ff_local, d_model), bf16), jax.ShapeDtypeStruct((RING, head_dim, d_model), bf16)]
        out_specs = [vmem_spec, vmem_spec] + [any_spec] * 4
        extra = [pltpu.SemaphoreType.DMA((2, DIRS, 2)), pltpu.SemaphoreType.DMA((2, DIRS, 2))]
    return pl.pallas_call(
        functools.partial(head_kernel, layer, spread),
        out_shape=out_shape,
        in_specs=in_specs,
        out_specs=out_specs,
        scratch_shapes=extra + [
            pltpu.VMEM((tok_count, d_model), bf16),
            pltpu.VMEM((2, rows_per, d_model), bf16),
            pltpu.VMEM((3, d_model, head_dim), bf16),
            pltpu.VMEM((2, 2, d_model, W_TILE), bf16),
            pltpu.VMEM((2 * CHIPS * tok_count, 2 * head_dim), bf16),
            pltpu.VMEM((tok_count, head_dim), bf16),
            pltpu.VMEM((tok_count, head_dim), jnp.float32),
            pltpu.VMEM((tok_count, 128), jnp.float32),
            pltpu.VMEM((tok_count, 128), jnp.float32),
            pltpu.SemaphoreType.DMA((2,)),
            pltpu.SemaphoreType.DMA((3,)),
            pltpu.SemaphoreType.DMA((2, 2)),
            pltpu.SemaphoreType.DMA((2,)),
            pltpu.SemaphoreType.DMA((3, KV_CHUNKS)),
            pltpu.SemaphoreType.DMA((4, KV_CHUNKS)),
            pltpu.SemaphoreType.DMA((3, KV_CHUNKS)),
            pltpu.SemaphoreType.DMA((4, KV_CHUNKS)),
        ],
        compiler_params=pltpu.CompilerParams(collective_id=2 + layer, has_side_effects=True, vmem_limit_bytes=63 * 1024 * 1024),
        cost_estimate=pl.CostEstimate(flops=2 * tok_count * d_model * (3 * head_dim + 2 * ff_local), bytes_accessed=d_model * (3 * head_dim + 2 * ff_local) * 2, transcendentals=0),
        name='head',
    )(*args)


STEPS = 8
SKEW = 2
W_GROUPS = 4


def tail_kernel(layer, chunk_rows, hid_ref, att_ref, x_ref, wd_ref, wo_ref, gd_in_ref, go_in_ref, out_ref, gd_ref, go_ref,
                part, xbuf, wbuf, recv_a, recv_b, load_sem, store_sem, send_sem, recv_sem, pass_send, pass_recv, side_send, side_recv):
    tok_count, d_model = xbuf.shape
    ff_local = hid_ref.shape[1]
    chunk_count = CHUNKS
    quarter, eighth = chunk_rows // RING, chunk_rows // (2 * RING)
    half_cols = d_model // HALVES
    piece_cols = half_cols // RING
    my_head = lax.axis_index('head')
    pos_z, pos_y = my_head // RING, my_head % RING
    sign = (1, -1)

    def y_peer(d):
        return pos_z * RING + (pos_y + sign[d] + RING) % RING

    def z_peer(d):
        return ((pos_z + sign[d] + RING) % RING) * RING + pos_y

    first_pos, second_pos = (pos_y, pos_z), (pos_z, pos_y)
    first_peer, second_peer = (y_peer, z_peer), (z_peer, y_peer)

    group_cols = d_model // W_GROUPS

    def w_load(g):
        cols = pl.ds(pl.multiple_of(g * group_cols, group_cols), group_cols)
        return (pltpu.make_async_copy(wd_ref.at[layer, :, cols], wbuf.at[pl.ds(0, ff_local), cols], load_sem.at[g, 0]),
                pltpu.make_async_copy(wo_ref.at[layer, 0, :, cols], wbuf.at[pl.ds(ff_local, wo_ref.shape[2]), cols], load_sem.at[g, 1]))

    x_load = pltpu.make_async_copy(x_ref, xbuf, load_sem.at[W_GROUPS, 0])
    for g in range(W_GROUPS):
        for load in w_load(g):
            load.start()
    x_load.start()
    barrier = pltpu.get_barrier_semaphore()
    for peer in (y_peer, z_peer):
        for d in range(DIRS):
            pl.semaphore_signal(barrier, inc=1, device_id={'head': peer(d)}, device_id_type=pl.DeviceIdType.MESH)
    my_seq = lax.axis_index('seq')
    chip, core = my_seq // 2, my_seq % 2
    other = chip * 2 + 1 - core

    def x_chip(n):
        return (chip + n + CHIPS) % CHIPS

    for peer in (x_chip(1) * 2 + core, x_chip(-1) * 2 + core, other):
        pl.semaphore_signal(barrier, inc=1, device_id={'seq': peer}, device_id_type=pl.DeviceIdType.MESH)
    pl.semaphore_wait(barrier, 2 * DIRS + 3)

    def weight_copies(j, part_chip, part_core, half, send, recv, to):
        copies = []
        for n, ref in enumerate((gd_ref, go_ref)):
            size = ref.shape[1] // (2 * CHIPS)
            start = (part_chip * 2 + part_core) * size
            if half is None:
                rows = pl.ds(pl.multiple_of(start, size), size)
            else:
                rows = pl.ds(pl.multiple_of(start + half * (size // 2), size // 2), size // 2)
            place = ref.at[(pos_z + j) % RING, rows, :]
            copies.append(pltpu.make_async_remote_copy(src_ref=place, dst_ref=place, send_sem=send.at[n], recv_sem=recv.at[n], device_id={'seq': to}, device_id_type=pl.DeviceIdType.MESH))
        return copies

    def own_pass(j, d):
        return weight_copies(j, chip, core, None, pass_send.at[0, j - 1, d], pass_recv.at[0, j - 1, d], x_chip(sign[d]) * 2 + core)

    def far_pass(j, d):
        return weight_copies(j, x_chip(-sign[d]), core, d, pass_send.at[1, j - 1, d], pass_recv.at[1, j - 1, d], x_chip(sign[d]) * 2 + core)

    def side_pass(j, n, side):
        return weight_copies(j, x_chip(n), side, None, side_send.at[j - 1, n], side_recv.at[j - 1, n], other)

    def serve_near(j):
        for d in range(DIRS):
            for copy in own_pass(j, d):
                copy.wait_recv()
            for copy in far_pass(j, d) + side_pass(j, 3 if d == 0 else 1, core):
                copy.start()

    def serve_far(j):
        for d in range(DIRS):
            for copy in far_pass(j, d):
                copy.wait_recv()
        for copy in side_pass(j, 2, core):
            copy.start()

    for j in range(1, RING):
        for d in range(DIRS):
            for copy in own_pass(j, d):
                copy.start()
        for copy in side_pass(j, 0, core):
            copy.start()

    def rows_of(chunk, piece, offset, count):
        return pl.ds(pl.multiple_of(chunk * chunk_rows + piece * quarter + offset, eighth), count)

    def cols_of(h, piece):
        return pl.ds(pl.multiple_of(h * half_cols + piece * piece_cols, piece_cols), piece_cols)

    def half_of(h):
        return pl.ds(h * half_cols, half_cols)

    def message(step, chunk, h, d):
        p1, p2, s = first_pos[h], second_pos[h], sign[d]
        far1, near1, behind1 = (p1 + 2) % RING, (p1 + s + RING) % RING, (p1 - s + RING) % RING
        far2, near2, behind2 = (p2 + 2) % RING, (p2 + s + RING) % RING, (p2 - s + RING) % RING
        if step == 0:
            src, dst = part.at[rows_of(chunk, far1, d * eighth, eighth), half_of(h)], recv_a.at[chunk, h, d, pl.ds(quarter, eighth), :]
        elif step == 1:
            src, dst = part.at[rows_of(chunk, near1, 0, quarter), half_of(h)], recv_a.at[chunk, h, d, pl.ds(0, quarter), :]
        elif step == 2:
            src, dst = part.at[rows_of(chunk, p1, d * eighth, eighth), cols_of(h, far2)], recv_b.at[chunk, h, d, pl.ds(quarter, eighth), :]
        elif step == 3:
            src, dst = part.at[rows_of(chunk, p1, 0, quarter), cols_of(h, near2)], recv_b.at[chunk, h, d, pl.ds(0, quarter), :]
        elif step == 4:
            src = dst = xbuf.at[rows_of(chunk, p1, 0, quarter), cols_of(h, p2)]
        elif step == 5:
            src = dst = xbuf.at[rows_of(chunk, p1, d * eighth, eighth), cols_of(h, behind2)]
        elif step == 6:
            src = dst = xbuf.at[rows_of(chunk, p1, 0, quarter), half_of(h)]
        else:
            src = dst = xbuf.at[rows_of(chunk, behind1, d * eighth, eighth), half_of(h)]
        peer = (first_peer if step in (0, 1, 6, 7) else second_peer)[h](d)
        return pltpu.make_async_remote_copy(
            src_ref=src, dst_ref=dst, send_sem=send_sem.at[chunk, step, h * DIRS + d], recv_sem=recv_sem.at[chunk, step, h * DIRS + d],
            device_id={'head': peer}, device_id_type=pl.DeviceIdType.MESH)

    def project(chunk):
        rows = pl.ds(pl.multiple_of(chunk * chunk_rows, chunk_rows), chunk_rows)

        def one_tile(i, carry):
            cols = pl.ds(pl.multiple_of(i * piece_cols, piece_cols), piece_cols)
            per_group = group_cols // piece_cols

            @pl.when(jnp.logical_and(chunk == 0, i % per_group == 0))
            def _():
                for load in w_load(i // per_group):
                    load.wait()

            total = jnp.dot(hid_ref[rows, :], wbuf[:ff_local, cols], preferred_element_type=jnp.float32)
            part[rows, cols] = total + jnp.dot(att_ref[rows, :], wbuf[ff_local:, cols], preferred_element_type=jnp.float32)
            return carry

        lax.fori_loop(0, d_model // piece_cols, one_tile, 0)

    def store(chunk):
        rows = pl.ds(pl.multiple_of(chunk * chunk_rows, chunk_rows), chunk_rows)
        return pltpu.make_async_copy(xbuf.at[rows, :], out_ref.at[rows, :], store_sem.at[chunk])

    def stage(number, chunk):
        if number == 0:
            project(chunk)
        if number == 1:
            @pl.when(chunk == 0)
            def _():
                x_load.wait()
        for h in range(HALVES):
            p1, p2 = first_pos[h], second_pos[h]
            if number:
                for d in range(DIRS):
                    message(number - 1, chunk, h, d).wait_recv()
            if number in (1, 3):
                for d in range(DIRS):
                    if number == 1:
                        rows, cols, arrived = rows_of(chunk, (p1 + sign[d] + RING) % RING, d * eighth, eighth), half_of(h), recv_a
                    else:
                        rows, cols, arrived = rows_of(chunk, p1, d * eighth, eighth), cols_of(h, (p2 + sign[d] + RING) % RING), recv_b
                    part[rows, cols] = part[rows, cols] + arrived[chunk, h, d, pl.ds(quarter, eighth), :]
            if number == 2:
                rows = rows_of(chunk, p1, 0, quarter)
                part[rows, half_of(h)] = part[rows, half_of(h)] + recv_a[chunk, h, 0, pl.ds(0, quarter), :] + recv_a[chunk, h, 1, pl.ds(0, quarter), :]
            if number == 4:
                rows, cols = rows_of(chunk, p1, 0, quarter), cols_of(h, p2)
                total = part[rows, cols] + recv_b[chunk, h, 0, pl.ds(0, quarter), :] + recv_b[chunk, h, 1, pl.ds(0, quarter), :]
                update = total.astype(jnp.bfloat16).astype(jnp.float32)
                xbuf[rows, cols] = (xbuf[rows, cols].astype(jnp.float32) + update).astype(jnp.bfloat16)
            if number < STEPS:
                for d in range(DIRS):
                    message(number, chunk, h, d).start()
        if number == STEPS:
            store(chunk).start()

    def tick(t, carry):
        for number in range(STEPS, -1, -1):
            chunk = t - SKEW * number

            @pl.when(jnp.logical_and(chunk >= 0, chunk < chunk_count))
            def _():
                stage(number, chunk)
        for j in range(1, RING):
            @pl.when(t == NEAR_TICKS[j - 1])
            def _():
                serve_near(j)

            @pl.when(t == FAR_TICKS[j - 1])
            def _():
                serve_far(j)
        return carry

    lax.fori_loop(0, CHUNKS + SKEW * STEPS, tick, 0)

    def drain(chunk, carry):
        for step in range(STEPS):
            for h in range(HALVES):
                for d in range(DIRS):
                    message(step, chunk, h, d).wait_send()
        store(chunk).wait()
        return carry

    lax.fori_loop(0, chunk_count, drain, 0)
    for j in range(1, RING):
        for d in range(DIRS):
            for copy in own_pass(j, d) + far_pass(j, d):
                copy.wait_send()
        for n in range(CHIPS):
            for copy in side_pass(j, n, 1 - core):
                copy.wait_recv()
            for copy in side_pass(j, n, core):
                copy.wait_send()


def layer_tail(layer, hidden, attn_heads, x_cur, w_down, w_o, all_down, all_out):
    tok_count, d_model = x_cur.shape
    chunk_rows = tok_count // CHUNKS
    depth = hidden.shape[1] + attn_heads.shape[1]
    landed = 3 * chunk_rows // (2 * RING)
    any_spec = pl.BlockSpec(memory_space=pl.ANY)
    vmem_spec = pl.BlockSpec(memory_space=pltpu.VMEM)
    return pl.pallas_call(
        functools.partial(tail_kernel, layer, chunk_rows),
        out_shape=[jax.ShapeDtypeStruct((tok_count, d_model), jnp.bfloat16), jax.ShapeDtypeStruct(all_down.shape, jnp.bfloat16), jax.ShapeDtypeStruct(all_out.shape, jnp.bfloat16)],
        in_specs=[vmem_spec, vmem_spec] + [any_spec] * 5,
        out_specs=[any_spec] * 3,
        input_output_aliases={5: 1, 6: 2},
        scratch_shapes=[
            pltpu.VMEM((tok_count, d_model), jnp.float32),
            pltpu.VMEM((tok_count, d_model), jnp.bfloat16),
            pltpu.VMEM((depth, d_model), jnp.bfloat16),
            pltpu.VMEM((CHUNKS, HALVES, DIRS, landed, d_model // HALVES), jnp.float32),
            pltpu.VMEM((CHUNKS, HALVES, DIRS, landed, d_model // HALVES // RING), jnp.float32),
            pltpu.SemaphoreType.DMA((W_GROUPS + 1, 2)),
            pltpu.SemaphoreType.DMA((CHUNKS,)),
            pltpu.SemaphoreType.DMA((CHUNKS, STEPS, HALVES * DIRS)),
            pltpu.SemaphoreType.DMA((CHUNKS, STEPS, HALVES * DIRS)),
            pltpu.SemaphoreType.DMA((2, RING - 1, DIRS, 2)),
            pltpu.SemaphoreType.DMA((2, RING - 1, DIRS, 2)),
            pltpu.SemaphoreType.DMA((RING - 1, CHIPS, 2)),
            pltpu.SemaphoreType.DMA((RING - 1, CHIPS, 2)),
        ],
        compiler_params=pltpu.CompilerParams(collective_id=layer, has_side_effects=True, vmem_limit_bytes=63 * 1024 * 1024),
        cost_estimate=pl.CostEstimate(flops=2 * tok_count * depth * d_model, bytes_accessed=depth * d_model * 2, transcendentals=0),
        name='tail',
    )(hidden, attn_heads, x_cur, w_down, w_o, all_down, all_out)


LAST_STEPS = 6
LAST_COLS = 256


def last_kernel(layer, hid_ref, att_ref, x_ref, wd_ref, wo_ref, gd_ref, go_ref, out_ref, part, xres, xbuf, wtile, landed, w_sem, x_sem, store_sem, send_sem, recv_sem):
    rows, d_model = part.shape
    block = wtile.shape[3]
    block_count = d_model // block
    ff_local = hid_ref.shape[2]
    quarter, eighth = rows // RING, rows // (2 * RING)
    my_head = lax.axis_index('head')
    pos_z, pos_y = my_head // RING, my_head % RING
    sign = (1, -1)

    def cols_of(c):
        return pl.ds(pl.multiple_of(c * block, block), block)

    def w_loads(c):
        copies = []
        for j in range(RING):
            z = (pos_z + j) % RING
            down = wd_ref.at[layer, :, cols_of(c)] if j == 0 else gd_ref.at[z, :, cols_of(c)]
            out = wo_ref.at[layer, 0, :, cols_of(c)] if j == 0 else go_ref.at[z, :, cols_of(c)]
            copies.append(pltpu.make_async_copy(down, wtile.at[c % 2, j, pl.ds(0, ff_local), :], w_sem.at[c % 2, j, 0]))
            copies.append(pltpu.make_async_copy(out, wtile.at[c % 2, j, pl.ds(ff_local, wo_ref.shape[2]), :], w_sem.at[c % 2, j, 1]))
        return copies

    for copy in w_loads(0):
        copy.start()
    x_load = pltpu.make_async_copy(x_ref.at[pl.ds(pl.multiple_of(pos_z * rows + pos_y * quarter, quarter), quarter), :], xres, x_sem)
    x_load.start()

    def y_device(d):
        return pos_z * RING + (pos_y + sign[d] + RING) % RING

    def z_device(d):
        return (pos_z + sign[d] + RING) % RING * RING + pos_y

    barrier = pltpu.get_barrier_semaphore()
    for device in (y_device, z_device):
        for d in range(DIRS):
            pl.semaphore_signal(barrier, inc=1, device_id={'head': device(d)}, device_id_type=pl.DeviceIdType.MESH)
    pl.semaphore_wait(barrier, 2 * DIRS)
    x_load.wait()

    def rows_of(piece, offset, count):
        return pl.ds(pl.multiple_of(piece * quarter + offset, eighth), count)

    def message(step, c, d):
        s = sign[d]
        near, behind = (pos_y + s + RING) % RING, (pos_y - s + RING) % RING
        if step == 0:
            src, dst = part.at[rows_of((pos_y + 2) % RING, d * eighth, eighth), cols_of(c)], landed.at[c, d, pl.ds(quarter, eighth), :]
        elif step == 1:
            src, dst = part.at[rows_of(near, 0, quarter), cols_of(c)], landed.at[c, d, pl.ds(0, quarter), :]
        elif step == 2:
            src = dst = xbuf.at[pos_z, rows_of(pos_y, 0, quarter), cols_of(c)]
        elif step == 3:
            src = dst = xbuf.at[pos_z, rows_of(behind, d * eighth, eighth), cols_of(c)]
        elif step == 4:
            src = dst = xbuf.at[pos_z, :, cols_of(c)]
        else:
            src = dst = xbuf.at[(pos_z - s + RING) % RING, pl.ds(d * (rows // 2), rows // 2), cols_of(c)]
        return pltpu.make_async_remote_copy(
            src_ref=src, dst_ref=dst, send_sem=send_sem.at[c, step, d], recv_sem=recv_sem.at[c, step, d],
            device_id={'head': (y_device if step < 4 else z_device)(d)}, device_id_type=pl.DeviceIdType.MESH)

    def store(c):
        return pltpu.make_async_copy(xbuf.at[:, :, cols_of(c)], out_ref.at[:, :, cols_of(c)], store_sem.at[c])

    def project(c):
        @pl.when(c + 1 < block_count)
        def _():
            for copy in w_loads(c + 1):
                copy.start()

        for copy in w_loads(c):
            copy.wait()
        total = None
        for j in range(RING):
            z = (pos_z + j) % RING
            down = jnp.dot(hid_ref[z], wtile[c % 2, j, :ff_local, :], preferred_element_type=jnp.float32)
            down = down + jnp.dot(att_ref[z], wtile[c % 2, j, ff_local:, :], preferred_element_type=jnp.float32)
            total = down if total is None else total + down
        part[:, cols_of(c)] = total

    def stage(number, c):
        if number == 0:
            project(c)
        else:
            for d in range(DIRS):
                message(number - 1, c, d).wait_recv()
        if number == 1:
            for d in range(DIRS):
                piece = rows_of((pos_y + sign[d] + RING) % RING, d * eighth, eighth)
                part[piece, cols_of(c)] = part[piece, cols_of(c)] + landed[c, d, pl.ds(quarter, eighth), :]
        if number == 2:
            own = rows_of(pos_y, 0, quarter)
            total = part[own, cols_of(c)] + landed[c, 0, pl.ds(0, quarter), :] + landed[c, 1, pl.ds(0, quarter), :]
            update = total.astype(jnp.bfloat16).astype(jnp.float32)
            xbuf[pos_z, own, cols_of(c)] = (xres[:, cols_of(c)].astype(jnp.float32) + update).astype(jnp.bfloat16)
        if number < LAST_STEPS:
            for d in range(DIRS):
                message(number, c, d).start()
        else:
            store(c).start()

    def tick(t, carry):
        for number in range(LAST_STEPS, -1, -1):
            c = t - SKEW * number

            @pl.when(jnp.logical_and(c >= 0, c < block_count))
            def _():
                stage(number, c)
        return carry

    lax.fori_loop(0, block_count + SKEW * LAST_STEPS, tick, 0)

    def drain(c, carry):
        for step in range(LAST_STEPS):
            for d in range(DIRS):
                message(step, c, d).wait_send()
        store(c).wait()
        return carry

    lax.fori_loop(0, block_count, drain, 0)


def layer_last(layer, hid_all, att_all, x_cur, w_down, w_o, all_down, all_out):
    tok_count, d_model = x_cur.shape
    rows = tok_count // RING
    depth = hid_all.shape[2] + att_all.shape[2]
    any_spec = pl.BlockSpec(memory_space=pl.ANY)
    vmem_spec = pl.BlockSpec(memory_space=pltpu.VMEM)
    blocks = d_model // LAST_COLS
    out = pl.pallas_call(
        functools.partial(last_kernel, layer),
        out_shape=jax.ShapeDtypeStruct((RING, rows, d_model), jnp.bfloat16),
        in_specs=[vmem_spec, vmem_spec] + [any_spec] * 5,
        out_specs=any_spec,
        scratch_shapes=[
            pltpu.VMEM((rows, d_model), jnp.float32),
            pltpu.VMEM((rows // RING, d_model), jnp.bfloat16),
            pltpu.VMEM((RING, rows, d_model), jnp.bfloat16),
            pltpu.VMEM((2, RING, depth, LAST_COLS), jnp.bfloat16),
            pltpu.VMEM((blocks, DIRS, 3 * rows // (2 * RING), LAST_COLS), jnp.float32),
            pltpu.SemaphoreType.DMA((2, RING, 2)),
            pltpu.SemaphoreType.DMA,
            pltpu.SemaphoreType.DMA((blocks,)),
            pltpu.SemaphoreType.DMA((blocks, LAST_STEPS, DIRS)),
            pltpu.SemaphoreType.DMA((blocks, LAST_STEPS, DIRS)),
        ],
        compiler_params=pltpu.CompilerParams(collective_id=layer, has_side_effects=True, vmem_limit_bytes=63 * 1024 * 1024),
        cost_estimate=pl.CostEstimate(flops=2 * tok_count * depth * d_model, bytes_accessed=4 * depth * d_model * 2, transcendentals=0),
        name='last',
    )(hid_all, att_all, x_cur, w_down, w_o, all_down, all_out)
    return out.reshape(tok_count, d_model)


def solution(mesh):
    row_spec = P(('batch', 'seq'), None)
    pos_spec = P(('batch', 'seq'))
    head_spec = P(None, None, 'head', None)
    out_proj_spec = P(None, 'head', None, None)
    col_spec = P(None, None, 'head')
    down_spec = P(None, 'head', None)
    cache_spec = P(None, ('batch', 'seq'), 'head', None)

    def local_forward(x_loc, pos_loc, w_q, w_k, w_v, w_o, w_gate, w_up, w_down, norm_gain):
        tok_count, d_model = x_loc.shape
        layer_count = w_q.shape[0]
        head_dim = w_q.shape[3]
        flat_q, flat_k, flat_v = (w.reshape(layer_count, d_model, head_dim) for w in (w_q, w_k, w_v))
        cos_t, sin_t = rope_tables(pos_loc, head_dim)
        hidden, attn_heads, k_first, v_first, all_down, all_out = layer_head(0, x_loc, cos_t, sin_t, norm_gain, flat_q, flat_k, flat_v, w_gate, w_up, w_down, w_o, False)
        x_mid, all_down, all_out = layer_tail(0, hidden, attn_heads, x_loc, w_down, w_o, all_down, all_out)
        hid_all, att_all, k_second, v_second = layer_head(1, x_mid, cos_t, sin_t, norm_gain, flat_q, flat_k, flat_v, w_gate, w_up, w_down, w_o, True)
        x_out = layer_last(1, hid_all, att_all, x_mid, w_down, w_o, all_down, all_out)
        caches = [jnp.stack([a.reshape(tok_count, 1, head_dim), b.reshape(tok_count, 1, head_dim)]) for a, b in ((k_first, k_second), (v_first, v_second))]
        return x_out, caches[0], caches[1]

    return jax.shard_map(local_forward, mesh=mesh, in_specs=(row_spec, pos_spec, head_spec, head_spec, head_spec, out_proj_spec, col_spec, col_spec, down_spec, P(None, None)), out_specs=(row_spec, cache_spec, cache_spec), check_vma=False)
```

```python
import functools
import math
import jax
import jax.numpy as jnp
from jax import lax
from jax.experimental import pallas as pl
from jax.experimental.pallas import tpu as pltpu
from jax.sharding import PartitionSpec as P

ROPE_BASE = 500000.0
EPS = 1e-5


def rope_tables(positions, head_dim):
    half_dim = head_dim // 2
    inv_freq = ROPE_BASE ** (-(jnp.arange(half_dim, dtype=jnp.float32) * 2.0 / head_dim))
    angles = positions.astype(jnp.float32)[..., None] * inv_freq
    return jnp.cos(angles), jnp.sin(angles)


LOG2E = 1.4426950408889634
CHUNKS = 8
NEAR_TICKS = (6, 9, 13)
FAR_TICKS = (16, 19, 23)


CHIPS = 4
RING = 4
HALVES = 2
DIRS = 2
KV_CHUNKS = 4
W_TILE = 256
NORM_ROWS = 64


def head_kernel(layer, spread, *refs):
    x_ref, cos_ref, sin_ref, gain_ref, wq_ref, wk_ref, wv_ref, wg_ref, wu_ref = refs[:9]
    if spread:
        hid_all_ref, att_all_ref, k_ref, v_ref, hid_ref, att_ref, give_send, give_recv, keep_sem = refs[9:18]
    else:
        wd_ref, wo_ref, hid_ref, att_ref, k_ref, v_ref, gd_ref, go_ref, give_send, give_recv = refs[9:19]
    hbuf, xs, wqkv, wtile, kv, qbuf, acc, row_max, row_sum, x_sem, w_sem, t_sem, out_sem, own_send, pass_send, ici_recv, core_recv = refs[-17:]
    my_head = lax.axis_index('head')
    pos_z, pos_y = my_head // RING, my_head % RING
    sign = (1, -1)

    def z_device(z):
        return (z + RING) % RING * RING + pos_y

    tok_count, d_model = hbuf.shape
    head_dim = qbuf.shape[1]
    half_dim = head_dim // 2
    rows_per = tok_count // KV_CHUNKS
    half_rows = tok_count // 2
    my_seq = lax.axis_index('seq')
    chip, core = my_seq // 2, my_seq % 2
    other = chip * 2 + 1 - core
    right = ((chip + 1) % CHIPS) * 2 + core
    left = ((chip + CHIPS - 1) % CHIPS) * 2 + core

    def x_load(i):
        return pltpu.make_async_copy(x_ref.at[pl.ds(pl.multiple_of(i * rows_per, rows_per), rows_per), :], xs.at[i % 2], x_sem.at[i % 2])

    def tile_load(i, which):
        ref = (wg_ref, wu_ref)[which]
        return pltpu.make_async_copy(ref.at[layer, :, pl.ds(pl.multiple_of(i * W_TILE, W_TILE), W_TILE)], wtile.at[i % 2, which], t_sem.at[i % 2, which])

    x_load(0).start()
    w_loads = [pltpu.make_async_copy(ref.at[layer], wqkv.at[n], w_sem.at[n]) for n, ref in enumerate((wk_ref, wv_ref, wq_ref))]
    for load in w_loads:
        load.start()
    x_load(1).start()
    for which in range(2):
        tile_load(0, which).start()

    barrier = pltpu.get_barrier_semaphore()
    for peer in (left, right, other):
        pl.semaphore_signal(barrier, inc=1, device_id={'seq': peer}, device_id_type=pl.DeviceIdType.MESH)
    for j in range(1, RING):
        pl.semaphore_signal(barrier, inc=1, device_id={'head': z_device(pos_z + j)}, device_id_type=pl.DeviceIdType.MESH)
    pl.semaphore_wait(barrier, 6)

    def weight_part(step, d):
        copies = []
        for n, (own_ref, all_ref) in enumerate(((wd_ref, gd_ref), (wo_ref, go_ref))):
            size = all_ref.shape[1] // (2 * CHIPS)
            if step == 0:
                rows = pl.ds(pl.multiple_of(my_seq * size, size), size)
                src = own_ref.at[layer + 1, rows, :] if n == 0 else own_ref.at[layer + 1, 0, rows, :]
                dst = all_ref.at[pos_z, rows, :]
            else:
                rows = pl.ds(pl.multiple_of(my_seq * size + d * (size // 2), size // 2), size // 2)
                src = dst = all_ref.at[(pos_z - sign[d] + RING) % RING, rows, :]
            copies.append(pltpu.make_async_remote_copy(
                src_ref=src, dst_ref=dst, send_sem=give_send.at[step, d, n], recv_sem=give_recv.at[step, d, n],
                device_id={'head': z_device(pos_z + sign[d])}, device_id_type=pl.DeviceIdType.MESH))
        return copies

    def give(src, dst, send, recv, z):
        return pltpu.make_async_remote_copy(src_ref=src, dst_ref=dst, send_sem=send, recv_sem=recv, device_id={'head': z_device(z)}, device_id_type=pl.DeviceIdType.MESH)

    def give_hidden(z, i, source):
        rows = pl.ds(pl.multiple_of(z * rows_per, rows_per), rows_per)
        cols = pl.ds(pl.multiple_of(i * W_TILE, W_TILE), W_TILE)
        return give(hid_ref.at[rows, cols], hid_all_ref.at[source, :, cols], give_send.at[z, i], give_recv.at[source, i], z)

    def keep_hidden(i):
        rows = pl.ds(pl.multiple_of(pos_z * rows_per, rows_per), rows_per)
        cols = pl.ds(pl.multiple_of(i * W_TILE, W_TILE), W_TILE)
        return pltpu.make_async_copy(hid_ref.at[rows, cols], hid_all_ref.at[pos_z, :, cols], keep_sem.at[i])

    def give_rows(z, source):
        rows = pl.ds(pl.multiple_of(z * rows_per, rows_per), rows_per)
        return give(att_ref.at[rows, :], att_all_ref.at[source], give_send.at[z, KV_CHUNKS], give_recv.at[source, KV_CHUNKS], z)

    def keep_rows():
        rows = pl.ds(pl.multiple_of(pos_z * rows_per, rows_per), rows_per)
        return pltpu.make_async_copy(att_ref.at[rows, :], att_all_ref.at[pos_z], keep_sem.at[KV_CHUNKS])

    if not spread:
        for d in range(DIRS):
            for copy in weight_part(0, d):
                copy.start()

    def kv_copy(origin_chip, origin_core, i, to, send, recv):
        rows = kv.at[pl.ds(pl.multiple_of((origin_chip * 2 + origin_core) * tok_count + i * rows_per, rows_per), rows_per), :]
        return pltpu.make_async_remote_copy(src_ref=rows, dst_ref=rows, send_sem=send, recv_sem=recv, device_id={'seq': to}, device_id_type=pl.DeviceIdType.MESH)

    def to_right(i):
        return kv_copy(chip, core, i, right, own_send.at[0, i], ici_recv.at[0, i])

    def to_wrap(i):
        return kv_copy(chip, core, i, left, own_send.at[1, i], ici_recv.at[2, i])

    def to_other(i):
        return kv_copy(chip, core, i, other, own_send.at[2, i], core_recv.at[0, i])

    def on_right(i):
        return kv_copy(chip - 1, core, i, right, pass_send.at[0, i], ici_recv.at[1, i])

    def to_relay(i):
        return kv_copy(chip, core, i, left, own_send.at[3, i], ici_recv.at[3, i])

    def from_relay(i):
        return kv_copy(1, core, i, left, pass_send.at[0, i], ici_recv.at[1, i])

    def on_left(i):
        return kv_copy(0, core, i, left, pass_send.at[0, i], ici_recv.at[1, i])

    def relay(i):
        @pl.when(chip == 0)
        def _():
            kv_copy(1, core, i, left, own_send.at[3, i], ici_recv.at[3, i]).wait_recv()
            from_relay(i).start()

    def on_other(back, i):
        return kv_copy(chip - back, core, i, other, pass_send.at[back, i], core_recv.at[back, i])

    def arrival(back, i):
        return kv_copy(chip - back, core, i, other, pass_send.at[back, i], ici_recv.at[back - 1, i])

    def serve(back, i):
        @pl.when(chip >= back)
        def _():
            arrival(back, i).wait_recv()
            on_other(back, i).start()
        if back == 1:
            @pl.when(jnp.logical_and(i < KV_CHUNKS // 2, jnp.logical_and(chip >= 1, chip < CHIPS - 1)))
            def _():
                on_right(i).start()
        if back == 3:
            @pl.when(jnp.logical_and(i >= KV_CHUNKS // 2, chip == CHIPS - 1))
            def _():
                on_left(i).start()

    def rope(values, rows):
        cos_t, sin_t = cos_ref[rows, :], sin_ref[rows, :]
        wide = values.astype(jnp.bfloat16).astype(jnp.float32)
        first, second = wide[:, :half_dim], wide[:, half_dim:]
        return jnp.concatenate([first * cos_t - second * sin_t, second * cos_t + first * sin_t], axis=1).astype(jnp.bfloat16)

    gain = gain_ref[pl.ds(layer, 1), :].astype(jnp.float32)

    def prepare(i, carry):
        x_load(i).wait()
        rows = pl.ds(pl.multiple_of(i * rows_per, rows_per), rows_per)

        def norm(j, inner):
            few = pl.ds(pl.multiple_of(j * NORM_ROWS, NORM_ROWS), NORM_ROWS)
            x_f32 = xs[i % 2, few, :].astype(jnp.float32)
            inv_rms = lax.rsqrt(jnp.mean(x_f32 * x_f32, axis=-1, keepdims=True) + EPS)
            hbuf[pl.ds(pl.multiple_of(i * rows_per + j * NORM_ROWS, NORM_ROWS), NORM_ROWS), :] = (x_f32 * inv_rms * gain).astype(jnp.bfloat16)
            return inner

        lax.fori_loop(0, rows_per // NORM_ROWS, norm, 0)

        @pl.when(i + 2 < KV_CHUNKS)
        def _():
            x_load(i + 2).start()

        @pl.when(i == 0)
        def _():
            w_loads[0].wait()
            w_loads[1].wait()

        normed = hbuf[rows, :]
        own = pl.ds(pl.multiple_of(my_seq * tok_count + i * rows_per, rows_per), rows_per)
        kv[own, :head_dim] = rope(jnp.dot(normed, wqkv[0], preferred_element_type=jnp.float32), rows)
        kv[own, head_dim:] = jnp.dot(normed, wqkv[1], preferred_element_type=jnp.float32).astype(jnp.bfloat16)

        @pl.when(chip < CHIPS - 1)
        def _():
            to_right(i).start()

        @pl.when(chip == 0)
        def _():
            to_wrap(i).start()

        @pl.when(jnp.logical_and(i >= KV_CHUNKS // 2, chip == 1))
        def _():
            to_relay(i).start()

        @pl.when(core == 0)
        def _():
            to_other(i).start()
        return carry

    lax.fori_loop(0, KV_CHUNKS, prepare, 0)
    w_loads[2].wait()
    own_rows = pl.ds(pl.multiple_of(my_seq * tok_count, tok_count), tok_count)
    k_store = pltpu.make_async_copy(kv.at[own_rows, pl.ds(0, head_dim)], k_ref, out_sem.at[0])
    v_store = pltpu.make_async_copy(kv.at[own_rows, pl.ds(head_dim, head_dim)], v_ref, out_sem.at[1])
    k_store.start()
    v_store.start()

    def query(i, carry):
        rows = pl.ds(pl.multiple_of(i * rows_per, rows_per), rows_per)
        qbuf[rows, :] = rope(jnp.dot(hbuf[rows, :], wqkv[2], preferred_element_type=jnp.float32), rows)
        return carry

    lax.fori_loop(0, KV_CHUNKS, query, 0)

    def gated(i, carry):
        for which in range(2):
            tile_load(i, which).wait()

        @pl.when(i + 1 < wg_ref.shape[2] // W_TILE)
        def _():
            for which in range(2):
                tile_load(i + 1, which).start()

        def rows_step(j, inner):
            rows = pl.ds(pl.multiple_of(j * rows_per, rows_per), rows_per)
            normed = hbuf[rows, :]
            gate = jnp.dot(normed, wtile[i % 2, 0], preferred_element_type=jnp.float32)
            up = jnp.dot(normed, wtile[i % 2, 1], preferred_element_type=jnp.float32)
            hid_ref[rows, pl.ds(pl.multiple_of(i * W_TILE, W_TILE), W_TILE)] = (gate * jax.nn.sigmoid(gate) * up).astype(jnp.bfloat16)
            if spread:
                @pl.when(j == pos_z)
                def _():
                    keep_hidden(i).start()

                @pl.when(j != pos_z)
                def _():
                    give_hidden(j, i, pos_z).start()
            return inner

        lax.fori_loop(0, KV_CHUNKS, rows_step, 0)
        serve(1, i)
        serve(3, i)

        @pl.when(i >= KV_CHUNKS // 2)
        def _():
            relay(i)
        return carry

    lax.fori_loop(0, KV_CHUNKS, gated, 0)
    if not spread:
        for d in range(DIRS):
            for copy in weight_part(0, d):
                copy.wait_recv()
            for copy in weight_part(1, d):
                copy.start()

    scale = LOG2E / math.sqrt(head_dim)
    lanes = row_max.shape[1]

    def attend(key_start, q_half, masked, first):
        rows = pl.ds(q_half * half_rows, half_rows)
        some = pl.ds(key_start, half_rows)
        logits = lax.dot_general(qbuf[rows, :], kv[some, :head_dim], (((1,), (1,)), ((), ())), preferred_element_type=jnp.float32) * scale
        if masked:
            seen = lax.broadcasted_iota(jnp.int32, logits.shape, 0) >= lax.broadcasted_iota(jnp.int32, logits.shape, 1)
            logits = jnp.where(seen, logits, -jnp.inf)
        block_max = jnp.max(logits, axis=-1, keepdims=True)
        if first:
            new_max = jnp.broadcast_to(block_max, (half_rows, lanes))
        else:
            new_max = jnp.maximum(row_max[rows, :], block_max)
        prob = jnp.exp2(logits - jnp.concatenate([new_max] * (half_rows // lanes), axis=1))
        block_sum = jnp.sum(prob, axis=-1, keepdims=True)
        block_out = jnp.dot(prob.astype(jnp.bfloat16), kv[some, head_dim:], preferred_element_type=jnp.float32)
        if first:
            row_sum[rows, :] = jnp.broadcast_to(block_sum, (half_rows, lanes))
            acc[rows, :] = block_out
        else:
            rescale = jnp.exp2(row_max[rows, :] - new_max)
            row_sum[rows, :] = row_sum[rows, :] * rescale + block_sum
            acc[rows, :] = acc[rows, :] * jnp.concatenate([rescale] * (head_dim // lanes), axis=1) + block_out
        row_max[rows, :] = new_max

    own_start = pl.multiple_of(my_seq * tok_count, tok_count)
    attend(own_start, 0, True, True)
    attend(own_start, 1, False, True)
    attend(pl.multiple_of(own_start + half_rows, half_rows), 1, True, False)

    def past(block_chip, block_core):
        def one(n, carry):
            start = pl.multiple_of((block_chip * 2 + block_core) * tok_count + n * half_rows, half_rows)
            attend(start, 0, False, False)
            attend(start, 1, False, False)
            return carry
        lax.fori_loop(0, 2, one, 0)

    def taken(back):
        for i in range(KV_CHUNKS):
            kv_copy(chip - back, 1 - core, i, other, pass_send.at[0, i], core_recv.at[back, i]).wait_recv()

    @pl.when(core == 1)
    def _():
        taken(0)
        past(chip, 0)

    for back in (1, 3, 2):
        if back == 2:
            for i in range(KV_CHUNKS):
                serve(2, i)

        @pl.when(chip >= back)
        def _():
            past(chip - back, core)
            taken(back)
            past(chip - back, 1 - core)

    def finish(i, carry):
        rows = pl.ds(pl.multiple_of(i * rows_per, rows_per), rows_per)
        att_ref[rows, :] = (acc[rows, :] / jnp.concatenate([row_sum[rows, :]] * (head_dim // lanes), axis=1)).astype(jnp.bfloat16)
        if spread:
            @pl.when(i == pos_z)
            def _():
                keep_rows().start()

            @pl.when(i != pos_z)
            def _():
                give_rows(i, pos_z).start()
        return carry

    lax.fori_loop(0, KV_CHUNKS, finish, 0)
    if spread:
        for i in range(KV_CHUNKS):
            keep_hidden(i).wait()
        keep_rows().wait()
        for j in range(1, RING):
            z = (pos_z + j) % RING
            for i in range(KV_CHUNKS):
                give_hidden(z, i, z).wait_recv()
                give_hidden(z, i, pos_z).wait_send()
            give_rows(z, z).wait_recv()
            give_rows(z, pos_z).wait_send()
    else:
        for d in range(DIRS):
            for copy in weight_part(1, d):
                copy.wait_recv()
            for step in range(2):
                for copy in weight_part(step, d):
                    copy.wait_send()
    k_store.wait()
    v_store.wait()
    for i in range(KV_CHUNKS):
        @pl.when(chip < CHIPS - 1)
        def _():
            to_right(i).wait_send()

        @pl.when(chip == 0)
        def _():
            to_wrap(i).wait_send()

        @pl.when(core == 0)
        def _():
            to_other(i).wait_send()

        if i < KV_CHUNKS // 2:
            @pl.when(jnp.logical_and(chip >= 1, chip < CHIPS - 1))
            def _():
                on_right(i).wait_send()
        else:
            @pl.when(chip == 0)
            def _():
                from_relay(i).wait_send()

            @pl.when(chip == 1)
            def _():
                to_relay(i).wait_send()

            @pl.when(chip == CHIPS - 1)
            def _():
                on_left(i).wait_send()

        for back in (1, 2, 3):
            @pl.when(chip >= back)
            def _():
                on_other(back, i).wait_send()


def layer_head(layer, x_cur, cos_t, sin_t, norm_gain, w_q, w_k, w_v, w_gate, w_up, w_down, w_o, spread):
    tok_count, d_model = x_cur.shape
    head_dim = w_q.shape[2]
    ff_local = w_gate.shape[2]
    rows_per = tok_count // KV_CHUNKS
    any_spec = pl.BlockSpec(memory_space=pl.ANY)
    vmem_spec = pl.BlockSpec(memory_space=pltpu.VMEM)
    bf16 = jnp.bfloat16
    rows_shape = jax.ShapeDtypeStruct((tok_count, head_dim), bf16)
    args = (x_cur, cos_t, sin_t, norm_gain, w_q, w_k, w_v, w_gate, w_up)
    in_specs = [any_spec, vmem_spec, vmem_spec, vmem_spec, any_spec, any_spec, any_spec, any_spec, any_spec]
    if spread:
        out_shape = [jax.ShapeDtypeStruct((RING, rows_per, ff_local), bf16), jax.ShapeDtypeStruct((RING, rows_per, head_dim), bf16), rows_shape, rows_shape]
        out_specs = [any_spec] * 4
        extra = [pltpu.VMEM((tok_count, ff_local), bf16), pltpu.VMEM((tok_count, head_dim), bf16), pltpu.SemaphoreType.DMA((RING, KV_CHUNKS + 1)),
                 pltpu.SemaphoreType.DMA((RING, KV_CHUNKS + 1)), pltpu.SemaphoreType.DMA((KV_CHUNKS + 1,))]
    else:
        args += (w_down, w_o)
        in_specs += [any_spec, any_spec]
        out_shape = [jax.ShapeDtypeStruct((tok_count, ff_local), bf16), rows_shape, rows_shape, rows_shape,
                     jax.ShapeDtypeStruct((RING, ff_local, d_model), bf16), jax.ShapeDtypeStruct((RING, head_dim, d_model), bf16)]
        out_specs = [vmem_spec, vmem_spec] + [any_spec] * 4
        extra = [pltpu.SemaphoreType.DMA((2, DIRS, 2)), pltpu.SemaphoreType.DMA((2, DIRS, 2))]
    return pl.pallas_call(
        functools.partial(head_kernel, layer, spread),
        out_shape=out_shape,
        in_specs=in_specs,
        out_specs=out_specs,
        scratch_shapes=extra + [
            pltpu.VMEM((tok_count, d_model), bf16),
            pltpu.VMEM((2, rows_per, d_model), bf16),
            pltpu.VMEM((3, d_model, head_dim), bf16),
            pltpu.VMEM((2, 2, d_model, W_TILE), bf16),
            pltpu.VMEM((2 * CHIPS * tok_count, 2 * head_dim), bf16),
            pltpu.VMEM((tok_count, head_dim), bf16),
            pltpu.VMEM((tok_count, head_dim), jnp.float32),
            pltpu.VMEM((tok_count, 128), jnp.float32),
            pltpu.VMEM((tok_count, 128), jnp.float32),
            pltpu.SemaphoreType.DMA((2,)),
            pltpu.SemaphoreType.DMA((3,)),
            pltpu.SemaphoreType.DMA((2, 2)),
            pltpu.SemaphoreType.DMA((2,)),
            pltpu.SemaphoreType.DMA((4, KV_CHUNKS)),
            pltpu.SemaphoreType.DMA((4, KV_CHUNKS)),
            pltpu.SemaphoreType.DMA((4, KV_CHUNKS)),
            pltpu.SemaphoreType.DMA((4, KV_CHUNKS)),
        ],
        compiler_params=pltpu.CompilerParams(collective_id=2 + layer, has_side_effects=True, vmem_limit_bytes=63 * 1024 * 1024),
        cost_estimate=pl.CostEstimate(flops=2 * tok_count * d_model * (3 * head_dim + 2 * ff_local), bytes_accessed=d_model * (3 * head_dim + 2 * ff_local) * 2, transcendentals=0),
        name='head',
    )(*args)


STEPS = 8
SKEW = 2
W_GROUPS = 4


def tail_kernel(layer, chunk_rows, hid_ref, att_ref, x_ref, wd_ref, wo_ref, gd_in_ref, go_in_ref, out_ref, gd_ref, go_ref,
                part, xbuf, wbuf, recv_a, recv_b, load_sem, store_sem, send_sem, recv_sem, pass_send, pass_recv, side_send, side_recv):
    tok_count, d_model = xbuf.shape
    ff_local = hid_ref.shape[1]
    chunk_count = CHUNKS
    quarter, eighth = chunk_rows // RING, chunk_rows // (2 * RING)
    half_cols = d_model // HALVES
    piece_cols = half_cols // RING
    my_head = lax.axis_index('head')
    pos_z, pos_y = my_head // RING, my_head % RING
    sign = (1, -1)

    def y_peer(d):
        return pos_z * RING + (pos_y + sign[d] + RING) % RING

    def z_peer(d):
        return ((pos_z + sign[d] + RING) % RING) * RING + pos_y

    first_pos, second_pos = (pos_y, pos_z), (pos_z, pos_y)
    first_peer, second_peer = (y_peer, z_peer), (z_peer, y_peer)

    group_cols = d_model // W_GROUPS

    def w_load(g):
        cols = pl.ds(pl.multiple_of(g * group_cols, group_cols), group_cols)
        return (pltpu.make_async_copy(wd_ref.at[layer, :, cols], wbuf.at[pl.ds(0, ff_local), cols], load_sem.at[g, 0]),
                pltpu.make_async_copy(wo_ref.at[layer, 0, :, cols], wbuf.at[pl.ds(ff_local, wo_ref.shape[2]), cols], load_sem.at[g, 1]))

    x_load = pltpu.make_async_copy(x_ref, xbuf, load_sem.at[W_GROUPS, 0])
    for g in range(W_GROUPS):
        for load in w_load(g):
            load.start()
    x_load.start()
    barrier = pltpu.get_barrier_semaphore()
    for peer in (y_peer, z_peer):
        for d in range(DIRS):
            pl.semaphore_signal(barrier, inc=1, device_id={'head': peer(d)}, device_id_type=pl.DeviceIdType.MESH)
    my_seq = lax.axis_index('seq')
    chip, core = my_seq // 2, my_seq % 2
    other = chip * 2 + 1 - core

    def x_chip(n):
        return (chip + n + CHIPS) % CHIPS

    for peer in (x_chip(1) * 2 + core, x_chip(-1) * 2 + core, other):
        pl.semaphore_signal(barrier, inc=1, device_id={'seq': peer}, device_id_type=pl.DeviceIdType.MESH)
    pl.semaphore_wait(barrier, 2 * DIRS + 3)

    def weight_copies(j, part_chip, part_core, half, send, recv, to):
        copies = []
        for n, ref in enumerate((gd_ref, go_ref)):
            size = ref.shape[1] // (2 * CHIPS)
            start = (part_chip * 2 + part_core) * size
            if half is None:
                rows = pl.ds(pl.multiple_of(start, size), size)
            else:
                rows = pl.ds(pl.multiple_of(start + half * (size // 2), size // 2), size // 2)
            place = ref.at[(pos_z + j) % RING, rows, :]
            copies.append(pltpu.make_async_remote_copy(src_ref=place, dst_ref=place, send_sem=send.at[n], recv_sem=recv.at[n], device_id={'seq': to}, device_id_type=pl.DeviceIdType.MESH))
        return copies

    def own_pass(j, d):
        return weight_copies(j, chip, core, None, pass_send.at[0, j - 1, d], pass_recv.at[0, j - 1, d], x_chip(sign[d]) * 2 + core)

    def far_pass(j, d):
        return weight_copies(j, x_chip(-sign[d]), core, d, pass_send.at[1, j - 1, d], pass_recv.at[1, j - 1, d], x_chip(sign[d]) * 2 + core)

    def side_pass(j, n, side):
        return weight_copies(j, x_chip(n), side, None, side_send.at[j - 1, n], side_recv.at[j - 1, n], other)

    def serve_near(j):
        for d in range(DIRS):
            for copy in own_pass(j, d):
                copy.wait_recv()
            for copy in far_pass(j, d) + side_pass(j, 3 if d == 0 else 1, core):
                copy.start()

    def serve_far(j):
        for d in range(DIRS):
            for copy in far_pass(j, d):
                copy.wait_recv()
        for copy in side_pass(j, 2, core):
            copy.start()

    for j in range(1, RING):
        for d in range(DIRS):
            for copy in own_pass(j, d):
                copy.start()
        for copy in side_pass(j, 0, core):
            copy.start()

    def rows_of(chunk, piece, offset, count):
        return pl.ds(pl.multiple_of(chunk * chunk_rows + piece * quarter + offset, eighth), count)

    def cols_of(h, piece):
        return pl.ds(pl.multiple_of(h * half_cols + piece * piece_cols, piece_cols), piece_cols)

    def half_of(h):
        return pl.ds(h * half_cols, half_cols)

    def message(step, chunk, h, d):
        p1, p2, s = first_pos[h], second_pos[h], sign[d]
        far1, near1, behind1 = (p1 + 2) % RING, (p1 + s + RING) % RING, (p1 - s + RING) % RING
        far2, near2, behind2 = (p2 + 2) % RING, (p2 + s + RING) % RING, (p2 - s + RING) % RING
        if step == 0:
            src, dst = part.at[rows_of(chunk, far1, d * eighth, eighth), half_of(h)], recv_a.at[chunk, h, d, pl.ds(quarter, eighth), :]
        elif step == 1:
            src, dst = part.at[rows_of(chunk, near1, 0, quarter), half_of(h)], recv_a.at[chunk, h, d, pl.ds(0, quarter), :]
        elif step == 2:
            src, dst = part.at[rows_of(chunk, p1, d * eighth, eighth), cols_of(h, far2)], recv_b.at[chunk, h, d, pl.ds(quarter, eighth), :]
        elif step == 3:
            src, dst = part.at[rows_of(chunk, p1, 0, quarter), cols_of(h, near2)], recv_b.at[chunk, h, d, pl.ds(0, quarter), :]
        elif step == 4:
            src = dst = xbuf.at[rows_of(chunk, p1, 0, quarter), cols_of(h, p2)]
        elif step == 5:
            src = dst = xbuf.at[rows_of(chunk, p1, d * eighth, eighth), cols_of(h, behind2)]
        elif step == 6:
            src = dst = xbuf.at[rows_of(chunk, p1, 0, quarter), half_of(h)]
        else:
            src = dst = xbuf.at[rows_of(chunk, behind1, d * eighth, eighth), half_of(h)]
        peer = (first_peer if step in (0, 1, 6, 7) else second_peer)[h](d)
        return pltpu.make_async_remote_copy(
            src_ref=src, dst_ref=dst, send_sem=send_sem.at[chunk, step, h * DIRS + d], recv_sem=recv_sem.at[chunk, step, h * DIRS + d],
            device_id={'head': peer}, device_id_type=pl.DeviceIdType.MESH)

    def project(chunk):
        rows = pl.ds(pl.multiple_of(chunk * chunk_rows, chunk_rows), chunk_rows)

        def one_tile(i, carry):
            cols = pl.ds(pl.multiple_of(i * piece_cols, piece_cols), piece_cols)
            per_group = group_cols // piece_cols

            @pl.when(jnp.logical_and(chunk == 0, i % per_group == 0))
            def _():
                for load in w_load(i // per_group):
                    load.wait()

            total = jnp.dot(hid_ref[rows, :], wbuf[:ff_local, cols], preferred_element_type=jnp.float32)
            part[rows, cols] = total + jnp.dot(att_ref[rows, :], wbuf[ff_local:, cols], preferred_element_type=jnp.float32)
            return carry

        lax.fori_loop(0, d_model // piece_cols, one_tile, 0)

    def store(chunk):
        rows = pl.ds(pl.multiple_of(chunk * chunk_rows, chunk_rows), chunk_rows)
        return pltpu.make_async_copy(xbuf.at[rows, :], out_ref.at[rows, :], store_sem.at[chunk])

    def stage(number, chunk):
        if number == 0:
            project(chunk)
        if number == 1:
            @pl.when(chunk == 0)
            def _():
                x_load.wait()
        for h in range(HALVES):
            p1, p2 = first_pos[h], second_pos[h]
            if number:
                for d in range(DIRS):
                    message(number - 1, chunk, h, d).wait_recv()
            if number in (1, 3):
                for d in range(DIRS):
                    if number == 1:
                        rows, cols, arrived = rows_of(chunk, (p1 + sign[d] + RING) % RING, d * eighth, eighth), half_of(h), recv_a
                    else:
                        rows, cols, arrived = rows_of(chunk, p1, d * eighth, eighth), cols_of(h, (p2 + sign[d] + RING) % RING), recv_b
                    part[rows, cols] = part[rows, cols] + arrived[chunk, h, d, pl.ds(quarter, eighth), :]
            if number == 2:
                rows = rows_of(chunk, p1, 0, quarter)
                part[rows, half_of(h)] = part[rows, half_of(h)] + recv_a[chunk, h, 0, pl.ds(0, quarter), :] + recv_a[chunk, h, 1, pl.ds(0, quarter), :]
            if number == 4:
                rows, cols = rows_of(chunk, p1, 0, quarter), cols_of(h, p2)
                total = part[rows, cols] + recv_b[chunk, h, 0, pl.ds(0, quarter), :] + recv_b[chunk, h, 1, pl.ds(0, quarter), :]
                update = total.astype(jnp.bfloat16).astype(jnp.float32)
                xbuf[rows, cols] = (xbuf[rows, cols].astype(jnp.float32) + update).astype(jnp.bfloat16)
            if number < STEPS:
                for d in range(DIRS):
                    message(number, chunk, h, d).start()
        if number == STEPS:
            store(chunk).start()

    def tick(t, carry):
        for number in range(STEPS, -1, -1):
            chunk = t - SKEW * number

            @pl.when(jnp.logical_and(chunk >= 0, chunk < chunk_count))
            def _():
                stage(number, chunk)
        for j in range(1, RING):
            @pl.when(t == NEAR_TICKS[j - 1])
            def _():
                serve_near(j)

            @pl.when(t == FAR_TICKS[j - 1])
            def _():
                serve_far(j)
        return carry

    lax.fori_loop(0, CHUNKS + SKEW * STEPS, tick, 0)

    def drain(chunk, carry):
        for step in range(STEPS):
            for h in range(HALVES):
                for d in range(DIRS):
                    message(step, chunk, h, d).wait_send()
        store(chunk).wait()
        return carry

    lax.fori_loop(0, chunk_count, drain, 0)
    for j in range(1, RING):
        for d in range(DIRS):
            for copy in own_pass(j, d) + far_pass(j, d):
                copy.wait_send()
        for n in range(CHIPS):
            for copy in side_pass(j, n, 1 - core):
                copy.wait_recv()
            for copy in side_pass(j, n, core):
                copy.wait_send()


def layer_tail(layer, hidden, attn_heads, x_cur, w_down, w_o, all_down, all_out):
    tok_count, d_model = x_cur.shape
    chunk_rows = tok_count // CHUNKS
    depth = hidden.shape[1] + attn_heads.shape[1]
    landed = 3 * chunk_rows // (2 * RING)
    any_spec = pl.BlockSpec(memory_space=pl.ANY)
    vmem_spec = pl.BlockSpec(memory_space=pltpu.VMEM)
    return pl.pallas_call(
        functools.partial(tail_kernel, layer, chunk_rows),
        out_shape=[jax.ShapeDtypeStruct((tok_count, d_model), jnp.bfloat16), jax.ShapeDtypeStruct(all_down.shape, jnp.bfloat16), jax.ShapeDtypeStruct(all_out.shape, jnp.bfloat16)],
        in_specs=[vmem_spec, vmem_spec] + [any_spec] * 5,
        out_specs=[any_spec] * 3,
        input_output_aliases={5: 1, 6: 2},
        scratch_shapes=[
            pltpu.VMEM((tok_count, d_model), jnp.float32),
            pltpu.VMEM((tok_count, d_model), jnp.bfloat16),
            pltpu.VMEM((depth, d_model), jnp.bfloat16),
            pltpu.VMEM((CHUNKS, HALVES, DIRS, landed, d_model // HALVES), jnp.float32),
            pltpu.VMEM((CHUNKS, HALVES, DIRS, landed, d_model // HALVES // RING), jnp.float32),
            pltpu.SemaphoreType.DMA((W_GROUPS + 1, 2)),
            pltpu.SemaphoreType.DMA((CHUNKS,)),
            pltpu.SemaphoreType.DMA((CHUNKS, STEPS, HALVES * DIRS)),
            pltpu.SemaphoreType.DMA((CHUNKS, STEPS, HALVES * DIRS)),
            pltpu.SemaphoreType.DMA((2, RING - 1, DIRS, 2)),
            pltpu.SemaphoreType.DMA((2, RING - 1, DIRS, 2)),
            pltpu.SemaphoreType.DMA((RING - 1, CHIPS, 2)),
            pltpu.SemaphoreType.DMA((RING - 1, CHIPS, 2)),
        ],
        compiler_params=pltpu.CompilerParams(collective_id=layer, has_side_effects=True, vmem_limit_bytes=63 * 1024 * 1024),
        cost_estimate=pl.CostEstimate(flops=2 * tok_count * depth * d_model, bytes_accessed=depth * d_model * 2, transcendentals=0),
        name='tail',
    )(hidden, attn_heads, x_cur, w_down, w_o, all_down, all_out)


LAST_STEPS = 6
LAST_COLS = 256


def last_kernel(layer, hid_ref, att_ref, x_ref, wd_ref, wo_ref, gd_ref, go_ref, out_ref, part, xres, xbuf, wtile, landed, w_sem, x_sem, store_sem, send_sem, recv_sem):
    rows, d_model = part.shape
    block = wtile.shape[3]
    block_count = d_model // block
    ff_local = hid_ref.shape[2]
    quarter, eighth = rows // RING, rows // (2 * RING)
    my_head = lax.axis_index('head')
    pos_z, pos_y = my_head // RING, my_head % RING
    sign = (1, -1)

    def cols_of(c):
        return pl.ds(pl.multiple_of(c * block, block), block)

    def w_loads(c):
        copies = []
        for j in range(RING):
            z = (pos_z + j) % RING
            down = wd_ref.at[layer, :, cols_of(c)] if j == 0 else gd_ref.at[z, :, cols_of(c)]
            out = wo_ref.at[layer, 0, :, cols_of(c)] if j == 0 else go_ref.at[z, :, cols_of(c)]
            copies.append(pltpu.make_async_copy(down, wtile.at[c % 2, j, pl.ds(0, ff_local), :], w_sem.at[c % 2, j, 0]))
            copies.append(pltpu.make_async_copy(out, wtile.at[c % 2, j, pl.ds(ff_local, wo_ref.shape[2]), :], w_sem.at[c % 2, j, 1]))
        return copies

    for copy in w_loads(0):
        copy.start()
    x_load = pltpu.make_async_copy(x_ref.at[pl.ds(pl.multiple_of(pos_z * rows + pos_y * quarter, quarter), quarter), :], xres, x_sem)
    x_load.start()

    def y_device(d):
        return pos_z * RING + (pos_y + sign[d] + RING) % RING

    def z_device(d):
        return (pos_z + sign[d] + RING) % RING * RING + pos_y

    barrier = pltpu.get_barrier_semaphore()
    for device in (y_device, z_device):
        for d in range(DIRS):
            pl.semaphore_signal(barrier, inc=1, device_id={'head': device(d)}, device_id_type=pl.DeviceIdType.MESH)
    pl.semaphore_wait(barrier, 2 * DIRS)
    x_load.wait()

    def rows_of(piece, offset, count):
        return pl.ds(pl.multiple_of(piece * quarter + offset, eighth), count)

    def message(step, c, d, z_first):
        s = sign[d]
        near, behind = (pos_y + s + RING) % RING, (pos_y - s + RING) % RING
        if step == 0:
            src, dst = part.at[rows_of((pos_y + 2) % RING, d * eighth, eighth), cols_of(c)], landed.at[c, d, pl.ds(quarter, eighth), :]
        elif step == 1:
            src, dst = part.at[rows_of(near, 0, quarter), cols_of(c)], landed.at[c, d, pl.ds(0, quarter), :]
        elif z_first:
            back = (pos_z - s + RING) % RING
            if step == 2:
                src = dst = xbuf.at[pos_z, rows_of(pos_y, 0, quarter), cols_of(c)]
            elif step == 3:
                src = dst = xbuf.at[back, rows_of(pos_y, d * eighth, eighth), cols_of(c)]
            elif step == 4:
                src = dst = xbuf.at[:, rows_of(pos_y, 0, quarter), cols_of(c)]
            else:
                src = dst = xbuf.at[:, rows_of(behind, d * eighth, eighth), cols_of(c)]
        else:
            if step == 2:
                src = dst = xbuf.at[pos_z, rows_of(pos_y, 0, quarter), cols_of(c)]
            elif step == 3:
                src = dst = xbuf.at[pos_z, rows_of(behind, d * eighth, eighth), cols_of(c)]
            elif step == 4:
                src = dst = xbuf.at[pos_z, :, cols_of(c)]
            else:
                src = dst = xbuf.at[(pos_z - s + RING) % RING, pl.ds(d * (rows // 2), rows // 2), cols_of(c)]
        along_y = step < 2 or (step < 4) != z_first
        return pltpu.make_async_remote_copy(
            src_ref=src, dst_ref=dst, send_sem=send_sem.at[c, step, d], recv_sem=recv_sem.at[c, step, d],
            device_id={'head': (y_device if along_y else z_device)(d)}, device_id_type=pl.DeviceIdType.MESH)

    def on_messages(step, c, act):
        if step < 2:
            for d in range(DIRS):
                act(message(step, c, d, False))
            return

        @pl.when(c % 4 == 3)
        def _():
            for d in range(DIRS):
                act(message(step, c, d, True))

        @pl.when(c % 4 != 3)
        def _():
            for d in range(DIRS):
                act(message(step, c, d, False))

    def store(c):
        return pltpu.make_async_copy(xbuf.at[:, :, cols_of(c)], out_ref.at[:, :, cols_of(c)], store_sem.at[c])

    def project(c):
        @pl.when(c + 1 < block_count)
        def _():
            for copy in w_loads(c + 1):
                copy.start()

        for copy in w_loads(c):
            copy.wait()
        total = None
        for j in range(RING):
            z = (pos_z + j) % RING
            down = jnp.dot(hid_ref[z], wtile[c % 2, j, :ff_local, :], preferred_element_type=jnp.float32)
            down = down + jnp.dot(att_ref[z], wtile[c % 2, j, ff_local:, :], preferred_element_type=jnp.float32)
            total = down if total is None else total + down
        part[:, cols_of(c)] = total

    def stage(number, c):
        if number == 0:
            project(c)
        else:
            on_messages(number - 1, c, lambda copy: copy.wait_recv())
        if number == 1:
            for d in range(DIRS):
                piece = rows_of((pos_y + sign[d] + RING) % RING, d * eighth, eighth)
                part[piece, cols_of(c)] = part[piece, cols_of(c)] + landed[c, d, pl.ds(quarter, eighth), :]
        if number == 2:
            own = rows_of(pos_y, 0, quarter)
            total = part[own, cols_of(c)] + landed[c, 0, pl.ds(0, quarter), :] + landed[c, 1, pl.ds(0, quarter), :]
            update = total.astype(jnp.bfloat16).astype(jnp.float32)
            xbuf[pos_z, own, cols_of(c)] = (xres[:, cols_of(c)].astype(jnp.float32) + update).astype(jnp.bfloat16)
        if number < LAST_STEPS:
            on_messages(number, c, lambda copy: copy.start())
        else:
            store(c).start()

    def tick(t, carry):
        for number in range(LAST_STEPS, -1, -1):
            c = t - SKEW * number

            @pl.when(jnp.logical_and(c >= 0, c < block_count))
            def _():
                stage(number, c)
        return carry

    lax.fori_loop(0, block_count + SKEW * LAST_STEPS, tick, 0)

    def drain(c, carry):
        for step in range(LAST_STEPS):
            on_messages(step, c, lambda copy: copy.wait_send())
        store(c).wait()
        return carry

    lax.fori_loop(0, block_count, drain, 0)


def layer_last(layer, hid_all, att_all, x_cur, w_down, w_o, all_down, all_out):
    tok_count, d_model = x_cur.shape
    rows = tok_count // RING
    depth = hid_all.shape[2] + att_all.shape[2]
    any_spec = pl.BlockSpec(memory_space=pl.ANY)
    vmem_spec = pl.BlockSpec(memory_space=pltpu.VMEM)
    blocks = d_model // LAST_COLS
    out = pl.pallas_call(
        functools.partial(last_kernel, layer),
        out_shape=jax.ShapeDtypeStruct((RING, rows, d_model), jnp.bfloat16),
        in_specs=[vmem_spec, vmem_spec] + [any_spec] * 5,
        out_specs=any_spec,
        scratch_shapes=[
            pltpu.VMEM((rows, d_model), jnp.float32),
            pltpu.VMEM((rows // RING, d_model), jnp.bfloat16),
            pltpu.VMEM((RING, rows, d_model), jnp.bfloat16),
            pltpu.VMEM((2, RING, depth, LAST_COLS), jnp.bfloat16),
            pltpu.VMEM((blocks, DIRS, 3 * rows // (2 * RING), LAST_COLS), jnp.float32),
            pltpu.SemaphoreType.DMA((2, RING, 2)),
            pltpu.SemaphoreType.DMA,
            pltpu.SemaphoreType.DMA((blocks,)),
            pltpu.SemaphoreType.DMA((blocks, LAST_STEPS, DIRS)),
            pltpu.SemaphoreType.DMA((blocks, LAST_STEPS, DIRS)),
        ],
        compiler_params=pltpu.CompilerParams(collective_id=layer, has_side_effects=True, vmem_limit_bytes=63 * 1024 * 1024),
        cost_estimate=pl.CostEstimate(flops=2 * tok_count * depth * d_model, bytes_accessed=4 * depth * d_model * 2, transcendentals=0),
        name='last',
    )(hid_all, att_all, x_cur, w_down, w_o, all_down, all_out)
    return out.reshape(tok_count, d_model)


EMIT_PARTS = 8


def emit_kernel(x_ref, k_first, k_second, v_first, v_second, x_out, k_out, v_out, xbuf, rows, load_sem, store_sem):
    size = x_ref.shape[0] // EMIT_PARTS
    loads, stores = [], []
    for n in range(EMIT_PARTS):
        part = pl.ds(n * size, size)
        loads.append(pltpu.make_async_copy(x_ref.at[part, :], xbuf.at[part, :], load_sem.at[n]))
        stores.append(pltpu.make_async_copy(xbuf.at[part, :], x_out.at[part, :], store_sem.at[n]))
    for n, (ref, out) in enumerate(((k_first, k_out.at[0]), (k_second, k_out.at[1]), (v_first, v_out.at[0]), (v_second, v_out.at[1]))):
        loads.append(pltpu.make_async_copy(ref, rows.at[n], load_sem.at[EMIT_PARTS + n]))
        stores.append(pltpu.make_async_copy(rows.at[n], out, store_sem.at[EMIT_PARTS + n]))
    for copy in loads:
        copy.start()
    for load, store in zip(loads, stores):
        load.wait()
        store.start()
    for copy in stores:
        copy.wait()


def emit(x_out, k_first, k_second, v_first, v_second):
    any_spec = pl.BlockSpec(memory_space=pl.ANY)
    cache = jax.ShapeDtypeStruct((2,) + k_first.shape, jnp.bfloat16)
    return pl.pallas_call(
        emit_kernel,
        out_shape=[jax.ShapeDtypeStruct(x_out.shape, jnp.bfloat16), cache, cache],
        in_specs=[any_spec] * 5,
        out_specs=[any_spec] * 3,
        scratch_shapes=[
            pltpu.VMEM(x_out.shape, jnp.bfloat16),
            pltpu.VMEM((4,) + k_first.shape, jnp.bfloat16),
            pltpu.SemaphoreType.DMA((EMIT_PARTS + 4,)),
            pltpu.SemaphoreType.DMA((EMIT_PARTS + 4,)),
        ],
        compiler_params=pltpu.CompilerParams(vmem_limit_bytes=63 * 1024 * 1024),
        name='emit',
    )(x_out, k_first, k_second, v_first, v_second)


def solution(mesh):
    row_spec = P(('batch', 'seq'), None)
    pos_spec = P(('batch', 'seq'))
    head_spec = P(None, None, 'head', None)
    out_proj_spec = P(None, 'head', None, None)
    col_spec = P(None, None, 'head')
    down_spec = P(None, 'head', None)
    cache_spec = P(None, ('batch', 'seq'), 'head', None)

    def local_forward(x_loc, pos_loc, w_q, w_k, w_v, w_o, w_gate, w_up, w_down, norm_gain):
        tok_count, d_model = x_loc.shape
        layer_count = w_q.shape[0]
        head_dim = w_q.shape[3]
        flat_q, flat_k, flat_v = (w.reshape(layer_count, d_model, head_dim) for w in (w_q, w_k, w_v))
        cos_t, sin_t = rope_tables(pos_loc, head_dim)
        hidden, attn_heads, k_first, v_first, all_down, all_out = layer_head(0, x_loc, cos_t, sin_t, norm_gain, flat_q, flat_k, flat_v, w_gate, w_up, w_down, w_o, False)
        x_mid, all_down, all_out = layer_tail(0, hidden, attn_heads, x_loc, w_down, w_o, all_down, all_out)
        hid_all, att_all, k_second, v_second = layer_head(1, x_mid, cos_t, sin_t, norm_gain, flat_q, flat_k, flat_v, w_gate, w_up, w_down, w_o, True)
        x_out = layer_last(1, hid_all, att_all, x_mid, w_down, w_o, all_down, all_out)
        x_out, k_all, v_all = emit(x_out, k_first, k_second, v_first, v_second)
        cache_shape = (layer_count, tok_count, 1, head_dim)
        return x_out, k_all.reshape(cache_shape), v_all.reshape(cache_shape)

    return jax.shard_map(local_forward, mesh=mesh, in_specs=(row_spec, pos_spec, head_spec, head_spec, head_spec, out_proj_spec, col_spec, col_spec, down_spec, P(None, None)), out_specs=(row_spec, cache_spec, cache_spec), check_vma=False)
```

```python
import functools
import math
import jax
import jax.numpy as jnp
from jax import lax
from jax.experimental import pallas as pl
from jax.experimental.pallas import tpu as pltpu
from jax.sharding import PartitionSpec as P

ROPE_BASE = 500000.0
EPS = 1e-5


def rope_tables(positions, head_dim):
    half_dim = head_dim // 2
    inv_freq = ROPE_BASE ** (-(jnp.arange(half_dim, dtype=jnp.float32) * 2.0 / head_dim))
    angles = positions.astype(jnp.float32)[..., None] * inv_freq
    return jnp.cos(angles), jnp.sin(angles)


CHUNKS = 8
NEAR_TICKS = (6, 9, 13)
FAR_TICKS = (16, 19, 23)


CHIPS = 4
RING = 4
HALVES = 2
DIRS = 2
KV_CHUNKS = 4
W_TILE = 256
NORM_ROWS = 64


def head_kernel(layer, spread, *refs):
    x_ref, cos_ref, sin_ref, gain_ref, wq_ref, wk_ref, wv_ref, wg_ref, wu_ref = refs[:9]
    if spread:
        hid_all_ref, att_all_ref, k_ref, v_ref, hid_ref, att_ref, give_send, give_recv, keep_sem = refs[9:18]
    else:
        wd_ref, wo_ref, hid_ref, att_ref, k_ref, v_ref, gd_ref, go_ref, give_send, give_recv = refs[9:19]
    hbuf, xs, wqkv, wtile, kv, qbuf, acc, row_max, row_sum, x_sem, w_sem, t_sem, out_sem, own_send, pass_send, ici_recv, core_recv = refs[-17:]
    my_head = lax.axis_index('head')
    pos_z, pos_y = my_head // RING, my_head % RING
    sign = (1, -1)

    def z_device(z):
        return (z + RING) % RING * RING + pos_y

    tok_count, d_model = hbuf.shape
    head_dim = qbuf.shape[1]
    half_dim = head_dim // 2
    rows_per = tok_count // KV_CHUNKS
    half_rows = tok_count // 2
    my_seq = lax.axis_index('seq')
    chip, core = my_seq // 2, my_seq % 2
    other = chip * 2 + 1 - core
    right = ((chip + 1) % CHIPS) * 2 + core
    left = ((chip + CHIPS - 1) % CHIPS) * 2 + core

    def x_load(i):
        return pltpu.make_async_copy(x_ref.at[pl.ds(pl.multiple_of(i * rows_per, rows_per), rows_per), :], xs.at[i % 2], x_sem.at[i % 2])

    def tile_load(i, which):
        ref = (wg_ref, wu_ref)[which]
        return pltpu.make_async_copy(ref.at[layer, :, pl.ds(pl.multiple_of(i * W_TILE, W_TILE), W_TILE)], wtile.at[i % 2, which], t_sem.at[i % 2, which])

    x_load(0).start()
    w_loads = [pltpu.make_async_copy(ref.at[layer], wqkv.at[n], w_sem.at[n]) for n, ref in enumerate((wk_ref, wv_ref, wq_ref))]
    for load in w_loads:
        load.start()
    x_load(1).start()
    for which in range(2):
        tile_load(0, which).start()

    barrier = pltpu.get_barrier_semaphore()
    for peer in (left, right, other):
        pl.semaphore_signal(barrier, inc=1, device_id={'seq': peer}, device_id_type=pl.DeviceIdType.MESH)
    for j in range(1, RING):
        pl.semaphore_signal(barrier, inc=1, device_id={'head': z_device(pos_z + j)}, device_id_type=pl.DeviceIdType.MESH)
    pl.semaphore_wait(barrier, 6)

    def weight_part(step, d):
        copies = []
        for n, (own_ref, all_ref) in enumerate(((wd_ref, gd_ref), (wo_ref, go_ref))):
            size = all_ref.shape[1] // (2 * CHIPS)
            if step == 0:
                rows = pl.ds(pl.multiple_of(my_seq * size, size), size)
                src = own_ref.at[layer + 1, rows, :] if n == 0 else own_ref.at[layer + 1, 0, rows, :]
                dst = all_ref.at[pos_z, rows, :]
            else:
                rows = pl.ds(pl.multiple_of(my_seq * size + d * (size // 2), size // 2), size // 2)
                src = dst = all_ref.at[(pos_z - sign[d] + RING) % RING, rows, :]
            copies.append(pltpu.make_async_remote_copy(
                src_ref=src, dst_ref=dst, send_sem=give_send.at[step, d, n], recv_sem=give_recv.at[step, d, n],
                device_id={'head': z_device(pos_z + sign[d])}, device_id_type=pl.DeviceIdType.MESH))
        return copies

    def give(src, dst, send, recv, z):
        return pltpu.make_async_remote_copy(src_ref=src, dst_ref=dst, send_sem=send, recv_sem=recv, device_id={'head': z_device(z)}, device_id_type=pl.DeviceIdType.MESH)

    def give_hidden(z, i, source):
        rows = pl.ds(pl.multiple_of(z * rows_per, rows_per), rows_per)
        cols = pl.ds(pl.multiple_of(i * W_TILE, W_TILE), W_TILE)
        return give(hid_ref.at[rows, cols], hid_all_ref.at[source, :, cols], give_send.at[z, i], give_recv.at[source, i], z)

    def keep_hidden(i):
        rows = pl.ds(pl.multiple_of(pos_z * rows_per, rows_per), rows_per)
        cols = pl.ds(pl.multiple_of(i * W_TILE, W_TILE), W_TILE)
        return pltpu.make_async_copy(hid_ref.at[rows, cols], hid_all_ref.at[pos_z, :, cols], keep_sem.at[i])

    def give_rows(z, source):
        rows = pl.ds(pl.multiple_of(z * rows_per, rows_per), rows_per)
        return give(att_ref.at[rows, :], att_all_ref.at[source], give_send.at[z, KV_CHUNKS], give_recv.at[source, KV_CHUNKS], z)

    def keep_rows():
        rows = pl.ds(pl.multiple_of(pos_z * rows_per, rows_per), rows_per)
        return pltpu.make_async_copy(att_ref.at[rows, :], att_all_ref.at[pos_z], keep_sem.at[KV_CHUNKS])

    if not spread:
        for d in range(DIRS):
            for copy in weight_part(0, d):
                copy.start()

    def kv_copy(origin_chip, origin_core, i, to, send, recv):
        rows = kv.at[pl.ds(pl.multiple_of((origin_chip * 2 + origin_core) * tok_count + i * rows_per, rows_per), rows_per), :]
        return pltpu.make_async_remote_copy(src_ref=rows, dst_ref=rows, send_sem=send, recv_sem=recv, device_id={'seq': to}, device_id_type=pl.DeviceIdType.MESH)

    def to_right(i):
        return kv_copy(chip, core, i, right, own_send.at[0, i], ici_recv.at[0, i])

    def to_wrap(i):
        return kv_copy(chip, core, i, left, own_send.at[1, i], ici_recv.at[2, i])

    def to_other(i):
        return kv_copy(chip, core, i, other, own_send.at[2, i], core_recv.at[0, i])

    def on_right(i):
        return kv_copy(chip - 1, core, i, right, pass_send.at[0, i], ici_recv.at[1, i])

    def to_relay(i):
        return kv_copy(chip, core, i, left, own_send.at[3, i], ici_recv.at[3, i])

    def from_relay(i):
        return kv_copy(1, core, i, left, pass_send.at[0, i], ici_recv.at[1, i])

    def on_left(i):
        return kv_copy(0, core, i, left, pass_send.at[0, i], ici_recv.at[1, i])

    def relay(i):
        @pl.when(chip == 0)
        def _():
            kv_copy(1, core, i, left, own_send.at[3, i], ici_recv.at[3, i]).wait_recv()
            from_relay(i).start()

    def on_other(back, i):
        return kv_copy(chip - back, core, i, other, pass_send.at[back, i], core_recv.at[back, i])

    def arrival(back, i):
        return kv_copy(chip - back, core, i, other, pass_send.at[back, i], ici_recv.at[back - 1, i])

    def serve(back, i):
        @pl.when(chip >= back)
        def _():
            arrival(back, i).wait_recv()
            on_other(back, i).start()
        if back == 1:
            @pl.when(jnp.logical_and(i < KV_CHUNKS // 2, jnp.logical_and(chip >= 1, chip < CHIPS - 1)))
            def _():
                on_right(i).start()
        if back == 3:
            @pl.when(jnp.logical_and(i >= KV_CHUNKS // 2, chip == CHIPS - 1))
            def _():
                on_left(i).start()

    def rope(values, rows):
        cos_t, sin_t = cos_ref[rows, :], sin_ref[rows, :]
        wide = values.astype(jnp.bfloat16).astype(jnp.float32)
        first, second = wide[:, :half_dim], wide[:, half_dim:]
        return jnp.concatenate([first * cos_t - second * sin_t, second * cos_t + first * sin_t], axis=1).astype(jnp.bfloat16)

    gain = gain_ref[pl.ds(layer, 1), :].astype(jnp.float32)

    def prepare(i, carry):
        x_load(i).wait()
        rows = pl.ds(pl.multiple_of(i * rows_per, rows_per), rows_per)

        def norm(j, inner):
            few = pl.ds(pl.multiple_of(j * NORM_ROWS, NORM_ROWS), NORM_ROWS)
            x_f32 = xs[i % 2, few, :].astype(jnp.float32)
            inv_rms = lax.rsqrt(jnp.mean(x_f32 * x_f32, axis=-1, keepdims=True) + EPS)
            hbuf[pl.ds(pl.multiple_of(i * rows_per + j * NORM_ROWS, NORM_ROWS), NORM_ROWS), :] = (x_f32 * inv_rms * gain).astype(jnp.bfloat16)
            return inner

        lax.fori_loop(0, rows_per // NORM_ROWS, norm, 0)

        @pl.when(i + 2 < KV_CHUNKS)
        def _():
            x_load(i + 2).start()

        @pl.when(i == 0)
        def _():
            w_loads[0].wait()
            w_loads[1].wait()

        normed = hbuf[rows, :]
        own = pl.ds(pl.multiple_of(my_seq * tok_count + i * rows_per, rows_per), rows_per)
        kv[own, :head_dim] = rope(jnp.dot(normed, wqkv[0], preferred_element_type=jnp.float32), rows)
        kv[own, head_dim:] = jnp.dot(normed, wqkv[1], preferred_element_type=jnp.float32).astype(jnp.bfloat16)

        @pl.when(chip < CHIPS - 1)
        def _():
            to_right(i).start()

        @pl.when(chip == 0)
        def _():
            to_wrap(i).start()

        @pl.when(jnp.logical_and(i >= KV_CHUNKS // 2, chip == 1))
        def _():
            to_relay(i).start()

        @pl.when(core == 0)
        def _():
            to_other(i).start()
        return carry

    lax.fori_loop(0, KV_CHUNKS, prepare, 0)
    w_loads[2].wait()
    own_rows = pl.ds(pl.multiple_of(my_seq * tok_count, tok_count), tok_count)
    k_store = pltpu.make_async_copy(kv.at[own_rows, pl.ds(0, head_dim)], k_ref, out_sem.at[0])
    v_store = pltpu.make_async_copy(kv.at[own_rows, pl.ds(head_dim, head_dim)], v_ref, out_sem.at[1])
    k_store.start()
    v_store.start()

    scale = 1.0 / math.sqrt(head_dim)

    def query(i, carry):
        rows = pl.ds(pl.multiple_of(i * rows_per, rows_per), rows_per)
        query_rows = rope(jnp.dot(hbuf[rows, :], wqkv[2], preferred_element_type=jnp.float32), rows)
        qbuf[rows, :] = (query_rows.astype(jnp.float32) * scale).astype(jnp.bfloat16)
        return carry

    lax.fori_loop(0, KV_CHUNKS, query, 0)

    def gated(i, carry):
        for which in range(2):
            tile_load(i, which).wait()

        @pl.when(i + 1 < wg_ref.shape[2] // W_TILE)
        def _():
            for which in range(2):
                tile_load(i + 1, which).start()

        def rows_step(j, inner):
            rows = pl.ds(pl.multiple_of(j * rows_per, rows_per), rows_per)
            normed = hbuf[rows, :]
            gate = jnp.dot(normed, wtile[i % 2, 0], preferred_element_type=jnp.float32)
            up = jnp.dot(normed, wtile[i % 2, 1], preferred_element_type=jnp.float32)
            hid_ref[rows, pl.ds(pl.multiple_of(i * W_TILE, W_TILE), W_TILE)] = (gate * jax.nn.sigmoid(gate) * up).astype(jnp.bfloat16)
            if spread:
                @pl.when(j == pos_z)
                def _():
                    keep_hidden(i).start()

                @pl.when(j != pos_z)
                def _():
                    give_hidden(j, i, pos_z).start()
            return inner

        lax.fori_loop(0, KV_CHUNKS, rows_step, 0)
        serve(1, i)
        serve(3, i)

        @pl.when(i >= KV_CHUNKS // 2)
        def _():
            relay(i)

        if not spread:
            @pl.when(i == 2)
            def _():
                for d in range(DIRS):
                    for copy in weight_part(0, d):
                        copy.wait_recv()
                    for copy in weight_part(1, d):
                        copy.start()
        return carry

    lax.fori_loop(0, KV_CHUNKS, gated, 0)

    lanes = row_max.shape[2]

    def attend(key_start, q_half, side, masked, first):
        rows = pl.ds(q_half * half_rows, half_rows)
        some = pl.ds(key_start, half_rows)
        logits = lax.dot_general(qbuf[rows, :], kv[some, :head_dim], (((1,), (1,)), ((), ())), preferred_element_type=jnp.float32)
        if masked:
            seen = lax.broadcasted_iota(jnp.int32, logits.shape, 0) >= lax.broadcasted_iota(jnp.int32, logits.shape, 1)
            logits = jnp.where(seen, logits, -jnp.inf)
        block_max = jnp.max(logits, axis=-1, keepdims=True)
        if first:
            new_max = jnp.broadcast_to(block_max, (half_rows, lanes))
        else:
            new_max = jnp.maximum(row_max[side, rows, :], block_max)
        prob = jnp.exp(logits - jnp.concatenate([new_max] * (half_rows // lanes), axis=1))
        block_sum = jnp.sum(prob, axis=-1, keepdims=True)
        block_out = jnp.dot(prob.astype(jnp.bfloat16), kv[some, head_dim:], preferred_element_type=jnp.float32)
        if first:
            row_sum[side, rows, :] = jnp.broadcast_to(block_sum, (half_rows, lanes))
            acc[side, rows, :] = block_out
        else:
            rescale = jnp.exp(row_max[side, rows, :] - new_max)
            row_sum[side, rows, :] = row_sum[side, rows, :] * rescale + block_sum
            acc[side, rows, :] = acc[side, rows, :] * jnp.concatenate([rescale] * (head_dim // lanes), axis=1) + block_out
        row_max[side, rows, :] = new_max

    def taken(back):
        for i in range(KV_CHUNKS):
            kv_copy(chip - back, 1 - core, i, other, pass_send.at[0, i], core_recv.at[back, i]).wait_recv()

    def finish(i):
        rows = pl.ds(i * rows_per, rows_per)
        top = jnp.maximum(row_max[0, rows, :], row_max[1, rows, :])
        weights = [jnp.exp(row_max[side, rows, :] - top) for side in range(2)]
        total = weights[0] * row_sum[0, rows, :] + weights[1] * row_sum[1, rows, :]
        wide = [jnp.concatenate([w] * (head_dim // lanes), axis=1) for w in weights + [total]]
        att_ref[rows, :] = ((acc[0, rows, :] * wide[0] + acc[1, rows, :] * wide[1]) / wide[2]).astype(jnp.bfloat16)
        if spread:
            @pl.when(i == pos_z)
            def _():
                keep_rows().start()

            @pl.when(i != pos_z)
            def _():
                give_rows(i, pos_z).start()

    own_start = pl.multiple_of(my_seq * tok_count, tok_count)
    second = pl.multiple_of(own_start + half_rows, half_rows)
    attend(own_start, 0, 0, True, True)
    attend(own_start, 1, 0, False, True)
    attend(second, 1, 1, True, True)
    top_rows = pl.ds(0, half_rows)
    row_max[1, top_rows, :] = jnp.full((half_rows, lanes), -jnp.inf, jnp.float32)
    row_sum[1, top_rows, :] = jnp.zeros((half_rows, lanes), jnp.float32)
    acc[1, top_rows, :] = jnp.zeros((half_rows, head_dim), jnp.float32)

    def past_block(n):
        later = n - core
        back = jnp.where(later < 2, 1, jnp.where(chip == CHIPS - 1, jnp.where(later < 4, 3, 2), 2))
        block = (chip - back) * 2 + jnp.where(later % 2 == 0, core, 1 - core)
        return jnp.where(jnp.logical_and(core == 1, n == 0), chip * 2, block)

    for q_half in range(2):
        def past(n, carry):
            if q_half == 0:
                @pl.when(jnp.logical_and(core == 1, n == 0))
                def _():
                    taken(0)

                for back in (1, 3, 2):
                    place = 0 if back == 1 else 2 if back == 3 else jnp.where(chip == CHIPS - 1, 4, 2)

                    @pl.when(jnp.logical_and(chip >= back, n == core + place))
                    def _():
                        if back == 2:
                            for i in range(KV_CHUNKS):
                                serve(2, i)

                    @pl.when(jnp.logical_and(chip >= back, n == core + place + 1))
                    def _():
                        taken(back)
            start = past_block(n) * tok_count
            attend(pl.multiple_of(start, half_rows), q_half, 0, False, False)
            attend(pl.multiple_of(start + half_rows, half_rows), q_half, 1, False, False)
            return carry

        lax.fori_loop(0, my_seq, past, 0)
        for i in range(q_half * KV_CHUNKS // 2, (q_half + 1) * KV_CHUNKS // 2):
            finish(i)

    if spread:
        for i in range(KV_CHUNKS):
            keep_hidden(i).wait()
        keep_rows().wait()
        for j in range(1, RING):
            z = (pos_z + j) % RING
            for i in range(KV_CHUNKS):
                give_hidden(z, i, z).wait_recv()
                give_hidden(z, i, pos_z).wait_send()
            give_rows(z, z).wait_recv()
            give_rows(z, pos_z).wait_send()
    else:
        for d in range(DIRS):
            for copy in weight_part(1, d):
                copy.wait_recv()
            for step in range(2):
                for copy in weight_part(step, d):
                    copy.wait_send()
    k_store.wait()
    v_store.wait()
    for i in range(KV_CHUNKS):
        @pl.when(chip < CHIPS - 1)
        def _():
            to_right(i).wait_send()

        @pl.when(chip == 0)
        def _():
            to_wrap(i).wait_send()

        @pl.when(core == 0)
        def _():
            to_other(i).wait_send()

        if i < KV_CHUNKS // 2:
            @pl.when(jnp.logical_and(chip >= 1, chip < CHIPS - 1))
            def _():
                on_right(i).wait_send()
        else:
            @pl.when(chip == 0)
            def _():
                from_relay(i).wait_send()

            @pl.when(chip == 1)
            def _():
                to_relay(i).wait_send()

            @pl.when(chip == CHIPS - 1)
            def _():
                on_left(i).wait_send()

        for back in (1, 2, 3):
            @pl.when(chip >= back)
            def _():
                on_other(back, i).wait_send()


def layer_head(layer, x_cur, cos_t, sin_t, norm_gain, w_q, w_k, w_v, w_gate, w_up, w_down, w_o, spread):
    tok_count, d_model = x_cur.shape
    head_dim = w_q.shape[2]
    ff_local = w_gate.shape[2]
    rows_per = tok_count // KV_CHUNKS
    any_spec = pl.BlockSpec(memory_space=pl.ANY)
    vmem_spec = pl.BlockSpec(memory_space=pltpu.VMEM)
    bf16 = jnp.bfloat16
    rows_shape = jax.ShapeDtypeStruct((tok_count, head_dim), bf16)
    args = (x_cur, cos_t, sin_t, norm_gain, w_q, w_k, w_v, w_gate, w_up)
    in_specs = [any_spec, vmem_spec, vmem_spec, vmem_spec, any_spec, any_spec, any_spec, any_spec, any_spec]
    if spread:
        out_shape = [jax.ShapeDtypeStruct((RING, rows_per, ff_local), bf16), jax.ShapeDtypeStruct((RING, rows_per, head_dim), bf16), rows_shape, rows_shape]
        out_specs = [any_spec] * 4
        extra = [pltpu.VMEM((tok_count, ff_local), bf16), pltpu.VMEM((tok_count, head_dim), bf16), pltpu.SemaphoreType.DMA((RING, KV_CHUNKS + 1)),
                 pltpu.SemaphoreType.DMA((RING, KV_CHUNKS + 1)), pltpu.SemaphoreType.DMA((KV_CHUNKS + 1,))]
    else:
        args += (w_down, w_o)
        in_specs += [any_spec, any_spec]
        out_shape = [jax.ShapeDtypeStruct((tok_count, ff_local), bf16), rows_shape, rows_shape, rows_shape,
                     jax.ShapeDtypeStruct((RING, ff_local, d_model), bf16), jax.ShapeDtypeStruct((RING, head_dim, d_model), bf16)]
        out_specs = [vmem_spec, vmem_spec] + [any_spec] * 4
        extra = [pltpu.SemaphoreType.DMA((2, DIRS, 2)), pltpu.SemaphoreType.DMA((2, DIRS, 2))]
    return pl.pallas_call(
        functools.partial(head_kernel, layer, spread),
        out_shape=out_shape,
        in_specs=in_specs,
        out_specs=out_specs,
        scratch_shapes=extra + [
            pltpu.VMEM((tok_count, d_model), bf16),
            pltpu.VMEM((2, rows_per, d_model), bf16),
            pltpu.VMEM((3, d_model, head_dim), bf16),
            pltpu.VMEM((2, 2, d_model, W_TILE), bf16),
            pltpu.VMEM((2 * CHIPS * tok_count, 2 * head_dim), bf16),
            pltpu.VMEM((tok_count, head_dim), bf16),
            pltpu.VMEM((2, tok_count, head_dim), jnp.float32),
            pltpu.VMEM((2, tok_count, 128), jnp.float32),
            pltpu.VMEM((2, tok_count, 128), jnp.float32),
            pltpu.SemaphoreType.DMA((2,)),
            pltpu.SemaphoreType.DMA((3,)),
            pltpu.SemaphoreType.DMA((2, 2)),
            pltpu.SemaphoreType.DMA((2,)),
            pltpu.SemaphoreType.DMA((4, KV_CHUNKS)),
            pltpu.SemaphoreType.DMA((4, KV_CHUNKS)),
            pltpu.SemaphoreType.DMA((4, KV_CHUNKS)),
            pltpu.SemaphoreType.DMA((4, KV_CHUNKS)),
        ],
        compiler_params=pltpu.CompilerParams(collective_id=2 + layer, has_side_effects=True, vmem_limit_bytes=63 * 1024 * 1024),
        cost_estimate=pl.CostEstimate(flops=2 * tok_count * d_model * (3 * head_dim + 2 * ff_local), bytes_accessed=d_model * (3 * head_dim + 2 * ff_local) * 2, transcendentals=0),
        name='head',
    )(*args)


STEPS = 8
SKEW = 2
W_GROUPS = 4


def tail_kernel(layer, chunk_rows, hid_ref, att_ref, x_ref, wd_ref, wo_ref, gd_in_ref, go_in_ref, out_ref, gd_ref, go_ref,
                part, xbuf, wbuf, recv_a, recv_b, load_sem, store_sem, send_sem, recv_sem, pass_send, pass_recv, side_send, side_recv):
    tok_count, d_model = xbuf.shape
    ff_local = hid_ref.shape[1]
    chunk_count = CHUNKS
    quarter, eighth = chunk_rows // RING, chunk_rows // (2 * RING)
    half_cols = d_model // HALVES
    piece_cols = half_cols // RING
    my_head = lax.axis_index('head')
    pos_z, pos_y = my_head // RING, my_head % RING
    sign = (1, -1)

    def y_peer(d):
        return pos_z * RING + (pos_y + sign[d] + RING) % RING

    def z_peer(d):
        return ((pos_z + sign[d] + RING) % RING) * RING + pos_y

    first_pos, second_pos = (pos_y, pos_z), (pos_z, pos_y)
    first_peer, second_peer = (y_peer, z_peer), (z_peer, y_peer)

    group_cols = d_model // W_GROUPS

    def w_load(g):
        cols = pl.ds(pl.multiple_of(g * group_cols, group_cols), group_cols)
        return (pltpu.make_async_copy(wd_ref.at[layer, :, cols], wbuf.at[pl.ds(0, ff_local), cols], load_sem.at[g, 0]),
                pltpu.make_async_copy(wo_ref.at[layer, 0, :, cols], wbuf.at[pl.ds(ff_local, wo_ref.shape[2]), cols], load_sem.at[g, 1]))

    x_load = pltpu.make_async_copy(x_ref, xbuf, load_sem.at[W_GROUPS, 0])
    for g in range(W_GROUPS):
        for load in w_load(g):
            load.start()
    x_load.start()
    barrier = pltpu.get_barrier_semaphore()
    for peer in (y_peer, z_peer):
        for d in range(DIRS):
            pl.semaphore_signal(barrier, inc=1, device_id={'head': peer(d)}, device_id_type=pl.DeviceIdType.MESH)
    my_seq = lax.axis_index('seq')
    chip, core = my_seq // 2, my_seq % 2
    other = chip * 2 + 1 - core

    def x_chip(n):
        return (chip + n + CHIPS) % CHIPS

    for peer in (x_chip(1) * 2 + core, x_chip(-1) * 2 + core, other):
        pl.semaphore_signal(barrier, inc=1, device_id={'seq': peer}, device_id_type=pl.DeviceIdType.MESH)
    pl.semaphore_wait(barrier, 2 * DIRS + 3)

    def weight_copies(j, part_chip, part_core, half, send, recv, to):
        copies = []
        for n, ref in enumerate((gd_ref, go_ref)):
            size = ref.shape[1] // (2 * CHIPS)
            start = (part_chip * 2 + part_core) * size
            if half is None:
                rows = pl.ds(pl.multiple_of(start, size), size)
            else:
                rows = pl.ds(pl.multiple_of(start + half * (size // 2), size // 2), size // 2)
            place = ref.at[(pos_z + j) % RING, rows, :]
            copies.append(pltpu.make_async_remote_copy(src_ref=place, dst_ref=place, send_sem=send.at[n], recv_sem=recv.at[n], device_id={'seq': to}, device_id_type=pl.DeviceIdType.MESH))
        return copies

    def own_pass(j, d):
        return weight_copies(j, chip, core, None, pass_send.at[0, j - 1, d], pass_recv.at[0, j - 1, d], x_chip(sign[d]) * 2 + core)

    def far_pass(j, d):
        return weight_copies(j, x_chip(-sign[d]), core, d, pass_send.at[1, j - 1, d], pass_recv.at[1, j - 1, d], x_chip(sign[d]) * 2 + core)

    def side_pass(j, n, side):
        return weight_copies(j, x_chip(n), side, None, side_send.at[j - 1, n], side_recv.at[j - 1, n], other)

    def serve_near(j):
        for d in range(DIRS):
            for copy in own_pass(j, d):
                copy.wait_recv()
            for copy in far_pass(j, d) + side_pass(j, 3 if d == 0 else 1, core):
                copy.start()

    def serve_far(j):
        for d in range(DIRS):
            for copy in far_pass(j, d):
                copy.wait_recv()
        for copy in side_pass(j, 2, core):
            copy.start()

    for j in range(1, RING):
        for d in range(DIRS):
            for copy in own_pass(j, d):
                copy.start()
        for copy in side_pass(j, 0, core):
            copy.start()

    def rows_of(chunk, piece, offset, count):
        return pl.ds(pl.multiple_of(chunk * chunk_rows + piece * quarter + offset, eighth), count)

    def cols_of(h, piece):
        return pl.ds(pl.multiple_of(h * half_cols + piece * piece_cols, piece_cols), piece_cols)

    def half_of(h):
        return pl.ds(h * half_cols, half_cols)

    def message(step, chunk, h, d):
        p1, p2, s = first_pos[h], second_pos[h], sign[d]
        far1, near1, behind1 = (p1 + 2) % RING, (p1 + s + RING) % RING, (p1 - s + RING) % RING
        far2, near2, behind2 = (p2 + 2) % RING, (p2 + s + RING) % RING, (p2 - s + RING) % RING
        if step == 0:
            src, dst = part.at[rows_of(chunk, far1, d * eighth, eighth), half_of(h)], recv_a.at[chunk, h, d, pl.ds(quarter, eighth), :]
        elif step == 1:
            src, dst = part.at[rows_of(chunk, near1, 0, quarter), half_of(h)], recv_a.at[chunk, h, d, pl.ds(0, quarter), :]
        elif step == 2:
            src, dst = part.at[rows_of(chunk, p1, d * eighth, eighth), cols_of(h, far2)], recv_b.at[chunk, h, d, pl.ds(quarter, eighth), :]
        elif step == 3:
            src, dst = part.at[rows_of(chunk, p1, 0, quarter), cols_of(h, near2)], recv_b.at[chunk, h, d, pl.ds(0, quarter), :]
        elif step == 4:
            src = dst = xbuf.at[rows_of(chunk, p1, 0, quarter), cols_of(h, p2)]
        elif step == 5:
            src = dst = xbuf.at[rows_of(chunk, p1, d * eighth, eighth), cols_of(h, behind2)]
        elif step == 6:
            src = dst = xbuf.at[rows_of(chunk, p1, 0, quarter), half_of(h)]
        else:
            src = dst = xbuf.at[rows_of(chunk, behind1, d * eighth, eighth), half_of(h)]
        peer = (first_peer if step in (0, 1, 6, 7) else second_peer)[h](d)
        return pltpu.make_async_remote_copy(
            src_ref=src, dst_ref=dst, send_sem=send_sem.at[chunk, step, h * DIRS + d], recv_sem=recv_sem.at[chunk, step, h * DIRS + d],
            device_id={'head': peer}, device_id_type=pl.DeviceIdType.MESH)

    def project(chunk):
        rows = pl.ds(pl.multiple_of(chunk * chunk_rows, chunk_rows), chunk_rows)

        def one_tile(i, carry):
            cols = pl.ds(pl.multiple_of(i * piece_cols, piece_cols), piece_cols)
            per_group = group_cols // piece_cols

            @pl.when(jnp.logical_and(chunk == 0, i % per_group == 0))
            def _():
                for load in w_load(i // per_group):
                    load.wait()

            total = jnp.dot(hid_ref[rows, :], wbuf[:ff_local, cols], preferred_element_type=jnp.float32)
            part[rows, cols] = total + jnp.dot(att_ref[rows, :], wbuf[ff_local:, cols], preferred_element_type=jnp.float32)
            return carry

        lax.fori_loop(0, d_model // piece_cols, one_tile, 0)

    def store(chunk):
        rows = pl.ds(pl.multiple_of(chunk * chunk_rows, chunk_rows), chunk_rows)
        return pltpu.make_async_copy(xbuf.at[rows, :], out_ref.at[rows, :], store_sem.at[chunk])

    def stage(number, chunk):
        if number == 0:
            project(chunk)
        if number == 1:
            @pl.when(chunk == 0)
            def _():
                x_load.wait()
        for h in range(HALVES):
            p1, p2 = first_pos[h], second_pos[h]
            if number:
                for d in range(DIRS):
                    message(number - 1, chunk, h, d).wait_recv()
            if number in (1, 3):
                for d in range(DIRS):
                    if number == 1:
                        rows, cols, arrived = rows_of(chunk, (p1 + sign[d] + RING) % RING, d * eighth, eighth), half_of(h), recv_a
                    else:
                        rows, cols, arrived = rows_of(chunk, p1, d * eighth, eighth), cols_of(h, (p2 + sign[d] + RING) % RING), recv_b
                    part[rows, cols] = part[rows, cols] + arrived[chunk, h, d, pl.ds(quarter, eighth), :]
            if number == 2:
                rows = rows_of(chunk, p1, 0, quarter)
                part[rows, half_of(h)] = part[rows, half_of(h)] + recv_a[chunk, h, 0, pl.ds(0, quarter), :] + recv_a[chunk, h, 1, pl.ds(0, quarter), :]
            if number == 4:
                rows, cols = rows_of(chunk, p1, 0, quarter), cols_of(h, p2)
                total = part[rows, cols] + recv_b[chunk, h, 0, pl.ds(0, quarter), :] + recv_b[chunk, h, 1, pl.ds(0, quarter), :]
                update = total.astype(jnp.bfloat16).astype(jnp.float32)
                xbuf[rows, cols] = (xbuf[rows, cols].astype(jnp.float32) + update).astype(jnp.bfloat16)
            if number < STEPS:
                for d in range(DIRS):
                    message(number, chunk, h, d).start()
        if number == STEPS:
            store(chunk).start()

    def tick(t, carry):
        for number in range(STEPS, -1, -1):
            chunk = t - SKEW * number

            @pl.when(jnp.logical_and(chunk >= 0, chunk < chunk_count))
            def _():
                stage(number, chunk)
        for j in range(1, RING):
            @pl.when(t == NEAR_TICKS[j - 1])
            def _():
                serve_near(j)

            @pl.when(t == FAR_TICKS[j - 1])
            def _():
                serve_far(j)
        return carry

    lax.fori_loop(0, CHUNKS + SKEW * STEPS, tick, 0)

    def drain(chunk, carry):
        for step in range(STEPS):
            for h in range(HALVES):
                for d in range(DIRS):
                    message(step, chunk, h, d).wait_send()
        store(chunk).wait()
        return carry

    lax.fori_loop(0, chunk_count, drain, 0)
    for j in range(1, RING):
        for d in range(DIRS):
            for copy in own_pass(j, d) + far_pass(j, d):
                copy.wait_send()
        for n in range(CHIPS):
            for copy in side_pass(j, n, 1 - core):
                copy.wait_recv()
            for copy in side_pass(j, n, core):
                copy.wait_send()


def layer_tail(layer, hidden, attn_heads, x_cur, w_down, w_o, all_down, all_out):
    tok_count, d_model = x_cur.shape
    chunk_rows = tok_count // CHUNKS
    depth = hidden.shape[1] + attn_heads.shape[1]
    landed = 3 * chunk_rows // (2 * RING)
    any_spec = pl.BlockSpec(memory_space=pl.ANY)
    vmem_spec = pl.BlockSpec(memory_space=pltpu.VMEM)
    return pl.pallas_call(
        functools.partial(tail_kernel, layer, chunk_rows),
        out_shape=[jax.ShapeDtypeStruct((tok_count, d_model), jnp.bfloat16), jax.ShapeDtypeStruct(all_down.shape, jnp.bfloat16), jax.ShapeDtypeStruct(all_out.shape, jnp.bfloat16)],
        in_specs=[vmem_spec, vmem_spec] + [any_spec] * 5,
        out_specs=[any_spec] * 3,
        input_output_aliases={5: 1, 6: 2},
        scratch_shapes=[
            pltpu.VMEM((tok_count, d_model), jnp.float32),
            pltpu.VMEM((tok_count, d_model), jnp.bfloat16),
            pltpu.VMEM((depth, d_model), jnp.bfloat16),
            pltpu.VMEM((CHUNKS, HALVES, DIRS, landed, d_model // HALVES), jnp.float32),
            pltpu.VMEM((CHUNKS, HALVES, DIRS, landed, d_model // HALVES // RING), jnp.float32),
            pltpu.SemaphoreType.DMA((W_GROUPS + 1, 2)),
            pltpu.SemaphoreType.DMA((CHUNKS,)),
            pltpu.SemaphoreType.DMA((CHUNKS, STEPS, HALVES * DIRS)),
            pltpu.SemaphoreType.DMA((CHUNKS, STEPS, HALVES * DIRS)),
            pltpu.SemaphoreType.DMA((2, RING - 1, DIRS, 2)),
            pltpu.SemaphoreType.DMA((2, RING - 1, DIRS, 2)),
            pltpu.SemaphoreType.DMA((RING - 1, CHIPS, 2)),
            pltpu.SemaphoreType.DMA((RING - 1, CHIPS, 2)),
        ],
        compiler_params=pltpu.CompilerParams(collective_id=layer, has_side_effects=True, vmem_limit_bytes=63 * 1024 * 1024),
        cost_estimate=pl.CostEstimate(flops=2 * tok_count * depth * d_model, bytes_accessed=depth * d_model * 2, transcendentals=0),
        name='tail',
    )(hidden, attn_heads, x_cur, w_down, w_o, all_down, all_out)


LAST_STEPS = 6
LAST_COLS = 256


def last_kernel(layer, hid_ref, att_ref, x_ref, wd_ref, wo_ref, gd_ref, go_ref, out_ref, part, xres, xbuf, wtile, landed, w_sem, x_sem, store_sem, send_sem, recv_sem):
    rows, d_model = part.shape
    block = wtile.shape[3]
    block_count = d_model // block
    ff_local = hid_ref.shape[2]
    quarter, eighth = rows // RING, rows // (2 * RING)
    my_head = lax.axis_index('head')
    pos_z, pos_y = my_head // RING, my_head % RING
    sign = (1, -1)

    def cols_of(c):
        return pl.ds(pl.multiple_of(c * block, block), block)

    def w_loads(c):
        copies = []
        for j in range(RING):
            z = (pos_z + j) % RING
            down = wd_ref.at[layer, :, cols_of(c)] if j == 0 else gd_ref.at[z, :, cols_of(c)]
            out = wo_ref.at[layer, 0, :, cols_of(c)] if j == 0 else go_ref.at[z, :, cols_of(c)]
            copies.append(pltpu.make_async_copy(down, wtile.at[c % 2, j, pl.ds(0, ff_local), :], w_sem.at[c % 2, j, 0]))
            copies.append(pltpu.make_async_copy(out, wtile.at[c % 2, j, pl.ds(ff_local, wo_ref.shape[2]), :], w_sem.at[c % 2, j, 1]))
        return copies

    for copy in w_loads(0):
        copy.start()
    x_load = pltpu.make_async_copy(x_ref.at[pl.ds(pl.multiple_of(pos_z * rows + pos_y * quarter, quarter), quarter), :], xres, x_sem)
    x_load.start()

    def y_device(d):
        return pos_z * RING + (pos_y + sign[d] + RING) % RING

    def z_device(d):
        return (pos_z + sign[d] + RING) % RING * RING + pos_y

    barrier = pltpu.get_barrier_semaphore()
    for device in (y_device, z_device):
        for d in range(DIRS):
            pl.semaphore_signal(barrier, inc=1, device_id={'head': device(d)}, device_id_type=pl.DeviceIdType.MESH)
    pl.semaphore_wait(barrier, 2 * DIRS)
    x_load.wait()

    def rows_of(piece, offset, count):
        return pl.ds(pl.multiple_of(piece * quarter + offset, eighth), count)

    def message(step, c, d, z_first):
        s = sign[d]
        near, behind = (pos_y + s + RING) % RING, (pos_y - s + RING) % RING
        if step == 0:
            src, dst = part.at[rows_of((pos_y + 2) % RING, d * eighth, eighth), cols_of(c)], landed.at[c, d, pl.ds(quarter, eighth), :]
        elif step == 1:
            src, dst = part.at[rows_of(near, 0, quarter), cols_of(c)], landed.at[c, d, pl.ds(0, quarter), :]
        elif z_first:
            back = (pos_z - s + RING) % RING
            if step == 2:
                src = dst = xbuf.at[pos_z, rows_of(pos_y, 0, quarter), cols_of(c)]
            elif step == 3:
                src = dst = xbuf.at[back, rows_of(pos_y, d * eighth, eighth), cols_of(c)]
            elif step == 4:
                src = dst = xbuf.at[:, rows_of(pos_y, 0, quarter), cols_of(c)]
            else:
                src = dst = xbuf.at[:, rows_of(behind, d * eighth, eighth), cols_of(c)]
        else:
            if step == 2:
                src = dst = xbuf.at[pos_z, rows_of(pos_y, 0, quarter), cols_of(c)]
            elif step == 3:
                src = dst = xbuf.at[pos_z, rows_of(behind, d * eighth, eighth), cols_of(c)]
            elif step == 4:
                src = dst = xbuf.at[pos_z, :, cols_of(c)]
            else:
                src = dst = xbuf.at[(pos_z - s + RING) % RING, pl.ds(d * (rows // 2), rows // 2), cols_of(c)]
        along_y = step < 2 or (step < 4) != z_first
        return pltpu.make_async_remote_copy(
            src_ref=src, dst_ref=dst, send_sem=send_sem.at[c, step, d], recv_sem=recv_sem.at[c, step, d],
            device_id={'head': (y_device if along_y else z_device)(d)}, device_id_type=pl.DeviceIdType.MESH)

    def on_messages(step, c, act):
        if step < 2:
            for d in range(DIRS):
                act(message(step, c, d, False))
            return

        @pl.when(c % 4 == 3)
        def _():
            for d in range(DIRS):
                act(message(step, c, d, True))

        @pl.when(c % 4 != 3)
        def _():
            for d in range(DIRS):
                act(message(step, c, d, False))

    def store(c):
        return pltpu.make_async_copy(xbuf.at[:, :, cols_of(c)], out_ref.at[:, :, cols_of(c)], store_sem.at[c])

    def project(c):
        @pl.when(c + 1 < block_count)
        def _():
            for copy in w_loads(c + 1):
                copy.start()

        for copy in w_loads(c):
            copy.wait()
        total = None
        for j in range(RING):
            z = (pos_z + j) % RING
            down = jnp.dot(hid_ref[z], wtile[c % 2, j, :ff_local, :], preferred_element_type=jnp.float32)
            down = down + jnp.dot(att_ref[z], wtile[c % 2, j, ff_local:, :], preferred_element_type=jnp.float32)
            total = down if total is None else total + down
        part[:, cols_of(c)] = total

    def stage(number, c):
        if number == 0:
            project(c)
        else:
            on_messages(number - 1, c, lambda copy: copy.wait_recv())
        if number == 1:
            for d in range(DIRS):
                piece = rows_of((pos_y + sign[d] + RING) % RING, d * eighth, eighth)
                part[piece, cols_of(c)] = part[piece, cols_of(c)] + landed[c, d, pl.ds(quarter, eighth), :]
        if number == 2:
            own = rows_of(pos_y, 0, quarter)
            total = part[own, cols_of(c)] + landed[c, 0, pl.ds(0, quarter), :] + landed[c, 1, pl.ds(0, quarter), :]
            update = total.astype(jnp.bfloat16).astype(jnp.float32)
            xbuf[pos_z, own, cols_of(c)] = (xres[:, cols_of(c)].astype(jnp.float32) + update).astype(jnp.bfloat16)
        if number < LAST_STEPS:
            on_messages(number, c, lambda copy: copy.start())
        else:
            store(c).start()

    def tick(t, carry):
        for number in range(LAST_STEPS, -1, -1):
            c = t - SKEW * number

            @pl.when(jnp.logical_and(c >= 0, c < block_count))
            def _():
                stage(number, c)
        return carry

    lax.fori_loop(0, block_count + SKEW * LAST_STEPS, tick, 0)

    def drain(c, carry):
        for step in range(LAST_STEPS):
            on_messages(step, c, lambda copy: copy.wait_send())
        store(c).wait()
        return carry

    lax.fori_loop(0, block_count, drain, 0)


def layer_last(layer, hid_all, att_all, x_cur, w_down, w_o, all_down, all_out):
    tok_count, d_model = x_cur.shape
    rows = tok_count // RING
    depth = hid_all.shape[2] + att_all.shape[2]
    any_spec = pl.BlockSpec(memory_space=pl.ANY)
    vmem_spec = pl.BlockSpec(memory_space=pltpu.VMEM)
    blocks = d_model // LAST_COLS
    out = pl.pallas_call(
        functools.partial(last_kernel, layer),
        out_shape=jax.ShapeDtypeStruct((RING, rows, d_model), jnp.bfloat16),
        in_specs=[vmem_spec, vmem_spec] + [any_spec] * 5,
        out_specs=any_spec,
        scratch_shapes=[
            pltpu.VMEM((rows, d_model), jnp.float32),
            pltpu.VMEM((rows // RING, d_model), jnp.bfloat16),
            pltpu.VMEM((RING, rows, d_model), jnp.bfloat16),
            pltpu.VMEM((2, RING, depth, LAST_COLS), jnp.bfloat16),
            pltpu.VMEM((blocks, DIRS, 3 * rows // (2 * RING), LAST_COLS), jnp.float32),
            pltpu.SemaphoreType.DMA((2, RING, 2)),
            pltpu.SemaphoreType.DMA,
            pltpu.SemaphoreType.DMA((blocks,)),
            pltpu.SemaphoreType.DMA((blocks, LAST_STEPS, DIRS)),
            pltpu.SemaphoreType.DMA((blocks, LAST_STEPS, DIRS)),
        ],
        compiler_params=pltpu.CompilerParams(collective_id=layer, has_side_effects=True, vmem_limit_bytes=63 * 1024 * 1024),
        cost_estimate=pl.CostEstimate(flops=2 * tok_count * depth * d_model, bytes_accessed=4 * depth * d_model * 2, transcendentals=0),
        name='last',
    )(hid_all, att_all, x_cur, w_down, w_o, all_down, all_out)
    return out.reshape(tok_count, d_model)


EMIT_PARTS = 8


def emit_kernel(x_ref, k_first, k_second, v_first, v_second, x_out, k_out, v_out, xbuf, rows, load_sem, store_sem):
    size = x_ref.shape[0] // EMIT_PARTS
    loads, stores = [], []
    for n in range(EMIT_PARTS):
        part = pl.ds(n * size, size)
        loads.append(pltpu.make_async_copy(x_ref.at[part, :], xbuf.at[part, :], load_sem.at[n]))
        stores.append(pltpu.make_async_copy(xbuf.at[part, :], x_out.at[part, :], store_sem.at[n]))
    for n, (ref, out) in enumerate(((k_first, k_out.at[0]), (k_second, k_out.at[1]), (v_first, v_out.at[0]), (v_second, v_out.at[1]))):
        loads.append(pltpu.make_async_copy(ref, rows.at[n], load_sem.at[EMIT_PARTS + n]))
        stores.append(pltpu.make_async_copy(rows.at[n], out, store_sem.at[EMIT_PARTS + n]))
    for copy in loads:
        copy.start()
    for load, store in zip(loads, stores):
        load.wait()
        store.start()
    for copy in stores:
        copy.wait()


def emit(x_out, k_first, k_second, v_first, v_second):
    any_spec = pl.BlockSpec(memory_space=pl.ANY)
    cache = jax.ShapeDtypeStruct((2,) + k_first.shape, jnp.bfloat16)
    return pl.pallas_call(
        emit_kernel,
        out_shape=[jax.ShapeDtypeStruct(x_out.shape, jnp.bfloat16), cache, cache],
        in_specs=[any_spec] * 5,
        out_specs=[any_spec] * 3,
        scratch_shapes=[
            pltpu.VMEM(x_out.shape, jnp.bfloat16),
            pltpu.VMEM((4,) + k_first.shape, jnp.bfloat16),
            pltpu.SemaphoreType.DMA((EMIT_PARTS + 4,)),
            pltpu.SemaphoreType.DMA((EMIT_PARTS + 4,)),
        ],
        compiler_params=pltpu.CompilerParams(vmem_limit_bytes=63 * 1024 * 1024),
        name='emit',
    )(x_out, k_first, k_second, v_first, v_second)


def solution(mesh):
    row_spec = P(('batch', 'seq'), None)
    pos_spec = P(('batch', 'seq'))
    head_spec = P(None, None, 'head', None)
    out_proj_spec = P(None, 'head', None, None)
    col_spec = P(None, None, 'head')
    down_spec = P(None, 'head', None)
    cache_spec = P(None, ('batch', 'seq'), 'head', None)

    def local_forward(x_loc, pos_loc, w_q, w_k, w_v, w_o, w_gate, w_up, w_down, norm_gain):
        tok_count, d_model = x_loc.shape
        layer_count = w_q.shape[0]
        head_dim = w_q.shape[3]
        flat_q, flat_k, flat_v = (w.reshape(layer_count, d_model, head_dim) for w in (w_q, w_k, w_v))
        cos_t, sin_t = rope_tables(pos_loc, head_dim)
        hidden, attn_heads, k_first, v_first, all_down, all_out = layer_head(0, x_loc, cos_t, sin_t, norm_gain, flat_q, flat_k, flat_v, w_gate, w_up, w_down, w_o, False)
        x_mid, all_down, all_out = layer_tail(0, hidden, attn_heads, x_loc, w_down, w_o, all_down, all_out)
        hid_all, att_all, k_second, v_second = layer_head(1, x_mid, cos_t, sin_t, norm_gain, flat_q, flat_k, flat_v, w_gate, w_up, w_down, w_o, True)
        x_out = layer_last(1, hid_all, att_all, x_mid, w_down, w_o, all_down, all_out)
        x_out, k_all, v_all = emit(x_out, k_first, k_second, v_first, v_second)
        cache_shape = (layer_count, tok_count, 1, head_dim)
        return x_out, k_all.reshape(cache_shape), v_all.reshape(cache_shape)

    return jax.shard_map(local_forward, mesh=mesh, in_specs=(row_spec, pos_spec, head_spec, head_spec, head_spec, out_proj_spec, col_spec, col_spec, down_spec, P(None, None)), out_specs=(row_spec, cache_spec, cache_spec), check_vma=False)
```

```python
import functools
import math
import jax
import jax.numpy as jnp
from jax import lax
from jax.experimental import pallas as pl
from jax.experimental.pallas import tpu as pltpu
from jax.sharding import PartitionSpec as P

ROPE_BASE = 500000.0
EPS = 1e-5


def rope_tables(positions, head_dim):
    half_dim = head_dim // 2
    inv_freq = ROPE_BASE ** (-(jnp.arange(half_dim, dtype=jnp.float32) * 2.0 / head_dim))
    angles = positions.astype(jnp.float32)[..., None] * inv_freq
    return jnp.cos(angles), jnp.sin(angles)


CHIPS = 4
RING = 4
HALVES = 2
DIRS = 2
KV_CHUNKS = 4
W_TILE = 256
NORM_ROWS = 64
CHUNKS = 8
STEPS = 8
PART_SLOTS = 4
RECV_SLOTS = 5
DOWN_TILE = 512
START_GAP = 3
STAGE_GAP = 2
BLOCK_TICK = 19
BLOCK_GAP = 6
LAST_TICK = 43
NEAR_TICKS = ((9, 1), (15, 3))
FAR_TICKS = ((24, 1), (26, 3))
SERVE_TICKS = (31, 35, 39, 42)


def front_kernel(x_ref, cos_ref, sin_ref, gain_ref, wq_ref, wk_ref, wv_ref, wg_ref, wu_ref, wd_ref, wo_ref,
                 hid_all_ref, att_all_ref, k1_ref, v1_ref, k2_ref, v2_ref, gd_ref, go_ref, rest_ref,
                 xbuf, part, recv_a, recv_b, hid, att, wdo, wtile, kv, qbuf, acc, row_max, row_sum, xs, xres,
                 x_sem, res_sem, w_sem, down_sem, cache_sem, rest_sem, own_send, pass_send, ici_recv, core_recv, part_send, part_recv,
                 round_send, round_recv, side_send, side_recv, give_send, give_recv, keep_sem, ring_send, ring_recv, ready_sem):
    tok_count, d_model = xbuf.shape
    head_dim = qbuf.shape[1]
    half_dim = head_dim // 2
    ff_local = hid.shape[1]
    rows_per = tok_count // KV_CHUNKS
    half_rows = tok_count // 2
    lanes = row_max.shape[2]
    chunk_rows = tok_count // CHUNKS
    quarter, eighth = chunk_rows // RING, chunk_rows // (2 * RING)
    half_cols = d_model // HALVES
    piece_cols = half_cols // RING
    bf16, f32 = jnp.bfloat16, jnp.float32
    sign = (1, -1)
    mesh_id = pl.DeviceIdType.MESH

    my_head = lax.axis_index('head')
    pos_z, pos_y = my_head // RING, my_head % RING
    my_seq = lax.axis_index('seq')
    chip, core = my_seq // 2, my_seq % 2
    other = chip * 2 + 1 - core

    def wrap(n):
        return (n + RING) % RING

    def y_peer(d):
        return pos_z * RING + wrap(pos_y + sign[d])

    def z_device(z):
        return wrap(z) * RING + pos_y

    def z_peer(d):
        return z_device(pos_z + sign[d])

    def x_device(n):
        return wrap(chip + n) * 2 + core

    right, left = x_device(1), x_device(-1)

    def span(start, size, unit=None):
        return pl.ds(pl.multiple_of(start, unit or size), size)

    def remote(src, dst, send, recv, **to):
        return pltpu.make_async_remote_copy(src_ref=src, dst_ref=dst, send_sem=send, recv_sem=recv, device_id=to, device_id_type=mesh_id)

    def x_load(i):
        return pltpu.make_async_copy(x_ref.at[span(i * rows_per, rows_per), :], xs.at[i % 2], x_sem.at[i % 2])

    def weights(layer, piece):
        slot = piece % 2
        if isinstance(piece, int) and piece < 2:
            refs = ((wk_ref, wv_ref), (wq_ref,))[piece]
            return [pltpu.make_async_copy(ref.at[layer], wtile.at[slot, n], w_sem.at[slot, n]) for n, ref in enumerate(refs)]
        cols = span((piece - 2) * W_TILE, W_TILE)
        return [pltpu.make_async_copy(ref.at[layer, :, cols], wtile.at[slot, n], w_sem.at[slot, n]) for n, ref in enumerate((wg_ref, wu_ref))]

    def start(copies):
        for copy in copies:
            copy.start()

    def wait(copies):
        for copy in copies:
            copy.wait()

    down_tiles = d_model // DOWN_TILE

    def down_load(i):
        cols = span(i * DOWN_TILE, DOWN_TILE)
        return [pltpu.make_async_copy(wd_ref.at[0, :, cols], wdo.at[i % 2, pl.ds(0, ff_local), :], down_sem.at[i % 2, 0]),
                pltpu.make_async_copy(wo_ref.at[0, 0, :, cols], wdo.at[i % 2, pl.ds(ff_local, head_dim), :], down_sem.at[i % 2, 1])]

    def kv_copy(origin_chip, origin_core, i, to, send, recv):
        rows = kv.at[span((origin_chip * 2 + origin_core) * tok_count + i * rows_per, rows_per), :]
        return remote(rows, rows, send, recv, seq=to)

    def kv_routes(layer, i):
        late = i >= KV_CHUNKS // 2
        early = jnp.logical_not(late) if not isinstance(i, int) else not late

        def to(send, recv, origin_chip, origin_core, device):
            return kv_copy(origin_chip, origin_core, i, device, send, recv)
        own, passed, ici, side = own_send.at[layer], pass_send.at[layer], ici_recv.at[layer], core_recv.at[layer]
        return {
            'right': (chip < CHIPS - 1, lambda: to(own.at[0, i], ici.at[0, i], chip, core, right)),
            'wrap': (chip == 0, lambda: to(own.at[1, i], ici.at[2, i], chip, core, left)),
            'relay': (jnp.logical_and(late, chip == 1), lambda: to(own.at[3, i], ici.at[3, i], chip, core, left)),
            'other': (core == 0, lambda: to(own.at[2, i], side.at[0, i], chip, core, other)),
            'on_right': (jnp.logical_and(early, jnp.logical_and(chip >= 1, chip < CHIPS - 1)), lambda: to(passed.at[0, i], ici.at[1, i], chip - 1, core, right)),
            'from_relay': (jnp.logical_and(late, chip == 0), lambda: to(passed.at[0, i], ici.at[1, i], 1, core, left)),
            'on_left': (jnp.logical_and(late, chip == CHIPS - 1), lambda: to(passed.at[0, i], ici.at[1, i], 0, core, left)),
            'side1': (chip >= 1, lambda: to(passed.at[1, i], side.at[1, i], chip - 1, core, other)),
            'side2': (chip >= 2, lambda: to(passed.at[2, i], side.at[2, i], chip - 2, core, other)),
            'side3': (chip >= 3, lambda: to(passed.at[3, i], side.at[3, i], chip - 3, core, other)),
        }

    def start_route(layer, i, name):
        condition, copy = kv_routes(layer, i)[name]

        @pl.when(condition)
        def _():
            copy().start()

    def send_kv(layer, i):
        for name in ('right', 'wrap', 'relay', 'other'):
            start_route(layer, i, name)

    def kv_sent(layer):
        for i in range(KV_CHUNKS):
            for condition, copy in kv_routes(layer, i).values():
                @pl.when(condition)
                def _():
                    copy().wait_send()

    def serve(layer, back, i):
        @pl.when(chip >= back)
        def _():
            kv_copy(chip - back, core, i, other, pass_send.at[layer, back, i], ici_recv.at[layer, back - 1, i]).wait_recv()
        start_route(layer, i, 'side%d' % back)
        if back == 1:
            start_route(layer, i, 'on_right')
        if back == 3:
            start_route(layer, i, 'on_left')

    def relay(layer, i):
        condition, copy = kv_routes(layer, i)['from_relay']

        @pl.when(condition)
        def _():
            kv_copy(1, core, i, left, pass_send.at[layer, 0, i], ici_recv.at[layer, 3, i]).wait_recv()
            copy().start()

    def serve_all(layer, i):
        serve(layer, 1, i)
        serve(layer, 3, i)
        relay(layer, i)

    def taken(layer, back, chunks):
        for i in chunks:
            kv_copy(chip - back, 1 - core, i, other, pass_send.at[layer, 0, i], core_recv.at[layer, back, i]).wait_recv()

    def z_parts(step, d):
        copies = []
        for n, (own_ref, all_ref) in enumerate(((wd_ref, gd_ref), (wo_ref, go_ref))):
            size = all_ref.shape[1] // (2 * CHIPS)
            if step == 0:
                rows = span(my_seq * size, size)
                src = own_ref.at[1, rows, :] if n == 0 else own_ref.at[1, 0, rows, :]
                dst = all_ref.at[pos_z, rows, :]
            else:
                rows = span(my_seq * size + d * (size // 2), size // 2)
                src = dst = all_ref.at[wrap(pos_z - sign[d]), rows, :]
            copies.append(remote(src, dst, part_send.at[step, d, n], part_recv.at[step, d, n], head=z_peer(d)))
        return copies

    def part_copies(j, part_chip, part_core, half, send, recv, to):
        copies = []
        for n, ref in enumerate((gd_ref, go_ref)):
            size = ref.shape[1] // (2 * CHIPS)
            first = (part_chip * 2 + part_core) * size
            rows = span(first, size) if half is None else span(first + half * (size // 2), size // 2)
            place = ref.at[wrap(pos_z + j), rows, :]
            copies.append(remote(place, place, send.at[n], recv.at[n], seq=to))
        return copies

    def own_part(j, d):
        return part_copies(j, chip, core, None, round_send.at[0, j - 1, d], round_recv.at[0, j - 1, d], x_device(sign[d]))

    def far_part(j, d):
        return part_copies(j, wrap(chip - sign[d]), core, d, round_send.at[1, j - 1, d], round_recv.at[1, j - 1, d], x_device(sign[d]))

    def side_part(j, n, side):
        return part_copies(j, wrap(chip + n), side, None, side_send.at[j - 1, n], side_recv.at[j - 1, n], other)

    def round_start(j):
        for d in range(DIRS):
            start(own_part(j, d))
        start(side_part(j, 0, core))

    def near_parts(j):
        for d in range(DIRS):
            for copy in own_part(j, d):
                copy.wait_recv()
            start(far_part(j, d) + side_part(j, 3 if d == 0 else 1, core))

    def far_parts(j):
        for d in range(DIRS):
            for copy in far_part(j, d):
                copy.wait_recv()
        start(side_part(j, 2, core))

    def give_hidden(z, i, source):
        cols = span(i * W_TILE, W_TILE)
        return remote(hid.at[span(z * rows_per, rows_per), cols], hid_all_ref.at[source, :, cols], give_send.at[z, i], give_recv.at[source, i], head=z_device(z))

    def keep_hidden(i):
        cols = span(i * W_TILE, W_TILE)
        return pltpu.make_async_copy(hid.at[span(pos_z * rows_per, rows_per), cols], hid_all_ref.at[pos_z, :, cols], keep_sem.at[i])

    def give_rows(z, source):
        return remote(att.at[span(z * rows_per, rows_per), :], att_all_ref.at[source], give_send.at[z, KV_CHUNKS], give_recv.at[source, KV_CHUNKS], head=z_device(z))

    def keep_rows():
        return pltpu.make_async_copy(att.at[span(pos_z * rows_per, rows_per), :], att_all_ref.at[pos_z], keep_sem.at[KV_CHUNKS])

    def norm_rows(x_few, layer):
        x_f32 = x_few.astype(f32)
        inv_rms = lax.rsqrt(jnp.mean(x_f32 * x_f32, axis=-1, keepdims=True) + EPS)
        return (x_f32 * inv_rms * gain_ref[pl.ds(layer, 1), :].astype(f32)).astype(bf16)

    def rope(values, rows):
        cos_t, sin_t = cos_ref[rows, :], sin_ref[rows, :]
        wide = values.astype(bf16).astype(f32)
        first, second = wide[:, :half_dim], wide[:, half_dim:]
        return jnp.concatenate([first * cos_t - second * sin_t, second * cos_t + first * sin_t], axis=1).astype(bf16)

    def dot(a, b):
        return jnp.dot(a, b, preferred_element_type=f32)

    scale = 1.0 / math.sqrt(head_dim)

    def keys_values(normed, i):
        rows = span(i * rows_per, rows_per)
        own = span(my_seq * tok_count + i * rows_per, rows_per)
        kv[own, :head_dim] = rope(dot(normed, wtile[0, 0]), rows)
        kv[own, head_dim:] = dot(normed, wtile[0, 1]).astype(bf16)

    def queries(normed, i):
        rows = span(i * rows_per, rows_per)
        qbuf[rows, :] = (rope(dot(normed, wtile[1, 0]), rows).astype(f32) * scale).astype(bf16)

    def gated(normed, i, tile):
        gate = dot(normed, wtile[tile % 2, 0])
        up = dot(normed, wtile[tile % 2, 1])
        hid[span(i * rows_per, rows_per), span(tile * W_TILE, W_TILE)] = (gate * jax.nn.sigmoid(gate) * up).astype(bf16)

    def attend(key_start, q_half, side, masked, first):
        rows = pl.ds(q_half * half_rows, half_rows)
        some = span(key_start, half_rows)
        logits = lax.dot_general(qbuf[rows, :], kv[some, :head_dim], (((1,), (1,)), ((), ())), preferred_element_type=f32)
        if masked:
            seen = lax.broadcasted_iota(jnp.int32, logits.shape, 0) >= lax.broadcasted_iota(jnp.int32, logits.shape, 1)
            logits = jnp.where(seen, logits, -jnp.inf)
        block_max = jnp.max(logits, axis=-1, keepdims=True)
        if first:
            new_max = jnp.broadcast_to(block_max, (half_rows, lanes))
        else:
            new_max = jnp.maximum(row_max[side, rows, :], block_max)
        prob = jnp.exp(logits - jnp.concatenate([new_max] * (half_rows // lanes), axis=1))
        block_sum = jnp.sum(prob, axis=-1, keepdims=True)
        block_out = dot(prob.astype(bf16), kv[some, head_dim:])
        if first:
            row_sum[side, rows, :] = jnp.broadcast_to(block_sum, (half_rows, lanes))
            acc[side, rows, :] = block_out
        else:
            rescale = jnp.exp(row_max[side, rows, :] - new_max)
            row_sum[side, rows, :] = row_sum[side, rows, :] * rescale + block_sum
            acc[side, rows, :] = acc[side, rows, :] * jnp.concatenate([rescale] * (head_dim // lanes), axis=1) + block_out
        row_max[side, rows, :] = new_max

    def attend_own():
        own_start = my_seq * tok_count
        attend(own_start, 0, 0, True, True)
        attend(own_start, 1, 0, False, True)
        attend(own_start + half_rows, 1, 1, True, True)
        top_rows = pl.ds(0, half_rows)
        row_max[1, top_rows, :] = jnp.full((half_rows, lanes), -jnp.inf, f32)
        row_sum[1, top_rows, :] = jnp.zeros((half_rows, lanes), f32)
        acc[1, top_rows, :] = jnp.zeros((half_rows, head_dim), f32)

    def past_start(n):
        later = n - core
        back = jnp.where(later < 2, 1, jnp.where(chip == CHIPS - 1, jnp.where(later < 4, 3, 2), 2))
        block = (chip - back) * 2 + jnp.where(later % 2 == 0, core, 1 - core)
        return jnp.where(jnp.logical_and(core == 1, n == 0), chip * 2, block) * tok_count

    def attend_past(layer, chunks, visits):
        def past(n, carry):
            @pl.when(jnp.logical_and(core == 1, n == 0))
            def _():
                taken(layer, 0, chunks)

            for back in (1, 3, 2):
                place = 0 if back == 1 else 2 if back == 3 else jnp.where(chip == CHIPS - 1, 4, 2)
                if back == 2:
                    @pl.when(jnp.logical_and(chip >= back, n == core + place))
                    def _():
                        for i in chunks:
                            serve(layer, 2, i)

                @pl.when(jnp.logical_and(chip >= back, n == core + place + 1))
                def _():
                    taken(layer, back, chunks)
            for q_half, side in visits:
                attend(past_start(n) + side * half_rows, q_half, side, False, False)
            return carry

        lax.fori_loop(0, my_seq, past, 0)

    def finish(i, spread):
        rows = pl.ds(i * rows_per, rows_per)
        top = jnp.maximum(row_max[0, rows, :], row_max[1, rows, :])
        shares = [jnp.exp(row_max[side, rows, :] - top) for side in range(2)]
        total = shares[0] * row_sum[0, rows, :] + shares[1] * row_sum[1, rows, :]
        wide = [jnp.concatenate([w] * (head_dim // lanes), axis=1) for w in shares + [total]]
        att[rows, :] = ((acc[0, rows, :] * wide[0] + acc[1, rows, :] * wide[1]) / wide[2]).astype(bf16)
        if spread:
            @pl.when(i == pos_z)
            def _():
                keep_rows().start()

            @pl.when(i != pos_z)
            def _():
                give_rows(i, pos_z).start()

    first_pos, second_pos = (pos_y, pos_z), (pos_z, pos_y)
    first_peer, second_peer = (y_peer, z_peer), (z_peer, y_peer)

    def part_rows(chunk, piece, offset, count):
        return span((chunk % PART_SLOTS) * chunk_rows + piece * quarter + offset, count, eighth)

    def x_rows(chunk, piece, offset, count):
        return span(chunk * chunk_rows + piece * quarter + offset, count, eighth)

    def cols_of(h, piece):
        return span(h * half_cols + piece * piece_cols, piece_cols)

    def half_of(h):
        return pl.ds(h * half_cols, half_cols)

    def message(step, chunk, h, d):
        p1, p2, s = first_pos[h], second_pos[h], sign[d]
        slot = chunk % RECV_SLOTS
        if step == 0:
            src, dst = part.at[part_rows(chunk, wrap(p1 + 2), d * eighth, eighth), half_of(h)], recv_a.at[slot, h, d, pl.ds(quarter, eighth), :]
        elif step == 1:
            src, dst = part.at[part_rows(chunk, wrap(p1 + s), 0, quarter), half_of(h)], recv_a.at[slot, h, d, pl.ds(0, quarter), :]
        elif step == 2:
            src, dst = part.at[part_rows(chunk, p1, d * eighth, eighth), cols_of(h, wrap(p2 + 2))], recv_b.at[slot, h, d, pl.ds(quarter, eighth), :]
        elif step == 3:
            src, dst = part.at[part_rows(chunk, p1, 0, quarter), cols_of(h, wrap(p2 + s))], recv_b.at[slot, h, d, pl.ds(0, quarter), :]
        elif step == 4:
            src = dst = xbuf.at[x_rows(chunk, p1, 0, quarter), cols_of(h, p2)]
        elif step == 5:
            src = dst = xbuf.at[x_rows(chunk, p1, d * eighth, eighth), cols_of(h, wrap(p2 - s))]
        elif step == 6:
            src = dst = xbuf.at[x_rows(chunk, p1, 0, quarter), half_of(h)]
        else:
            src = dst = xbuf.at[x_rows(chunk, wrap(p1 - s), d * eighth, eighth), half_of(h)]
        peer = (first_peer if step in (0, 1, 6, 7) else second_peer)[h](d)
        return remote(src, dst, ring_send.at[chunk, step, h * DIRS + d], ring_recv.at[chunk, step, h * DIRS + d], head=peer)

    def each_message(chunk, steps, act):
        for step in steps:
            for h in range(HALVES):
                for d in range(DIRS):
                    act(message(step, chunk, h, d))

    def residual_load(chunk, h):
        return pltpu.make_async_copy(x_ref.at[x_rows(chunk, first_pos[h], 0, quarter), cols_of(h, second_pos[h])], xres.at[chunk, h], res_sem.at[chunk, h])

    def project(chunk):
        rows = span(chunk * chunk_rows, chunk_rows)
        slot_rows = span((chunk % PART_SLOTS) * chunk_rows, chunk_rows)

        def one_tile(i, carry):
            @pl.when(jnp.logical_or(chunk < CHUNKS - 1, i < down_tiles - 1))
            def _():
                start(down_load((i + 1) % down_tiles))

            wait(down_load(i))
            total = dot(hid[rows, :], wdo[i % 2, :ff_local, :])
            part[slot_rows, span(i * DOWN_TILE, DOWN_TILE)] = total + dot(att[rows, :], wdo[i % 2, ff_local:, :])
            return carry

        lax.fori_loop(0, down_tiles, one_tile, 0)

    def stage(number, chunk):
        slot = chunk % RECV_SLOTS
        if number == 0:
            @pl.when(chunk >= PART_SLOTS)
            def _():
                each_message(chunk - PART_SLOTS, range(4), lambda copy: copy.wait_send())
            project(chunk)
        for h in range(HALVES):
            p1, p2 = first_pos[h], second_pos[h]
            if number:
                for d in range(DIRS):
                    message(number - 1, chunk, h, d).wait_recv()
            if number in (1, 3):
                for d in range(DIRS):
                    if number == 1:
                        rows, cols, arrived = part_rows(chunk, wrap(p1 + sign[d]), d * eighth, eighth), half_of(h), recv_a
                    else:
                        rows, cols, arrived = part_rows(chunk, p1, d * eighth, eighth), cols_of(h, wrap(p2 + sign[d])), recv_b
                    part[rows, cols] = part[rows, cols] + arrived[slot, h, d, pl.ds(quarter, eighth), :]
            if number == 2:
                rows = part_rows(chunk, p1, 0, quarter)
                part[rows, half_of(h)] = part[rows, half_of(h)] + recv_a[slot, h, 0, pl.ds(0, quarter), :] + recv_a[slot, h, 1, pl.ds(0, quarter), :]
            if number == 4:
                residual_load(chunk, h).wait()
                rows, cols = part_rows(chunk, p1, 0, quarter), cols_of(h, p2)
                total = part[rows, cols] + recv_b[slot, h, 0, pl.ds(0, quarter), :] + recv_b[slot, h, 1, pl.ds(0, quarter), :]
                update = total.astype(bf16).astype(f32)
                xbuf[x_rows(chunk, p1, 0, quarter), cols] = (xres[chunk, h].astype(f32) + update).astype(bf16)
            if number < STEPS:
                for d in range(DIRS):
                    message(number, chunk, h, d).start()

    x_load(0).start()
    start(weights(0, 0))
    x_load(1).start()
    start(weights(0, 1))
    barrier = pltpu.get_barrier_semaphore()
    for peer in (left, right, other):
        pl.semaphore_signal(barrier, inc=1, device_id={'seq': peer}, device_id_type=mesh_id)
    for peer in [z_device(pos_z + j) for j in range(1, RING)] + [y_peer(d) for d in range(DIRS)]:
        pl.semaphore_signal(barrier, inc=1, device_id={'head': peer}, device_id_type=mesh_id)
    pl.semaphore_wait(barrier, 8)
    for d in range(DIRS):
        start(z_parts(0, d))

    def prepare(i, carry):
        x_load(i).wait()

        def few(n, inner):
            xbuf[span(i * rows_per + n * NORM_ROWS, NORM_ROWS), :] = norm_rows(xs[i % 2, span(n * NORM_ROWS, NORM_ROWS), :], 0)
            return inner

        lax.fori_loop(0, rows_per // NORM_ROWS, few, 0)

        @pl.when(i + 2 < KV_CHUNKS)
        def _():
            x_load(i + 2).start()

        @pl.when(i == 0)
        def _():
            wait(weights(0, 0))

        keys_values(xbuf[span(i * rows_per, rows_per), :], i)
        send_kv(0, i)
        return carry

    lax.fori_loop(0, KV_CHUNKS, prepare, 0)
    start(weights(0, 2))
    own_rows = span(my_seq * tok_count, tok_count)

    def cache_stores(layer):
        k_ref, v_ref = ((k1_ref, v1_ref), (k2_ref, v2_ref))[layer]
        return [pltpu.make_async_copy(kv.at[own_rows, pl.ds(0, head_dim)], k_ref, cache_sem.at[layer, 0]),
                pltpu.make_async_copy(kv.at[own_rows, pl.ds(head_dim, head_dim)], v_ref, cache_sem.at[layer, 1])]

    start(cache_stores(0))
    wait(weights(0, 1))

    def query(i, carry):
        queries(xbuf[span(i * rows_per, rows_per), :], i)
        return carry

    lax.fori_loop(0, KV_CHUNKS, query, 0)
    start(weights(0, 3))
    start(down_load(0))

    def residuals(n, carry):
        for h in range(HALVES):
            residual_load(n, h).start()
        return carry

    lax.fori_loop(0, CHUNKS, residuals, 0)

    def gate_tile(tile, carry):
        wait(weights(0, tile + 2))

        def rows_step(i, inner):
            gated(xbuf[span(i * rows_per, rows_per), :], i, tile)
            return inner

        lax.fori_loop(0, KV_CHUNKS, rows_step, 0)

        @pl.when(tile < 2)
        def _():
            start(weights(0, tile + 4))

        @pl.when(tile == 2)
        def _():
            start(weights(1, 0))
            for d in range(DIRS):
                for copy in z_parts(0, d):
                    copy.wait_recv()
                start(z_parts(1, d))

        @pl.when(tile == 3)
        def _():
            start(weights(1, 1))
        serve_all(0, tile)
        return carry

    lax.fori_loop(0, ff_local // W_TILE, gate_tile, 0)
    attend_own()
    attend_past(0, range(KV_CHUNKS), ((0, 0), (0, 1)))
    finish(0, False)
    finish(1, False)
    round_start(1)
    round_start(3)

    def block_work(j, phase):
        @pl.when(phase == 0)
        def _():
            @pl.when(j == 0)
            def _():
                for n in range(3):
                    pl.semaphore_wait(ready_sem.at[n], 1)

            def few(n, inner):
                xs[0, span(n * NORM_ROWS, NORM_ROWS), :] = norm_rows(xbuf[span(j * rows_per + n * NORM_ROWS, NORM_ROWS), :], 1)
                return inner

            lax.fori_loop(0, rows_per // NORM_ROWS, few, 0)
            wait(weights(1, 0))
            keys_values(xs[0], j)
            send_kv(1, j)
            start(weights(1, 2))

        @pl.when(phase == 1)
        def _():
            wait(weights(1, 1))
            queries(xs[0], j)
            start(weights(1, 3))

        @pl.when(jnp.logical_and(phase >= 1, phase <= 4))
        def _():
            tile = phase - 1
            wait(weights(1, tile + 2))
            gated(xs[0], j, tile)

            @pl.when(tile < 2)
            def _():
                start(weights(1, tile + 4))

            @pl.when(jnp.logical_and(tile == 2, j < KV_CHUNKS - 1))
            def _():
                start(weights(1, 0))

            @pl.when(jnp.logical_and(tile == 3, j < KV_CHUNKS - 1))
            def _():
                start(weights(1, 1))

            @pl.when(j == pos_z)
            def _():
                keep_hidden(tile).start()

            @pl.when(j != pos_z)
            def _():
                give_hidden(j, tile, pos_z).start()

    def tick(t, carry):
        for number in range(STEPS, -1, -1):
            place = t - STAGE_GAP * number
            chunk = place // START_GAP

            @pl.when(jnp.logical_and(place >= 0, jnp.logical_and(place % START_GAP == 0, chunk < CHUNKS)))
            def _():
                stage(number, chunk)

        @pl.when(jnp.logical_and(t >= 1, jnp.logical_and(t < 8, t <= my_seq)))
        def _():
            for side in range(2):
                attend(past_start(t - 1) + side * half_rows, 1, side, False, False)

        @pl.when(t == 2)
        def _():
            for d in range(DIRS):
                for copy in z_parts(1, d):
                    copy.wait_recv()
            round_start(2)

        @pl.when(t == 8)
        def _():
            finish(2, False)
            finish(3, False)
            kv_sent(0)
            wait(cache_stores(0))
            for n, peer in enumerate((left, right, other)):
                pl.semaphore_signal(ready_sem.at[n], inc=1, device_id={'seq': peer}, device_id_type=mesh_id)

        for when, j in NEAR_TICKS:
            @pl.when(t == when)
            def _():
                near_parts(j)

        for when, j in FAR_TICKS:
            @pl.when(t == when)
            def _():
                far_parts(j)

        late = t - BLOCK_TICK

        @pl.when(late >= 0)
        def _():
            block_work(late // BLOCK_GAP, late % BLOCK_GAP)

        for i, when in enumerate(SERVE_TICKS):
            @pl.when(t == when)
            def _():
                serve_all(1, i)
        return carry

    lax.fori_loop(0, LAST_TICK, tick, 0)

    start(cache_stores(1))
    rest_store = pltpu.make_async_copy(xbuf.at[span(pos_z * rows_per + pos_y * (rows_per // RING), rows_per // RING), :], rest_ref, rest_sem)
    rest_store.start()
    near_parts(2)
    attend_own()
    attend_past(1, (0, 1), ((0, 0), (1, 0)))
    attend_past(1, (2, 3), ((0, 1), (1, 1)))
    for i in range(KV_CHUNKS):
        finish(i, True)
    far_parts(2)

    wait(cache_stores(1))
    rest_store.wait()
    for i in range(KV_CHUNKS):
        keep_hidden(i).wait()
    keep_rows().wait()
    kv_sent(1)
    for d in range(DIRS):
        for step in range(2):
            for copy in z_parts(step, d):
                copy.wait_send()
    for j in range(1, RING):
        for d in range(DIRS):
            for copy in own_part(j, d) + far_part(j, d):
                copy.wait_send()
        for n in range(CHIPS):
            for copy in side_part(j, n, 1 - core):
                copy.wait_recv()
            for copy in side_part(j, n, core):
                copy.wait_send()
        z = wrap(pos_z + j)
        for i in range(KV_CHUNKS):
            give_hidden(z, i, z).wait_recv()
            give_hidden(z, i, pos_z).wait_send()
        give_rows(z, z).wait_recv()
        give_rows(z, pos_z).wait_send()

    def drain(chunk, carry):
        @pl.when(chunk >= CHUNKS - PART_SLOTS)
        def _():
            each_message(chunk, range(4), lambda copy: copy.wait_send())
        each_message(chunk, range(4, STEPS), lambda copy: copy.wait_send())
        return carry

    lax.fori_loop(0, CHUNKS, drain, 0)


def front(x_loc, cos_t, sin_t, norm_gain, w_q, w_k, w_v, w_gate, w_up, w_down, w_o):
    tok_count, d_model = x_loc.shape
    head_dim = w_q.shape[2]
    ff_local = w_gate.shape[2]
    rows_per = tok_count // KV_CHUNKS
    chunk_rows = tok_count // CHUNKS
    landed = 3 * chunk_rows // (2 * RING)
    half_cols = d_model // HALVES
    any_spec = pl.BlockSpec(memory_space=pl.ANY)
    vmem_spec = pl.BlockSpec(memory_space=pltpu.VMEM)
    bf16, f32 = jnp.bfloat16, jnp.float32
    dma = pltpu.SemaphoreType.DMA
    shape = jax.ShapeDtypeStruct
    return pl.pallas_call(
        front_kernel,
        out_shape=[shape((RING, rows_per, ff_local), bf16), shape((RING, rows_per, head_dim), bf16)] + [shape((tok_count, head_dim), bf16)] * 4
        + [shape((RING, ff_local, d_model), bf16), shape((RING, head_dim, d_model), bf16), shape((rows_per // RING, d_model), bf16)],
        in_specs=[any_spec, vmem_spec, vmem_spec, vmem_spec] + [any_spec] * 7,
        out_specs=[any_spec] * 9,
        scratch_shapes=[
            pltpu.VMEM((tok_count, d_model), bf16),
            pltpu.VMEM((PART_SLOTS * chunk_rows, d_model), f32),
            pltpu.VMEM((RECV_SLOTS, HALVES, DIRS, landed, half_cols), f32),
            pltpu.VMEM((RECV_SLOTS, HALVES, DIRS, landed, half_cols // RING), f32),
            pltpu.VMEM((tok_count, ff_local), bf16),
            pltpu.VMEM((tok_count, head_dim), bf16),
            pltpu.VMEM((2, ff_local + head_dim, DOWN_TILE), bf16),
            pltpu.VMEM((2, 2, d_model, W_TILE), bf16),
            pltpu.VMEM((2 * CHIPS * tok_count, 2 * head_dim), bf16),
            pltpu.VMEM((tok_count, head_dim), bf16),
            pltpu.VMEM((2, tok_count, head_dim), f32),
            pltpu.VMEM((2, tok_count, 128), f32),
            pltpu.VMEM((2, tok_count, 128), f32),
            pltpu.VMEM((2, rows_per, d_model), bf16),
            pltpu.VMEM((CHUNKS, HALVES, chunk_rows // RING, half_cols // RING), bf16),
            dma((2,)), dma((CHUNKS, HALVES)), dma((2, 2)), dma((2, 2)), dma((2, 2)), dma,
            dma((2, 4, KV_CHUNKS)), dma((2, 4, KV_CHUNKS)), dma((2, 4, KV_CHUNKS)), dma((2, 4, KV_CHUNKS)), dma((2, DIRS, 2)), dma((2, DIRS, 2)),
            dma((2, RING - 1, DIRS, 2)), dma((2, RING - 1, DIRS, 2)), dma((RING - 1, CHIPS, 2)), dma((RING - 1, CHIPS, 2)),
            dma((RING, KV_CHUNKS + 1)), dma((RING, KV_CHUNKS + 1)), dma((KV_CHUNKS + 1,)),
            dma((CHUNKS, STEPS, HALVES * DIRS)), dma((CHUNKS, STEPS, HALVES * DIRS)),
            pltpu.SemaphoreType.REGULAR((3,)),
        ],
        compiler_params=pltpu.CompilerParams(collective_id=0, has_side_effects=True, vmem_limit_bytes=67043328),
        name='front',
    )(x_loc, cos_t, sin_t, norm_gain, w_q, w_k, w_v, w_gate, w_up, w_down, w_o)


SKEW = 2
LAST_STEPS = 6
LAST_COLS = 256


def last_kernel(layer, hid_ref, att_ref, rest_ref, wd_ref, wo_ref, gd_ref, go_ref, out_ref, part, xres, xbuf, wtile, landed, w_sem, x_sem, store_sem, send_sem, recv_sem):
    rows, d_model = part.shape
    block = wtile.shape[3]
    block_count = d_model // block
    ff_local = hid_ref.shape[2]
    quarter, eighth = rows // RING, rows // (2 * RING)
    my_head = lax.axis_index('head')
    pos_z, pos_y = my_head // RING, my_head % RING
    sign = (1, -1)

    def cols_of(c):
        return pl.ds(pl.multiple_of(c * block, block), block)

    def w_loads(c):
        copies = []
        for j in range(RING):
            z = (pos_z + j) % RING
            down = wd_ref.at[layer, :, cols_of(c)] if j == 0 else gd_ref.at[z, :, cols_of(c)]
            out = wo_ref.at[layer, 0, :, cols_of(c)] if j == 0 else go_ref.at[z, :, cols_of(c)]
            copies.append(pltpu.make_async_copy(down, wtile.at[c % 2, j, pl.ds(0, ff_local), :], w_sem.at[c % 2, j, 0]))
            copies.append(pltpu.make_async_copy(out, wtile.at[c % 2, j, pl.ds(ff_local, wo_ref.shape[2]), :], w_sem.at[c % 2, j, 1]))
        return copies

    for copy in w_loads(0):
        copy.start()
    x_load = pltpu.make_async_copy(rest_ref, xres, x_sem)
    x_load.start()

    def y_device(d):
        return pos_z * RING + (pos_y + sign[d] + RING) % RING

    def z_device(d):
        return (pos_z + sign[d] + RING) % RING * RING + pos_y

    barrier = pltpu.get_barrier_semaphore()
    for device in (y_device, z_device):
        for d in range(DIRS):
            pl.semaphore_signal(barrier, inc=1, device_id={'head': device(d)}, device_id_type=pl.DeviceIdType.MESH)
    pl.semaphore_wait(barrier, 2 * DIRS)
    x_load.wait()

    def rows_of(piece, offset, count):
        return pl.ds(pl.multiple_of(piece * quarter + offset, eighth), count)

    def message(step, c, d, z_first):
        s = sign[d]
        near, behind = (pos_y + s + RING) % RING, (pos_y - s + RING) % RING
        if step == 0:
            src, dst = part.at[rows_of((pos_y + 2) % RING, d * eighth, eighth), cols_of(c)], landed.at[c, d, pl.ds(quarter, eighth), :]
        elif step == 1:
            src, dst = part.at[rows_of(near, 0, quarter), cols_of(c)], landed.at[c, d, pl.ds(0, quarter), :]
        elif z_first:
            back = (pos_z - s + RING) % RING
            if step == 2:
                src = dst = xbuf.at[pos_z, rows_of(pos_y, 0, quarter), cols_of(c)]
            elif step == 3:
                src = dst = xbuf.at[back, rows_of(pos_y, d * eighth, eighth), cols_of(c)]
            elif step == 4:
                src = dst = xbuf.at[:, rows_of(pos_y, 0, quarter), cols_of(c)]
            else:
                src = dst = xbuf.at[:, rows_of(behind, d * eighth, eighth), cols_of(c)]
        else:
            if step == 2:
                src = dst = xbuf.at[pos_z, rows_of(pos_y, 0, quarter), cols_of(c)]
            elif step == 3:
                src = dst = xbuf.at[pos_z, rows_of(behind, d * eighth, eighth), cols_of(c)]
            elif step == 4:
                src = dst = xbuf.at[pos_z, :, cols_of(c)]
            else:
                src = dst = xbuf.at[(pos_z - s + RING) % RING, pl.ds(d * (rows // 2), rows // 2), cols_of(c)]
        along_y = step < 2 or (step < 4) != z_first
        return pltpu.make_async_remote_copy(
            src_ref=src, dst_ref=dst, send_sem=send_sem.at[c, step, d], recv_sem=recv_sem.at[c, step, d],
            device_id={'head': (y_device if along_y else z_device)(d)}, device_id_type=pl.DeviceIdType.MESH)

    def on_messages(step, c, act):
        if step < 2:
            for d in range(DIRS):
                act(message(step, c, d, False))
            return

        @pl.when(c % 4 == 3)
        def _():
            for d in range(DIRS):
                act(message(step, c, d, True))

        @pl.when(c % 4 != 3)
        def _():
            for d in range(DIRS):
                act(message(step, c, d, False))

    def store(c):
        return pltpu.make_async_copy(xbuf.at[:, :, cols_of(c)], out_ref.at[:, :, cols_of(c)], store_sem.at[c])

    def project(c):
        @pl.when(c + 1 < block_count)
        def _():
            for copy in w_loads(c + 1):
                copy.start()

        for copy in w_loads(c):
            copy.wait()
        total = None
        for j in range(RING):
            z = (pos_z + j) % RING
            down = jnp.dot(hid_ref[z], wtile[c % 2, j, :ff_local, :], preferred_element_type=jnp.float32)
            down = down + jnp.dot(att_ref[z], wtile[c % 2, j, ff_local:, :], preferred_element_type=jnp.float32)
            total = down if total is None else total + down
        part[:, cols_of(c)] = total

    def stage(number, c):
        if number == 0:
            project(c)
        else:
            on_messages(number - 1, c, lambda copy: copy.wait_recv())
        if number == 1:
            for d in range(DIRS):
                piece = rows_of((pos_y + sign[d] + RING) % RING, d * eighth, eighth)
                part[piece, cols_of(c)] = part[piece, cols_of(c)] + landed[c, d, pl.ds(quarter, eighth), :]
        if number == 2:
            own = rows_of(pos_y, 0, quarter)
            total = part[own, cols_of(c)] + landed[c, 0, pl.ds(0, quarter), :] + landed[c, 1, pl.ds(0, quarter), :]
            update = total.astype(jnp.bfloat16).astype(jnp.float32)
            xbuf[pos_z, own, cols_of(c)] = (xres[:, cols_of(c)].astype(jnp.float32) + update).astype(jnp.bfloat16)
        if number < LAST_STEPS:
            on_messages(number, c, lambda copy: copy.start())
        else:
            store(c).start()

    def tick(t, carry):
        for number in range(LAST_STEPS, -1, -1):
            c = t - SKEW * number

            @pl.when(jnp.logical_and(c >= 0, c < block_count))
            def _():
                stage(number, c)
        return carry

    lax.fori_loop(0, block_count + SKEW * LAST_STEPS, tick, 0)

    def drain(c, carry):
        for step in range(LAST_STEPS):
            on_messages(step, c, lambda copy: copy.wait_send())
        store(c).wait()
        return carry

    lax.fori_loop(0, block_count, drain, 0)


def layer_last(layer, hid_all, att_all, rest, w_down, w_o, all_down, all_out):
    rows, d_model = hid_all.shape[1], rest.shape[1]
    tok_count = RING * rows
    depth = hid_all.shape[2] + att_all.shape[2]
    any_spec = pl.BlockSpec(memory_space=pl.ANY)
    vmem_spec = pl.BlockSpec(memory_space=pltpu.VMEM)
    blocks = d_model // LAST_COLS
    out = pl.pallas_call(
        functools.partial(last_kernel, layer),
        out_shape=jax.ShapeDtypeStruct((RING, rows, d_model), jnp.bfloat16),
        in_specs=[vmem_spec, vmem_spec] + [any_spec] * 5,
        out_specs=any_spec,
        scratch_shapes=[
            pltpu.VMEM((rows, d_model), jnp.float32),
            pltpu.VMEM((rows // RING, d_model), jnp.bfloat16),
            pltpu.VMEM((RING, rows, d_model), jnp.bfloat16),
            pltpu.VMEM((2, RING, depth, LAST_COLS), jnp.bfloat16),
            pltpu.VMEM((blocks, DIRS, 3 * rows // (2 * RING), LAST_COLS), jnp.float32),
            pltpu.SemaphoreType.DMA((2, RING, 2)),
            pltpu.SemaphoreType.DMA,
            pltpu.SemaphoreType.DMA((blocks,)),
            pltpu.SemaphoreType.DMA((blocks, LAST_STEPS, DIRS)),
            pltpu.SemaphoreType.DMA((blocks, LAST_STEPS, DIRS)),
        ],
        compiler_params=pltpu.CompilerParams(collective_id=layer, has_side_effects=True, vmem_limit_bytes=63 * 1024 * 1024),
        cost_estimate=pl.CostEstimate(flops=2 * tok_count * depth * d_model, bytes_accessed=4 * depth * d_model * 2, transcendentals=0),
        name='last',
    )(hid_all, att_all, rest, w_down, w_o, all_down, all_out)
    return out.reshape(tok_count, d_model)


EMIT_PARTS = 8


def emit_kernel(x_ref, k_first, k_second, v_first, v_second, x_out, k_out, v_out, xbuf, rows, load_sem, store_sem):
    size = x_ref.shape[0] // EMIT_PARTS
    loads, stores = [], []
    for n in range(EMIT_PARTS):
        part = pl.ds(n * size, size)
        loads.append(pltpu.make_async_copy(x_ref.at[part, :], xbuf.at[part, :], load_sem.at[n]))
        stores.append(pltpu.make_async_copy(xbuf.at[part, :], x_out.at[part, :], store_sem.at[n]))
    for n, (ref, out) in enumerate(((k_first, k_out.at[0]), (k_second, k_out.at[1]), (v_first, v_out.at[0]), (v_second, v_out.at[1]))):
        loads.append(pltpu.make_async_copy(ref, rows.at[n], load_sem.at[EMIT_PARTS + n]))
        stores.append(pltpu.make_async_copy(rows.at[n], out, store_sem.at[EMIT_PARTS + n]))
    for copy in loads:
        copy.start()
    for load, store in zip(loads, stores):
        load.wait()
        store.start()
    for copy in stores:
        copy.wait()


def emit(x_out, k_first, k_second, v_first, v_second):
    any_spec = pl.BlockSpec(memory_space=pl.ANY)
    cache = jax.ShapeDtypeStruct((2,) + k_first.shape, jnp.bfloat16)
    return pl.pallas_call(
        emit_kernel,
        out_shape=[jax.ShapeDtypeStruct(x_out.shape, jnp.bfloat16), cache, cache],
        in_specs=[any_spec] * 5,
        out_specs=[any_spec] * 3,
        scratch_shapes=[
            pltpu.VMEM(x_out.shape, jnp.bfloat16),
            pltpu.VMEM((4,) + k_first.shape, jnp.bfloat16),
            pltpu.SemaphoreType.DMA((EMIT_PARTS + 4,)),
            pltpu.SemaphoreType.DMA((EMIT_PARTS + 4,)),
        ],
        compiler_params=pltpu.CompilerParams(vmem_limit_bytes=63 * 1024 * 1024),
        name='emit',
    )(x_out, k_first, k_second, v_first, v_second)


def solution(mesh):
    row_spec = P(('batch', 'seq'), None)
    pos_spec = P(('batch', 'seq'))
    head_spec = P(None, None, 'head', None)
    out_proj_spec = P(None, 'head', None, None)
    col_spec = P(None, None, 'head')
    down_spec = P(None, 'head', None)
    cache_spec = P(None, ('batch', 'seq'), 'head', None)

    def local_forward(x_loc, pos_loc, w_q, w_k, w_v, w_o, w_gate, w_up, w_down, norm_gain):
        tok_count, d_model = x_loc.shape
        layer_count = w_q.shape[0]
        head_dim = w_q.shape[3]
        flat_q, flat_k, flat_v = (w.reshape(layer_count, d_model, head_dim) for w in (w_q, w_k, w_v))
        cos_t, sin_t = rope_tables(pos_loc, head_dim)
        hid_all, att_all, k_first, v_first, k_second, v_second, all_down, all_out, rest = front(x_loc, cos_t, sin_t, norm_gain, flat_q, flat_k, flat_v, w_gate, w_up, w_down, w_o)
        x_out = layer_last(1, hid_all, att_all, rest, w_down, w_o, all_down, all_out)
        x_out, k_all, v_all = emit(x_out, k_first, k_second, v_first, v_second)
        cache_shape = (layer_count, tok_count, 1, head_dim)
        return x_out, k_all.reshape(cache_shape), v_all.reshape(cache_shape)

    return jax.shard_map(local_forward, mesh=mesh, in_specs=(row_spec, pos_spec, head_spec, head_spec, head_spec, out_proj_spec, col_spec, col_spec, down_spec, P(None, None)), out_specs=(row_spec, cache_spec, cache_spec), check_vma=False)
```

```python
import functools
import math
import jax
import jax.numpy as jnp
from jax import lax
from jax.experimental import pallas as pl
from jax.experimental.pallas import tpu as pltpu
from jax.sharding import PartitionSpec as P

ROPE_BASE = 500000.0
EPS = 1e-5


def rope_tables(positions, head_dim):
    half_dim = head_dim // 2
    inv_freq = ROPE_BASE ** (-(jnp.arange(half_dim, dtype=jnp.float32) * 2.0 / head_dim))
    angles = positions.astype(jnp.float32)[..., None] * inv_freq
    return jnp.cos(angles), jnp.sin(angles)


CHIPS = 4
RING = 4
HALVES = 2
DIRS = 2
KV_CHUNKS = 4
W_TILE = 256
NORM_ROWS = 64
CHUNKS = 8
STEPS = 8
PART_SLOTS = 4
RECV_SLOTS = 5
DOWN_TILE = 512
START_GAP = 3
STAGE_GAP = 2
BLOCK_TICK = 19
BLOCK_GAP = 6
LAST_TICK = 43
NEAR_TICKS = ((9, 1), (15, 3))
FAR_TICKS = ((24, 1), (26, 3))
SERVE_TICKS = (27, 31, 35, 42)
GIVE_TICK = 37


def front_kernel(x_ref, cos_ref, sin_ref, gain_ref, wq_ref, wk_ref, wv_ref, wg_ref, wu_ref, wd_ref, wo_ref,
                 hid_all_ref, att_all_ref, k1_ref, v1_ref, k2_ref, v2_ref, gd_ref, go_ref, rest_ref,
                 xbuf, part, recv_a, recv_b, hid, att, wdo, wtile, kv, qbuf, acc, row_max, row_sum, xs, xres,
                 x_sem, res_sem, w_sem, down_sem, cache_sem, rest_sem, own_send, pass_send, ici_recv, core_recv, part_send, part_recv,
                 round_send, round_recv, side_send, side_recv, give_send, give_recv, keep_sem, relay_buf, relay_send, relay_recv, ring_send, ring_recv, ready_sem):
    tok_count, d_model = xbuf.shape
    head_dim = qbuf.shape[1]
    half_dim = head_dim // 2
    ff_local = hid.shape[1]
    rows_per = tok_count // KV_CHUNKS
    half_rows = tok_count // 2
    lanes = row_max.shape[2]
    chunk_rows = tok_count // CHUNKS
    quarter, eighth = chunk_rows // RING, chunk_rows // (2 * RING)
    half_cols = d_model // HALVES
    piece_cols = half_cols // RING
    bf16, f32 = jnp.bfloat16, jnp.float32
    sign = (1, -1)
    mesh_id = pl.DeviceIdType.MESH

    my_head = lax.axis_index('head')
    pos_z, pos_y = my_head // RING, my_head % RING
    my_seq = lax.axis_index('seq')
    chip, core = my_seq // 2, my_seq % 2
    other = chip * 2 + 1 - core

    def wrap(n):
        return (n + RING) % RING

    def y_peer(d):
        return pos_z * RING + wrap(pos_y + sign[d])

    def z_device(z):
        return wrap(z) * RING + pos_y

    def z_peer(d):
        return z_device(pos_z + sign[d])

    def x_device(n):
        return wrap(chip + n) * 2 + core

    right, left = x_device(1), x_device(-1)

    def span(start, size, unit=None):
        return pl.ds(pl.multiple_of(start, unit or size), size)

    def remote(src, dst, send, recv, **to):
        return pltpu.make_async_remote_copy(src_ref=src, dst_ref=dst, send_sem=send, recv_sem=recv, device_id=to, device_id_type=mesh_id)

    def x_load(i):
        return pltpu.make_async_copy(x_ref.at[span(i * rows_per, rows_per), :], xs.at[i % 2], x_sem.at[i % 2])

    def weights(layer, piece):
        slot = piece % 2
        if isinstance(piece, int) and piece < 2:
            refs = ((wk_ref, wv_ref), (wq_ref,))[piece]
            return [pltpu.make_async_copy(ref.at[layer], wtile.at[slot, n], w_sem.at[slot, n]) for n, ref in enumerate(refs)]
        cols = span((piece - 2) * W_TILE, W_TILE)
        return [pltpu.make_async_copy(ref.at[layer, :, cols], wtile.at[slot, n], w_sem.at[slot, n]) for n, ref in enumerate((wg_ref, wu_ref))]

    def start(copies):
        for copy in copies:
            copy.start()

    def wait(copies):
        for copy in copies:
            copy.wait()

    down_tiles = d_model // DOWN_TILE

    def down_load(i):
        cols = span(i * DOWN_TILE, DOWN_TILE)
        return [pltpu.make_async_copy(wd_ref.at[0, :, cols], wdo.at[i % 2, pl.ds(0, ff_local), :], down_sem.at[i % 2, 0]),
                pltpu.make_async_copy(wo_ref.at[0, 0, :, cols], wdo.at[i % 2, pl.ds(ff_local, head_dim), :], down_sem.at[i % 2, 1])]

    def kv_copy(origin_chip, origin_core, i, to, send, recv):
        rows = kv.at[span((origin_chip * 2 + origin_core) * tok_count + i * rows_per, rows_per), :]
        return remote(rows, rows, send, recv, seq=to)

    def kv_routes(layer, i):
        late = i >= KV_CHUNKS // 2
        early = jnp.logical_not(late) if not isinstance(i, int) else not late

        def to(send, recv, origin_chip, origin_core, device):
            return kv_copy(origin_chip, origin_core, i, device, send, recv)
        own, passed, ici, side = own_send.at[layer], pass_send.at[layer], ici_recv.at[layer], core_recv.at[layer]
        return {
            'right': (chip < CHIPS - 1, lambda: to(own.at[0, i], ici.at[0, i], chip, core, right)),
            'wrap': (chip == 0, lambda: to(own.at[1, i], ici.at[2, i], chip, core, left)),
            'relay': (jnp.logical_and(late, chip == 1), lambda: to(own.at[3, i], ici.at[3, i], chip, core, left)),
            'other': (core == 0, lambda: to(own.at[2, i], side.at[0, i], chip, core, other)),
            'on_right': (jnp.logical_and(early, jnp.logical_and(chip >= 1, chip < CHIPS - 1)), lambda: to(passed.at[0, i], ici.at[1, i], chip - 1, core, right)),
            'from_relay': (jnp.logical_and(late, chip == 0), lambda: to(passed.at[0, i], ici.at[1, i], 1, core, left)),
            'on_left': (jnp.logical_and(late, chip == CHIPS - 1), lambda: to(passed.at[0, i], ici.at[1, i], 0, core, left)),
            'side1': (chip >= 1, lambda: to(passed.at[1, i], side.at[1, i], chip - 1, core, other)),
            'side2': (chip >= 2, lambda: to(passed.at[2, i], side.at[2, i], chip - 2, core, other)),
            'side3': (chip >= 3, lambda: to(passed.at[3, i], side.at[3, i], chip - 3, core, other)),
        }

    def start_route(layer, i, name):
        condition, copy = kv_routes(layer, i)[name]

        @pl.when(condition)
        def _():
            copy().start()

    def send_kv(layer, i):
        for name in ('right', 'wrap', 'relay', 'other'):
            start_route(layer, i, name)

    def kv_sent(layer):
        for i in range(KV_CHUNKS):
            for condition, copy in kv_routes(layer, i).values():
                @pl.when(condition)
                def _():
                    copy().wait_send()

    def serve(layer, back, i):
        @pl.when(chip >= back)
        def _():
            kv_copy(chip - back, core, i, other, pass_send.at[layer, back, i], ici_recv.at[layer, back - 1, i]).wait_recv()
        start_route(layer, i, 'side%d' % back)
        if back == 1:
            start_route(layer, i, 'on_right')
        if back == 3:
            start_route(layer, i, 'on_left')

    def relay(layer, i):
        condition, copy = kv_routes(layer, i)['from_relay']

        @pl.when(condition)
        def _():
            kv_copy(1, core, i, left, pass_send.at[layer, 0, i], ici_recv.at[layer, 3, i]).wait_recv()
            copy().start()

    def serve_all(layer, i):
        serve(layer, 1, i)
        serve(layer, 3, i)
        relay(layer, i)

    def taken(layer, back, chunks):
        for i in chunks:
            kv_copy(chip - back, 1 - core, i, other, pass_send.at[layer, 0, i], core_recv.at[layer, back, i]).wait_recv()

    def z_parts(step, d):
        copies = []
        for n, (own_ref, all_ref) in enumerate(((wd_ref, gd_ref), (wo_ref, go_ref))):
            size = all_ref.shape[1] // (2 * CHIPS)
            if step == 0:
                rows = span(my_seq * size, size)
                src = own_ref.at[1, rows, :] if n == 0 else own_ref.at[1, 0, rows, :]
                dst = all_ref.at[pos_z, rows, :]
            else:
                rows = span(my_seq * size + d * (size // 2), size // 2)
                src = dst = all_ref.at[wrap(pos_z - sign[d]), rows, :]
            copies.append(remote(src, dst, part_send.at[step, d, n], part_recv.at[step, d, n], head=z_peer(d)))
        return copies

    def part_copies(j, part_chip, part_core, half, send, recv, to):
        copies = []
        for n, ref in enumerate((gd_ref, go_ref)):
            size = ref.shape[1] // (2 * CHIPS)
            first = (part_chip * 2 + part_core) * size
            rows = span(first, size) if half is None else span(first + half * (size // 2), size // 2)
            place = ref.at[wrap(pos_z + j), rows, :]
            copies.append(remote(place, place, send.at[n], recv.at[n], seq=to))
        return copies

    def own_part(j, d):
        return part_copies(j, chip, core, None, round_send.at[0, j - 1, d], round_recv.at[0, j - 1, d], x_device(sign[d]))

    def far_part(j, d):
        return part_copies(j, wrap(chip - sign[d]), core, d, round_send.at[1, j - 1, d], round_recv.at[1, j - 1, d], x_device(sign[d]))

    def side_part(j, n, side):
        return part_copies(j, wrap(chip + n), side, None, side_send.at[j - 1, n], side_recv.at[j - 1, n], other)

    def round_start(j):
        for d in range(DIRS):
            start(own_part(j, d))
        start(side_part(j, 0, core))

    def near_parts(j):
        for d in range(DIRS):
            for copy in own_part(j, d):
                copy.wait_recv()
            start(far_part(j, d) + side_part(j, 3 if d == 0 else 1, core))

    def far_parts(j):
        for d in range(DIRS):
            for copy in far_part(j, d):
                copy.wait_recv()
        start(side_part(j, 2, core))

    def give_hidden(z, i, source):
        cols = span(i * W_TILE, W_TILE)
        return remote(hid.at[span(z * rows_per, rows_per), cols], hid_all_ref.at[source, :, cols], give_send.at[z, i], give_recv.at[source, i], head=z_device(z))

    def keep_hidden(i):
        cols = span(i * W_TILE, W_TILE)
        return pltpu.make_async_copy(hid.at[span(pos_z * rows_per, rows_per), cols], hid_all_ref.at[pos_z, :, cols], keep_sem.at[i])

    def via_neighbor(z, i):
        step = jnp.where(i < KV_CHUNKS // 2, 1, -1)
        return remote(hid.at[span(z * rows_per, rows_per), span(i * W_TILE, W_TILE)], relay_buf.at[i], give_send.at[z, i], relay_recv.at[i], head=z_device(pos_z + step))

    def relay_hidden(i):
        step = 1 if i < KV_CHUNKS // 2 else -1
        source = wrap(pos_z - step)
        return remote(relay_buf.at[i], hid_all_ref.at[source, :, span(i * W_TILE, W_TILE)], relay_send.at[i], give_recv.at[source, i], head=z_device(pos_z + step))

    def send_hidden(z, i):
        away = wrap(z - pos_z)

        @pl.when(away == 2)
        def _():
            via_neighbor(z, i).start()

        @pl.when(away % 2 == 1)
        def _():
            give_hidden(z, i, pos_z).start()

        @pl.when(away == 0)
        def _():
            keep_hidden(i).start()

    def give_rows(z, source):
        return remote(att.at[span(z * rows_per, rows_per), :], att_all_ref.at[source], give_send.at[z, KV_CHUNKS], give_recv.at[source, KV_CHUNKS], head=z_device(z))

    def keep_rows():
        return pltpu.make_async_copy(att.at[span(pos_z * rows_per, rows_per), :], att_all_ref.at[pos_z], keep_sem.at[KV_CHUNKS])

    def norm_rows(x_few, layer):
        x_f32 = x_few.astype(f32)
        inv_rms = lax.rsqrt(jnp.mean(x_f32 * x_f32, axis=-1, keepdims=True) + EPS)
        return (x_f32 * inv_rms * gain_ref[pl.ds(layer, 1), :].astype(f32)).astype(bf16)

    def rope(values, rows):
        cos_t, sin_t = cos_ref[rows, :], sin_ref[rows, :]
        wide = values.astype(bf16).astype(f32)
        first, second = wide[:, :half_dim], wide[:, half_dim:]
        return jnp.concatenate([first * cos_t - second * sin_t, second * cos_t + first * sin_t], axis=1).astype(bf16)

    def dot(a, b):
        return jnp.dot(a, b, preferred_element_type=f32)

    scale = 1.0 / math.sqrt(head_dim)

    def keys_values(normed, i):
        rows = span(i * rows_per, rows_per)
        own = span(my_seq * tok_count + i * rows_per, rows_per)
        kv[own, :head_dim] = rope(dot(normed, wtile[0, 0]), rows)
        kv[own, head_dim:] = dot(normed, wtile[0, 1]).astype(bf16)

    def queries(normed, i):
        rows = span(i * rows_per, rows_per)
        qbuf[rows, :] = (rope(dot(normed, wtile[1, 0]), rows).astype(f32) * scale).astype(bf16)

    def gated(normed, i, tile):
        gate = dot(normed, wtile[tile % 2, 0])
        up = dot(normed, wtile[tile % 2, 1])
        hid[span(i * rows_per, rows_per), span(tile * W_TILE, W_TILE)] = (gate * jax.nn.sigmoid(gate) * up).astype(bf16)

    def attend(key_start, q_half, side, masked, first):
        rows = pl.ds(q_half * half_rows, half_rows)
        some = span(key_start, half_rows)
        logits = lax.dot_general(qbuf[rows, :], kv[some, :head_dim], (((1,), (1,)), ((), ())), preferred_element_type=f32)
        if masked:
            seen = lax.broadcasted_iota(jnp.int32, logits.shape, 0) >= lax.broadcasted_iota(jnp.int32, logits.shape, 1)
            logits = jnp.where(seen, logits, -jnp.inf)
        block_max = jnp.max(logits, axis=-1, keepdims=True)
        if first:
            new_max = jnp.broadcast_to(block_max, (half_rows, lanes))
        else:
            new_max = jnp.maximum(row_max[side, rows, :], block_max)
        prob = jnp.exp(logits - jnp.concatenate([new_max] * (half_rows // lanes), axis=1))
        block_sum = jnp.sum(prob, axis=-1, keepdims=True)
        block_out = dot(prob.astype(bf16), kv[some, head_dim:])
        if first:
            row_sum[side, rows, :] = jnp.broadcast_to(block_sum, (half_rows, lanes))
            acc[side, rows, :] = block_out
        else:
            rescale = jnp.exp(row_max[side, rows, :] - new_max)
            row_sum[side, rows, :] = row_sum[side, rows, :] * rescale + block_sum
            acc[side, rows, :] = acc[side, rows, :] * jnp.concatenate([rescale] * (head_dim // lanes), axis=1) + block_out
        row_max[side, rows, :] = new_max

    def attend_own():
        own_start = my_seq * tok_count
        attend(own_start, 0, 0, True, True)
        attend(own_start, 1, 0, False, True)
        attend(own_start + half_rows, 1, 1, True, True)
        top_rows = pl.ds(0, half_rows)
        row_max[1, top_rows, :] = jnp.full((half_rows, lanes), -jnp.inf, f32)
        row_sum[1, top_rows, :] = jnp.zeros((half_rows, lanes), f32)
        acc[1, top_rows, :] = jnp.zeros((half_rows, head_dim), f32)

    def past_start(n):
        later = n - core
        back = jnp.where(later < 2, 1, jnp.where(chip == CHIPS - 1, jnp.where(later < 4, 3, 2), 2))
        block = (chip - back) * 2 + jnp.where(later % 2 == 0, core, 1 - core)
        return jnp.where(jnp.logical_and(core == 1, n == 0), chip * 2, block) * tok_count

    def attend_past(layer, chunks, visits):
        def past(n, carry):
            @pl.when(jnp.logical_and(core == 1, n == 0))
            def _():
                taken(layer, 0, chunks)

            for back in (1, 3, 2):
                place = 0 if back == 1 else 2 if back == 3 else jnp.where(chip == CHIPS - 1, 4, 2)
                if back == 2:
                    @pl.when(jnp.logical_and(chip >= back, n == core + place))
                    def _():
                        for i in chunks:
                            serve(layer, 2, i)

                @pl.when(jnp.logical_and(chip >= back, n == core + place + 1))
                def _():
                    taken(layer, back, chunks)
            for q_half, side in visits:
                attend(past_start(n) + side * half_rows, q_half, side, False, False)
            return carry

        lax.fori_loop(0, my_seq, past, 0)

    def finish(i, spread):
        rows = pl.ds(i * rows_per, rows_per)
        top = jnp.maximum(row_max[0, rows, :], row_max[1, rows, :])
        shares = [jnp.exp(row_max[side, rows, :] - top) for side in range(2)]
        total = shares[0] * row_sum[0, rows, :] + shares[1] * row_sum[1, rows, :]
        wide = [jnp.concatenate([w] * (head_dim // lanes), axis=1) for w in shares + [total]]
        att[rows, :] = ((acc[0, rows, :] * wide[0] + acc[1, rows, :] * wide[1]) / wide[2]).astype(bf16)
        if spread:
            @pl.when(i == pos_z)
            def _():
                keep_rows().start()

            @pl.when(i != pos_z)
            def _():
                give_rows(i, pos_z).start()

    first_pos, second_pos = (pos_y, pos_z), (pos_z, pos_y)
    first_peer, second_peer = (y_peer, z_peer), (z_peer, y_peer)

    def part_rows(chunk, piece, offset, count):
        return span((chunk % PART_SLOTS) * chunk_rows + piece * quarter + offset, count, eighth)

    def x_rows(chunk, piece, offset, count):
        return span(chunk * chunk_rows + piece * quarter + offset, count, eighth)

    def cols_of(h, piece):
        return span(h * half_cols + piece * piece_cols, piece_cols)

    def half_of(h):
        return pl.ds(h * half_cols, half_cols)

    def message(step, chunk, h, d):
        p1, p2, s = first_pos[h], second_pos[h], sign[d]
        slot = chunk % RECV_SLOTS
        if step == 0:
            src, dst = part.at[part_rows(chunk, wrap(p1 + 2), d * eighth, eighth), half_of(h)], recv_a.at[slot, h, d, pl.ds(quarter, eighth), :]
        elif step == 1:
            src, dst = part.at[part_rows(chunk, wrap(p1 + s), 0, quarter), half_of(h)], recv_a.at[slot, h, d, pl.ds(0, quarter), :]
        elif step == 2:
            src, dst = part.at[part_rows(chunk, p1, d * eighth, eighth), cols_of(h, wrap(p2 + 2))], recv_b.at[slot, h, d, pl.ds(quarter, eighth), :]
        elif step == 3:
            src, dst = part.at[part_rows(chunk, p1, 0, quarter), cols_of(h, wrap(p2 + s))], recv_b.at[slot, h, d, pl.ds(0, quarter), :]
        elif step == 4:
            src = dst = xbuf.at[x_rows(chunk, p1, 0, quarter), cols_of(h, p2)]
        elif step == 5:
            src = dst = xbuf.at[x_rows(chunk, p1, d * eighth, eighth), cols_of(h, wrap(p2 - s))]
        elif step == 6:
            src = dst = xbuf.at[x_rows(chunk, p1, 0, quarter), half_of(h)]
        else:
            src = dst = xbuf.at[x_rows(chunk, wrap(p1 - s), d * eighth, eighth), half_of(h)]
        peer = (first_peer if step in (0, 1, 6, 7) else second_peer)[h](d)
        return remote(src, dst, ring_send.at[chunk, step, h * DIRS + d], ring_recv.at[chunk, step, h * DIRS + d], head=peer)

    def each_message(chunk, steps, act):
        for step in steps:
            for h in range(HALVES):
                for d in range(DIRS):
                    act(message(step, chunk, h, d))

    def residual_load(chunk, h):
        return pltpu.make_async_copy(x_ref.at[x_rows(chunk, first_pos[h], 0, quarter), cols_of(h, second_pos[h])], xres.at[chunk, h], res_sem.at[chunk, h])

    def project(chunk):
        rows = span(chunk * chunk_rows, chunk_rows)
        slot_rows = span((chunk % PART_SLOTS) * chunk_rows, chunk_rows)

        def one_tile(i, carry):
            @pl.when(jnp.logical_or(chunk < CHUNKS - 1, i < down_tiles - 1))
            def _():
                start(down_load((i + 1) % down_tiles))

            wait(down_load(i))
            total = dot(hid[rows, :], wdo[i % 2, :ff_local, :])
            part[slot_rows, span(i * DOWN_TILE, DOWN_TILE)] = total + dot(att[rows, :], wdo[i % 2, ff_local:, :])
            return carry

        lax.fori_loop(0, down_tiles, one_tile, 0)

    def stage(number, chunk):
        slot = chunk % RECV_SLOTS
        if number == 0:
            @pl.when(chunk >= PART_SLOTS)
            def _():
                each_message(chunk - PART_SLOTS, range(4), lambda copy: copy.wait_send())
            project(chunk)
        for h in range(HALVES):
            p1, p2 = first_pos[h], second_pos[h]
            if number:
                for d in range(DIRS):
                    message(number - 1, chunk, h, d).wait_recv()
            if number in (1, 3):
                for d in range(DIRS):
                    if number == 1:
                        rows, cols, arrived = part_rows(chunk, wrap(p1 + sign[d]), d * eighth, eighth), half_of(h), recv_a
                    else:
                        rows, cols, arrived = part_rows(chunk, p1, d * eighth, eighth), cols_of(h, wrap(p2 + sign[d])), recv_b
                    part[rows, cols] = part[rows, cols] + arrived[slot, h, d, pl.ds(quarter, eighth), :]
            if number == 2:
                rows = part_rows(chunk, p1, 0, quarter)
                part[rows, half_of(h)] = part[rows, half_of(h)] + recv_a[slot, h, 0, pl.ds(0, quarter), :] + recv_a[slot, h, 1, pl.ds(0, quarter), :]
            if number == 4:
                residual_load(chunk, h).wait()
                rows, cols = part_rows(chunk, p1, 0, quarter), cols_of(h, p2)
                total = part[rows, cols] + recv_b[slot, h, 0, pl.ds(0, quarter), :] + recv_b[slot, h, 1, pl.ds(0, quarter), :]
                update = total.astype(bf16).astype(f32)
                xbuf[x_rows(chunk, p1, 0, quarter), cols] = (xres[chunk, h].astype(f32) + update).astype(bf16)
            if number < STEPS:
                for d in range(DIRS):
                    message(number, chunk, h, d).start()

    x_load(0).start()
    start(weights(0, 0))
    x_load(1).start()
    start(weights(0, 1))
    barrier = pltpu.get_barrier_semaphore()
    for peer in (left, right, other):
        pl.semaphore_signal(barrier, inc=1, device_id={'seq': peer}, device_id_type=mesh_id)
    for peer in [z_device(pos_z + j) for j in range(1, RING)] + [y_peer(d) for d in range(DIRS)]:
        pl.semaphore_signal(barrier, inc=1, device_id={'head': peer}, device_id_type=mesh_id)
    pl.semaphore_wait(barrier, 8)
    for d in range(DIRS):
        start(z_parts(0, d))

    def prepare(i, carry):
        x_load(i).wait()

        def few(n, inner):
            xbuf[span(i * rows_per + n * NORM_ROWS, NORM_ROWS), :] = norm_rows(xs[i % 2, span(n * NORM_ROWS, NORM_ROWS), :], 0)
            return inner

        lax.fori_loop(0, rows_per // NORM_ROWS, few, 0)

        @pl.when(i + 2 < KV_CHUNKS)
        def _():
            x_load(i + 2).start()

        @pl.when(i == 0)
        def _():
            wait(weights(0, 0))

        keys_values(xbuf[span(i * rows_per, rows_per), :], i)
        send_kv(0, i)
        return carry

    lax.fori_loop(0, KV_CHUNKS, prepare, 0)
    start(weights(0, 2))
    own_rows = span(my_seq * tok_count, tok_count)

    def cache_stores(layer):
        k_ref, v_ref = ((k1_ref, v1_ref), (k2_ref, v2_ref))[layer]
        return [pltpu.make_async_copy(kv.at[own_rows, pl.ds(0, head_dim)], k_ref, cache_sem.at[layer, 0]),
                pltpu.make_async_copy(kv.at[own_rows, pl.ds(head_dim, head_dim)], v_ref, cache_sem.at[layer, 1])]

    start(cache_stores(0))
    wait(weights(0, 1))

    def query(i, carry):
        queries(xbuf[span(i * rows_per, rows_per), :], i)
        return carry

    lax.fori_loop(0, KV_CHUNKS, query, 0)
    start(weights(0, 3))
    start(down_load(0))

    def residuals(n, carry):
        for h in range(HALVES):
            residual_load(n, h).start()
        return carry

    lax.fori_loop(0, CHUNKS, residuals, 0)

    def gate_tile(tile, carry):
        wait(weights(0, tile + 2))

        def rows_step(i, inner):
            gated(xbuf[span(i * rows_per, rows_per), :], i, tile)
            return inner

        lax.fori_loop(0, KV_CHUNKS, rows_step, 0)

        @pl.when(tile < 2)
        def _():
            start(weights(0, tile + 4))

        @pl.when(tile == 2)
        def _():
            start(weights(1, 0))
            for d in range(DIRS):
                for copy in z_parts(0, d):
                    copy.wait_recv()
                start(z_parts(1, d))

        @pl.when(tile == 3)
        def _():
            start(weights(1, 1))
        serve_all(0, tile)
        return carry

    lax.fori_loop(0, ff_local // W_TILE, gate_tile, 0)
    attend_own()
    attend_past(0, range(KV_CHUNKS), ((0, 0), (0, 1)))
    finish(0, False)
    finish(1, False)
    round_start(1)
    round_start(3)

    def block_work(j, phase):
        @pl.when(phase == 0)
        def _():
            @pl.when(j == 0)
            def _():
                for n in range(3):
                    pl.semaphore_wait(ready_sem.at[n], 1)

            def few(n, inner):
                xs[0, span(n * NORM_ROWS, NORM_ROWS), :] = norm_rows(xbuf[span(j * rows_per + n * NORM_ROWS, NORM_ROWS), :], 1)
                return inner

            lax.fori_loop(0, rows_per // NORM_ROWS, few, 0)
            wait(weights(1, 0))
            keys_values(xs[0], j)
            send_kv(1, j)
            start(weights(1, 2))

        @pl.when(phase == 1)
        def _():
            wait(weights(1, 1))
            queries(xs[0], j)
            start(weights(1, 3))

        @pl.when(jnp.logical_and(phase >= 1, phase <= 4))
        def _():
            tile = phase - 1
            wait(weights(1, tile + 2))
            gated(xs[0], j, tile)

            @pl.when(tile < 2)
            def _():
                start(weights(1, tile + 4))

            @pl.when(jnp.logical_and(tile == 2, j < KV_CHUNKS - 1))
            def _():
                start(weights(1, 0))

            @pl.when(jnp.logical_and(tile == 3, j < KV_CHUNKS - 1))
            def _():
                start(weights(1, 1))

            @pl.when(j == KV_CHUNKS - 1)
            def _():
                send_hidden(j, tile)

    def tick(t, carry):
        for number in range(STEPS, -1, -1):
            place = t - STAGE_GAP * number
            chunk = place // START_GAP

            @pl.when(jnp.logical_and(place >= 0, jnp.logical_and(place % START_GAP == 0, chunk < CHUNKS)))
            def _():
                stage(number, chunk)

        @pl.when(jnp.logical_and(t >= 1, jnp.logical_and(t < 8, t <= my_seq)))
        def _():
            for side in range(2):
                attend(past_start(t - 1) + side * half_rows, 1, side, False, False)

        @pl.when(t == 2)
        def _():
            for d in range(DIRS):
                for copy in z_parts(1, d):
                    copy.wait_recv()
            round_start(2)

        @pl.when(t == 8)
        def _():
            finish(2, False)
            finish(3, False)
            kv_sent(0)
            wait(cache_stores(0))
            for n, peer in enumerate((left, right, other)):
                pl.semaphore_signal(ready_sem.at[n], inc=1, device_id={'seq': peer}, device_id_type=mesh_id)

        for when, j in NEAR_TICKS:
            @pl.when(t == when)
            def _():
                near_parts(j)

        for when, j in FAR_TICKS:
            @pl.when(t == when)
            def _():
                far_parts(j)

        @pl.when(t == GIVE_TICK)
        def _():
            for i in range(KV_CHUNKS):
                for z in range(KV_CHUNKS - 1):
                    send_hidden(z, i)

        late = t - BLOCK_TICK

        @pl.when(late >= 0)
        def _():
            block_work(late // BLOCK_GAP, late % BLOCK_GAP)

        for i, when in enumerate(SERVE_TICKS):
            @pl.when(t == when)
            def _():
                serve_all(1, i)
        return carry

    lax.fori_loop(0, LAST_TICK, tick, 0)

    start(cache_stores(1))
    rest_store = pltpu.make_async_copy(xbuf.at[span(pos_z * rows_per + pos_y * (rows_per // RING), rows_per // RING), :], rest_ref, rest_sem)
    rest_store.start()
    near_parts(2)
    attend_own()
    attend_past(1, (0, 1), ((0, 0), (1, 0)))
    for i in range(KV_CHUNKS):
        via_neighbor(0, i).wait_recv()
        relay_hidden(i).start()
    attend_past(1, (2, 3), ((0, 1), (1, 1)))
    for i in range(KV_CHUNKS):
        finish(i, True)
    far_parts(2)

    wait(cache_stores(1))
    rest_store.wait()
    for i in range(KV_CHUNKS):
        keep_hidden(i).wait()
        relay_hidden(i).wait_send()
    keep_rows().wait()
    kv_sent(1)
    for d in range(DIRS):
        for step in range(2):
            for copy in z_parts(step, d):
                copy.wait_send()
    for j in range(1, RING):
        for d in range(DIRS):
            for copy in own_part(j, d) + far_part(j, d):
                copy.wait_send()
        for n in range(CHIPS):
            for copy in side_part(j, n, 1 - core):
                copy.wait_recv()
            for copy in side_part(j, n, core):
                copy.wait_send()
        z = wrap(pos_z + j)
        for i in range(KV_CHUNKS):
            give_hidden(z, i, z).wait_recv()
            give_hidden(z, i, pos_z).wait_send()
        give_rows(z, z).wait_recv()
        give_rows(z, pos_z).wait_send()

    def drain(chunk, carry):
        @pl.when(chunk >= CHUNKS - PART_SLOTS)
        def _():
            each_message(chunk, range(4), lambda copy: copy.wait_send())
        each_message(chunk, range(4, STEPS), lambda copy: copy.wait_send())
        return carry

    lax.fori_loop(0, CHUNKS, drain, 0)


def front(x_loc, cos_t, sin_t, norm_gain, w_q, w_k, w_v, w_gate, w_up, w_down, w_o):
    tok_count, d_model = x_loc.shape
    head_dim = w_q.shape[2]
    ff_local = w_gate.shape[2]
    rows_per = tok_count // KV_CHUNKS
    chunk_rows = tok_count // CHUNKS
    landed = 3 * chunk_rows // (2 * RING)
    half_cols = d_model // HALVES
    any_spec = pl.BlockSpec(memory_space=pl.ANY)
    vmem_spec = pl.BlockSpec(memory_space=pltpu.VMEM)
    bf16, f32 = jnp.bfloat16, jnp.float32
    dma = pltpu.SemaphoreType.DMA
    shape = jax.ShapeDtypeStruct
    return pl.pallas_call(
        front_kernel,
        out_shape=[shape((RING, rows_per, ff_local), bf16), shape((RING, rows_per, head_dim), bf16)] + [shape((tok_count, head_dim), bf16)] * 4
        + [shape((RING, ff_local, d_model), bf16), shape((RING, head_dim, d_model), bf16), shape((rows_per // RING, d_model), bf16)],
        in_specs=[any_spec, vmem_spec, vmem_spec, vmem_spec] + [any_spec] * 7,
        out_specs=[any_spec] * 9,
        scratch_shapes=[
            pltpu.VMEM((tok_count, d_model), bf16),
            pltpu.VMEM((PART_SLOTS * chunk_rows, d_model), f32),
            pltpu.VMEM((RECV_SLOTS, HALVES, DIRS, landed, half_cols), f32),
            pltpu.VMEM((RECV_SLOTS, HALVES, DIRS, landed, half_cols // RING), f32),
            pltpu.VMEM((tok_count, ff_local), bf16),
            pltpu.VMEM((tok_count, head_dim), bf16),
            pltpu.VMEM((2, ff_local + head_dim, DOWN_TILE), bf16),
            pltpu.VMEM((2, 2, d_model, W_TILE), bf16),
            pltpu.VMEM((2 * CHIPS * tok_count, 2 * head_dim), bf16),
            pltpu.VMEM((tok_count, head_dim), bf16),
            pltpu.VMEM((2, tok_count, head_dim), f32),
            pltpu.VMEM((2, tok_count, 128), f32),
            pltpu.VMEM((2, tok_count, 128), f32),
            pltpu.VMEM((2, rows_per, d_model), bf16),
            pltpu.VMEM((CHUNKS, HALVES, chunk_rows // RING, half_cols // RING), bf16),
            dma((2,)), dma((CHUNKS, HALVES)), dma((2, 2)), dma((2, 2)), dma((2, 2)), dma,
            dma((2, 4, KV_CHUNKS)), dma((2, 4, KV_CHUNKS)), dma((2, 4, KV_CHUNKS)), dma((2, 4, KV_CHUNKS)), dma((2, DIRS, 2)), dma((2, DIRS, 2)),
            dma((2, RING - 1, DIRS, 2)), dma((2, RING - 1, DIRS, 2)), dma((RING - 1, CHIPS, 2)), dma((RING - 1, CHIPS, 2)),
            dma((RING, KV_CHUNKS + 1)), dma((RING, KV_CHUNKS + 1)), dma((KV_CHUNKS + 1,)),
            pltpu.VMEM((KV_CHUNKS, rows_per, W_TILE), bf16), dma((KV_CHUNKS,)), dma((KV_CHUNKS,)),
            dma((CHUNKS, STEPS, HALVES * DIRS)), dma((CHUNKS, STEPS, HALVES * DIRS)),
            pltpu.SemaphoreType.REGULAR((3,)),
        ],
        compiler_params=pltpu.CompilerParams(collective_id=0, has_side_effects=True, vmem_limit_bytes=67043328),
        name='front',
    )(x_loc, cos_t, sin_t, norm_gain, w_q, w_k, w_v, w_gate, w_up, w_down, w_o)


SKEW = 2
LAST_STEPS = 6
LAST_COLS = 256


def last_kernel(layer, hid_ref, att_ref, rest_ref, wd_ref, wo_ref, gd_ref, go_ref, out_ref, part, xres, xbuf, wtile, landed, w_sem, x_sem, store_sem, send_sem, recv_sem):
    rows, d_model = part.shape
    block = wtile.shape[3]
    block_count = d_model // block
    ff_local = hid_ref.shape[2]
    quarter, eighth = rows // RING, rows // (2 * RING)
    my_head = lax.axis_index('head')
    pos_z, pos_y = my_head // RING, my_head % RING
    sign = (1, -1)

    def cols_of(c):
        return pl.ds(pl.multiple_of(c * block, block), block)

    def w_loads(c):
        copies = []
        for j in range(RING):
            z = (pos_z + j) % RING
            down = wd_ref.at[layer, :, cols_of(c)] if j == 0 else gd_ref.at[z, :, cols_of(c)]
            out = wo_ref.at[layer, 0, :, cols_of(c)] if j == 0 else go_ref.at[z, :, cols_of(c)]
            copies.append(pltpu.make_async_copy(down, wtile.at[c % 2, j, pl.ds(0, ff_local), :], w_sem.at[c % 2, j, 0]))
            copies.append(pltpu.make_async_copy(out, wtile.at[c % 2, j, pl.ds(ff_local, wo_ref.shape[2]), :], w_sem.at[c % 2, j, 1]))
        return copies

    for copy in w_loads(0):
        copy.start()
    x_load = pltpu.make_async_copy(rest_ref, xres, x_sem)
    x_load.start()

    def y_device(d):
        return pos_z * RING + (pos_y + sign[d] + RING) % RING

    def z_device(d):
        return (pos_z + sign[d] + RING) % RING * RING + pos_y

    barrier = pltpu.get_barrier_semaphore()
    for device in (y_device, z_device):
        for d in range(DIRS):
            pl.semaphore_signal(barrier, inc=1, device_id={'head': device(d)}, device_id_type=pl.DeviceIdType.MESH)
    pl.semaphore_wait(barrier, 2 * DIRS)
    x_load.wait()

    def rows_of(piece, offset, count):
        return pl.ds(pl.multiple_of(piece * quarter + offset, eighth), count)

    def message(step, c, d, z_first):
        s = sign[d]
        near, behind = (pos_y + s + RING) % RING, (pos_y - s + RING) % RING
        if step == 0:
            src, dst = part.at[rows_of((pos_y + 2) % RING, d * eighth, eighth), cols_of(c)], landed.at[c, d, pl.ds(quarter, eighth), :]
        elif step == 1:
            src, dst = part.at[rows_of(near, 0, quarter), cols_of(c)], landed.at[c, d, pl.ds(0, quarter), :]
        elif z_first:
            back = (pos_z - s + RING) % RING
            if step == 2:
                src = dst = xbuf.at[pos_z, rows_of(pos_y, 0, quarter), cols_of(c)]
            elif step == 3:
                src = dst = xbuf.at[back, rows_of(pos_y, d * eighth, eighth), cols_of(c)]
            elif step == 4:
                src = dst = xbuf.at[:, rows_of(pos_y, 0, quarter), cols_of(c)]
            else:
                src = dst = xbuf.at[:, rows_of(behind, d * eighth, eighth), cols_of(c)]
        else:
            if step == 2:
                src = dst = xbuf.at[pos_z, rows_of(pos_y, 0, quarter), cols_of(c)]
            elif step == 3:
                src = dst = xbuf.at[pos_z, rows_of(behind, d * eighth, eighth), cols_of(c)]
            elif step == 4:
                src = dst = xbuf.at[pos_z, :, cols_of(c)]
            else:
                src = dst = xbuf.at[(pos_z - s + RING) % RING, pl.ds(d * (rows // 2), rows // 2), cols_of(c)]
        along_y = step < 2 or (step < 4) != z_first
        return pltpu.make_async_remote_copy(
            src_ref=src, dst_ref=dst, send_sem=send_sem.at[c, step, d], recv_sem=recv_sem.at[c, step, d],
            device_id={'head': (y_device if along_y else z_device)(d)}, device_id_type=pl.DeviceIdType.MESH)

    def on_messages(step, c, act):
        if step < 2:
            for d in range(DIRS):
                act(message(step, c, d, False))
            return

        @pl.when(c % 4 == 3)
        def _():
            for d in range(DIRS):
                act(message(step, c, d, True))

        @pl.when(c % 4 != 3)
        def _():
            for d in range(DIRS):
                act(message(step, c, d, False))

    def store(c):
        return pltpu.make_async_copy(xbuf.at[:, :, cols_of(c)], out_ref.at[:, :, cols_of(c)], store_sem.at[c])

    def project(c):
        @pl.when(c + 1 < block_count)
        def _():
            for copy in w_loads(c + 1):
                copy.start()

        for copy in w_loads(c):
            copy.wait()
        total = None
        for j in range(RING):
            z = (pos_z + j) % RING
            down = jnp.dot(hid_ref[z], wtile[c % 2, j, :ff_local, :], preferred_element_type=jnp.float32)
            down = down + jnp.dot(att_ref[z], wtile[c % 2, j, ff_local:, :], preferred_element_type=jnp.float32)
            total = down if total is None else total + down
        part[:, cols_of(c)] = total

    def stage(number, c):
        if number == 0:
            project(c)
        else:
            on_messages(number - 1, c, lambda copy: copy.wait_recv())
        if number == 1:
            for d in range(DIRS):
                piece = rows_of((pos_y + sign[d] + RING) % RING, d * eighth, eighth)
                part[piece, cols_of(c)] = part[piece, cols_of(c)] + landed[c, d, pl.ds(quarter, eighth), :]
        if number == 2:
            own = rows_of(pos_y, 0, quarter)
            total = part[own, cols_of(c)] + landed[c, 0, pl.ds(0, quarter), :] + landed[c, 1, pl.ds(0, quarter), :]
            update = total.astype(jnp.bfloat16).astype(jnp.float32)
            xbuf[pos_z, own, cols_of(c)] = (xres[:, cols_of(c)].astype(jnp.float32) + update).astype(jnp.bfloat16)
        if number < LAST_STEPS:
            on_messages(number, c, lambda copy: copy.start())
        else:
            store(c).start()

    def tick(t, carry):
        for number in range(LAST_STEPS, -1, -1):
            c = t - SKEW * number

            @pl.when(jnp.logical_and(c >= 0, c < block_count))
            def _():
                stage(number, c)
        return carry

    lax.fori_loop(0, block_count + SKEW * LAST_STEPS, tick, 0)

    def drain(c, carry):
        for step in range(LAST_STEPS):
            on_messages(step, c, lambda copy: copy.wait_send())
        store(c).wait()
        return carry

    lax.fori_loop(0, block_count, drain, 0)


def layer_last(layer, hid_all, att_all, rest, w_down, w_o, all_down, all_out):
    rows, d_model = hid_all.shape[1], rest.shape[1]
    tok_count = RING * rows
    depth = hid_all.shape[2] + att_all.shape[2]
    any_spec = pl.BlockSpec(memory_space=pl.ANY)
    vmem_spec = pl.BlockSpec(memory_space=pltpu.VMEM)
    blocks = d_model // LAST_COLS
    out = pl.pallas_call(
        functools.partial(last_kernel, layer),
        out_shape=jax.ShapeDtypeStruct((RING, rows, d_model), jnp.bfloat16),
        in_specs=[vmem_spec, vmem_spec] + [any_spec] * 5,
        out_specs=any_spec,
        scratch_shapes=[
            pltpu.VMEM((rows, d_model), jnp.float32),
            pltpu.VMEM((rows // RING, d_model), jnp.bfloat16),
            pltpu.VMEM((RING, rows, d_model), jnp.bfloat16),
            pltpu.VMEM((2, RING, depth, LAST_COLS), jnp.bfloat16),
            pltpu.VMEM((blocks, DIRS, 3 * rows // (2 * RING), LAST_COLS), jnp.float32),
            pltpu.SemaphoreType.DMA((2, RING, 2)),
            pltpu.SemaphoreType.DMA,
            pltpu.SemaphoreType.DMA((blocks,)),
            pltpu.SemaphoreType.DMA((blocks, LAST_STEPS, DIRS)),
            pltpu.SemaphoreType.DMA((blocks, LAST_STEPS, DIRS)),
        ],
        compiler_params=pltpu.CompilerParams(collective_id=layer, has_side_effects=True, vmem_limit_bytes=63 * 1024 * 1024),
        cost_estimate=pl.CostEstimate(flops=2 * tok_count * depth * d_model, bytes_accessed=4 * depth * d_model * 2, transcendentals=0),
        name='last',
    )(hid_all, att_all, rest, w_down, w_o, all_down, all_out)
    return out.reshape(tok_count, d_model)


EMIT_PARTS = 8


def emit_kernel(x_ref, k_first, k_second, v_first, v_second, x_out, k_out, v_out, xbuf, rows, load_sem, store_sem):
    size = x_ref.shape[0] // EMIT_PARTS
    loads, stores = [], []
    for n in range(EMIT_PARTS):
        part = pl.ds(n * size, size)
        loads.append(pltpu.make_async_copy(x_ref.at[part, :], xbuf.at[part, :], load_sem.at[n]))
        stores.append(pltpu.make_async_copy(xbuf.at[part, :], x_out.at[part, :], store_sem.at[n]))
    for n, (ref, out) in enumerate(((k_first, k_out.at[0]), (k_second, k_out.at[1]), (v_first, v_out.at[0]), (v_second, v_out.at[1]))):
        loads.append(pltpu.make_async_copy(ref, rows.at[n], load_sem.at[EMIT_PARTS + n]))
        stores.append(pltpu.make_async_copy(rows.at[n], out, store_sem.at[EMIT_PARTS + n]))
    for copy in loads:
        copy.start()
    for load, store in zip(loads, stores):
        load.wait()
        store.start()
    for copy in stores:
        copy.wait()


def emit(x_out, k_first, k_second, v_first, v_second):
    any_spec = pl.BlockSpec(memory_space=pl.ANY)
    cache = jax.ShapeDtypeStruct((2,) + k_first.shape, jnp.bfloat16)
    return pl.pallas_call(
        emit_kernel,
        out_shape=[jax.ShapeDtypeStruct(x_out.shape, jnp.bfloat16), cache, cache],
        in_specs=[any_spec] * 5,
        out_specs=[any_spec] * 3,
        scratch_shapes=[
            pltpu.VMEM(x_out.shape, jnp.bfloat16),
            pltpu.VMEM((4,) + k_first.shape, jnp.bfloat16),
            pltpu.SemaphoreType.DMA((EMIT_PARTS + 4,)),
            pltpu.SemaphoreType.DMA((EMIT_PARTS + 4,)),
        ],
        compiler_params=pltpu.CompilerParams(vmem_limit_bytes=63 * 1024 * 1024),
        name='emit',
    )(x_out, k_first, k_second, v_first, v_second)


def solution(mesh):
    row_spec = P(('batch', 'seq'), None)
    pos_spec = P(('batch', 'seq'))
    head_spec = P(None, None, 'head', None)
    out_proj_spec = P(None, 'head', None, None)
    col_spec = P(None, None, 'head')
    down_spec = P(None, 'head', None)
    cache_spec = P(None, ('batch', 'seq'), 'head', None)

    def local_forward(x_loc, pos_loc, w_q, w_k, w_v, w_o, w_gate, w_up, w_down, norm_gain):
        tok_count, d_model = x_loc.shape
        layer_count = w_q.shape[0]
        head_dim = w_q.shape[3]
        flat_q, flat_k, flat_v = (w.reshape(layer_count, d_model, head_dim) for w in (w_q, w_k, w_v))
        cos_t, sin_t = rope_tables(pos_loc, head_dim)
        hid_all, att_all, k_first, v_first, k_second, v_second, all_down, all_out, rest = front(x_loc, cos_t, sin_t, norm_gain, flat_q, flat_k, flat_v, w_gate, w_up, w_down, w_o)
        x_out = layer_last(1, hid_all, att_all, rest, w_down, w_o, all_down, all_out)
        x_out, k_all, v_all = emit(x_out, k_first, k_second, v_first, v_second)
        cache_shape = (layer_count, tok_count, 1, head_dim)
        return x_out, k_all.reshape(cache_shape), v_all.reshape(cache_shape)

    return jax.shard_map(local_forward, mesh=mesh, in_specs=(row_spec, pos_spec, head_spec, head_spec, head_spec, out_proj_spec, col_spec, col_spec, down_spec, P(None, None)), out_specs=(row_spec, cache_spec, cache_spec), check_vma=False)
```

```python
import functools
import math
import jax
import jax.numpy as jnp
from jax import lax
from jax.experimental import pallas as pl
from jax.experimental.pallas import tpu as pltpu
from jax.sharding import PartitionSpec as P

ROPE_BASE = 500000.0
EPS = 1e-5


def rope_tables(positions, head_dim):
    half_dim = head_dim // 2
    inv_freq = ROPE_BASE ** (-(jnp.arange(half_dim, dtype=jnp.float32) * 2.0 / head_dim))
    angles = positions.astype(jnp.float32)[..., None] * inv_freq
    return jnp.cos(angles), jnp.sin(angles)


CHIPS = 4
RING = 4
HALVES = 2
DIRS = 2
KV_CHUNKS = 4
W_TILE = 256
NORM_ROWS = 64
CHUNKS = 8
STEPS = 8
PART_SLOTS = 4
RECV_SLOTS = 5
DOWN_TILE = 512
START_GAP = 3
STAGE_GAP = 2
BLOCK_TICK = 19
BLOCK_GAP = 6
LAST_TICK = 43
NEAR_TICKS = ((9, 1), (15, 3))
FAR_TICKS = ((24, 1), (26, 3))
SERVE_TICKS = (27, 31, 35, 42)
GIVE_TICK = 37
OWN_TICK = 3
DONE_TICK = 11
EARLY_TICK = 31


def front_kernel(x_ref, cos_ref, sin_ref, gain_ref, wq_ref, wk_ref, wv_ref, wg_ref, wu_ref, wd_ref, wo_ref,
                 hid_all_ref, att_all_ref, k1_ref, v1_ref, k2_ref, v2_ref, gd_ref, go_ref, rest_ref,
                 xbuf, part, recv_a, recv_b, hid, att, wdo, wtile, kv, qbuf, acc, row_max, row_sum, xs, xres,
                 x_sem, res_sem, w_sem, down_sem, cache_sem, rest_sem, own_send, pass_send, ici_recv, core_recv, part_send, part_recv,
                 round_send, round_recv, side_send, side_recv, give_send, give_recv, keep_sem, relay_buf, relay_send, relay_recv, ring_send, ring_recv, ready_sem):
    tok_count, d_model = xbuf.shape
    head_dim = qbuf.shape[1]
    half_dim = head_dim // 2
    ff_local = hid.shape[1]
    rows_per = tok_count // KV_CHUNKS
    half_rows = tok_count // 2
    lanes = row_max.shape[2]
    chunk_rows = tok_count // CHUNKS
    quarter, eighth = chunk_rows // RING, chunk_rows // (2 * RING)
    half_cols = d_model // HALVES
    piece_cols = half_cols // RING
    bf16, f32 = jnp.bfloat16, jnp.float32
    sign = (1, -1)
    mesh_id = pl.DeviceIdType.MESH

    my_head = lax.axis_index('head')
    pos_z, pos_y = my_head // RING, my_head % RING
    my_seq = lax.axis_index('seq')
    chip, core = my_seq // 2, my_seq % 2
    other = chip * 2 + 1 - core

    def wrap(n):
        return (n + RING) % RING

    def y_peer(d):
        return pos_z * RING + wrap(pos_y + sign[d])

    def z_device(z):
        return wrap(z) * RING + pos_y

    def z_peer(d):
        return z_device(pos_z + sign[d])

    def x_device(n):
        return wrap(chip + n) * 2 + core

    right, left = x_device(1), x_device(-1)

    def span(start, size, unit=None):
        return pl.ds(pl.multiple_of(start, unit or size), size)

    def remote(src, dst, send, recv, **to):
        return pltpu.make_async_remote_copy(src_ref=src, dst_ref=dst, send_sem=send, recv_sem=recv, device_id=to, device_id_type=mesh_id)

    def x_load(i):
        return pltpu.make_async_copy(x_ref.at[span(i * rows_per, rows_per), :], xs.at[i % 2], x_sem.at[i % 2])

    def weights(layer, piece):
        slot = piece % 2
        if isinstance(piece, int) and piece < 2:
            refs = ((wk_ref, wv_ref), (wq_ref,))[piece]
            return [pltpu.make_async_copy(ref.at[layer], wtile.at[slot, n], w_sem.at[slot, n]) for n, ref in enumerate(refs)]
        cols = span((piece - 2) * W_TILE, W_TILE)
        return [pltpu.make_async_copy(ref.at[layer, :, cols], wtile.at[slot, n], w_sem.at[slot, n]) for n, ref in enumerate((wg_ref, wu_ref))]

    def start(copies):
        for copy in copies:
            copy.start()

    def wait(copies):
        for copy in copies:
            copy.wait()

    down_tiles = d_model // DOWN_TILE

    def down_load(i):
        cols = span(i * DOWN_TILE, DOWN_TILE)
        return [pltpu.make_async_copy(wd_ref.at[0, :, cols], wdo.at[i % 2, pl.ds(0, ff_local), :], down_sem.at[i % 2, 0]),
                pltpu.make_async_copy(wo_ref.at[0, 0, :, cols], wdo.at[i % 2, pl.ds(ff_local, head_dim), :], down_sem.at[i % 2, 1])]

    def kv_copy(origin_chip, origin_core, i, to, send, recv):
        rows = kv.at[span((origin_chip * 2 + origin_core) * tok_count + i * rows_per, rows_per), :]
        return remote(rows, rows, send, recv, seq=to)

    def kv_routes(layer, i):
        late = i >= KV_CHUNKS // 2
        early = jnp.logical_not(late) if not isinstance(i, int) else not late

        def to(send, recv, origin_chip, origin_core, device):
            return kv_copy(origin_chip, origin_core, i, device, send, recv)
        own, passed, ici, side = own_send.at[layer], pass_send.at[layer], ici_recv.at[layer], core_recv.at[layer]
        return {
            'right': (chip < CHIPS - 1, lambda: to(own.at[0, i], ici.at[0, i], chip, core, right)),
            'wrap': (chip == 0, lambda: to(own.at[1, i], ici.at[2, i], chip, core, left)),
            'relay': (jnp.logical_and(late, chip == 1), lambda: to(own.at[3, i], ici.at[3, i], chip, core, left)),
            'other': (core == 0, lambda: to(own.at[2, i], side.at[0, i], chip, core, other)),
            'on_right': (jnp.logical_and(early, jnp.logical_and(chip >= 1, chip < CHIPS - 1)), lambda: to(passed.at[0, i], ici.at[1, i], chip - 1, core, right)),
            'from_relay': (jnp.logical_and(late, chip == 0), lambda: to(passed.at[0, i], ici.at[1, i], 1, core, left)),
            'on_left': (jnp.logical_and(late, chip == CHIPS - 1), lambda: to(passed.at[0, i], ici.at[1, i], 0, core, left)),
            'side1': (chip >= 1, lambda: to(passed.at[1, i], side.at[1, i], chip - 1, core, other)),
            'side2': (chip >= 2, lambda: to(passed.at[2, i], side.at[2, i], chip - 2, core, other)),
            'side3': (chip >= 3, lambda: to(passed.at[3, i], side.at[3, i], chip - 3, core, other)),
        }

    def start_route(layer, i, name):
        condition, copy = kv_routes(layer, i)[name]

        @pl.when(condition)
        def _():
            copy().start()

    def send_kv(layer, i):
        for name in ('right', 'wrap', 'relay', 'other'):
            start_route(layer, i, name)

    def kv_sent(layer):
        for i in range(KV_CHUNKS):
            for condition, copy in kv_routes(layer, i).values():
                @pl.when(condition)
                def _():
                    copy().wait_send()

    def serve(layer, back, i):
        @pl.when(chip >= back)
        def _():
            kv_copy(chip - back, core, i, other, pass_send.at[layer, back, i], ici_recv.at[layer, back - 1, i]).wait_recv()
        start_route(layer, i, 'side%d' % back)
        if back == 1:
            start_route(layer, i, 'on_right')
        if back == 3:
            start_route(layer, i, 'on_left')

    def relay(layer, i):
        condition, copy = kv_routes(layer, i)['from_relay']

        @pl.when(condition)
        def _():
            kv_copy(1, core, i, left, pass_send.at[layer, 0, i], ici_recv.at[layer, 3, i]).wait_recv()
            copy().start()

    def serve_all(layer, i):
        serve(layer, 1, i)
        serve(layer, 3, i)
        relay(layer, i)

    def taken(layer, back, chunks):
        for i in chunks:
            kv_copy(chip - back, 1 - core, i, other, pass_send.at[layer, 0, i], core_recv.at[layer, back, i]).wait_recv()

    def z_parts(step, d):
        copies = []
        for n, (own_ref, all_ref) in enumerate(((wd_ref, gd_ref), (wo_ref, go_ref))):
            size = all_ref.shape[1] // (2 * CHIPS)
            if step == 0:
                rows = span(my_seq * size, size)
                src = own_ref.at[1, rows, :] if n == 0 else own_ref.at[1, 0, rows, :]
                dst = all_ref.at[pos_z, rows, :]
            else:
                rows = span(my_seq * size + d * (size // 2), size // 2)
                src = dst = all_ref.at[wrap(pos_z - sign[d]), rows, :]
            copies.append(remote(src, dst, part_send.at[step, d, n], part_recv.at[step, d, n], head=z_peer(d)))
        return copies

    def part_copies(j, part_chip, part_core, half, send, recv, to):
        copies = []
        for n, ref in enumerate((gd_ref, go_ref)):
            size = ref.shape[1] // (2 * CHIPS)
            first = (part_chip * 2 + part_core) * size
            rows = span(first, size) if half is None else span(first + half * (size // 2), size // 2)
            place = ref.at[wrap(pos_z + j), rows, :]
            copies.append(remote(place, place, send.at[n], recv.at[n], seq=to))
        return copies

    def own_part(j, d):
        return part_copies(j, chip, core, None, round_send.at[0, j - 1, d], round_recv.at[0, j - 1, d], x_device(sign[d]))

    def far_part(j, d):
        return part_copies(j, wrap(chip - sign[d]), core, d, round_send.at[1, j - 1, d], round_recv.at[1, j - 1, d], x_device(sign[d]))

    def side_part(j, n, side):
        return part_copies(j, wrap(chip + n), side, None, side_send.at[j - 1, n], side_recv.at[j - 1, n], other)

    def round_start(j):
        for d in range(DIRS):
            start(own_part(j, d))
        start(side_part(j, 0, core))

    def near_parts(j):
        for d in range(DIRS):
            for copy in own_part(j, d):
                copy.wait_recv()
            start(far_part(j, d) + side_part(j, 3 if d == 0 else 1, core))

    def far_parts(j):
        for d in range(DIRS):
            for copy in far_part(j, d):
                copy.wait_recv()
        start(side_part(j, 2, core))

    def give_hidden(z, i, source):
        cols = span(i * W_TILE, W_TILE)
        return remote(hid.at[span(z * rows_per, rows_per), cols], hid_all_ref.at[source, :, cols], give_send.at[z, i], give_recv.at[source, i], head=z_device(z))

    def keep_hidden(i):
        cols = span(i * W_TILE, W_TILE)
        return pltpu.make_async_copy(hid.at[span(pos_z * rows_per, rows_per), cols], hid_all_ref.at[pos_z, :, cols], keep_sem.at[i])

    def via_neighbor(z, i):
        step = jnp.where(i < KV_CHUNKS // 2, 1, -1)
        return remote(hid.at[span(z * rows_per, rows_per), span(i * W_TILE, W_TILE)], relay_buf.at[i], give_send.at[z, i], relay_recv.at[i], head=z_device(pos_z + step))

    def relay_hidden(i):
        step = 1 if i < KV_CHUNKS // 2 else -1
        source = wrap(pos_z - step)
        return remote(relay_buf.at[i], hid_all_ref.at[source, :, span(i * W_TILE, W_TILE)], relay_send.at[i], give_recv.at[source, i], head=z_device(pos_z + step))

    def send_hidden(z, i):
        away = wrap(z - pos_z)

        @pl.when(away == 2)
        def _():
            via_neighbor(z, i).start()

        @pl.when(away % 2 == 1)
        def _():
            give_hidden(z, i, pos_z).start()

        @pl.when(away == 0)
        def _():
            keep_hidden(i).start()

    def give_rows(z, source):
        return remote(att.at[span(z * rows_per, rows_per), :], att_all_ref.at[source], give_send.at[z, KV_CHUNKS], give_recv.at[source, KV_CHUNKS], head=z_device(z))

    def keep_rows():
        return pltpu.make_async_copy(att.at[span(pos_z * rows_per, rows_per), :], att_all_ref.at[pos_z], keep_sem.at[KV_CHUNKS])

    def norm_rows(x_few, layer):
        x_f32 = x_few.astype(f32)
        inv_rms = lax.rsqrt(jnp.mean(x_f32 * x_f32, axis=-1, keepdims=True) + EPS)
        return (x_f32 * inv_rms * gain_ref[pl.ds(layer, 1), :].astype(f32)).astype(bf16)

    def rope(values, rows):
        cos_t, sin_t = cos_ref[rows, :], sin_ref[rows, :]
        wide = values.astype(bf16).astype(f32)
        first, second = wide[:, :half_dim], wide[:, half_dim:]
        return jnp.concatenate([first * cos_t - second * sin_t, second * cos_t + first * sin_t], axis=1).astype(bf16)

    def dot(a, b):
        return jnp.dot(a, b, preferred_element_type=f32)

    scale = 1.0 / math.sqrt(head_dim)

    def keys_values(normed, i):
        rows = span(i * rows_per, rows_per)
        own = span(my_seq * tok_count + i * rows_per, rows_per)
        kv[own, :head_dim] = rope(dot(normed, wtile[0, 0]), rows)
        kv[own, head_dim:] = dot(normed, wtile[0, 1]).astype(bf16)

    def queries(normed, i):
        rows = span(i * rows_per, rows_per)
        qbuf[rows, :] = (rope(dot(normed, wtile[1, 0]), rows).astype(f32) * scale).astype(bf16)

    def gated(normed, i, tile):
        gate = dot(normed, wtile[tile % 2, 0])
        up = dot(normed, wtile[tile % 2, 1])
        hid[span(i * rows_per, rows_per), span(tile * W_TILE, W_TILE)] = (gate * jax.nn.sigmoid(gate) * up).astype(bf16)

    def attend(key_start, q_half, side, masked, first):
        rows = pl.ds(q_half * half_rows, half_rows)
        some = span(key_start, half_rows)
        logits = lax.dot_general(qbuf[rows, :], kv[some, :head_dim], (((1,), (1,)), ((), ())), preferred_element_type=f32)
        if masked:
            seen = lax.broadcasted_iota(jnp.int32, logits.shape, 0) >= lax.broadcasted_iota(jnp.int32, logits.shape, 1)
            logits = jnp.where(seen, logits, -jnp.inf)
        block_max = jnp.max(logits, axis=-1, keepdims=True)
        if first:
            new_max = jnp.broadcast_to(block_max, (half_rows, lanes))
        else:
            new_max = jnp.maximum(row_max[side, rows, :], block_max)
        prob = jnp.exp(logits - jnp.concatenate([new_max] * (half_rows // lanes), axis=1))
        block_sum = jnp.sum(prob, axis=-1, keepdims=True)
        block_out = dot(prob.astype(bf16), kv[some, head_dim:])
        if first:
            row_sum[side, rows, :] = jnp.broadcast_to(block_sum, (half_rows, lanes))
            acc[side, rows, :] = block_out
        else:
            rescale = jnp.exp(row_max[side, rows, :] - new_max)
            row_sum[side, rows, :] = row_sum[side, rows, :] * rescale + block_sum
            acc[side, rows, :] = acc[side, rows, :] * jnp.concatenate([rescale] * (head_dim // lanes), axis=1) + block_out
        row_max[side, rows, :] = new_max

    def attend_own(layer_half):
        own_start = my_seq * tok_count
        if layer_half == 0:
            attend(own_start, 0, 0, True, True)
            top_rows = pl.ds(0, half_rows)
            row_max[1, top_rows, :] = jnp.full((half_rows, lanes), -jnp.inf, f32)
            row_sum[1, top_rows, :] = jnp.zeros((half_rows, lanes), f32)
            acc[1, top_rows, :] = jnp.zeros((half_rows, head_dim), f32)
        else:
            attend(own_start, 1, 0, False, True)
            attend(own_start + half_rows, 1, 1, True, True)

    def past_start(n):
        later = n - core
        back = jnp.where(later < 2, 1, jnp.where(chip == CHIPS - 1, jnp.where(later < 4, 3, 2), 2))
        block = (chip - back) * 2 + jnp.where(later % 2 == 0, core, 1 - core)
        return jnp.where(jnp.logical_and(core == 1, n == 0), chip * 2, block) * tok_count

    def arrivals(layer, n, chunks):
        @pl.when(jnp.logical_and(core == 1, n == 0))
        def _():
            taken(layer, 0, chunks)

        for back in (1, 3, 2):
            place = 0 if back == 1 else 2 if back == 3 else jnp.where(chip == CHIPS - 1, 4, 2)
            if back == 2:
                @pl.when(jnp.logical_and(chip >= back, n == core + place))
                def _():
                    for i in chunks:
                        serve(layer, 2, i)

            @pl.when(jnp.logical_and(chip >= back, n == core + place + 1))
            def _():
                taken(layer, back, chunks)

    def visit(n, visits):
        for q_half, side in visits:
            attend(past_start(n) + side * half_rows, q_half, side, False, False)

    def attend_past(layer, first_n, last_n, chunks, visits):
        def past(n, carry):
            if chunks:
                arrivals(layer, n, chunks)
            visit(n, visits)
            return carry

        lax.fori_loop(first_n, last_n, past, 0)

    near_count = my_seq - jnp.where(chip >= 2, 2, 0)

    def finish(i, spread):
        rows = pl.ds(i * rows_per, rows_per)
        top = jnp.maximum(row_max[0, rows, :], row_max[1, rows, :])
        shares = [jnp.exp(row_max[side, rows, :] - top) for side in range(2)]
        total = shares[0] * row_sum[0, rows, :] + shares[1] * row_sum[1, rows, :]
        wide = [jnp.concatenate([w] * (head_dim // lanes), axis=1) for w in shares + [total]]
        att[rows, :] = ((acc[0, rows, :] * wide[0] + acc[1, rows, :] * wide[1]) / wide[2]).astype(bf16)
        if spread:
            @pl.when(i == pos_z)
            def _():
                keep_rows().start()

            @pl.when(i != pos_z)
            def _():
                give_rows(i, pos_z).start()

    first_pos, second_pos = (pos_y, pos_z), (pos_z, pos_y)
    first_peer, second_peer = (y_peer, z_peer), (z_peer, y_peer)

    def part_rows(chunk, piece, offset, count):
        return span((chunk % PART_SLOTS) * chunk_rows + piece * quarter + offset, count, eighth)

    def x_rows(chunk, piece, offset, count):
        return span(chunk * chunk_rows + piece * quarter + offset, count, eighth)

    def cols_of(h, piece):
        return span(h * half_cols + piece * piece_cols, piece_cols)

    def half_of(h):
        return pl.ds(h * half_cols, half_cols)

    def message(step, chunk, h, d):
        p1, p2, s = first_pos[h], second_pos[h], sign[d]
        slot = chunk % RECV_SLOTS
        if step == 0:
            src, dst = part.at[part_rows(chunk, wrap(p1 + 2), d * eighth, eighth), half_of(h)], recv_a.at[slot, h, d, pl.ds(quarter, eighth), :]
        elif step == 1:
            src, dst = part.at[part_rows(chunk, wrap(p1 + s), 0, quarter), half_of(h)], recv_a.at[slot, h, d, pl.ds(0, quarter), :]
        elif step == 2:
            src, dst = part.at[part_rows(chunk, p1, d * eighth, eighth), cols_of(h, wrap(p2 + 2))], recv_b.at[slot, h, d, pl.ds(quarter, eighth), :]
        elif step == 3:
            src, dst = part.at[part_rows(chunk, p1, 0, quarter), cols_of(h, wrap(p2 + s))], recv_b.at[slot, h, d, pl.ds(0, quarter), :]
        elif step == 4:
            src = dst = xbuf.at[x_rows(chunk, p1, 0, quarter), cols_of(h, p2)]
        elif step == 5:
            src = dst = xbuf.at[x_rows(chunk, p1, d * eighth, eighth), cols_of(h, wrap(p2 - s))]
        elif step == 6:
            src = dst = xbuf.at[x_rows(chunk, p1, 0, quarter), half_of(h)]
        else:
            src = dst = xbuf.at[x_rows(chunk, wrap(p1 - s), d * eighth, eighth), half_of(h)]
        peer = (first_peer if step in (0, 1, 6, 7) else second_peer)[h](d)
        return remote(src, dst, ring_send.at[chunk, step, h * DIRS + d], ring_recv.at[chunk, step, h * DIRS + d], head=peer)

    def each_message(chunk, steps, act):
        for step in steps:
            for h in range(HALVES):
                for d in range(DIRS):
                    act(message(step, chunk, h, d))

    def residual_load(chunk, h):
        return pltpu.make_async_copy(x_ref.at[x_rows(chunk, first_pos[h], 0, quarter), cols_of(h, second_pos[h])], xres.at[chunk, h], res_sem.at[chunk, h])

    def project(chunk):
        rows = span(chunk * chunk_rows, chunk_rows)
        slot_rows = span((chunk % PART_SLOTS) * chunk_rows, chunk_rows)

        def one_tile(i, carry):
            @pl.when(jnp.logical_or(chunk < CHUNKS - 1, i < down_tiles - 1))
            def _():
                start(down_load((i + 1) % down_tiles))

            wait(down_load(i))
            total = dot(hid[rows, :], wdo[i % 2, :ff_local, :])
            part[slot_rows, span(i * DOWN_TILE, DOWN_TILE)] = total + dot(att[rows, :], wdo[i % 2, ff_local:, :])
            return carry

        lax.fori_loop(0, down_tiles, one_tile, 0)

    def stage(number, chunk):
        slot = chunk % RECV_SLOTS
        if number == 0:
            @pl.when(chunk >= PART_SLOTS)
            def _():
                each_message(chunk - PART_SLOTS, range(4), lambda copy: copy.wait_send())
            project(chunk)
        for h in range(HALVES):
            p1, p2 = first_pos[h], second_pos[h]
            if number:
                for d in range(DIRS):
                    message(number - 1, chunk, h, d).wait_recv()
            if number in (1, 3):
                for d in range(DIRS):
                    if number == 1:
                        rows, cols, arrived = part_rows(chunk, wrap(p1 + sign[d]), d * eighth, eighth), half_of(h), recv_a
                    else:
                        rows, cols, arrived = part_rows(chunk, p1, d * eighth, eighth), cols_of(h, wrap(p2 + sign[d])), recv_b
                    part[rows, cols] = part[rows, cols] + arrived[slot, h, d, pl.ds(quarter, eighth), :]
            if number == 2:
                rows = part_rows(chunk, p1, 0, quarter)
                part[rows, half_of(h)] = part[rows, half_of(h)] + recv_a[slot, h, 0, pl.ds(0, quarter), :] + recv_a[slot, h, 1, pl.ds(0, quarter), :]
            if number == 4:
                residual_load(chunk, h).wait()
                rows, cols = part_rows(chunk, p1, 0, quarter), cols_of(h, p2)
                total = part[rows, cols] + recv_b[slot, h, 0, pl.ds(0, quarter), :] + recv_b[slot, h, 1, pl.ds(0, quarter), :]
                update = total.astype(bf16).astype(f32)
                xbuf[x_rows(chunk, p1, 0, quarter), cols] = (xres[chunk, h].astype(f32) + update).astype(bf16)
            if number < STEPS:
                for d in range(DIRS):
                    message(number, chunk, h, d).start()

    x_load(0).start()
    start(weights(0, 0))
    x_load(1).start()
    start(weights(0, 1))
    barrier = pltpu.get_barrier_semaphore()
    for peer in (left, right, other):
        pl.semaphore_signal(barrier, inc=1, device_id={'seq': peer}, device_id_type=mesh_id)
    for peer in [z_device(pos_z + j) for j in range(1, RING)] + [y_peer(d) for d in range(DIRS)]:
        pl.semaphore_signal(barrier, inc=1, device_id={'head': peer}, device_id_type=mesh_id)

    def prepare(i, carry):
        x_load(i).wait()

        def few(n, inner):
            xbuf[span(i * rows_per + n * NORM_ROWS, NORM_ROWS), :] = norm_rows(xs[i % 2, span(n * NORM_ROWS, NORM_ROWS), :], 0)
            return inner

        lax.fori_loop(0, rows_per // NORM_ROWS, few, 0)

        @pl.when(i + 2 < KV_CHUNKS)
        def _():
            x_load(i + 2).start()

        @pl.when(i == 0)
        def _():
            wait(weights(0, 0))

        keys_values(xbuf[span(i * rows_per, rows_per), :], i)

        @pl.when(i == 0)
        def _():
            pl.semaphore_wait(barrier, 8)

        send_kv(0, i)

        @pl.when(i == 0)
        def _():
            for d in range(DIRS):
                start(z_parts(0, d))
        return carry

    lax.fori_loop(0, KV_CHUNKS, prepare, 0)
    start(weights(0, 2))
    own_rows = span(my_seq * tok_count, tok_count)

    def cache_stores(layer):
        k_ref, v_ref = ((k1_ref, v1_ref), (k2_ref, v2_ref))[layer]
        return [pltpu.make_async_copy(kv.at[own_rows, pl.ds(0, head_dim)], k_ref, cache_sem.at[layer, 0]),
                pltpu.make_async_copy(kv.at[own_rows, pl.ds(head_dim, head_dim)], v_ref, cache_sem.at[layer, 1])]

    start(cache_stores(0))
    wait(weights(0, 1))

    def query(i, carry):
        queries(xbuf[span(i * rows_per, rows_per), :], i)
        return carry

    lax.fori_loop(0, KV_CHUNKS, query, 0)
    start(weights(0, 3))
    start(down_load(0))

    def residuals(n, carry):
        for h in range(HALVES):
            residual_load(n, h).start()
        return carry

    lax.fori_loop(0, CHUNKS, residuals, 0)

    def gate_half(half, tile):
        wait(weights(0, tile + 2))

        def rows_step(i, inner):
            gated(xbuf[span(i * rows_per, rows_per), :], i, tile)
            return inner

        lax.fori_loop(half * KV_CHUNKS // 2, (half + 1) * KV_CHUNKS // 2, rows_step, 0)

        @pl.when(tile < 2)
        def _():
            start(weights(0, tile + 4))

        for last in (2, 3):
            @pl.when(tile == last)
            def _():
                start(weights(1, last - 2) if half else weights(0, last))

    def first_half(tile, carry):
        gate_half(0, tile)

        @pl.when(tile < 3)
        def _():
            serve_all(0, tile)
        return carry

    def second_half(tile, carry):
        gate_half(1, tile)

        @pl.when(tile == 0)
        def _():
            serve_all(0, 3)
            attend_past(0, 0, near_count, range(KV_CHUNKS), ((0, 0), (0, 1)))
            for d in range(DIRS):
                for copy in z_parts(0, d):
                    copy.wait_recv()
                start(z_parts(1, d))
        return carry

    lax.fori_loop(0, ff_local // W_TILE, first_half, 0)
    attend_own(0)
    lax.fori_loop(0, 2, second_half, 0)
    attend_past(0, near_count, my_seq, range(KV_CHUNKS), ((0, 0), (0, 1)))
    finish(0, False)
    finish(1, False)
    round_start(1)
    round_start(3)

    def block_work(j, phase):
        @pl.when(phase == 0)
        def _():
            @pl.when(j == 0)
            def _():
                for n in range(3):
                    pl.semaphore_wait(ready_sem.at[n], 1)

            def few(n, inner):
                xs[0, span(n * NORM_ROWS, NORM_ROWS), :] = norm_rows(xbuf[span(j * rows_per + n * NORM_ROWS, NORM_ROWS), :], 1)
                return inner

            lax.fori_loop(0, rows_per // NORM_ROWS, few, 0)
            wait(weights(1, 0))
            keys_values(xs[0], j)
            send_kv(1, j)
            start(weights(1, 2))

        @pl.when(phase == 1)
        def _():
            wait(weights(1, 1))
            queries(xs[0], j)
            start(weights(1, 3))

        @pl.when(jnp.logical_and(phase >= 1, phase <= 4))
        def _():
            tile = phase - 1
            wait(weights(1, tile + 2))
            gated(xs[0], j, tile)

            @pl.when(tile < 2)
            def _():
                start(weights(1, tile + 4))

            @pl.when(jnp.logical_and(tile == 2, j < KV_CHUNKS - 1))
            def _():
                start(weights(1, 0))

            @pl.when(jnp.logical_and(tile == 3, j < KV_CHUNKS - 1))
            def _():
                start(weights(1, 1))

            @pl.when(j == KV_CHUNKS - 1)
            def _():
                send_hidden(j, tile)

    def tick(t, carry):
        for number in range(STEPS, -1, -1):
            place = t - STAGE_GAP * number
            chunk = place // START_GAP

            @pl.when(jnp.logical_and(place >= 0, jnp.logical_and(place % START_GAP == 0, chunk < CHUNKS)))
            def _():
                stage(number, chunk)

        @pl.when(jnp.logical_or(t == 1, t == 3))
        def _():
            gate_half(1, 2 + t // 2)

        @pl.when(t == OWN_TICK)
        def _():
            attend_own(1)

        @pl.when(jnp.logical_and(t > OWN_TICK, jnp.logical_and(t < DONE_TICK, t - OWN_TICK <= my_seq)))
        def _():
            visit(t - OWN_TICK - 1, ((1, 0), (1, 1)))

        @pl.when(t == EARLY_TICK)
        def _():
            attend_own(0)

        early = t - EARLY_TICK - 1

        @pl.when(jnp.logical_and(early >= 0, jnp.logical_and(early < 7, early < my_seq)))
        def _():
            arrivals(1, early, (0, 1))
            visit(early, ((0, 0),))

        @pl.when(t == 2)
        def _():
            for d in range(DIRS):
                for copy in z_parts(1, d):
                    copy.wait_recv()
            round_start(2)

        @pl.when(t == DONE_TICK)
        def _():
            finish(2, False)
            finish(3, False)
            kv_sent(0)
            wait(cache_stores(0))
            for n, peer in enumerate((left, right, other)):
                pl.semaphore_signal(ready_sem.at[n], inc=1, device_id={'seq': peer}, device_id_type=mesh_id)

        for when, j in NEAR_TICKS:
            @pl.when(t == when)
            def _():
                near_parts(j)

        for when, j in FAR_TICKS:
            @pl.when(t == when)
            def _():
                far_parts(j)

        @pl.when(t == GIVE_TICK)
        def _():
            for i in range(KV_CHUNKS):
                for z in range(KV_CHUNKS - 1):
                    send_hidden(z, i)

        late = t - BLOCK_TICK

        @pl.when(late >= 0)
        def _():
            block_work(late // BLOCK_GAP, late % BLOCK_GAP)

        for i, when in enumerate(SERVE_TICKS):
            @pl.when(t == when)
            def _():
                serve_all(1, i)
        return carry

    lax.fori_loop(0, LAST_TICK, tick, 0)

    start(cache_stores(1))
    rest_store = pltpu.make_async_copy(xbuf.at[span(pos_z * rows_per + pos_y * (rows_per // RING), rows_per // RING), :], rest_ref, rest_sem)
    rest_store.start()
    near_parts(2)
    attend_own(1)
    attend_past(1, 0, my_seq, (), ((1, 0),))
    for i in range(KV_CHUNKS):
        via_neighbor(0, i).wait_recv()
        relay_hidden(i).start()
    attend_past(1, 0, near_count, (2, 3), ((0, 1), (1, 1)))
    attend_past(1, near_count, my_seq, (2, 3), ((0, 1),))
    finish(0, True)
    finish(1, True)
    attend_past(1, near_count, my_seq, (), ((1, 1),))
    finish(2, True)
    finish(3, True)
    far_parts(2)

    wait(cache_stores(1))
    rest_store.wait()
    for i in range(KV_CHUNKS):
        keep_hidden(i).wait()
        relay_hidden(i).wait_send()
    keep_rows().wait()
    kv_sent(1)
    for d in range(DIRS):
        for step in range(2):
            for copy in z_parts(step, d):
                copy.wait_send()
    for j in range(1, RING):
        for d in range(DIRS):
            for copy in own_part(j, d) + far_part(j, d):
                copy.wait_send()
        for n in range(CHIPS):
            for copy in side_part(j, n, 1 - core):
                copy.wait_recv()
            for copy in side_part(j, n, core):
                copy.wait_send()
        z = wrap(pos_z + j)
        for i in range(KV_CHUNKS):
            give_hidden(z, i, z).wait_recv()
            give_hidden(z, i, pos_z).wait_send()
        give_rows(z, z).wait_recv()
        give_rows(z, pos_z).wait_send()

    def drain(chunk, carry):
        @pl.when(chunk >= CHUNKS - PART_SLOTS)
        def _():
            each_message(chunk, range(4), lambda copy: copy.wait_send())
        each_message(chunk, range(4, STEPS), lambda copy: copy.wait_send())
        return carry

    lax.fori_loop(0, CHUNKS, drain, 0)


def front(x_loc, cos_t, sin_t, norm_gain, w_q, w_k, w_v, w_gate, w_up, w_down, w_o):
    tok_count, d_model = x_loc.shape
    head_dim = w_q.shape[2]
    ff_local = w_gate.shape[2]
    rows_per = tok_count // KV_CHUNKS
    chunk_rows = tok_count // CHUNKS
    landed = 3 * chunk_rows // (2 * RING)
    half_cols = d_model // HALVES
    any_spec = pl.BlockSpec(memory_space=pl.ANY)
    vmem_spec = pl.BlockSpec(memory_space=pltpu.VMEM)
    bf16, f32 = jnp.bfloat16, jnp.float32
    dma = pltpu.SemaphoreType.DMA
    shape = jax.ShapeDtypeStruct
    return pl.pallas_call(
        front_kernel,
        out_shape=[shape((RING, rows_per, ff_local), bf16), shape((RING, rows_per, head_dim), bf16)] + [shape((tok_count, head_dim), bf16)] * 4
        + [shape((RING, ff_local, d_model), bf16), shape((RING, head_dim, d_model), bf16), shape((rows_per // RING, d_model), bf16)],
        in_specs=[any_spec, vmem_spec, vmem_spec, vmem_spec] + [any_spec] * 7,
        out_specs=[any_spec] * 9,
        scratch_shapes=[
            pltpu.VMEM((tok_count, d_model), bf16),
            pltpu.VMEM((PART_SLOTS * chunk_rows, d_model), f32),
            pltpu.VMEM((RECV_SLOTS, HALVES, DIRS, landed, half_cols), f32),
            pltpu.VMEM((RECV_SLOTS, HALVES, DIRS, landed, half_cols // RING), f32),
            pltpu.VMEM((tok_count, ff_local), bf16),
            pltpu.VMEM((tok_count, head_dim), bf16),
            pltpu.VMEM((2, ff_local + head_dim, DOWN_TILE), bf16),
            pltpu.VMEM((2, 2, d_model, W_TILE), bf16),
            pltpu.VMEM((2 * CHIPS * tok_count, 2 * head_dim), bf16),
            pltpu.VMEM((tok_count, head_dim), bf16),
            pltpu.VMEM((2, tok_count, head_dim), f32),
            pltpu.VMEM((2, tok_count, 128), f32),
            pltpu.VMEM((2, tok_count, 128), f32),
            pltpu.VMEM((2, rows_per, d_model), bf16),
            pltpu.VMEM((CHUNKS, HALVES, chunk_rows // RING, half_cols // RING), bf16),
            dma((2,)), dma((CHUNKS, HALVES)), dma((2, 2)), dma((2, 2)), dma((2, 2)), dma,
            dma((2, 4, KV_CHUNKS)), dma((2, 4, KV_CHUNKS)), dma((2, 4, KV_CHUNKS)), dma((2, 4, KV_CHUNKS)), dma((2, DIRS, 2)), dma((2, DIRS, 2)),
            dma((2, RING - 1, DIRS, 2)), dma((2, RING - 1, DIRS, 2)), dma((RING - 1, CHIPS, 2)), dma((RING - 1, CHIPS, 2)),
            dma((RING, KV_CHUNKS + 1)), dma((RING, KV_CHUNKS + 1)), dma((KV_CHUNKS + 1,)),
            pltpu.VMEM((KV_CHUNKS, rows_per, W_TILE), bf16), dma((KV_CHUNKS,)), dma((KV_CHUNKS,)),
            dma((CHUNKS, STEPS, HALVES * DIRS)), dma((CHUNKS, STEPS, HALVES * DIRS)),
            pltpu.SemaphoreType.REGULAR((3,)),
        ],
        compiler_params=pltpu.CompilerParams(collective_id=0, has_side_effects=True, vmem_limit_bytes=67043328),
        name='front',
    )(x_loc, cos_t, sin_t, norm_gain, w_q, w_k, w_v, w_gate, w_up, w_down, w_o)


SKEW = 2
LAST_STEPS = 6
LAST_COLS = 256


def last_kernel(layer, hid_ref, att_ref, rest_ref, wd_ref, wo_ref, gd_ref, go_ref, out_ref, part, xres, xbuf, wtile, landed, w_sem, x_sem, store_sem, send_sem, recv_sem):
    rows, d_model = part.shape
    block = wtile.shape[3]
    block_count = d_model // block
    ff_local = hid_ref.shape[2]
    quarter, eighth = rows // RING, rows // (2 * RING)
    my_head = lax.axis_index('head')
    pos_z, pos_y = my_head // RING, my_head % RING
    sign = (1, -1)

    def cols_of(c):
        return pl.ds(pl.multiple_of(c * block, block), block)

    def w_loads(c):
        copies = []
        for j in range(RING):
            z = (pos_z + j) % RING
            down = wd_ref.at[layer, :, cols_of(c)] if j == 0 else gd_ref.at[z, :, cols_of(c)]
            out = wo_ref.at[layer, 0, :, cols_of(c)] if j == 0 else go_ref.at[z, :, cols_of(c)]
            copies.append(pltpu.make_async_copy(down, wtile.at[c % 2, j, pl.ds(0, ff_local), :], w_sem.at[c % 2, j, 0]))
            copies.append(pltpu.make_async_copy(out, wtile.at[c % 2, j, pl.ds(ff_local, wo_ref.shape[2]), :], w_sem.at[c % 2, j, 1]))
        return copies

    for copy in w_loads(0):
        copy.start()
    x_load = pltpu.make_async_copy(rest_ref, xres, x_sem)
    x_load.start()

    def y_device(d):
        return pos_z * RING + (pos_y + sign[d] + RING) % RING

    def z_device(d):
        return (pos_z + sign[d] + RING) % RING * RING + pos_y

    barrier = pltpu.get_barrier_semaphore()
    for device in (y_device, z_device):
        for d in range(DIRS):
            pl.semaphore_signal(barrier, inc=1, device_id={'head': device(d)}, device_id_type=pl.DeviceIdType.MESH)
    pl.semaphore_wait(barrier, 2 * DIRS)
    x_load.wait()

    def rows_of(piece, offset, count):
        return pl.ds(pl.multiple_of(piece * quarter + offset, eighth), count)

    def message(step, c, d, z_first):
        s = sign[d]
        near, behind = (pos_y + s + RING) % RING, (pos_y - s + RING) % RING
        if step == 0:
            src, dst = part.at[rows_of((pos_y + 2) % RING, d * eighth, eighth), cols_of(c)], landed.at[c, d, pl.ds(quarter, eighth), :]
        elif step == 1:
            src, dst = part.at[rows_of(near, 0, quarter), cols_of(c)], landed.at[c, d, pl.ds(0, quarter), :]
        elif z_first:
            back = (pos_z - s + RING) % RING
            if step == 2:
                src = dst = xbuf.at[pos_z, rows_of(pos_y, 0, quarter), cols_of(c)]
            elif step == 3:
                src = dst = xbuf.at[back, rows_of(pos_y, d * eighth, eighth), cols_of(c)]
            elif step == 4:
                src = dst = xbuf.at[:, rows_of(pos_y, 0, quarter), cols_of(c)]
            else:
                src = dst = xbuf.at[:, rows_of(behind, d * eighth, eighth), cols_of(c)]
        else:
            if step == 2:
                src = dst = xbuf.at[pos_z, rows_of(pos_y, 0, quarter), cols_of(c)]
            elif step == 3:
                src = dst = xbuf.at[pos_z, rows_of(behind, d * eighth, eighth), cols_of(c)]
            elif step == 4:
                src = dst = xbuf.at[pos_z, :, cols_of(c)]
            else:
                src = dst = xbuf.at[(pos_z - s + RING) % RING, pl.ds(d * (rows // 2), rows // 2), cols_of(c)]
        along_y = step < 2 or (step < 4) != z_first
        return pltpu.make_async_remote_copy(
            src_ref=src, dst_ref=dst, send_sem=send_sem.at[c, step, d], recv_sem=recv_sem.at[c, step, d],
            device_id={'head': (y_device if along_y else z_device)(d)}, device_id_type=pl.DeviceIdType.MESH)

    def on_messages(step, c, act):
        if step < 2:
            for d in range(DIRS):
                act(message(step, c, d, False))
            return

        @pl.when(c % 4 == 3)
        def _():
            for d in range(DIRS):
                act(message(step, c, d, True))

        @pl.when(c % 4 != 3)
        def _():
            for d in range(DIRS):
                act(message(step, c, d, False))

    def store(c):
        return pltpu.make_async_copy(xbuf.at[:, :, cols_of(c)], out_ref.at[:, :, cols_of(c)], store_sem.at[c])

    def project(c):
        @pl.when(c + 1 < block_count)
        def _():
            for copy in w_loads(c + 1):
                copy.start()

        for copy in w_loads(c):
            copy.wait()
        total = None
        for j in range(RING):
            z = (pos_z + j) % RING
            down = jnp.dot(hid_ref[z], wtile[c % 2, j, :ff_local, :], preferred_element_type=jnp.float32)
            down = down + jnp.dot(att_ref[z], wtile[c % 2, j, ff_local:, :], preferred_element_type=jnp.float32)
            total = down if total is None else total + down
        part[:, cols_of(c)] = total

    def stage(number, c):
        if number == 0:
            project(c)
        else:
            on_messages(number - 1, c, lambda copy: copy.wait_recv())
        if number == 1:
            for d in range(DIRS):
                piece = rows_of((pos_y + sign[d] + RING) % RING, d * eighth, eighth)
                part[piece, cols_of(c)] = part[piece, cols_of(c)] + landed[c, d, pl.ds(quarter, eighth), :]
        if number == 2:
            own = rows_of(pos_y, 0, quarter)
            total = part[own, cols_of(c)] + landed[c, 0, pl.ds(0, quarter), :] + landed[c, 1, pl.ds(0, quarter), :]
            update = total.astype(jnp.bfloat16).astype(jnp.float32)
            xbuf[pos_z, own, cols_of(c)] = (xres[:, cols_of(c)].astype(jnp.float32) + update).astype(jnp.bfloat16)
        if number < LAST_STEPS:
            on_messages(number, c, lambda copy: copy.start())
        else:
            store(c).start()

    def tick(t, carry):
        for number in range(LAST_STEPS, -1, -1):
            c = t - SKEW * number

            @pl.when(jnp.logical_and(c >= 0, c < block_count))
            def _():
                stage(number, c)
        return carry

    lax.fori_loop(0, block_count + SKEW * LAST_STEPS, tick, 0)

    def drain(c, carry):
        for step in range(LAST_STEPS):
            on_messages(step, c, lambda copy: copy.wait_send())
        store(c).wait()
        return carry

    lax.fori_loop(0, block_count, drain, 0)


def layer_last(layer, hid_all, att_all, rest, w_down, w_o, all_down, all_out):
    rows, d_model = hid_all.shape[1], rest.shape[1]
    tok_count = RING * rows
    depth = hid_all.shape[2] + att_all.shape[2]
    any_spec = pl.BlockSpec(memory_space=pl.ANY)
    vmem_spec = pl.BlockSpec(memory_space=pltpu.VMEM)
    blocks = d_model // LAST_COLS
    out = pl.pallas_call(
        functools.partial(last_kernel, layer),
        out_shape=jax.ShapeDtypeStruct((RING, rows, d_model), jnp.bfloat16),
        in_specs=[vmem_spec, vmem_spec] + [any_spec] * 5,
        out_specs=any_spec,
        scratch_shapes=[
            pltpu.VMEM((rows, d_model), jnp.float32),
            pltpu.VMEM((rows // RING, d_model), jnp.bfloat16),
            pltpu.VMEM((RING, rows, d_model), jnp.bfloat16),
            pltpu.VMEM((2, RING, depth, LAST_COLS), jnp.bfloat16),
            pltpu.VMEM((blocks, DIRS, 3 * rows // (2 * RING), LAST_COLS), jnp.float32),
            pltpu.SemaphoreType.DMA((2, RING, 2)),
            pltpu.SemaphoreType.DMA,
            pltpu.SemaphoreType.DMA((blocks,)),
            pltpu.SemaphoreType.DMA((blocks, LAST_STEPS, DIRS)),
            pltpu.SemaphoreType.DMA((blocks, LAST_STEPS, DIRS)),
        ],
        compiler_params=pltpu.CompilerParams(collective_id=layer, has_side_effects=True, vmem_limit_bytes=63 * 1024 * 1024),
        cost_estimate=pl.CostEstimate(flops=2 * tok_count * depth * d_model, bytes_accessed=4 * depth * d_model * 2, transcendentals=0),
        name='last',
    )(hid_all, att_all, rest, w_down, w_o, all_down, all_out)
    return out.reshape(tok_count, d_model)


EMIT_PARTS = 8


def emit_kernel(x_ref, k_first, k_second, v_first, v_second, x_out, k_out, v_out, xbuf, rows, load_sem, store_sem):
    size = x_ref.shape[0] // EMIT_PARTS
    loads, stores = [], []
    for n in range(EMIT_PARTS):
        part = pl.ds(n * size, size)
        loads.append(pltpu.make_async_copy(x_ref.at[part, :], xbuf.at[part, :], load_sem.at[n]))
        stores.append(pltpu.make_async_copy(xbuf.at[part, :], x_out.at[part, :], store_sem.at[n]))
    for n, (ref, out) in enumerate(((k_first, k_out.at[0]), (k_second, k_out.at[1]), (v_first, v_out.at[0]), (v_second, v_out.at[1]))):
        loads.append(pltpu.make_async_copy(ref, rows.at[n], load_sem.at[EMIT_PARTS + n]))
        stores.append(pltpu.make_async_copy(rows.at[n], out, store_sem.at[EMIT_PARTS + n]))
    for copy in loads:
        copy.start()
    for load, store in zip(loads, stores):
        load.wait()
        store.start()
    for copy in stores:
        copy.wait()


def emit(x_out, k_first, k_second, v_first, v_second):
    any_spec = pl.BlockSpec(memory_space=pl.ANY)
    cache = jax.ShapeDtypeStruct((2,) + k_first.shape, jnp.bfloat16)
    return pl.pallas_call(
        emit_kernel,
        out_shape=[jax.ShapeDtypeStruct(x_out.shape, jnp.bfloat16), cache, cache],
        in_specs=[any_spec] * 5,
        out_specs=[any_spec] * 3,
        scratch_shapes=[
            pltpu.VMEM(x_out.shape, jnp.bfloat16),
            pltpu.VMEM((4,) + k_first.shape, jnp.bfloat16),
            pltpu.SemaphoreType.DMA((EMIT_PARTS + 4,)),
            pltpu.SemaphoreType.DMA((EMIT_PARTS + 4,)),
        ],
        compiler_params=pltpu.CompilerParams(vmem_limit_bytes=63 * 1024 * 1024),
        name='emit',
    )(x_out, k_first, k_second, v_first, v_second)


def solution(mesh):
    row_spec = P(('batch', 'seq'), None)
    pos_spec = P(('batch', 'seq'))
    head_spec = P(None, None, 'head', None)
    out_proj_spec = P(None, 'head', None, None)
    col_spec = P(None, None, 'head')
    down_spec = P(None, 'head', None)
    cache_spec = P(None, ('batch', 'seq'), 'head', None)

    def local_forward(x_loc, pos_loc, w_q, w_k, w_v, w_o, w_gate, w_up, w_down, norm_gain):
        tok_count, d_model = x_loc.shape
        layer_count = w_q.shape[0]
        head_dim = w_q.shape[3]
        flat_q, flat_k, flat_v = (w.reshape(layer_count, d_model, head_dim) for w in (w_q, w_k, w_v))
        cos_t, sin_t = rope_tables(pos_loc, head_dim)
        hid_all, att_all, k_first, v_first, k_second, v_second, all_down, all_out, rest = front(x_loc, cos_t, sin_t, norm_gain, flat_q, flat_k, flat_v, w_gate, w_up, w_down, w_o)
        x_out = layer_last(1, hid_all, att_all, rest, w_down, w_o, all_down, all_out)
        x_out, k_all, v_all = emit(x_out, k_first, k_second, v_first, v_second)
        cache_shape = (layer_count, tok_count, 1, head_dim)
        return x_out, k_all.reshape(cache_shape), v_all.reshape(cache_shape)

    return jax.shard_map(local_forward, mesh=mesh, in_specs=(row_spec, pos_spec, head_spec, head_spec, head_spec, out_proj_spec, col_spec, col_spec, down_spec, P(None, None)), out_specs=(row_spec, cache_spec, cache_spec), check_vma=False)
```

```python
import functools
import math
import jax
import jax.numpy as jnp
from jax import lax
from jax.experimental import pallas as pl
from jax.experimental.pallas import tpu as pltpu
from jax.sharding import PartitionSpec as P

ROPE_BASE = 500000.0
EPS = 1e-5


def rope_tables(positions, head_dim):
    half_dim = head_dim // 2
    inv_freq = ROPE_BASE ** (-(jnp.arange(half_dim, dtype=jnp.float32) * 2.0 / head_dim))
    angles = positions.astype(jnp.float32)[..., None] * inv_freq
    return jnp.cos(angles), jnp.sin(angles)


CHIPS = 4
RING = 4
HALVES = 2
DIRS = 2
KV_CHUNKS = 4
W_TILE = 256
NORM_ROWS = 64
CHUNKS = 8
STEPS = 8
PART_SLOTS = 4
RECV_SLOTS = 5
DOWN_TILE = 512
START_GAP = 3
STAGE_GAP = 2
BLOCK_TICK = 19
BLOCK_GAP = 6
LAST_TICK = 43
NEAR_TICKS = ((9, 1), (15, 3))
FAR_TICKS = ((24, 1), (26, 3))
SERVE_TICKS = (27, 31, 35, 42)
GIVE_TICK = 37
OWN_TICK = 3
DONE_TICK = 11
EARLY_TICK = 31
LAST_STEPS = 6
LAST_COLS = 256
LAST_BLOCKS = 16
LAST_GAP = 3


def layers_kernel(x_ref, cos_ref, sin_ref, gain_ref, wq_ref, wk_ref, wv_ref, wg_ref, wu_ref, wd_ref, wo_ref,
                 out_ref, k1_ref, v1_ref, k2_ref, v2_ref, gd_ref, go_ref,
                 xbuf, part, recv_a, recv_b, hid, att, wdo, wtile, kv, qbuf, acc, row_max, row_sum, xs, xres,
                 x_sem, res_sem, w_sem, down_sem, cache_sem, store_sem, own_send, pass_send, ici_recv, core_recv, part_send, part_recv,
                 round_send, round_recv, side_send, side_recv, give_send, give_recv, relay_buf, relay_send, relay_recv, att_all, ring_send, ring_recv,
                 last_send, last_recv, tile_sem, ready_sem, drained_sem):
    tok_count, d_model = xbuf.shape
    head_dim = qbuf.shape[1]
    half_dim = head_dim // 2
    ff_local = hid.shape[1]
    rows_per = tok_count // KV_CHUNKS
    half_rows = tok_count // 2
    lanes = row_max.shape[2]
    chunk_rows = tok_count // CHUNKS
    quarter, eighth = chunk_rows // RING, chunk_rows // (2 * RING)
    half_cols = d_model // HALVES
    piece_cols = half_cols // RING
    bf16, f32 = jnp.bfloat16, jnp.float32
    sign = (1, -1)
    mesh_id = pl.DeviceIdType.MESH

    my_head = lax.axis_index('head')
    pos_z, pos_y = my_head // RING, my_head % RING
    my_seq = lax.axis_index('seq')
    chip, core = my_seq // 2, my_seq % 2
    other = chip * 2 + 1 - core

    def wrap(n):
        return (n + RING) % RING

    def y_peer(d):
        return pos_z * RING + wrap(pos_y + sign[d])

    def z_device(z):
        return wrap(z) * RING + pos_y

    def z_peer(d):
        return z_device(pos_z + sign[d])

    def x_device(n):
        return wrap(chip + n) * 2 + core

    right, left = x_device(1), x_device(-1)

    def span(start, size, unit=None):
        return pl.ds(pl.multiple_of(start, unit or size), size)

    def remote(src, dst, send, recv, **to):
        return pltpu.make_async_remote_copy(src_ref=src, dst_ref=dst, send_sem=send, recv_sem=recv, device_id=to, device_id_type=mesh_id)

    def x_load(i):
        return pltpu.make_async_copy(x_ref.at[span(i * rows_per, rows_per), :], xs.at[i % 2], x_sem.at[i % 2])

    def weights(layer, piece):
        slot = piece % 2
        if isinstance(piece, int) and piece < 2:
            refs = ((wk_ref, wv_ref), (wq_ref,))[piece]
            return [pltpu.make_async_copy(ref.at[layer], wtile.at[slot, n], w_sem.at[slot, n]) for n, ref in enumerate(refs)]
        cols = span((piece - 2) * W_TILE, W_TILE)
        return [pltpu.make_async_copy(ref.at[layer, :, cols], wtile.at[slot, n], w_sem.at[slot, n]) for n, ref in enumerate((wg_ref, wu_ref))]

    def start(copies):
        for copy in copies:
            copy.start()

    def wait(copies):
        for copy in copies:
            copy.wait()

    down_tiles = d_model // DOWN_TILE

    def down_load(i):
        cols = span(i * DOWN_TILE, DOWN_TILE)
        return [pltpu.make_async_copy(wd_ref.at[0, :, cols], wdo.at[i % 2, pl.ds(0, ff_local), :], down_sem.at[i % 2, 0]),
                pltpu.make_async_copy(wo_ref.at[0, 0, :, cols], wdo.at[i % 2, pl.ds(ff_local, head_dim), :], down_sem.at[i % 2, 1])]

    def kv_copy(origin_chip, origin_core, i, to, send, recv):
        rows = kv.at[span((origin_chip * 2 + origin_core) * tok_count + i * rows_per, rows_per), :]
        return remote(rows, rows, send, recv, seq=to)

    def kv_routes(layer, i):
        late = i >= KV_CHUNKS // 2
        early = jnp.logical_not(late) if not isinstance(i, int) else not late

        def to(send, recv, origin_chip, origin_core, device):
            return kv_copy(origin_chip, origin_core, i, device, send, recv)
        own, passed, ici, side = own_send.at[layer], pass_send.at[layer], ici_recv.at[layer], core_recv.at[layer]
        return {
            'right': (chip < CHIPS - 1, lambda: to(own.at[0, i], ici.at[0, i], chip, core, right)),
            'wrap': (chip == 0, lambda: to(own.at[1, i], ici.at[2, i], chip, core, left)),
            'relay': (jnp.logical_and(late, chip == 1), lambda: to(own.at[3, i], ici.at[3, i], chip, core, left)),
            'other': (core == 0, lambda: to(own.at[2, i], side.at[0, i], chip, core, other)),
            'on_right': (jnp.logical_and(early, jnp.logical_and(chip >= 1, chip < CHIPS - 1)), lambda: to(passed.at[0, i], ici.at[1, i], chip - 1, core, right)),
            'from_relay': (jnp.logical_and(late, chip == 0), lambda: to(passed.at[0, i], ici.at[1, i], 1, core, left)),
            'on_left': (jnp.logical_and(late, chip == CHIPS - 1), lambda: to(passed.at[0, i], ici.at[1, i], 0, core, left)),
            'side1': (chip >= 1, lambda: to(passed.at[1, i], side.at[1, i], chip - 1, core, other)),
            'side2': (chip >= 2, lambda: to(passed.at[2, i], side.at[2, i], chip - 2, core, other)),
            'side3': (chip >= 3, lambda: to(passed.at[3, i], side.at[3, i], chip - 3, core, other)),
        }

    def start_route(layer, i, name):
        condition, copy = kv_routes(layer, i)[name]

        @pl.when(condition)
        def _():
            copy().start()

    def send_kv(layer, i):
        for name in ('right', 'wrap', 'relay', 'other'):
            start_route(layer, i, name)

    def kv_sent(layer):
        for i in range(KV_CHUNKS):
            for condition, copy in kv_routes(layer, i).values():
                @pl.when(condition)
                def _():
                    copy().wait_send()

    def serve(layer, back, i):
        @pl.when(chip >= back)
        def _():
            kv_copy(chip - back, core, i, other, pass_send.at[layer, back, i], ici_recv.at[layer, back - 1, i]).wait_recv()
        start_route(layer, i, 'side%d' % back)
        if back == 1:
            start_route(layer, i, 'on_right')
        if back == 3:
            start_route(layer, i, 'on_left')

    def relay(layer, i):
        condition, copy = kv_routes(layer, i)['from_relay']

        @pl.when(condition)
        def _():
            kv_copy(1, core, i, left, pass_send.at[layer, 0, i], ici_recv.at[layer, 3, i]).wait_recv()
            copy().start()

    def serve_all(layer, i):
        serve(layer, 1, i)
        serve(layer, 3, i)
        relay(layer, i)

    def taken(layer, back, chunks):
        for i in chunks:
            kv_copy(chip - back, 1 - core, i, other, pass_send.at[layer, 0, i], core_recv.at[layer, back, i]).wait_recv()

    def z_parts(step, d):
        copies = []
        for n, (own_ref, all_ref) in enumerate(((wd_ref, gd_ref), (wo_ref, go_ref))):
            size = all_ref.shape[1] // (2 * CHIPS)
            if step == 0:
                rows = span(my_seq * size, size)
                src = own_ref.at[1, rows, :] if n == 0 else own_ref.at[1, 0, rows, :]
                dst = all_ref.at[pos_z, rows, :]
            else:
                rows = span(my_seq * size + d * (size // 2), size // 2)
                src = dst = all_ref.at[wrap(pos_z - sign[d]), rows, :]
            copies.append(remote(src, dst, part_send.at[step, d, n], part_recv.at[step, d, n], head=z_peer(d)))
        return copies

    def part_copies(j, part_chip, part_core, half, send, recv, to):
        copies = []
        for n, ref in enumerate((gd_ref, go_ref)):
            size = ref.shape[1] // (2 * CHIPS)
            first = (part_chip * 2 + part_core) * size
            rows = span(first, size) if half is None else span(first + half * (size // 2), size // 2)
            place = ref.at[wrap(pos_z + j), rows, :]
            copies.append(remote(place, place, send.at[n], recv.at[n], seq=to))
        return copies

    def own_part(j, d):
        return part_copies(j, chip, core, None, round_send.at[0, j - 1, d], round_recv.at[0, j - 1, d], x_device(sign[d]))

    def far_part(j, d):
        return part_copies(j, wrap(chip - sign[d]), core, d, round_send.at[1, j - 1, d], round_recv.at[1, j - 1, d], x_device(sign[d]))

    def side_part(j, n, side):
        return part_copies(j, wrap(chip + n), side, None, side_send.at[j - 1, n], side_recv.at[j - 1, n], other)

    def round_start(j):
        for d in range(DIRS):
            start(own_part(j, d))
        start(side_part(j, 0, core))

    def near_parts(j):
        for d in range(DIRS):
            for copy in own_part(j, d):
                copy.wait_recv()
            start(far_part(j, d) + side_part(j, 3 if d == 0 else 1, core))

    def far_parts(j):
        for d in range(DIRS):
            for copy in far_part(j, d):
                copy.wait_recv()
        start(side_part(j, 2, core))

    def give_hidden(z, i, source):
        cols = span(i * W_TILE, W_TILE)
        return remote(hid.at[span(z * rows_per, rows_per), cols], hidden_place(source, i), give_send.at[z, i], give_recv.at[source, i], head=z_device(z))

    def hidden_place(source, i):
        return xs.at[1, :, span(source * ff_local + i * W_TILE, W_TILE)]

    def via_neighbor(z, i):
        step = jnp.where(i < KV_CHUNKS // 2, 1, -1)
        return remote(hid.at[span(z * rows_per, rows_per), span(i * W_TILE, W_TILE)], relay_buf.at[i], give_send.at[z, i], relay_recv.at[i], head=z_device(pos_z + step))

    def relay_hidden(i):
        step = 1 if i < KV_CHUNKS // 2 else -1
        source = wrap(pos_z - step)
        return remote(relay_buf.at[i], hidden_place(source, i), relay_send.at[i], give_recv.at[source, i], head=z_device(pos_z + step))

    def send_hidden(z, i):
        away = wrap(z - pos_z)

        @pl.when(away == 2)
        def _():
            via_neighbor(z, i).start()

        @pl.when(away % 2 == 1)
        def _():
            give_hidden(z, i, pos_z).start()

    def give_rows(z, source):
        return remote(att.at[span(z * rows_per, rows_per), :], att_all.at[source], give_send.at[z, KV_CHUNKS], give_recv.at[source, KV_CHUNKS], head=z_device(z))

    def norm_rows(x_few, layer):
        x_f32 = x_few.astype(f32)
        inv_rms = lax.rsqrt(jnp.mean(x_f32 * x_f32, axis=-1, keepdims=True) + EPS)
        return (x_f32 * inv_rms * gain_ref[pl.ds(layer, 1), :].astype(f32)).astype(bf16)

    def rope(values, rows):
        cos_t, sin_t = cos_ref[rows, :], sin_ref[rows, :]
        wide = values.astype(bf16).astype(f32)
        first, second = wide[:, :half_dim], wide[:, half_dim:]
        return jnp.concatenate([first * cos_t - second * sin_t, second * cos_t + first * sin_t], axis=1).astype(bf16)

    def dot(a, b):
        return jnp.dot(a, b, preferred_element_type=f32)

    scale = 1.0 / math.sqrt(head_dim)

    def keys_values(normed, i):
        rows = span(i * rows_per, rows_per)
        own = span(my_seq * tok_count + i * rows_per, rows_per)
        kv[own, :head_dim] = rope(dot(normed, wtile[0, 0]), rows)
        kv[own, head_dim:] = dot(normed, wtile[0, 1]).astype(bf16)

    def queries(normed, i):
        rows = span(i * rows_per, rows_per)
        qbuf[rows, :] = (rope(dot(normed, wtile[1, 0]), rows).astype(f32) * scale).astype(bf16)

    def gated(normed, i, tile):
        gate = dot(normed, wtile[tile % 2, 0])
        up = dot(normed, wtile[tile % 2, 1])
        hid[span(i * rows_per, rows_per), span(tile * W_TILE, W_TILE)] = (gate * jax.nn.sigmoid(gate) * up).astype(bf16)

    def attend(key_start, q_half, side, masked, first):
        rows = pl.ds(q_half * half_rows, half_rows)
        some = span(key_start, half_rows)
        logits = lax.dot_general(qbuf[rows, :], kv[some, :head_dim], (((1,), (1,)), ((), ())), preferred_element_type=f32)
        if masked:
            seen = lax.broadcasted_iota(jnp.int32, logits.shape, 0) >= lax.broadcasted_iota(jnp.int32, logits.shape, 1)
            logits = jnp.where(seen, logits, -jnp.inf)
        block_max = jnp.max(logits, axis=-1, keepdims=True)
        if first:
            new_max = jnp.broadcast_to(block_max, (half_rows, lanes))
        else:
            new_max = jnp.maximum(row_max[side, rows, :], block_max)
        prob = jnp.exp(logits - jnp.concatenate([new_max] * (half_rows // lanes), axis=1))
        block_sum = jnp.sum(prob, axis=-1, keepdims=True)
        block_out = dot(prob.astype(bf16), kv[some, head_dim:])
        if first:
            row_sum[side, rows, :] = jnp.broadcast_to(block_sum, (half_rows, lanes))
            acc[side, rows, :] = block_out
        else:
            rescale = jnp.exp(row_max[side, rows, :] - new_max)
            row_sum[side, rows, :] = row_sum[side, rows, :] * rescale + block_sum
            acc[side, rows, :] = acc[side, rows, :] * jnp.concatenate([rescale] * (head_dim // lanes), axis=1) + block_out
        row_max[side, rows, :] = new_max

    def attend_own(layer_half):
        own_start = my_seq * tok_count
        if layer_half == 0:
            attend(own_start, 0, 0, True, True)
            top_rows = pl.ds(0, half_rows)
            row_max[1, top_rows, :] = jnp.full((half_rows, lanes), -jnp.inf, f32)
            row_sum[1, top_rows, :] = jnp.zeros((half_rows, lanes), f32)
            acc[1, top_rows, :] = jnp.zeros((half_rows, head_dim), f32)
        else:
            attend(own_start, 1, 0, False, True)
            attend(own_start + half_rows, 1, 1, True, True)

    def past_start(n):
        later = n - core
        back = jnp.where(later < 2, 1, jnp.where(chip == CHIPS - 1, jnp.where(later < 4, 3, 2), 2))
        block = (chip - back) * 2 + jnp.where(later % 2 == 0, core, 1 - core)
        return jnp.where(jnp.logical_and(core == 1, n == 0), chip * 2, block) * tok_count

    def arrivals(layer, n, chunks):
        @pl.when(jnp.logical_and(core == 1, n == 0))
        def _():
            taken(layer, 0, chunks)

        for back in (1, 3, 2):
            place = 0 if back == 1 else 2 if back == 3 else jnp.where(chip == CHIPS - 1, 4, 2)
            if back == 2:
                @pl.when(jnp.logical_and(chip >= back, n == core + place))
                def _():
                    for i in chunks:
                        serve(layer, 2, i)

            @pl.when(jnp.logical_and(chip >= back, n == core + place + 1))
            def _():
                taken(layer, back, chunks)

    def visit(n, visits):
        for q_half, side in visits:
            attend(past_start(n) + side * half_rows, q_half, side, False, False)

    def attend_past(layer, first_n, last_n, chunks, visits):
        def past(n, carry):
            if chunks:
                arrivals(layer, n, chunks)
            visit(n, visits)
            return carry

        lax.fori_loop(first_n, last_n, past, 0)

    near_count = my_seq - jnp.where(chip >= 2, 2, 0)

    def finish(i, spread):
        rows = pl.ds(i * rows_per, rows_per)
        top = jnp.maximum(row_max[0, rows, :], row_max[1, rows, :])
        shares = [jnp.exp(row_max[side, rows, :] - top) for side in range(2)]
        total = shares[0] * row_sum[0, rows, :] + shares[1] * row_sum[1, rows, :]
        wide = [jnp.concatenate([w] * (head_dim // lanes), axis=1) for w in shares + [total]]
        att[rows, :] = ((acc[0, rows, :] * wide[0] + acc[1, rows, :] * wide[1]) / wide[2]).astype(bf16)
        if spread:
            @pl.when(i != pos_z)
            def _():
                give_rows(i, pos_z).start()

    first_pos, second_pos = (pos_y, pos_z), (pos_z, pos_y)
    first_peer, second_peer = (y_peer, z_peer), (z_peer, y_peer)

    def part_rows(chunk, piece, offset, count):
        return span((chunk % PART_SLOTS) * chunk_rows + piece * quarter + offset, count, eighth)

    def x_rows(chunk, piece, offset, count):
        return span(chunk * chunk_rows + piece * quarter + offset, count, eighth)

    def cols_of(h, piece):
        return span(h * half_cols + piece * piece_cols, piece_cols)

    def half_of(h):
        return pl.ds(h * half_cols, half_cols)

    def message(step, chunk, h, d):
        p1, p2, s = first_pos[h], second_pos[h], sign[d]
        slot = chunk % RECV_SLOTS
        if step == 0:
            src, dst = part.at[part_rows(chunk, wrap(p1 + 2), d * eighth, eighth), half_of(h)], recv_a.at[slot, h, d, pl.ds(quarter, eighth), :]
        elif step == 1:
            src, dst = part.at[part_rows(chunk, wrap(p1 + s), 0, quarter), half_of(h)], recv_a.at[slot, h, d, pl.ds(0, quarter), :]
        elif step == 2:
            src, dst = part.at[part_rows(chunk, p1, d * eighth, eighth), cols_of(h, wrap(p2 + 2))], recv_b.at[slot, h, d, pl.ds(quarter, eighth), :]
        elif step == 3:
            src, dst = part.at[part_rows(chunk, p1, 0, quarter), cols_of(h, wrap(p2 + s))], recv_b.at[slot, h, d, pl.ds(0, quarter), :]
        elif step == 4:
            src = dst = xbuf.at[x_rows(chunk, p1, 0, quarter), cols_of(h, p2)]
        elif step == 5:
            src = dst = xbuf.at[x_rows(chunk, p1, d * eighth, eighth), cols_of(h, wrap(p2 - s))]
        elif step == 6:
            src = dst = xbuf.at[x_rows(chunk, p1, 0, quarter), half_of(h)]
        else:
            src = dst = xbuf.at[x_rows(chunk, wrap(p1 - s), d * eighth, eighth), half_of(h)]
        peer = (first_peer if step in (0, 1, 6, 7) else second_peer)[h](d)
        return remote(src, dst, ring_send.at[chunk, step, h * DIRS + d], ring_recv.at[chunk, step, h * DIRS + d], head=peer)

    def each_message(chunk, steps, act):
        for step in steps:
            for h in range(HALVES):
                for d in range(DIRS):
                    act(message(step, chunk, h, d))

    def residual_load(chunk, h):
        return pltpu.make_async_copy(x_ref.at[x_rows(chunk, first_pos[h], 0, quarter), cols_of(h, second_pos[h])], xres.at[chunk, h], res_sem.at[chunk, h])

    def project(chunk):
        rows = span(chunk * chunk_rows, chunk_rows)
        slot_rows = span((chunk % PART_SLOTS) * chunk_rows, chunk_rows)

        def one_tile(i, carry):
            @pl.when(jnp.logical_or(chunk < CHUNKS - 1, i < down_tiles - 1))
            def _():
                start(down_load((i + 1) % down_tiles))

            wait(down_load(i))
            total = dot(hid[rows, :], wdo[i % 2, :ff_local, :])
            part[slot_rows, span(i * DOWN_TILE, DOWN_TILE)] = total + dot(att[rows, :], wdo[i % 2, ff_local:, :])
            return carry

        lax.fori_loop(0, down_tiles, one_tile, 0)

    def stage(number, chunk):
        slot = chunk % RECV_SLOTS
        if number == 0:
            @pl.when(chunk >= PART_SLOTS)
            def _():
                each_message(chunk - PART_SLOTS, range(4), lambda copy: copy.wait_send())
            project(chunk)
        for h in range(HALVES):
            p1, p2 = first_pos[h], second_pos[h]
            if number:
                for d in range(DIRS):
                    message(number - 1, chunk, h, d).wait_recv()
            if number in (1, 3):
                for d in range(DIRS):
                    if number == 1:
                        rows, cols, arrived = part_rows(chunk, wrap(p1 + sign[d]), d * eighth, eighth), half_of(h), recv_a
                    else:
                        rows, cols, arrived = part_rows(chunk, p1, d * eighth, eighth), cols_of(h, wrap(p2 + sign[d])), recv_b
                    part[rows, cols] = part[rows, cols] + arrived[slot, h, d, pl.ds(quarter, eighth), :]
            if number == 2:
                rows = part_rows(chunk, p1, 0, quarter)
                part[rows, half_of(h)] = part[rows, half_of(h)] + recv_a[slot, h, 0, pl.ds(0, quarter), :] + recv_a[slot, h, 1, pl.ds(0, quarter), :]
            if number == 4:
                residual_load(chunk, h).wait()
                rows, cols = part_rows(chunk, p1, 0, quarter), cols_of(h, p2)
                total = part[rows, cols] + recv_b[slot, h, 0, pl.ds(0, quarter), :] + recv_b[slot, h, 1, pl.ds(0, quarter), :]
                update = total.astype(bf16).astype(f32)
                xbuf[x_rows(chunk, p1, 0, quarter), cols] = (xres[chunk, h].astype(f32) + update).astype(bf16)
            if number < STEPS:
                for d in range(DIRS):
                    message(number, chunk, h, d).start()

    x_load(0).start()
    start(weights(0, 0))
    x_load(1).start()
    start(weights(0, 1))
    barrier = pltpu.get_barrier_semaphore()
    for peer in (left, right, other):
        pl.semaphore_signal(barrier, inc=1, device_id={'seq': peer}, device_id_type=mesh_id)
    for peer in [z_device(pos_z + j) for j in range(1, RING)] + [y_peer(d) for d in range(DIRS)]:
        pl.semaphore_signal(barrier, inc=1, device_id={'head': peer}, device_id_type=mesh_id)

    def prepare(i, carry):
        x_load(i).wait()

        def few(n, inner):
            xbuf[span(i * rows_per + n * NORM_ROWS, NORM_ROWS), :] = norm_rows(xs[i % 2, span(n * NORM_ROWS, NORM_ROWS), :], 0)
            return inner

        lax.fori_loop(0, rows_per // NORM_ROWS, few, 0)

        @pl.when(i + 2 < KV_CHUNKS)
        def _():
            x_load(i + 2).start()

        @pl.when(i == 0)
        def _():
            wait(weights(0, 0))

        keys_values(xbuf[span(i * rows_per, rows_per), :], i)

        @pl.when(i == 0)
        def _():
            pl.semaphore_wait(barrier, 8)

        send_kv(0, i)

        @pl.when(i == 0)
        def _():
            for d in range(DIRS):
                start(z_parts(0, d))
        return carry

    lax.fori_loop(0, KV_CHUNKS, prepare, 0)
    start(weights(0, 2))
    own_rows = span(my_seq * tok_count, tok_count)

    def cache_stores(layer):
        k_ref, v_ref = ((k1_ref, v1_ref), (k2_ref, v2_ref))[layer]
        return [pltpu.make_async_copy(kv.at[own_rows, pl.ds(0, head_dim)], k_ref, cache_sem.at[layer, 0]),
                pltpu.make_async_copy(kv.at[own_rows, pl.ds(head_dim, head_dim)], v_ref, cache_sem.at[layer, 1])]

    start(cache_stores(0))
    wait(weights(0, 1))

    def query(i, carry):
        queries(xbuf[span(i * rows_per, rows_per), :], i)
        return carry

    lax.fori_loop(0, KV_CHUNKS, query, 0)
    start(weights(0, 3))
    start(down_load(0))

    def residuals(n, carry):
        for h in range(HALVES):
            residual_load(n, h).start()
        return carry

    lax.fori_loop(0, CHUNKS, residuals, 0)

    def gate_half(half, tile):
        wait(weights(0, tile + 2))

        def rows_step(i, inner):
            gated(xbuf[span(i * rows_per, rows_per), :], i, tile)
            return inner

        lax.fori_loop(half * KV_CHUNKS // 2, (half + 1) * KV_CHUNKS // 2, rows_step, 0)

        @pl.when(tile < 2)
        def _():
            start(weights(0, tile + 4))

        for last in (2, 3):
            @pl.when(tile == last)
            def _():
                start(weights(1, last - 2) if half else weights(0, last))

    def first_half(tile, carry):
        gate_half(0, tile)

        @pl.when(tile < 3)
        def _():
            serve_all(0, tile)
        return carry

    def second_half(tile, carry):
        gate_half(1, tile)

        @pl.when(tile == 0)
        def _():
            serve_all(0, 3)
            attend_past(0, 0, near_count, range(KV_CHUNKS), ((0, 0), (0, 1)))
            for d in range(DIRS):
                for copy in z_parts(0, d):
                    copy.wait_recv()
                start(z_parts(1, d))
        return carry

    lax.fori_loop(0, ff_local // W_TILE, first_half, 0)
    attend_own(0)
    lax.fori_loop(0, 2, second_half, 0)
    attend_past(0, near_count, my_seq, range(KV_CHUNKS), ((0, 0), (0, 1)))
    finish(0, False)
    finish(1, False)
    round_start(1)
    round_start(3)

    def block_work(j, phase):
        @pl.when(phase == 0)
        def _():
            @pl.when(j == 0)
            def _():
                for n in range(3):
                    pl.semaphore_wait(ready_sem.at[n], 1)

            def few(n, inner):
                xs[0, span(n * NORM_ROWS, NORM_ROWS), :] = norm_rows(xbuf[span(j * rows_per + n * NORM_ROWS, NORM_ROWS), :], 1)
                return inner

            lax.fori_loop(0, rows_per // NORM_ROWS, few, 0)
            wait(weights(1, 0))
            keys_values(xs[0], j)
            send_kv(1, j)
            start(weights(1, 2))

        @pl.when(phase == 1)
        def _():
            wait(weights(1, 1))
            queries(xs[0], j)
            start(weights(1, 3))

        @pl.when(jnp.logical_and(phase >= 1, phase <= 4))
        def _():
            tile = phase - 1
            wait(weights(1, tile + 2))
            gated(xs[0], j, tile)

            @pl.when(tile < 2)
            def _():
                start(weights(1, tile + 4))

            @pl.when(jnp.logical_and(tile == 2, j < KV_CHUNKS - 1))
            def _():
                start(weights(1, 0))

            @pl.when(jnp.logical_and(tile == 3, j < KV_CHUNKS - 1))
            def _():
                start(weights(1, 1))

            @pl.when(j == KV_CHUNKS - 1)
            def _():
                send_hidden(j, tile)

    def tick(t, carry):
        for number in range(STEPS, -1, -1):
            place = t - STAGE_GAP * number
            chunk = place // START_GAP

            @pl.when(jnp.logical_and(place >= 0, jnp.logical_and(place % START_GAP == 0, chunk < CHUNKS)))
            def _():
                stage(number, chunk)

        @pl.when(jnp.logical_or(t == 1, t == 3))
        def _():
            gate_half(1, 2 + t // 2)

        @pl.when(t == OWN_TICK)
        def _():
            attend_own(1)

        @pl.when(jnp.logical_and(t > OWN_TICK, jnp.logical_and(t < DONE_TICK, t - OWN_TICK <= my_seq)))
        def _():
            visit(t - OWN_TICK - 1, ((1, 0), (1, 1)))

        @pl.when(t == EARLY_TICK)
        def _():
            attend_own(0)

        early = t - EARLY_TICK - 1

        @pl.when(jnp.logical_and(early >= 0, jnp.logical_and(early < 7, early < my_seq)))
        def _():
            arrivals(1, early, (0, 1))
            visit(early, ((0, 0),))

        @pl.when(t == 2)
        def _():
            for d in range(DIRS):
                for copy in z_parts(1, d):
                    copy.wait_recv()
            round_start(2)

        @pl.when(t == DONE_TICK)
        def _():
            finish(2, False)
            finish(3, False)
            kv_sent(0)
            wait(cache_stores(0))
            for n, peer in enumerate((left, right, other)):
                pl.semaphore_signal(ready_sem.at[n], inc=1, device_id={'seq': peer}, device_id_type=mesh_id)

        for when, j in NEAR_TICKS:
            @pl.when(t == when)
            def _():
                near_parts(j)

        for when, j in FAR_TICKS:
            @pl.when(t == when)
            def _():
                far_parts(j)

        @pl.when(t == GIVE_TICK)
        def _():
            for i in range(KV_CHUNKS):
                for z in range(KV_CHUNKS - 1):
                    send_hidden(z, i)

        late = t - BLOCK_TICK

        @pl.when(late >= 0)
        def _():
            block_work(late // BLOCK_GAP, late % BLOCK_GAP)

        for i, when in enumerate(SERVE_TICKS):
            @pl.when(t == when)
            def _():
                serve_all(1, i)
        return carry

    lax.fori_loop(0, LAST_TICK, tick, 0)

    def drain(chunk, carry):
        @pl.when(chunk >= CHUNKS - PART_SLOTS)
        def _():
            each_message(chunk, range(4), lambda copy: copy.wait_send())
        each_message(chunk, range(4, STEPS), lambda copy: copy.wait_send())
        return carry

    lax.fori_loop(0, CHUNKS, drain, 0)
    for d in range(DIRS):
        pl.semaphore_signal(drained_sem.at[d], inc=1, device_id={'head': y_peer(d)}, device_id_type=mesh_id)
    start(cache_stores(1))
    near_parts(2)
    attend_own(1)
    attend_past(1, 0, my_seq, (), ((1, 0),))
    for i in range(KV_CHUNKS):
        via_neighbor(0, i).wait_recv()
        relay_hidden(i).start()
    attend_past(1, 0, near_count, (2, 3), ((0, 1), (1, 1)))
    attend_past(1, near_count, my_seq, (2, 3), ((0, 1),))
    finish(0, True)
    finish(1, True)
    attend_past(1, near_count, my_seq, (), ((1, 1),))
    finish(2, True)
    finish(3, True)
    far_parts(2)
    for j in range(1, RING):
        for n in range(CHIPS):
            for copy in side_part(j, n, 1 - core):
                copy.wait_recv()

    quarter_rows = rows_per // RING
    depth = ff_local + head_dim

    def block_cols(c):
        return span(c * LAST_COLS, LAST_COLS)

    def tile_place(c, j, first, size):
        return wtile.at[c % 2, j // 2, pl.ds((j % 2) * depth + first, size), :]

    def tile_loads(c):
        copies = []
        for j in range(RING):
            z = wrap(pos_z + j)
            down = wd_ref.at[1, :, block_cols(c)] if j == 0 else gd_ref.at[z, :, block_cols(c)]
            out = wo_ref.at[1, 0, :, block_cols(c)] if j == 0 else go_ref.at[z, :, block_cols(c)]
            copies.append(pltpu.make_async_copy(down, tile_place(c, j, 0, ff_local), tile_sem.at[c % 2, j, 0]))
            copies.append(pltpu.make_async_copy(out, tile_place(c, j, ff_local, head_dim), tile_sem.at[c % 2, j, 1]))
        return copies

    start(tile_loads(0))
    for j in range(1, RING):
        z = wrap(pos_z + j)
        for i in range(KV_CHUNKS):
            give_hidden(z, i, z).wait_recv()
        give_rows(z, z).wait_recv()
    for d in range(DIRS):
        pl.semaphore_wait(drained_sem.at[d], 1)

    def quarter_of(piece, offset, size):
        return span(piece * quarter_rows + offset, size, quarter_rows // 2)

    def landed(d, first, size):
        return pl.ds(rows_per + d * (3 * quarter_rows // 2) + first, size)

    def rows_at(z, piece, offset, size):
        return span(z * rows_per + piece * quarter_rows + offset, size, quarter_rows // 2)

    def last_messages(step, c, d, z_first):
        s, cols, half = sign[d], block_cols(c), quarter_rows // 2
        near, behind, back = wrap(pos_y + s), wrap(pos_y - s), wrap(pos_z - s)
        along_y = step < 2 or (step < 4) != z_first
        if step == 0:
            pairs = [(part.at[quarter_of(wrap(pos_y + 2), d * half, half), cols], part.at[landed(d, quarter_rows, half), cols])]
        elif step == 1:
            pairs = [(part.at[quarter_of(near, 0, quarter_rows), cols], part.at[landed(d, 0, quarter_rows), cols])]
        else:
            if step == 2:
                rows = [rows_at(pos_z, pos_y, 0, quarter_rows)]
            elif step == 3:
                rows = [rows_at(back, pos_y, d * half, half) if z_first else rows_at(pos_z, behind, d * half, half)]
            elif step == 4:
                rows = [rows_at(z, pos_y, 0, quarter_rows) for z in range(RING)] if z_first else [rows_at(pos_z, 0, 0, rows_per)]
            else:
                rows = [rows_at(z, behind, d * half, half) for z in range(RING)] if z_first else [rows_at(back, 0, d * (rows_per // 2), rows_per // 2)]
            pairs = [(xbuf.at[r, cols], xbuf.at[r, cols]) for r in rows]
        to = (y_peer if along_y else z_peer)(d)
        return [remote(src, dst, last_send.at[c, step, d, n], last_recv.at[c, step, d, n], head=to) for n, (src, dst) in enumerate(pairs)]

    def on_last(step, c, act):
        def both(z_first):
            for d in range(DIRS):
                for copy in last_messages(step, c, d, z_first):
                    act(copy)

        if step < 2:
            both(False)
            return
        z_first = jnp.logical_and(c >= 5, c % 2 == 1)

        @pl.when(z_first)
        def _():
            both(True)

        @pl.when(jnp.logical_not(z_first))
        def _():
            both(False)

    def out_store(c):
        return pltpu.make_async_copy(xbuf.at[:, block_cols(c)], out_ref.at[:, block_cols(c)], store_sem.at[c])

    def last_project(c):
        @pl.when(c + 1 < LAST_BLOCKS)
        def _():
            start(tile_loads(c + 1))

        wait(tile_loads(c))
        total = None
        for j in range(RING):
            z = wrap(pos_z + j)
            own = span(pos_z * rows_per, rows_per)
            hidden_rows = hid[own, :] if j == 0 else xs[1, :, span(z * ff_local, ff_local)]
            out_rows = att[own, :] if j == 0 else att_all[z]
            term = dot(hidden_rows, wtile[c % 2, j // 2, pl.ds((j % 2) * depth, ff_local), :])
            term = term + dot(out_rows, wtile[c % 2, j // 2, pl.ds((j % 2) * depth + ff_local, head_dim), :])
            total = term if total is None else total + term
        part[pl.ds(0, rows_per), block_cols(c)] = total

    def last_stage(number, c):
        cols, half = block_cols(c), quarter_rows // 2
        if number == 0:
            last_project(c)
        else:
            on_last(number - 1, c, lambda copy: copy.wait_recv())
        if number == 1:
            for d in range(DIRS):
                piece = quarter_of(wrap(pos_y + sign[d]), d * half, half)
                part[piece, cols] = part[piece, cols] + part[landed(d, quarter_rows, half), cols]
        if number == 2:
            own = quarter_of(pos_y, 0, quarter_rows)
            total = part[own, cols] + part[landed(0, 0, quarter_rows), cols] + part[landed(1, 0, quarter_rows), cols]
            update = total.astype(bf16).astype(f32)
            rows = rows_at(pos_z, pos_y, 0, quarter_rows)
            xbuf[rows, cols] = (xbuf[rows, cols].astype(f32) + update).astype(bf16)
        if number < LAST_STEPS:
            on_last(number, c, lambda copy: copy.start())
        else:
            out_store(c).start()

    def last_tick(t, carry):
        for number in range(LAST_STEPS, -1, -1):
            c = t - LAST_GAP * number

            @pl.when(jnp.logical_and(c >= 0, c < LAST_BLOCKS))
            def _():
                last_stage(number, c)
        return carry

    lax.fori_loop(0, LAST_BLOCKS + LAST_GAP * LAST_STEPS, last_tick, 0)

    wait(cache_stores(1))
    for i in range(KV_CHUNKS):
        relay_hidden(i).wait_send()
    kv_sent(1)
    for d in range(DIRS):
        for step in range(2):
            for copy in z_parts(step, d):
                copy.wait_send()
    for j in range(1, RING):
        for d in range(DIRS):
            for copy in own_part(j, d) + far_part(j, d):
                copy.wait_send()
        for n in range(CHIPS):
            for copy in side_part(j, n, core):
                copy.wait_send()
        z = wrap(pos_z + j)
        for i in range(KV_CHUNKS):
            give_hidden(z, i, pos_z).wait_send()
        give_rows(z, pos_z).wait_send()

    def last_drain(c, carry):
        for step in range(LAST_STEPS):
            on_last(step, c, lambda copy: copy.wait_send())
        out_store(c).wait()
        return carry

    lax.fori_loop(0, LAST_BLOCKS, last_drain, 0)


def layers(x_loc, cos_t, sin_t, norm_gain, w_q, w_k, w_v, w_gate, w_up, w_down, w_o):
    tok_count, d_model = x_loc.shape
    head_dim = w_q.shape[2]
    ff_local = w_gate.shape[2]
    rows_per = tok_count // KV_CHUNKS
    chunk_rows = tok_count // CHUNKS
    landed = 3 * chunk_rows // (2 * RING)
    half_cols = d_model // HALVES
    any_spec = pl.BlockSpec(memory_space=pl.ANY)
    vmem_spec = pl.BlockSpec(memory_space=pltpu.VMEM)
    bf16, f32 = jnp.bfloat16, jnp.float32
    dma = pltpu.SemaphoreType.DMA
    shape = jax.ShapeDtypeStruct
    return pl.pallas_call(
        layers_kernel,
        out_shape=[shape((tok_count, d_model), bf16)] + [shape((tok_count, head_dim), bf16)] * 4
        + [shape((RING, ff_local, d_model), bf16), shape((RING, head_dim, d_model), bf16)],
        in_specs=[any_spec, vmem_spec, vmem_spec, vmem_spec] + [any_spec] * 7,
        out_specs=[any_spec] * 7,
        scratch_shapes=[
            pltpu.VMEM((tok_count, d_model), bf16),
            pltpu.VMEM((PART_SLOTS * chunk_rows, d_model), f32),
            pltpu.VMEM((RECV_SLOTS, HALVES, DIRS, landed, half_cols), f32),
            pltpu.VMEM((RECV_SLOTS, HALVES, DIRS, landed, half_cols // RING), f32),
            pltpu.VMEM((tok_count, ff_local), bf16),
            pltpu.VMEM((tok_count, head_dim), bf16),
            pltpu.VMEM((2, ff_local + head_dim, DOWN_TILE), bf16),
            pltpu.VMEM((2, 2, d_model, W_TILE), bf16),
            pltpu.VMEM((2 * CHIPS * tok_count, 2 * head_dim), bf16),
            pltpu.VMEM((tok_count, head_dim), bf16),
            pltpu.VMEM((2, tok_count, head_dim), f32),
            pltpu.VMEM((2, tok_count, 128), f32),
            pltpu.VMEM((2, tok_count, 128), f32),
            pltpu.VMEM((2, rows_per, d_model), bf16),
            pltpu.VMEM((CHUNKS, HALVES, chunk_rows // RING, half_cols // RING), bf16),
            dma((2,)), dma((CHUNKS, HALVES)), dma((2, 2)), dma((2, 2)), dma((2, 2)), dma((LAST_BLOCKS,)),
            dma((2, 4, KV_CHUNKS)), dma((2, 4, KV_CHUNKS)), dma((2, 4, KV_CHUNKS)), dma((2, 4, KV_CHUNKS)), dma((2, DIRS, 2)), dma((2, DIRS, 2)),
            dma((2, RING - 1, DIRS, 2)), dma((2, RING - 1, DIRS, 2)), dma((RING - 1, CHIPS, 2)), dma((RING - 1, CHIPS, 2)),
            dma((RING, KV_CHUNKS + 1)), dma((RING, KV_CHUNKS + 1)),
            pltpu.VMEM((KV_CHUNKS, rows_per, W_TILE), bf16), dma((KV_CHUNKS,)), dma((KV_CHUNKS,)),
            pltpu.VMEM((RING, rows_per, head_dim), bf16),
            dma((CHUNKS, STEPS, HALVES * DIRS)), dma((CHUNKS, STEPS, HALVES * DIRS)),
            dma((LAST_BLOCKS, LAST_STEPS, DIRS, RING)), dma((LAST_BLOCKS, LAST_STEPS, DIRS, RING)), dma((2, RING, 2)),
            pltpu.SemaphoreType.REGULAR((3,)), pltpu.SemaphoreType.REGULAR((DIRS,)),
        ],
        compiler_params=pltpu.CompilerParams(collective_id=0, has_side_effects=True, vmem_limit_bytes=67043328),
        name='layers',
    )(x_loc, cos_t, sin_t, norm_gain, w_q, w_k, w_v, w_gate, w_up, w_down, w_o)


EMIT_PARTS = 8


def emit_kernel(x_ref, k_first, k_second, v_first, v_second, x_out, k_out, v_out, xbuf, rows, load_sem, store_sem):
    size = x_ref.shape[0] // EMIT_PARTS
    loads, stores = [], []
    for n in range(EMIT_PARTS):
        part = pl.ds(n * size, size)
        loads.append(pltpu.make_async_copy(x_ref.at[part, :], xbuf.at[part, :], load_sem.at[n]))
        stores.append(pltpu.make_async_copy(xbuf.at[part, :], x_out.at[part, :], store_sem.at[n]))
    for n, (ref, out) in enumerate(((k_first, k_out.at[0]), (k_second, k_out.at[1]), (v_first, v_out.at[0]), (v_second, v_out.at[1]))):
        loads.append(pltpu.make_async_copy(ref, rows.at[n], load_sem.at[EMIT_PARTS + n]))
        stores.append(pltpu.make_async_copy(rows.at[n], out, store_sem.at[EMIT_PARTS + n]))
    for copy in loads:
        copy.start()
    for load, store in zip(loads, stores):
        load.wait()
        store.start()
    for copy in stores:
        copy.wait()


def emit(x_out, k_first, k_second, v_first, v_second):
    any_spec = pl.BlockSpec(memory_space=pl.ANY)
    cache = jax.ShapeDtypeStruct((2,) + k_first.shape, jnp.bfloat16)
    return pl.pallas_call(
        emit_kernel,
        out_shape=[jax.ShapeDtypeStruct(x_out.shape, jnp.bfloat16), cache, cache],
        in_specs=[any_spec] * 5,
        out_specs=[any_spec] * 3,
        scratch_shapes=[
            pltpu.VMEM(x_out.shape, jnp.bfloat16),
            pltpu.VMEM((4,) + k_first.shape, jnp.bfloat16),
            pltpu.SemaphoreType.DMA((EMIT_PARTS + 4,)),
            pltpu.SemaphoreType.DMA((EMIT_PARTS + 4,)),
        ],
        compiler_params=pltpu.CompilerParams(vmem_limit_bytes=63 * 1024 * 1024),
        name='emit',
    )(x_out, k_first, k_second, v_first, v_second)


def solution(mesh):
    row_spec = P(('batch', 'seq'), None)
    pos_spec = P(('batch', 'seq'))
    head_spec = P(None, None, 'head', None)
    out_proj_spec = P(None, 'head', None, None)
    col_spec = P(None, None, 'head')
    down_spec = P(None, 'head', None)
    cache_spec = P(None, ('batch', 'seq'), 'head', None)

    def local_forward(x_loc, pos_loc, w_q, w_k, w_v, w_o, w_gate, w_up, w_down, norm_gain):
        tok_count, d_model = x_loc.shape
        layer_count = w_q.shape[0]
        head_dim = w_q.shape[3]
        flat_q, flat_k, flat_v = (w.reshape(layer_count, d_model, head_dim) for w in (w_q, w_k, w_v))
        cos_t, sin_t = rope_tables(pos_loc, head_dim)
        x_out, k_first, v_first, k_second, v_second, _, _ = layers(x_loc, cos_t, sin_t, norm_gain, flat_q, flat_k, flat_v, w_gate, w_up, w_down, w_o)
        x_out, k_all, v_all = emit(x_out, k_first, k_second, v_first, v_second)
        cache_shape = (layer_count, tok_count, 1, head_dim)
        return x_out, k_all.reshape(cache_shape), v_all.reshape(cache_shape)

    return jax.shard_map(local_forward, mesh=mesh, in_specs=(row_spec, pos_spec, head_spec, head_spec, head_spec, out_proj_spec, col_spec, col_spec, down_spec, P(None, None)), out_specs=(row_spec, cache_spec, cache_spec), check_vma=False)
```

```python
import functools
import math
import jax
import jax.numpy as jnp
from jax import lax
from jax.experimental import pallas as pl
from jax.experimental.pallas import tpu as pltpu
from jax.sharding import PartitionSpec as P

ROPE_BASE = 500000.0
EPS = 1e-5


def rope_tables(positions, head_dim):
    half_dim = head_dim // 2
    inv_freq = ROPE_BASE ** (-(jnp.arange(half_dim, dtype=jnp.float32) * 2.0 / head_dim))
    angles = positions.astype(jnp.float32)[..., None] * inv_freq
    return jnp.cos(angles), jnp.sin(angles)


CHIPS = 4
RING = 4
HALVES = 2
DIRS = 2
KV_CHUNKS = 4
W_TILE = 256
NORM_ROWS = 64
CHUNKS = 8
STEPS = 8
PART_SLOTS = 4
RECV_SLOTS = 5
DOWN_TILE = 512
START_GAP = 3
STAGE_GAP = 2
BLOCK_TICK = 19
BLOCK_GAP = 6
LAST_TICK = 43
NEAR_TICKS = ((9, 1), (15, 3))
FAR_TICKS = ((24, 1), (26, 3))
SERVE_TICKS = (27, 31, 35, 42)
GIVE_TICK = 37
OWN_TICK = 3
DONE_TICK = 11
EARLY_TICK = 31
LAST_STEPS = 6
LAST_COLS = 256
LAST_BLOCKS = 16
LAST_GAP = 2


def layers_kernel(x_ref, cos_ref, sin_ref, gain_ref, wq_ref, wk_ref, wv_ref, wg_ref, wu_ref, wd_ref, wo_ref,
                 out_ref, k1_ref, v1_ref, k2_ref, v2_ref, gd_ref, go_ref,
                 xbuf, part, recv_a, recv_b, hid, att, wdo, wtile, kv, qbuf, acc, row_max, row_sum, xs, xres,
                 x_sem, res_sem, w_sem, down_sem, cache_sem, store_sem, own_send, pass_send, ici_recv, core_recv, part_send, part_recv,
                 round_send, round_recv, side_send, side_recv, give_send, give_recv, relay_buf, relay_send, relay_recv, att_all, ring_send, ring_recv,
                 last_send, last_recv, tile_sem, ready_sem, drained_sem):
    tok_count, d_model = xbuf.shape
    head_dim = qbuf.shape[1]
    half_dim = head_dim // 2
    ff_local = hid.shape[1]
    rows_per = tok_count // KV_CHUNKS
    half_rows = tok_count // 2
    lanes = row_max.shape[2]
    chunk_rows = tok_count // CHUNKS
    quarter, eighth = chunk_rows // RING, chunk_rows // (2 * RING)
    half_cols = d_model // HALVES
    piece_cols = half_cols // RING
    bf16, f32 = jnp.bfloat16, jnp.float32
    sign = (1, -1)
    mesh_id = pl.DeviceIdType.MESH

    my_head = lax.axis_index('head')
    pos_z, pos_y = my_head // RING, my_head % RING
    my_seq = lax.axis_index('seq')
    chip, core = my_seq // 2, my_seq % 2
    other = chip * 2 + 1 - core

    def wrap(n):
        return (n + RING) % RING

    def y_peer(d):
        return pos_z * RING + wrap(pos_y + sign[d])

    def z_device(z):
        return wrap(z) * RING + pos_y

    def z_peer(d):
        return z_device(pos_z + sign[d])

    def x_device(n):
        return wrap(chip + n) * 2 + core

    right, left = x_device(1), x_device(-1)

    def span(start, size, unit=None):
        return pl.ds(pl.multiple_of(start, unit or size), size)

    def remote(src, dst, send, recv, **to):
        return pltpu.make_async_remote_copy(src_ref=src, dst_ref=dst, send_sem=send, recv_sem=recv, device_id=to, device_id_type=mesh_id)

    def x_load(i):
        return pltpu.make_async_copy(x_ref.at[span(i * rows_per, rows_per), :], xs.at[i % 2], x_sem.at[i % 2])

    def weights(layer, piece):
        slot = piece % 2
        if isinstance(piece, int) and piece < 2:
            refs = ((wk_ref, wv_ref), (wq_ref,))[piece]
            return [pltpu.make_async_copy(ref.at[layer], wtile.at[slot, n], w_sem.at[slot, n]) for n, ref in enumerate(refs)]
        cols = span((piece - 2) * W_TILE, W_TILE)
        return [pltpu.make_async_copy(ref.at[layer, :, cols], wtile.at[slot, n], w_sem.at[slot, n]) for n, ref in enumerate((wg_ref, wu_ref))]

    def start(copies):
        for copy in copies:
            copy.start()

    def wait(copies):
        for copy in copies:
            copy.wait()

    down_tiles = d_model // DOWN_TILE

    def down_load(i):
        cols = span(i * DOWN_TILE, DOWN_TILE)
        return [pltpu.make_async_copy(wd_ref.at[0, :, cols], wdo.at[i % 2, pl.ds(0, ff_local), :], down_sem.at[i % 2, 0]),
                pltpu.make_async_copy(wo_ref.at[0, 0, :, cols], wdo.at[i % 2, pl.ds(ff_local, head_dim), :], down_sem.at[i % 2, 1])]

    def kv_copy(origin_chip, origin_core, i, to, send, recv):
        rows = kv.at[span((origin_chip * 2 + origin_core) * tok_count + i * rows_per, rows_per), :]
        return remote(rows, rows, send, recv, seq=to)

    def kv_routes(layer, i):
        late = i >= KV_CHUNKS // 2
        early = jnp.logical_not(late) if not isinstance(i, int) else not late

        def to(send, recv, origin_chip, origin_core, device):
            return kv_copy(origin_chip, origin_core, i, device, send, recv)
        own, passed, ici, side = own_send.at[layer], pass_send.at[layer], ici_recv.at[layer], core_recv.at[layer]
        return {
            'right': (chip < CHIPS - 1, lambda: to(own.at[0, i], ici.at[0, i], chip, core, right)),
            'wrap': (chip == 0, lambda: to(own.at[1, i], ici.at[2, i], chip, core, left)),
            'relay': (jnp.logical_and(late, chip == 1), lambda: to(own.at[3, i], ici.at[3, i], chip, core, left)),
            'other': (core == 0, lambda: to(own.at[2, i], side.at[0, i], chip, core, other)),
            'on_right': (jnp.logical_and(early, jnp.logical_and(chip >= 1, chip < CHIPS - 1)), lambda: to(passed.at[0, i], ici.at[1, i], chip - 1, core, right)),
            'from_relay': (jnp.logical_and(late, chip == 0), lambda: to(passed.at[0, i], ici.at[1, i], 1, core, left)),
            'on_left': (jnp.logical_and(late, chip == CHIPS - 1), lambda: to(passed.at[0, i], ici.at[1, i], 0, core, left)),
            'side1': (chip >= 1, lambda: to(passed.at[1, i], side.at[1, i], chip - 1, core, other)),
            'side2': (chip >= 2, lambda: to(passed.at[2, i], side.at[2, i], chip - 2, core, other)),
            'side3': (chip >= 3, lambda: to(passed.at[3, i], side.at[3, i], chip - 3, core, other)),
        }

    def start_route(layer, i, name):
        condition, copy = kv_routes(layer, i)[name]

        @pl.when(condition)
        def _():
            copy().start()

    def send_kv(layer, i):
        for name in ('right', 'wrap', 'relay', 'other'):
            start_route(layer, i, name)

    def kv_sent(layer):
        for i in range(KV_CHUNKS):
            for condition, copy in kv_routes(layer, i).values():
                @pl.when(condition)
                def _():
                    copy().wait_send()

    def serve(layer, back, i):
        @pl.when(chip >= back)
        def _():
            kv_copy(chip - back, core, i, other, pass_send.at[layer, back, i], ici_recv.at[layer, back - 1, i]).wait_recv()
        start_route(layer, i, 'side%d' % back)
        if back == 1:
            start_route(layer, i, 'on_right')
        if back == 3:
            start_route(layer, i, 'on_left')

    def relay(layer, i):
        condition, copy = kv_routes(layer, i)['from_relay']

        @pl.when(condition)
        def _():
            kv_copy(1, core, i, left, pass_send.at[layer, 0, i], ici_recv.at[layer, 3, i]).wait_recv()
            copy().start()

    def serve_all(layer, i):
        serve(layer, 1, i)
        serve(layer, 3, i)
        relay(layer, i)

    def taken(layer, back, chunks):
        for i in chunks:
            kv_copy(chip - back, 1 - core, i, other, pass_send.at[layer, 0, i], core_recv.at[layer, back, i]).wait_recv()

    def z_parts(step, d):
        copies = []
        for n, (own_ref, all_ref) in enumerate(((wd_ref, gd_ref), (wo_ref, go_ref))):
            size = all_ref.shape[1] // (2 * CHIPS)
            if step == 0:
                rows = span(my_seq * size, size)
                src = own_ref.at[1, rows, :] if n == 0 else own_ref.at[1, 0, rows, :]
                dst = all_ref.at[pos_z, rows, :]
            else:
                rows = span(my_seq * size + d * (size // 2), size // 2)
                src = dst = all_ref.at[wrap(pos_z - sign[d]), rows, :]
            copies.append(remote(src, dst, part_send.at[step, d, n], part_recv.at[step, d, n], head=z_peer(d)))
        return copies

    def part_copies(j, part_chip, part_core, half, send, recv, to):
        copies = []
        for n, ref in enumerate((gd_ref, go_ref)):
            size = ref.shape[1] // (2 * CHIPS)
            first = (part_chip * 2 + part_core) * size
            rows = span(first, size) if half is None else span(first + half * (size // 2), size // 2)
            place = ref.at[wrap(pos_z + j), rows, :]
            copies.append(remote(place, place, send.at[n], recv.at[n], seq=to))
        return copies

    def own_part(j, d):
        return part_copies(j, chip, core, None, round_send.at[0, j - 1, d], round_recv.at[0, j - 1, d], x_device(sign[d]))

    def far_part(j, d):
        return part_copies(j, wrap(chip - sign[d]), core, d, round_send.at[1, j - 1, d], round_recv.at[1, j - 1, d], x_device(sign[d]))

    def side_part(j, n, side):
        return part_copies(j, wrap(chip + n), side, None, side_send.at[j - 1, n], side_recv.at[j - 1, n], other)

    def round_start(j):
        for d in range(DIRS):
            start(own_part(j, d))
        start(side_part(j, 0, core))

    def near_parts(j):
        for d in range(DIRS):
            for copy in own_part(j, d):
                copy.wait_recv()
            start(far_part(j, d) + side_part(j, 3 if d == 0 else 1, core))

    def far_parts(j):
        for d in range(DIRS):
            for copy in far_part(j, d):
                copy.wait_recv()
        start(side_part(j, 2, core))

    def give_hidden(z, i, source):
        cols = span(i * W_TILE, W_TILE)
        return remote(hid.at[span(z * rows_per, rows_per), cols], hidden_place(source, i), give_send.at[z, i], give_recv.at[source, i], head=z_device(z))

    def hidden_place(source, i):
        return xs.at[1, :, span(source * ff_local + i * W_TILE, W_TILE)]

    def via_neighbor(z, i):
        step = jnp.where(i < KV_CHUNKS // 2, 1, -1)
        return remote(hid.at[span(z * rows_per, rows_per), span(i * W_TILE, W_TILE)], relay_buf.at[i], give_send.at[z, i], relay_recv.at[i], head=z_device(pos_z + step))

    def relay_hidden(i):
        step = 1 if i < KV_CHUNKS // 2 else -1
        source = wrap(pos_z - step)
        return remote(relay_buf.at[i], hidden_place(source, i), relay_send.at[i], give_recv.at[source, i], head=z_device(pos_z + step))

    def send_hidden(z, i):
        away = wrap(z - pos_z)

        @pl.when(away == 2)
        def _():
            via_neighbor(z, i).start()

        @pl.when(away % 2 == 1)
        def _():
            give_hidden(z, i, pos_z).start()

    def give_rows(z, source):
        return remote(att.at[span(z * rows_per, rows_per), :], att_all.at[source], give_send.at[z, KV_CHUNKS], give_recv.at[source, KV_CHUNKS], head=z_device(z))

    def norm_rows(x_few, layer):
        x_f32 = x_few.astype(f32)
        inv_rms = lax.rsqrt(jnp.mean(x_f32 * x_f32, axis=-1, keepdims=True) + EPS)
        return (x_f32 * inv_rms * gain_ref[pl.ds(layer, 1), :].astype(f32)).astype(bf16)

    def rope(values, rows):
        cos_t, sin_t = cos_ref[rows, :], sin_ref[rows, :]
        wide = values.astype(bf16).astype(f32)
        first, second = wide[:, :half_dim], wide[:, half_dim:]
        return jnp.concatenate([first * cos_t - second * sin_t, second * cos_t + first * sin_t], axis=1).astype(bf16)

    def dot(a, b):
        return jnp.dot(a, b, preferred_element_type=f32)

    scale = 1.0 / math.sqrt(head_dim)

    def keys_values(normed, i):
        rows = span(i * rows_per, rows_per)
        own = span(my_seq * tok_count + i * rows_per, rows_per)
        kv[own, :head_dim] = rope(dot(normed, wtile[0, 0]), rows)
        kv[own, head_dim:] = dot(normed, wtile[0, 1]).astype(bf16)

    def queries(normed, i):
        rows = span(i * rows_per, rows_per)
        qbuf[rows, :] = (rope(dot(normed, wtile[1, 0]), rows).astype(f32) * scale).astype(bf16)

    def gated(normed, i, tile):
        gate = dot(normed, wtile[tile % 2, 0])
        up = dot(normed, wtile[tile % 2, 1])
        hid[span(i * rows_per, rows_per), span(tile * W_TILE, W_TILE)] = (gate * jax.nn.sigmoid(gate) * up).astype(bf16)

    def attend(key_start, q_half, side, masked, first):
        rows = pl.ds(q_half * half_rows, half_rows)
        some = span(key_start, half_rows)
        logits = lax.dot_general(qbuf[rows, :], kv[some, :head_dim], (((1,), (1,)), ((), ())), preferred_element_type=f32)
        if masked:
            seen = lax.broadcasted_iota(jnp.int32, logits.shape, 0) >= lax.broadcasted_iota(jnp.int32, logits.shape, 1)
            logits = jnp.where(seen, logits, -jnp.inf)
        block_max = jnp.max(logits, axis=-1, keepdims=True)
        if first:
            new_max = jnp.broadcast_to(block_max, (half_rows, lanes))
        else:
            new_max = jnp.maximum(row_max[side, rows, :], block_max)
        prob = jnp.exp(logits - jnp.concatenate([new_max] * (half_rows // lanes), axis=1))
        block_sum = jnp.sum(prob, axis=-1, keepdims=True)
        block_out = dot(prob.astype(bf16), kv[some, head_dim:])
        if first:
            row_sum[side, rows, :] = jnp.broadcast_to(block_sum, (half_rows, lanes))
            acc[side, rows, :] = block_out
        else:
            rescale = jnp.exp(row_max[side, rows, :] - new_max)
            row_sum[side, rows, :] = row_sum[side, rows, :] * rescale + block_sum
            acc[side, rows, :] = acc[side, rows, :] * jnp.concatenate([rescale] * (head_dim // lanes), axis=1) + block_out
        row_max[side, rows, :] = new_max

    def attend_own(layer_half):
        own_start = my_seq * tok_count
        if layer_half == 0:
            attend(own_start, 0, 0, True, True)
            top_rows = pl.ds(0, half_rows)
            row_max[1, top_rows, :] = jnp.full((half_rows, lanes), -jnp.inf, f32)
            row_sum[1, top_rows, :] = jnp.zeros((half_rows, lanes), f32)
            acc[1, top_rows, :] = jnp.zeros((half_rows, head_dim), f32)
        else:
            attend(own_start, 1, 0, False, True)
            attend(own_start + half_rows, 1, 1, True, True)

    def past_start(n):
        later = n - core
        back = jnp.where(later < 2, 1, jnp.where(chip == CHIPS - 1, jnp.where(later < 4, 3, 2), 2))
        block = (chip - back) * 2 + jnp.where(later % 2 == 0, core, 1 - core)
        return jnp.where(jnp.logical_and(core == 1, n == 0), chip * 2, block) * tok_count

    def arrivals(layer, n, chunks):
        @pl.when(jnp.logical_and(core == 1, n == 0))
        def _():
            taken(layer, 0, chunks)

        for back in (1, 3, 2):
            place = 0 if back == 1 else 2 if back == 3 else jnp.where(chip == CHIPS - 1, 4, 2)
            if back == 2:
                @pl.when(jnp.logical_and(chip >= back, n == core + place))
                def _():
                    for i in chunks:
                        serve(layer, 2, i)

            @pl.when(jnp.logical_and(chip >= back, n == core + place + 1))
            def _():
                taken(layer, back, chunks)

    def visit(n, visits):
        for q_half, side in visits:
            attend(past_start(n) + side * half_rows, q_half, side, False, False)

    def attend_past(layer, first_n, last_n, chunks, visits):
        def past(n, carry):
            if chunks:
                arrivals(layer, n, chunks)
            visit(n, visits)
            return carry

        lax.fori_loop(first_n, last_n, past, 0)

    near_count = my_seq - jnp.where(chip >= 2, 2, 0)

    def finish(i, spread):
        rows = pl.ds(i * rows_per, rows_per)
        top = jnp.maximum(row_max[0, rows, :], row_max[1, rows, :])
        shares = [jnp.exp(row_max[side, rows, :] - top) for side in range(2)]
        total = shares[0] * row_sum[0, rows, :] + shares[1] * row_sum[1, rows, :]
        wide = [jnp.concatenate([w] * (head_dim // lanes), axis=1) for w in shares + [total]]
        att[rows, :] = ((acc[0, rows, :] * wide[0] + acc[1, rows, :] * wide[1]) / wide[2]).astype(bf16)
        if spread:
            @pl.when(i != pos_z)
            def _():
                give_rows(i, pos_z).start()

    first_pos, second_pos = (pos_y, pos_z), (pos_z, pos_y)
    first_peer, second_peer = (y_peer, z_peer), (z_peer, y_peer)

    def part_rows(chunk, piece, offset, count):
        return span((chunk % PART_SLOTS) * chunk_rows + piece * quarter + offset, count, eighth)

    def x_rows(chunk, piece, offset, count):
        return span(chunk * chunk_rows + piece * quarter + offset, count, eighth)

    def cols_of(h, piece):
        return span(h * half_cols + piece * piece_cols, piece_cols)

    def half_of(h):
        return pl.ds(h * half_cols, half_cols)

    def message(step, chunk, h, d):
        p1, p2, s = first_pos[h], second_pos[h], sign[d]
        slot = chunk % RECV_SLOTS
        if step == 0:
            src, dst = part.at[part_rows(chunk, wrap(p1 + 2), d * eighth, eighth), half_of(h)], recv_a.at[slot, h, d, pl.ds(quarter, eighth), :]
        elif step == 1:
            src, dst = part.at[part_rows(chunk, wrap(p1 + s), 0, quarter), half_of(h)], recv_a.at[slot, h, d, pl.ds(0, quarter), :]
        elif step == 2:
            src, dst = part.at[part_rows(chunk, p1, d * eighth, eighth), cols_of(h, wrap(p2 + 2))], recv_b.at[slot, h, d, pl.ds(quarter, eighth), :]
        elif step == 3:
            src, dst = part.at[part_rows(chunk, p1, 0, quarter), cols_of(h, wrap(p2 + s))], recv_b.at[slot, h, d, pl.ds(0, quarter), :]
        elif step == 4:
            src = dst = xbuf.at[x_rows(chunk, p1, 0, quarter), cols_of(h, p2)]
        elif step == 5:
            src = dst = xbuf.at[x_rows(chunk, p1, d * eighth, eighth), cols_of(h, wrap(p2 - s))]
        elif step == 6:
            src = dst = xbuf.at[x_rows(chunk, p1, 0, quarter), half_of(h)]
        else:
            src = dst = xbuf.at[x_rows(chunk, wrap(p1 - s), d * eighth, eighth), half_of(h)]
        peer = (first_peer if step in (0, 1, 6, 7) else second_peer)[h](d)
        return remote(src, dst, ring_send.at[chunk, step, h * DIRS + d], ring_recv.at[chunk, step, h * DIRS + d], head=peer)

    def each_message(chunk, steps, act):
        for step in steps:
            for h in range(HALVES):
                for d in range(DIRS):
                    act(message(step, chunk, h, d))

    def residual_load(chunk, h):
        return pltpu.make_async_copy(x_ref.at[x_rows(chunk, first_pos[h], 0, quarter), cols_of(h, second_pos[h])], xres.at[chunk, h], res_sem.at[chunk, h])

    def project(chunk):
        rows = span(chunk * chunk_rows, chunk_rows)
        slot_rows = span((chunk % PART_SLOTS) * chunk_rows, chunk_rows)

        def one_tile(i, carry):
            @pl.when(jnp.logical_or(chunk < CHUNKS - 1, i < down_tiles - 1))
            def _():
                start(down_load((i + 1) % down_tiles))

            wait(down_load(i))
            total = dot(hid[rows, :], wdo[i % 2, :ff_local, :])
            part[slot_rows, span(i * DOWN_TILE, DOWN_TILE)] = total + dot(att[rows, :], wdo[i % 2, ff_local:, :])
            return carry

        lax.fori_loop(0, down_tiles, one_tile, 0)

    def stage(number, chunk):
        slot = chunk % RECV_SLOTS
        if number == 0:
            @pl.when(chunk >= PART_SLOTS)
            def _():
                each_message(chunk - PART_SLOTS, range(4), lambda copy: copy.wait_send())
            project(chunk)
        for h in range(HALVES):
            p1, p2 = first_pos[h], second_pos[h]
            if number:
                for d in range(DIRS):
                    message(number - 1, chunk, h, d).wait_recv()
            if number in (1, 3):
                for d in range(DIRS):
                    if number == 1:
                        rows, cols, arrived = part_rows(chunk, wrap(p1 + sign[d]), d * eighth, eighth), half_of(h), recv_a
                    else:
                        rows, cols, arrived = part_rows(chunk, p1, d * eighth, eighth), cols_of(h, wrap(p2 + sign[d])), recv_b
                    part[rows, cols] = part[rows, cols] + arrived[slot, h, d, pl.ds(quarter, eighth), :]
            if number == 2:
                rows = part_rows(chunk, p1, 0, quarter)
                part[rows, half_of(h)] = part[rows, half_of(h)] + recv_a[slot, h, 0, pl.ds(0, quarter), :] + recv_a[slot, h, 1, pl.ds(0, quarter), :]
            if number == 4:
                residual_load(chunk, h).wait()
                rows, cols = part_rows(chunk, p1, 0, quarter), cols_of(h, p2)
                total = part[rows, cols] + recv_b[slot, h, 0, pl.ds(0, quarter), :] + recv_b[slot, h, 1, pl.ds(0, quarter), :]
                update = total.astype(bf16).astype(f32)
                xbuf[x_rows(chunk, p1, 0, quarter), cols] = (xres[chunk, h].astype(f32) + update).astype(bf16)
            if number < STEPS:
                for d in range(DIRS):
                    message(number, chunk, h, d).start()

    x_load(0).start()
    start(weights(0, 0))
    x_load(1).start()
    start(weights(0, 1))
    barrier = pltpu.get_barrier_semaphore()
    for peer in (left, right, other):
        pl.semaphore_signal(barrier, inc=1, device_id={'seq': peer}, device_id_type=mesh_id)
    for peer in [z_device(pos_z + j) for j in range(1, RING)] + [y_peer(d) for d in range(DIRS)]:
        pl.semaphore_signal(barrier, inc=1, device_id={'head': peer}, device_id_type=mesh_id)

    def prepare(i, carry):
        x_load(i).wait()

        def few(n, inner):
            xbuf[span(i * rows_per + n * NORM_ROWS, NORM_ROWS), :] = norm_rows(xs[i % 2, span(n * NORM_ROWS, NORM_ROWS), :], 0)
            return inner

        lax.fori_loop(0, rows_per // NORM_ROWS, few, 0)

        @pl.when(i + 2 < KV_CHUNKS)
        def _():
            x_load(i + 2).start()

        @pl.when(i == 0)
        def _():
            wait(weights(0, 0))

        keys_values(xbuf[span(i * rows_per, rows_per), :], i)

        @pl.when(i == 0)
        def _():
            pl.semaphore_wait(barrier, 8)

        send_kv(0, i)

        @pl.when(i == 0)
        def _():
            for d in range(DIRS):
                start(z_parts(0, d))
        return carry

    lax.fori_loop(0, KV_CHUNKS, prepare, 0)
    start(weights(0, 2))
    own_rows = span(my_seq * tok_count, tok_count)

    def cache_stores(layer):
        k_ref, v_ref = ((k1_ref, v1_ref), (k2_ref, v2_ref))[layer]
        return [pltpu.make_async_copy(kv.at[own_rows, pl.ds(0, head_dim)], k_ref, cache_sem.at[layer, 0]),
                pltpu.make_async_copy(kv.at[own_rows, pl.ds(head_dim, head_dim)], v_ref, cache_sem.at[layer, 1])]

    start(cache_stores(0))
    wait(weights(0, 1))

    def query(i, carry):
        queries(xbuf[span(i * rows_per, rows_per), :], i)
        return carry

    lax.fori_loop(0, KV_CHUNKS, query, 0)
    start(weights(0, 3))
    start(down_load(0))

    def residuals(n, carry):
        for h in range(HALVES):
            residual_load(n, h).start()
        return carry

    lax.fori_loop(0, CHUNKS, residuals, 0)

    def gate_half(half, tile):
        wait(weights(0, tile + 2))

        def rows_step(i, inner):
            gated(xbuf[span(i * rows_per, rows_per), :], i, tile)
            return inner

        lax.fori_loop(half * KV_CHUNKS // 2, (half + 1) * KV_CHUNKS // 2, rows_step, 0)

        @pl.when(tile < 2)
        def _():
            start(weights(0, tile + 4))

        for last in (2, 3):
            @pl.when(tile == last)
            def _():
                start(weights(1, last - 2) if half else weights(0, last))

    def first_half(tile, carry):
        gate_half(0, tile)

        @pl.when(tile < 3)
        def _():
            serve_all(0, tile)
        return carry

    def second_half(tile, carry):
        gate_half(1, tile)

        @pl.when(tile == 0)
        def _():
            serve_all(0, 3)
            attend_past(0, 0, near_count, range(KV_CHUNKS), ((0, 0), (0, 1)))
            for d in range(DIRS):
                for copy in z_parts(0, d):
                    copy.wait_recv()
                start(z_parts(1, d))
        return carry

    lax.fori_loop(0, ff_local // W_TILE, first_half, 0)
    attend_own(0)
    lax.fori_loop(0, 2, second_half, 0)
    attend_past(0, near_count, my_seq, range(KV_CHUNKS), ((0, 0), (0, 1)))
    finish(0, False)
    finish(1, False)
    round_start(1)
    round_start(3)

    def block_work(j, phase):
        @pl.when(phase == 0)
        def _():
            @pl.when(j == 0)
            def _():
                for n in range(3):
                    pl.semaphore_wait(ready_sem.at[n], 1)

            def few(n, inner):
                xs[0, span(n * NORM_ROWS, NORM_ROWS), :] = norm_rows(xbuf[span(j * rows_per + n * NORM_ROWS, NORM_ROWS), :], 1)
                return inner

            lax.fori_loop(0, rows_per // NORM_ROWS, few, 0)
            wait(weights(1, 0))
            keys_values(xs[0], j)
            send_kv(1, j)
            start(weights(1, 2))

        @pl.when(phase == 1)
        def _():
            wait(weights(1, 1))
            queries(xs[0], j)
            start(weights(1, 3))

        @pl.when(jnp.logical_and(phase >= 1, phase <= 4))
        def _():
            tile = phase - 1
            wait(weights(1, tile + 2))
            gated(xs[0], j, tile)

            @pl.when(tile < 2)
            def _():
                start(weights(1, tile + 4))

            @pl.when(jnp.logical_and(tile == 2, j < KV_CHUNKS - 1))
            def _():
                start(weights(1, 0))

            @pl.when(jnp.logical_and(tile == 3, j < KV_CHUNKS - 1))
            def _():
                start(weights(1, 1))

            @pl.when(j == KV_CHUNKS - 1)
            def _():
                send_hidden(j, tile)

    def tick(t, carry):
        for number in range(STEPS, -1, -1):
            place = t - STAGE_GAP * number
            chunk = place // START_GAP

            @pl.when(jnp.logical_and(place >= 0, jnp.logical_and(place % START_GAP == 0, chunk < CHUNKS)))
            def _():
                stage(number, chunk)

        @pl.when(jnp.logical_or(t == 1, t == 3))
        def _():
            gate_half(1, 2 + t // 2)

        @pl.when(t == OWN_TICK)
        def _():
            attend_own(1)

        @pl.when(jnp.logical_and(t > OWN_TICK, jnp.logical_and(t < DONE_TICK, t - OWN_TICK <= my_seq)))
        def _():
            visit(t - OWN_TICK - 1, ((1, 0), (1, 1)))

        @pl.when(t == EARLY_TICK)
        def _():
            attend_own(0)

        early = t - EARLY_TICK - 1

        @pl.when(jnp.logical_and(early >= 0, jnp.logical_and(early < 7, early < my_seq)))
        def _():
            arrivals(1, early, (0, 1))
            visit(early, ((0, 0),))

        @pl.when(t == 2)
        def _():
            for d in range(DIRS):
                for copy in z_parts(1, d):
                    copy.wait_recv()
            round_start(2)

        @pl.when(t == DONE_TICK)
        def _():
            finish(2, False)
            finish(3, False)
            kv_sent(0)
            wait(cache_stores(0))
            for n, peer in enumerate((left, right, other)):
                pl.semaphore_signal(ready_sem.at[n], inc=1, device_id={'seq': peer}, device_id_type=mesh_id)

        for when, j in NEAR_TICKS:
            @pl.when(t == when)
            def _():
                near_parts(j)

        for when, j in FAR_TICKS:
            @pl.when(t == when)
            def _():
                far_parts(j)

        @pl.when(t == GIVE_TICK)
        def _():
            for i in range(KV_CHUNKS):
                for z in range(KV_CHUNKS - 1):
                    send_hidden(z, i)

        late = t - BLOCK_TICK

        @pl.when(late >= 0)
        def _():
            block_work(late // BLOCK_GAP, late % BLOCK_GAP)

        for i, when in enumerate(SERVE_TICKS):
            @pl.when(t == when)
            def _():
                serve_all(1, i)
        return carry

    lax.fori_loop(0, LAST_TICK, tick, 0)

    def drain(chunk, carry):
        @pl.when(chunk >= CHUNKS - PART_SLOTS)
        def _():
            each_message(chunk, range(4), lambda copy: copy.wait_send())
        each_message(chunk, range(4, STEPS), lambda copy: copy.wait_send())
        return carry

    lax.fori_loop(0, CHUNKS, drain, 0)
    for d in range(DIRS):
        pl.semaphore_signal(drained_sem.at[d], inc=1, device_id={'head': y_peer(d)}, device_id_type=mesh_id)
    start(cache_stores(1))
    near_parts(2)
    attend_own(1)
    attend_past(1, 0, my_seq, (), ((1, 0),))
    for i in range(KV_CHUNKS):
        via_neighbor(0, i).wait_recv()
        relay_hidden(i).start()
    attend_past(1, 0, near_count, (2, 3), ((0, 1), (1, 1)))
    attend_past(1, near_count, my_seq, (2, 3), ((0, 1),))
    finish(0, True)
    finish(1, True)
    attend_past(1, near_count, my_seq, (), ((1, 1),))
    finish(2, True)
    finish(3, True)
    far_parts(2)
    for j in range(1, RING):
        for n in range(CHIPS):
            for copy in side_part(j, n, 1 - core):
                copy.wait_recv()

    quarter_rows = rows_per // RING
    depth = ff_local + head_dim

    def block_cols(c):
        return span(c * LAST_COLS, LAST_COLS)

    def tile_place(c, j, first, size):
        return wtile.at[c % 2, j // 2, pl.ds((j % 2) * depth + first, size), :]

    def tile_loads(c):
        copies = []
        for j in range(RING):
            z = wrap(pos_z + j)
            down = wd_ref.at[1, :, block_cols(c)] if j == 0 else gd_ref.at[z, :, block_cols(c)]
            out = wo_ref.at[1, 0, :, block_cols(c)] if j == 0 else go_ref.at[z, :, block_cols(c)]
            copies.append(pltpu.make_async_copy(down, tile_place(c, j, 0, ff_local), tile_sem.at[c % 2, j, 0]))
            copies.append(pltpu.make_async_copy(out, tile_place(c, j, ff_local, head_dim), tile_sem.at[c % 2, j, 1]))
        return copies

    start(tile_loads(0))
    for j in range(1, RING):
        z = wrap(pos_z + j)
        for i in range(KV_CHUNKS):
            give_hidden(z, i, z).wait_recv()
        give_rows(z, z).wait_recv()
    for d in range(DIRS):
        pl.semaphore_wait(drained_sem.at[d], 1)

    def quarter_of(piece, offset, size):
        return span(piece * quarter_rows + offset, size, quarter_rows // 2)

    def landed(d, first, size):
        return pl.ds(rows_per + d * (3 * quarter_rows // 2) + first, size)

    def rows_at(z, piece, offset, size):
        return span(z * rows_per + piece * quarter_rows + offset, size, quarter_rows // 2)

    def last_messages(step, c, d, z_first):
        s, cols, half = sign[d], block_cols(c), quarter_rows // 2
        near, behind, back = wrap(pos_y + s), wrap(pos_y - s), wrap(pos_z - s)
        along_y = step < 2 or (step < 4) != z_first
        if step == 0:
            pairs = [(part.at[quarter_of(wrap(pos_y + 2), d * half, half), cols], part.at[landed(d, quarter_rows, half), cols])]
        elif step == 1:
            pairs = [(part.at[quarter_of(near, 0, quarter_rows), cols], part.at[landed(d, 0, quarter_rows), cols])]
        else:
            if step == 2:
                rows = [rows_at(pos_z, pos_y, 0, quarter_rows)]
            elif step == 3:
                rows = [rows_at(back, pos_y, d * half, half) if z_first else rows_at(pos_z, behind, d * half, half)]
            elif step == 4:
                rows = [rows_at(z, pos_y, 0, quarter_rows) for z in range(RING)] if z_first else [rows_at(pos_z, 0, 0, rows_per)]
            else:
                rows = [rows_at(z, behind, d * half, half) for z in range(RING)] if z_first else [rows_at(back, 0, d * (rows_per // 2), rows_per // 2)]
            pairs = [(xbuf.at[r, cols], xbuf.at[r, cols]) for r in rows]
        to = (y_peer if along_y else z_peer)(d)
        return [remote(src, dst, last_send.at[c, step, d, n], last_recv.at[c, step, d, n], head=to) for n, (src, dst) in enumerate(pairs)]

    def on_last(step, c, act):
        def both(z_first):
            for d in range(DIRS):
                for copy in last_messages(step, c, d, z_first):
                    act(copy)

        if step < 2:
            both(False)
            return
        z_first = c % 4 == 3

        @pl.when(z_first)
        def _():
            both(True)

        @pl.when(jnp.logical_not(z_first))
        def _():
            both(False)

    def out_store(c):
        return pltpu.make_async_copy(xbuf.at[:, block_cols(c)], out_ref.at[:, block_cols(c)], store_sem.at[c])

    def last_project(c):
        @pl.when(c + 1 < LAST_BLOCKS)
        def _():
            start(tile_loads(c + 1))

        wait(tile_loads(c))
        total = None
        for j in range(RING):
            z = wrap(pos_z + j)
            own = span(pos_z * rows_per, rows_per)
            hidden_rows = hid[own, :] if j == 0 else xs[1, :, span(z * ff_local, ff_local)]
            out_rows = att[own, :] if j == 0 else att_all[z]
            term = dot(hidden_rows, wtile[c % 2, j // 2, pl.ds((j % 2) * depth, ff_local), :])
            term = term + dot(out_rows, wtile[c % 2, j // 2, pl.ds((j % 2) * depth + ff_local, head_dim), :])
            total = term if total is None else total + term
        part[pl.ds(0, rows_per), block_cols(c)] = total

    def last_stage(number, c):
        cols, half = block_cols(c), quarter_rows // 2
        if number == 0:
            last_project(c)
        else:
            on_last(number - 1, c, lambda copy: copy.wait_recv())
        if number == 1:
            for d in range(DIRS):
                piece = quarter_of(wrap(pos_y + sign[d]), d * half, half)
                part[piece, cols] = part[piece, cols] + part[landed(d, quarter_rows, half), cols]
        if number == 2:
            own = quarter_of(pos_y, 0, quarter_rows)
            total = part[own, cols] + part[landed(0, 0, quarter_rows), cols] + part[landed(1, 0, quarter_rows), cols]
            update = total.astype(bf16).astype(f32)
            rows = rows_at(pos_z, pos_y, 0, quarter_rows)
            xbuf[rows, cols] = (xbuf[rows, cols].astype(f32) + update).astype(bf16)
        if number < LAST_STEPS:
            on_last(number, c, lambda copy: copy.start())
        else:
            out_store(c).start()

    def last_tick(t, carry):
        for number in range(LAST_STEPS, -1, -1):
            c = t - LAST_GAP * number

            @pl.when(jnp.logical_and(c >= 0, c < LAST_BLOCKS))
            def _():
                last_stage(number, c)
        return carry

    lax.fori_loop(0, LAST_BLOCKS + LAST_GAP * LAST_STEPS, last_tick, 0)

    wait(cache_stores(1))
    for i in range(KV_CHUNKS):
        relay_hidden(i).wait_send()
    kv_sent(1)
    for d in range(DIRS):
        for step in range(2):
            for copy in z_parts(step, d):
                copy.wait_send()
    for j in range(1, RING):
        for d in range(DIRS):
            for copy in own_part(j, d) + far_part(j, d):
                copy.wait_send()
        for n in range(CHIPS):
            for copy in side_part(j, n, core):
                copy.wait_send()
        z = wrap(pos_z + j)
        for i in range(KV_CHUNKS):
            give_hidden(z, i, pos_z).wait_send()
        give_rows(z, pos_z).wait_send()

    def last_drain(c, carry):
        for step in range(LAST_STEPS):
            on_last(step, c, lambda copy: copy.wait_send())
        out_store(c).wait()
        return carry

    lax.fori_loop(0, LAST_BLOCKS, last_drain, 0)


def layers(x_loc, cos_t, sin_t, norm_gain, w_q, w_k, w_v, w_gate, w_up, w_down, w_o):
    tok_count, d_model = x_loc.shape
    head_dim = w_q.shape[2]
    ff_local = w_gate.shape[2]
    rows_per = tok_count // KV_CHUNKS
    chunk_rows = tok_count // CHUNKS
    landed = 3 * chunk_rows // (2 * RING)
    half_cols = d_model // HALVES
    any_spec = pl.BlockSpec(memory_space=pl.ANY)
    vmem_spec = pl.BlockSpec(memory_space=pltpu.VMEM)
    bf16, f32 = jnp.bfloat16, jnp.float32
    dma = pltpu.SemaphoreType.DMA
    shape = jax.ShapeDtypeStruct
    return pl.pallas_call(
        layers_kernel,
        out_shape=[shape((tok_count, d_model), bf16)] + [shape((tok_count, head_dim), bf16)] * 4
        + [shape((RING, ff_local, d_model), bf16), shape((RING, head_dim, d_model), bf16)],
        in_specs=[any_spec, vmem_spec, vmem_spec, vmem_spec] + [any_spec] * 7,
        out_specs=[any_spec] * 7,
        scratch_shapes=[
            pltpu.VMEM((tok_count, d_model), bf16),
            pltpu.VMEM((PART_SLOTS * chunk_rows, d_model), f32),
            pltpu.VMEM((RECV_SLOTS, HALVES, DIRS, landed, half_cols), f32),
            pltpu.VMEM((RECV_SLOTS, HALVES, DIRS, landed, half_cols // RING), f32),
            pltpu.VMEM((tok_count, ff_local), bf16),
            pltpu.VMEM((tok_count, head_dim), bf16),
            pltpu.VMEM((2, ff_local + head_dim, DOWN_TILE), bf16),
            pltpu.VMEM((2, 2, d_model, W_TILE), bf16),
            pltpu.VMEM((2 * CHIPS * tok_count, 2 * head_dim), bf16),
            pltpu.VMEM((tok_count, head_dim), bf16),
            pltpu.VMEM((2, tok_count, head_dim), f32),
            pltpu.VMEM((2, tok_count, 128), f32),
            pltpu.VMEM((2, tok_count, 128), f32),
            pltpu.VMEM((2, rows_per, d_model), bf16),
            pltpu.VMEM((CHUNKS, HALVES, chunk_rows // RING, half_cols // RING), bf16),
            dma((2,)), dma((CHUNKS, HALVES)), dma((2, 2)), dma((2, 2)), dma((2, 2)), dma((LAST_BLOCKS,)),
            dma((2, 4, KV_CHUNKS)), dma((2, 4, KV_CHUNKS)), dma((2, 4, KV_CHUNKS)), dma((2, 4, KV_CHUNKS)), dma((2, DIRS, 2)), dma((2, DIRS, 2)),
            dma((2, RING - 1, DIRS, 2)), dma((2, RING - 1, DIRS, 2)), dma((RING - 1, CHIPS, 2)), dma((RING - 1, CHIPS, 2)),
            dma((RING, KV_CHUNKS + 1)), dma((RING, KV_CHUNKS + 1)),
            pltpu.VMEM((KV_CHUNKS, rows_per, W_TILE), bf16), dma((KV_CHUNKS,)), dma((KV_CHUNKS,)),
            pltpu.VMEM((RING, rows_per, head_dim), bf16),
            dma((CHUNKS, STEPS, HALVES * DIRS)), dma((CHUNKS, STEPS, HALVES * DIRS)),
            dma((LAST_BLOCKS, LAST_STEPS, DIRS, RING)), dma((LAST_BLOCKS, LAST_STEPS, DIRS, RING)), dma((2, RING, 2)),
            pltpu.SemaphoreType.REGULAR((3,)), pltpu.SemaphoreType.REGULAR((DIRS,)),
        ],
        compiler_params=pltpu.CompilerParams(collective_id=0, has_side_effects=True, vmem_limit_bytes=67043328),
        name='layers',
    )(x_loc, cos_t, sin_t, norm_gain, w_q, w_k, w_v, w_gate, w_up, w_down, w_o)


EMIT_PARTS = 8


def emit_kernel(x_ref, k_first, k_second, v_first, v_second, x_out, k_out, v_out, xbuf, rows, load_sem, store_sem):
    size = x_ref.shape[0] // EMIT_PARTS
    loads, stores = [], []
    for n in range(EMIT_PARTS):
        part = pl.ds(n * size, size)
        loads.append(pltpu.make_async_copy(x_ref.at[part, :], xbuf.at[part, :], load_sem.at[n]))
        stores.append(pltpu.make_async_copy(xbuf.at[part, :], x_out.at[part, :], store_sem.at[n]))
    for n, (ref, out) in enumerate(((k_first, k_out.at[0]), (k_second, k_out.at[1]), (v_first, v_out.at[0]), (v_second, v_out.at[1]))):
        loads.append(pltpu.make_async_copy(ref, rows.at[n], load_sem.at[EMIT_PARTS + n]))
        stores.append(pltpu.make_async_copy(rows.at[n], out, store_sem.at[EMIT_PARTS + n]))
    for copy in loads:
        copy.start()
    for load, store in zip(loads, stores):
        load.wait()
        store.start()
    for copy in stores:
        copy.wait()


def emit(x_out, k_first, k_second, v_first, v_second):
    any_spec = pl.BlockSpec(memory_space=pl.ANY)
    cache = jax.ShapeDtypeStruct((2,) + k_first.shape, jnp.bfloat16)
    return pl.pallas_call(
        emit_kernel,
        out_shape=[jax.ShapeDtypeStruct(x_out.shape, jnp.bfloat16), cache, cache],
        in_specs=[any_spec] * 5,
        out_specs=[any_spec] * 3,
        scratch_shapes=[
            pltpu.VMEM(x_out.shape, jnp.bfloat16),
            pltpu.VMEM((4,) + k_first.shape, jnp.bfloat16),
            pltpu.SemaphoreType.DMA((EMIT_PARTS + 4,)),
            pltpu.SemaphoreType.DMA((EMIT_PARTS + 4,)),
        ],
        compiler_params=pltpu.CompilerParams(vmem_limit_bytes=63 * 1024 * 1024),
        name='emit',
    )(x_out, k_first, k_second, v_first, v_second)


def solution(mesh):
    row_spec = P(('batch', 'seq'), None)
    pos_spec = P(('batch', 'seq'))
    head_spec = P(None, None, 'head', None)
    out_proj_spec = P(None, 'head', None, None)
    col_spec = P(None, None, 'head')
    down_spec = P(None, 'head', None)
    cache_spec = P(None, ('batch', 'seq'), 'head', None)

    def local_forward(x_loc, pos_loc, w_q, w_k, w_v, w_o, w_gate, w_up, w_down, norm_gain):
        tok_count, d_model = x_loc.shape
        layer_count = w_q.shape[0]
        head_dim = w_q.shape[3]
        flat_q, flat_k, flat_v = (w.reshape(layer_count, d_model, head_dim) for w in (w_q, w_k, w_v))
        cos_t, sin_t = rope_tables(pos_loc, head_dim)
        x_out, k_first, v_first, k_second, v_second, _, _ = layers(x_loc, cos_t, sin_t, norm_gain, flat_q, flat_k, flat_v, w_gate, w_up, w_down, w_o)
        x_out, k_all, v_all = emit(x_out, k_first, k_second, v_first, v_second)
        cache_shape = (layer_count, tok_count, 1, head_dim)
        return x_out, k_all.reshape(cache_shape), v_all.reshape(cache_shape)

    return jax.shard_map(local_forward, mesh=mesh, in_specs=(row_spec, pos_spec, head_spec, head_spec, head_spec, out_proj_spec, col_spec, col_spec, down_spec, P(None, None)), out_specs=(row_spec, cache_spec, cache_spec), check_vma=False)
```

```python
import functools
import math
import jax
import jax.numpy as jnp
from jax import lax
from jax.experimental import pallas as pl
from jax.experimental.pallas import tpu as pltpu
from jax.sharding import PartitionSpec as P

ROPE_BASE = 500000.0
EPS = 1e-5


def rope_tables(positions, head_dim):
    half_dim = head_dim // 2
    inv_freq = ROPE_BASE ** (-(jnp.arange(half_dim, dtype=jnp.float32) * 2.0 / head_dim))
    angles = positions.astype(jnp.float32)[..., None] * inv_freq
    return jnp.cos(angles), jnp.sin(angles)


CHIPS = 4
RING = 4
HALVES = 2
DIRS = 2
KV_CHUNKS = 4
W_TILE = 256
NORM_ROWS = 64
CHUNKS = 8
STEPS = 8
PART_SLOTS = 4
RECV_SLOTS = 5
DOWN_TILE = 512
START_GAP = 3
STAGE_GAP = 2
BLOCK_TICK = 19
BLOCK_GAP = 6
LAST_TICK = 43
NEAR_TICKS = ((9, 1), (15, 3))
FAR_TICKS = ((24, 1), (26, 3))
SERVE_TICKS = (27, 31, 35, 42)
GIVE_TICK = 37
OWN_TICK = 3
DONE_TICK = 11
EARLY_TICK = 31
LAST_STEPS = 6
LAST_COLS = 256
LAST_BLOCKS = 16
LAST_GAP = 3


def layers_kernel(x_ref, cos_ref, sin_ref, gain_ref, wq_ref, wk_ref, wv_ref, wg_ref, wu_ref, wd_ref, wo_ref,
                 out_ref, k1_ref, v1_ref, k2_ref, v2_ref, gd_ref, go_ref,
                 xbuf, part, recv_a, recv_b, hid, att, wdo, wtile, kv, qbuf, acc, row_max, row_sum, xs, xres,
                 x_sem, res_sem, w_sem, down_sem, cache_sem, store_sem, kv_send, ici_recv, core_recv, part_send, part_recv,
                 round_send, round_recv, side_send, side_recv, give_send, give_recv, relay_buf, relay_send, relay_recv, att_all, ring_send, gather_send, ring_recv,
                 last_send, last_recv, tile_sem, ready_sem, drained_sem):
    tok_count, d_model = xbuf.shape
    head_dim = qbuf.shape[1]
    half_dim = head_dim // 2
    ff_local = hid.shape[1]
    depth = ff_local + head_dim
    rows_per = tok_count // KV_CHUNKS
    half_rows = tok_count // 2
    lanes = row_max.shape[2]
    chunk_rows = tok_count // CHUNKS
    quarter, eighth = chunk_rows // RING, chunk_rows // (2 * RING)
    half_cols = d_model // HALVES
    piece_cols = half_cols // RING
    bf16, f32 = jnp.bfloat16, jnp.float32
    sign = (1, -1)
    mesh_id = pl.DeviceIdType.MESH

    my_head = lax.axis_index('head')
    pos_z, pos_y = my_head // RING, my_head % RING
    my_seq = lax.axis_index('seq')
    chip, core = my_seq // 2, my_seq % 2
    other = chip * 2 + 1 - core

    def wrap(n):
        return (n + RING) % RING

    def y_peer(d):
        return pos_z * RING + wrap(pos_y + sign[d])

    def z_device(z):
        return wrap(z) * RING + pos_y

    def z_peer(d):
        return z_device(pos_z + sign[d])

    def x_device(n):
        return wrap(chip + n) * 2 + core

    right, left = x_device(1), x_device(-1)

    def span(start, size, unit=None):
        return pl.ds(pl.multiple_of(start, unit or size), size)

    def remote(src, dst, send, recv, **to):
        return pltpu.make_async_remote_copy(src_ref=src, dst_ref=dst, send_sem=send, recv_sem=recv, device_id=to, device_id_type=mesh_id)

    def take(sem, ref):
        remote(ref, ref, sem, sem, head=my_head).wait_recv()

    def x_load(i):
        return pltpu.make_async_copy(x_ref.at[span(i * rows_per, rows_per), :], xs.at[i % 2], x_sem.at[i % 2])

    def weights(layer, piece):
        slot = piece % 2
        if isinstance(piece, int) and piece < 2:
            refs = ((wk_ref, wv_ref), (wq_ref,))[piece]
            return [pltpu.make_async_copy(ref.at[layer], wtile.at[slot, n], w_sem.at[slot, n]) for n, ref in enumerate(refs)]
        cols = span((piece - 2) * W_TILE, W_TILE)
        return [pltpu.make_async_copy(ref.at[layer, :, cols], wtile.at[slot, n], w_sem.at[slot, n]) for n, ref in enumerate((wg_ref, wu_ref))]

    def start(copies):
        for copy in copies:
            copy.start()

    def wait(copies):
        for copy in copies:
            copy.wait()

    down_tiles = d_model // DOWN_TILE

    def down_load(i):
        cols = span(i * DOWN_TILE, DOWN_TILE)
        return [pltpu.make_async_copy(wd_ref.at[0, :, cols], wdo.at[i % 2, pl.ds(0, ff_local), :], down_sem.at[i % 2, 0]),
                pltpu.make_async_copy(wo_ref.at[0, 0, :, cols], wdo.at[i % 2, pl.ds(ff_local, head_dim), :], down_sem.at[i % 2, 1])]

    def kv_copy(origin_chip, origin_core, i, to, send, recv):
        rows = kv.at[span((origin_chip * 2 + origin_core) * tok_count + i * rows_per, rows_per), :]
        return remote(rows, rows, send, recv, seq=to)

    def kv_routes(i):
        def to(number, recv, origin_chip, origin_core, device):
            return lambda: kv_copy(origin_chip, origin_core, i, device, kv_send.at[number], recv)
        inner = jnp.logical_and(chip >= 1, chip < CHIPS - 1)
        return {
            'right': (chip < CHIPS - 1, 'all', to(0, ici_recv.at[0, i], chip, core, right)),
            'wrap': (chip == 0, 'all', to(1, ici_recv.at[2, i], chip, core, left)),
            'relay': (chip == 1, 'late', to(2, ici_recv.at[3, i], chip, core, left)),
            'other': (core == 0, 'all', to(3, core_recv.at[0, i], chip, core, other)),
            'on_right': (inner, 'early', to(4, ici_recv.at[1, i], chip - 1, core, right)),
            'from_relay': (chip == 0, 'late', to(5, ici_recv.at[1, i], 1, core, left)),
            'on_left': (chip == CHIPS - 1, 'late', to(6, ici_recv.at[1, i], 0, core, left)),
            'side1': (chip >= 1, 'all', to(7, core_recv.at[1, i], chip - 1, core, other)),
            'side2': (chip >= 2, 'all', to(8, core_recv.at[2, i], chip - 2, core, other)),
            'side3': (chip >= 3, 'all', to(9, core_recv.at[3, i], chip - 3, core, other)),
        }

    def start_route(i, name):
        condition, which, copy = kv_routes(i)[name]
        if which != 'all':
            late = i >= KV_CHUNKS // 2
            if isinstance(i, int):
                if late != (which == 'late'):
                    return
            else:
                condition = jnp.logical_and(condition, late if which == 'late' else jnp.logical_not(late))

        @pl.when(condition)
        def _():
            copy().start()

    def send_kv(i):
        for name in ('right', 'wrap', 'relay', 'other'):
            start_route(i, name)

    def kv_sent():
        for number, (condition, which, _) in enumerate(kv_routes(0).values()):
            @pl.when(condition)
            def _():
                take(kv_send.at[number], kv.at[pl.ds(0, tok_count if which == 'all' else half_rows), :])

    def serve(back, i):
        @pl.when(chip >= back)
        def _():
            kv_copy(chip - back, core, i, other, kv_send.at[0], ici_recv.at[back - 1, i]).wait_recv()
        start_route(i, 'side%d' % back)
        if back == 1:
            start_route(i, 'on_right')
        if back == 3:
            start_route(i, 'on_left')

    def relay(i):
        def pass_on():
            @pl.when(chip == 0)
            def _():
                kv_copy(1, core, i, left, kv_send.at[0], ici_recv.at[3, i]).wait_recv()
            start_route(i, 'from_relay')
        if not isinstance(i, int):
            pl.when(i >= KV_CHUNKS // 2)(pass_on)
        elif i >= KV_CHUNKS // 2:
            pass_on()

    def serve_all(i):
        serve(1, i)
        serve(3, i)
        relay(i)

    def taken(back, chunks):
        for i in chunks:
            kv_copy(chip - back, 1 - core, i, other, kv_send.at[0], core_recv.at[back, i]).wait_recv()

    def z_parts(step, d):
        copies = []
        for n, (own_ref, all_ref) in enumerate(((wd_ref, gd_ref), (wo_ref, go_ref))):
            size = all_ref.shape[1] // (2 * CHIPS)
            if step == 0:
                rows = span(my_seq * size, size)
                src = own_ref.at[1, rows, :] if n == 0 else own_ref.at[1, 0, rows, :]
                dst = all_ref.at[pos_z, rows, :]
            else:
                rows = span(my_seq * size + d * (size // 2), size // 2)
                src = dst = all_ref.at[wrap(pos_z - sign[d]), rows, :]
            copies.append(remote(src, dst, part_send, part_recv.at[step], head=z_peer(d)))
        return copies

    def part_copies(j, part_chip, part_core, half, send, recv, to):
        copies = []
        for n, ref in enumerate((gd_ref, go_ref)):
            size = ref.shape[1] // (2 * CHIPS)
            first = (part_chip * 2 + part_core) * size
            rows = span(first, size) if half is None else span(first + half * (size // 2), size // 2)
            place = ref.at[wrap(pos_z + j), rows, :]
            copies.append(remote(place, place, send, recv, seq=to))
        return copies

    def own_part(j, d):
        return part_copies(j, chip, core, None, round_send, round_recv.at[0, j - 1], x_device(sign[d]))

    def far_part(j, d):
        return part_copies(j, wrap(chip - sign[d]), core, d, round_send, round_recv.at[1, j - 1], x_device(sign[d]))

    def side_part(j, n, side):
        return part_copies(j, wrap(chip + n), side, None, side_send, side_recv, other)

    def round_start(j):
        for d in range(DIRS):
            start(own_part(j, d))
        start(side_part(j, 0, core))

    def near_parts(j):
        take(round_recv.at[0, j - 1], xbuf.at[pl.ds(0, depth // CHIPS), :])
        for d in range(DIRS):
            start(far_part(j, d) + side_part(j, 3 if d == 0 else 1, core))

    def far_parts(j):
        take(round_recv.at[1, j - 1], xbuf.at[pl.ds(0, depth // (2 * CHIPS)), :])
        start(side_part(j, 2, core))

    def give_hidden(z, i, source):
        cols = span(i * W_TILE, W_TILE)
        return remote(hid.at[span(z * rows_per, rows_per), cols], hidden_place(source, i), give_send, give_recv, head=z_device(z))

    def hidden_place(source, i):
        return xs.at[1, :, span(source * ff_local + i * W_TILE, W_TILE)]

    def via_neighbor(z, i):
        step = jnp.where(i < KV_CHUNKS // 2, 1, -1)
        return remote(hid.at[span(z * rows_per, rows_per), span(i * W_TILE, W_TILE)], relay_buf.at[i], give_send, relay_recv, head=z_device(pos_z + step))

    def relay_hidden(i):
        step = 1 if i < KV_CHUNKS // 2 else -1
        source = wrap(pos_z - step)
        return remote(relay_buf.at[i], hidden_place(source, i), relay_send, give_recv, head=z_device(pos_z + step))

    def send_hidden(z, i):
        away = wrap(z - pos_z)

        @pl.when(away == 2)
        def _():
            via_neighbor(z, i).start()

        @pl.when(away % 2 == 1)
        def _():
            give_hidden(z, i, pos_z).start()

    def give_rows(z, source):
        return remote(att.at[span(z * rows_per, rows_per), :], att_all.at[source], give_send, give_recv, head=z_device(z))

    def norm_rows(x_few, layer):
        x_f32 = x_few.astype(f32)
        inv_rms = lax.rsqrt(jnp.mean(x_f32 * x_f32, axis=-1, keepdims=True) + EPS)
        return (x_f32 * inv_rms * gain_ref[pl.ds(layer, 1), :].astype(f32)).astype(bf16)

    def rope(values, rows):
        cos_t, sin_t = cos_ref[rows, :], sin_ref[rows, :]
        wide = values.astype(bf16).astype(f32)
        first, second = wide[:, :half_dim], wide[:, half_dim:]
        return jnp.concatenate([first * cos_t - second * sin_t, second * cos_t + first * sin_t], axis=1).astype(bf16)

    def dot(a, b):
        return jnp.dot(a, b, preferred_element_type=f32)

    scale = 1.0 / math.sqrt(head_dim)

    def keys_values(normed, i):
        rows = span(i * rows_per, rows_per)
        own = span(my_seq * tok_count + i * rows_per, rows_per)
        kv[own, :head_dim] = rope(dot(normed, wtile[0, 0]), rows)
        kv[own, head_dim:] = dot(normed, wtile[0, 1]).astype(bf16)

    def queries(normed, i):
        rows = span(i * rows_per, rows_per)
        qbuf[rows, :] = (rope(dot(normed, wtile[1, 0]), rows).astype(f32) * scale).astype(bf16)

    def gated(normed, i, tile):
        gate = dot(normed, wtile[tile % 2, 0])
        up = dot(normed, wtile[tile % 2, 1])
        hid[span(i * rows_per, rows_per), span(tile * W_TILE, W_TILE)] = (gate * jax.nn.sigmoid(gate) * up).astype(bf16)

    def attend(key_start, q_half, side, masked, first):
        rows = pl.ds(q_half * half_rows, half_rows)
        some = span(key_start, half_rows)
        logits = lax.dot_general(qbuf[rows, :], kv[some, :head_dim], (((1,), (1,)), ((), ())), preferred_element_type=f32)
        if masked:
            seen = lax.broadcasted_iota(jnp.int32, logits.shape, 0) >= lax.broadcasted_iota(jnp.int32, logits.shape, 1)
            logits = jnp.where(seen, logits, -jnp.inf)
        block_max = jnp.max(logits, axis=-1, keepdims=True)
        if first:
            new_max = jnp.broadcast_to(block_max, (half_rows, lanes))
        else:
            new_max = jnp.maximum(row_max[side, rows, :], block_max)
        prob = jnp.exp(logits - jnp.concatenate([new_max] * (half_rows // lanes), axis=1))
        block_sum = jnp.sum(prob, axis=-1, keepdims=True)
        block_out = dot(prob.astype(bf16), kv[some, head_dim:])
        if first:
            row_sum[side, rows, :] = jnp.broadcast_to(block_sum, (half_rows, lanes))
            acc[side, rows, :] = block_out
        else:
            rescale = jnp.exp(row_max[side, rows, :] - new_max)
            row_sum[side, rows, :] = row_sum[side, rows, :] * rescale + block_sum
            acc[side, rows, :] = acc[side, rows, :] * jnp.concatenate([rescale] * (head_dim // lanes), axis=1) + block_out
        row_max[side, rows, :] = new_max

    def attend_own(layer_half):
        own_start = my_seq * tok_count
        if layer_half == 0:
            attend(own_start, 0, 0, True, True)
            top_rows = pl.ds(0, half_rows)
            row_max[1, top_rows, :] = jnp.full((half_rows, lanes), -jnp.inf, f32)
            row_sum[1, top_rows, :] = jnp.zeros((half_rows, lanes), f32)
            acc[1, top_rows, :] = jnp.zeros((half_rows, head_dim), f32)
        else:
            attend(own_start, 1, 0, False, True)
            attend(own_start + half_rows, 1, 1, True, True)

    def past_start(n):
        later = n - core
        back = jnp.where(later < 2, 1, jnp.where(chip == CHIPS - 1, jnp.where(later < 4, 3, 2), 2))
        block = (chip - back) * 2 + jnp.where(later % 2 == 0, core, 1 - core)
        return jnp.where(jnp.logical_and(core == 1, n == 0), chip * 2, block) * tok_count

    def arrivals(n, chunks):
        @pl.when(jnp.logical_and(core == 1, n == 0))
        def _():
            taken(0, chunks)

        for back in (1, 3, 2):
            place = 0 if back == 1 else 2 if back == 3 else jnp.where(chip == CHIPS - 1, 4, 2)
            if back == 2:
                @pl.when(jnp.logical_and(chip >= back, n == core + place))
                def _():
                    for i in chunks:
                        serve(2, i)

            @pl.when(jnp.logical_and(chip >= back, n == core + place + 1))
            def _():
                taken(back, chunks)

    def visit(n, visits):
        for q_half, side in visits:
            attend(past_start(n) + side * half_rows, q_half, side, False, False)

    def attend_past(first_n, last_n, chunks, visits):
        def past(n, carry):
            if chunks:
                arrivals(n, chunks)
            visit(n, visits)
            return carry

        lax.fori_loop(first_n, last_n, past, 0)

    near_count = my_seq - jnp.where(chip >= 2, 2, 0)

    def finish(i, spread):
        rows = pl.ds(i * rows_per, rows_per)
        top = jnp.maximum(row_max[0, rows, :], row_max[1, rows, :])
        shares = [jnp.exp(row_max[side, rows, :] - top) for side in range(2)]
        total = shares[0] * row_sum[0, rows, :] + shares[1] * row_sum[1, rows, :]
        wide = [jnp.concatenate([w] * (head_dim // lanes), axis=1) for w in shares + [total]]
        att[rows, :] = ((acc[0, rows, :] * wide[0] + acc[1, rows, :] * wide[1]) / wide[2]).astype(bf16)
        if spread:
            @pl.when(i != pos_z)
            def _():
                give_rows(i, pos_z).start()

    first_pos, second_pos = (pos_y, pos_z), (pos_z, pos_y)
    first_peer, second_peer = (y_peer, z_peer), (z_peer, y_peer)

    def part_rows(chunk, piece, offset, count):
        return span((chunk % PART_SLOTS) * chunk_rows + piece * quarter + offset, count, eighth)

    def x_rows(chunk, piece, offset, count):
        return span(chunk * chunk_rows + piece * quarter + offset, count, eighth)

    def cols_of(h, piece):
        return span(h * half_cols + piece * piece_cols, piece_cols)

    def half_of(h):
        return pl.ds(h * half_cols, half_cols)

    def message(step, chunk, h, d):
        p1, p2, s = first_pos[h], second_pos[h], sign[d]
        slot = chunk % RECV_SLOTS
        if step == 0:
            src, dst = part.at[part_rows(chunk, wrap(p1 + 2), d * eighth, eighth), half_of(h)], recv_a.at[slot, h, d, pl.ds(quarter, eighth), :]
        elif step == 1:
            src, dst = part.at[part_rows(chunk, wrap(p1 + s), 0, quarter), half_of(h)], recv_a.at[slot, h, d, pl.ds(0, quarter), :]
        elif step == 2:
            src, dst = part.at[part_rows(chunk, p1, d * eighth, eighth), cols_of(h, wrap(p2 + 2))], recv_b.at[slot, h, d, pl.ds(quarter, eighth), :]
        elif step == 3:
            src, dst = part.at[part_rows(chunk, p1, 0, quarter), cols_of(h, wrap(p2 + s))], recv_b.at[slot, h, d, pl.ds(0, quarter), :]
        elif step == 4:
            src = dst = xbuf.at[x_rows(chunk, p1, 0, quarter), cols_of(h, p2)]
        elif step == 5:
            src = dst = xbuf.at[x_rows(chunk, p1, d * eighth, eighth), cols_of(h, wrap(p2 - s))]
        elif step == 6:
            src = dst = xbuf.at[x_rows(chunk, p1, 0, quarter), half_of(h)]
        else:
            src = dst = xbuf.at[x_rows(chunk, wrap(p1 - s), d * eighth, eighth), half_of(h)]
        peer = (first_peer if step in (0, 1, 6, 7) else second_peer)[h](d)
        return remote(src, dst, ring_send.at[chunk % PART_SLOTS] if step < 4 else gather_send.at[step - 4], ring_recv.at[slot, step], head=peer)

    def arrived_in(step, count=1):
        rows = (2 * eighth, 2 * quarter, eighth // 2, quarter // 2, quarter // 2, quarter // 2, 2 * quarter, quarter)[step] * count
        return (part if step < 4 else xbuf).at[pl.ds(0, rows), pl.ds(0, half_cols if step == 5 else d_model)]

    def partials_sent(slot):
        take(ring_send.at[slot], part.at[pl.ds(0, 2 * eighth + 2 * quarter + eighth // 2 + quarter // 2), :])

    def residual_load(chunk, h):
        return pltpu.make_async_copy(x_ref.at[x_rows(chunk, first_pos[h], 0, quarter), cols_of(h, second_pos[h])], xres.at[chunk, h], res_sem)

    def project(chunk):
        rows = span(chunk * chunk_rows, chunk_rows)
        slot_rows = span((chunk % PART_SLOTS) * chunk_rows, chunk_rows)

        def one_tile(i, carry):
            @pl.when(jnp.logical_or(chunk < CHUNKS - 1, i < down_tiles - 1))
            def _():
                start(down_load((i + 1) % down_tiles))

            wait(down_load(i))
            total = dot(hid[rows, :], wdo[i % 2, :ff_local, :])
            part[slot_rows, span(i * DOWN_TILE, DOWN_TILE)] = total + dot(att[rows, :], wdo[i % 2, ff_local:, :])
            return carry

        lax.fori_loop(0, down_tiles, one_tile, 0)

    def stage(number, chunk):
        slot = chunk % RECV_SLOTS
        if number == 0:
            @pl.when(chunk >= PART_SLOTS)
            def _():
                partials_sent(chunk % PART_SLOTS)
            project(chunk)
        else:
            take(ring_recv.at[slot, number - 1], arrived_in(number - 1))
        if number == 4:
            @pl.when(chunk == 0)
            def _():
                take(res_sem, xres)
        for h in range(HALVES):
            p1, p2 = first_pos[h], second_pos[h]
            if number in (1, 3):
                for d in range(DIRS):
                    if number == 1:
                        rows, cols, arrived = part_rows(chunk, wrap(p1 + sign[d]), d * eighth, eighth), half_of(h), recv_a
                    else:
                        rows, cols, arrived = part_rows(chunk, p1, d * eighth, eighth), cols_of(h, wrap(p2 + sign[d])), recv_b
                    part[rows, cols] = part[rows, cols] + arrived[slot, h, d, pl.ds(quarter, eighth), :]
            if number == 2:
                rows = part_rows(chunk, p1, 0, quarter)
                part[rows, half_of(h)] = part[rows, half_of(h)] + recv_a[slot, h, 0, pl.ds(0, quarter), :] + recv_a[slot, h, 1, pl.ds(0, quarter), :]
            if number == 4:
                rows, cols = part_rows(chunk, p1, 0, quarter), cols_of(h, p2)
                total = part[rows, cols] + recv_b[slot, h, 0, pl.ds(0, quarter), :] + recv_b[slot, h, 1, pl.ds(0, quarter), :]
                update = total.astype(bf16).astype(f32)
                xbuf[x_rows(chunk, p1, 0, quarter), cols] = (xres[chunk, h].astype(f32) + update).astype(bf16)
            if number < STEPS:
                for d in range(DIRS):
                    message(number, chunk, h, d).start()

    x_load(0).start()
    start(weights(0, 0))
    x_load(1).start()
    start(weights(0, 1))
    barrier = pltpu.get_barrier_semaphore()
    for peer in (left, right, other):
        pl.semaphore_signal(barrier, inc=1, device_id={'seq': peer}, device_id_type=mesh_id)
    for peer in [z_device(pos_z + j) for j in range(1, RING)] + [y_peer(d) for d in range(DIRS)]:
        pl.semaphore_signal(barrier, inc=1, device_id={'head': peer}, device_id_type=mesh_id)

    def prepare(i, carry):
        x_load(i).wait()

        def few(n, inner):
            xbuf[span(i * rows_per + n * NORM_ROWS, NORM_ROWS), :] = norm_rows(xs[i % 2, span(n * NORM_ROWS, NORM_ROWS), :], 0)
            return inner

        lax.fori_loop(0, rows_per // NORM_ROWS, few, 0)

        @pl.when(i + 2 < KV_CHUNKS)
        def _():
            x_load(i + 2).start()

        @pl.when(i == 0)
        def _():
            wait(weights(0, 0))

        keys_values(xbuf[span(i * rows_per, rows_per), :], i)

        @pl.when(i == 0)
        def _():
            pl.semaphore_wait(barrier, 8)

        send_kv(i)

        @pl.when(i == 0)
        def _():
            for d in range(DIRS):
                start(z_parts(0, d))
        return carry

    lax.fori_loop(0, KV_CHUNKS, prepare, 0)
    start(weights(0, 2))
    own_rows = span(my_seq * tok_count, tok_count)

    def cache_stores(layer):
        k_ref, v_ref = ((k1_ref, v1_ref), (k2_ref, v2_ref))[layer]
        return [pltpu.make_async_copy(kv.at[own_rows, pl.ds(0, head_dim)], k_ref, cache_sem),
                pltpu.make_async_copy(kv.at[own_rows, pl.ds(head_dim, head_dim)], v_ref, cache_sem)]

    start(cache_stores(0))
    wait(weights(0, 1))

    def query(i, carry):
        queries(xbuf[span(i * rows_per, rows_per), :], i)
        return carry

    lax.fori_loop(0, KV_CHUNKS, query, 0)
    start(weights(0, 3))
    start(down_load(0))

    def residuals(n, carry):
        for h in range(HALVES):
            residual_load(n, h).start()
        return carry

    lax.fori_loop(0, CHUNKS, residuals, 0)

    def gate_half(half, tile):
        wait(weights(0, tile + 2))

        def rows_step(i, inner):
            gated(xbuf[span(i * rows_per, rows_per), :], i, tile)
            return inner

        lax.fori_loop(half * KV_CHUNKS // 2, (half + 1) * KV_CHUNKS // 2, rows_step, 0)

        @pl.when(tile < 2)
        def _():
            start(weights(0, tile + 4))

        for last in (2, 3):
            @pl.when(tile == last)
            def _():
                start(weights(1, last - 2) if half else weights(0, last))

    def first_half(tile, carry):
        gate_half(0, tile)

        @pl.when(tile < 3)
        def _():
            serve_all(tile)
        return carry

    def second_half(tile, carry):
        gate_half(1, tile)

        @pl.when(tile == 0)
        def _():
            serve_all(3)
            attend_past(0, near_count, range(KV_CHUNKS), ((0, 0), (0, 1)))
            take(part_recv.at[0], xbuf.at[pl.ds(0, depth // CHIPS), :])
            for d in range(DIRS):
                start(z_parts(1, d))
        return carry

    lax.fori_loop(0, ff_local // W_TILE, first_half, 0)
    attend_own(0)
    lax.fori_loop(0, 2, second_half, 0)
    attend_past(near_count, my_seq, range(KV_CHUNKS), ((0, 0), (0, 1)))
    finish(0, False)
    finish(1, False)
    round_start(1)
    round_start(3)

    def block_work(j, phase):
        @pl.when(phase == 0)
        def _():
            @pl.when(j == 0)
            def _():
                for n in range(3):
                    pl.semaphore_wait(ready_sem.at[n], 1)

            def few(n, inner):
                xs[0, span(n * NORM_ROWS, NORM_ROWS), :] = norm_rows(xbuf[span(j * rows_per + n * NORM_ROWS, NORM_ROWS), :], 1)
                return inner

            lax.fori_loop(0, rows_per // NORM_ROWS, few, 0)
            wait(weights(1, 0))
            keys_values(xs[0], j)
            send_kv(j)
            start(weights(1, 2))

        @pl.when(phase == 1)
        def _():
            wait(weights(1, 1))
            queries(xs[0], j)
            start(weights(1, 3))

        @pl.when(jnp.logical_and(phase >= 1, phase <= 4))
        def _():
            tile = phase - 1
            wait(weights(1, tile + 2))
            gated(xs[0], j, tile)

            @pl.when(tile < 2)
            def _():
                start(weights(1, tile + 4))

            @pl.when(jnp.logical_and(tile == 2, j < KV_CHUNKS - 1))
            def _():
                start(weights(1, 0))

            @pl.when(jnp.logical_and(tile == 3, j < KV_CHUNKS - 1))
            def _():
                start(weights(1, 1))

            @pl.when(j == KV_CHUNKS - 1)
            def _():
                send_hidden(j, tile)

    def tick(t, carry):
        for number in range(STEPS, -1, -1):
            place = t - STAGE_GAP * number
            chunk = place // START_GAP

            @pl.when(jnp.logical_and(place >= 0, jnp.logical_and(place % START_GAP == 0, chunk < CHUNKS)))
            def _():
                stage(number, chunk)

        @pl.when(jnp.logical_or(t == 1, t == 3))
        def _():
            gate_half(1, 2 + t // 2)

        @pl.when(t == OWN_TICK)
        def _():
            attend_own(1)

        @pl.when(jnp.logical_and(t > OWN_TICK, jnp.logical_and(t < DONE_TICK, t - OWN_TICK <= my_seq)))
        def _():
            visit(t - OWN_TICK - 1, ((1, 0), (1, 1)))

        @pl.when(t == EARLY_TICK)
        def _():
            attend_own(0)

        early = t - EARLY_TICK - 1

        @pl.when(jnp.logical_and(early >= 0, jnp.logical_and(early < 7, early < my_seq)))
        def _():
            arrivals(early, (0, 1))
            visit(early, ((0, 0),))

        @pl.when(t == 2)
        def _():
            take(part_recv.at[1], xbuf.at[pl.ds(0, depth // (2 * CHIPS)), :])
            round_start(2)

        @pl.when(t == DONE_TICK)
        def _():
            finish(2, False)
            finish(3, False)
            kv_sent()
            take(cache_sem, kv.at[own_rows, :])
            for n, peer in enumerate((left, right, other)):
                pl.semaphore_signal(ready_sem.at[n], inc=1, device_id={'seq': peer}, device_id_type=mesh_id)

        for when, j in NEAR_TICKS:
            @pl.when(t == when)
            def _():
                near_parts(j)

        for when, j in FAR_TICKS:
            @pl.when(t == when)
            def _():
                far_parts(j)

        @pl.when(t == GIVE_TICK)
        def _():
            for i in range(KV_CHUNKS):
                for z in range(KV_CHUNKS - 1):
                    send_hidden(z, i)

        late = t - BLOCK_TICK

        @pl.when(late >= 0)
        def _():
            block_work(late // BLOCK_GAP, late % BLOCK_GAP)

        for i, when in enumerate(SERVE_TICKS):
            @pl.when(t == when)
            def _():
                serve_all(i)
        return carry

    lax.fori_loop(0, LAST_TICK, tick, 0)

    for slot in range(PART_SLOTS):
        partials_sent(slot)
    for step in range(4, STEPS):
        take(gather_send.at[step - 4], arrived_in(step, CHUNKS))
    for d in range(DIRS):
        pl.semaphore_signal(drained_sem.at[d], inc=1, device_id={'head': y_peer(d)}, device_id_type=mesh_id)
    start(cache_stores(1))
    near_parts(2)
    attend_own(1)
    attend_past(0, my_seq, (), ((1, 0),))
    take(relay_recv, relay_buf)
    for i in range(KV_CHUNKS):
        relay_hidden(i).start()
    attend_past(0, near_count, (2, 3), ((0, 1), (1, 1)))
    attend_past(near_count, my_seq, (2, 3), ((0, 1),))
    finish(0, True)
    finish(1, True)
    attend_past(near_count, my_seq, (), ((1, 1),))
    finish(2, True)
    finish(3, True)
    far_parts(2)
    parts_ref = gd_ref.at[pl.ds(0, 2), pl.ds(0, 3 * depth // 4), :]
    take(side_recv, parts_ref)

    quarter_rows = rows_per // RING

    def block_cols(c):
        return span(c * LAST_COLS, LAST_COLS)

    def tile_place(c, j, first, size):
        return wtile.at[c % 2, j // 2, pl.ds((j % 2) * depth + first, size), :]

    def tile_loads(c):
        copies = []
        for j in range(RING):
            z = wrap(pos_z + j)
            down = wd_ref.at[1, :, block_cols(c)] if j == 0 else gd_ref.at[z, :, block_cols(c)]
            out = wo_ref.at[1, 0, :, block_cols(c)] if j == 0 else go_ref.at[z, :, block_cols(c)]
            copies.append(pltpu.make_async_copy(down, tile_place(c, j, 0, ff_local), tile_sem.at[c % 2]))
            copies.append(pltpu.make_async_copy(out, tile_place(c, j, ff_local, head_dim), tile_sem.at[c % 2]))
        return copies

    start(tile_loads(0))
    given = hid.at[pl.ds(0, (RING - 1) * rows_per * depth // ff_local), :]
    take(give_recv, given)
    for d in range(DIRS):
        pl.semaphore_wait(drained_sem.at[d], 1)

    def quarter_of(piece, offset, size):
        return span(piece * quarter_rows + offset, size, quarter_rows // 2)

    def landed(d, first, size):
        return pl.ds(rows_per + d * (3 * quarter_rows // 2) + first, size)

    def rows_at(z, piece, offset, size):
        return span(z * rows_per + piece * quarter_rows + offset, size, quarter_rows // 2)

    def last_messages(step, c, d, z_first):
        s, cols, half = sign[d], block_cols(c), quarter_rows // 2
        near, behind, back = wrap(pos_y + s), wrap(pos_y - s), wrap(pos_z - s)
        along_y = step < 2 or (step < 4) != z_first
        if step == 0:
            pairs = [(part.at[quarter_of(wrap(pos_y + 2), d * half, half), cols], part.at[landed(d, quarter_rows, half), cols])]
        elif step == 1:
            pairs = [(part.at[quarter_of(near, 0, quarter_rows), cols], part.at[landed(d, 0, quarter_rows), cols])]
        else:
            if step == 2:
                rows = [rows_at(pos_z, pos_y, 0, quarter_rows)]
            elif step == 3:
                rows = [rows_at(back, pos_y, d * half, half) if z_first else rows_at(pos_z, behind, d * half, half)]
            elif step == 4:
                rows = [rows_at(z, pos_y, 0, quarter_rows) for z in range(RING)] if z_first else [rows_at(pos_z, 0, 0, rows_per)]
            else:
                rows = [rows_at(z, behind, d * half, half) for z in range(RING)] if z_first else [rows_at(back, 0, d * (rows_per // 2), rows_per // 2)]
            pairs = [(xbuf.at[r, cols], xbuf.at[r, cols]) for r in rows]
        to = (y_peer if along_y else z_peer)(d)
        return [remote(src, dst, last_send.at[step], last_recv.at[c, step], head=to) for src, dst in pairs]

    def last_arrived(step, cols):
        rows = (quarter_rows, 2 * quarter_rows, 2 * quarter_rows, quarter_rows, 2 * rows_per, rows_per)[step]
        return (part if step < 2 else xbuf).at[pl.ds(0, rows), cols]

    def send_last(step, c):
        def both(z_first):
            for d in range(DIRS):
                start(last_messages(step, c, d, z_first))

        if step < 2:
            both(False)
            return
        z_first = jnp.logical_and(c >= 5, c % 2 == 1)

        @pl.when(z_first)
        def _():
            both(True)

        @pl.when(jnp.logical_not(z_first))
        def _():
            both(False)

    def out_store(c):
        return pltpu.make_async_copy(xbuf.at[:, block_cols(c)], out_ref.at[:, block_cols(c)], store_sem)

    def last_project(c):
        @pl.when(c + 1 < LAST_BLOCKS)
        def _():
            start(tile_loads(c + 1))

        take(tile_sem.at[c % 2], wtile.at[c % 2, :, pl.ds(0, 2 * depth), :])
        total = None
        for j in range(RING):
            z = wrap(pos_z + j)
            own = span(pos_z * rows_per, rows_per)
            hidden_rows = hid[own, :] if j == 0 else xs[1, :, span(z * ff_local, ff_local)]
            out_rows = att[own, :] if j == 0 else att_all[z]
            term = dot(hidden_rows, wtile[c % 2, j // 2, pl.ds((j % 2) * depth, ff_local), :])
            term = term + dot(out_rows, wtile[c % 2, j // 2, pl.ds((j % 2) * depth + ff_local, head_dim), :])
            total = term if total is None else total + term
        part[pl.ds(0, rows_per), block_cols(c)] = total

    def last_stage(number, c):
        cols, half = block_cols(c), quarter_rows // 2
        if number == 0:
            last_project(c)
        else:
            take(last_recv.at[c, number - 1], last_arrived(number - 1, cols))
        if number == 1:
            for d in range(DIRS):
                piece = quarter_of(wrap(pos_y + sign[d]), d * half, half)
                part[piece, cols] = part[piece, cols] + part[landed(d, quarter_rows, half), cols]
        if number == 2:
            own = quarter_of(pos_y, 0, quarter_rows)
            total = part[own, cols] + part[landed(0, 0, quarter_rows), cols] + part[landed(1, 0, quarter_rows), cols]
            update = total.astype(bf16).astype(f32)
            rows = rows_at(pos_z, pos_y, 0, quarter_rows)
            xbuf[rows, cols] = (xbuf[rows, cols].astype(f32) + update).astype(bf16)
        if number < LAST_STEPS:
            send_last(number, c)
        else:
            out_store(c).start()

    def last_tick(t, carry):
        for number in range(LAST_STEPS, -1, -1):
            c = t - LAST_GAP * number

            @pl.when(jnp.logical_and(c >= 0, c < LAST_BLOCKS))
            def _():
                last_stage(number, c)
        return carry

    lax.fori_loop(0, LAST_BLOCKS + LAST_GAP * LAST_STEPS, last_tick, 0)

    take(cache_sem, kv.at[own_rows, :])
    take(relay_send, relay_buf)
    kv_sent()
    take(part_send, xbuf.at[pl.ds(0, 3 * depth // 8), :])
    take(round_send, gd_ref.at[pl.ds(0, 2), pl.ds(0, 9 * depth // 16), :])
    take(side_send, parts_ref)
    take(give_send, given)
    for step in range(LAST_STEPS):
        take(last_send.at[step], last_arrived(step, pl.ds(0, d_model)))
    take(store_sem, xbuf)


def layers(x_loc, cos_t, sin_t, norm_gain, w_q, w_k, w_v, w_gate, w_up, w_down, w_o):
    tok_count, d_model = x_loc.shape
    head_dim = w_q.shape[2]
    ff_local = w_gate.shape[2]
    rows_per = tok_count // KV_CHUNKS
    chunk_rows = tok_count // CHUNKS
    landed = 3 * chunk_rows // (2 * RING)
    half_cols = d_model // HALVES
    any_spec = pl.BlockSpec(memory_space=pl.ANY)
    vmem_spec = pl.BlockSpec(memory_space=pltpu.VMEM)
    bf16, f32 = jnp.bfloat16, jnp.float32
    dma = pltpu.SemaphoreType.DMA
    shape = jax.ShapeDtypeStruct
    return pl.pallas_call(
        layers_kernel,
        out_shape=[shape((tok_count, d_model), bf16)] + [shape((tok_count, head_dim), bf16)] * 4
        + [shape((RING, ff_local, d_model), bf16), shape((RING, head_dim, d_model), bf16)],
        in_specs=[any_spec, vmem_spec, vmem_spec, vmem_spec] + [any_spec] * 7,
        out_specs=[any_spec] * 7,
        scratch_shapes=[
            pltpu.VMEM((tok_count, d_model), bf16),
            pltpu.VMEM((PART_SLOTS * chunk_rows, d_model), f32),
            pltpu.VMEM((RECV_SLOTS, HALVES, DIRS, landed, half_cols), f32),
            pltpu.VMEM((RECV_SLOTS, HALVES, DIRS, landed, half_cols // RING), f32),
            pltpu.VMEM((tok_count, ff_local), bf16),
            pltpu.VMEM((tok_count, head_dim), bf16),
            pltpu.VMEM((2, ff_local + head_dim, DOWN_TILE), bf16),
            pltpu.VMEM((2, 2, d_model, W_TILE), bf16),
            pltpu.VMEM((2 * CHIPS * tok_count, 2 * head_dim), bf16),
            pltpu.VMEM((tok_count, head_dim), bf16),
            pltpu.VMEM((2, tok_count, head_dim), f32),
            pltpu.VMEM((2, tok_count, 128), f32),
            pltpu.VMEM((2, tok_count, 128), f32),
            pltpu.VMEM((2, rows_per, d_model), bf16),
            pltpu.VMEM((CHUNKS, HALVES, chunk_rows // RING, half_cols // RING), bf16),
            dma((2,)), dma, dma((2, 2)), dma((2, 2)), dma, dma,
            dma((10,)), dma((4, KV_CHUNKS)), dma((4, KV_CHUNKS)), dma, dma((2,)),
            dma, dma((2, RING - 1)), dma, dma,
            dma, dma,
            pltpu.VMEM((KV_CHUNKS, rows_per, W_TILE), bf16), dma, dma,
            pltpu.VMEM((RING, rows_per, head_dim), bf16),
            dma((PART_SLOTS,)), dma((4,)), dma((RECV_SLOTS, STEPS)),
            dma((LAST_STEPS,)), dma((LAST_BLOCKS, LAST_STEPS)), dma((2,)),
            pltpu.SemaphoreType.REGULAR((3,)), pltpu.SemaphoreType.REGULAR((DIRS,)),
        ],
        compiler_params=pltpu.CompilerParams(collective_id=0, has_side_effects=True, vmem_limit_bytes=67043328),
        name='layers',
    )(x_loc, cos_t, sin_t, norm_gain, w_q, w_k, w_v, w_gate, w_up, w_down, w_o)


EMIT_PARTS = 8


def emit_kernel(x_ref, k_first, k_second, v_first, v_second, x_out, k_out, v_out, xbuf, rows, load_sem, store_sem):
    size = x_ref.shape[0] // EMIT_PARTS
    loads, stores = [], []
    for n in range(EMIT_PARTS):
        part = pl.ds(n * size, size)
        loads.append(pltpu.make_async_copy(x_ref.at[part, :], xbuf.at[part, :], load_sem.at[n]))
        stores.append(pltpu.make_async_copy(xbuf.at[part, :], x_out.at[part, :], store_sem.at[n]))
    for n, (ref, out) in enumerate(((k_first, k_out.at[0]), (k_second, k_out.at[1]), (v_first, v_out.at[0]), (v_second, v_out.at[1]))):
        loads.append(pltpu.make_async_copy(ref, rows.at[n], load_sem.at[EMIT_PARTS + n]))
        stores.append(pltpu.make_async_copy(rows.at[n], out, store_sem.at[EMIT_PARTS + n]))
    for copy in loads:
        copy.start()
    for load, store in zip(loads, stores):
        load.wait()
        store.start()
    for copy in stores:
        copy.wait()


def emit(x_out, k_first, k_second, v_first, v_second):
    any_spec = pl.BlockSpec(memory_space=pl.ANY)
    cache = jax.ShapeDtypeStruct((2,) + k_first.shape, jnp.bfloat16)
    return pl.pallas_call(
        emit_kernel,
        out_shape=[jax.ShapeDtypeStruct(x_out.shape, jnp.bfloat16), cache, cache],
        in_specs=[any_spec] * 5,
        out_specs=[any_spec] * 3,
        scratch_shapes=[
            pltpu.VMEM(x_out.shape, jnp.bfloat16),
            pltpu.VMEM((4,) + k_first.shape, jnp.bfloat16),
            pltpu.SemaphoreType.DMA((EMIT_PARTS + 4,)),
            pltpu.SemaphoreType.DMA((EMIT_PARTS + 4,)),
        ],
        compiler_params=pltpu.CompilerParams(vmem_limit_bytes=63 * 1024 * 1024),
        name='emit',
    )(x_out, k_first, k_second, v_first, v_second)


def solution(mesh):
    row_spec = P(('batch', 'seq'), None)
    pos_spec = P(('batch', 'seq'))
    head_spec = P(None, None, 'head', None)
    out_proj_spec = P(None, 'head', None, None)
    col_spec = P(None, None, 'head')
    down_spec = P(None, 'head', None)
    cache_spec = P(None, ('batch', 'seq'), 'head', None)

    def local_forward(x_loc, pos_loc, w_q, w_k, w_v, w_o, w_gate, w_up, w_down, norm_gain):
        tok_count, d_model = x_loc.shape
        layer_count = w_q.shape[0]
        head_dim = w_q.shape[3]
        flat_q, flat_k, flat_v = (w.reshape(layer_count, d_model, head_dim) for w in (w_q, w_k, w_v))
        cos_t, sin_t = rope_tables(pos_loc, head_dim)
        x_out, k_first, v_first, k_second, v_second, _, _ = layers(x_loc, cos_t, sin_t, norm_gain, flat_q, flat_k, flat_v, w_gate, w_up, w_down, w_o)
        x_out, k_all, v_all = emit(x_out, k_first, k_second, v_first, v_second)
        cache_shape = (layer_count, tok_count, 1, head_dim)
        return x_out, k_all.reshape(cache_shape), v_all.reshape(cache_shape)

    return jax.shard_map(local_forward, mesh=mesh, in_specs=(row_spec, pos_spec, head_spec, head_spec, head_spec, out_proj_spec, col_spec, col_spec, down_spec, P(None, None)), out_specs=(row_spec, cache_spec, cache_spec), check_vma=False)
```

```python
import functools
import math
import jax
import jax.numpy as jnp
from jax import lax
from jax.experimental import pallas as pl
from jax.experimental.pallas import tpu as pltpu
from jax.sharding import PartitionSpec as P

ROPE_BASE = 500000.0
EPS = 1e-5


def rope_tables(positions, head_dim):
    half_dim = head_dim // 2
    inv_freq = ROPE_BASE ** (-(jnp.arange(half_dim, dtype=jnp.float32) * 2.0 / head_dim))
    angles = positions.astype(jnp.float32)[..., None] * inv_freq
    return jnp.cos(angles), jnp.sin(angles)


CHIPS = 4
RING = 4
HALVES = 2
DIRS = 2
KV_CHUNKS = 4
W_TILE = 256
NORM_ROWS = 64
CHUNKS = 8
STEPS = 8
PART_SLOTS = 4
RECV_SLOTS = 5
DOWN_TILE = 512
START_GAP = 3
STAGE_GAP = 2
BLOCK_TICK = 19
BLOCK_GAP = 6
LAST_TICK = 43
NEAR_TICKS = ((9, 1), (15, 3))
FAR_TICKS = ((24, 1), (26, 3))
SERVE_TICKS = (27, 31, 35, 42)
GIVE_TICK = 37
OWN_TICK = 3
DONE_TICK = 11
EARLY_TICK = 31
LAST_STEPS = 6
LAST_COLS = 256
LAST_BLOCKS = 16
LAST_GAP = 3


def layers_kernel(x_ref, cos_ref, sin_ref, gain_ref, wq_ref, wk_ref, wv_ref, wg_ref, wu_ref, wd_ref, wo_ref,
                 out_ref, k1_ref, v1_ref, k2_ref, v2_ref, gd_ref, go_ref,
                 xbuf, part, recv_a, recv_b, hid, att, wdo, wtile, kv, qbuf, acc, row_max, row_sum, xs, xres,
                 x_sem, res_sem, w_sem, down_sem, cache_sem, store_sem, kv_send, ici_recv, core_recv, part_send, part_recv,
                 round_send, round_recv, side_send, side_recv, give_send, give_recv, relay_buf, relay_send, relay_recv, att_all, ring_send, gather_send, ring_recv,
                 last_send, last_recv, tile_sem, ready_sem, drained_sem):
    tok_count, d_model = xbuf.shape
    head_dim = qbuf.shape[1]
    half_dim = head_dim // 2
    ff_local = hid.shape[1]
    depth = ff_local + head_dim
    rows_per = tok_count // KV_CHUNKS
    half_rows = tok_count // 2
    lanes = row_max.shape[2]
    chunk_rows = tok_count // CHUNKS
    quarter, eighth = chunk_rows // RING, chunk_rows // (2 * RING)
    half_cols = d_model // HALVES
    piece_cols = half_cols // RING
    bf16, f32 = jnp.bfloat16, jnp.float32
    sign = (1, -1)
    mesh_id = pl.DeviceIdType.MESH

    my_head = lax.axis_index('head')
    pos_z, pos_y = my_head // RING, my_head % RING
    my_seq = lax.axis_index('seq')
    chip, core = my_seq // 2, my_seq % 2
    other = chip * 2 + 1 - core

    def wrap(n):
        return (n + RING) % RING

    def y_peer(d):
        return pos_z * RING + wrap(pos_y + sign[d])

    def z_device(z):
        return wrap(z) * RING + pos_y

    def z_peer(d):
        return z_device(pos_z + sign[d])

    def x_device(n):
        return wrap(chip + n) * 2 + core

    right, left = x_device(1), x_device(-1)

    def span(start, size, unit=None):
        return pl.ds(pl.multiple_of(start, unit or size), size)

    def remote(src, dst, send, recv, **to):
        return pltpu.make_async_remote_copy(src_ref=src, dst_ref=dst, send_sem=send, recv_sem=recv, device_id=to, device_id_type=mesh_id)

    def take(sem, ref):
        remote(ref, ref, sem, sem, head=my_head).wait_recv()

    def x_load(i):
        return pltpu.make_async_copy(x_ref.at[span(i * rows_per, rows_per), :], xs.at[i % 2], x_sem.at[i % 2])

    def weights(layer, piece):
        slot = piece % 2
        if isinstance(piece, int) and piece < 2:
            refs = ((wk_ref, wv_ref), (wq_ref,))[piece]
            return [pltpu.make_async_copy(ref.at[layer], wtile.at[slot, n], w_sem.at[slot, n]) for n, ref in enumerate(refs)]
        cols = span((piece - 2) * W_TILE, W_TILE)
        return [pltpu.make_async_copy(ref.at[layer, :, cols], wtile.at[slot, n], w_sem.at[slot, n]) for n, ref in enumerate((wg_ref, wu_ref))]

    def start(copies):
        for copy in copies:
            copy.start()

    def wait(copies):
        for copy in copies:
            copy.wait()

    down_tiles = d_model // DOWN_TILE

    def down_load(i):
        cols = span(i * DOWN_TILE, DOWN_TILE)
        return [pltpu.make_async_copy(wd_ref.at[0, :, cols], wdo.at[i % 2, pl.ds(0, ff_local), :], down_sem.at[i % 2, 0]),
                pltpu.make_async_copy(wo_ref.at[0, 0, :, cols], wdo.at[i % 2, pl.ds(ff_local, head_dim), :], down_sem.at[i % 2, 1])]

    def kv_copy(origin_chip, origin_core, i, to, send, recv):
        rows = kv.at[span((origin_chip * 2 + origin_core) * tok_count + i * rows_per, rows_per), :]
        return remote(rows, rows, send, recv, seq=to)

    def kv_routes(i):
        def to(number, recv, origin_chip, origin_core, device):
            return lambda: kv_copy(origin_chip, origin_core, i, device, kv_send.at[number], recv)
        inner = jnp.logical_and(chip >= 1, chip < CHIPS - 1)
        return {
            'right': (chip < CHIPS - 1, 'all', to(0, ici_recv.at[0, i], chip, core, right)),
            'wrap': (chip == 0, 'all', to(1, ici_recv.at[2, i], chip, core, left)),
            'relay': (chip == 1, 'late', to(2, ici_recv.at[3, i], chip, core, left)),
            'other': (core == 0, 'all', to(3, core_recv.at[0, i], chip, core, other)),
            'on_right': (inner, 'early', to(4, ici_recv.at[1, i], chip - 1, core, right)),
            'from_relay': (chip == 0, 'late', to(5, ici_recv.at[1, i], 1, core, left)),
            'on_left': (chip == CHIPS - 1, 'late', to(6, ici_recv.at[1, i], 0, core, left)),
            'side1': (chip >= 1, 'all', to(7, core_recv.at[1, i], chip - 1, core, other)),
            'side2': (chip >= 2, 'all', to(8, core_recv.at[2, i], chip - 2, core, other)),
            'side3': (chip >= 3, 'all', to(9, core_recv.at[3, i], chip - 3, core, other)),
        }

    def start_route(i, name):
        condition, which, copy = kv_routes(i)[name]
        if which != 'all':
            late = i >= KV_CHUNKS // 2
            if isinstance(i, int):
                if late != (which == 'late'):
                    return
            else:
                condition = jnp.logical_and(condition, late if which == 'late' else jnp.logical_not(late))

        @pl.when(condition)
        def _():
            copy().start()

    def send_kv(i):
        for name in ('right', 'wrap', 'relay', 'other'):
            start_route(i, name)

    def kv_sent():
        for number, (condition, which, _) in enumerate(kv_routes(0).values()):
            @pl.when(condition)
            def _():
                take(kv_send.at[number], kv.at[pl.ds(0, tok_count if which == 'all' else half_rows), :])

    def serve(back, i):
        @pl.when(chip >= back)
        def _():
            kv_copy(chip - back, core, i, other, kv_send.at[0], ici_recv.at[back - 1, i]).wait_recv()
        start_route(i, 'side%d' % back)
        if back == 1:
            start_route(i, 'on_right')
        if back == 3:
            start_route(i, 'on_left')

    def relay(i):
        def pass_on():
            @pl.when(chip == 0)
            def _():
                kv_copy(1, core, i, left, kv_send.at[0], ici_recv.at[3, i]).wait_recv()
            start_route(i, 'from_relay')
        if not isinstance(i, int):
            pl.when(i >= KV_CHUNKS // 2)(pass_on)
        elif i >= KV_CHUNKS // 2:
            pass_on()

    def serve_all(i):
        serve(1, i)
        serve(3, i)
        relay(i)

    def taken(back, chunks):
        for i in chunks:
            kv_copy(chip - back, 1 - core, i, other, kv_send.at[0], core_recv.at[back, i]).wait_recv()

    def z_parts(step, d):
        copies = []
        for n, (own_ref, all_ref) in enumerate(((wd_ref, gd_ref), (wo_ref, go_ref))):
            size = all_ref.shape[1] // (2 * CHIPS)
            if step == 0:
                rows = span(my_seq * size, size)
                src = own_ref.at[1, rows, :] if n == 0 else own_ref.at[1, 0, rows, :]
                dst = all_ref.at[pos_z, rows, :]
            else:
                rows = span(my_seq * size + d * (size // 2), size // 2)
                src = dst = all_ref.at[wrap(pos_z - sign[d]), rows, :]
            copies.append(remote(src, dst, part_send, part_recv.at[step], head=z_peer(d)))
        return copies

    def part_copies(j, part_chip, part_core, half, send, recv, to):
        copies = []
        for n, ref in enumerate((gd_ref, go_ref)):
            size = ref.shape[1] // (2 * CHIPS)
            first = (part_chip * 2 + part_core) * size
            rows = span(first, size) if half is None else span(first + half * (size // 2), size // 2)
            place = ref.at[wrap(pos_z + j), rows, :]
            copies.append(remote(place, place, send, recv, seq=to))
        return copies

    def own_part(j, d):
        return part_copies(j, chip, core, None, round_send, round_recv.at[0, j - 1], x_device(sign[d]))

    def far_part(j, d):
        return part_copies(j, wrap(chip - sign[d]), core, d, round_send, round_recv.at[1, j - 1], x_device(sign[d]))

    def side_part(j, n, side):
        return part_copies(j, wrap(chip + n), side, None, side_send, side_recv, other)

    def round_start(j):
        for d in range(DIRS):
            start(own_part(j, d))
        start(side_part(j, 0, core))

    def near_parts(j):
        take(round_recv.at[0, j - 1], xbuf.at[pl.ds(0, depth // CHIPS), :])
        for d in range(DIRS):
            start(far_part(j, d) + side_part(j, 3 if d == 0 else 1, core))

    def far_parts(j):
        take(round_recv.at[1, j - 1], xbuf.at[pl.ds(0, depth // (2 * CHIPS)), :])
        start(side_part(j, 2, core))

    def give_hidden(z, i, source):
        cols = span(i * W_TILE, W_TILE)
        return remote(hid.at[span(z * rows_per, rows_per), cols], hidden_place(source, i), give_send, give_recv, head=z_device(z))

    def hidden_place(source, i):
        return xs.at[1, :, span(source * ff_local + i * W_TILE, W_TILE)]

    def via_neighbor(z, i):
        step = jnp.where(i < KV_CHUNKS // 2, 1, -1)
        return remote(hid.at[span(z * rows_per, rows_per), span(i * W_TILE, W_TILE)], relay_buf.at[i], give_send, relay_recv, head=z_device(pos_z + step))

    def relay_hidden(i):
        step = 1 if i < KV_CHUNKS // 2 else -1
        source = wrap(pos_z - step)
        return remote(relay_buf.at[i], hidden_place(source, i), relay_send, give_recv, head=z_device(pos_z + step))

    def send_hidden(z, i):
        away = wrap(z - pos_z)

        @pl.when(away == 2)
        def _():
            via_neighbor(z, i).start()

        @pl.when(away % 2 == 1)
        def _():
            give_hidden(z, i, pos_z).start()

    def give_rows(z, source):
        return remote(att.at[span(z * rows_per, rows_per), :], att_all.at[source], give_send, give_recv, head=z_device(z))

    def norm_rows(x_few, layer):
        x_f32 = x_few.astype(f32)
        inv_rms = lax.rsqrt(jnp.mean(x_f32 * x_f32, axis=-1, keepdims=True) + EPS)
        return (x_f32 * inv_rms * gain_ref[pl.ds(layer, 1), :].astype(f32)).astype(bf16)

    def rope(values, rows):
        cos_t, sin_t = cos_ref[rows, :], sin_ref[rows, :]
        wide = values.astype(bf16).astype(f32)
        first, second = wide[:, :half_dim], wide[:, half_dim:]
        return jnp.concatenate([first * cos_t - second * sin_t, second * cos_t + first * sin_t], axis=1).astype(bf16)

    def dot(a, b):
        return jnp.dot(a, b, preferred_element_type=f32)

    scale = 1.0 / math.sqrt(head_dim)

    def keys_values(normed, i):
        rows = span(i * rows_per, rows_per)
        own = span(my_seq * tok_count + i * rows_per, rows_per)
        kv[own, :head_dim] = rope(dot(normed, wtile[0, 0]), rows)
        kv[own, head_dim:] = dot(normed, wtile[0, 1]).astype(bf16)

    def queries(normed, i):
        rows = span(i * rows_per, rows_per)
        qbuf[rows, :] = (rope(dot(normed, wtile[1, 0]), rows).astype(f32) * scale).astype(bf16)

    def gated(normed, i, tile):
        gate = dot(normed, wtile[tile % 2, 0])
        up = dot(normed, wtile[tile % 2, 1])
        hid[span(i * rows_per, rows_per), span(tile * W_TILE, W_TILE)] = (gate * jax.nn.sigmoid(gate) * up).astype(bf16)

    def attend(key_start, q_half, side, masked, first):
        rows = pl.ds(q_half * half_rows, half_rows)
        some = span(key_start, half_rows)
        logits = lax.dot_general(qbuf[rows, :], kv[some, :head_dim], (((1,), (1,)), ((), ())), preferred_element_type=f32)
        if masked:
            seen = lax.broadcasted_iota(jnp.int32, logits.shape, 0) >= lax.broadcasted_iota(jnp.int32, logits.shape, 1)
            logits = jnp.where(seen, logits, -jnp.inf)
        block_max = jnp.max(logits, axis=-1, keepdims=True)
        if first:
            new_max = jnp.broadcast_to(block_max, (half_rows, lanes))
        else:
            new_max = jnp.maximum(row_max[side, rows, :], block_max)
        prob = jnp.exp(logits - jnp.concatenate([new_max] * (half_rows // lanes), axis=1))
        block_sum = jnp.sum(prob, axis=-1, keepdims=True)
        block_out = dot(prob.astype(bf16), kv[some, head_dim:])
        if first:
            row_sum[side, rows, :] = jnp.broadcast_to(block_sum, (half_rows, lanes))
            acc[side, rows, :] = block_out
        else:
            rescale = jnp.exp(row_max[side, rows, :] - new_max)
            row_sum[side, rows, :] = row_sum[side, rows, :] * rescale + block_sum
            acc[side, rows, :] = acc[side, rows, :] * jnp.concatenate([rescale] * (head_dim // lanes), axis=1) + block_out
        row_max[side, rows, :] = new_max

    def attend_own(layer_half):
        own_start = my_seq * tok_count
        if layer_half == 0:
            attend(own_start, 0, 0, True, True)
            top_rows = pl.ds(0, half_rows)
            row_max[1, top_rows, :] = jnp.full((half_rows, lanes), -jnp.inf, f32)
            row_sum[1, top_rows, :] = jnp.zeros((half_rows, lanes), f32)
            acc[1, top_rows, :] = jnp.zeros((half_rows, head_dim), f32)
        else:
            attend(own_start, 1, 0, False, True)
            attend(own_start + half_rows, 1, 1, True, True)

    def past_start(n):
        later = n - core
        back = jnp.where(later < 2, 1, jnp.where(chip == CHIPS - 1, jnp.where(later < 4, 3, 2), 2))
        block = (chip - back) * 2 + jnp.where(later % 2 == 0, core, 1 - core)
        return jnp.where(jnp.logical_and(core == 1, n == 0), chip * 2, block) * tok_count

    def arrivals(n, chunks):
        @pl.when(jnp.logical_and(core == 1, n == 0))
        def _():
            taken(0, chunks)

        for back in (1, 3, 2):
            place = 0 if back == 1 else 2 if back == 3 else jnp.where(chip == CHIPS - 1, 4, 2)
            if back == 2:
                @pl.when(jnp.logical_and(chip >= back, n == core + place))
                def _():
                    for i in chunks:
                        serve(2, i)

            @pl.when(jnp.logical_and(chip >= back, n == core + place + 1))
            def _():
                taken(back, chunks)

    def visit(n, visits):
        for q_half, side in visits:
            attend(past_start(n) + side * half_rows, q_half, side, False, False)

    def attend_past(first_n, last_n, chunks, visits):
        def past(n, carry):
            if chunks:
                arrivals(n, chunks)
            visit(n, visits)
            return carry

        lax.fori_loop(first_n, last_n, past, 0)

    few_near = jnp.minimum(my_seq, 1)
    near_count = my_seq - jnp.where(chip >= 2, 2, 0)

    def finish(i, spread):
        rows = pl.ds(i * rows_per, rows_per)
        top = jnp.maximum(row_max[0, rows, :], row_max[1, rows, :])
        shares = [jnp.exp(row_max[side, rows, :] - top) for side in range(2)]
        total = shares[0] * row_sum[0, rows, :] + shares[1] * row_sum[1, rows, :]
        wide = [jnp.concatenate([w] * (head_dim // lanes), axis=1) for w in shares + [total]]
        att[rows, :] = ((acc[0, rows, :] * wide[0] + acc[1, rows, :] * wide[1]) / wide[2]).astype(bf16)
        if spread:
            @pl.when(i != pos_z)
            def _():
                give_rows(i, pos_z).start()

    first_pos, second_pos = (pos_y, pos_z), (pos_z, pos_y)
    first_peer, second_peer = (y_peer, z_peer), (z_peer, y_peer)

    def part_rows(chunk, piece, offset, count):
        return span((chunk % PART_SLOTS) * chunk_rows + piece * quarter + offset, count, eighth)

    def x_rows(chunk, piece, offset, count):
        return span(chunk * chunk_rows + piece * quarter + offset, count, eighth)

    def cols_of(h, piece):
        return span(h * half_cols + piece * piece_cols, piece_cols)

    def half_of(h):
        return pl.ds(h * half_cols, half_cols)

    def ring_copies(step, chunk, h, d):
        p1, p2, s = first_pos[h], second_pos[h], sign[d]
        slot, mine, rest = chunk % RECV_SLOTS, d * eighth, (1 - d) * eighth
        if step < 4:
            box, piece_of, cols = (recv_a, wrap(p1 + s), half_of(h)) if step < 2 else (recv_b, p1, cols_of(h, wrap(p2 + s)))
            far_piece, far_cols = (wrap(p1 + 2), half_of(h)) if step < 2 else (p1, cols_of(h, wrap(p2 + 2)))
            if step % 2 == 0:
                places = [(part.at[part_rows(chunk, far_piece, mine, eighth), far_cols], box.at[slot, h, d, pl.ds(quarter, eighth), :]),
                          (part.at[part_rows(chunk, piece_of, rest, eighth), cols], box.at[slot, h, d, pl.ds(rest, eighth), :])]
            else:
                places = [(part.at[part_rows(chunk, piece_of, mine, eighth), cols], box.at[slot, h, d, pl.ds(mine, eighth), :])]
        else:
            piece_of, cols = (p1, cols_of(h, p2 if step == 4 else wrap(p2 - s))) if step < 6 else (p1 if step == 6 else wrap(p1 - s), half_of(h))
            refs = [xbuf.at[x_rows(chunk, piece_of, offset, eighth), cols] for offset in ((mine, rest) if step % 2 == 0 else (mine,))]
            places = [(ref, ref) for ref in refs]
        peer = (first_peer if step in (0, 1, 6, 7) else second_peer)[h](d)
        return [remote(src, dst, ring_send.at[chunk % PART_SLOTS] if step < 4 else gather_send.at[step + n - 4], ring_recv.at[slot, step + n], head=peer)
                for n, (src, dst) in enumerate(places)]

    def arrived_in(step, count=1):
        rows = (2 * eighth, 2 * quarter, eighth // 2, quarter // 2, quarter // 2, quarter // 2, quarter, 2 * quarter)[step] * count
        return (part if step < 4 else xbuf).at[pl.ds(0, rows), pl.ds(0, half_cols if step == 4 else d_model)]

    def partials_sent(slot):
        take(ring_send.at[slot], part.at[pl.ds(0, 2 * eighth + 2 * quarter + eighth // 2 + quarter // 2), :])

    def residual_load(chunk, h):
        return pltpu.make_async_copy(x_ref.at[x_rows(chunk, first_pos[h], 0, quarter), cols_of(h, second_pos[h])], xres.at[chunk, h], res_sem)

    def project(chunk):
        rows = span(chunk * chunk_rows, chunk_rows)
        slot_rows = span((chunk % PART_SLOTS) * chunk_rows, chunk_rows)

        def one_tile(i, carry):
            @pl.when(jnp.logical_or(chunk < CHUNKS - 1, i < down_tiles - 1))
            def _():
                start(down_load((i + 1) % down_tiles))

            wait(down_load(i))
            total = dot(hid[rows, :], wdo[i % 2, :ff_local, :])
            part[slot_rows, span(i * DOWN_TILE, DOWN_TILE)] = total + dot(att[rows, :], wdo[i % 2, ff_local:, :])
            return carry

        lax.fori_loop(0, down_tiles, one_tile, 0)

    def stage(number, chunk):
        slot = chunk % RECV_SLOTS
        if number == 0:
            @pl.when(chunk >= PART_SLOTS)
            def _():
                partials_sent(chunk % PART_SLOTS)
            project(chunk)
        else:
            take(ring_recv.at[slot, number - 1], arrived_in(number - 1))
        if number == 4:
            @pl.when(chunk == 0)
            def _():
                take(res_sem, xres)
        for h in range(HALVES):
            p1, p2 = first_pos[h], second_pos[h]
            if number in (1, 3):
                for d in range(DIRS):
                    if number == 1:
                        rows, cols, arrived = part_rows(chunk, wrap(p1 + sign[d]), d * eighth, eighth), half_of(h), recv_a
                    else:
                        rows, cols, arrived = part_rows(chunk, p1, d * eighth, eighth), cols_of(h, wrap(p2 + sign[d])), recv_b
                    part[rows, cols] = part[rows, cols] + arrived[slot, h, d, pl.ds(quarter, eighth), :]
            if number == 2:
                rows = part_rows(chunk, p1, 0, quarter)
                part[rows, half_of(h)] = part[rows, half_of(h)] + recv_a[slot, h, 0, pl.ds(0, quarter), :] + recv_a[slot, h, 1, pl.ds(0, quarter), :]
            if number == 4:
                rows, cols = part_rows(chunk, p1, 0, quarter), cols_of(h, p2)
                total = part[rows, cols] + recv_b[slot, h, 0, pl.ds(0, quarter), :] + recv_b[slot, h, 1, pl.ds(0, quarter), :]
                update = total.astype(bf16).astype(f32)
                xbuf[x_rows(chunk, p1, 0, quarter), cols] = (xres[chunk, h].astype(f32) + update).astype(bf16)
        if number < STEPS:
            copies = [ring_copies(number, chunk, h, d) for h in range(HALVES) for d in range(DIRS)]
            for n in range(len(copies[0])):
                start([copy[n] for copy in copies])

    x_load(0).start()
    start(weights(0, 0))
    x_load(1).start()
    start(weights(0, 1))
    barrier = pltpu.get_barrier_semaphore()
    for peer in (left, right, other):
        pl.semaphore_signal(barrier, inc=1, device_id={'seq': peer}, device_id_type=mesh_id)
    for peer in [z_device(pos_z + j) for j in range(1, RING)] + [y_peer(d) for d in range(DIRS)]:
        pl.semaphore_signal(barrier, inc=1, device_id={'head': peer}, device_id_type=mesh_id)
    pl.semaphore_wait(barrier, 8)
    for d in range(DIRS):
        start(z_parts(0, d))

    def prepare(i, carry):
        x_load(i).wait()

        def few(n, inner):
            xbuf[span(i * rows_per + n * NORM_ROWS, NORM_ROWS), :] = norm_rows(xs[i % 2, span(n * NORM_ROWS, NORM_ROWS), :], 0)
            return inner

        lax.fori_loop(0, rows_per // NORM_ROWS, few, 0)

        @pl.when(i + 2 < KV_CHUNKS)
        def _():
            x_load(i + 2).start()

        @pl.when(i == 0)
        def _():
            wait(weights(0, 0))

        keys_values(xbuf[span(i * rows_per, rows_per), :], i)
        send_kv(i)
        return carry

    lax.fori_loop(0, KV_CHUNKS, prepare, 0)
    start(weights(0, 2))
    own_rows = span(my_seq * tok_count, tok_count)

    def cache_stores(layer):
        k_ref, v_ref = ((k1_ref, v1_ref), (k2_ref, v2_ref))[layer]
        return [pltpu.make_async_copy(kv.at[own_rows, pl.ds(0, head_dim)], k_ref, cache_sem),
                pltpu.make_async_copy(kv.at[own_rows, pl.ds(head_dim, head_dim)], v_ref, cache_sem)]

    start(cache_stores(0))
    wait(weights(0, 1))

    def query(i, carry):
        queries(xbuf[span(i * rows_per, rows_per), :], i)
        return carry

    lax.fori_loop(0, KV_CHUNKS, query, 0)
    start(weights(0, 3))
    start(down_load(0))

    def residuals(n, carry):
        for h in range(HALVES):
            residual_load(n, h).start()
        return carry

    lax.fori_loop(0, CHUNKS, residuals, 0)

    def gate_half(half, tile):
        wait(weights(0, tile + 2))

        def rows_step(i, inner):
            gated(xbuf[span(i * rows_per, rows_per), :], i, tile)
            return inner

        lax.fori_loop(half * KV_CHUNKS // 2, (half + 1) * KV_CHUNKS // 2, rows_step, 0)

        @pl.when(tile < 2)
        def _():
            start(weights(0, tile + 4))

        for last in (2, 3):
            @pl.when(tile == last)
            def _():
                start(weights(1, last - 2) if half else weights(0, last))

    def first_half(tile, carry):
        gate_half(0, tile)

        @pl.when(tile < 3)
        def _():
            serve_all(tile)
        return carry

    def second_half(tile, carry):
        gate_half(1, tile)

        @pl.when(tile == 0)
        def _():
            serve_all(3)
            attend_past(0, few_near, range(KV_CHUNKS), ((0, 0), (0, 1)))
            take(part_recv.at[0], xbuf.at[pl.ds(0, depth // CHIPS), :])
            for d in range(DIRS):
                start(z_parts(1, d))
            attend_past(few_near, near_count, range(KV_CHUNKS), ((0, 0), (0, 1)))
        return carry

    lax.fori_loop(0, ff_local // W_TILE, first_half, 0)
    attend_own(0)
    lax.fori_loop(0, 2, second_half, 0)
    attend_past(near_count, my_seq, range(KV_CHUNKS), ((0, 0), (0, 1)))
    finish(0, False)
    finish(1, False)
    round_start(1)
    round_start(3)

    def block_work(j, phase):
        @pl.when(phase == 0)
        def _():
            @pl.when(j == 0)
            def _():
                for n in range(3):
                    pl.semaphore_wait(ready_sem.at[n], 1)

            def few(n, inner):
                xs[0, span(n * NORM_ROWS, NORM_ROWS), :] = norm_rows(xbuf[span(j * rows_per + n * NORM_ROWS, NORM_ROWS), :], 1)
                return inner

            lax.fori_loop(0, rows_per // NORM_ROWS, few, 0)
            wait(weights(1, 0))
            keys_values(xs[0], j)
            send_kv(j)
            start(weights(1, 2))

        @pl.when(phase == 1)
        def _():
            wait(weights(1, 1))
            queries(xs[0], j)
            start(weights(1, 3))

        @pl.when(jnp.logical_and(phase >= 1, phase <= 4))
        def _():
            tile = phase - 1
            wait(weights(1, tile + 2))
            gated(xs[0], j, tile)

            @pl.when(tile < 2)
            def _():
                start(weights(1, tile + 4))

            @pl.when(jnp.logical_and(tile == 2, j < KV_CHUNKS - 1))
            def _():
                start(weights(1, 0))

            @pl.when(jnp.logical_and(tile == 3, j < KV_CHUNKS - 1))
            def _():
                start(weights(1, 1))

            @pl.when(j == KV_CHUNKS - 1)
            def _():
                send_hidden(j, tile)

    def tick(t, carry):
        for number in range(STEPS, -1, -1):
            place = t - STAGE_GAP * number
            chunk = place // START_GAP

            @pl.when(jnp.logical_and(place >= 0, jnp.logical_and(place % START_GAP == 0, chunk < CHUNKS)))
            def _():
                stage(number, chunk)

        @pl.when(jnp.logical_or(t == 1, t == 3))
        def _():
            gate_half(1, 2 + t // 2)

        @pl.when(t == OWN_TICK)
        def _():
            attend_own(1)

        @pl.when(jnp.logical_and(t > OWN_TICK, jnp.logical_and(t < DONE_TICK, t - OWN_TICK <= my_seq)))
        def _():
            visit(t - OWN_TICK - 1, ((1, 0), (1, 1)))

        @pl.when(t == EARLY_TICK)
        def _():
            attend_own(0)

        early = t - EARLY_TICK - 1

        @pl.when(jnp.logical_and(early >= 0, jnp.logical_and(early < 7, early < my_seq)))
        def _():
            arrivals(early, (0, 1))
            visit(early, ((0, 0),))

        @pl.when(t == 2)
        def _():
            take(part_recv.at[1], xbuf.at[pl.ds(0, depth // (2 * CHIPS)), :])
            round_start(2)

        @pl.when(t == DONE_TICK)
        def _():
            finish(2, False)
            finish(3, False)
            kv_sent()
            take(cache_sem, kv.at[own_rows, :])
            for n, peer in enumerate((left, right, other)):
                pl.semaphore_signal(ready_sem.at[n], inc=1, device_id={'seq': peer}, device_id_type=mesh_id)

        for when, j in NEAR_TICKS:
            @pl.when(t == when)
            def _():
                near_parts(j)

        for when, j in FAR_TICKS:
            @pl.when(t == when)
            def _():
                far_parts(j)

        @pl.when(t == GIVE_TICK)
        def _():
            for i in range(KV_CHUNKS):
                for z in range(KV_CHUNKS - 1):
                    send_hidden(z, i)

        late = t - BLOCK_TICK

        @pl.when(late >= 0)
        def _():
            block_work(late // BLOCK_GAP, late % BLOCK_GAP)

        for i, when in enumerate(SERVE_TICKS):
            @pl.when(t == when)
            def _():
                serve_all(i)
        return carry

    lax.fori_loop(0, LAST_TICK, tick, 0)

    for slot in range(PART_SLOTS):
        partials_sent(slot)
    for step in range(4, STEPS):
        take(gather_send.at[step - 4], arrived_in(step, CHUNKS))
    for d in range(DIRS):
        pl.semaphore_signal(drained_sem.at[d], inc=1, device_id={'head': y_peer(d)}, device_id_type=mesh_id)
    start(cache_stores(1))
    near_parts(2)
    attend_own(1)
    attend_past(0, my_seq, (), ((1, 0),))
    take(relay_recv, relay_buf)
    for i in range(KV_CHUNKS):
        relay_hidden(i).start()
    attend_past(0, near_count, (2, 3), ((0, 1), (1, 1)))
    attend_past(near_count, my_seq, (2, 3), ((0, 1),))
    finish(0, True)
    finish(1, True)
    attend_past(near_count, my_seq, (), ((1, 1),))
    finish(2, True)
    finish(3, True)
    far_parts(2)
    parts_ref = gd_ref.at[pl.ds(0, 2), pl.ds(0, 3 * depth // 4), :]
    take(side_recv, parts_ref)

    quarter_rows = rows_per // RING

    def block_cols(c):
        return span(c * LAST_COLS, LAST_COLS)

    def tile_place(c, j, first, size):
        return wtile.at[c % 2, j // 2, pl.ds((j % 2) * depth + first, size), :]

    def tile_loads(c):
        copies = []
        for j in range(RING):
            z = wrap(pos_z + j)
            down = wd_ref.at[1, :, block_cols(c)] if j == 0 else gd_ref.at[z, :, block_cols(c)]
            out = wo_ref.at[1, 0, :, block_cols(c)] if j == 0 else go_ref.at[z, :, block_cols(c)]
            copies.append(pltpu.make_async_copy(down, tile_place(c, j, 0, ff_local), tile_sem.at[c % 2]))
            copies.append(pltpu.make_async_copy(out, tile_place(c, j, ff_local, head_dim), tile_sem.at[c % 2]))
        return copies

    start(tile_loads(0))
    given = hid.at[pl.ds(0, (RING - 1) * rows_per * depth // ff_local), :]
    take(give_recv, given)
    for d in range(DIRS):
        pl.semaphore_wait(drained_sem.at[d], 1)

    def quarter_of(piece, offset, size):
        return span(piece * quarter_rows + offset, size, quarter_rows // 2)

    def landed(d, first, size):
        return pl.ds(rows_per + d * (3 * quarter_rows // 2) + first, size)

    def rows_at(z, piece, offset, size):
        return span(z * rows_per + piece * quarter_rows + offset, size, quarter_rows // 2)

    def last_messages(step, c, d, z_first):
        s, cols, half = sign[d], block_cols(c), quarter_rows // 2
        near, behind, back = wrap(pos_y + s), wrap(pos_y - s), wrap(pos_z - s)
        mine, rest = d * half, (1 - d) * half
        along_y = step < 2 or (step < 4) != z_first
        if step == 0:
            groups = [[(part.at[quarter_of(wrap(pos_y + 2), mine, half), cols], part.at[landed(d, quarter_rows, half), cols])],
                      [(part.at[quarter_of(near, rest, half), cols], part.at[landed(d, rest, half), cols])]]
        elif step == 1:
            groups = [[(part.at[quarter_of(near, mine, half), cols], part.at[landed(d, mine, half), cols])]]
        else:
            if step == 2:
                rows = [[rows_at(pos_z, pos_y, offset, half)] for offset in (mine, rest)]
            elif step == 3:
                rows = [[rows_at(back, pos_y, mine, half) if z_first else rows_at(pos_z, behind, mine, half)]]
            elif step == 4:
                rows = [[rows_at(z, pos_y, offset, half) for z in range(RING)] if z_first else [rows_at(pos_z, 0, 4 * offset, 4 * half)] for offset in (mine, rest)]
            else:
                rows = [[rows_at(z, behind, mine, half) for z in range(RING)] if z_first else [rows_at(back, 0, 4 * mine, 4 * half)]]
            groups = [[(xbuf.at[r, cols], xbuf.at[r, cols]) for r in group] for group in rows]
        to = (y_peer if along_y else z_peer)(d)
        return [[remote(src, dst, last_send.at[step + n], last_recv.at[c, step + n], head=to) for src, dst in group] for n, group in enumerate(groups)]

    def last_arrived(step, cols):
        rows = (quarter_rows, 2 * quarter_rows, quarter_rows, 2 * quarter_rows, rows_per, 2 * rows_per)[step]
        return (part if step < 2 else xbuf).at[pl.ds(0, rows), cols]

    def send_last(step, c):
        def both(z_first):
            copies = [last_messages(step, c, d, z_first) for d in range(DIRS)]
            for n in range(len(copies[0])):
                for d in range(DIRS):
                    start(copies[d][n])

        if step < 2:
            both(False)
            return
        z_first = jnp.logical_and(c >= 5, c % 2 == 1)

        @pl.when(z_first)
        def _():
            both(True)

        @pl.when(jnp.logical_not(z_first))
        def _():
            both(False)

    def out_store(c):
        return pltpu.make_async_copy(xbuf.at[:, block_cols(c)], out_ref.at[:, block_cols(c)], store_sem)

    def last_project(c):
        @pl.when(c + 1 < LAST_BLOCKS)
        def _():
            start(tile_loads(c + 1))

        take(tile_sem.at[c % 2], wtile.at[c % 2, :, pl.ds(0, 2 * depth), :])
        total = None
        for j in range(RING):
            z = wrap(pos_z + j)
            own = span(pos_z * rows_per, rows_per)
            hidden_rows = hid[own, :] if j == 0 else xs[1, :, span(z * ff_local, ff_local)]
            out_rows = att[own, :] if j == 0 else att_all[z]
            term = dot(hidden_rows, wtile[c % 2, j // 2, pl.ds((j % 2) * depth, ff_local), :])
            term = term + dot(out_rows, wtile[c % 2, j // 2, pl.ds((j % 2) * depth + ff_local, head_dim), :])
            total = term if total is None else total + term
        part[pl.ds(0, rows_per), block_cols(c)] = total

    def last_stage(number, c):
        cols, half = block_cols(c), quarter_rows // 2
        if number == 0:
            last_project(c)
        else:
            take(last_recv.at[c, number - 1], last_arrived(number - 1, cols))
        if number == 1:
            for d in range(DIRS):
                piece = quarter_of(wrap(pos_y + sign[d]), d * half, half)
                part[piece, cols] = part[piece, cols] + part[landed(d, quarter_rows, half), cols]
        if number == 2:
            own = quarter_of(pos_y, 0, quarter_rows)
            total = part[own, cols] + part[landed(0, 0, quarter_rows), cols] + part[landed(1, 0, quarter_rows), cols]
            update = total.astype(bf16).astype(f32)
            rows = rows_at(pos_z, pos_y, 0, quarter_rows)
            xbuf[rows, cols] = (xbuf[rows, cols].astype(f32) + update).astype(bf16)
        if number < LAST_STEPS:
            send_last(number, c)
        else:
            out_store(c).start()

    def last_tick(t, carry):
        for number in range(LAST_STEPS, -1, -1):
            c = t - LAST_GAP * number

            @pl.when(jnp.logical_and(c >= 0, c < LAST_BLOCKS))
            def _():
                last_stage(number, c)
        return carry

    lax.fori_loop(0, LAST_BLOCKS + LAST_GAP * LAST_STEPS, last_tick, 0)

    take(cache_sem, kv.at[own_rows, :])
    take(relay_send, relay_buf)
    kv_sent()
    take(part_send, xbuf.at[pl.ds(0, 3 * depth // 8), :])
    take(round_send, gd_ref.at[pl.ds(0, 2), pl.ds(0, 9 * depth // 16), :])
    take(side_send, parts_ref)
    take(give_send, given)
    for step in range(LAST_STEPS):
        take(last_send.at[step], last_arrived(step, pl.ds(0, d_model)))
    take(store_sem, xbuf)


def layers(x_loc, cos_t, sin_t, norm_gain, w_q, w_k, w_v, w_gate, w_up, w_down, w_o):
    tok_count, d_model = x_loc.shape
    head_dim = w_q.shape[2]
    ff_local = w_gate.shape[2]
    rows_per = tok_count // KV_CHUNKS
    chunk_rows = tok_count // CHUNKS
    landed = 3 * chunk_rows // (2 * RING)
    half_cols = d_model // HALVES
    any_spec = pl.BlockSpec(memory_space=pl.ANY)
    vmem_spec = pl.BlockSpec(memory_space=pltpu.VMEM)
    bf16, f32 = jnp.bfloat16, jnp.float32
    dma = pltpu.SemaphoreType.DMA
    shape = jax.ShapeDtypeStruct
    return pl.pallas_call(
        layers_kernel,
        out_shape=[shape((tok_count, d_model), bf16)] + [shape((tok_count, head_dim), bf16)] * 4
        + [shape((RING, ff_local, d_model), bf16), shape((RING, head_dim, d_model), bf16)],
        in_specs=[any_spec, vmem_spec, vmem_spec, vmem_spec] + [any_spec] * 7,
        out_specs=[any_spec] * 7,
        scratch_shapes=[
            pltpu.VMEM((tok_count, d_model), bf16),
            pltpu.VMEM((PART_SLOTS * chunk_rows, d_model), f32),
            pltpu.VMEM((RECV_SLOTS, HALVES, DIRS, landed, half_cols), f32),
            pltpu.VMEM((RECV_SLOTS, HALVES, DIRS, landed, half_cols // RING), f32),
            pltpu.VMEM((tok_count, ff_local), bf16),
            pltpu.VMEM((tok_count, head_dim), bf16),
            pltpu.VMEM((2, ff_local + head_dim, DOWN_TILE), bf16),
            pltpu.VMEM((2, 2, d_model, W_TILE), bf16),
            pltpu.VMEM((2 * CHIPS * tok_count, 2 * head_dim), bf16),
            pltpu.VMEM((tok_count, head_dim), bf16),
            pltpu.VMEM((2, tok_count, head_dim), f32),
            pltpu.VMEM((2, tok_count, 128), f32),
            pltpu.VMEM((2, tok_count, 128), f32),
            pltpu.VMEM((2, rows_per, d_model), bf16),
            pltpu.VMEM((CHUNKS, HALVES, chunk_rows // RING, half_cols // RING), bf16),
            dma((2,)), dma, dma((2, 2)), dma((2, 2)), dma, dma,
            dma((10,)), dma((4, KV_CHUNKS)), dma((4, KV_CHUNKS)), dma, dma((2,)),
            dma, dma((2, RING - 1)), dma, dma,
            dma, dma,
            pltpu.VMEM((KV_CHUNKS, rows_per, W_TILE), bf16), dma, dma,
            pltpu.VMEM((RING, rows_per, head_dim), bf16),
            dma((PART_SLOTS,)), dma((4,)), dma((RECV_SLOTS, STEPS)),
            dma((LAST_STEPS,)), dma((LAST_BLOCKS, LAST_STEPS)), dma((2,)),
            pltpu.SemaphoreType.REGULAR((3,)), pltpu.SemaphoreType.REGULAR((DIRS,)),
        ],
        compiler_params=pltpu.CompilerParams(collective_id=0, has_side_effects=True, vmem_limit_bytes=67043328),
        name='layers',
    )(x_loc, cos_t, sin_t, norm_gain, w_q, w_k, w_v, w_gate, w_up, w_down, w_o)


EMIT_PARTS = 8


def emit_kernel(x_ref, k_first, k_second, v_first, v_second, x_out, k_out, v_out, xbuf, rows, load_sem, store_sem):
    size = x_ref.shape[0] // EMIT_PARTS
    loads, stores = [], []
    for n in range(EMIT_PARTS):
        part = pl.ds(n * size, size)
        loads.append(pltpu.make_async_copy(x_ref.at[part, :], xbuf.at[part, :], load_sem.at[n]))
        stores.append(pltpu.make_async_copy(xbuf.at[part, :], x_out.at[part, :], store_sem.at[n]))
    for n, (ref, out) in enumerate(((k_first, k_out.at[0]), (k_second, k_out.at[1]), (v_first, v_out.at[0]), (v_second, v_out.at[1]))):
        loads.append(pltpu.make_async_copy(ref, rows.at[n], load_sem.at[EMIT_PARTS + n]))
        stores.append(pltpu.make_async_copy(rows.at[n], out, store_sem.at[EMIT_PARTS + n]))
    for copy in loads:
        copy.start()
    for load, store in zip(loads, stores):
        load.wait()
        store.start()
    for copy in stores:
        copy.wait()


def emit(x_out, k_first, k_second, v_first, v_second):
    any_spec = pl.BlockSpec(memory_space=pl.ANY)
    cache = jax.ShapeDtypeStruct((2,) + k_first.shape, jnp.bfloat16)
    return pl.pallas_call(
        emit_kernel,
        out_shape=[jax.ShapeDtypeStruct(x_out.shape, jnp.bfloat16), cache, cache],
        in_specs=[any_spec] * 5,
        out_specs=[any_spec] * 3,
        scratch_shapes=[
            pltpu.VMEM(x_out.shape, jnp.bfloat16),
            pltpu.VMEM((4,) + k_first.shape, jnp.bfloat16),
            pltpu.SemaphoreType.DMA((EMIT_PARTS + 4,)),
            pltpu.SemaphoreType.DMA((EMIT_PARTS + 4,)),
        ],
        compiler_params=pltpu.CompilerParams(vmem_limit_bytes=63 * 1024 * 1024),
        name='emit',
    )(x_out, k_first, k_second, v_first, v_second)


def solution(mesh):
    row_spec = P(('batch', 'seq'), None)
    pos_spec = P(('batch', 'seq'))
    head_spec = P(None, None, 'head', None)
    out_proj_spec = P(None, 'head', None, None)
    col_spec = P(None, None, 'head')
    down_spec = P(None, 'head', None)
    cache_spec = P(None, ('batch', 'seq'), 'head', None)

    def local_forward(x_loc, pos_loc, w_q, w_k, w_v, w_o, w_gate, w_up, w_down, norm_gain):
        tok_count, d_model = x_loc.shape
        layer_count = w_q.shape[0]
        head_dim = w_q.shape[3]
        flat_q, flat_k, flat_v = (w.reshape(layer_count, d_model, head_dim) for w in (w_q, w_k, w_v))
        cos_t, sin_t = rope_tables(pos_loc, head_dim)
        x_out, k_first, v_first, k_second, v_second, _, _ = layers(x_loc, cos_t, sin_t, norm_gain, flat_q, flat_k, flat_v, w_gate, w_up, w_down, w_o)
        x_out, k_all, v_all = emit(x_out, k_first, k_second, v_first, v_second)
        cache_shape = (layer_count, tok_count, 1, head_dim)
        return x_out, k_all.reshape(cache_shape), v_all.reshape(cache_shape)

    return jax.shard_map(local_forward, mesh=mesh, in_specs=(row_spec, pos_spec, head_spec, head_spec, head_spec, out_proj_spec, col_spec, col_spec, down_spec, P(None, None)), out_specs=(row_spec, cache_spec, cache_spec), check_vma=False)
```

```python
import functools
import math
import jax
import jax.numpy as jnp
from jax import lax
from jax.experimental import pallas as pl
from jax.experimental.pallas import tpu as pltpu
from jax.sharding import PartitionSpec as P

ROPE_BASE = 500000.0
EPS = 1e-5


def rope_tables(positions, head_dim):
    half_dim = head_dim // 2
    inv_freq = ROPE_BASE ** (-(jnp.arange(half_dim, dtype=jnp.float32) * 2.0 / head_dim))
    angles = positions.astype(jnp.float32)[..., None] * inv_freq
    return jnp.cos(angles), jnp.sin(angles)


CHIPS = 4
RING = 4
HALVES = 2
DIRS = 2
KV_CHUNKS = 4
W_TILE = 256
NORM_ROWS = 64
CHUNKS = 8
STEPS = 8
PART_SLOTS = 4
RECV_SLOTS = 5
DOWN_TILE = 512
START_GAP = 3
STAGE_GAP = 2
BLOCK_TICK = 19
BLOCK_GAP = 6
LAST_TICK = 43
NEAR_TICKS = ((9, 1), (15, 3))
FAR_TICKS = ((24, 1), (26, 3))
SERVE_TICKS = (27, 31, 35, 42)
GIVE_TICK = 38
OWN_TICK = 3
DONE_TICK = 11
EARLY_TICK = 31
LAST_STEPS = 6
LAST_COLS = 256
LAST_BLOCKS = 16
LAST_GAP = 3


def layers_kernel(x_ref, cos_ref, sin_ref, gain_ref, wq_ref, wk_ref, wv_ref, wg_ref, wu_ref, wd_ref, wo_ref,
                 out_ref, k1_ref, v1_ref, k2_ref, v2_ref, gd_ref, go_ref,
                 xbuf, part, recv_a, recv_b, hid, att, wdo, wtile, kv, qbuf, acc, row_max, row_sum, xs, xres,
                 x_sem, res_sem, w_sem, down_sem, cache_sem, store_sem, kv_send, ici_recv, core_recv, part_send, part_recv,
                 round_send, round_recv, side_send, side_recv, give_send, give_recv, relay_buf, relay_send, relay_recv, att_all, ring_send, gather_send, ring_recv,
                 last_send, last_recv, tile_sem, ready_sem, drained_sem):
    tok_count, d_model = xbuf.shape
    head_dim = qbuf.shape[1]
    half_dim = head_dim // 2
    ff_local = hid.shape[1]
    depth = ff_local + head_dim
    rows_per = tok_count // KV_CHUNKS
    half_rows = tok_count // 2
    lanes = row_max.shape[2]
    chunk_rows = tok_count // CHUNKS
    quarter, eighth = chunk_rows // RING, chunk_rows // (2 * RING)
    half_cols = d_model // HALVES
    piece_cols = half_cols // RING
    bf16, f32 = jnp.bfloat16, jnp.float32
    sign = (1, -1)
    mesh_id = pl.DeviceIdType.MESH

    my_head = lax.axis_index('head')
    pos_z, pos_y = my_head // RING, my_head % RING
    my_seq = lax.axis_index('seq')
    chip, core = my_seq // 2, my_seq % 2
    other = chip * 2 + 1 - core

    def wrap(n):
        return (n + RING) % RING

    def y_peer(d):
        return pos_z * RING + wrap(pos_y + sign[d])

    def z_device(z):
        return wrap(z) * RING + pos_y

    def z_peer(d):
        return z_device(pos_z + sign[d])

    def x_device(n):
        return wrap(chip + n) * 2 + core

    right, left = x_device(1), x_device(-1)

    def span(start, size, unit=None):
        return pl.ds(pl.multiple_of(start, unit or size), size)

    def remote(src, dst, send, recv, **to):
        return pltpu.make_async_remote_copy(src_ref=src, dst_ref=dst, send_sem=send, recv_sem=recv, device_id=to, device_id_type=mesh_id)

    def take(sem, ref):
        remote(ref, ref, sem, sem, head=my_head).wait_recv()

    def x_load(i):
        return pltpu.make_async_copy(x_ref.at[span(i * rows_per, rows_per), :], xs.at[i % 2], x_sem.at[i % 2])

    def weights(layer, piece):
        slot = piece % 2
        if isinstance(piece, int) and piece < 2:
            refs = ((wk_ref, wv_ref), (wq_ref,))[piece]
            return [pltpu.make_async_copy(ref.at[layer], wtile.at[slot, n], w_sem.at[slot, n]) for n, ref in enumerate(refs)]
        cols = span((piece - 2) * W_TILE, W_TILE)
        return [pltpu.make_async_copy(ref.at[layer, :, cols], wtile.at[slot, n], w_sem.at[slot, n]) for n, ref in enumerate((wg_ref, wu_ref))]

    def start(copies):
        for copy in copies:
            copy.start()

    def wait(copies):
        for copy in copies:
            copy.wait()

    down_tiles = d_model // DOWN_TILE

    def down_load(i):
        cols = span(i * DOWN_TILE, DOWN_TILE)
        return [pltpu.make_async_copy(wd_ref.at[0, :, cols], wdo.at[i % 2, pl.ds(0, ff_local), :], down_sem.at[i % 2, 0]),
                pltpu.make_async_copy(wo_ref.at[0, 0, :, cols], wdo.at[i % 2, pl.ds(ff_local, head_dim), :], down_sem.at[i % 2, 1])]

    def kv_copy(origin_chip, origin_core, i, to, send, recv):
        rows = kv.at[span((origin_chip * 2 + origin_core) * tok_count + i * rows_per, rows_per), :]
        return remote(rows, rows, send, recv, seq=to)

    def kv_routes(i):
        def to(number, recv, origin_chip, origin_core, device):
            return lambda: kv_copy(origin_chip, origin_core, i, device, kv_send.at[number], recv)
        inner = jnp.logical_and(chip >= 1, chip < CHIPS - 1)
        return {
            'right': (chip < CHIPS - 1, 'all', to(0, ici_recv.at[0, i], chip, core, right)),
            'wrap': (chip == 0, 'all', to(1, ici_recv.at[2, i], chip, core, left)),
            'relay': (chip == 1, 'late', to(2, ici_recv.at[3, i], chip, core, left)),
            'other': (core == 0, 'all', to(3, core_recv.at[0, i], chip, core, other)),
            'on_right': (inner, 'early', to(4, ici_recv.at[1, i], chip - 1, core, right)),
            'from_relay': (chip == 0, 'late', to(5, ici_recv.at[1, i], 1, core, left)),
            'on_left': (chip == CHIPS - 1, 'late', to(6, ici_recv.at[1, i], 0, core, left)),
            'side1': (chip >= 1, 'all', to(7, core_recv.at[1, i], chip - 1, core, other)),
            'side2': (chip >= 2, 'all', to(8, core_recv.at[2, i], chip - 2, core, other)),
            'side3': (chip >= 3, 'all', to(9, core_recv.at[3, i], chip - 3, core, other)),
        }

    def start_route(i, name):
        condition, which, copy = kv_routes(i)[name]
        if which != 'all':
            late = i >= KV_CHUNKS // 2
            if isinstance(i, int):
                if late != (which == 'late'):
                    return
            else:
                condition = jnp.logical_and(condition, late if which == 'late' else jnp.logical_not(late))

        @pl.when(condition)
        def _():
            copy().start()

    def send_kv(i):
        for name in ('right', 'wrap', 'relay', 'other'):
            start_route(i, name)

    def kv_sent():
        for number, (condition, which, _) in enumerate(kv_routes(0).values()):
            @pl.when(condition)
            def _():
                take(kv_send.at[number], kv.at[pl.ds(0, tok_count if which == 'all' else half_rows), :])

    def serve(back, i):
        @pl.when(chip >= back)
        def _():
            kv_copy(chip - back, core, i, other, kv_send.at[0], ici_recv.at[back - 1, i]).wait_recv()
        start_route(i, 'side%d' % back)
        if back == 1:
            start_route(i, 'on_right')
        if back == 3:
            start_route(i, 'on_left')

    def relay(i):
        def pass_on():
            @pl.when(chip == 0)
            def _():
                kv_copy(1, core, i, left, kv_send.at[0], ici_recv.at[3, i]).wait_recv()
            start_route(i, 'from_relay')
        if not isinstance(i, int):
            pl.when(i >= KV_CHUNKS // 2)(pass_on)
        elif i >= KV_CHUNKS // 2:
            pass_on()

    def serve_all(i):
        serve(1, i)
        serve(3, i)
        relay(i)

    def taken(back, chunks):
        for i in chunks:
            kv_copy(chip - back, 1 - core, i, other, kv_send.at[0], core_recv.at[back, i]).wait_recv()

    def z_parts(step, d):
        copies = []
        for n, (own_ref, all_ref) in enumerate(((wd_ref, gd_ref), (wo_ref, go_ref))):
            size = all_ref.shape[1] // (2 * CHIPS)
            if step == 0:
                rows = span(my_seq * size, size)
                src = own_ref.at[1, rows, :] if n == 0 else own_ref.at[1, 0, rows, :]
                dst = all_ref.at[pos_z, rows, :]
            else:
                rows = span(my_seq * size + d * (size // 2), size // 2)
                src = dst = all_ref.at[wrap(pos_z - sign[d]), rows, :]
            copies.append(remote(src, dst, part_send, part_recv.at[step], head=z_peer(d)))
        return copies

    def part_copies(j, part_chip, part_core, half, send, recv, to):
        copies = []
        for n, ref in enumerate((gd_ref, go_ref)):
            size = ref.shape[1] // (2 * CHIPS)
            first = (part_chip * 2 + part_core) * size
            rows = span(first, size) if half is None else span(first + half * (size // 2), size // 2)
            place = ref.at[wrap(pos_z + j), rows, :]
            copies.append(remote(place, place, send, recv, seq=to))
        return copies

    def own_part(j, d):
        return part_copies(j, chip, core, None, round_send, round_recv.at[0, j - 1], x_device(sign[d]))

    def far_part(j, d):
        return part_copies(j, wrap(chip - sign[d]), core, d, round_send, round_recv.at[1, j - 1], x_device(sign[d]))

    def side_part(j, n, side):
        return part_copies(j, wrap(chip + n), side, None, side_send, side_recv, other)

    def round_start(j):
        for d in range(DIRS):
            start(own_part(j, d))
        start(side_part(j, 0, core))

    def near_parts(j):
        take(round_recv.at[0, j - 1], xbuf.at[pl.ds(0, depth // CHIPS), :])
        for d in range(DIRS):
            start(far_part(j, d) + side_part(j, 3 if d == 0 else 1, core))

    def far_parts(j):
        take(round_recv.at[1, j - 1], xbuf.at[pl.ds(0, depth // (2 * CHIPS)), :])
        start(side_part(j, 2, core))

    def give_hidden(z, i, source):
        cols = span(i * W_TILE, W_TILE)
        return remote(hid.at[span(z * rows_per, rows_per), cols], hidden_place(source, i), give_send, give_recv, head=z_device(z))

    def hidden_place(source, i):
        return xs.at[1, :, span(source * ff_local + i * W_TILE, W_TILE)]

    def via_neighbor(z, i):
        step = jnp.where(i < KV_CHUNKS // 2, 1, -1)
        return remote(hid.at[span(z * rows_per, rows_per), span(i * W_TILE, W_TILE)], relay_buf.at[i], give_send, relay_recv, head=z_device(pos_z + step))

    def relay_hidden(i):
        step = 1 if i < KV_CHUNKS // 2 else -1
        source = wrap(pos_z - step)
        return remote(relay_buf.at[i], hidden_place(source, i), relay_send, give_recv, head=z_device(pos_z + step))

    def send_hidden(z, i):
        away = wrap(z - pos_z)

        @pl.when(away == 2)
        def _():
            via_neighbor(z, i).start()

        @pl.when(away % 2 == 1)
        def _():
            give_hidden(z, i, pos_z).start()

    def give_rows(z, source):
        return remote(att.at[span(z * rows_per, rows_per), :], att_all.at[source], give_send, give_recv, head=z_device(z))

    def norm_rows(x_few, layer):
        x_f32 = x_few.astype(f32)
        inv_rms = lax.rsqrt(jnp.mean(x_f32 * x_f32, axis=-1, keepdims=True) + EPS)
        return (x_f32 * inv_rms * gain_ref[pl.ds(layer, 1), :].astype(f32)).astype(bf16)

    def rope(values, rows):
        cos_t, sin_t = cos_ref[rows, :], sin_ref[rows, :]
        wide = values.astype(bf16).astype(f32)
        first, second = wide[:, :half_dim], wide[:, half_dim:]
        return jnp.concatenate([first * cos_t - second * sin_t, second * cos_t + first * sin_t], axis=1).astype(bf16)

    def dot(a, b):
        return jnp.dot(a, b, preferred_element_type=f32)

    scale = 1.0 / math.sqrt(head_dim)

    def keys_values(normed, i):
        rows = span(i * rows_per, rows_per)
        own = span(my_seq * tok_count + i * rows_per, rows_per)
        kv[own, :head_dim] = rope(dot(normed, wtile[0, 0]), rows)
        kv[own, head_dim:] = dot(normed, wtile[0, 1]).astype(bf16)

    def queries(normed, i):
        rows = span(i * rows_per, rows_per)
        qbuf[rows, :] = (rope(dot(normed, wtile[1, 0]), rows).astype(f32) * scale).astype(bf16)

    def gated(normed, i, tile):
        gate = dot(normed, wtile[tile % 2, 0])
        up = dot(normed, wtile[tile % 2, 1])
        hid[span(i * rows_per, rows_per), span(tile * W_TILE, W_TILE)] = (gate * jax.nn.sigmoid(gate) * up).astype(bf16)

    def attend(key_start, q_half, side, masked, first):
        rows = pl.ds(q_half * half_rows, half_rows)
        some = span(key_start, half_rows)
        logits = lax.dot_general(qbuf[rows, :], kv[some, :head_dim], (((1,), (1,)), ((), ())), preferred_element_type=f32)
        if masked:
            seen = lax.broadcasted_iota(jnp.int32, logits.shape, 0) >= lax.broadcasted_iota(jnp.int32, logits.shape, 1)
            logits = jnp.where(seen, logits, -jnp.inf)
        block_max = jnp.max(logits, axis=-1, keepdims=True)
        if first:
            new_max = jnp.broadcast_to(block_max, (half_rows, lanes))
        else:
            new_max = jnp.maximum(row_max[side, rows, :], block_max)
        prob = jnp.exp(logits - jnp.concatenate([new_max] * (half_rows // lanes), axis=1))
        block_sum = jnp.sum(prob, axis=-1, keepdims=True)
        block_out = dot(prob.astype(bf16), kv[some, head_dim:])
        if first:
            row_sum[side, rows, :] = jnp.broadcast_to(block_sum, (half_rows, lanes))
            acc[side, rows, :] = block_out
        else:
            rescale = jnp.exp(row_max[side, rows, :] - new_max)
            row_sum[side, rows, :] = row_sum[side, rows, :] * rescale + block_sum
            acc[side, rows, :] = acc[side, rows, :] * jnp.concatenate([rescale] * (head_dim // lanes), axis=1) + block_out
        row_max[side, rows, :] = new_max

    def attend_own(layer_half):
        own_start = my_seq * tok_count
        if layer_half == 0:
            attend(own_start, 0, 0, True, True)
            top_rows = pl.ds(0, half_rows)
            row_max[1, top_rows, :] = jnp.full((half_rows, lanes), -jnp.inf, f32)
            row_sum[1, top_rows, :] = jnp.zeros((half_rows, lanes), f32)
            acc[1, top_rows, :] = jnp.zeros((half_rows, head_dim), f32)
        else:
            attend(own_start, 1, 0, False, True)
            attend(own_start + half_rows, 1, 1, True, True)

    def past_start(n):
        later = n - core
        back = jnp.where(later < 2, 1, jnp.where(chip == CHIPS - 1, jnp.where(later < 4, 3, 2), 2))
        block = (chip - back) * 2 + jnp.where(later % 2 == 0, core, 1 - core)
        return jnp.where(jnp.logical_and(core == 1, n == 0), chip * 2, block) * tok_count

    def arrivals(n, chunks):
        @pl.when(jnp.logical_and(core == 1, n == 0))
        def _():
            taken(0, chunks)

        for back in (1, 3, 2):
            place = 0 if back == 1 else 2 if back == 3 else jnp.where(chip == CHIPS - 1, 4, 2)
            if back == 2:
                @pl.when(jnp.logical_and(chip >= back, n == core + place))
                def _():
                    for i in chunks:
                        serve(2, i)

            @pl.when(jnp.logical_and(chip >= back, n == core + place + 1))
            def _():
                taken(back, chunks)

    def visit(n, visits):
        for q_half, side in visits:
            attend(past_start(n) + side * half_rows, q_half, side, False, False)

    def attend_past(first_n, last_n, chunks, visits):
        def past(n, carry):
            if chunks:
                arrivals(n, chunks)
            visit(n, visits)
            return carry

        lax.fori_loop(first_n, last_n, past, 0)

    few_near = jnp.minimum(my_seq, 1)
    near_count = my_seq - jnp.where(chip >= 2, 2, 0)

    def finish(i, spread):
        rows = pl.ds(i * rows_per, rows_per)
        top = jnp.maximum(row_max[0, rows, :], row_max[1, rows, :])
        shares = [jnp.exp(row_max[side, rows, :] - top) for side in range(2)]
        total = shares[0] * row_sum[0, rows, :] + shares[1] * row_sum[1, rows, :]
        wide = [jnp.concatenate([w] * (head_dim // lanes), axis=1) for w in shares + [total]]
        att[rows, :] = ((acc[0, rows, :] * wide[0] + acc[1, rows, :] * wide[1]) / wide[2]).astype(bf16)
        if spread:
            @pl.when(i != pos_z)
            def _():
                give_rows(i, pos_z).start()

    first_pos, second_pos = (pos_y, pos_z), (pos_z, pos_y)
    first_peer, second_peer = (y_peer, z_peer), (z_peer, y_peer)

    def part_rows(chunk, piece, offset, count):
        return span((chunk % PART_SLOTS) * chunk_rows + piece * quarter + offset, count, eighth)

    def x_rows(chunk, piece, offset, count):
        return span(chunk * chunk_rows + piece * quarter + offset, count, eighth)

    def cols_of(h, piece):
        return span(h * half_cols + piece * piece_cols, piece_cols)

    def half_of(h):
        return pl.ds(h * half_cols, half_cols)

    def message(step, chunk, h, d):
        p1, p2, s = first_pos[h], second_pos[h], sign[d]
        slot = chunk % RECV_SLOTS
        if step == 0:
            src, dst = part.at[part_rows(chunk, wrap(p1 + 2), d * eighth, eighth), half_of(h)], recv_a.at[slot, h, d, pl.ds(quarter, eighth), :]
        elif step == 1:
            src, dst = part.at[part_rows(chunk, wrap(p1 + s), 0, quarter), half_of(h)], recv_a.at[slot, h, d, pl.ds(0, quarter), :]
        elif step == 2:
            src, dst = part.at[part_rows(chunk, p1, d * eighth, eighth), cols_of(h, wrap(p2 + 2))], recv_b.at[slot, h, d, pl.ds(quarter, eighth), :]
        elif step == 3:
            src, dst = part.at[part_rows(chunk, p1, 0, quarter), cols_of(h, wrap(p2 + s))], recv_b.at[slot, h, d, pl.ds(0, quarter), :]
        elif step == 4:
            src = dst = xbuf.at[x_rows(chunk, p1, 0, quarter), cols_of(h, p2)]
        elif step == 5:
            src = dst = xbuf.at[x_rows(chunk, p1, d * eighth, eighth), cols_of(h, wrap(p2 - s))]
        elif step == 6:
            src = dst = xbuf.at[x_rows(chunk, p1, 0, quarter), half_of(h)]
        else:
            src = dst = xbuf.at[x_rows(chunk, wrap(p1 - s), d * eighth, eighth), half_of(h)]
        peer = (first_peer if step in (0, 1, 6, 7) else second_peer)[h](d)
        return remote(src, dst, ring_send.at[chunk % PART_SLOTS] if step < 4 else gather_send.at[step - 4], ring_recv.at[slot, step], head=peer)

    def arrived_in(step, count=1):
        rows = (2 * eighth, 2 * quarter, eighth // 2, quarter // 2, quarter // 2, quarter // 2, 2 * quarter, quarter)[step] * count
        return (part if step < 4 else xbuf).at[pl.ds(0, rows), pl.ds(0, half_cols if step == 5 else d_model)]

    def partials_sent(slot):
        take(ring_send.at[slot], part.at[pl.ds(0, 2 * eighth + 2 * quarter + eighth // 2 + quarter // 2), :])

    def residual_load(chunk, h):
        return pltpu.make_async_copy(x_ref.at[x_rows(chunk, first_pos[h], 0, quarter), cols_of(h, second_pos[h])], xres.at[chunk, h], res_sem)

    def project(chunk):
        rows = span(chunk * chunk_rows, chunk_rows)
        slot_rows = span((chunk % PART_SLOTS) * chunk_rows, chunk_rows)

        def one_tile(i, carry):
            @pl.when(jnp.logical_or(chunk < CHUNKS - 1, i < down_tiles - 1))
            def _():
                start(down_load((i + 1) % down_tiles))

            wait(down_load(i))
            total = dot(hid[rows, :], wdo[i % 2, :ff_local, :])
            part[slot_rows, span(i * DOWN_TILE, DOWN_TILE)] = total + dot(att[rows, :], wdo[i % 2, ff_local:, :])
            return carry

        lax.fori_loop(0, down_tiles, one_tile, 0)

    def stage(number, chunk):
        slot = chunk % RECV_SLOTS
        if number == 0:
            @pl.when(chunk >= PART_SLOTS)
            def _():
                partials_sent(chunk % PART_SLOTS)
            project(chunk)
        else:
            take(ring_recv.at[slot, number - 1], arrived_in(number - 1))
        if number == 4:
            @pl.when(chunk == 0)
            def _():
                take(res_sem, xres)
        for h in range(HALVES):
            p1, p2 = first_pos[h], second_pos[h]
            if number in (1, 3):
                for d in range(DIRS):
                    if number == 1:
                        rows, cols, arrived = part_rows(chunk, wrap(p1 + sign[d]), d * eighth, eighth), half_of(h), recv_a
                    else:
                        rows, cols, arrived = part_rows(chunk, p1, d * eighth, eighth), cols_of(h, wrap(p2 + sign[d])), recv_b
                    part[rows, cols] = part[rows, cols] + arrived[slot, h, d, pl.ds(quarter, eighth), :]
            if number == 2:
                rows = part_rows(chunk, p1, 0, quarter)
                part[rows, half_of(h)] = part[rows, half_of(h)] + recv_a[slot, h, 0, pl.ds(0, quarter), :] + recv_a[slot, h, 1, pl.ds(0, quarter), :]
            if number == 4:
                rows, cols = part_rows(chunk, p1, 0, quarter), cols_of(h, p2)
                total = part[rows, cols] + recv_b[slot, h, 0, pl.ds(0, quarter), :] + recv_b[slot, h, 1, pl.ds(0, quarter), :]
                update = total.astype(bf16).astype(f32)
                xbuf[x_rows(chunk, p1, 0, quarter), cols] = (xres[chunk, h].astype(f32) + update).astype(bf16)
            if number < STEPS:
                for d in range(DIRS):
                    message(number, chunk, h, d).start()

    x_load(0).start()
    start(weights(0, 0))
    x_load(1).start()
    start(weights(0, 1))
    barrier = pltpu.get_barrier_semaphore()
    for peer in (left, right, other):
        pl.semaphore_signal(barrier, inc=1, device_id={'seq': peer}, device_id_type=mesh_id)
    for peer in [z_device(pos_z + j) for j in range(1, RING)] + [y_peer(d) for d in range(DIRS)]:
        pl.semaphore_signal(barrier, inc=1, device_id={'head': peer}, device_id_type=mesh_id)
    pl.semaphore_wait(barrier, 8)
    for d in range(DIRS):
        start(z_parts(0, d))

    def prepare(i, carry):
        x_load(i).wait()

        def few(n, inner):
            xbuf[span(i * rows_per + n * NORM_ROWS, NORM_ROWS), :] = norm_rows(xs[i % 2, span(n * NORM_ROWS, NORM_ROWS), :], 0)
            return inner

        lax.fori_loop(0, rows_per // NORM_ROWS, few, 0)

        @pl.when(i + 2 < KV_CHUNKS)
        def _():
            x_load(i + 2).start()

        @pl.when(i == 0)
        def _():
            wait(weights(0, 0))

        keys_values(xbuf[span(i * rows_per, rows_per), :], i)
        send_kv(i)
        return carry

    lax.fori_loop(0, KV_CHUNKS, prepare, 0)
    start(weights(0, 2))
    own_rows = span(my_seq * tok_count, tok_count)

    def cache_stores(layer):
        k_ref, v_ref = ((k1_ref, v1_ref), (k2_ref, v2_ref))[layer]
        return [pltpu.make_async_copy(kv.at[own_rows, pl.ds(0, head_dim)], k_ref, cache_sem),
                pltpu.make_async_copy(kv.at[own_rows, pl.ds(head_dim, head_dim)], v_ref, cache_sem)]

    start(cache_stores(0))
    wait(weights(0, 1))

    def query(i, carry):
        queries(xbuf[span(i * rows_per, rows_per), :], i)
        return carry

    lax.fori_loop(0, KV_CHUNKS, query, 0)
    start(weights(0, 3))
    start(down_load(0))

    def residuals(n, carry):
        for h in range(HALVES):
            residual_load(n, h).start()
        return carry

    lax.fori_loop(0, CHUNKS, residuals, 0)

    def gate_half(half, tile):
        wait(weights(0, tile + 2))

        def rows_step(i, inner):
            gated(xbuf[span(i * rows_per, rows_per), :], i, tile)
            return inner

        lax.fori_loop(half * KV_CHUNKS // 2, (half + 1) * KV_CHUNKS // 2, rows_step, 0)

        @pl.when(tile < 2)
        def _():
            start(weights(0, tile + 4))

        for last in (2, 3):
            @pl.when(tile == last)
            def _():
                start(weights(1, last - 2) if half else weights(0, last))

    def first_half(tile, carry):
        gate_half(0, tile)

        @pl.when(tile < 3)
        def _():
            serve_all(tile)
        return carry

    def second_half(tile, carry):
        gate_half(1, tile)

        @pl.when(tile == 0)
        def _():
            serve_all(3)
            attend_past(0, few_near, range(KV_CHUNKS), ((0, 0), (0, 1)))
            take(part_recv.at[0], xbuf.at[pl.ds(0, depth // CHIPS), :])
            for d in range(DIRS):
                start(z_parts(1, d))
            attend_past(few_near, near_count, range(KV_CHUNKS), ((0, 0), (0, 1)))
        return carry

    lax.fori_loop(0, ff_local // W_TILE, first_half, 0)
    attend_own(0)
    lax.fori_loop(0, 2, second_half, 0)
    attend_past(near_count, my_seq, range(KV_CHUNKS), ((0, 0), (0, 1)))
    finish(0, False)
    finish(1, False)
    round_start(1)
    round_start(3)

    def block_work(j, phase):
        @pl.when(phase == 0)
        def _():
            @pl.when(j == 0)
            def _():
                for n in range(3):
                    pl.semaphore_wait(ready_sem.at[n], 1)

            def few(n, inner):
                xs[0, span(n * NORM_ROWS, NORM_ROWS), :] = norm_rows(xbuf[span(j * rows_per + n * NORM_ROWS, NORM_ROWS), :], 1)
                return inner

            lax.fori_loop(0, rows_per // NORM_ROWS, few, 0)
            wait(weights(1, 0))
            keys_values(xs[0], j)
            send_kv(j)
            start(weights(1, 2))

        @pl.when(phase == 1)
        def _():
            wait(weights(1, 1))
            queries(xs[0], j)
            start(weights(1, 3))

        @pl.when(jnp.logical_and(phase >= 1, phase <= 4))
        def _():
            tile = phase - 1
            wait(weights(1, tile + 2))
            gated(xs[0], j, tile)

            @pl.when(tile < 2)
            def _():
                start(weights(1, tile + 4))

            @pl.when(jnp.logical_and(tile == 2, j < KV_CHUNKS - 1))
            def _():
                start(weights(1, 0))

            @pl.when(jnp.logical_and(tile == 3, j < KV_CHUNKS - 1))
            def _():
                start(weights(1, 1))

            @pl.when(j == KV_CHUNKS - 1)
            def _():
                send_hidden(j, tile)

    def tick(t, carry):
        for number in range(STEPS, -1, -1):
            place = t - STAGE_GAP * number
            chunk = place // START_GAP

            @pl.when(jnp.logical_and(place >= 0, jnp.logical_and(place % START_GAP == 0, chunk < CHUNKS)))
            def _():
                stage(number, chunk)

        @pl.when(jnp.logical_or(t == 1, t == 3))
        def _():
            gate_half(1, 2 + t // 2)

        @pl.when(t == OWN_TICK)
        def _():
            attend_own(1)

        @pl.when(jnp.logical_and(t > OWN_TICK, jnp.logical_and(t < DONE_TICK, t - OWN_TICK <= my_seq)))
        def _():
            visit(t - OWN_TICK - 1, ((1, 0), (1, 1)))

        @pl.when(t == EARLY_TICK)
        def _():
            attend_own(0)

        early = t - EARLY_TICK - 1

        @pl.when(jnp.logical_and(early >= 0, jnp.logical_and(early < 7, early < my_seq)))
        def _():
            arrivals(early, (0, 1))
            visit(early, ((0, 0),))

        @pl.when(t == 2)
        def _():
            take(part_recv.at[1], xbuf.at[pl.ds(0, depth // (2 * CHIPS)), :])
            round_start(2)

        @pl.when(t == DONE_TICK)
        def _():
            finish(2, False)
            finish(3, False)
            kv_sent()
            take(cache_sem, kv.at[own_rows, :])
            for n, peer in enumerate((left, right, other)):
                pl.semaphore_signal(ready_sem.at[n], inc=1, device_id={'seq': peer}, device_id_type=mesh_id)

        for when, j in NEAR_TICKS:
            @pl.when(t == when)
            def _():
                near_parts(j)

        for when, j in FAR_TICKS:
            @pl.when(t == when)
            def _():
                far_parts(j)

        @pl.when(t == GIVE_TICK)
        def _():
            for i in range(KV_CHUNKS):
                for z in range(KV_CHUNKS - 1):
                    send_hidden(z, i)

        late = t - BLOCK_TICK

        @pl.when(late >= 0)
        def _():
            block_work(late // BLOCK_GAP, late % BLOCK_GAP)

        for i, when in enumerate(SERVE_TICKS):
            @pl.when(t == when)
            def _():
                serve_all(i)
        return carry

    lax.fori_loop(0, LAST_TICK, tick, 0)

    for slot in range(PART_SLOTS):
        partials_sent(slot)
    for step in range(4, STEPS):
        take(gather_send.at[step - 4], arrived_in(step, CHUNKS))
    for d in range(DIRS):
        pl.semaphore_signal(drained_sem.at[d], inc=1, device_id={'head': y_peer(d)}, device_id_type=mesh_id)
    start(cache_stores(1))
    near_parts(2)
    attend_own(1)
    attend_past(0, my_seq, (), ((1, 0),))
    take(relay_recv, relay_buf)
    for i in range(KV_CHUNKS):
        relay_hidden(i).start()
    attend_past(0, near_count, (2, 3), ((0, 1), (1, 1)))
    attend_past(near_count, my_seq, (2, 3), ((0, 1),))
    finish(0, True)
    finish(1, True)
    attend_past(near_count, my_seq, (), ((1, 1),))
    finish(2, True)
    finish(3, True)
    far_parts(2)
    parts_ref = gd_ref.at[pl.ds(0, 2), pl.ds(0, 3 * depth // 4), :]
    take(side_recv, parts_ref)

    quarter_rows = rows_per // RING

    def block_cols(c):
        return span(c * LAST_COLS, LAST_COLS)

    def tile_place(c, j, first, size):
        return wtile.at[c % 2, j // 2, pl.ds((j % 2) * depth + first, size), :]

    def tile_loads(c):
        copies = []
        for j in range(RING):
            z = wrap(pos_z + j)
            down = wd_ref.at[1, :, block_cols(c)] if j == 0 else gd_ref.at[z, :, block_cols(c)]
            out = wo_ref.at[1, 0, :, block_cols(c)] if j == 0 else go_ref.at[z, :, block_cols(c)]
            copies.append(pltpu.make_async_copy(down, tile_place(c, j, 0, ff_local), tile_sem.at[c % 2]))
            copies.append(pltpu.make_async_copy(out, tile_place(c, j, ff_local, head_dim), tile_sem.at[c % 2]))
        return copies

    start(tile_loads(0))
    given = hid.at[pl.ds(0, (RING - 1) * rows_per * depth // ff_local), :]
    take(give_recv, given)
    for d in range(DIRS):
        pl.semaphore_wait(drained_sem.at[d], 1)

    def quarter_of(piece, offset, size):
        return span(piece * quarter_rows + offset, size, quarter_rows // 2)

    def landed(d, first, size):
        return pl.ds(rows_per + d * (3 * quarter_rows // 2) + first, size)

    def rows_at(z, piece, offset, size):
        return span(z * rows_per + piece * quarter_rows + offset, size, quarter_rows // 2)

    def last_messages(step, c, d, z_first):
        s, cols, half = sign[d], block_cols(c), quarter_rows // 2
        near, behind, back = wrap(pos_y + s), wrap(pos_y - s), wrap(pos_z - s)
        along_y = step < 2 or (step < 4) != z_first
        if step == 0:
            pairs = [(part.at[quarter_of(wrap(pos_y + 2), d * half, half), cols], part.at[landed(d, quarter_rows, half), cols])]
        elif step == 1:
            pairs = [(part.at[quarter_of(near, 0, quarter_rows), cols], part.at[landed(d, 0, quarter_rows), cols])]
        else:
            if step == 2:
                rows = [rows_at(pos_z, pos_y, 0, quarter_rows)]
            elif step == 3:
                rows = [rows_at(back, pos_y, d * half, half) if z_first else rows_at(pos_z, behind, d * half, half)]
            elif step == 4:
                rows = [rows_at(z, pos_y, 0, quarter_rows) for z in range(RING)] if z_first else [rows_at(pos_z, 0, 0, rows_per)]
            else:
                rows = [rows_at(z, behind, d * half, half) for z in range(RING)] if z_first else [rows_at(back, 0, d * (rows_per // 2), rows_per // 2)]
            pairs = [(xbuf.at[r, cols], xbuf.at[r, cols]) for r in rows]
        to = (y_peer if along_y else z_peer)(d)
        return [remote(src, dst, last_send.at[step], last_recv.at[c, step], head=to) for src, dst in pairs]

    def last_arrived(step, cols):
        rows = (quarter_rows, 2 * quarter_rows, 2 * quarter_rows, quarter_rows, 2 * rows_per, rows_per)[step]
        return (part if step < 2 else xbuf).at[pl.ds(0, rows), cols]

    def send_last(step, c):
        def both(z_first):
            for d in range(DIRS):
                start(last_messages(step, c, d, z_first))

        if step < 2:
            both(False)
            return
        z_first = jnp.logical_and(c >= 5, c % 2 == 1)

        @pl.when(z_first)
        def _():
            both(True)

        @pl.when(jnp.logical_not(z_first))
        def _():
            both(False)

    def out_store(c):
        return pltpu.make_async_copy(xbuf.at[:, block_cols(c)], out_ref.at[:, block_cols(c)], store_sem)

    def last_project(c):
        @pl.when(c + 1 < LAST_BLOCKS)
        def _():
            start(tile_loads(c + 1))

        take(tile_sem.at[c % 2], wtile.at[c % 2, :, pl.ds(0, 2 * depth), :])
        total = None
        for j in range(RING):
            z = wrap(pos_z + j)
            own = span(pos_z * rows_per, rows_per)
            hidden_rows = hid[own, :] if j == 0 else xs[1, :, span(z * ff_local, ff_local)]
            out_rows = att[own, :] if j == 0 else att_all[z]
            term = dot(hidden_rows, wtile[c % 2, j // 2, pl.ds((j % 2) * depth, ff_local), :])
            term = term + dot(out_rows, wtile[c % 2, j // 2, pl.ds((j % 2) * depth + ff_local, head_dim), :])
            total = term if total is None else total + term
        part[pl.ds(0, rows_per), block_cols(c)] = total

    def last_stage(number, c):
        cols, half = block_cols(c), quarter_rows // 2
        if number == 0:
            last_project(c)
        else:
            take(last_recv.at[c, number - 1], last_arrived(number - 1, cols))
        if number == 1:
            for d in range(DIRS):
                piece = quarter_of(wrap(pos_y + sign[d]), d * half, half)
                part[piece, cols] = part[piece, cols] + part[landed(d, quarter_rows, half), cols]
        if number == 2:
            own = quarter_of(pos_y, 0, quarter_rows)
            total = part[own, cols] + part[landed(0, 0, quarter_rows), cols] + part[landed(1, 0, quarter_rows), cols]
            update = total.astype(bf16).astype(f32)
            rows = rows_at(pos_z, pos_y, 0, quarter_rows)
            xbuf[rows, cols] = (xbuf[rows, cols].astype(f32) + update).astype(bf16)
        if number < LAST_STEPS:
            send_last(number, c)
        else:
            out_store(c).start()

    def last_tick(t, carry):
        for number in range(LAST_STEPS, -1, -1):
            c = t - LAST_GAP * number

            @pl.when(jnp.logical_and(c >= 0, c < LAST_BLOCKS))
            def _():
                last_stage(number, c)
        return carry

    lax.fori_loop(0, LAST_BLOCKS + LAST_GAP * LAST_STEPS, last_tick, 0)

    take(cache_sem, kv.at[own_rows, :])
    take(relay_send, relay_buf)
    kv_sent()
    take(part_send, xbuf.at[pl.ds(0, 3 * depth // 8), :])
    take(round_send, gd_ref.at[pl.ds(0, 2), pl.ds(0, 9 * depth // 16), :])
    take(side_send, parts_ref)
    take(give_send, given)
    for step in range(LAST_STEPS):
        take(last_send.at[step], last_arrived(step, pl.ds(0, d_model)))
    take(store_sem, xbuf)


def layers(x_loc, cos_t, sin_t, norm_gain, w_q, w_k, w_v, w_gate, w_up, w_down, w_o):
    tok_count, d_model = x_loc.shape
    head_dim = w_q.shape[2]
    ff_local = w_gate.shape[2]
    rows_per = tok_count // KV_CHUNKS
    chunk_rows = tok_count // CHUNKS
    landed = 3 * chunk_rows // (2 * RING)
    half_cols = d_model // HALVES
    any_spec = pl.BlockSpec(memory_space=pl.ANY)
    vmem_spec = pl.BlockSpec(memory_space=pltpu.VMEM)
    bf16, f32 = jnp.bfloat16, jnp.float32
    dma = pltpu.SemaphoreType.DMA
    shape = jax.ShapeDtypeStruct
    return pl.pallas_call(
        layers_kernel,
        out_shape=[shape((tok_count, d_model), bf16)] + [shape((tok_count, head_dim), bf16)] * 4
        + [shape((RING, ff_local, d_model), bf16), shape((RING, head_dim, d_model), bf16)],
        in_specs=[any_spec, vmem_spec, vmem_spec, vmem_spec] + [any_spec] * 7,
        out_specs=[any_spec] * 7,
        scratch_shapes=[
            pltpu.VMEM((tok_count, d_model), bf16),
            pltpu.VMEM((PART_SLOTS * chunk_rows, d_model), f32),
            pltpu.VMEM((RECV_SLOTS, HALVES, DIRS, landed, half_cols), f32),
            pltpu.VMEM((RECV_SLOTS, HALVES, DIRS, landed, half_cols // RING), f32),
            pltpu.VMEM((tok_count, ff_local), bf16),
            pltpu.VMEM((tok_count, head_dim), bf16),
            pltpu.VMEM((2, ff_local + head_dim, DOWN_TILE), bf16),
            pltpu.VMEM((2, 2, d_model, W_TILE), bf16),
            pltpu.VMEM((2 * CHIPS * tok_count, 2 * head_dim), bf16),
            pltpu.VMEM((tok_count, head_dim), bf16),
            pltpu.VMEM((2, tok_count, head_dim), f32),
            pltpu.VMEM((2, tok_count, 128), f32),
            pltpu.VMEM((2, tok_count, 128), f32),
            pltpu.VMEM((2, rows_per, d_model), bf16),
            pltpu.VMEM((CHUNKS, HALVES, chunk_rows // RING, half_cols // RING), bf16),
            dma((2,)), dma, dma((2, 2)), dma((2, 2)), dma, dma,
            dma((10,)), dma((4, KV_CHUNKS)), dma((4, KV_CHUNKS)), dma, dma((2,)),
            dma, dma((2, RING - 1)), dma, dma,
            dma, dma,
            pltpu.VMEM((KV_CHUNKS, rows_per, W_TILE), bf16), dma, dma,
            pltpu.VMEM((RING, rows_per, head_dim), bf16),
            dma((PART_SLOTS,)), dma((4,)), dma((RECV_SLOTS, STEPS)),
            dma((LAST_STEPS,)), dma((LAST_BLOCKS, LAST_STEPS)), dma((2,)),
            pltpu.SemaphoreType.REGULAR((3,)), pltpu.SemaphoreType.REGULAR((DIRS,)),
        ],
        compiler_params=pltpu.CompilerParams(collective_id=0, has_side_effects=True, vmem_limit_bytes=67043328),
        name='layers',
    )(x_loc, cos_t, sin_t, norm_gain, w_q, w_k, w_v, w_gate, w_up, w_down, w_o)


EMIT_PARTS = 8


def emit_kernel(x_ref, k_first, k_second, v_first, v_second, x_out, k_out, v_out, xbuf, rows, load_sem, store_sem):
    size = x_ref.shape[0] // EMIT_PARTS
    parts = [pl.ds(n * size, size) for n in range(EMIT_PARTS)]
    caches = ((k_first, k_out.at[0]), (k_second, k_out.at[1]), (v_first, v_out.at[0]), (v_second, v_out.at[1]))
    loads = [pltpu.make_async_copy(x_ref.at[part, :], xbuf.at[part, :], load_sem.at[n]) for n, part in enumerate(parts)]
    stores = [pltpu.make_async_copy(xbuf.at[part, :], x_out.at[part, :], store_sem.at[0]) for part in parts]
    row_loads = [pltpu.make_async_copy(ref, rows.at[n], load_sem.at[EMIT_PARTS]) for n, (ref, _) in enumerate(caches)]
    row_stores = [pltpu.make_async_copy(rows.at[n], out, store_sem.at[1]) for n, (_, out) in enumerate(caches)]
    for copy in loads + row_loads:
        copy.start()
    for load, store in zip(loads, stores):
        load.wait()
        store.start()
    for copy in row_loads:
        copy.wait()
    for copy in row_stores:
        copy.start()
    for copy in stores + row_stores:
        copy.wait()


def emit(x_out, k_first, k_second, v_first, v_second):
    any_spec = pl.BlockSpec(memory_space=pl.ANY)
    cache = jax.ShapeDtypeStruct((2,) + k_first.shape, jnp.bfloat16)
    return pl.pallas_call(
        emit_kernel,
        out_shape=[jax.ShapeDtypeStruct(x_out.shape, jnp.bfloat16), cache, cache],
        in_specs=[any_spec] * 5,
        out_specs=[any_spec] * 3,
        scratch_shapes=[
            pltpu.VMEM(x_out.shape, jnp.bfloat16),
            pltpu.VMEM((4,) + k_first.shape, jnp.bfloat16),
            pltpu.SemaphoreType.DMA((EMIT_PARTS + 1,)),
            pltpu.SemaphoreType.DMA((2,)),
        ],
        compiler_params=pltpu.CompilerParams(vmem_limit_bytes=63 * 1024 * 1024),
        name='emit',
    )(x_out, k_first, k_second, v_first, v_second)


def solution(mesh):
    row_spec = P(('batch', 'seq'), None)
    pos_spec = P(('batch', 'seq'))
    head_spec = P(None, None, 'head', None)
    out_proj_spec = P(None, 'head', None, None)
    col_spec = P(None, None, 'head')
    down_spec = P(None, 'head', None)
    cache_spec = P(None, ('batch', 'seq'), 'head', None)

    def local_forward(x_loc, pos_loc, w_q, w_k, w_v, w_o, w_gate, w_up, w_down, norm_gain):
        tok_count, d_model = x_loc.shape
        layer_count = w_q.shape[0]
        head_dim = w_q.shape[3]
        flat_q, flat_k, flat_v = (w.reshape(layer_count, d_model, head_dim) for w in (w_q, w_k, w_v))
        cos_t, sin_t = rope_tables(pos_loc, head_dim)
        x_out, k_first, v_first, k_second, v_second, _, _ = layers(x_loc, cos_t, sin_t, norm_gain, flat_q, flat_k, flat_v, w_gate, w_up, w_down, w_o)
        x_out, k_all, v_all = emit(x_out, k_first, k_second, v_first, v_second)
        cache_shape = (layer_count, tok_count, 1, head_dim)
        return x_out, k_all.reshape(cache_shape), v_all.reshape(cache_shape)

    return jax.shard_map(local_forward, mesh=mesh, in_specs=(row_spec, pos_spec, head_spec, head_spec, head_spec, out_proj_spec, col_spec, col_spec, down_spec, P(None, None)), out_specs=(row_spec, cache_spec, cache_spec), check_vma=False)
```

```python
import functools
import math
import jax
import jax.numpy as jnp
from jax import lax
from jax.experimental import pallas as pl
from jax.experimental.pallas import tpu as pltpu
from jax.sharding import PartitionSpec as P

ROPE_BASE = 500000.0
EPS = 1e-5


def rope_tables(positions, head_dim):
    half_dim = head_dim // 2
    inv_freq = ROPE_BASE ** (-(jnp.arange(half_dim, dtype=jnp.float32) * 2.0 / head_dim))
    angles = positions.astype(jnp.float32)[..., None] * inv_freq
    return jnp.cos(angles), jnp.sin(angles)


CHIPS = 4
RING = 4
HALVES = 2
DIRS = 2
KV_CHUNKS = 4
W_TILE = 256
NORM_ROWS = 64
CHUNKS = 8
STEPS = 8
PART_SLOTS = 4
RECV_SLOTS = 5
DOWN_TILE = 512
START_GAP = 3
STAGE_GAP = 2
BLOCK_TICK = 19
BLOCK_GAP = 6
LAST_TICK = 43
NEAR_TICKS = ((9, 1), (15, 3), (21, 2))
FAR_TICKS = ((24, 1), (26, 3), (34, 2))
SERVE_TICKS = (27, 32, 36, 42)
GIVE_TICK = 37
OWN_TICK = 3
DONE_TICK = 11
EARLY_TICK = 32
FAR_VISIT_TICK = 39
LAST_STEPS = 6
LAST_COLS = 256
LAST_BLOCKS = 16
LAST_GAP = 3


def layers_kernel(x_ref, cos_ref, sin_ref, gain_ref, wq_ref, wk_ref, wv_ref, wg_ref, wu_ref, wd_ref, wo_ref,
                 out_ref, k1_ref, v1_ref, k2_ref, v2_ref, gd_ref, go_ref,
                 xbuf, part, recv_a, recv_b, hid, att, wdo, wtile, kv, qbuf, acc, row_max, row_sum, xs, xres,
                 x_sem, res_sem, w_sem, down_sem, cache_sem, store_sem, kv_send, ici_recv, core_recv, part_send, part_recv,
                 round_send, round_recv, side_send, side_recv, give_send, give_recv, relay_buf, relay_send, relay_recv, att_all, ring_send, gather_send, ring_recv,
                 last_send, last_recv, tile_sem, ready_sem, drained_sem):
    tok_count, d_model = xbuf.shape
    head_dim = qbuf.shape[1]
    half_dim = head_dim // 2
    ff_local = hid.shape[1]
    depth = ff_local + head_dim
    rows_per = tok_count // KV_CHUNKS
    half_rows = tok_count // 2
    lanes = row_max.shape[2]
    chunk_rows = tok_count // CHUNKS
    quarter, eighth = chunk_rows // RING, chunk_rows // (2 * RING)
    half_cols = d_model // HALVES
    piece_cols = half_cols // RING
    bf16, f32 = jnp.bfloat16, jnp.float32
    sign = (1, -1)
    mesh_id = pl.DeviceIdType.MESH

    my_head = lax.axis_index('head')
    pos_z, pos_y = my_head // RING, my_head % RING
    my_seq = lax.axis_index('seq')
    chip, core = my_seq // 2, my_seq % 2
    other = chip * 2 + 1 - core

    def wrap(n):
        return (n + RING) % RING

    def y_peer(d):
        return pos_z * RING + wrap(pos_y + sign[d])

    def z_device(z):
        return wrap(z) * RING + pos_y

    def z_peer(d):
        return z_device(pos_z + sign[d])

    def x_device(n):
        return wrap(chip + n) * 2 + core

    right, left = x_device(1), x_device(-1)

    def span(start, size, unit=None):
        return pl.ds(pl.multiple_of(start, unit or size), size)

    def remote(src, dst, send, recv, **to):
        return pltpu.make_async_remote_copy(src_ref=src, dst_ref=dst, send_sem=send, recv_sem=recv, device_id=to, device_id_type=mesh_id)

    def take(sem, ref):
        remote(ref, ref, sem, sem, head=my_head).wait_recv()

    def x_load(i):
        return pltpu.make_async_copy(x_ref.at[span(i * rows_per, rows_per), :], xs.at[i % 2], x_sem.at[i % 2])

    def weights(layer, piece):
        slot = piece % 2
        if isinstance(piece, int) and piece < 2:
            refs = ((wk_ref, wv_ref), (wq_ref,))[piece]
            return [pltpu.make_async_copy(ref.at[layer], wtile.at[slot, n], w_sem.at[slot, n]) for n, ref in enumerate(refs)]
        cols = span((piece - 2) * W_TILE, W_TILE)
        return [pltpu.make_async_copy(ref.at[layer, :, cols], wtile.at[slot, n], w_sem.at[slot, n]) for n, ref in enumerate((wg_ref, wu_ref))]

    def start(copies):
        for copy in copies:
            copy.start()

    def wait(copies):
        for copy in copies:
            copy.wait()

    down_tiles = d_model // DOWN_TILE

    def down_load(i):
        cols = span(i * DOWN_TILE, DOWN_TILE)
        return [pltpu.make_async_copy(wd_ref.at[0, :, cols], wdo.at[i % 2, pl.ds(0, ff_local), :], down_sem.at[i % 2, 0]),
                pltpu.make_async_copy(wo_ref.at[0, 0, :, cols], wdo.at[i % 2, pl.ds(ff_local, head_dim), :], down_sem.at[i % 2, 1])]

    def kv_copy(origin_chip, origin_core, i, to, send, recv):
        rows = kv.at[span((origin_chip * 2 + origin_core) * tok_count + i * rows_per, rows_per), :]
        return remote(rows, rows, send, recv, seq=to)

    def kv_routes(i):
        def to(number, recv, origin_chip, origin_core, device):
            return lambda: kv_copy(origin_chip, origin_core, i, device, kv_send.at[number], recv)
        inner = jnp.logical_and(chip >= 1, chip < CHIPS - 1)
        return {
            'right': (chip < CHIPS - 1, 'all', to(0, ici_recv.at[0, i], chip, core, right)),
            'wrap': (chip == 0, 'all', to(1, ici_recv.at[2, i], chip, core, left)),
            'relay': (chip == 1, 'late', to(2, ici_recv.at[3, i], chip, core, left)),
            'other': (core == 0, 'all', to(3, core_recv.at[0, i], chip, core, other)),
            'on_right': (inner, 'early', to(4, ici_recv.at[1, i], chip - 1, core, right)),
            'from_relay': (chip == 0, 'late', to(5, ici_recv.at[1, i], 1, core, left)),
            'on_left': (chip == CHIPS - 1, 'late', to(6, ici_recv.at[1, i], 0, core, left)),
            'side1': (chip >= 1, 'all', to(7, core_recv.at[1, i], chip - 1, core, other)),
            'side2': (chip >= 2, 'all', to(8, core_recv.at[2, i], chip - 2, core, other)),
            'side3': (chip >= 3, 'all', to(9, core_recv.at[3, i], chip - 3, core, other)),
        }

    def start_route(i, name):
        condition, which, copy = kv_routes(i)[name]
        if which != 'all':
            late = i >= KV_CHUNKS // 2
            if isinstance(i, int):
                if late != (which == 'late'):
                    return
            else:
                condition = jnp.logical_and(condition, late if which == 'late' else jnp.logical_not(late))

        @pl.when(condition)
        def _():
            copy().start()

    def send_kv(i):
        for name in ('right', 'wrap', 'relay', 'other'):
            start_route(i, name)

    def kv_sent():
        for number, (condition, which, _) in enumerate(kv_routes(0).values()):
            @pl.when(condition)
            def _():
                take(kv_send.at[number], kv.at[pl.ds(0, tok_count if which == 'all' else half_rows), :])

    def serve(back, i):
        @pl.when(chip >= back)
        def _():
            kv_copy(chip - back, core, i, other, kv_send.at[0], ici_recv.at[back - 1, i]).wait_recv()
        start_route(i, 'side%d' % back)
        if back == 1:
            start_route(i, 'on_right')
        if back == 3:
            start_route(i, 'on_left')

    def relay(i):
        def pass_on():
            @pl.when(chip == 0)
            def _():
                kv_copy(1, core, i, left, kv_send.at[0], ici_recv.at[3, i]).wait_recv()
            start_route(i, 'from_relay')
        if not isinstance(i, int):
            pl.when(i >= KV_CHUNKS // 2)(pass_on)
        elif i >= KV_CHUNKS // 2:
            pass_on()

    def serve_all(i):
        serve(1, i)
        serve(3, i)
        relay(i)

    def taken(back, chunks):
        for i in chunks:
            kv_copy(chip - back, 1 - core, i, other, kv_send.at[0], core_recv.at[back, i]).wait_recv()

    def z_parts(step, d):
        copies = []
        for n, (own_ref, all_ref) in enumerate(((wd_ref, gd_ref), (wo_ref, go_ref))):
            size = all_ref.shape[1] // (2 * CHIPS)
            if step == 0:
                rows = span(my_seq * size, size)
                src = own_ref.at[1, rows, :] if n == 0 else own_ref.at[1, 0, rows, :]
                dst = all_ref.at[pos_z, rows, :]
            else:
                rows = span(my_seq * size + d * (size // 2), size // 2)
                src = dst = all_ref.at[wrap(pos_z - sign[d]), rows, :]
            copies.append(remote(src, dst, part_send, part_recv.at[step], head=z_peer(d)))
        return copies

    def part_copies(j, part_chip, part_core, half, send, recv, to):
        copies = []
        for n, ref in enumerate((gd_ref, go_ref)):
            size = ref.shape[1] // (2 * CHIPS)
            first = (part_chip * 2 + part_core) * size
            rows = span(first, size) if half is None else span(first + half * (size // 2), size // 2)
            place = ref.at[wrap(pos_z + j), rows, :]
            copies.append(remote(place, place, send, recv, seq=to))
        return copies

    def own_part(j, d):
        return part_copies(j, chip, core, None, round_send, round_recv.at[0, j - 1], x_device(sign[d]))

    def far_part(j, d):
        return part_copies(j, wrap(chip - sign[d]), core, d, round_send, round_recv.at[1, j - 1], x_device(sign[d]))

    def side_part(j, n, side):
        return part_copies(j, wrap(chip + n), side, None, side_send, side_recv, other)

    def round_start(j):
        for d in range(DIRS):
            start(own_part(j, d))
        start(side_part(j, 0, core))

    def near_parts(j):
        take(round_recv.at[0, j - 1], xbuf.at[pl.ds(0, depth // CHIPS), :])
        for d in range(DIRS):
            start(far_part(j, d) + side_part(j, 3 if d == 0 else 1, core))

    def far_parts(j):
        take(round_recv.at[1, j - 1], xbuf.at[pl.ds(0, depth // (2 * CHIPS)), :])
        start(side_part(j, 2, core))

    def give_hidden(z, i, source):
        cols = span(i * W_TILE, W_TILE)
        return remote(hid.at[span(z * rows_per, rows_per), cols], hidden_place(source, i), give_send, give_recv, head=z_device(z))

    def hidden_place(source, i):
        return xs.at[1, :, span(source * ff_local + i * W_TILE, W_TILE)]

    def via_neighbor(z, i):
        step = jnp.where(i < KV_CHUNKS // 2, 1, -1)
        return remote(hid.at[span(z * rows_per, rows_per), span(i * W_TILE, W_TILE)], relay_buf.at[i], give_send, relay_recv, head=z_device(pos_z + step))

    def relay_hidden(i):
        step = 1 if i < KV_CHUNKS // 2 else -1
        source = wrap(pos_z - step)
        return remote(relay_buf.at[i], hidden_place(source, i), relay_send, give_recv, head=z_device(pos_z + step))

    def send_hidden(z, i):
        away = wrap(z - pos_z)

        @pl.when(away == 2)
        def _():
            via_neighbor(z, i).start()

        @pl.when(away % 2 == 1)
        def _():
            give_hidden(z, i, pos_z).start()

    def give_rows(z, source):
        return remote(att.at[span(z * rows_per, rows_per), :], att_all.at[source], give_send, give_recv, head=z_device(z))

    def norm_rows(x_few, layer):
        x_f32 = x_few.astype(f32)
        inv_rms = lax.rsqrt(jnp.mean(x_f32 * x_f32, axis=-1, keepdims=True) + EPS)
        return (x_f32 * inv_rms * gain_ref[pl.ds(layer, 1), :].astype(f32)).astype(bf16)

    def rope(values, rows):
        cos_t, sin_t = cos_ref[rows, :], sin_ref[rows, :]
        wide = values.astype(bf16).astype(f32)
        first, second = wide[:, :half_dim], wide[:, half_dim:]
        return jnp.concatenate([first * cos_t - second * sin_t, second * cos_t + first * sin_t], axis=1).astype(bf16)

    def dot(a, b):
        return jnp.dot(a, b, preferred_element_type=f32)

    scale = 1.0 / math.sqrt(head_dim)

    def keys_values(normed, i):
        rows = span(i * rows_per, rows_per)
        own = span(my_seq * tok_count + i * rows_per, rows_per)
        kv[own, :head_dim] = rope(dot(normed, wtile[0, 0]), rows)
        kv[own, head_dim:] = dot(normed, wtile[0, 1]).astype(bf16)

    def queries(normed, i):
        rows = span(i * rows_per, rows_per)
        qbuf[rows, :] = (rope(dot(normed, wtile[1, 0]), rows).astype(f32) * scale).astype(bf16)

    def gated(normed, i, tile):
        gate = dot(normed, wtile[tile % 2, 0])
        up = dot(normed, wtile[tile % 2, 1])
        hid[span(i * rows_per, rows_per), span(tile * W_TILE, W_TILE)] = (gate * jax.nn.sigmoid(gate) * up).astype(bf16)

    def attend(key_start, q_half, side, masked, first):
        rows = pl.ds(q_half * half_rows, half_rows)
        some = span(key_start, half_rows)
        logits = lax.dot_general(qbuf[rows, :], kv[some, :head_dim], (((1,), (1,)), ((), ())), preferred_element_type=f32)
        if masked:
            seen = lax.broadcasted_iota(jnp.int32, logits.shape, 0) >= lax.broadcasted_iota(jnp.int32, logits.shape, 1)
            logits = jnp.where(seen, logits, -jnp.inf)
        block_max = jnp.max(logits, axis=-1, keepdims=True)
        if first:
            new_max = jnp.broadcast_to(block_max, (half_rows, lanes))
        else:
            new_max = jnp.maximum(row_max[side, rows, :], block_max)
        prob = jnp.exp(logits - jnp.concatenate([new_max] * (half_rows // lanes), axis=1))
        block_sum = jnp.sum(prob, axis=-1, keepdims=True)
        block_out = dot(prob.astype(bf16), kv[some, head_dim:])
        if first:
            row_sum[side, rows, :] = jnp.broadcast_to(block_sum, (half_rows, lanes))
            acc[side, rows, :] = block_out
        else:
            rescale = jnp.exp(row_max[side, rows, :] - new_max)
            row_sum[side, rows, :] = row_sum[side, rows, :] * rescale + block_sum
            acc[side, rows, :] = acc[side, rows, :] * jnp.concatenate([rescale] * (head_dim // lanes), axis=1) + block_out
        row_max[side, rows, :] = new_max

    def attend_own(layer_half):
        own_start = my_seq * tok_count
        if layer_half == 0:
            attend(own_start, 0, 0, True, True)
            top_rows = pl.ds(0, half_rows)
            row_max[1, top_rows, :] = jnp.full((half_rows, lanes), -jnp.inf, f32)
            row_sum[1, top_rows, :] = jnp.zeros((half_rows, lanes), f32)
            acc[1, top_rows, :] = jnp.zeros((half_rows, head_dim), f32)
        else:
            attend(own_start, 1, 0, False, True)
            attend(own_start + half_rows, 1, 1, True, True)

    def past_start(n):
        later = n - core
        back = jnp.where(later < 2, 1, jnp.where(chip == CHIPS - 1, jnp.where(later < 4, 3, 2), 2))
        block = (chip - back) * 2 + jnp.where(later % 2 == 0, core, 1 - core)
        return jnp.where(jnp.logical_and(core == 1, n == 0), chip * 2, block) * tok_count

    def arrivals(n, chunks):
        @pl.when(jnp.logical_and(core == 1, n == 0))
        def _():
            taken(0, chunks)

        for back in (1, 3, 2):
            place = 0 if back == 1 else 2 if back == 3 else jnp.where(chip == CHIPS - 1, 4, 2)
            if back == 2:
                @pl.when(jnp.logical_and(chip >= back, n == core + place))
                def _():
                    for i in chunks:
                        serve(2, i)

            @pl.when(jnp.logical_and(chip >= back, n == core + place + 1))
            def _():
                taken(back, chunks)

    def visit(n, visits):
        for q_half, side in visits:
            attend(past_start(n) + side * half_rows, q_half, side, False, False)

    def attend_past(first_n, last_n, chunks, visits):
        def past(n, carry):
            if chunks:
                arrivals(n, chunks)
            visit(n, visits)
            return carry

        lax.fori_loop(first_n, last_n, past, 0)

    near_count = my_seq - jnp.where(chip >= 2, 2, 0)

    def finish(i, spread):
        rows = pl.ds(i * rows_per, rows_per)
        top = jnp.maximum(row_max[0, rows, :], row_max[1, rows, :])
        shares = [jnp.exp(row_max[side, rows, :] - top) for side in range(2)]
        total = shares[0] * row_sum[0, rows, :] + shares[1] * row_sum[1, rows, :]
        wide = [jnp.concatenate([w] * (head_dim // lanes), axis=1) for w in shares + [total]]
        att[rows, :] = ((acc[0, rows, :] * wide[0] + acc[1, rows, :] * wide[1]) / wide[2]).astype(bf16)
        if spread:
            @pl.when(i != pos_z)
            def _():
                give_rows(i, pos_z).start()

    first_pos, second_pos = (pos_y, pos_z), (pos_z, pos_y)
    first_peer, second_peer = (y_peer, z_peer), (z_peer, y_peer)

    def part_rows(chunk, piece, offset, count):
        return span((chunk % PART_SLOTS) * chunk_rows + piece * quarter + offset, count, eighth)

    def x_rows(chunk, piece, offset, count):
        return span(chunk * chunk_rows + piece * quarter + offset, count, eighth)

    def cols_of(h, piece):
        return span(h * half_cols + piece * piece_cols, piece_cols)

    def half_of(h):
        return pl.ds(h * half_cols, half_cols)

    def message(step, chunk, h, d):
        p1, p2, s = first_pos[h], second_pos[h], sign[d]
        slot = chunk % RECV_SLOTS
        if step == 0:
            src, dst = part.at[part_rows(chunk, wrap(p1 + 2), d * eighth, eighth), half_of(h)], recv_a.at[slot, h, d, pl.ds(quarter, eighth), :]
        elif step == 1:
            src, dst = part.at[part_rows(chunk, wrap(p1 + s), 0, quarter), half_of(h)], recv_a.at[slot, h, d, pl.ds(0, quarter), :]
        elif step == 2:
            src, dst = part.at[part_rows(chunk, p1, d * eighth, eighth), cols_of(h, wrap(p2 + 2))], recv_b.at[slot, h, d, pl.ds(quarter, eighth), :]
        elif step == 3:
            src, dst = part.at[part_rows(chunk, p1, 0, quarter), cols_of(h, wrap(p2 + s))], recv_b.at[slot, h, d, pl.ds(0, quarter), :]
        elif step == 4:
            src = dst = xbuf.at[x_rows(chunk, p1, 0, quarter), cols_of(h, p2)]
        elif step == 5:
            src = dst = xbuf.at[x_rows(chunk, p1, d * eighth, eighth), cols_of(h, wrap(p2 - s))]
        elif step == 6:
            src = dst = xbuf.at[x_rows(chunk, p1, 0, quarter), half_of(h)]
        else:
            src = dst = xbuf.at[x_rows(chunk, wrap(p1 - s), d * eighth, eighth), half_of(h)]
        peer = (first_peer if step in (0, 1, 6, 7) else second_peer)[h](d)
        return remote(src, dst, ring_send.at[chunk % PART_SLOTS] if step < 4 else gather_send.at[step - 4], ring_recv.at[slot, step], head=peer)

    def arrived_in(step, count=1):
        rows = (2 * eighth, 2 * quarter, eighth // 2, quarter // 2, quarter // 2, quarter // 2, 2 * quarter, quarter)[step] * count
        return (part if step < 4 else xbuf).at[pl.ds(0, rows), pl.ds(0, half_cols if step == 5 else d_model)]

    def partials_sent(slot):
        take(ring_send.at[slot], part.at[pl.ds(0, 2 * eighth + 2 * quarter + eighth // 2 + quarter // 2), :])

    def residual_load(chunk, h):
        return pltpu.make_async_copy(x_ref.at[x_rows(chunk, first_pos[h], 0, quarter), cols_of(h, second_pos[h])], xres.at[chunk, h], res_sem)

    def project(chunk):
        rows = span(chunk * chunk_rows, chunk_rows)
        slot_rows = span((chunk % PART_SLOTS) * chunk_rows, chunk_rows)

        def one_tile(i, carry):
            @pl.when(jnp.logical_or(chunk < CHUNKS - 1, i < down_tiles - 1))
            def _():
                start(down_load((i + 1) % down_tiles))

            wait(down_load(i))
            total = dot(hid[rows, :], wdo[i % 2, :ff_local, :])
            part[slot_rows, span(i * DOWN_TILE, DOWN_TILE)] = total + dot(att[rows, :], wdo[i % 2, ff_local:, :])
            return carry

        lax.fori_loop(0, down_tiles, one_tile, 0)

    def stage(number, chunk):
        slot = chunk % RECV_SLOTS
        if number == 0:
            @pl.when(chunk >= PART_SLOTS)
            def _():
                partials_sent(chunk % PART_SLOTS)
            project(chunk)
        else:
            take(ring_recv.at[slot, number - 1], arrived_in(number - 1))
        if number == 4:
            @pl.when(chunk == 0)
            def _():
                take(res_sem, xres)
        for h in range(HALVES):
            p1, p2 = first_pos[h], second_pos[h]
            if number in (1, 3):
                for d in range(DIRS):
                    if number == 1:
                        rows, cols, arrived = part_rows(chunk, wrap(p1 + sign[d]), d * eighth, eighth), half_of(h), recv_a
                    else:
                        rows, cols, arrived = part_rows(chunk, p1, d * eighth, eighth), cols_of(h, wrap(p2 + sign[d])), recv_b
                    part[rows, cols] = part[rows, cols] + arrived[slot, h, d, pl.ds(quarter, eighth), :]
            if number == 2:
                rows = part_rows(chunk, p1, 0, quarter)
                part[rows, half_of(h)] = part[rows, half_of(h)] + recv_a[slot, h, 0, pl.ds(0, quarter), :] + recv_a[slot, h, 1, pl.ds(0, quarter), :]
            if number == 4:
                rows, cols = part_rows(chunk, p1, 0, quarter), cols_of(h, p2)
                total = part[rows, cols] + recv_b[slot, h, 0, pl.ds(0, quarter), :] + recv_b[slot, h, 1, pl.ds(0, quarter), :]
                update = total.astype(bf16).astype(f32)
                xbuf[x_rows(chunk, p1, 0, quarter), cols] = (xres[chunk, h].astype(f32) + update).astype(bf16)
            if number < STEPS:
                for d in range(DIRS):
                    message(number, chunk, h, d).start()

    x_load(0).start()
    start(weights(0, 0))
    x_load(1).start()
    start(weights(0, 1))
    barrier = pltpu.get_barrier_semaphore()
    for peer in (left, right, other):
        pl.semaphore_signal(barrier, inc=1, device_id={'seq': peer}, device_id_type=mesh_id)
    for peer in [z_device(pos_z + j) for j in range(1, RING)] + [y_peer(d) for d in range(DIRS)]:
        pl.semaphore_signal(barrier, inc=1, device_id={'head': peer}, device_id_type=mesh_id)

    def prepare(i, carry):
        x_load(i).wait()

        def few(n, inner):
            xbuf[span(i * rows_per + n * NORM_ROWS, NORM_ROWS), :] = norm_rows(xs[i % 2, span(n * NORM_ROWS, NORM_ROWS), :], 0)
            return inner

        lax.fori_loop(0, rows_per // NORM_ROWS, few, 0)

        @pl.when(i + 2 < KV_CHUNKS)
        def _():
            x_load(i + 2).start()

        @pl.when(i == 0)
        def _():
            wait(weights(0, 0))

        keys_values(xbuf[span(i * rows_per, rows_per), :], i)

        @pl.when(i == 0)
        def _():
            pl.semaphore_wait(barrier, 8)

        send_kv(i)

        @pl.when(i == 0)
        def _():
            for d in range(DIRS):
                start(z_parts(0, d))
        return carry

    lax.fori_loop(0, KV_CHUNKS, prepare, 0)
    start(weights(0, 2))
    own_rows = span(my_seq * tok_count, tok_count)

    def cache_stores(layer):
        k_ref, v_ref = ((k1_ref, v1_ref), (k2_ref, v2_ref))[layer]
        return [pltpu.make_async_copy(kv.at[own_rows, pl.ds(0, head_dim)], k_ref, cache_sem),
                pltpu.make_async_copy(kv.at[own_rows, pl.ds(head_dim, head_dim)], v_ref, cache_sem)]

    start(cache_stores(0))
    wait(weights(0, 1))

    def query(i, carry):
        queries(xbuf[span(i * rows_per, rows_per), :], i)
        return carry

    lax.fori_loop(0, KV_CHUNKS, query, 0)
    start(weights(0, 3))
    start(down_load(0))

    def residuals(n, carry):
        for h in range(HALVES):
            residual_load(n, h).start()
        return carry

    lax.fori_loop(0, CHUNKS, residuals, 0)

    def gate_half(half, tile):
        wait(weights(0, tile + 2))

        def rows_step(i, inner):
            gated(xbuf[span(i * rows_per, rows_per), :], i, tile)
            return inner

        lax.fori_loop(half * KV_CHUNKS // 2, (half + 1) * KV_CHUNKS // 2, rows_step, 0)

        @pl.when(tile < 2)
        def _():
            start(weights(0, tile + 4))

        for last in (2, 3):
            @pl.when(tile == last)
            def _():
                start(weights(1, last - 2) if half else weights(0, last))

    def first_half(tile, carry):
        gate_half(0, tile)

        @pl.when(tile < 3)
        def _():
            serve_all(tile)
        return carry

    def second_half(tile, carry):
        gate_half(1, tile)

        @pl.when(tile == 0)
        def _():
            serve_all(3)
            attend_past(0, near_count, range(KV_CHUNKS), ((0, 0), (0, 1)))
            take(part_recv.at[0], xbuf.at[pl.ds(0, depth // CHIPS), :])
            for d in range(DIRS):
                start(z_parts(1, d))
        return carry

    lax.fori_loop(0, ff_local // W_TILE, first_half, 0)
    attend_own(0)
    lax.fori_loop(0, 2, second_half, 0)
    attend_past(near_count, my_seq, range(KV_CHUNKS), ((0, 0), (0, 1)))
    finish(0, False)
    finish(1, False)
    round_start(1)
    round_start(3)

    def block_work(j, phase):
        @pl.when(phase == 0)
        def _():
            @pl.when(j == 0)
            def _():
                for n in range(3):
                    pl.semaphore_wait(ready_sem.at[n], 1)

            def few(n, inner):
                xs[0, span(n * NORM_ROWS, NORM_ROWS), :] = norm_rows(xbuf[span(j * rows_per + n * NORM_ROWS, NORM_ROWS), :], 1)
                return inner

            lax.fori_loop(0, rows_per // NORM_ROWS, few, 0)
            wait(weights(1, 0))
            keys_values(xs[0], j)
            send_kv(j)
            start(weights(1, 2))

        @pl.when(phase == 1)
        def _():
            wait(weights(1, 1))
            queries(xs[0], j)
            start(weights(1, 3))

        @pl.when(jnp.logical_and(phase >= 1, phase <= 4))
        def _():
            tile = phase - 1
            wait(weights(1, tile + 2))
            gated(xs[0], j, tile)

            @pl.when(tile < 2)
            def _():
                start(weights(1, tile + 4))

            @pl.when(jnp.logical_and(tile == 2, j < KV_CHUNKS - 1))
            def _():
                start(weights(1, 0))

            @pl.when(jnp.logical_and(tile == 3, j < KV_CHUNKS - 1))
            def _():
                start(weights(1, 1))

            @pl.when(j == KV_CHUNKS - 1)
            def _():
                send_hidden(j, tile)

    def tick(t, carry):
        for number in range(STEPS, -1, -1):
            place = t - STAGE_GAP * number
            chunk = place // START_GAP

            @pl.when(jnp.logical_and(place >= 0, jnp.logical_and(place % START_GAP == 0, chunk < CHUNKS)))
            def _():
                stage(number, chunk)

        @pl.when(jnp.logical_or(t == 1, t == 3))
        def _():
            gate_half(1, 2 + t // 2)

        @pl.when(t == OWN_TICK)
        def _():
            attend_own(1)

        @pl.when(jnp.logical_and(t > OWN_TICK, jnp.logical_and(t < DONE_TICK, t - OWN_TICK <= my_seq)))
        def _():
            visit(t - OWN_TICK - 1, ((1, 0), (1, 1)))

        @pl.when(t == EARLY_TICK)
        def _():
            attend_own(0)

        def early_visit(n, due, last_n):
            @pl.when(jnp.logical_and(due, jnp.logical_and(n >= 0, n < last_n)))
            def _():
                arrivals(n, (0, 1))
                visit(n, ((0, 0),))

        for r in range(2):
            early_visit(2 * (t - EARLY_TICK - 1) + r, t > EARLY_TICK, near_count)
        early_visit(near_count + t - FAR_VISIT_TICK, t >= FAR_VISIT_TICK, my_seq)

        @pl.when(t == 2)
        def _():
            take(part_recv.at[1], xbuf.at[pl.ds(0, depth // (2 * CHIPS)), :])
            round_start(2)

        @pl.when(t == DONE_TICK)
        def _():
            finish(2, False)
            finish(3, False)
            kv_sent()
            take(cache_sem, kv.at[own_rows, :])
            for n, peer in enumerate((left, right, other)):
                pl.semaphore_signal(ready_sem.at[n], inc=1, device_id={'seq': peer}, device_id_type=mesh_id)

        for when, j in NEAR_TICKS:
            @pl.when(t == when)
            def _():
                near_parts(j)

        for when, j in FAR_TICKS:
            @pl.when(t == when)
            def _():
                far_parts(j)

        @pl.when(t == GIVE_TICK)
        def _():
            for i in range(KV_CHUNKS):
                for z in range(KV_CHUNKS - 1):
                    send_hidden(z, i)

        late = t - BLOCK_TICK

        @pl.when(late >= 0)
        def _():
            block_work(late // BLOCK_GAP, late % BLOCK_GAP)

        for i, when in enumerate(SERVE_TICKS):
            @pl.when(t == when)
            def _():
                serve_all(i)
        return carry

    lax.fori_loop(0, LAST_TICK, tick, 0)

    for slot in range(PART_SLOTS):
        partials_sent(slot)
    for step in range(4, STEPS):
        take(gather_send.at[step - 4], arrived_in(step, CHUNKS))
    for d in range(DIRS):
        pl.semaphore_signal(drained_sem.at[d], inc=1, device_id={'head': y_peer(d)}, device_id_type=mesh_id)
    start(cache_stores(1))
    attend_own(1)
    attend_past(0, my_seq, (), ((1, 0),))
    take(relay_recv, relay_buf)
    for i in range(KV_CHUNKS):
        relay_hidden(i).start()
    attend_past(0, near_count, (2, 3), ((0, 1), (1, 1)))
    attend_past(near_count, my_seq, (2, 3), ((0, 1),))
    finish(0, True)
    finish(1, True)
    attend_past(near_count, my_seq, (), ((1, 1),))
    finish(2, True)
    finish(3, True)
    parts_ref = gd_ref.at[pl.ds(0, 2), pl.ds(0, 3 * depth // 4), :]
    take(side_recv, parts_ref)

    quarter_rows = rows_per // RING

    def block_cols(c):
        return span(c * LAST_COLS, LAST_COLS)

    def tile_place(c, j, first, size):
        return wtile.at[c % 2, j // 2, pl.ds((j % 2) * depth + first, size), :]

    def tile_loads(c):
        copies = []
        for j in range(RING):
            z = wrap(pos_z + j)
            down = wd_ref.at[1, :, block_cols(c)] if j == 0 else gd_ref.at[z, :, block_cols(c)]
            out = wo_ref.at[1, 0, :, block_cols(c)] if j == 0 else go_ref.at[z, :, block_cols(c)]
            copies.append(pltpu.make_async_copy(down, tile_place(c, j, 0, ff_local), tile_sem.at[c % 2]))
            copies.append(pltpu.make_async_copy(out, tile_place(c, j, ff_local, head_dim), tile_sem.at[c % 2]))
        return copies

    start(tile_loads(0))
    given = hid.at[pl.ds(0, (RING - 1) * rows_per * depth // ff_local), :]
    take(give_recv, given)
    for d in range(DIRS):
        pl.semaphore_wait(drained_sem.at[d], 1)

    def quarter_of(piece, offset, size):
        return span(piece * quarter_rows + offset, size, quarter_rows // 2)

    def landed(d, first, size):
        return pl.ds(rows_per + d * (3 * quarter_rows // 2) + first, size)

    def rows_at(z, piece, offset, size):
        return span(z * rows_per + piece * quarter_rows + offset, size, quarter_rows // 2)

    def last_messages(step, c, d, z_first):
        s, cols, half = sign[d], block_cols(c), quarter_rows // 2
        near, behind, back = wrap(pos_y + s), wrap(pos_y - s), wrap(pos_z - s)
        along_y = step < 2 or (step < 4) != z_first
        if step == 0:
            pairs = [(part.at[quarter_of(wrap(pos_y + 2), d * half, half), cols], part.at[landed(d, quarter_rows, half), cols])]
        elif step == 1:
            pairs = [(part.at[quarter_of(near, 0, quarter_rows), cols], part.at[landed(d, 0, quarter_rows), cols])]
        else:
            if step == 2:
                rows = [rows_at(pos_z, pos_y, 0, quarter_rows)]
            elif step == 3:
                rows = [rows_at(back, pos_y, d * half, half) if z_first else rows_at(pos_z, behind, d * half, half)]
            elif step == 4:
                rows = [rows_at(z, pos_y, 0, quarter_rows) for z in range(RING)] if z_first else [rows_at(pos_z, 0, 0, rows_per)]
            else:
                rows = [rows_at(z, behind, d * half, half) for z in range(RING)] if z_first else [rows_at(back, 0, d * (rows_per // 2), rows_per // 2)]
            pairs = [(xbuf.at[r, cols], xbuf.at[r, cols]) for r in rows]
        to = (y_peer if along_y else z_peer)(d)
        return [remote(src, dst, last_send.at[step], last_recv.at[c, step], head=to) for src, dst in pairs]

    def last_arrived(step, cols):
        rows = (quarter_rows, 2 * quarter_rows, 2 * quarter_rows, quarter_rows, 2 * rows_per, rows_per)[step]
        return (part if step < 2 else xbuf).at[pl.ds(0, rows), cols]

    def send_last(step, c):
        def both(z_first):
            for d in range(DIRS):
                start(last_messages(step, c, d, z_first))

        if step < 2:
            both(False)
            return
        z_first = jnp.logical_and(c >= 5, c % 2 == 1)

        @pl.when(z_first)
        def _():
            both(True)

        @pl.when(jnp.logical_not(z_first))
        def _():
            both(False)

    def out_store(c):
        return pltpu.make_async_copy(xbuf.at[:, block_cols(c)], out_ref.at[:, block_cols(c)], store_sem)

    def last_project(c):
        @pl.when(c + 1 < LAST_BLOCKS)
        def _():
            start(tile_loads(c + 1))

        take(tile_sem.at[c % 2], wtile.at[c % 2, :, pl.ds(0, 2 * depth), :])
        total = None
        for j in range(RING):
            z = wrap(pos_z + j)
            own = span(pos_z * rows_per, rows_per)
            hidden_rows = hid[own, :] if j == 0 else xs[1, :, span(z * ff_local, ff_local)]
            out_rows = att[own, :] if j == 0 else att_all[z]
            term = dot(hidden_rows, wtile[c % 2, j // 2, pl.ds((j % 2) * depth, ff_local), :])
            term = term + dot(out_rows, wtile[c % 2, j // 2, pl.ds((j % 2) * depth + ff_local, head_dim), :])
            total = term if total is None else total + term
        part[pl.ds(0, rows_per), block_cols(c)] = total

    def last_stage(number, c):
        cols, half = block_cols(c), quarter_rows // 2
        if number == 0:
            last_project(c)
        else:
            take(last_recv.at[c, number - 1], last_arrived(number - 1, cols))
        if number == 1:
            for d in range(DIRS):
                piece = quarter_of(wrap(pos_y + sign[d]), d * half, half)
                part[piece, cols] = part[piece, cols] + part[landed(d, quarter_rows, half), cols]
        if number == 2:
            own = quarter_of(pos_y, 0, quarter_rows)
            total = part[own, cols] + part[landed(0, 0, quarter_rows), cols] + part[landed(1, 0, quarter_rows), cols]
            update = total.astype(bf16).astype(f32)
            rows = rows_at(pos_z, pos_y, 0, quarter_rows)
            xbuf[rows, cols] = (xbuf[rows, cols].astype(f32) + update).astype(bf16)
        if number < LAST_STEPS:
            send_last(number, c)
        else:
            out_store(c).start()

    def last_tick(t, carry):
        for number in range(LAST_STEPS, -1, -1):
            c = t - LAST_GAP * number

            @pl.when(jnp.logical_and(c >= 0, c < LAST_BLOCKS))
            def _():
                last_stage(number, c)
        return carry

    lax.fori_loop(0, LAST_BLOCKS + LAST_GAP * LAST_STEPS, last_tick, 0)

    take(cache_sem, kv.at[own_rows, :])
    take(relay_send, relay_buf)
    kv_sent()
    take(part_send, xbuf.at[pl.ds(0, 3 * depth // 8), :])
    take(round_send, gd_ref.at[pl.ds(0, 2), pl.ds(0, 9 * depth // 16), :])
    take(side_send, parts_ref)
    take(give_send, given)
    for step in range(LAST_STEPS):
        take(last_send.at[step], last_arrived(step, pl.ds(0, d_model)))
    take(store_sem, xbuf)


def layers(x_loc, cos_t, sin_t, norm_gain, w_q, w_k, w_v, w_gate, w_up, w_down, w_o):
    tok_count, d_model = x_loc.shape
    head_dim = w_q.shape[2]
    ff_local = w_gate.shape[2]
    rows_per = tok_count // KV_CHUNKS
    chunk_rows = tok_count // CHUNKS
    landed = 3 * chunk_rows // (2 * RING)
    half_cols = d_model // HALVES
    any_spec = pl.BlockSpec(memory_space=pl.ANY)
    vmem_spec = pl.BlockSpec(memory_space=pltpu.VMEM)
    bf16, f32 = jnp.bfloat16, jnp.float32
    dma = pltpu.SemaphoreType.DMA
    shape = jax.ShapeDtypeStruct
    return pl.pallas_call(
        layers_kernel,
        out_shape=[shape((tok_count, d_model), bf16)] + [shape((tok_count, head_dim), bf16)] * 4
        + [shape((RING, ff_local, d_model), bf16), shape((RING, head_dim, d_model), bf16)],
        in_specs=[any_spec, vmem_spec, vmem_spec, vmem_spec] + [any_spec] * 7,
        out_specs=[any_spec] * 7,
        scratch_shapes=[
            pltpu.VMEM((tok_count, d_model), bf16),
            pltpu.VMEM((PART_SLOTS * chunk_rows, d_model), f32),
            pltpu.VMEM((RECV_SLOTS, HALVES, DIRS, landed, half_cols), f32),
            pltpu.VMEM((RECV_SLOTS, HALVES, DIRS, landed, half_cols // RING), f32),
            pltpu.VMEM((tok_count, ff_local), bf16),
            pltpu.VMEM((tok_count, head_dim), bf16),
            pltpu.VMEM((2, ff_local + head_dim, DOWN_TILE), bf16),
            pltpu.VMEM((2, 2, d_model, W_TILE), bf16),
            pltpu.VMEM((2 * CHIPS * tok_count, 2 * head_dim), bf16),
            pltpu.VMEM((tok_count, head_dim), bf16),
            pltpu.VMEM((2, tok_count, head_dim), f32),
            pltpu.VMEM((2, tok_count, 128), f32),
            pltpu.VMEM((2, tok_count, 128), f32),
            pltpu.VMEM((2, rows_per, d_model), bf16),
            pltpu.VMEM((CHUNKS, HALVES, chunk_rows // RING, half_cols // RING), bf16),
            dma((2,)), dma, dma((2, 2)), dma((2, 2)), dma, dma,
            dma((10,)), dma((4, KV_CHUNKS)), dma((4, KV_CHUNKS)), dma, dma((2,)),
            dma, dma((2, RING - 1)), dma, dma,
            dma, dma,
            pltpu.VMEM((KV_CHUNKS, rows_per, W_TILE), bf16), dma, dma,
            pltpu.VMEM((RING, rows_per, head_dim), bf16),
            dma((PART_SLOTS,)), dma((4,)), dma((RECV_SLOTS, STEPS)),
            dma((LAST_STEPS,)), dma((LAST_BLOCKS, LAST_STEPS)), dma((2,)),
            pltpu.SemaphoreType.REGULAR((3,)), pltpu.SemaphoreType.REGULAR((DIRS,)),
        ],
        compiler_params=pltpu.CompilerParams(collective_id=0, has_side_effects=True, vmem_limit_bytes=67043328),
        name='layers',
    )(x_loc, cos_t, sin_t, norm_gain, w_q, w_k, w_v, w_gate, w_up, w_down, w_o)


EMIT_PARTS = 8


def emit_kernel(x_ref, k_first, k_second, v_first, v_second, x_out, k_out, v_out, xbuf, rows, load_sem, store_sem):
    size = x_ref.shape[0] // EMIT_PARTS
    loads, stores = [], []
    for n in range(EMIT_PARTS):
        part = pl.ds(n * size, size)
        loads.append(pltpu.make_async_copy(x_ref.at[part, :], xbuf.at[part, :], load_sem.at[n]))
        stores.append(pltpu.make_async_copy(xbuf.at[part, :], x_out.at[part, :], store_sem.at[n]))
    for n, (ref, out) in enumerate(((k_first, k_out.at[0]), (k_second, k_out.at[1]), (v_first, v_out.at[0]), (v_second, v_out.at[1]))):
        loads.append(pltpu.make_async_copy(ref, rows.at[n], load_sem.at[EMIT_PARTS + n]))
        stores.append(pltpu.make_async_copy(rows.at[n], out, store_sem.at[EMIT_PARTS + n]))
    for copy in loads:
        copy.start()
    for load, store in zip(loads, stores):
        load.wait()
        store.start()
    for copy in stores:
        copy.wait()


def emit(x_out, k_first, k_second, v_first, v_second):
    any_spec = pl.BlockSpec(memory_space=pl.ANY)
    cache = jax.ShapeDtypeStruct((2,) + k_first.shape, jnp.bfloat16)
    return pl.pallas_call(
        emit_kernel,
        out_shape=[jax.ShapeDtypeStruct(x_out.shape, jnp.bfloat16), cache, cache],
        in_specs=[any_spec] * 5,
        out_specs=[any_spec] * 3,
        scratch_shapes=[
            pltpu.VMEM(x_out.shape, jnp.bfloat16),
            pltpu.VMEM((4,) + k_first.shape, jnp.bfloat16),
            pltpu.SemaphoreType.DMA((EMIT_PARTS + 4,)),
            pltpu.SemaphoreType.DMA((EMIT_PARTS + 4,)),
        ],
        compiler_params=pltpu.CompilerParams(vmem_limit_bytes=63 * 1024 * 1024),
        name='emit',
    )(x_out, k_first, k_second, v_first, v_second)


def solution(mesh):
    row_spec = P(('batch', 'seq'), None)
    pos_spec = P(('batch', 'seq'))
    head_spec = P(None, None, 'head', None)
    out_proj_spec = P(None, 'head', None, None)
    col_spec = P(None, None, 'head')
    down_spec = P(None, 'head', None)
    cache_spec = P(None, ('batch', 'seq'), 'head', None)

    def local_forward(x_loc, pos_loc, w_q, w_k, w_v, w_o, w_gate, w_up, w_down, norm_gain):
        tok_count, d_model = x_loc.shape
        layer_count = w_q.shape[0]
        head_dim = w_q.shape[3]
        flat_q, flat_k, flat_v = (w.reshape(layer_count, d_model, head_dim) for w in (w_q, w_k, w_v))
        cos_t, sin_t = rope_tables(pos_loc, head_dim)
        x_out, k_first, v_first, k_second, v_second, _, _ = layers(x_loc, cos_t, sin_t, norm_gain, flat_q, flat_k, flat_v, w_gate, w_up, w_down, w_o)
        x_out, k_all, v_all = emit(x_out, k_first, k_second, v_first, v_second)
        cache_shape = (layer_count, tok_count, 1, head_dim)
        return x_out, k_all.reshape(cache_shape), v_all.reshape(cache_shape)

    return jax.shard_map(local_forward, mesh=mesh, in_specs=(row_spec, pos_spec, head_spec, head_spec, head_spec, out_proj_spec, col_spec, col_spec, down_spec, P(None, None)), out_specs=(row_spec, cache_spec, cache_spec), check_vma=False)
```

```python
import functools
import math
import jax
import jax.numpy as jnp
from jax import lax
from jax.experimental import pallas as pl
from jax.experimental.pallas import tpu as pltpu
from jax.sharding import PartitionSpec as P

ROPE_BASE = 500000.0
EPS = 1e-5


def rope_tables(positions, head_dim):
    half_dim = head_dim // 2
    inv_freq = ROPE_BASE ** (-(jnp.arange(half_dim, dtype=jnp.float32) * 2.0 / head_dim))
    angles = positions.astype(jnp.float32)[..., None] * inv_freq
    return jnp.cos(angles), jnp.sin(angles)


CHIPS = 4
RING = 4
HALVES = 2
DIRS = 2
KV_CHUNKS = 4
W_TILE = 256
NORM_ROWS = 64
CHUNKS = 8
STEPS = 8
PART_SLOTS = 4
RECV_SLOTS = 5
DOWN_TILE = 512
START_GAP = 3
STAGE_GAP = 2
BLOCK_TICK = 19
BLOCK_GAP = 6
LAST_TICK = 43
NEAR_TICKS = ((9, 1), (15, 3), (28, 2))
FAR_TICKS = ((24, 1), (26, 3), (41, 2))
SERVE_TICKS = (27, 31, 36, 42)
GIVE_TICK = 37
OWN_TICK = 3
DONE_TICK = 11
EARLY_TICK = 31
LAST_STEPS = 6
LAST_COLS = 256
LAST_BLOCKS = 16
LAST_GAP = 3


def layers_kernel(x_ref, cos_ref, sin_ref, gain_ref, wq_ref, wk_ref, wv_ref, wg_ref, wu_ref, wd_ref, wo_ref,
                 out_ref, k1_ref, v1_ref, k2_ref, v2_ref, gd_ref, go_ref,
                 xbuf, part, recv_a, recv_b, hid, att, wdo, wtile, kv, qbuf, acc, row_max, row_sum, xs, xres,
                 x_sem, res_sem, w_sem, down_sem, cache_sem, store_sem, kv_send, ici_recv, core_recv, part_send, part_recv,
                 round_send, round_recv, side_send, side_recv, give_send, give_recv, relay_buf, relay_send, relay_recv, att_all, ring_send, gather_send, ring_recv,
                 last_send, last_recv, tile_sem, ready_sem, drained_sem):
    tok_count, d_model = xbuf.shape
    head_dim = qbuf.shape[1]
    half_dim = head_dim // 2
    ff_local = hid.shape[1]
    depth = ff_local + head_dim
    rows_per = tok_count // KV_CHUNKS
    half_rows = tok_count // 2
    lanes = row_max.shape[2]
    chunk_rows = tok_count // CHUNKS
    quarter, eighth = chunk_rows // RING, chunk_rows // (2 * RING)
    half_cols = d_model // HALVES
    piece_cols = half_cols // RING
    bf16, f32 = jnp.bfloat16, jnp.float32
    sign = (1, -1)
    mesh_id = pl.DeviceIdType.MESH

    my_head = lax.axis_index('head')
    pos_z, pos_y = my_head // RING, my_head % RING
    my_seq = lax.axis_index('seq')
    chip, core = my_seq // 2, my_seq % 2
    other = chip * 2 + 1 - core

    def wrap(n):
        return (n + RING) % RING

    def y_peer(d):
        return pos_z * RING + wrap(pos_y + sign[d])

    def z_device(z):
        return wrap(z) * RING + pos_y

    def z_peer(d):
        return z_device(pos_z + sign[d])

    def x_device(n):
        return wrap(chip + n) * 2 + core

    right, left = x_device(1), x_device(-1)

    def span(start, size, unit=None):
        return pl.ds(pl.multiple_of(start, unit or size), size)

    def remote(src, dst, send, recv, **to):
        return pltpu.make_async_remote_copy(src_ref=src, dst_ref=dst, send_sem=send, recv_sem=recv, device_id=to, device_id_type=mesh_id)

    def take(sem, ref):
        remote(ref, ref, sem, sem, head=my_head).wait_recv()

    def x_load(i):
        return pltpu.make_async_copy(x_ref.at[span(i * rows_per, rows_per), :], xs.at[i % 2], x_sem.at[i % 2])

    def weights(layer, piece):
        slot = piece % 2
        if isinstance(piece, int) and piece < 2:
            refs = ((wk_ref, wv_ref), (wq_ref,))[piece]
            return [pltpu.make_async_copy(ref.at[layer], wtile.at[slot, n], w_sem.at[slot, n]) for n, ref in enumerate(refs)]
        cols = span((piece - 2) * W_TILE, W_TILE)
        return [pltpu.make_async_copy(ref.at[layer, :, cols], wtile.at[slot, n], w_sem.at[slot, n]) for n, ref in enumerate((wg_ref, wu_ref))]

    def start(copies):
        for copy in copies:
            copy.start()

    def wait(copies):
        for copy in copies:
            copy.wait()

    down_tiles = d_model // DOWN_TILE

    def down_load(i):
        cols = span(i * DOWN_TILE, DOWN_TILE)
        return [pltpu.make_async_copy(wd_ref.at[0, :, cols], wdo.at[i % 2, pl.ds(0, ff_local), :], down_sem.at[i % 2, 0]),
                pltpu.make_async_copy(wo_ref.at[0, 0, :, cols], wdo.at[i % 2, pl.ds(ff_local, head_dim), :], down_sem.at[i % 2, 1])]

    def kv_copy(origin_chip, origin_core, i, to, send, recv):
        rows = kv.at[span((origin_chip * 2 + origin_core) * tok_count + i * rows_per, rows_per), :]
        return remote(rows, rows, send, recv, seq=to)

    def kv_routes(i):
        def to(number, recv, origin_chip, origin_core, device):
            return lambda: kv_copy(origin_chip, origin_core, i, device, kv_send.at[number], recv)
        inner = jnp.logical_and(chip >= 1, chip < CHIPS - 1)
        return {
            'right': (chip < CHIPS - 1, 'all', to(0, ici_recv.at[0, i], chip, core, right)),
            'wrap': (chip == 0, 'all', to(1, ici_recv.at[2, i], chip, core, left)),
            'relay': (chip == 1, 'late', to(2, ici_recv.at[3, i], chip, core, left)),
            'other': (core == 0, 'all', to(3, core_recv.at[0, i], chip, core, other)),
            'on_right': (inner, 'early', to(4, ici_recv.at[1, i], chip - 1, core, right)),
            'from_relay': (chip == 0, 'late', to(5, ici_recv.at[1, i], 1, core, left)),
            'on_left': (chip == CHIPS - 1, 'late', to(6, ici_recv.at[1, i], 0, core, left)),
            'side1': (chip >= 1, 'all', to(7, core_recv.at[1, i], chip - 1, core, other)),
            'side2': (chip >= 2, 'all', to(8, core_recv.at[2, i], chip - 2, core, other)),
            'side3': (chip >= 3, 'all', to(9, core_recv.at[3, i], chip - 3, core, other)),
        }

    def start_route(i, name):
        condition, which, copy = kv_routes(i)[name]
        if which != 'all':
            late = i >= KV_CHUNKS // 2
            if isinstance(i, int):
                if late != (which == 'late'):
                    return
            else:
                condition = jnp.logical_and(condition, late if which == 'late' else jnp.logical_not(late))

        @pl.when(condition)
        def _():
            copy().start()

    def send_kv(i):
        for name in ('right', 'wrap', 'relay', 'other'):
            start_route(i, name)

    def kv_sent():
        for number, (condition, which, _) in enumerate(kv_routes(0).values()):
            @pl.when(condition)
            def _():
                take(kv_send.at[number], kv.at[pl.ds(0, tok_count if which == 'all' else half_rows), :])

    def serve(back, i):
        @pl.when(chip >= back)
        def _():
            kv_copy(chip - back, core, i, other, kv_send.at[0], ici_recv.at[back - 1, i]).wait_recv()
        start_route(i, 'side%d' % back)
        if back == 1:
            start_route(i, 'on_right')
        if back == 3:
            start_route(i, 'on_left')

    def relay(i):
        def pass_on():
            @pl.when(chip == 0)
            def _():
                kv_copy(1, core, i, left, kv_send.at[0], ici_recv.at[3, i]).wait_recv()
            start_route(i, 'from_relay')
        if not isinstance(i, int):
            pl.when(i >= KV_CHUNKS // 2)(pass_on)
        elif i >= KV_CHUNKS // 2:
            pass_on()

    def serve_all(i):
        serve(1, i)
        serve(3, i)
        relay(i)

    def taken(back, chunks):
        for i in chunks:
            kv_copy(chip - back, 1 - core, i, other, kv_send.at[0], core_recv.at[back, i]).wait_recv()

    def z_parts(step, d):
        copies = []
        for n, (own_ref, all_ref) in enumerate(((wd_ref, gd_ref), (wo_ref, go_ref))):
            size = all_ref.shape[1] // (2 * CHIPS)
            if step == 0:
                rows = span(my_seq * size, size)
                src = own_ref.at[1, rows, :] if n == 0 else own_ref.at[1, 0, rows, :]
                dst = all_ref.at[pos_z, rows, :]
            else:
                rows = span(my_seq * size + d * (size // 2), size // 2)
                src = dst = all_ref.at[wrap(pos_z - sign[d]), rows, :]
            copies.append(remote(src, dst, part_send, part_recv.at[step], head=z_peer(d)))
        return copies

    def part_copies(j, part_chip, part_core, half, send, recv, to):
        copies = []
        for n, ref in enumerate((gd_ref, go_ref)):
            size = ref.shape[1] // (2 * CHIPS)
            first = (part_chip * 2 + part_core) * size
            rows = span(first, size) if half is None else span(first + half * (size // 2), size // 2)
            place = ref.at[wrap(pos_z + j), rows, :]
            copies.append(remote(place, place, send, recv, seq=to))
        return copies

    def own_part(j, d):
        return part_copies(j, chip, core, None, round_send, round_recv.at[0, j - 1], x_device(sign[d]))

    def far_part(j, d):
        return part_copies(j, wrap(chip - sign[d]), core, d, round_send, round_recv.at[1, j - 1], x_device(sign[d]))

    def side_part(j, n, side):
        return part_copies(j, wrap(chip + n), side, None, side_send, side_recv, other)

    def round_start(j):
        for d in range(DIRS):
            start(own_part(j, d))
        start(side_part(j, 0, core))

    def near_parts(j):
        take(round_recv.at[0, j - 1], xbuf.at[pl.ds(0, depth // CHIPS), :])
        for d in range(DIRS):
            start(far_part(j, d) + side_part(j, 3 if d == 0 else 1, core))

    def far_parts(j):
        take(round_recv.at[1, j - 1], xbuf.at[pl.ds(0, depth // (2 * CHIPS)), :])
        start(side_part(j, 2, core))

    def give_hidden(z, i, source):
        cols = span(i * W_TILE, W_TILE)
        return remote(hid.at[span(z * rows_per, rows_per), cols], hidden_place(source, i), give_send, give_recv, head=z_device(z))

    def hidden_place(source, i):
        return xs.at[1, :, span(source * ff_local + i * W_TILE, W_TILE)]

    def via_neighbor(z, i):
        step = jnp.where(i < KV_CHUNKS // 2, 1, -1)
        return remote(hid.at[span(z * rows_per, rows_per), span(i * W_TILE, W_TILE)], relay_buf.at[i], give_send, relay_recv, head=z_device(pos_z + step))

    def relay_hidden(i):
        step = 1 if i < KV_CHUNKS // 2 else -1
        source = wrap(pos_z - step)
        return remote(relay_buf.at[i], hidden_place(source, i), relay_send, give_recv, head=z_device(pos_z + step))

    def send_hidden(z, i):
        away = wrap(z - pos_z)

        @pl.when(away == 2)
        def _():
            via_neighbor(z, i).start()

        @pl.when(away % 2 == 1)
        def _():
            give_hidden(z, i, pos_z).start()

    def give_rows(z, source):
        return remote(att.at[span(z * rows_per, rows_per), :], att_all.at[source], give_send, give_recv, head=z_device(z))

    def norm_rows(x_few, layer):
        x_f32 = x_few.astype(f32)
        inv_rms = lax.rsqrt(jnp.mean(x_f32 * x_f32, axis=-1, keepdims=True) + EPS)
        return (x_f32 * inv_rms * gain_ref[pl.ds(layer, 1), :].astype(f32)).astype(bf16)

    def rope(values, rows):
        cos_t, sin_t = cos_ref[rows, :], sin_ref[rows, :]
        wide = values.astype(bf16).astype(f32)
        first, second = wide[:, :half_dim], wide[:, half_dim:]
        return jnp.concatenate([first * cos_t - second * sin_t, second * cos_t + first * sin_t], axis=1).astype(bf16)

    def dot(a, b):
        return jnp.dot(a, b, preferred_element_type=f32)

    scale = 1.0 / math.sqrt(head_dim)

    def keys_values(normed, i):
        rows = span(i * rows_per, rows_per)
        own = span(my_seq * tok_count + i * rows_per, rows_per)
        kv[own, :head_dim] = rope(dot(normed, wtile[0, 0]), rows)
        kv[own, head_dim:] = dot(normed, wtile[0, 1]).astype(bf16)

    def queries(normed, i):
        rows = span(i * rows_per, rows_per)
        qbuf[rows, :] = (rope(dot(normed, wtile[1, 0]), rows).astype(f32) * scale).astype(bf16)

    def gated(normed, i, tile):
        gate = dot(normed, wtile[tile % 2, 0])
        up = dot(normed, wtile[tile % 2, 1])
        hid[span(i * rows_per, rows_per), span(tile * W_TILE, W_TILE)] = (gate * jax.nn.sigmoid(gate) * up).astype(bf16)

    def attend(key_start, q_half, side, masked, first):
        rows = pl.ds(q_half * half_rows, half_rows)
        some = span(key_start, half_rows)
        logits = lax.dot_general(qbuf[rows, :], kv[some, :head_dim], (((1,), (1,)), ((), ())), preferred_element_type=f32)
        if masked:
            seen = lax.broadcasted_iota(jnp.int32, logits.shape, 0) >= lax.broadcasted_iota(jnp.int32, logits.shape, 1)
            logits = jnp.where(seen, logits, -jnp.inf)
        block_max = jnp.max(logits, axis=-1, keepdims=True)
        if first:
            new_max = jnp.broadcast_to(block_max, (half_rows, lanes))
        else:
            new_max = jnp.maximum(row_max[side, rows, :], block_max)
        prob = jnp.exp(logits - jnp.concatenate([new_max] * (half_rows // lanes), axis=1))
        block_sum = jnp.sum(prob, axis=-1, keepdims=True)
        block_out = dot(prob.astype(bf16), kv[some, head_dim:])
        if first:
            row_sum[side, rows, :] = jnp.broadcast_to(block_sum, (half_rows, lanes))
            acc[side, rows, :] = block_out
        else:
            rescale = jnp.exp(row_max[side, rows, :] - new_max)
            row_sum[side, rows, :] = row_sum[side, rows, :] * rescale + block_sum
            acc[side, rows, :] = acc[side, rows, :] * jnp.concatenate([rescale] * (head_dim // lanes), axis=1) + block_out
        row_max[side, rows, :] = new_max

    def attend_own(layer_half):
        own_start = my_seq * tok_count
        if layer_half == 0:
            attend(own_start, 0, 0, True, True)
            top_rows = pl.ds(0, half_rows)
            row_max[1, top_rows, :] = jnp.full((half_rows, lanes), -jnp.inf, f32)
            row_sum[1, top_rows, :] = jnp.zeros((half_rows, lanes), f32)
            acc[1, top_rows, :] = jnp.zeros((half_rows, head_dim), f32)
        else:
            attend(own_start, 1, 0, False, True)
            attend(own_start + half_rows, 1, 1, True, True)

    def past_start(n):
        later = n - core
        back = jnp.where(later < 2, 1, jnp.where(chip == CHIPS - 1, jnp.where(later < 4, 3, 2), 2))
        block = (chip - back) * 2 + jnp.where(later % 2 == 0, core, 1 - core)
        return jnp.where(jnp.logical_and(core == 1, n == 0), chip * 2, block) * tok_count

    def arrivals(n, chunks):
        @pl.when(jnp.logical_and(core == 1, n == 0))
        def _():
            taken(0, chunks)

        for back in (1, 3, 2):
            place = 0 if back == 1 else 2 if back == 3 else jnp.where(chip == CHIPS - 1, 4, 2)
            if back == 2:
                @pl.when(jnp.logical_and(chip >= back, n == core + place))
                def _():
                    for i in chunks:
                        serve(2, i)

            @pl.when(jnp.logical_and(chip >= back, n == core + place + 1))
            def _():
                taken(back, chunks)

    def visit(n, visits):
        for q_half, side in visits:
            attend(past_start(n) + side * half_rows, q_half, side, False, False)

    def attend_past(first_n, last_n, chunks, visits):
        def past(n, count):
            for r in range(count if chunks else 0):
                arrivals(n + r, chunks)
            for r in range(count):
                visit(n + r, visits)

        def two(p, carry):
            past(first_n + 2 * p, 2)
            return carry

        count = last_n - first_n
        lax.fori_loop(0, count // 2, two, 0)

        @pl.when(count % 2 == 1)
        def _():
            past(last_n - 1, 1)

    near_count = my_seq - jnp.where(chip >= 2, 2, 0)

    def finish(i, spread):
        rows = pl.ds(i * rows_per, rows_per)
        top = jnp.maximum(row_max[0, rows, :], row_max[1, rows, :])
        shares = [jnp.exp(row_max[side, rows, :] - top) for side in range(2)]
        total = shares[0] * row_sum[0, rows, :] + shares[1] * row_sum[1, rows, :]
        wide = [jnp.concatenate([w] * (head_dim // lanes), axis=1) for w in shares + [total]]
        att[rows, :] = ((acc[0, rows, :] * wide[0] + acc[1, rows, :] * wide[1]) / wide[2]).astype(bf16)
        if spread:
            @pl.when(i != pos_z)
            def _():
                give_rows(i, pos_z).start()

    first_pos, second_pos = (pos_y, pos_z), (pos_z, pos_y)
    first_peer, second_peer = (y_peer, z_peer), (z_peer, y_peer)

    def part_rows(chunk, piece, offset, count):
        return span((chunk % PART_SLOTS) * chunk_rows + piece * quarter + offset, count, eighth)

    def x_rows(chunk, piece, offset, count):
        return span(chunk * chunk_rows + piece * quarter + offset, count, eighth)

    def cols_of(h, piece):
        return span(h * half_cols + piece * piece_cols, piece_cols)

    def half_of(h):
        return pl.ds(h * half_cols, half_cols)

    def message(step, chunk, h, d):
        p1, p2, s = first_pos[h], second_pos[h], sign[d]
        slot = chunk % RECV_SLOTS
        if step == 0:
            src, dst = part.at[part_rows(chunk, wrap(p1 + 2), d * eighth, eighth), half_of(h)], recv_a.at[slot, h, d, pl.ds(quarter, eighth), :]
        elif step == 1:
            src, dst = part.at[part_rows(chunk, wrap(p1 + s), 0, quarter), half_of(h)], recv_a.at[slot, h, d, pl.ds(0, quarter), :]
        elif step == 2:
            src, dst = part.at[part_rows(chunk, p1, d * eighth, eighth), cols_of(h, wrap(p2 + 2))], recv_b.at[slot, h, d, pl.ds(quarter, eighth), :]
        elif step == 3:
            src, dst = part.at[part_rows(chunk, p1, 0, quarter), cols_of(h, wrap(p2 + s))], recv_b.at[slot, h, d, pl.ds(0, quarter), :]
        elif step == 4:
            src = dst = xbuf.at[x_rows(chunk, p1, 0, quarter), cols_of(h, p2)]
        elif step == 5:
            src = dst = xbuf.at[x_rows(chunk, p1, d * eighth, eighth), cols_of(h, wrap(p2 - s))]
        elif step == 6:
            src = dst = xbuf.at[x_rows(chunk, p1, 0, quarter), half_of(h)]
        else:
            src = dst = xbuf.at[x_rows(chunk, wrap(p1 - s), d * eighth, eighth), half_of(h)]
        peer = (first_peer if step in (0, 1, 6, 7) else second_peer)[h](d)
        return remote(src, dst, ring_send.at[chunk % PART_SLOTS] if step < 4 else gather_send.at[step - 4], ring_recv.at[slot, step], head=peer)

    def arrived_in(step, count=1):
        rows = (2 * eighth, 2 * quarter, eighth // 2, quarter // 2, quarter // 2, quarter // 2, 2 * quarter, quarter)[step] * count
        return (part if step < 4 else xbuf).at[pl.ds(0, rows), pl.ds(0, half_cols if step == 5 else d_model)]

    def partials_sent(slot):
        take(ring_send.at[slot], part.at[pl.ds(0, 2 * eighth + 2 * quarter + eighth // 2 + quarter // 2), :])

    def residual_load(chunk, h):
        return pltpu.make_async_copy(x_ref.at[x_rows(chunk, first_pos[h], 0, quarter), cols_of(h, second_pos[h])], xres.at[chunk, h], res_sem)

    def project(chunk):
        rows = span(chunk * chunk_rows, chunk_rows)
        slot_rows = span((chunk % PART_SLOTS) * chunk_rows, chunk_rows)

        def one_tile(i, carry):
            @pl.when(jnp.logical_or(chunk < CHUNKS - 1, i < down_tiles - 1))
            def _():
                start(down_load((i + 1) % down_tiles))

            wait(down_load(i))
            total = dot(hid[rows, :], wdo[i % 2, :ff_local, :])
            part[slot_rows, span(i * DOWN_TILE, DOWN_TILE)] = total + dot(att[rows, :], wdo[i % 2, ff_local:, :])
            return carry

        lax.fori_loop(0, down_tiles, one_tile, 0)

    def stage(number, chunk):
        slot = chunk % RECV_SLOTS
        if number == 0:
            @pl.when(chunk >= PART_SLOTS)
            def _():
                partials_sent(chunk % PART_SLOTS)
            project(chunk)
        else:
            take(ring_recv.at[slot, number - 1], arrived_in(number - 1))
        if number == 4:
            @pl.when(chunk == 0)
            def _():
                take(res_sem, xres)
        for h in range(HALVES):
            p1, p2 = first_pos[h], second_pos[h]
            if number in (1, 3):
                for d in range(DIRS):
                    if number == 1:
                        rows, cols, arrived = part_rows(chunk, wrap(p1 + sign[d]), d * eighth, eighth), half_of(h), recv_a
                    else:
                        rows, cols, arrived = part_rows(chunk, p1, d * eighth, eighth), cols_of(h, wrap(p2 + sign[d])), recv_b
                    part[rows, cols] = part[rows, cols] + arrived[slot, h, d, pl.ds(quarter, eighth), :]
            if number == 2:
                rows = part_rows(chunk, p1, 0, quarter)
                part[rows, half_of(h)] = part[rows, half_of(h)] + recv_a[slot, h, 0, pl.ds(0, quarter), :] + recv_a[slot, h, 1, pl.ds(0, quarter), :]
            if number == 4:
                rows, cols = part_rows(chunk, p1, 0, quarter), cols_of(h, p2)
                total = part[rows, cols] + recv_b[slot, h, 0, pl.ds(0, quarter), :] + recv_b[slot, h, 1, pl.ds(0, quarter), :]
                update = total.astype(bf16).astype(f32)
                xbuf[x_rows(chunk, p1, 0, quarter), cols] = (xres[chunk, h].astype(f32) + update).astype(bf16)
            if number < STEPS:
                for d in range(DIRS):
                    message(number, chunk, h, d).start()

    x_load(0).start()
    start(weights(0, 0))
    x_load(1).start()
    start(weights(0, 1))
    barrier = pltpu.get_barrier_semaphore()
    for peer in (left, right, other):
        pl.semaphore_signal(barrier, inc=1, device_id={'seq': peer}, device_id_type=mesh_id)
    for peer in [z_device(pos_z + j) for j in range(1, RING)] + [y_peer(d) for d in range(DIRS)]:
        pl.semaphore_signal(barrier, inc=1, device_id={'head': peer}, device_id_type=mesh_id)

    def prepare(i, carry):
        x_load(i).wait()

        def few(n, inner):
            xbuf[span(i * rows_per + n * NORM_ROWS, NORM_ROWS), :] = norm_rows(xs[i % 2, span(n * NORM_ROWS, NORM_ROWS), :], 0)
            return inner

        lax.fori_loop(0, rows_per // NORM_ROWS, few, 0)

        @pl.when(i + 2 < KV_CHUNKS)
        def _():
            x_load(i + 2).start()

        @pl.when(i == 0)
        def _():
            wait(weights(0, 0))

        keys_values(xbuf[span(i * rows_per, rows_per), :], i)

        @pl.when(i == 0)
        def _():
            pl.semaphore_wait(barrier, 8)

        send_kv(i)

        @pl.when(i == 0)
        def _():
            for d in range(DIRS):
                start(z_parts(0, d))
        return carry

    lax.fori_loop(0, KV_CHUNKS, prepare, 0)
    start(weights(0, 2))
    own_rows = span(my_seq * tok_count, tok_count)

    def cache_stores(layer):
        k_ref, v_ref = ((k1_ref, v1_ref), (k2_ref, v2_ref))[layer]
        return [pltpu.make_async_copy(kv.at[own_rows, pl.ds(0, head_dim)], k_ref, cache_sem),
                pltpu.make_async_copy(kv.at[own_rows, pl.ds(head_dim, head_dim)], v_ref, cache_sem)]

    start(cache_stores(0))
    wait(weights(0, 1))

    def query(i, carry):
        queries(xbuf[span(i * rows_per, rows_per), :], i)
        return carry

    lax.fori_loop(0, KV_CHUNKS, query, 0)
    start(weights(0, 3))
    start(down_load(0))

    def residuals(n, carry):
        for h in range(HALVES):
            residual_load(n, h).start()
        return carry

    lax.fori_loop(0, CHUNKS, residuals, 0)

    def gate_half(half, tile):
        wait(weights(0, tile + 2))

        def rows_step(i, inner):
            gated(xbuf[span(i * rows_per, rows_per), :], i, tile)
            return inner

        lax.fori_loop(half * KV_CHUNKS // 2, (half + 1) * KV_CHUNKS // 2, rows_step, 0)

        @pl.when(tile < 2)
        def _():
            start(weights(0, tile + 4))

        for last in (2, 3):
            @pl.when(tile == last)
            def _():
                start(weights(1, last - 2) if half else weights(0, last))

    def first_half(tile, carry):
        gate_half(0, tile)

        @pl.when(tile < 3)
        def _():
            serve_all(tile)
        return carry

    def second_half(tile, carry):
        gate_half(1, tile)

        @pl.when(tile == 0)
        def _():
            serve_all(3)
            attend_past(0, near_count, range(KV_CHUNKS), ((0, 0), (0, 1)))
            take(part_recv.at[0], xbuf.at[pl.ds(0, depth // CHIPS), :])
            for d in range(DIRS):
                start(z_parts(1, d))
        return carry

    lax.fori_loop(0, ff_local // W_TILE, first_half, 0)
    attend_own(0)
    lax.fori_loop(0, 2, second_half, 0)
    attend_past(near_count, my_seq, range(KV_CHUNKS), ((0, 0), (0, 1)))
    finish(0, False)
    finish(1, False)
    round_start(1)
    round_start(3)

    def block_work(j, phase):
        @pl.when(phase == 0)
        def _():
            @pl.when(j == 0)
            def _():
                for n in range(3):
                    pl.semaphore_wait(ready_sem.at[n], 1)

            def few(n, inner):
                xs[0, span(n * NORM_ROWS, NORM_ROWS), :] = norm_rows(xbuf[span(j * rows_per + n * NORM_ROWS, NORM_ROWS), :], 1)
                return inner

            lax.fori_loop(0, rows_per // NORM_ROWS, few, 0)
            wait(weights(1, 0))
            keys_values(xs[0], j)
            send_kv(j)
            start(weights(1, 2))

        @pl.when(phase == 1)
        def _():
            wait(weights(1, 1))
            queries(xs[0], j)
            start(weights(1, 3))

        @pl.when(jnp.logical_and(phase >= 1, phase <= 4))
        def _():
            tile = phase - 1
            wait(weights(1, tile + 2))
            gated(xs[0], j, tile)

            @pl.when(tile < 2)
            def _():
                start(weights(1, tile + 4))

            @pl.when(jnp.logical_and(tile == 2, j < KV_CHUNKS - 1))
            def _():
                start(weights(1, 0))

            @pl.when(jnp.logical_and(tile == 3, j < KV_CHUNKS - 1))
            def _():
                start(weights(1, 1))

            @pl.when(j == KV_CHUNKS - 1)
            def _():
                send_hidden(j, tile)

    def tick(t, carry):
        for number in range(STEPS, -1, -1):
            place = t - STAGE_GAP * number
            chunk = place // START_GAP

            @pl.when(jnp.logical_and(place >= 0, jnp.logical_and(place % START_GAP == 0, chunk < CHUNKS)))
            def _():
                stage(number, chunk)

        @pl.when(jnp.logical_or(t == 1, t == 3))
        def _():
            gate_half(1, 2 + t // 2)

        @pl.when(t == OWN_TICK)
        def _():
            attend_own(1)

        @pl.when(jnp.logical_and(t > OWN_TICK, jnp.logical_and(t < DONE_TICK, t - OWN_TICK <= my_seq)))
        def _():
            visit(t - OWN_TICK - 1, ((1, 0), (1, 1)))

        @pl.when(t == EARLY_TICK)
        def _():
            attend_own(0)

        early = t - EARLY_TICK - 1

        @pl.when(jnp.logical_and(early >= 0, jnp.logical_and(early < 7, early < my_seq)))
        def _():
            arrivals(early, (0, 1))
            visit(early, ((0, 0),))

        @pl.when(t == 2)
        def _():
            take(part_recv.at[1], xbuf.at[pl.ds(0, depth // (2 * CHIPS)), :])
            round_start(2)

        @pl.when(t == DONE_TICK)
        def _():
            finish(2, False)
            finish(3, False)
            kv_sent()
            take(cache_sem, kv.at[own_rows, :])
            for n, peer in enumerate((left, right, other)):
                pl.semaphore_signal(ready_sem.at[n], inc=1, device_id={'seq': peer}, device_id_type=mesh_id)

        for when, j in NEAR_TICKS:
            @pl.when(t == when)
            def _():
                near_parts(j)

        for when, j in FAR_TICKS:
            @pl.when(t == when)
            def _():
                far_parts(j)

        @pl.when(t == GIVE_TICK)
        def _():
            for i in range(KV_CHUNKS):
                for z in range(KV_CHUNKS - 1):
                    send_hidden(z, i)

        late = t - BLOCK_TICK

        @pl.when(late >= 0)
        def _():
            block_work(late // BLOCK_GAP, late % BLOCK_GAP)

        for i, when in enumerate(SERVE_TICKS):
            @pl.when(t == when)
            def _():
                serve_all(i)
        return carry

    lax.fori_loop(0, LAST_TICK, tick, 0)

    for slot in range(PART_SLOTS):
        partials_sent(slot)
    for step in range(4, STEPS):
        take(gather_send.at[step - 4], arrived_in(step, CHUNKS))
    for d in range(DIRS):
        pl.semaphore_signal(drained_sem.at[d], inc=1, device_id={'head': y_peer(d)}, device_id_type=mesh_id)
    start(cache_stores(1))
    attend_own(1)
    attend_past(0, my_seq, (), ((1, 0),))
    take(relay_recv, relay_buf)
    for i in range(KV_CHUNKS):
        relay_hidden(i).start()
    attend_past(0, near_count, (2, 3), ((0, 1), (1, 1)))
    attend_past(near_count, my_seq, (2, 3), ((0, 1),))
    finish(0, True)
    finish(1, True)
    attend_past(near_count, my_seq, (), ((1, 1),))
    finish(2, True)
    finish(3, True)
    parts_ref = gd_ref.at[pl.ds(0, 2), pl.ds(0, 3 * depth // 4), :]
    take(side_recv, parts_ref)

    quarter_rows = rows_per // RING

    def block_cols(c):
        return span(c * LAST_COLS, LAST_COLS)

    def tile_place(c, j, first, size):
        return wtile.at[c % 2, j // 2, pl.ds((j % 2) * depth + first, size), :]

    def tile_loads(c):
        copies = []
        for j in range(RING):
            z = wrap(pos_z + j)
            down = wd_ref.at[1, :, block_cols(c)] if j == 0 else gd_ref.at[z, :, block_cols(c)]
            out = wo_ref.at[1, 0, :, block_cols(c)] if j == 0 else go_ref.at[z, :, block_cols(c)]
            copies.append(pltpu.make_async_copy(down, tile_place(c, j, 0, ff_local), tile_sem.at[c % 2]))
            copies.append(pltpu.make_async_copy(out, tile_place(c, j, ff_local, head_dim), tile_sem.at[c % 2]))
        return copies

    start(tile_loads(0))
    given = hid.at[pl.ds(0, (RING - 1) * rows_per * depth // ff_local), :]
    take(give_recv, given)
    for d in range(DIRS):
        pl.semaphore_wait(drained_sem.at[d], 1)

    def quarter_of(piece, offset, size):
        return span(piece * quarter_rows + offset, size, quarter_rows // 2)

    def landed(d, first, size):
        return pl.ds(rows_per + d * (3 * quarter_rows // 2) + first, size)

    def rows_at(z, piece, offset, size):
        return span(z * rows_per + piece * quarter_rows + offset, size, quarter_rows // 2)

    def last_messages(step, c, d, z_first):
        s, cols, half = sign[d], block_cols(c), quarter_rows // 2
        near, behind, back = wrap(pos_y + s), wrap(pos_y - s), wrap(pos_z - s)
        along_y = step < 2 or (step < 4) != z_first
        if step == 0:
            pairs = [(part.at[quarter_of(wrap(pos_y + 2), d * half, half), cols], part.at[landed(d, quarter_rows, half), cols])]
        elif step == 1:
            pairs = [(part.at[quarter_of(near, 0, quarter_rows), cols], part.at[landed(d, 0, quarter_rows), cols])]
        else:
            if step == 2:
                rows = [rows_at(pos_z, pos_y, 0, quarter_rows)]
            elif step == 3:
                rows = [rows_at(back, pos_y, d * half, half) if z_first else rows_at(pos_z, behind, d * half, half)]
            elif step == 4:
                rows = [rows_at(z, pos_y, 0, quarter_rows) for z in range(RING)] if z_first else [rows_at(pos_z, 0, 0, rows_per)]
            else:
                rows = [rows_at(z, behind, d * half, half) for z in range(RING)] if z_first else [rows_at(back, 0, d * (rows_per // 2), rows_per // 2)]
            pairs = [(xbuf.at[r, cols], xbuf.at[r, cols]) for r in rows]
        to = (y_peer if along_y else z_peer)(d)
        return [remote(src, dst, last_send.at[step], last_recv.at[c, step], head=to) for src, dst in pairs]

    def last_arrived(step, cols):
        rows = (quarter_rows, 2 * quarter_rows, 2 * quarter_rows, quarter_rows, 2 * rows_per, rows_per)[step]
        return (part if step < 2 else xbuf).at[pl.ds(0, rows), cols]

    def send_last(step, c):
        def both(z_first):
            for d in range(DIRS):
                start(last_messages(step, c, d, z_first))

        if step < 2:
            both(False)
            return
        z_first = jnp.logical_and(c >= 5, c % 2 == 1)

        @pl.when(z_first)
        def _():
            both(True)

        @pl.when(jnp.logical_not(z_first))
        def _():
            both(False)

    def out_store(c):
        return pltpu.make_async_copy(xbuf.at[:, block_cols(c)], out_ref.at[:, block_cols(c)], store_sem)

    def last_project(c):
        @pl.when(c + 1 < LAST_BLOCKS)
        def _():
            start(tile_loads(c + 1))

        take(tile_sem.at[c % 2], wtile.at[c % 2, :, pl.ds(0, 2 * depth), :])
        total = None
        for j in range(RING):
            z = wrap(pos_z + j)
            own = span(pos_z * rows_per, rows_per)
            hidden_rows = hid[own, :] if j == 0 else xs[1, :, span(z * ff_local, ff_local)]
            out_rows = att[own, :] if j == 0 else att_all[z]
            term = dot(hidden_rows, wtile[c % 2, j // 2, pl.ds((j % 2) * depth, ff_local), :])
            term = term + dot(out_rows, wtile[c % 2, j // 2, pl.ds((j % 2) * depth + ff_local, head_dim), :])
            total = term if total is None else total + term
        part[pl.ds(0, rows_per), block_cols(c)] = total

    def last_stage(number, c):
        cols, half = block_cols(c), quarter_rows // 2
        if number == 0:
            last_project(c)
        else:
            take(last_recv.at[c, number - 1], last_arrived(number - 1, cols))
        if number == 1:
            for d in range(DIRS):
                piece = quarter_of(wrap(pos_y + sign[d]), d * half, half)
                part[piece, cols] = part[piece, cols] + part[landed(d, quarter_rows, half), cols]
        if number == 2:
            own = quarter_of(pos_y, 0, quarter_rows)
            total = part[own, cols] + part[landed(0, 0, quarter_rows), cols] + part[landed(1, 0, quarter_rows), cols]
            update = total.astype(bf16).astype(f32)
            rows = rows_at(pos_z, pos_y, 0, quarter_rows)
            xbuf[rows, cols] = (xbuf[rows, cols].astype(f32) + update).astype(bf16)
        if number < LAST_STEPS:
            send_last(number, c)
        else:
            out_store(c).start()

    def last_tick(t, carry):
        for number in range(LAST_STEPS, -1, -1):
            c = t - LAST_GAP * number

            @pl.when(jnp.logical_and(c >= 0, c < LAST_BLOCKS))
            def _():
                last_stage(number, c)
        return carry

    lax.fori_loop(0, LAST_BLOCKS + LAST_GAP * LAST_STEPS, last_tick, 0)

    take(cache_sem, kv.at[own_rows, :])
    take(relay_send, relay_buf)
    kv_sent()
    take(part_send, xbuf.at[pl.ds(0, 3 * depth // 8), :])
    take(round_send, gd_ref.at[pl.ds(0, 2), pl.ds(0, 9 * depth // 16), :])
    take(side_send, parts_ref)
    take(give_send, given)
    for step in range(LAST_STEPS):
        take(last_send.at[step], last_arrived(step, pl.ds(0, d_model)))
    take(store_sem, xbuf)


def layers(x_loc, cos_t, sin_t, norm_gain, w_q, w_k, w_v, w_gate, w_up, w_down, w_o):
    tok_count, d_model = x_loc.shape
    head_dim = w_q.shape[2]
    ff_local = w_gate.shape[2]
    rows_per = tok_count // KV_CHUNKS
    chunk_rows = tok_count // CHUNKS
    landed = 3 * chunk_rows // (2 * RING)
    half_cols = d_model // HALVES
    any_spec = pl.BlockSpec(memory_space=pl.ANY)
    vmem_spec = pl.BlockSpec(memory_space=pltpu.VMEM)
    bf16, f32 = jnp.bfloat16, jnp.float32
    dma = pltpu.SemaphoreType.DMA
    shape = jax.ShapeDtypeStruct
    return pl.pallas_call(
        layers_kernel,
        out_shape=[shape((tok_count, d_model), bf16)] + [shape((tok_count, head_dim), bf16)] * 4
        + [shape((RING, ff_local, d_model), bf16), shape((RING, head_dim, d_model), bf16)],
        in_specs=[any_spec, vmem_spec, vmem_spec, vmem_spec] + [any_spec] * 7,
        out_specs=[any_spec] * 7,
        scratch_shapes=[
            pltpu.VMEM((tok_count, d_model), bf16),
            pltpu.VMEM((PART_SLOTS * chunk_rows, d_model), f32),
            pltpu.VMEM((RECV_SLOTS, HALVES, DIRS, landed, half_cols), f32),
            pltpu.VMEM((RECV_SLOTS, HALVES, DIRS, landed, half_cols // RING), f32),
            pltpu.VMEM((tok_count, ff_local), bf16),
            pltpu.VMEM((tok_count, head_dim), bf16),
            pltpu.VMEM((2, ff_local + head_dim, DOWN_TILE), bf16),
            pltpu.VMEM((2, 2, d_model, W_TILE), bf16),
            pltpu.VMEM((2 * CHIPS * tok_count, 2 * head_dim), bf16),
            pltpu.VMEM((tok_count, head_dim), bf16),
            pltpu.VMEM((2, tok_count, head_dim), f32),
            pltpu.VMEM((2, tok_count, 128), f32),
            pltpu.VMEM((2, tok_count, 128), f32),
            pltpu.VMEM((2, rows_per, d_model), bf16),
            pltpu.VMEM((CHUNKS, HALVES, chunk_rows // RING, half_cols // RING), bf16),
            dma((2,)), dma, dma((2, 2)), dma((2, 2)), dma, dma,
            dma((10,)), dma((4, KV_CHUNKS)), dma((4, KV_CHUNKS)), dma, dma((2,)),
            dma, dma((2, RING - 1)), dma, dma,
            dma, dma,
            pltpu.VMEM((KV_CHUNKS, rows_per, W_TILE), bf16), dma, dma,
            pltpu.VMEM((RING, rows_per, head_dim), bf16),
            dma((PART_SLOTS,)), dma((4,)), dma((RECV_SLOTS, STEPS)),
            dma((LAST_STEPS,)), dma((LAST_BLOCKS, LAST_STEPS)), dma((2,)),
            pltpu.SemaphoreType.REGULAR((3,)), pltpu.SemaphoreType.REGULAR((DIRS,)),
        ],
        compiler_params=pltpu.CompilerParams(collective_id=0, has_side_effects=True, vmem_limit_bytes=67043328),
        name='layers',
    )(x_loc, cos_t, sin_t, norm_gain, w_q, w_k, w_v, w_gate, w_up, w_down, w_o)


EMIT_PARTS = 8


def emit_kernel(x_ref, k_first, k_second, v_first, v_second, x_out, k_out, v_out, xbuf, rows, load_sem, store_sem):
    size = x_ref.shape[0] // EMIT_PARTS
    loads, stores = [], []
    for n in range(EMIT_PARTS):
        part = pl.ds(n * size, size)
        loads.append(pltpu.make_async_copy(x_ref.at[part, :], xbuf.at[part, :], load_sem.at[n]))
        stores.append(pltpu.make_async_copy(xbuf.at[part, :], x_out.at[part, :], store_sem.at[n]))
    for n, (ref, out) in enumerate(((k_first, k_out.at[0]), (k_second, k_out.at[1]), (v_first, v_out.at[0]), (v_second, v_out.at[1]))):
        loads.append(pltpu.make_async_copy(ref, rows.at[n], load_sem.at[EMIT_PARTS + n]))
        stores.append(pltpu.make_async_copy(rows.at[n], out, store_sem.at[EMIT_PARTS + n]))
    for copy in loads:
        copy.start()
    for load, store in zip(loads, stores):
        load.wait()
        store.start()
    for copy in stores:
        copy.wait()


def emit(x_out, k_first, k_second, v_first, v_second):
    any_spec = pl.BlockSpec(memory_space=pl.ANY)
    cache = jax.ShapeDtypeStruct((2,) + k_first.shape, jnp.bfloat16)
    return pl.pallas_call(
        emit_kernel,
        out_shape=[jax.ShapeDtypeStruct(x_out.shape, jnp.bfloat16), cache, cache],
        in_specs=[any_spec] * 5,
        out_specs=[any_spec] * 3,
        scratch_shapes=[
            pltpu.VMEM(x_out.shape, jnp.bfloat16),
            pltpu.VMEM((4,) + k_first.shape, jnp.bfloat16),
            pltpu.SemaphoreType.DMA((EMIT_PARTS + 4,)),
            pltpu.SemaphoreType.DMA((EMIT_PARTS + 4,)),
        ],
        compiler_params=pltpu.CompilerParams(vmem_limit_bytes=63 * 1024 * 1024),
        name='emit',
    )(x_out, k_first, k_second, v_first, v_second)


def solution(mesh):
    row_spec = P(('batch', 'seq'), None)
    pos_spec = P(('batch', 'seq'))
    head_spec = P(None, None, 'head', None)
    out_proj_spec = P(None, 'head', None, None)
    col_spec = P(None, None, 'head')
    down_spec = P(None, 'head', None)
    cache_spec = P(None, ('batch', 'seq'), 'head', None)

    def local_forward(x_loc, pos_loc, w_q, w_k, w_v, w_o, w_gate, w_up, w_down, norm_gain):
        tok_count, d_model = x_loc.shape
        layer_count = w_q.shape[0]
        head_dim = w_q.shape[3]
        flat_q, flat_k, flat_v = (w.reshape(layer_count, d_model, head_dim) for w in (w_q, w_k, w_v))
        cos_t, sin_t = rope_tables(pos_loc, head_dim)
        x_out, k_first, v_first, k_second, v_second, _, _ = layers(x_loc, cos_t, sin_t, norm_gain, flat_q, flat_k, flat_v, w_gate, w_up, w_down, w_o)
        x_out, k_all, v_all = emit(x_out, k_first, k_second, v_first, v_second)
        cache_shape = (layer_count, tok_count, 1, head_dim)
        return x_out, k_all.reshape(cache_shape), v_all.reshape(cache_shape)

    return jax.shard_map(local_forward, mesh=mesh, in_specs=(row_spec, pos_spec, head_spec, head_spec, head_spec, out_proj_spec, col_spec, col_spec, down_spec, P(None, None)), out_specs=(row_spec, cache_spec, cache_spec), check_vma=False)
```

```python
import functools
import math
import jax
import jax.numpy as jnp
from jax import lax
from jax.experimental import pallas as pl
from jax.experimental.pallas import tpu as pltpu
from jax.sharding import PartitionSpec as P

ROPE_BASE = 500000.0
EPS = 1e-5


def rope_tables(positions, head_dim):
    half_dim = head_dim // 2
    inv_freq = ROPE_BASE ** (-(jnp.arange(half_dim, dtype=jnp.float32) * 2.0 / head_dim))
    angles = positions.astype(jnp.float32)[..., None] * inv_freq
    return jnp.cos(angles), jnp.sin(angles)


CHIPS = 4
RING = 4
HALVES = 2
DIRS = 2
KV_CHUNKS = 4
W_TILE = 256
NORM_ROWS = 64
CHUNKS = 8
STEPS = 8
PART_SLOTS = 4
RECV_SLOTS = 5
DOWN_TILE = 512
START_GAP = 3
STAGE_GAP = 2
BLOCK_TICK = 19
BLOCK_GAP = 6
LAST_TICK = 43
NEAR_TICKS = ((9, 1), (15, 3), (20, 2))
FAR_TICKS = ((24, 1), (26, 3), (36, 2))
SERVE_TICKS = (27, 31, 36, 42)
GIVE_TICK = 37
OWN_TICK = 3
DONE_TICK = 11
EARLY_TICK = 31
LAST_STEPS = 6
LAST_COLS = 256
LAST_BLOCKS = 16
LAST_GAP = 3


def layers_kernel(x_ref, cos_ref, sin_ref, gain_ref, wq_ref, wk_ref, wv_ref, wg_ref, wu_ref, wd_ref, wo_ref,
                 out_ref, k1_ref, v1_ref, k2_ref, v2_ref, gd_ref, go_ref,
                 xbuf, part, recv_a, recv_b, hid, att, wdo, wtile, kv, qbuf, acc, row_max, row_sum, xs, xres,
                 x_sem, res_sem, w_sem, down_sem, cache_sem, store_sem, kv_send, ici_recv, core_recv, part_send, part_recv,
                 round_send, round_recv, side_send, side_recv, give_send, give_recv, relay_buf, relay_send, relay_recv, att_all, ring_send, gather_send, ring_recv,
                 last_send, last_recv, tile_sem, ready_sem, drained_sem):
    tok_count, d_model = xbuf.shape
    head_dim = qbuf.shape[1]
    half_dim = head_dim // 2
    ff_local = hid.shape[1]
    depth = ff_local + head_dim
    rows_per = tok_count // KV_CHUNKS
    half_rows = tok_count // 2
    lanes = row_max.shape[2]
    chunk_rows = tok_count // CHUNKS
    quarter, eighth = chunk_rows // RING, chunk_rows // (2 * RING)
    half_cols = d_model // HALVES
    piece_cols = half_cols // RING
    bf16, f32 = jnp.bfloat16, jnp.float32
    sign = (1, -1)
    mesh_id = pl.DeviceIdType.MESH

    my_head = lax.axis_index('head')
    pos_z, pos_y = my_head // RING, my_head % RING
    my_seq = lax.axis_index('seq')
    chip, core = my_seq // 2, my_seq % 2
    other = chip * 2 + 1 - core

    def wrap(n):
        return (n + RING) % RING

    def y_peer(d):
        return pos_z * RING + wrap(pos_y + sign[d])

    def z_device(z):
        return wrap(z) * RING + pos_y

    def z_peer(d):
        return z_device(pos_z + sign[d])

    def x_device(n):
        return wrap(chip + n) * 2 + core

    right, left = x_device(1), x_device(-1)

    def span(start, size, unit=None):
        return pl.ds(pl.multiple_of(start, unit or size), size)

    def remote(src, dst, send, recv, **to):
        return pltpu.make_async_remote_copy(src_ref=src, dst_ref=dst, send_sem=send, recv_sem=recv, device_id=to, device_id_type=mesh_id)

    def take(sem, ref):
        remote(ref, ref, sem, sem, head=my_head).wait_recv()

    def x_load(i):
        return pltpu.make_async_copy(x_ref.at[span(i * rows_per, rows_per), :], xs.at[i % 2], x_sem.at[i % 2])

    def weights(layer, piece):
        slot = piece % 2
        if isinstance(piece, int) and piece < 2:
            refs = ((wk_ref, wv_ref), (wq_ref,))[piece]
            return [pltpu.make_async_copy(ref.at[layer], wtile.at[slot, n], w_sem.at[slot, n]) for n, ref in enumerate(refs)]
        cols = span((piece - 2) * W_TILE, W_TILE)
        return [pltpu.make_async_copy(ref.at[layer, :, cols], wtile.at[slot, n], w_sem.at[slot, n]) for n, ref in enumerate((wg_ref, wu_ref))]

    def start(copies):
        for copy in copies:
            copy.start()

    def wait(copies):
        for copy in copies:
            copy.wait()

    down_tiles = d_model // DOWN_TILE

    def down_load(i):
        cols = span(i * DOWN_TILE, DOWN_TILE)
        return [pltpu.make_async_copy(wd_ref.at[0, :, cols], wdo.at[i % 2, pl.ds(0, ff_local), :], down_sem.at[i % 2, 0]),
                pltpu.make_async_copy(wo_ref.at[0, 0, :, cols], wdo.at[i % 2, pl.ds(ff_local, head_dim), :], down_sem.at[i % 2, 1])]

    def kv_copy(origin_chip, origin_core, i, to, send, recv):
        rows = kv.at[span((origin_chip * 2 + origin_core) * tok_count + i * rows_per, rows_per), :]
        return remote(rows, rows, send, recv, seq=to)

    def kv_routes(i):
        def to(number, recv, origin_chip, origin_core, device):
            return lambda: kv_copy(origin_chip, origin_core, i, device, kv_send.at[number], recv)
        inner = jnp.logical_and(chip >= 1, chip < CHIPS - 1)
        return {
            'right': (chip < CHIPS - 1, 'all', to(0, ici_recv.at[0, i], chip, core, right)),
            'wrap': (chip == 0, 'all', to(1, ici_recv.at[2, i], chip, core, left)),
            'relay': (chip == 1, 'late', to(2, ici_recv.at[3, i], chip, core, left)),
            'other': (core == 0, 'all', to(3, core_recv.at[0, i], chip, core, other)),
            'on_right': (inner, 'early', to(4, ici_recv.at[1, i], chip - 1, core, right)),
            'from_relay': (chip == 0, 'late', to(5, ici_recv.at[1, i], 1, core, left)),
            'on_left': (chip == CHIPS - 1, 'late', to(6, ici_recv.at[1, i], 0, core, left)),
            'side1': (chip >= 1, 'all', to(7, core_recv.at[1, i], chip - 1, core, other)),
            'side2': (chip >= 2, 'all', to(8, core_recv.at[2, i], chip - 2, core, other)),
            'side3': (chip >= 3, 'all', to(9, core_recv.at[3, i], chip - 3, core, other)),
        }

    def start_route(i, name):
        condition, which, copy = kv_routes(i)[name]
        if which != 'all':
            late = i >= KV_CHUNKS // 2
            if isinstance(i, int):
                if late != (which == 'late'):
                    return
            else:
                condition = jnp.logical_and(condition, late if which == 'late' else jnp.logical_not(late))

        @pl.when(condition)
        def _():
            copy().start()

    def send_kv(i):
        for name in ('right', 'wrap', 'relay', 'other'):
            start_route(i, name)

    def kv_sent():
        for number, (condition, which, _) in enumerate(kv_routes(0).values()):
            @pl.when(condition)
            def _():
                take(kv_send.at[number], kv.at[pl.ds(0, tok_count if which == 'all' else half_rows), :])

    def serve(back, i):
        @pl.when(chip >= back)
        def _():
            kv_copy(chip - back, core, i, other, kv_send.at[0], ici_recv.at[back - 1, i]).wait_recv()
        start_route(i, 'side%d' % back)
        if back == 1:
            start_route(i, 'on_right')
        if back == 3:
            start_route(i, 'on_left')

    def relay(i):
        def pass_on():
            @pl.when(chip == 0)
            def _():
                kv_copy(1, core, i, left, kv_send.at[0], ici_recv.at[3, i]).wait_recv()
            start_route(i, 'from_relay')
        if not isinstance(i, int):
            pl.when(i >= KV_CHUNKS // 2)(pass_on)
        elif i >= KV_CHUNKS // 2:
            pass_on()

    def serve_all(i):
        serve(1, i)
        serve(3, i)
        relay(i)

    def taken(back, chunks):
        for i in chunks:
            kv_copy(chip - back, 1 - core, i, other, kv_send.at[0], core_recv.at[back, i]).wait_recv()

    def z_parts(step, d):
        copies = []
        for n, (own_ref, all_ref) in enumerate(((wd_ref, gd_ref), (wo_ref, go_ref))):
            size = all_ref.shape[1] // (2 * CHIPS)
            if step == 0:
                rows = span(my_seq * size, size)
                src = own_ref.at[1, rows, :] if n == 0 else own_ref.at[1, 0, rows, :]
                dst = all_ref.at[pos_z, rows, :]
            else:
                rows = span(my_seq * size + d * (size // 2), size // 2)
                src = dst = all_ref.at[wrap(pos_z - sign[d]), rows, :]
            copies.append(remote(src, dst, part_send, part_recv.at[step], head=z_peer(d)))
        return copies

    def part_copies(j, part_chip, part_core, half, send, recv, to):
        copies = []
        for n, ref in enumerate((gd_ref, go_ref)):
            size = ref.shape[1] // (2 * CHIPS)
            first = (part_chip * 2 + part_core) * size
            rows = span(first, size) if half is None else span(first + half * (size // 2), size // 2)
            place = ref.at[wrap(pos_z + j), rows, :]
            copies.append(remote(place, place, send, recv, seq=to))
        return copies

    def own_part(j, d):
        return part_copies(j, chip, core, None, round_send, round_recv.at[0, j - 1], x_device(sign[d]))

    def far_part(j, d):
        return part_copies(j, wrap(chip - sign[d]), core, d, round_send, round_recv.at[1, j - 1], x_device(sign[d]))

    def side_part(j, n, side):
        return part_copies(j, wrap(chip + n), side, None, side_send, side_recv, other)

    def round_start(j):
        for d in range(DIRS):
            start(own_part(j, d))
        start(side_part(j, 0, core))

    def near_parts(j):
        take(round_recv.at[0, j - 1], xbuf.at[pl.ds(0, depth // CHIPS), :])
        for d in range(DIRS):
            start(far_part(j, d) + side_part(j, 3 if d == 0 else 1, core))

    def far_parts(j):
        take(round_recv.at[1, j - 1], xbuf.at[pl.ds(0, depth // (2 * CHIPS)), :])
        start(side_part(j, 2, core))

    def give_hidden(z, i, source):
        cols = span(i * W_TILE, W_TILE)
        return remote(hid.at[span(z * rows_per, rows_per), cols], hidden_place(source, i), give_send, give_recv, head=z_device(z))

    def hidden_place(source, i):
        return xs.at[1, :, span(source * ff_local + i * W_TILE, W_TILE)]

    def via_neighbor(z, i):
        step = jnp.where(i < KV_CHUNKS // 2, 1, -1)
        return remote(hid.at[span(z * rows_per, rows_per), span(i * W_TILE, W_TILE)], relay_buf.at[i], give_send, relay_recv, head=z_device(pos_z + step))

    def relay_hidden(i):
        step = 1 if i < KV_CHUNKS // 2 else -1
        source = wrap(pos_z - step)
        return remote(relay_buf.at[i], hidden_place(source, i), relay_send, give_recv, head=z_device(pos_z + step))

    def send_hidden(z, i):
        away = wrap(z - pos_z)

        @pl.when(away == 2)
        def _():
            via_neighbor(z, i).start()

        @pl.when(away % 2 == 1)
        def _():
            give_hidden(z, i, pos_z).start()

    def give_rows(z, source):
        return remote(att.at[span(z * rows_per, rows_per), :], att_all.at[source], give_send, give_recv, head=z_device(z))

    def norm_rows(x_few, layer):
        x_f32 = x_few.astype(f32)
        inv_rms = lax.rsqrt(jnp.mean(x_f32 * x_f32, axis=-1, keepdims=True) + EPS)
        return (x_f32 * inv_rms * gain_ref[pl.ds(layer, 1), :].astype(f32)).astype(bf16)

    def rope(values, rows):
        cos_t, sin_t = cos_ref[rows, :], sin_ref[rows, :]
        wide = values.astype(bf16).astype(f32)
        first, second = wide[:, :half_dim], wide[:, half_dim:]
        return jnp.concatenate([first * cos_t - second * sin_t, second * cos_t + first * sin_t], axis=1).astype(bf16)

    def dot(a, b):
        return jnp.dot(a, b, preferred_element_type=f32)

    scale = 1.0 / math.sqrt(head_dim)

    def keys_values(normed, i):
        rows = span(i * rows_per, rows_per)
        own = span(my_seq * tok_count + i * rows_per, rows_per)
        kv[own, :head_dim] = rope(dot(normed, wtile[0, 0]), rows)
        kv[own, head_dim:] = dot(normed, wtile[0, 1]).astype(bf16)

    def queries(normed, i):
        rows = span(i * rows_per, rows_per)
        qbuf[rows, :] = (rope(dot(normed, wtile[1, 0]), rows).astype(f32) * scale).astype(bf16)

    def gated(normed, i, tile):
        gate = dot(normed, wtile[tile % 2, 0])
        up = dot(normed, wtile[tile % 2, 1])
        hid[span(i * rows_per, rows_per), span(tile * W_TILE, W_TILE)] = (gate * jax.nn.sigmoid(gate) * up).astype(bf16)

    def attend(key_start, q_half, side, masked, first):
        rows = pl.ds(q_half * half_rows, half_rows)
        some = span(key_start, half_rows)
        logits = lax.dot_general(qbuf[rows, :], kv[some, :head_dim], (((1,), (1,)), ((), ())), preferred_element_type=f32)
        if masked:
            seen = lax.broadcasted_iota(jnp.int32, logits.shape, 0) >= lax.broadcasted_iota(jnp.int32, logits.shape, 1)
            logits = jnp.where(seen, logits, -jnp.inf)
        block_max = jnp.max(logits, axis=-1, keepdims=True)
        if first:
            new_max = jnp.broadcast_to(block_max, (half_rows, lanes))
        else:
            new_max = jnp.maximum(row_max[side, rows, :], block_max)
        prob = jnp.exp(logits - jnp.concatenate([new_max] * (half_rows // lanes), axis=1))
        block_sum = jnp.sum(prob, axis=-1, keepdims=True)
        block_out = dot(prob.astype(bf16), kv[some, head_dim:])
        if first:
            row_sum[side, rows, :] = jnp.broadcast_to(block_sum, (half_rows, lanes))
            acc[side, rows, :] = block_out
        else:
            rescale = jnp.exp(row_max[side, rows, :] - new_max)
            row_sum[side, rows, :] = row_sum[side, rows, :] * rescale + block_sum
            acc[side, rows, :] = acc[side, rows, :] * jnp.concatenate([rescale] * (head_dim // lanes), axis=1) + block_out
        row_max[side, rows, :] = new_max

    def attend_own(layer_half):
        own_start = my_seq * tok_count
        if layer_half == 0:
            attend(own_start, 0, 0, True, True)
            top_rows = pl.ds(0, half_rows)
            row_max[1, top_rows, :] = jnp.full((half_rows, lanes), -jnp.inf, f32)
            row_sum[1, top_rows, :] = jnp.zeros((half_rows, lanes), f32)
            acc[1, top_rows, :] = jnp.zeros((half_rows, head_dim), f32)
        else:
            attend(own_start, 1, 0, False, True)
            attend(own_start + half_rows, 1, 1, True, True)

    def past_start(n):
        later = n - core
        back = jnp.where(later < 2, 1, jnp.where(chip == CHIPS - 1, jnp.where(later < 4, 3, 2), 2))
        block = (chip - back) * 2 + jnp.where(later % 2 == 0, core, 1 - core)
        return jnp.where(jnp.logical_and(core == 1, n == 0), chip * 2, block) * tok_count

    def arrivals(n, chunks):
        @pl.when(jnp.logical_and(core == 1, n == 0))
        def _():
            taken(0, chunks)

        for back in (1, 3, 2):
            place = 0 if back == 1 else 2 if back == 3 else jnp.where(chip == CHIPS - 1, 4, 2)
            if back == 2:
                @pl.when(jnp.logical_and(chip >= back, n == core + place))
                def _():
                    for i in chunks:
                        serve(2, i)

            @pl.when(jnp.logical_and(chip >= back, n == core + place + 1))
            def _():
                taken(back, chunks)

    def visit(n, visits):
        for q_half, side in visits:
            attend(past_start(n) + side * half_rows, q_half, side, False, False)

    def attend_past(first_n, last_n, chunks, visits):
        def past(n, count):
            for r in range(count if chunks else 0):
                arrivals(n + r, chunks)
            for r in range(count):
                visit(n + r, visits)

        def two(p, carry):
            past(first_n + 2 * p, 2)
            return carry

        count = last_n - first_n
        lax.fori_loop(0, count // 2, two, 0)

        @pl.when(count % 2 == 1)
        def _():
            past(last_n - 1, 1)

    near_count = my_seq - jnp.where(chip >= 2, 2, 0)

    def finish(i, spread):
        rows = pl.ds(i * rows_per, rows_per)
        top = jnp.maximum(row_max[0, rows, :], row_max[1, rows, :])
        shares = [jnp.exp(row_max[side, rows, :] - top) for side in range(2)]
        total = shares[0] * row_sum[0, rows, :] + shares[1] * row_sum[1, rows, :]
        wide = [jnp.concatenate([w] * (head_dim // lanes), axis=1) for w in shares + [total]]
        att[rows, :] = ((acc[0, rows, :] * wide[0] + acc[1, rows, :] * wide[1]) / wide[2]).astype(bf16)
        if spread:
            @pl.when(i != pos_z)
            def _():
                give_rows(i, pos_z).start()

    first_pos, second_pos = (pos_y, pos_z), (pos_z, pos_y)
    first_peer, second_peer = (y_peer, z_peer), (z_peer, y_peer)

    def part_rows(chunk, piece, offset, count):
        return span((chunk % PART_SLOTS) * chunk_rows + piece * quarter + offset, count, eighth)

    def x_rows(chunk, piece, offset, count):
        return span(chunk * chunk_rows + piece * quarter + offset, count, eighth)

    def cols_of(h, piece):
        return span(h * half_cols + piece * piece_cols, piece_cols)

    def half_of(h):
        return pl.ds(h * half_cols, half_cols)

    def message(step, chunk, h, d):
        p1, p2, s = first_pos[h], second_pos[h], sign[d]
        slot = chunk % RECV_SLOTS
        if step == 0:
            src, dst = part.at[part_rows(chunk, wrap(p1 + 2), d * eighth, eighth), half_of(h)], recv_a.at[slot, h, d, pl.ds(quarter, eighth), :]
        elif step == 1:
            src, dst = part.at[part_rows(chunk, wrap(p1 + s), 0, quarter), half_of(h)], recv_a.at[slot, h, d, pl.ds(0, quarter), :]
        elif step == 2:
            src, dst = part.at[part_rows(chunk, p1, d * eighth, eighth), cols_of(h, wrap(p2 + 2))], recv_b.at[slot, h, d, pl.ds(quarter, eighth), :]
        elif step == 3:
            src, dst = part.at[part_rows(chunk, p1, 0, quarter), cols_of(h, wrap(p2 + s))], recv_b.at[slot, h, d, pl.ds(0, quarter), :]
        elif step == 4:
            src = dst = xbuf.at[x_rows(chunk, p1, 0, quarter), cols_of(h, p2)]
        elif step == 5:
            src = dst = xbuf.at[x_rows(chunk, p1, d * eighth, eighth), cols_of(h, wrap(p2 - s))]
        elif step == 6:
            src = dst = xbuf.at[x_rows(chunk, p1, 0, quarter), half_of(h)]
        else:
            src = dst = xbuf.at[x_rows(chunk, wrap(p1 - s), d * eighth, eighth), half_of(h)]
        peer = (first_peer if step in (0, 1, 6, 7) else second_peer)[h](d)
        return remote(src, dst, ring_send.at[chunk % PART_SLOTS] if step < 4 else gather_send.at[step - 4], ring_recv.at[slot, step], head=peer)

    def arrived_in(step, count=1):
        rows = (2 * eighth, 2 * quarter, eighth // 2, quarter // 2, quarter // 2, quarter // 2, 2 * quarter, quarter)[step] * count
        return (part if step < 4 else xbuf).at[pl.ds(0, rows), pl.ds(0, half_cols if step == 5 else d_model)]

    def partials_sent(slot):
        take(ring_send.at[slot], part.at[pl.ds(0, 2 * eighth + 2 * quarter + eighth // 2 + quarter // 2), :])

    def residual_load(chunk, h):
        return pltpu.make_async_copy(x_ref.at[x_rows(chunk, first_pos[h], 0, quarter), cols_of(h, second_pos[h])], xres.at[chunk, h], res_sem)

    def project(chunk):
        rows = span(chunk * chunk_rows, chunk_rows)
        slot_rows = span((chunk % PART_SLOTS) * chunk_rows, chunk_rows)

        def one_tile(i, carry):
            @pl.when(jnp.logical_or(chunk < CHUNKS - 1, i < down_tiles - 1))
            def _():
                start(down_load((i + 1) % down_tiles))

            wait(down_load(i))
            total = dot(hid[rows, :], wdo[i % 2, :ff_local, :])
            part[slot_rows, span(i * DOWN_TILE, DOWN_TILE)] = total + dot(att[rows, :], wdo[i % 2, ff_local:, :])
            return carry

        lax.fori_loop(0, down_tiles, one_tile, 0)

    def stage(number, chunk):
        slot = chunk % RECV_SLOTS
        if number == 0:
            @pl.when(chunk >= PART_SLOTS)
            def _():
                partials_sent(chunk % PART_SLOTS)
            project(chunk)
        else:
            take(ring_recv.at[slot, number - 1], arrived_in(number - 1))
        if number == 4:
            @pl.when(chunk == 0)
            def _():
                take(res_sem, xres)
        for h in range(HALVES):
            p1, p2 = first_pos[h], second_pos[h]
            if number in (1, 3):
                for d in range(DIRS):
                    if number == 1:
                        rows, cols, arrived = part_rows(chunk, wrap(p1 + sign[d]), d * eighth, eighth), half_of(h), recv_a
                    else:
                        rows, cols, arrived = part_rows(chunk, p1, d * eighth, eighth), cols_of(h, wrap(p2 + sign[d])), recv_b
                    part[rows, cols] = part[rows, cols] + arrived[slot, h, d, pl.ds(quarter, eighth), :]
            if number == 2:
                rows = part_rows(chunk, p1, 0, quarter)
                part[rows, half_of(h)] = part[rows, half_of(h)] + recv_a[slot, h, 0, pl.ds(0, quarter), :] + recv_a[slot, h, 1, pl.ds(0, quarter), :]
            if number == 4:
                rows, cols = part_rows(chunk, p1, 0, quarter), cols_of(h, p2)
                total = part[rows, cols] + recv_b[slot, h, 0, pl.ds(0, quarter), :] + recv_b[slot, h, 1, pl.ds(0, quarter), :]
                update = total.astype(bf16).astype(f32)
                xbuf[x_rows(chunk, p1, 0, quarter), cols] = (xres[chunk, h].astype(f32) + update).astype(bf16)
            if number < STEPS:
                for d in range(DIRS):
                    message(number, chunk, h, d).start()

    x_load(0).start()
    start(weights(0, 0))
    x_load(1).start()
    start(weights(0, 1))
    barrier = pltpu.get_barrier_semaphore()
    for peer in (left, right, other):
        pl.semaphore_signal(barrier, inc=1, device_id={'seq': peer}, device_id_type=mesh_id)
    for peer in [z_device(pos_z + j) for j in range(1, RING)] + [y_peer(d) for d in range(DIRS)]:
        pl.semaphore_signal(barrier, inc=1, device_id={'head': peer}, device_id_type=mesh_id)

    def prepare(i, carry):
        x_load(i).wait()

        def few(n, inner):
            xbuf[span(i * rows_per + n * NORM_ROWS, NORM_ROWS), :] = norm_rows(xs[i % 2, span(n * NORM_ROWS, NORM_ROWS), :], 0)
            return inner

        lax.fori_loop(0, rows_per // NORM_ROWS, few, 0)

        @pl.when(i + 2 < KV_CHUNKS)
        def _():
            x_load(i + 2).start()

        @pl.when(i == 0)
        def _():
            wait(weights(0, 0))

        keys_values(xbuf[span(i * rows_per, rows_per), :], i)

        @pl.when(i == 0)
        def _():
            pl.semaphore_wait(barrier, 8)

        send_kv(i)

        @pl.when(i == 0)
        def _():
            for d in range(DIRS):
                start(z_parts(0, d))
        return carry

    lax.fori_loop(0, KV_CHUNKS, prepare, 0)
    start(weights(0, 2))
    own_rows = span(my_seq * tok_count, tok_count)

    def cache_stores(layer):
        k_ref, v_ref = ((k1_ref, v1_ref), (k2_ref, v2_ref))[layer]
        return [pltpu.make_async_copy(kv.at[own_rows, pl.ds(0, head_dim)], k_ref, cache_sem),
                pltpu.make_async_copy(kv.at[own_rows, pl.ds(head_dim, head_dim)], v_ref, cache_sem)]

    start(cache_stores(0))
    wait(weights(0, 1))

    def query(i, carry):
        queries(xbuf[span(i * rows_per, rows_per), :], i)
        return carry

    lax.fori_loop(0, KV_CHUNKS, query, 0)
    start(weights(0, 3))
    start(down_load(0))

    def residuals(n, carry):
        for h in range(HALVES):
            residual_load(n, h).start()
        return carry

    lax.fori_loop(0, CHUNKS, residuals, 0)

    def gate_half(half, tile):
        wait(weights(0, tile + 2))

        def rows_step(i, inner):
            gated(xbuf[span(i * rows_per, rows_per), :], i, tile)
            return inner

        lax.fori_loop(half * KV_CHUNKS // 2, (half + 1) * KV_CHUNKS // 2, rows_step, 0)

        @pl.when(tile < 2)
        def _():
            start(weights(0, tile + 4))

        for last in (2, 3):
            @pl.when(tile == last)
            def _():
                start(weights(1, last - 2) if half else weights(0, last))

    def first_half(tile, carry):
        gate_half(0, tile)

        @pl.when(tile < 3)
        def _():
            serve_all(tile)
        return carry

    def second_half(tile, carry):
        gate_half(1, tile)

        @pl.when(tile == 0)
        def _():
            serve_all(3)
            attend_past(0, near_count, range(KV_CHUNKS), ((0, 0), (0, 1)))
            take(part_recv.at[0], xbuf.at[pl.ds(0, depth // CHIPS), :])
            for d in range(DIRS):
                start(z_parts(1, d))
            round_start(1)
            round_start(3)
        return carry

    lax.fori_loop(0, ff_local // W_TILE, first_half, 0)
    attend_own(0)
    lax.fori_loop(0, 2, second_half, 0)
    attend_past(near_count, my_seq, range(KV_CHUNKS), ((0, 0), (0, 1)))
    finish(0, False)
    finish(1, False)

    def block_work(j, phase):
        @pl.when(phase == 0)
        def _():
            @pl.when(j == 0)
            def _():
                for n in range(3):
                    pl.semaphore_wait(ready_sem.at[n], 1)

            def few(n, inner):
                xs[0, span(n * NORM_ROWS, NORM_ROWS), :] = norm_rows(xbuf[span(j * rows_per + n * NORM_ROWS, NORM_ROWS), :], 1)
                return inner

            lax.fori_loop(0, rows_per // NORM_ROWS, few, 0)
            wait(weights(1, 0))
            keys_values(xs[0], j)
            send_kv(j)
            start(weights(1, 2))

        @pl.when(phase == 1)
        def _():
            wait(weights(1, 1))
            queries(xs[0], j)
            start(weights(1, 3))

        @pl.when(jnp.logical_and(phase >= 1, phase <= 4))
        def _():
            tile = phase - 1
            wait(weights(1, tile + 2))
            gated(xs[0], j, tile)

            @pl.when(tile < 2)
            def _():
                start(weights(1, tile + 4))

            @pl.when(jnp.logical_and(tile == 2, j < KV_CHUNKS - 1))
            def _():
                start(weights(1, 0))

            @pl.when(jnp.logical_and(tile == 3, j < KV_CHUNKS - 1))
            def _():
                start(weights(1, 1))

            @pl.when(j == KV_CHUNKS - 1)
            def _():
                send_hidden(j, tile)

    def tick(t, carry):
        for number in range(STEPS, -1, -1):
            place = t - STAGE_GAP * number
            chunk = place // START_GAP

            @pl.when(jnp.logical_and(place >= 0, jnp.logical_and(place % START_GAP == 0, chunk < CHUNKS)))
            def _():
                stage(number, chunk)

        @pl.when(jnp.logical_or(t == 1, t == 3))
        def _():
            gate_half(1, 2 + t // 2)

        @pl.when(t == OWN_TICK)
        def _():
            attend_own(1)

        @pl.when(jnp.logical_and(t > OWN_TICK, jnp.logical_and(t < DONE_TICK, t - OWN_TICK <= my_seq)))
        def _():
            visit(t - OWN_TICK - 1, ((1, 0), (1, 1)))

        @pl.when(t == EARLY_TICK)
        def _():
            attend_own(0)

        early = t - EARLY_TICK - 1

        @pl.when(jnp.logical_and(early >= 0, jnp.logical_and(early < 7, early < my_seq)))
        def _():
            arrivals(early, (0, 1))
            visit(early, ((0, 0),))

        @pl.when(t == 2)
        def _():
            take(part_recv.at[1], xbuf.at[pl.ds(0, depth // (2 * CHIPS)), :])
            round_start(2)

        @pl.when(t == DONE_TICK)
        def _():
            finish(2, False)
            finish(3, False)
            kv_sent()
            take(cache_sem, kv.at[own_rows, :])
            for n, peer in enumerate((left, right, other)):
                pl.semaphore_signal(ready_sem.at[n], inc=1, device_id={'seq': peer}, device_id_type=mesh_id)

        for when, j in NEAR_TICKS:
            @pl.when(t == when)
            def _():
                near_parts(j)

        for when, j in FAR_TICKS:
            @pl.when(t == when)
            def _():
                far_parts(j)

        @pl.when(t == GIVE_TICK)
        def _():
            for i in range(KV_CHUNKS):
                for z in range(KV_CHUNKS - 1):
                    send_hidden(z, i)

        late = t - BLOCK_TICK

        @pl.when(late >= 0)
        def _():
            block_work(late // BLOCK_GAP, late % BLOCK_GAP)

        for i, when in enumerate(SERVE_TICKS):
            @pl.when(t == when)
            def _():
                serve_all(i)
        return carry

    lax.fori_loop(0, LAST_TICK, tick, 0)

    for slot in range(PART_SLOTS):
        partials_sent(slot)
    for step in range(4, STEPS):
        take(gather_send.at[step - 4], arrived_in(step, CHUNKS))
    for d in range(DIRS):
        pl.semaphore_signal(drained_sem.at[d], inc=1, device_id={'head': y_peer(d)}, device_id_type=mesh_id)
    start(cache_stores(1))
    attend_own(1)
    attend_past(0, my_seq, (), ((1, 0),))
    take(relay_recv, relay_buf)
    for i in range(KV_CHUNKS):
        relay_hidden(i).start()
    attend_past(0, near_count, (2, 3), ((0, 1), (1, 1)))
    attend_past(near_count, my_seq, (2, 3), ((0, 1),))
    finish(0, True)
    finish(1, True)
    attend_past(near_count, my_seq, (), ((1, 1),))
    finish(2, True)
    finish(3, True)
    parts_ref = gd_ref.at[pl.ds(0, 2), pl.ds(0, 3 * depth // 4), :]
    take(side_recv, parts_ref)

    quarter_rows = rows_per // RING

    def block_cols(c):
        return span(c * LAST_COLS, LAST_COLS)

    def tile_place(c, j, first, size):
        return wtile.at[c % 2, j // 2, pl.ds((j % 2) * depth + first, size), :]

    def tile_loads(c):
        copies = []
        for j in range(RING):
            z = wrap(pos_z + j)
            down = wd_ref.at[1, :, block_cols(c)] if j == 0 else gd_ref.at[z, :, block_cols(c)]
            out = wo_ref.at[1, 0, :, block_cols(c)] if j == 0 else go_ref.at[z, :, block_cols(c)]
            copies.append(pltpu.make_async_copy(down, tile_place(c, j, 0, ff_local), tile_sem.at[c % 2]))
            copies.append(pltpu.make_async_copy(out, tile_place(c, j, ff_local, head_dim), tile_sem.at[c % 2]))
        return copies

    start(tile_loads(0))
    given = hid.at[pl.ds(0, (RING - 1) * rows_per * depth // ff_local), :]
    take(give_recv, given)
    for d in range(DIRS):
        pl.semaphore_wait(drained_sem.at[d], 1)

    def quarter_of(piece, offset, size):
        return span(piece * quarter_rows + offset, size, quarter_rows // 2)

    def landed(d, first, size):
        return pl.ds(rows_per + d * (3 * quarter_rows // 2) + first, size)

    def rows_at(z, piece, offset, size):
        return span(z * rows_per + piece * quarter_rows + offset, size, quarter_rows // 2)

    def last_messages(step, c, d, z_first):
        s, cols, half = sign[d], block_cols(c), quarter_rows // 2
        near, behind, back = wrap(pos_y + s), wrap(pos_y - s), wrap(pos_z - s)
        along_y = step < 2 or (step < 4) != z_first
        if step == 0:
            pairs = [(part.at[quarter_of(wrap(pos_y + 2), d * half, half), cols], part.at[landed(d, quarter_rows, half), cols])]
        elif step == 1:
            pairs = [(part.at[quarter_of(near, 0, quarter_rows), cols], part.at[landed(d, 0, quarter_rows), cols])]
        else:
            if step == 2:
                rows = [rows_at(pos_z, pos_y, 0, quarter_rows)]
            elif step == 3:
                rows = [rows_at(back, pos_y, d * half, half) if z_first else rows_at(pos_z, behind, d * half, half)]
            elif step == 4:
                rows = [rows_at(z, pos_y, 0, quarter_rows) for z in range(RING)] if z_first else [rows_at(pos_z, 0, 0, rows_per)]
            else:
                rows = [rows_at(z, behind, d * half, half) for z in range(RING)] if z_first else [rows_at(back, 0, d * (rows_per // 2), rows_per // 2)]
            pairs = [(xbuf.at[r, cols], xbuf.at[r, cols]) for r in rows]
        to = (y_peer if along_y else z_peer)(d)
        return [remote(src, dst, last_send.at[step], last_recv.at[c, step], head=to) for src, dst in pairs]

    def last_arrived(step, cols):
        rows = (quarter_rows, 2 * quarter_rows, 2 * quarter_rows, quarter_rows, 2 * rows_per, rows_per)[step]
        return (part if step < 2 else xbuf).at[pl.ds(0, rows), cols]

    def send_last(step, c):
        def both(z_first):
            for d in range(DIRS):
                start(last_messages(step, c, d, z_first))

        if step < 2:
            both(False)
            return
        z_first = jnp.logical_and(c >= 5, c % 2 == 1)

        @pl.when(z_first)
        def _():
            both(True)

        @pl.when(jnp.logical_not(z_first))
        def _():
            both(False)

    def out_store(c):
        return pltpu.make_async_copy(xbuf.at[:, block_cols(c)], out_ref.at[:, block_cols(c)], store_sem)

    def last_project(c):
        @pl.when(c + 1 < LAST_BLOCKS)
        def _():
            start(tile_loads(c + 1))

        take(tile_sem.at[c % 2], wtile.at[c % 2, :, pl.ds(0, 2 * depth), :])
        total = None
        for j in range(RING):
            z = wrap(pos_z + j)
            own = span(pos_z * rows_per, rows_per)
            hidden_rows = hid[own, :] if j == 0 else xs[1, :, span(z * ff_local, ff_local)]
            out_rows = att[own, :] if j == 0 else att_all[z]
            term = dot(hidden_rows, wtile[c % 2, j // 2, pl.ds((j % 2) * depth, ff_local), :])
            term = term + dot(out_rows, wtile[c % 2, j // 2, pl.ds((j % 2) * depth + ff_local, head_dim), :])
            total = term if total is None else total + term
        part[pl.ds(0, rows_per), block_cols(c)] = total

    def last_stage(number, c):
        cols, half = block_cols(c), quarter_rows // 2
        if number == 0:
            last_project(c)
        else:
            take(last_recv.at[c, number - 1], last_arrived(number - 1, cols))
        if number == 1:
            for d in range(DIRS):
                piece = quarter_of(wrap(pos_y + sign[d]), d * half, half)
                part[piece, cols] = part[piece, cols] + part[landed(d, quarter_rows, half), cols]
        if number == 2:
            own = quarter_of(pos_y, 0, quarter_rows)
            total = part[own, cols] + part[landed(0, 0, quarter_rows), cols] + part[landed(1, 0, quarter_rows), cols]
            update = total.astype(bf16).astype(f32)
            rows = rows_at(pos_z, pos_y, 0, quarter_rows)
            xbuf[rows, cols] = (xbuf[rows, cols].astype(f32) + update).astype(bf16)
        if number < LAST_STEPS:
            send_last(number, c)
        else:
            out_store(c).start()

    def last_tick(t, carry):
        for number in range(LAST_STEPS, -1, -1):
            c = t - LAST_GAP * number

            @pl.when(jnp.logical_and(c >= 0, c < LAST_BLOCKS))
            def _():
                last_stage(number, c)
        return carry

    lax.fori_loop(0, LAST_BLOCKS + LAST_GAP * LAST_STEPS, last_tick, 0)

    take(cache_sem, kv.at[own_rows, :])
    take(relay_send, relay_buf)
    kv_sent()
    take(part_send, xbuf.at[pl.ds(0, 3 * depth // 8), :])
    take(round_send, gd_ref.at[pl.ds(0, 2), pl.ds(0, 9 * depth // 16), :])
    take(side_send, parts_ref)
    take(give_send, given)
    for step in range(LAST_STEPS):
        take(last_send.at[step], last_arrived(step, pl.ds(0, d_model)))
    take(store_sem, xbuf)


def layers(x_loc, cos_t, sin_t, norm_gain, w_q, w_k, w_v, w_gate, w_up, w_down, w_o):
    tok_count, d_model = x_loc.shape
    head_dim = w_q.shape[2]
    ff_local = w_gate.shape[2]
    rows_per = tok_count // KV_CHUNKS
    chunk_rows = tok_count // CHUNKS
    landed = 3 * chunk_rows // (2 * RING)
    half_cols = d_model // HALVES
    any_spec = pl.BlockSpec(memory_space=pl.ANY)
    vmem_spec = pl.BlockSpec(memory_space=pltpu.VMEM)
    bf16, f32 = jnp.bfloat16, jnp.float32
    dma = pltpu.SemaphoreType.DMA
    shape = jax.ShapeDtypeStruct
    return pl.pallas_call(
        layers_kernel,
        out_shape=[shape((tok_count, d_model), bf16)] + [shape((tok_count, head_dim), bf16)] * 4
        + [shape((RING, ff_local, d_model), bf16), shape((RING, head_dim, d_model), bf16)],
        in_specs=[any_spec, vmem_spec, vmem_spec, vmem_spec] + [any_spec] * 7,
        out_specs=[any_spec] * 7,
        scratch_shapes=[
            pltpu.VMEM((tok_count, d_model), bf16),
            pltpu.VMEM((PART_SLOTS * chunk_rows, d_model), f32),
            pltpu.VMEM((RECV_SLOTS, HALVES, DIRS, landed, half_cols), f32),
            pltpu.VMEM((RECV_SLOTS, HALVES, DIRS, landed, half_cols // RING), f32),
            pltpu.VMEM((tok_count, ff_local), bf16),
            pltpu.VMEM((tok_count, head_dim), bf16),
            pltpu.VMEM((2, ff_local + head_dim, DOWN_TILE), bf16),
            pltpu.VMEM((2, 2, d_model, W_TILE), bf16),
            pltpu.VMEM((2 * CHIPS * tok_count, 2 * head_dim), bf16),
            pltpu.VMEM((tok_count, head_dim), bf16),
            pltpu.VMEM((2, tok_count, head_dim), f32),
            pltpu.VMEM((2, tok_count, 128), f32),
            pltpu.VMEM((2, tok_count, 128), f32),
            pltpu.VMEM((2, rows_per, d_model), bf16),
            pltpu.VMEM((CHUNKS, HALVES, chunk_rows // RING, half_cols // RING), bf16),
            dma((2,)), dma, dma((2, 2)), dma((2, 2)), dma, dma,
            dma((10,)), dma((4, KV_CHUNKS)), dma((4, KV_CHUNKS)), dma, dma((2,)),
            dma, dma((2, RING - 1)), dma, dma,
            dma, dma,
            pltpu.VMEM((KV_CHUNKS, rows_per, W_TILE), bf16), dma, dma,
            pltpu.VMEM((RING, rows_per, head_dim), bf16),
            dma((PART_SLOTS,)), dma((4,)), dma((RECV_SLOTS, STEPS)),
            dma((LAST_STEPS,)), dma((LAST_BLOCKS, LAST_STEPS)), dma((2,)),
            pltpu.SemaphoreType.REGULAR((3,)), pltpu.SemaphoreType.REGULAR((DIRS,)),
        ],
        compiler_params=pltpu.CompilerParams(collective_id=0, has_side_effects=True, vmem_limit_bytes=67043328),
        name='layers',
    )(x_loc, cos_t, sin_t, norm_gain, w_q, w_k, w_v, w_gate, w_up, w_down, w_o)


EMIT_PARTS = 8


def emit_kernel(x_ref, k_first, k_second, v_first, v_second, x_out, k_out, v_out, xbuf, rows, load_sem, store_sem):
    size = x_ref.shape[0] // EMIT_PARTS
    loads, stores = [], []
    for n in range(EMIT_PARTS):
        part = pl.ds(n * size, size)
        loads.append(pltpu.make_async_copy(x_ref.at[part, :], xbuf.at[part, :], load_sem.at[n]))
        stores.append(pltpu.make_async_copy(xbuf.at[part, :], x_out.at[part, :], store_sem.at[n]))
    for n, (ref, out) in enumerate(((k_first, k_out.at[0]), (k_second, k_out.at[1]), (v_first, v_out.at[0]), (v_second, v_out.at[1]))):
        loads.append(pltpu.make_async_copy(ref, rows.at[n], load_sem.at[EMIT_PARTS + n]))
        stores.append(pltpu.make_async_copy(rows.at[n], out, store_sem.at[EMIT_PARTS + n]))
    for copy in loads:
        copy.start()
    for load, store in zip(loads, stores):
        load.wait()
        store.start()
    for copy in stores:
        copy.wait()


def emit(x_out, k_first, k_second, v_first, v_second):
    any_spec = pl.BlockSpec(memory_space=pl.ANY)
    cache = jax.ShapeDtypeStruct((2,) + k_first.shape, jnp.bfloat16)
    return pl.pallas_call(
        emit_kernel,
        out_shape=[jax.ShapeDtypeStruct(x_out.shape, jnp.bfloat16), cache, cache],
        in_specs=[any_spec] * 5,
        out_specs=[any_spec] * 3,
        scratch_shapes=[
            pltpu.VMEM(x_out.shape, jnp.bfloat16),
            pltpu.VMEM((4,) + k_first.shape, jnp.bfloat16),
            pltpu.SemaphoreType.DMA((EMIT_PARTS + 4,)),
            pltpu.SemaphoreType.DMA((EMIT_PARTS + 4,)),
        ],
        compiler_params=pltpu.CompilerParams(vmem_limit_bytes=63 * 1024 * 1024),
        name='emit',
    )(x_out, k_first, k_second, v_first, v_second)


def solution(mesh):
    row_spec = P(('batch', 'seq'), None)
    pos_spec = P(('batch', 'seq'))
    head_spec = P(None, None, 'head', None)
    out_proj_spec = P(None, 'head', None, None)
    col_spec = P(None, None, 'head')
    down_spec = P(None, 'head', None)
    cache_spec = P(None, ('batch', 'seq'), 'head', None)

    def local_forward(x_loc, pos_loc, w_q, w_k, w_v, w_o, w_gate, w_up, w_down, norm_gain):
        tok_count, d_model = x_loc.shape
        layer_count = w_q.shape[0]
        head_dim = w_q.shape[3]
        flat_q, flat_k, flat_v = (w.reshape(layer_count, d_model, head_dim) for w in (w_q, w_k, w_v))
        cos_t, sin_t = rope_tables(pos_loc, head_dim)
        x_out, k_first, v_first, k_second, v_second, _, _ = layers(x_loc, cos_t, sin_t, norm_gain, flat_q, flat_k, flat_v, w_gate, w_up, w_down, w_o)
        x_out, k_all, v_all = emit(x_out, k_first, k_second, v_first, v_second)
        cache_shape = (layer_count, tok_count, 1, head_dim)
        return x_out, k_all.reshape(cache_shape), v_all.reshape(cache_shape)

    return jax.shard_map(local_forward, mesh=mesh, in_specs=(row_spec, pos_spec, head_spec, head_spec, head_spec, out_proj_spec, col_spec, col_spec, down_spec, P(None, None)), out_specs=(row_spec, cache_spec, cache_spec), check_vma=False)
```

```python
import functools
import math
import jax
import jax.numpy as jnp
from jax import lax
from jax.experimental import pallas as pl
from jax.experimental.pallas import tpu as pltpu
from jax.sharding import PartitionSpec as P

ROPE_BASE = 500000.0
EPS = 1e-5


def rope_tables(positions, head_dim):
    half_dim = head_dim // 2
    inv_freq = ROPE_BASE ** (-(jnp.arange(half_dim, dtype=jnp.float32) * 2.0 / head_dim))
    angles = positions.astype(jnp.float32)[..., None] * inv_freq
    return jnp.cos(angles), jnp.sin(angles)


CHIPS = 4
RING = 4
HALVES = 2
DIRS = 2
KV_CHUNKS = 4
W_TILE = 256
NORM_ROWS = 64
CHUNKS = 8
STEPS = 8
PART_SLOTS = 4
RECV_SLOTS = 5
DOWN_TILE = 512
START_GAP = 3
STAGE_GAP = 2
BLOCK_TICK = 19
BLOCK_GAP = 6
LAST_TICK = 43
NEAR_TICKS = ((9, 1), (15, 3), (20, 2))
FAR_TICKS = ((24, 1), (26, 3), (36, 2))
SERVE_TICKS = ((27, 0), (31, 1), (36, 2), (38, 4), (41, 5))
HALF_TICKS = (35, 37)
GIVE_TICK = 37
OWN_TICK = 3
DONE_TICK = 11
EARLY_TICK = 31
LAST_STEPS = 6
LAST_COLS = 256
LAST_BLOCKS = 16
LAST_GAP = 3


def layers_kernel(x_ref, cos_ref, sin_ref, gain_ref, wq_ref, wk_ref, wv_ref, wg_ref, wu_ref, wd_ref, wo_ref,
                 out_ref, k1_ref, v1_ref, k2_ref, v2_ref, gd_ref, go_ref,
                 xbuf, part, recv_a, recv_b, hid, att, wdo, wtile, kv, qbuf, acc, row_max, row_sum, xs, xres,
                 x_sem, res_sem, w_sem, down_sem, cache_sem, store_sem, kv_send, ici_recv, core_recv, part_send, part_recv,
                 round_send, round_recv, side_send, side_recv, give_send, give_recv, relay_buf, relay_send, relay_recv, att_all, ring_send, gather_send, ring_recv,
                 last_send, last_recv, tile_sem, ready_sem, drained_sem):
    tok_count, d_model = xbuf.shape
    head_dim = qbuf.shape[1]
    half_dim = head_dim // 2
    ff_local = hid.shape[1]
    depth = ff_local + head_dim
    rows_per = tok_count // KV_CHUNKS
    half_rows = tok_count // 2
    lanes = row_max.shape[2]
    chunk_rows = tok_count // CHUNKS
    quarter, eighth = chunk_rows // RING, chunk_rows // (2 * RING)
    half_cols = d_model // HALVES
    piece_cols = half_cols // RING
    bf16, f32 = jnp.bfloat16, jnp.float32
    sign = (1, -1)
    mesh_id = pl.DeviceIdType.MESH

    my_head = lax.axis_index('head')
    pos_z, pos_y = my_head // RING, my_head % RING
    my_seq = lax.axis_index('seq')
    chip, core = my_seq // 2, my_seq % 2
    other = chip * 2 + 1 - core

    def wrap(n):
        return (n + RING) % RING

    def y_peer(d):
        return pos_z * RING + wrap(pos_y + sign[d])

    def z_device(z):
        return wrap(z) * RING + pos_y

    def z_peer(d):
        return z_device(pos_z + sign[d])

    def x_device(n):
        return wrap(chip + n) * 2 + core

    right, left = x_device(1), x_device(-1)

    def span(start, size, unit=None):
        return pl.ds(pl.multiple_of(start, unit or size), size)

    def remote(src, dst, send, recv, **to):
        return pltpu.make_async_remote_copy(src_ref=src, dst_ref=dst, send_sem=send, recv_sem=recv, device_id=to, device_id_type=mesh_id)

    def take(sem, ref):
        remote(ref, ref, sem, sem, head=my_head).wait_recv()

    def x_load(i):
        return pltpu.make_async_copy(x_ref.at[span(i * rows_per, rows_per), :], xs.at[i % 2], x_sem.at[i % 2])

    def weights(layer, piece):
        slot = piece % 2
        if isinstance(piece, int) and piece < 2:
            refs = ((wk_ref, wv_ref), (wq_ref,))[piece]
            return [pltpu.make_async_copy(ref.at[layer], wtile.at[slot, n], w_sem.at[slot, n]) for n, ref in enumerate(refs)]
        cols = span((piece - 2) * W_TILE, W_TILE)
        return [pltpu.make_async_copy(ref.at[layer, :, cols], wtile.at[slot, n], w_sem.at[slot, n]) for n, ref in enumerate((wg_ref, wu_ref))]

    def start(copies):
        for copy in copies:
            copy.start()

    def wait(copies):
        for copy in copies:
            copy.wait()

    down_tiles = d_model // DOWN_TILE

    def down_load(i):
        cols = span(i * DOWN_TILE, DOWN_TILE)
        return [pltpu.make_async_copy(wd_ref.at[0, :, cols], wdo.at[i % 2, pl.ds(0, ff_local), :], down_sem.at[i % 2, 0]),
                pltpu.make_async_copy(wo_ref.at[0, 0, :, cols], wdo.at[i % 2, pl.ds(ff_local, head_dim), :], down_sem.at[i % 2, 1])]

    def kv_chunk(i):
        if isinstance(i, int) and i >= KV_CHUNKS:
            return (KV_CHUNKS - 1) * rows_per + (i - KV_CHUNKS) * (rows_per // 2), rows_per // 2
        return i * rows_per, rows_per

    def kv_copy(origin_chip, origin_core, i, to, send, recv):
        first, size = kv_chunk(i)
        rows = kv.at[span((origin_chip * 2 + origin_core) * tok_count + first, size), :]
        return remote(rows, rows, send, recv, seq=to)

    def kv_routes(i):
        def to(number, recv, origin_chip, origin_core, device):
            return lambda: kv_copy(origin_chip, origin_core, i, device, kv_send.at[number], recv)
        inner = jnp.logical_and(chip >= 1, chip < CHIPS - 1)
        return {
            'right': (chip < CHIPS - 1, 'all', to(0, ici_recv.at[0, i], chip, core, right)),
            'wrap': (chip == 0, 'all', to(1, ici_recv.at[2, i], chip, core, left)),
            'relay': (chip == 1, 'late', to(2, ici_recv.at[3, i], chip, core, left)),
            'other': (core == 0, 'all', to(3, core_recv.at[0, i], chip, core, other)),
            'on_right': (inner, 'early', to(4, ici_recv.at[1, i], chip - 1, core, right)),
            'from_relay': (chip == 0, 'late', to(5, ici_recv.at[1, i], 1, core, left)),
            'on_left': (chip == CHIPS - 1, 'late', to(6, ici_recv.at[1, i], 0, core, left)),
            'side1': (chip >= 1, 'all', to(7, core_recv.at[1, i], chip - 1, core, other)),
            'side2': (chip >= 2, 'all', to(8, core_recv.at[2, i], chip - 2, core, other)),
            'side3': (chip >= 3, 'all', to(9, core_recv.at[3, i], chip - 3, core, other)),
        }

    def start_route(i, name):
        condition, which, copy = kv_routes(i)[name]
        if which != 'all':
            late = i >= KV_CHUNKS // 2
            if isinstance(i, int):
                if late != (which == 'late'):
                    return
            else:
                condition = jnp.logical_and(condition, late if which == 'late' else jnp.logical_not(late))

        @pl.when(condition)
        def _():
            copy().start()

    def send_kv(i):
        for name in ('right', 'wrap', 'relay', 'other'):
            start_route(i, name)

    def kv_sent():
        for number, (condition, which, _) in enumerate(kv_routes(0).values()):
            @pl.when(condition)
            def _():
                take(kv_send.at[number], kv.at[pl.ds(0, tok_count if which == 'all' else half_rows), :])

    def serve(back, i):
        @pl.when(chip >= back)
        def _():
            kv_copy(chip - back, core, i, other, kv_send.at[0], ici_recv.at[back - 1, i]).wait_recv()
        start_route(i, 'side%d' % back)
        if back == 1:
            start_route(i, 'on_right')
        if back == 3:
            start_route(i, 'on_left')

    def relay(i):
        def pass_on():
            @pl.when(chip == 0)
            def _():
                kv_copy(1, core, i, left, kv_send.at[0], ici_recv.at[3, i]).wait_recv()
            start_route(i, 'from_relay')
        if not isinstance(i, int):
            pl.when(i >= KV_CHUNKS // 2)(pass_on)
        elif i >= KV_CHUNKS // 2:
            pass_on()

    def serve_all(i):
        serve(1, i)
        serve(3, i)
        relay(i)

    def taken(back, chunks):
        for i in chunks:
            kv_copy(chip - back, 1 - core, i, other, kv_send.at[0], core_recv.at[back, i]).wait_recv()

    def z_parts(step, d):
        copies = []
        for n, (own_ref, all_ref) in enumerate(((wd_ref, gd_ref), (wo_ref, go_ref))):
            size = all_ref.shape[1] // (2 * CHIPS)
            if step == 0:
                rows = span(my_seq * size, size)
                src = own_ref.at[1, rows, :] if n == 0 else own_ref.at[1, 0, rows, :]
                dst = all_ref.at[pos_z, rows, :]
            else:
                rows = span(my_seq * size + d * (size // 2), size // 2)
                src = dst = all_ref.at[wrap(pos_z - sign[d]), rows, :]
            copies.append(remote(src, dst, part_send, part_recv.at[step], head=z_peer(d)))
        return copies

    def part_copies(j, part_chip, part_core, half, send, recv, to):
        copies = []
        for n, ref in enumerate((gd_ref, go_ref)):
            size = ref.shape[1] // (2 * CHIPS)
            first = (part_chip * 2 + part_core) * size
            rows = span(first, size) if half is None else span(first + half * (size // 2), size // 2)
            place = ref.at[wrap(pos_z + j), rows, :]
            copies.append(remote(place, place, send, recv, seq=to))
        return copies

    def own_part(j, d):
        return part_copies(j, chip, core, None, round_send, round_recv.at[0, j - 1], x_device(sign[d]))

    def far_part(j, d):
        return part_copies(j, wrap(chip - sign[d]), core, d, round_send, round_recv.at[1, j - 1], x_device(sign[d]))

    def side_part(j, n, side):
        return part_copies(j, wrap(chip + n), side, None, side_send, side_recv, other)

    def round_start(j):
        for d in range(DIRS):
            start(own_part(j, d))
        start(side_part(j, 0, core))

    def near_parts(j):
        take(round_recv.at[0, j - 1], xbuf.at[pl.ds(0, depth // CHIPS), :])
        for d in range(DIRS):
            start(far_part(j, d) + side_part(j, 3 if d == 0 else 1, core))

    def far_parts(j):
        take(round_recv.at[1, j - 1], xbuf.at[pl.ds(0, depth // (2 * CHIPS)), :])
        start(side_part(j, 2, core))

    def give_hidden(z, i, source):
        cols = span(i * W_TILE, W_TILE)
        return remote(hid.at[span(z * rows_per, rows_per), cols], hidden_place(source, i), give_send, give_recv, head=z_device(z))

    def hidden_place(source, i):
        return xs.at[1, :, span(source * ff_local + i * W_TILE, W_TILE)]

    def via_neighbor(z, i):
        step = jnp.where(i < KV_CHUNKS // 2, 1, -1)
        return remote(hid.at[span(z * rows_per, rows_per), span(i * W_TILE, W_TILE)], relay_buf.at[i], give_send, relay_recv, head=z_device(pos_z + step))

    def relay_hidden(i):
        step = 1 if i < KV_CHUNKS // 2 else -1
        source = wrap(pos_z - step)
        return remote(relay_buf.at[i], hidden_place(source, i), relay_send, give_recv, head=z_device(pos_z + step))

    def send_hidden(z, i):
        away = wrap(z - pos_z)

        @pl.when(away == 2)
        def _():
            via_neighbor(z, i).start()

        @pl.when(away % 2 == 1)
        def _():
            give_hidden(z, i, pos_z).start()

    def give_rows(z, source):
        return remote(att.at[span(z * rows_per, rows_per), :], att_all.at[source], give_send, give_recv, head=z_device(z))

    def norm_rows(x_few, layer):
        x_f32 = x_few.astype(f32)
        inv_rms = lax.rsqrt(jnp.mean(x_f32 * x_f32, axis=-1, keepdims=True) + EPS)
        return (x_f32 * inv_rms * gain_ref[pl.ds(layer, 1), :].astype(f32)).astype(bf16)

    def rope(values, rows):
        cos_t, sin_t = cos_ref[rows, :], sin_ref[rows, :]
        wide = values.astype(bf16).astype(f32)
        first, second = wide[:, :half_dim], wide[:, half_dim:]
        return jnp.concatenate([first * cos_t - second * sin_t, second * cos_t + first * sin_t], axis=1).astype(bf16)

    def dot(a, b):
        return jnp.dot(a, b, preferred_element_type=f32)

    scale = 1.0 / math.sqrt(head_dim)

    def keys_values(normed, i):
        first, size = kv_chunk(i)
        rows = span(first, size)
        own = span(my_seq * tok_count + first, size)
        kv[own, :head_dim] = rope(dot(normed, wtile[0, 0]), rows)
        kv[own, head_dim:] = dot(normed, wtile[0, 1]).astype(bf16)

    def queries(normed, i):
        rows = span(i * rows_per, rows_per)
        qbuf[rows, :] = (rope(dot(normed, wtile[1, 0]), rows).astype(f32) * scale).astype(bf16)

    def gated(normed, i, tile):
        gate = dot(normed, wtile[tile % 2, 0])
        up = dot(normed, wtile[tile % 2, 1])
        hid[span(i * rows_per, rows_per), span(tile * W_TILE, W_TILE)] = (gate * jax.nn.sigmoid(gate) * up).astype(bf16)

    def attend(key_start, q_half, side, masked, first):
        rows = pl.ds(q_half * half_rows, half_rows)
        some = span(key_start, half_rows)
        logits = lax.dot_general(qbuf[rows, :], kv[some, :head_dim], (((1,), (1,)), ((), ())), preferred_element_type=f32)
        if masked:
            seen = lax.broadcasted_iota(jnp.int32, logits.shape, 0) >= lax.broadcasted_iota(jnp.int32, logits.shape, 1)
            logits = jnp.where(seen, logits, -jnp.inf)
        block_max = jnp.max(logits, axis=-1, keepdims=True)
        if first:
            new_max = jnp.broadcast_to(block_max, (half_rows, lanes))
        else:
            new_max = jnp.maximum(row_max[side, rows, :], block_max)
        prob = jnp.exp(logits - jnp.concatenate([new_max] * (half_rows // lanes), axis=1))
        block_sum = jnp.sum(prob, axis=-1, keepdims=True)
        block_out = dot(prob.astype(bf16), kv[some, head_dim:])
        if first:
            row_sum[side, rows, :] = jnp.broadcast_to(block_sum, (half_rows, lanes))
            acc[side, rows, :] = block_out
        else:
            rescale = jnp.exp(row_max[side, rows, :] - new_max)
            row_sum[side, rows, :] = row_sum[side, rows, :] * rescale + block_sum
            acc[side, rows, :] = acc[side, rows, :] * jnp.concatenate([rescale] * (head_dim // lanes), axis=1) + block_out
        row_max[side, rows, :] = new_max

    def attend_own(layer_half):
        own_start = my_seq * tok_count
        if layer_half == 0:
            attend(own_start, 0, 0, True, True)
            top_rows = pl.ds(0, half_rows)
            row_max[1, top_rows, :] = jnp.full((half_rows, lanes), -jnp.inf, f32)
            row_sum[1, top_rows, :] = jnp.zeros((half_rows, lanes), f32)
            acc[1, top_rows, :] = jnp.zeros((half_rows, head_dim), f32)
        else:
            attend(own_start, 1, 0, False, True)
            attend(own_start + half_rows, 1, 1, True, True)

    def past_start(n):
        later = n - core
        back = jnp.where(later < 2, 1, jnp.where(chip == CHIPS - 1, jnp.where(later < 4, 3, 2), 2))
        block = (chip - back) * 2 + jnp.where(later % 2 == 0, core, 1 - core)
        return jnp.where(jnp.logical_and(core == 1, n == 0), chip * 2, block) * tok_count

    def arrivals(n, chunks):
        @pl.when(jnp.logical_and(core == 1, n == 0))
        def _():
            taken(0, chunks)

        for back in (1, 3, 2):
            place = 0 if back == 1 else 2 if back == 3 else jnp.where(chip == CHIPS - 1, 4, 2)
            if back == 2:
                @pl.when(jnp.logical_and(chip >= back, n == core + place))
                def _():
                    for i in chunks:
                        serve(2, i)

            @pl.when(jnp.logical_and(chip >= back, n == core + place + 1))
            def _():
                taken(back, chunks)

    def visit(n, visits):
        for q_half, side in visits:
            attend(past_start(n) + side * half_rows, q_half, side, False, False)

    def attend_past(first_n, last_n, chunks, visits):
        def past(n, count):
            for r in range(count if chunks else 0):
                arrivals(n + r, chunks)
            for r in range(count):
                visit(n + r, visits)

        def two(p, carry):
            past(first_n + 2 * p, 2)
            return carry

        count = last_n - first_n
        lax.fori_loop(0, count // 2, two, 0)

        @pl.when(count % 2 == 1)
        def _():
            past(last_n - 1, 1)

    near_count = my_seq - jnp.where(chip >= 2, 2, 0)

    def finish(i, spread):
        rows = pl.ds(i * rows_per, rows_per)
        top = jnp.maximum(row_max[0, rows, :], row_max[1, rows, :])
        shares = [jnp.exp(row_max[side, rows, :] - top) for side in range(2)]
        total = shares[0] * row_sum[0, rows, :] + shares[1] * row_sum[1, rows, :]
        wide = [jnp.concatenate([w] * (head_dim // lanes), axis=1) for w in shares + [total]]
        att[rows, :] = ((acc[0, rows, :] * wide[0] + acc[1, rows, :] * wide[1]) / wide[2]).astype(bf16)
        if spread:
            @pl.when(i != pos_z)
            def _():
                give_rows(i, pos_z).start()

    first_pos, second_pos = (pos_y, pos_z), (pos_z, pos_y)
    first_peer, second_peer = (y_peer, z_peer), (z_peer, y_peer)

    def part_rows(chunk, piece, offset, count):
        return span((chunk % PART_SLOTS) * chunk_rows + piece * quarter + offset, count, eighth)

    def x_rows(chunk, piece, offset, count):
        return span(chunk * chunk_rows + piece * quarter + offset, count, eighth)

    def cols_of(h, piece):
        return span(h * half_cols + piece * piece_cols, piece_cols)

    def half_of(h):
        return pl.ds(h * half_cols, half_cols)

    def message(step, chunk, h, d):
        p1, p2, s = first_pos[h], second_pos[h], sign[d]
        slot = chunk % RECV_SLOTS
        if step == 0:
            src, dst = part.at[part_rows(chunk, wrap(p1 + 2), d * eighth, eighth), half_of(h)], recv_a.at[slot, h, d, pl.ds(quarter, eighth), :]
        elif step == 1:
            src, dst = part.at[part_rows(chunk, wrap(p1 + s), 0, quarter), half_of(h)], recv_a.at[slot, h, d, pl.ds(0, quarter), :]
        elif step == 2:
            src, dst = part.at[part_rows(chunk, p1, d * eighth, eighth), cols_of(h, wrap(p2 + 2))], recv_b.at[slot, h, d, pl.ds(quarter, eighth), :]
        elif step == 3:
            src, dst = part.at[part_rows(chunk, p1, 0, quarter), cols_of(h, wrap(p2 + s))], recv_b.at[slot, h, d, pl.ds(0, quarter), :]
        elif step == 4:
            src = dst = xbuf.at[x_rows(chunk, p1, 0, quarter), cols_of(h, p2)]
        elif step == 5:
            src = dst = xbuf.at[x_rows(chunk, p1, d * eighth, eighth), cols_of(h, wrap(p2 - s))]
        elif step == 6:
            src = dst = xbuf.at[x_rows(chunk, p1, 0, quarter), half_of(h)]
        else:
            src = dst = xbuf.at[x_rows(chunk, wrap(p1 - s), d * eighth, eighth), half_of(h)]
        peer = (first_peer if step in (0, 1, 6, 7) else second_peer)[h](d)
        return remote(src, dst, ring_send.at[chunk % PART_SLOTS] if step < 4 else gather_send.at[step - 4], ring_recv.at[slot, step], head=peer)

    def arrived_in(step, count=1):
        rows = (2 * eighth, 2 * quarter, eighth // 2, quarter // 2, quarter // 2, quarter // 2, 2 * quarter, quarter)[step] * count
        return (part if step < 4 else xbuf).at[pl.ds(0, rows), pl.ds(0, half_cols if step == 5 else d_model)]

    def partials_sent(slot):
        take(ring_send.at[slot], part.at[pl.ds(0, 2 * eighth + 2 * quarter + eighth // 2 + quarter // 2), :])

    def residual_load(chunk, h):
        return pltpu.make_async_copy(x_ref.at[x_rows(chunk, first_pos[h], 0, quarter), cols_of(h, second_pos[h])], xres.at[chunk, h], res_sem)

    def project(chunk):
        rows = span(chunk * chunk_rows, chunk_rows)
        slot_rows = span((chunk % PART_SLOTS) * chunk_rows, chunk_rows)

        def one_tile(i, carry):
            @pl.when(jnp.logical_or(chunk < CHUNKS - 1, i < down_tiles - 1))
            def _():
                start(down_load((i + 1) % down_tiles))

            wait(down_load(i))
            total = dot(hid[rows, :], wdo[i % 2, :ff_local, :])
            part[slot_rows, span(i * DOWN_TILE, DOWN_TILE)] = total + dot(att[rows, :], wdo[i % 2, ff_local:, :])
            return carry

        lax.fori_loop(0, down_tiles, one_tile, 0)

    def stage(number, chunk):
        slot = chunk % RECV_SLOTS
        if number == 0:
            @pl.when(chunk >= PART_SLOTS)
            def _():
                partials_sent(chunk % PART_SLOTS)
            project(chunk)
        else:
            take(ring_recv.at[slot, number - 1], arrived_in(number - 1))
        if number == 4:
            @pl.when(chunk == 0)
            def _():
                take(res_sem, xres)
        for h in range(HALVES):
            p1, p2 = first_pos[h], second_pos[h]
            if number in (1, 3):
                for d in range(DIRS):
                    if number == 1:
                        rows, cols, arrived = part_rows(chunk, wrap(p1 + sign[d]), d * eighth, eighth), half_of(h), recv_a
                    else:
                        rows, cols, arrived = part_rows(chunk, p1, d * eighth, eighth), cols_of(h, wrap(p2 + sign[d])), recv_b
                    part[rows, cols] = part[rows, cols] + arrived[slot, h, d, pl.ds(quarter, eighth), :]
            if number == 2:
                rows = part_rows(chunk, p1, 0, quarter)
                part[rows, half_of(h)] = part[rows, half_of(h)] + recv_a[slot, h, 0, pl.ds(0, quarter), :] + recv_a[slot, h, 1, pl.ds(0, quarter), :]
            if number == 4:
                rows, cols = part_rows(chunk, p1, 0, quarter), cols_of(h, p2)
                total = part[rows, cols] + recv_b[slot, h, 0, pl.ds(0, quarter), :] + recv_b[slot, h, 1, pl.ds(0, quarter), :]
                update = total.astype(bf16).astype(f32)
                xbuf[x_rows(chunk, p1, 0, quarter), cols] = (xres[chunk, h].astype(f32) + update).astype(bf16)
            if number < STEPS:
                for d in range(DIRS):
                    message(number, chunk, h, d).start()

    x_load(0).start()
    start(weights(0, 0))
    x_load(1).start()
    start(weights(0, 1))
    barrier = pltpu.get_barrier_semaphore()
    for peer in (left, right, other):
        pl.semaphore_signal(barrier, inc=1, device_id={'seq': peer}, device_id_type=mesh_id)
    for peer in [z_device(pos_z + j) for j in range(1, RING)] + [y_peer(d) for d in range(DIRS)]:
        pl.semaphore_signal(barrier, inc=1, device_id={'head': peer}, device_id_type=mesh_id)

    def prepare(i, carry):
        x_load(i).wait()

        def few(n, inner):
            xbuf[span(i * rows_per + n * NORM_ROWS, NORM_ROWS), :] = norm_rows(xs[i % 2, span(n * NORM_ROWS, NORM_ROWS), :], 0)
            return inner

        lax.fori_loop(0, rows_per // NORM_ROWS, few, 0)

        @pl.when(i + 2 < KV_CHUNKS)
        def _():
            x_load(i + 2).start()

        @pl.when(i == 0)
        def _():
            wait(weights(0, 0))

        keys_values(xbuf[span(i * rows_per, rows_per), :], i)

        @pl.when(i == 0)
        def _():
            pl.semaphore_wait(barrier, 8)

        send_kv(i)

        @pl.when(i == 0)
        def _():
            for d in range(DIRS):
                start(z_parts(0, d))
        return carry

    lax.fori_loop(0, KV_CHUNKS, prepare, 0)
    start(weights(0, 2))
    own_rows = span(my_seq * tok_count, tok_count)

    def cache_stores(layer):
        k_ref, v_ref = ((k1_ref, v1_ref), (k2_ref, v2_ref))[layer]
        return [pltpu.make_async_copy(kv.at[own_rows, pl.ds(0, head_dim)], k_ref, cache_sem),
                pltpu.make_async_copy(kv.at[own_rows, pl.ds(head_dim, head_dim)], v_ref, cache_sem)]

    start(cache_stores(0))
    wait(weights(0, 1))

    def query(i, carry):
        queries(xbuf[span(i * rows_per, rows_per), :], i)
        return carry

    lax.fori_loop(0, KV_CHUNKS, query, 0)
    start(weights(0, 3))
    start(down_load(0))

    def residuals(n, carry):
        for h in range(HALVES):
            residual_load(n, h).start()
        return carry

    lax.fori_loop(0, CHUNKS, residuals, 0)

    def gate_half(half, tile):
        wait(weights(0, tile + 2))

        def rows_step(i, inner):
            gated(xbuf[span(i * rows_per, rows_per), :], i, tile)
            return inner

        lax.fori_loop(half * KV_CHUNKS // 2, (half + 1) * KV_CHUNKS // 2, rows_step, 0)

        @pl.when(tile < 2)
        def _():
            start(weights(0, tile + 4))

        for last in (2, 3):
            @pl.when(tile == last)
            def _():
                start(weights(1, last - 2) if half else weights(0, last))

    def first_half(tile, carry):
        gate_half(0, tile)

        @pl.when(tile < 3)
        def _():
            serve_all(tile)
        return carry

    def second_half(tile, carry):
        gate_half(1, tile)

        @pl.when(tile == 0)
        def _():
            serve_all(3)
            attend_past(0, near_count, range(KV_CHUNKS), ((0, 0), (0, 1)))
            take(part_recv.at[0], xbuf.at[pl.ds(0, depth // CHIPS), :])
            for d in range(DIRS):
                start(z_parts(1, d))
            round_start(1)
            round_start(3)
        return carry

    lax.fori_loop(0, ff_local // W_TILE, first_half, 0)
    attend_own(0)
    lax.fori_loop(0, 2, second_half, 0)
    attend_past(near_count, my_seq, range(KV_CHUNKS), ((0, 0), (0, 1)))
    finish(0, False)
    finish(1, False)

    def last_half(r):
        half = rows_per // 2
        first = kv_chunk(KV_CHUNKS + r)[0]

        def few(n, inner):
            xs[0, span(r * half + n * NORM_ROWS, NORM_ROWS), :] = norm_rows(xbuf[span(first + n * NORM_ROWS, NORM_ROWS), :], 1)
            return inner

        lax.fori_loop(0, half // NORM_ROWS, few, 0)
        if r == 0:
            wait(weights(1, 0))
        keys_values(xs[0, pl.ds(r * half, half), :], KV_CHUNKS + r)
        send_kv(KV_CHUNKS + r)
        if r == 1:
            start(weights(1, 2))

    def block_work(j, phase):
        @pl.when(jnp.logical_and(phase == 0, j < KV_CHUNKS - 1))
        def _():
            @pl.when(j == 0)
            def _():
                for n in range(3):
                    pl.semaphore_wait(ready_sem.at[n], 1)

            def few(n, inner):
                xs[0, span(n * NORM_ROWS, NORM_ROWS), :] = norm_rows(xbuf[span(j * rows_per + n * NORM_ROWS, NORM_ROWS), :], 1)
                return inner

            lax.fori_loop(0, rows_per // NORM_ROWS, few, 0)
            wait(weights(1, 0))
            keys_values(xs[0], j)
            send_kv(j)
            start(weights(1, 2))

        @pl.when(phase == 1)
        def _():
            wait(weights(1, 1))
            queries(xs[0], j)
            start(weights(1, 3))

        @pl.when(jnp.logical_and(phase >= 1, phase <= 4))
        def _():
            tile = phase - 1
            wait(weights(1, tile + 2))
            gated(xs[0], j, tile)

            @pl.when(tile < 2)
            def _():
                start(weights(1, tile + 4))

            @pl.when(jnp.logical_and(tile == 2, j < KV_CHUNKS - 1))
            def _():
                start(weights(1, 0))

            @pl.when(jnp.logical_and(tile == 3, j < KV_CHUNKS - 1))
            def _():
                start(weights(1, 1))

            @pl.when(j == KV_CHUNKS - 1)
            def _():
                send_hidden(j, tile)

    def tick(t, carry):
        for number in range(STEPS, -1, -1):
            place = t - STAGE_GAP * number
            chunk = place // START_GAP

            @pl.when(jnp.logical_and(place >= 0, jnp.logical_and(place % START_GAP == 0, chunk < CHUNKS)))
            def _():
                stage(number, chunk)

        @pl.when(jnp.logical_or(t == 1, t == 3))
        def _():
            gate_half(1, 2 + t // 2)

        @pl.when(t == OWN_TICK)
        def _():
            attend_own(1)

        @pl.when(jnp.logical_and(t > OWN_TICK, jnp.logical_and(t < DONE_TICK, t - OWN_TICK <= my_seq)))
        def _():
            visit(t - OWN_TICK - 1, ((1, 0), (1, 1)))

        @pl.when(t == EARLY_TICK)
        def _():
            attend_own(0)

        early = t - EARLY_TICK - 1

        @pl.when(jnp.logical_and(early >= 0, jnp.logical_and(early < 7, early < my_seq)))
        def _():
            arrivals(early, (0, 1))
            visit(early, ((0, 0),))

        @pl.when(t == 2)
        def _():
            take(part_recv.at[1], xbuf.at[pl.ds(0, depth // (2 * CHIPS)), :])
            round_start(2)

        @pl.when(t == DONE_TICK)
        def _():
            finish(2, False)
            finish(3, False)
            kv_sent()
            take(cache_sem, kv.at[own_rows, :])
            for n, peer in enumerate((left, right, other)):
                pl.semaphore_signal(ready_sem.at[n], inc=1, device_id={'seq': peer}, device_id_type=mesh_id)

        for when, j in NEAR_TICKS:
            @pl.when(t == when)
            def _():
                near_parts(j)

        for when, j in FAR_TICKS:
            @pl.when(t == when)
            def _():
                far_parts(j)

        @pl.when(t == GIVE_TICK)
        def _():
            for i in range(KV_CHUNKS):
                for z in range(KV_CHUNKS - 1):
                    send_hidden(z, i)

        late = t - BLOCK_TICK

        @pl.when(late >= 0)
        def _():
            block_work(late // BLOCK_GAP, late % BLOCK_GAP)

        for r, when in enumerate(HALF_TICKS):
            @pl.when(t == when)
            def _():
                last_half(r)

        for when, i in SERVE_TICKS:
            @pl.when(t == when)
            def _():
                serve_all(i)
        return carry

    lax.fori_loop(0, LAST_TICK, tick, 0)

    for slot in range(PART_SLOTS):
        partials_sent(slot)
    for step in range(4, STEPS):
        take(gather_send.at[step - 4], arrived_in(step, CHUNKS))
    for d in range(DIRS):
        pl.semaphore_signal(drained_sem.at[d], inc=1, device_id={'head': y_peer(d)}, device_id_type=mesh_id)
    start(cache_stores(1))
    attend_own(1)
    attend_past(0, my_seq, (), ((1, 0),))
    take(relay_recv, relay_buf)
    for i in range(KV_CHUNKS):
        relay_hidden(i).start()
    attend_past(0, near_count, (2, 4, 5), ((0, 1), (1, 1)))
    attend_past(near_count, my_seq, (2, 4, 5), ((0, 1),))
    finish(0, True)
    finish(1, True)
    attend_past(near_count, my_seq, (), ((1, 1),))
    finish(2, True)
    finish(3, True)
    parts_ref = gd_ref.at[pl.ds(0, 2), pl.ds(0, 3 * depth // 4), :]
    take(side_recv, parts_ref)

    quarter_rows = rows_per // RING

    def block_cols(c):
        return span(c * LAST_COLS, LAST_COLS)

    def tile_place(c, j, first, size):
        return wtile.at[c % 2, j // 2, pl.ds((j % 2) * depth + first, size), :]

    def tile_loads(c):
        copies = []
        for j in range(RING):
            z = wrap(pos_z + j)
            down = wd_ref.at[1, :, block_cols(c)] if j == 0 else gd_ref.at[z, :, block_cols(c)]
            out = wo_ref.at[1, 0, :, block_cols(c)] if j == 0 else go_ref.at[z, :, block_cols(c)]
            copies.append(pltpu.make_async_copy(down, tile_place(c, j, 0, ff_local), tile_sem.at[c % 2]))
            copies.append(pltpu.make_async_copy(out, tile_place(c, j, ff_local, head_dim), tile_sem.at[c % 2]))
        return copies

    start(tile_loads(0))
    given = hid.at[pl.ds(0, (RING - 1) * rows_per * depth // ff_local), :]
    take(give_recv, given)
    for d in range(DIRS):
        pl.semaphore_wait(drained_sem.at[d], 1)

    def quarter_of(piece, offset, size):
        return span(piece * quarter_rows + offset, size, quarter_rows // 2)

    def landed(d, first, size):
        return pl.ds(rows_per + d * (3 * quarter_rows // 2) + first, size)

    def rows_at(z, piece, offset, size):
        return span(z * rows_per + piece * quarter_rows + offset, size, quarter_rows // 2)

    def last_messages(step, c, d, z_first):
        s, cols, half = sign[d], block_cols(c), quarter_rows // 2
        near, behind, back = wrap(pos_y + s), wrap(pos_y - s), wrap(pos_z - s)
        along_y = step < 2 or (step < 4) != z_first
        if step == 0:
            pairs = [(part.at[quarter_of(wrap(pos_y + 2), d * half, half), cols], part.at[landed(d, quarter_rows, half), cols])]
        elif step == 1:
            pairs = [(part.at[quarter_of(near, 0, quarter_rows), cols], part.at[landed(d, 0, quarter_rows), cols])]
        else:
            if step == 2:
                rows = [rows_at(pos_z, pos_y, 0, quarter_rows)]
            elif step == 3:
                rows = [rows_at(back, pos_y, d * half, half) if z_first else rows_at(pos_z, behind, d * half, half)]
            elif step == 4:
                rows = [rows_at(z, pos_y, 0, quarter_rows) for z in range(RING)] if z_first else [rows_at(pos_z, 0, 0, rows_per)]
            else:
                rows = [rows_at(z, behind, d * half, half) for z in range(RING)] if z_first else [rows_at(back, 0, d * (rows_per // 2), rows_per // 2)]
            pairs = [(xbuf.at[r, cols], xbuf.at[r, cols]) for r in rows]
        to = (y_peer if along_y else z_peer)(d)
        return [remote(src, dst, last_send.at[step], last_recv.at[c, step], head=to) for src, dst in pairs]

    def last_arrived(step, cols):
        rows = (quarter_rows, 2 * quarter_rows, 2 * quarter_rows, quarter_rows, 2 * rows_per, rows_per)[step]
        return (part if step < 2 else xbuf).at[pl.ds(0, rows), cols]

    def send_last(step, c):
        def both(z_first):
            for d in range(DIRS):
                start(last_messages(step, c, d, z_first))

        if step < 2:
            both(False)
            return
        z_first = jnp.logical_and(c >= 5, c % 2 == 1)

        @pl.when(z_first)
        def _():
            both(True)

        @pl.when(jnp.logical_not(z_first))
        def _():
            both(False)

    def out_store(c):
        return pltpu.make_async_copy(xbuf.at[:, block_cols(c)], out_ref.at[:, block_cols(c)], store_sem)

    def last_project(c):
        @pl.when(c + 1 < LAST_BLOCKS)
        def _():
            start(tile_loads(c + 1))

        take(tile_sem.at[c % 2], wtile.at[c % 2, :, pl.ds(0, 2 * depth), :])
        total = None
        for j in range(RING):
            z = wrap(pos_z + j)
            own = span(pos_z * rows_per, rows_per)
            hidden_rows = hid[own, :] if j == 0 else xs[1, :, span(z * ff_local, ff_local)]
            out_rows = att[own, :] if j == 0 else att_all[z]
            term = dot(hidden_rows, wtile[c % 2, j // 2, pl.ds((j % 2) * depth, ff_local), :])
            term = term + dot(out_rows, wtile[c % 2, j // 2, pl.ds((j % 2) * depth + ff_local, head_dim), :])
            total = term if total is None else total + term
        part[pl.ds(0, rows_per), block_cols(c)] = total

    def last_stage(number, c):
        cols, half = block_cols(c), quarter_rows // 2
        if number == 0:
            last_project(c)
        else:
            take(last_recv.at[c, number - 1], last_arrived(number - 1, cols))
        if number == 1:
            for d in range(DIRS):
                piece = quarter_of(wrap(pos_y + sign[d]), d * half, half)
                part[piece, cols] = part[piece, cols] + part[landed(d, quarter_rows, half), cols]
        if number == 2:
            own = quarter_of(pos_y, 0, quarter_rows)
            total = part[own, cols] + part[landed(0, 0, quarter_rows), cols] + part[landed(1, 0, quarter_rows), cols]
            update = total.astype(bf16).astype(f32)
            rows = rows_at(pos_z, pos_y, 0, quarter_rows)
            xbuf[rows, cols] = (xbuf[rows, cols].astype(f32) + update).astype(bf16)
        if number < LAST_STEPS:
            send_last(number, c)
        else:
            out_store(c).start()

    def last_tick(t, carry):
        for number in range(LAST_STEPS, -1, -1):
            c = t - LAST_GAP * number

            @pl.when(jnp.logical_and(c >= 0, c < LAST_BLOCKS))
            def _():
                last_stage(number, c)
        return carry

    lax.fori_loop(0, LAST_BLOCKS + LAST_GAP * LAST_STEPS, last_tick, 0)

    take(cache_sem, kv.at[own_rows, :])
    take(relay_send, relay_buf)
    kv_sent()
    take(part_send, xbuf.at[pl.ds(0, 3 * depth // 8), :])
    take(round_send, gd_ref.at[pl.ds(0, 2), pl.ds(0, 9 * depth // 16), :])
    take(side_send, parts_ref)
    take(give_send, given)
    for step in range(LAST_STEPS):
        take(last_send.at[step], last_arrived(step, pl.ds(0, d_model)))
    take(store_sem, xbuf)


def layers(x_loc, cos_t, sin_t, norm_gain, w_q, w_k, w_v, w_gate, w_up, w_down, w_o):
    tok_count, d_model = x_loc.shape
    head_dim = w_q.shape[2]
    ff_local = w_gate.shape[2]
    rows_per = tok_count // KV_CHUNKS
    chunk_rows = tok_count // CHUNKS
    landed = 3 * chunk_rows // (2 * RING)
    half_cols = d_model // HALVES
    any_spec = pl.BlockSpec(memory_space=pl.ANY)
    vmem_spec = pl.BlockSpec(memory_space=pltpu.VMEM)
    bf16, f32 = jnp.bfloat16, jnp.float32
    dma = pltpu.SemaphoreType.DMA
    shape = jax.ShapeDtypeStruct
    return pl.pallas_call(
        layers_kernel,
        out_shape=[shape((tok_count, d_model), bf16)] + [shape((tok_count, head_dim), bf16)] * 4
        + [shape((RING, ff_local, d_model), bf16), shape((RING, head_dim, d_model), bf16)],
        in_specs=[any_spec, vmem_spec, vmem_spec, vmem_spec] + [any_spec] * 7,
        out_specs=[any_spec] * 7,
        scratch_shapes=[
            pltpu.VMEM((tok_count, d_model), bf16),
            pltpu.VMEM((PART_SLOTS * chunk_rows, d_model), f32),
            pltpu.VMEM((RECV_SLOTS, HALVES, DIRS, landed, half_cols), f32),
            pltpu.VMEM((RECV_SLOTS, HALVES, DIRS, landed, half_cols // RING), f32),
            pltpu.VMEM((tok_count, ff_local), bf16),
            pltpu.VMEM((tok_count, head_dim), bf16),
            pltpu.VMEM((2, ff_local + head_dim, DOWN_TILE), bf16),
            pltpu.VMEM((2, 2, d_model, W_TILE), bf16),
            pltpu.VMEM((2 * CHIPS * tok_count, 2 * head_dim), bf16),
            pltpu.VMEM((tok_count, head_dim), bf16),
            pltpu.VMEM((2, tok_count, head_dim), f32),
            pltpu.VMEM((2, tok_count, 128), f32),
            pltpu.VMEM((2, tok_count, 128), f32),
            pltpu.VMEM((2, rows_per, d_model), bf16),
            pltpu.VMEM((CHUNKS, HALVES, chunk_rows // RING, half_cols // RING), bf16),
            dma((2,)), dma, dma((2, 2)), dma((2, 2)), dma, dma,
            dma((10,)), dma((4, KV_CHUNKS + 2)), dma((4, KV_CHUNKS + 2)), dma, dma((2,)),
            dma, dma((2, RING - 1)), dma, dma,
            dma, dma,
            pltpu.VMEM((KV_CHUNKS, rows_per, W_TILE), bf16), dma, dma,
            pltpu.VMEM((RING, rows_per, head_dim), bf16),
            dma((PART_SLOTS,)), dma((4,)), dma((RECV_SLOTS, STEPS)),
            dma((LAST_STEPS,)), dma((LAST_BLOCKS, LAST_STEPS)), dma((2,)),
            pltpu.SemaphoreType.REGULAR((3,)), pltpu.SemaphoreType.REGULAR((DIRS,)),
        ],
        compiler_params=pltpu.CompilerParams(collective_id=0, has_side_effects=True, vmem_limit_bytes=67043328),
        name='layers',
    )(x_loc, cos_t, sin_t, norm_gain, w_q, w_k, w_v, w_gate, w_up, w_down, w_o)


EMIT_PARTS = 8


def emit_kernel(x_ref, k_first, k_second, v_first, v_second, x_out, k_out, v_out, xbuf, rows, load_sem, store_sem):
    size = x_ref.shape[0] // EMIT_PARTS
    loads, stores = [], []
    for n in range(EMIT_PARTS):
        part = pl.ds(n * size, size)
        loads.append(pltpu.make_async_copy(x_ref.at[part, :], xbuf.at[part, :], load_sem.at[n]))
        stores.append(pltpu.make_async_copy(xbuf.at[part, :], x_out.at[part, :], store_sem.at[n]))
    for n, (ref, out) in enumerate(((k_first, k_out.at[0]), (k_second, k_out.at[1]), (v_first, v_out.at[0]), (v_second, v_out.at[1]))):
        loads.append(pltpu.make_async_copy(ref, rows.at[n], load_sem.at[EMIT_PARTS + n]))
        stores.append(pltpu.make_async_copy(rows.at[n], out, store_sem.at[EMIT_PARTS + n]))
    for copy in loads:
        copy.start()
    for load, store in zip(loads, stores):
        load.wait()
        store.start()
    for copy in stores:
        copy.wait()


def emit(x_out, k_first, k_second, v_first, v_second):
    any_spec = pl.BlockSpec(memory_space=pl.ANY)
    cache = jax.ShapeDtypeStruct((2,) + k_first.shape, jnp.bfloat16)
    return pl.pallas_call(
        emit_kernel,
        out_shape=[jax.ShapeDtypeStruct(x_out.shape, jnp.bfloat16), cache, cache],
        in_specs=[any_spec] * 5,
        out_specs=[any_spec] * 3,
        scratch_shapes=[
            pltpu.VMEM(x_out.shape, jnp.bfloat16),
            pltpu.VMEM((4,) + k_first.shape, jnp.bfloat16),
            pltpu.SemaphoreType.DMA((EMIT_PARTS + 4,)),
            pltpu.SemaphoreType.DMA((EMIT_PARTS + 4,)),
        ],
        compiler_params=pltpu.CompilerParams(vmem_limit_bytes=63 * 1024 * 1024),
        name='emit',
    )(x_out, k_first, k_second, v_first, v_second)


def solution(mesh):
    row_spec = P(('batch', 'seq'), None)
    pos_spec = P(('batch', 'seq'))
    head_spec = P(None, None, 'head', None)
    out_proj_spec = P(None, 'head', None, None)
    col_spec = P(None, None, 'head')
    down_spec = P(None, 'head', None)
    cache_spec = P(None, ('batch', 'seq'), 'head', None)

    def local_forward(x_loc, pos_loc, w_q, w_k, w_v, w_o, w_gate, w_up, w_down, norm_gain):
        tok_count, d_model = x_loc.shape
        layer_count = w_q.shape[0]
        head_dim = w_q.shape[3]
        flat_q, flat_k, flat_v = (w.reshape(layer_count, d_model, head_dim) for w in (w_q, w_k, w_v))
        cos_t, sin_t = rope_tables(pos_loc, head_dim)
        x_out, k_first, v_first, k_second, v_second, _, _ = layers(x_loc, cos_t, sin_t, norm_gain, flat_q, flat_k, flat_v, w_gate, w_up, w_down, w_o)
        x_out, k_all, v_all = emit(x_out, k_first, k_second, v_first, v_second)
        cache_shape = (layer_count, tok_count, 1, head_dim)
        return x_out, k_all.reshape(cache_shape), v_all.reshape(cache_shape)

    return jax.shard_map(local_forward, mesh=mesh, in_specs=(row_spec, pos_spec, head_spec, head_spec, head_spec, out_proj_spec, col_spec, col_spec, down_spec, P(None, None)), out_specs=(row_spec, cache_spec, cache_spec), check_vma=False)
```

```python
import functools
import math
import jax
import jax.numpy as jnp
from jax import lax
from jax.experimental import pallas as pl
from jax.experimental.pallas import tpu as pltpu
from jax.sharding import PartitionSpec as P

ROPE_BASE = 500000.0
EPS = 1e-5


def rope_tables(positions, head_dim):
    half_dim = head_dim // 2
    inv_freq = ROPE_BASE ** (-(jnp.arange(half_dim, dtype=jnp.float32) * 2.0 / head_dim))
    angles = positions.astype(jnp.float32)[..., None] * inv_freq
    return jnp.cos(angles), jnp.sin(angles)


CHIPS = 4
RING = 4
HALVES = 2
DIRS = 2
KV_CHUNKS = 4
W_TILE = 256
NORM_ROWS = 64
CHUNKS = 8
STEPS = 8
PART_SLOTS = 4
RECV_SLOTS = 5
DOWN_TILE = 512
START_GAP = 3
STAGE_GAP = 2
BLOCK_TICK = 19
BLOCK_GAP = 6
LAST_TICK = 43
NEAR_TICKS = ((9, 1), (15, 3), (20, 2))
FAR_TICKS = ((24, 1), (26, 3), (36, 2))
SERVE_TICKS = (27, 31, 36, 42)
GIVE_TICK = 37
OWN_TICK = 3
DONE_TICK = 11
EARLY_TICK = 31
LAST_STEPS = 6
LAST_COLS = 256
LAST_BLOCKS = 16
LAST_GAP = 3


def layers_kernel(x_ref, cos_ref, sin_ref, gain_ref, wq_ref, wk_ref, wv_ref, wg_ref, wu_ref, wd_ref, wo_ref,
                 out_ref, k1_ref, v1_ref, k2_ref, v2_ref, gd_ref, go_ref,
                 xbuf, part, recv_a, recv_b, hid, att, wdo, wtile, kv, qbuf, acc, row_max, row_sum, xs, xres,
                 x_sem, res_sem, w_sem, down_sem, cache_sem, store_sem, kv_send, ici_recv, core_recv, part_send, part_recv,
                 round_send, round_recv, side_send, side_recv, give_send, give_recv, relay_buf, relay_send, relay_recv, att_all, ring_send, gather_send, ring_recv,
                 last_send, last_recv, tile_sem, cos_buf, sin_buf, rope_sem, ready_sem, drained_sem):
    tok_count, d_model = xbuf.shape
    head_dim = qbuf.shape[1]
    half_dim = head_dim // 2
    ff_local = hid.shape[1]
    depth = ff_local + head_dim
    rows_per = tok_count // KV_CHUNKS
    half_rows = tok_count // 2
    lanes = row_max.shape[2]
    chunk_rows = tok_count // CHUNKS
    quarter, eighth = chunk_rows // RING, chunk_rows // (2 * RING)
    half_cols = d_model // HALVES
    piece_cols = half_cols // RING
    bf16, f32 = jnp.bfloat16, jnp.float32
    sign = (1, -1)
    mesh_id = pl.DeviceIdType.MESH

    my_head = lax.axis_index('head')
    pos_z, pos_y = my_head // RING, my_head % RING
    my_seq = lax.axis_index('seq')
    chip, core = my_seq // 2, my_seq % 2
    other = chip * 2 + 1 - core

    def wrap(n):
        return (n + RING) % RING

    def y_peer(d):
        return pos_z * RING + wrap(pos_y + sign[d])

    def z_device(z):
        return wrap(z) * RING + pos_y

    def z_peer(d):
        return z_device(pos_z + sign[d])

    def x_device(n):
        return wrap(chip + n) * 2 + core

    right, left = x_device(1), x_device(-1)

    def span(start, size, unit=None):
        return pl.ds(pl.multiple_of(start, unit or size), size)

    def remote(src, dst, send, recv, **to):
        return pltpu.make_async_remote_copy(src_ref=src, dst_ref=dst, send_sem=send, recv_sem=recv, device_id=to, device_id_type=mesh_id)

    def take(sem, ref):
        remote(ref, ref, sem, sem, head=my_head).wait_recv()

    def x_load(i):
        return pltpu.make_async_copy(x_ref.at[span(i * rows_per, rows_per), :], xs.at[i % 2], x_sem.at[i % 2])

    def weights(layer, piece):
        slot = piece % 2
        if isinstance(piece, int) and piece < 2:
            refs = ((wk_ref, wv_ref), (wq_ref,))[piece]
            return [pltpu.make_async_copy(ref.at[layer], wtile.at[slot, n], w_sem.at[slot, n]) for n, ref in enumerate(refs)]
        cols = span((piece - 2) * W_TILE, W_TILE)
        return [pltpu.make_async_copy(ref.at[layer, :, cols], wtile.at[slot, n], w_sem.at[slot, n]) for n, ref in enumerate((wg_ref, wu_ref))]

    def start(copies):
        for copy in copies:
            copy.start()

    def wait(copies):
        for copy in copies:
            copy.wait()

    down_tiles = d_model // DOWN_TILE

    def down_load(i):
        cols = span(i * DOWN_TILE, DOWN_TILE)
        return [pltpu.make_async_copy(wd_ref.at[0, :, cols], wdo.at[i % 2, pl.ds(0, ff_local), :], down_sem.at[i % 2, 0]),
                pltpu.make_async_copy(wo_ref.at[0, 0, :, cols], wdo.at[i % 2, pl.ds(ff_local, head_dim), :], down_sem.at[i % 2, 1])]

    def kv_copy(origin_chip, origin_core, i, to, send, recv):
        rows = kv.at[span((origin_chip * 2 + origin_core) * tok_count + i * rows_per, rows_per), :]
        return remote(rows, rows, send, recv, seq=to)

    def kv_routes(i):
        def to(number, recv, origin_chip, origin_core, device):
            return lambda: kv_copy(origin_chip, origin_core, i, device, kv_send.at[number], recv)
        inner = jnp.logical_and(chip >= 1, chip < CHIPS - 1)
        return {
            'right': (chip < CHIPS - 1, 'all', to(0, ici_recv.at[0, i], chip, core, right)),
            'wrap': (chip == 0, 'all', to(1, ici_recv.at[2, i], chip, core, left)),
            'relay': (chip == 1, 'late', to(2, ici_recv.at[3, i], chip, core, left)),
            'other': (core == 0, 'all', to(3, core_recv.at[0, i], chip, core, other)),
            'on_right': (inner, 'early', to(4, ici_recv.at[1, i], chip - 1, core, right)),
            'from_relay': (chip == 0, 'late', to(5, ici_recv.at[1, i], 1, core, left)),
            'on_left': (chip == CHIPS - 1, 'late', to(6, ici_recv.at[1, i], 0, core, left)),
            'side1': (chip >= 1, 'all', to(7, core_recv.at[1, i], chip - 1, core, other)),
            'side2': (chip >= 2, 'all', to(8, core_recv.at[2, i], chip - 2, core, other)),
            'side3': (chip >= 3, 'all', to(9, core_recv.at[3, i], chip - 3, core, other)),
        }

    def start_route(i, name):
        condition, which, copy = kv_routes(i)[name]
        if which != 'all':
            late = i >= KV_CHUNKS // 2
            if isinstance(i, int):
                if late != (which == 'late'):
                    return
            else:
                condition = jnp.logical_and(condition, late if which == 'late' else jnp.logical_not(late))

        @pl.when(condition)
        def _():
            copy().start()

    def send_kv(i):
        for name in ('right', 'wrap', 'relay', 'other'):
            start_route(i, name)

    def kv_sent():
        for number, (condition, which, _) in enumerate(kv_routes(0).values()):
            @pl.when(condition)
            def _():
                take(kv_send.at[number], kv.at[pl.ds(0, tok_count if which == 'all' else half_rows), :])

    def serve(back, i):
        @pl.when(chip >= back)
        def _():
            kv_copy(chip - back, core, i, other, kv_send.at[0], ici_recv.at[back - 1, i]).wait_recv()
        start_route(i, 'side%d' % back)
        if back == 1:
            start_route(i, 'on_right')
        if back == 3:
            start_route(i, 'on_left')

    def relay(i):
        def pass_on():
            @pl.when(chip == 0)
            def _():
                kv_copy(1, core, i, left, kv_send.at[0], ici_recv.at[3, i]).wait_recv()
            start_route(i, 'from_relay')
        if not isinstance(i, int):
            pl.when(i >= KV_CHUNKS // 2)(pass_on)
        elif i >= KV_CHUNKS // 2:
            pass_on()

    def serve_all(i):
        serve(1, i)
        serve(3, i)
        relay(i)

    def taken(back, chunks):
        for i in chunks:
            kv_copy(chip - back, 1 - core, i, other, kv_send.at[0], core_recv.at[back, i]).wait_recv()

    def z_parts(step, d):
        copies = []
        for n, (own_ref, all_ref) in enumerate(((wd_ref, gd_ref), (wo_ref, go_ref))):
            size = all_ref.shape[1] // (2 * CHIPS)
            if step == 0:
                rows = span(my_seq * size, size)
                src = own_ref.at[1, rows, :] if n == 0 else own_ref.at[1, 0, rows, :]
                dst = all_ref.at[pos_z, rows, :]
            else:
                rows = span(my_seq * size + d * (size // 2), size // 2)
                src = dst = all_ref.at[wrap(pos_z - sign[d]), rows, :]
            copies.append(remote(src, dst, part_send, part_recv.at[step], head=z_peer(d)))
        return copies

    def part_copies(j, part_chip, part_core, half, send, recv, to):
        copies = []
        for n, ref in enumerate((gd_ref, go_ref)):
            size = ref.shape[1] // (2 * CHIPS)
            first = (part_chip * 2 + part_core) * size
            rows = span(first, size) if half is None else span(first + half * (size // 2), size // 2)
            place = ref.at[wrap(pos_z + j), rows, :]
            copies.append(remote(place, place, send, recv, seq=to))
        return copies

    def own_part(j, d):
        return part_copies(j, chip, core, None, round_send, round_recv.at[0, j - 1], x_device(sign[d]))

    def far_part(j, d):
        return part_copies(j, wrap(chip - sign[d]), core, d, round_send, round_recv.at[1, j - 1], x_device(sign[d]))

    def side_part(j, n, side):
        return part_copies(j, wrap(chip + n), side, None, side_send, side_recv, other)

    def round_start(j):
        for d in range(DIRS):
            start(own_part(j, d))
        start(side_part(j, 0, core))

    def near_parts(j):
        take(round_recv.at[0, j - 1], xbuf.at[pl.ds(0, depth // CHIPS), :])
        for d in range(DIRS):
            start(far_part(j, d) + side_part(j, 3 if d == 0 else 1, core))

    def far_parts(j):
        take(round_recv.at[1, j - 1], xbuf.at[pl.ds(0, depth // (2 * CHIPS)), :])
        start(side_part(j, 2, core))

    def give_hidden(z, i, source):
        cols = span(i * W_TILE, W_TILE)
        return remote(hid.at[span(z * rows_per, rows_per), cols], hidden_place(source, i), give_send, give_recv, head=z_device(z))

    def hidden_place(source, i):
        return xs.at[1, :, span(source * ff_local + i * W_TILE, W_TILE)]

    def via_neighbor(z, i):
        step = jnp.where(i < KV_CHUNKS // 2, 1, -1)
        return remote(hid.at[span(z * rows_per, rows_per), span(i * W_TILE, W_TILE)], relay_buf.at[i], give_send, relay_recv, head=z_device(pos_z + step))

    def relay_hidden(i):
        step = 1 if i < KV_CHUNKS // 2 else -1
        source = wrap(pos_z - step)
        return remote(relay_buf.at[i], hidden_place(source, i), relay_send, give_recv, head=z_device(pos_z + step))

    def send_hidden(z, i):
        away = wrap(z - pos_z)

        @pl.when(away == 2)
        def _():
            via_neighbor(z, i).start()

        @pl.when(away % 2 == 1)
        def _():
            give_hidden(z, i, pos_z).start()

    def give_rows(z, source):
        return remote(att.at[span(z * rows_per, rows_per), :], att_all.at[source], give_send, give_recv, head=z_device(z))

    def norm_rows(x_few, layer):
        x_f32 = x_few.astype(f32)
        inv_rms = lax.rsqrt(jnp.mean(x_f32 * x_f32, axis=-1, keepdims=True) + EPS)
        return (x_f32 * inv_rms * gain_ref[pl.ds(layer, 1), :].astype(f32)).astype(bf16)

    def rope(values, rows):
        cos_t, sin_t = cos_buf[rows, :], sin_buf[rows, :]
        wide = values.astype(bf16).astype(f32)
        first, second = wide[:, :half_dim], wide[:, half_dim:]
        return jnp.concatenate([first * cos_t - second * sin_t, second * cos_t + first * sin_t], axis=1).astype(bf16)

    def dot(a, b):
        return jnp.dot(a, b, preferred_element_type=f32)

    scale = 1.0 / math.sqrt(head_dim)

    def keys_values(normed, i):
        rows = span(i * rows_per, rows_per)
        own = span(my_seq * tok_count + i * rows_per, rows_per)
        kv[own, :head_dim] = rope(dot(normed, wtile[0, 0]), rows)
        kv[own, head_dim:] = dot(normed, wtile[0, 1]).astype(bf16)

    def queries(normed, i):
        rows = span(i * rows_per, rows_per)
        qbuf[rows, :] = (rope(dot(normed, wtile[1, 0]), rows).astype(f32) * scale).astype(bf16)

    def gated(normed, i, tile):
        gate = dot(normed, wtile[tile % 2, 0])
        up = dot(normed, wtile[tile % 2, 1])
        hid[span(i * rows_per, rows_per), span(tile * W_TILE, W_TILE)] = (gate * jax.nn.sigmoid(gate) * up).astype(bf16)

    def attend(key_start, q_half, side, masked, first):
        rows = pl.ds(q_half * half_rows, half_rows)
        some = span(key_start, half_rows)
        logits = lax.dot_general(qbuf[rows, :], kv[some, :head_dim], (((1,), (1,)), ((), ())), preferred_element_type=f32)
        if masked:
            seen = lax.broadcasted_iota(jnp.int32, logits.shape, 0) >= lax.broadcasted_iota(jnp.int32, logits.shape, 1)
            logits = jnp.where(seen, logits, -jnp.inf)
        block_max = jnp.max(logits, axis=-1, keepdims=True)
        if first:
            new_max = jnp.broadcast_to(block_max, (half_rows, lanes))
        else:
            new_max = jnp.maximum(row_max[side, rows, :], block_max)
        prob = jnp.exp(logits - jnp.concatenate([new_max] * (half_rows // lanes), axis=1))
        block_sum = jnp.sum(prob, axis=-1, keepdims=True)
        block_out = dot(prob.astype(bf16), kv[some, head_dim:])
        if first:
            row_sum[side, rows, :] = jnp.broadcast_to(block_sum, (half_rows, lanes))
            acc[side, rows, :] = block_out
        else:
            rescale = jnp.exp(row_max[side, rows, :] - new_max)
            row_sum[side, rows, :] = row_sum[side, rows, :] * rescale + block_sum
            acc[side, rows, :] = acc[side, rows, :] * jnp.concatenate([rescale] * (head_dim // lanes), axis=1) + block_out
        row_max[side, rows, :] = new_max

    def attend_own(layer_half):
        own_start = my_seq * tok_count
        if layer_half == 0:
            attend(own_start, 0, 0, True, True)
            top_rows = pl.ds(0, half_rows)
            row_max[1, top_rows, :] = jnp.full((half_rows, lanes), -jnp.inf, f32)
            row_sum[1, top_rows, :] = jnp.zeros((half_rows, lanes), f32)
            acc[1, top_rows, :] = jnp.zeros((half_rows, head_dim), f32)
        else:
            attend(own_start, 1, 0, False, True)
            attend(own_start + half_rows, 1, 1, True, True)

    def past_start(n):
        later = n - core
        back = jnp.where(later < 2, 1, jnp.where(chip == CHIPS - 1, jnp.where(later < 4, 3, 2), 2))
        block = (chip - back) * 2 + jnp.where(later % 2 == 0, core, 1 - core)
        return jnp.where(jnp.logical_and(core == 1, n == 0), chip * 2, block) * tok_count

    def arrivals(n, chunks):
        @pl.when(jnp.logical_and(core == 1, n == 0))
        def _():
            taken(0, chunks)

        for back in (1, 3, 2):
            place = 0 if back == 1 else 2 if back == 3 else jnp.where(chip == CHIPS - 1, 4, 2)
            if back == 2:
                @pl.when(jnp.logical_and(chip >= back, n == core + place))
                def _():
                    for i in chunks:
                        serve(2, i)

            @pl.when(jnp.logical_and(chip >= back, n == core + place + 1))
            def _():
                taken(back, chunks)

    def visit(n, visits):
        for q_half, side in visits:
            attend(past_start(n) + side * half_rows, q_half, side, False, False)

    def attend_past(first_n, last_n, chunks, visits):
        def past(n, count):
            for r in range(count if chunks else 0):
                arrivals(n + r, chunks)
            for r in range(count):
                visit(n + r, visits)

        def two(p, carry):
            past(first_n + 2 * p, 2)
            return carry

        count = last_n - first_n
        lax.fori_loop(0, count // 2, two, 0)

        @pl.when(count % 2 == 1)
        def _():
            past(last_n - 1, 1)

    near_count = my_seq - jnp.where(chip >= 2, 2, 0)

    def finish(i, spread):
        rows = pl.ds(i * rows_per, rows_per)
        top = jnp.maximum(row_max[0, rows, :], row_max[1, rows, :])
        shares = [jnp.exp(row_max[side, rows, :] - top) for side in range(2)]
        total = shares[0] * row_sum[0, rows, :] + shares[1] * row_sum[1, rows, :]
        wide = [jnp.concatenate([w] * (head_dim // lanes), axis=1) for w in shares + [total]]
        att[rows, :] = ((acc[0, rows, :] * wide[0] + acc[1, rows, :] * wide[1]) / wide[2]).astype(bf16)
        if spread:
            @pl.when(i != pos_z)
            def _():
                give_rows(i, pos_z).start()

    first_pos, second_pos = (pos_y, pos_z), (pos_z, pos_y)
    first_peer, second_peer = (y_peer, z_peer), (z_peer, y_peer)

    def part_rows(chunk, piece, offset, count):
        return span((chunk % PART_SLOTS) * chunk_rows + piece * quarter + offset, count, eighth)

    def x_rows(chunk, piece, offset, count):
        return span(chunk * chunk_rows + piece * quarter + offset, count, eighth)

    def cols_of(h, piece):
        return span(h * half_cols + piece * piece_cols, piece_cols)

    def half_of(h):
        return pl.ds(h * half_cols, half_cols)

    def message(step, chunk, h, d):
        p1, p2, s = first_pos[h], second_pos[h], sign[d]
        slot = chunk % RECV_SLOTS
        if step == 0:
            src, dst = part.at[part_rows(chunk, wrap(p1 + 2), d * eighth, eighth), half_of(h)], recv_a.at[slot, h, d, pl.ds(quarter, eighth), :]
        elif step == 1:
            src, dst = part.at[part_rows(chunk, wrap(p1 + s), 0, quarter), half_of(h)], recv_a.at[slot, h, d, pl.ds(0, quarter), :]
        elif step == 2:
            src, dst = part.at[part_rows(chunk, p1, d * eighth, eighth), cols_of(h, wrap(p2 + 2))], recv_b.at[slot, h, d, pl.ds(quarter, eighth), :]
        elif step == 3:
            src, dst = part.at[part_rows(chunk, p1, 0, quarter), cols_of(h, wrap(p2 + s))], recv_b.at[slot, h, d, pl.ds(0, quarter), :]
        elif step == 4:
            src = dst = xbuf.at[x_rows(chunk, p1, 0, quarter), cols_of(h, p2)]
        elif step == 5:
            src = dst = xbuf.at[x_rows(chunk, p1, d * eighth, eighth), cols_of(h, wrap(p2 - s))]
        elif step == 6:
            src = dst = xbuf.at[x_rows(chunk, p1, 0, quarter), half_of(h)]
        else:
            src = dst = xbuf.at[x_rows(chunk, wrap(p1 - s), d * eighth, eighth), half_of(h)]
        peer = (first_peer if step in (0, 1, 6, 7) else second_peer)[h](d)
        return remote(src, dst, ring_send.at[chunk % PART_SLOTS] if step < 4 else gather_send.at[step - 4], ring_recv.at[slot, step], head=peer)

    def arrived_in(step, count=1):
        rows = (2 * eighth, 2 * quarter, eighth // 2, quarter // 2, quarter // 2, quarter // 2, 2 * quarter, quarter)[step] * count
        return (part if step < 4 else xbuf).at[pl.ds(0, rows), pl.ds(0, half_cols if step == 5 else d_model)]

    def partials_sent(slot):
        take(ring_send.at[slot], part.at[pl.ds(0, 2 * eighth + 2 * quarter + eighth // 2 + quarter // 2), :])

    def residual_load(chunk, h):
        return pltpu.make_async_copy(x_ref.at[x_rows(chunk, first_pos[h], 0, quarter), cols_of(h, second_pos[h])], xres.at[chunk, h], res_sem)

    def project(chunk):
        rows = span(chunk * chunk_rows, chunk_rows)
        slot_rows = span((chunk % PART_SLOTS) * chunk_rows, chunk_rows)

        def one_tile(i, carry):
            @pl.when(jnp.logical_or(chunk < CHUNKS - 1, i < down_tiles - 1))
            def _():
                start(down_load((i + 1) % down_tiles))

            wait(down_load(i))
            total = dot(hid[rows, :], wdo[i % 2, :ff_local, :])
            part[slot_rows, span(i * DOWN_TILE, DOWN_TILE)] = total + dot(att[rows, :], wdo[i % 2, ff_local:, :])
            return carry

        lax.fori_loop(0, down_tiles, one_tile, 0)

    def stage(number, chunk):
        slot = chunk % RECV_SLOTS
        if number == 0:
            @pl.when(chunk >= PART_SLOTS)
            def _():
                partials_sent(chunk % PART_SLOTS)
            project(chunk)
        else:
            take(ring_recv.at[slot, number - 1], arrived_in(number - 1))
        if number == 4:
            @pl.when(chunk == 0)
            def _():
                take(res_sem, xres)
        for h in range(HALVES):
            p1, p2 = first_pos[h], second_pos[h]
            if number in (1, 3):
                for d in range(DIRS):
                    if number == 1:
                        rows, cols, arrived = part_rows(chunk, wrap(p1 + sign[d]), d * eighth, eighth), half_of(h), recv_a
                    else:
                        rows, cols, arrived = part_rows(chunk, p1, d * eighth, eighth), cols_of(h, wrap(p2 + sign[d])), recv_b
                    part[rows, cols] = part[rows, cols] + arrived[slot, h, d, pl.ds(quarter, eighth), :]
            if number == 2:
                rows = part_rows(chunk, p1, 0, quarter)
                part[rows, half_of(h)] = part[rows, half_of(h)] + recv_a[slot, h, 0, pl.ds(0, quarter), :] + recv_a[slot, h, 1, pl.ds(0, quarter), :]
            if number == 4:
                rows, cols = part_rows(chunk, p1, 0, quarter), cols_of(h, p2)
                total = part[rows, cols] + recv_b[slot, h, 0, pl.ds(0, quarter), :] + recv_b[slot, h, 1, pl.ds(0, quarter), :]
                update = total.astype(bf16).astype(f32)
                xbuf[x_rows(chunk, p1, 0, quarter), cols] = (xres[chunk, h].astype(f32) + update).astype(bf16)
            if number < STEPS:
                for d in range(DIRS):
                    message(number, chunk, h, d).start()

    rope_loads = [pltpu.make_async_copy(ref, buf, rope_sem.at[n]) for n, (ref, buf) in enumerate(((cos_ref, cos_buf), (sin_ref, sin_buf)))]
    x_load(0).start()
    start(weights(0, 0))
    start(rope_loads)
    barrier = pltpu.get_barrier_semaphore()
    for peer in (left, right, other):
        pl.semaphore_signal(barrier, inc=1, device_id={'seq': peer}, device_id_type=mesh_id)
    for peer in [z_device(pos_z + j) for j in range(1, RING)] + [y_peer(d) for d in range(DIRS)]:
        pl.semaphore_signal(barrier, inc=1, device_id={'head': peer}, device_id_type=mesh_id)

    def prepare(i, carry):
        x_load(i).wait()

        @pl.when(i == 0)
        def _():
            x_load(1).start()
            start(weights(0, 1))

        def few(n, inner):
            xbuf[span(i * rows_per + n * NORM_ROWS, NORM_ROWS), :] = norm_rows(xs[i % 2, span(n * NORM_ROWS, NORM_ROWS), :], 0)
            return inner

        lax.fori_loop(0, rows_per // NORM_ROWS, few, 0)

        @pl.when(i + 2 < KV_CHUNKS)
        def _():
            x_load(i + 2).start()

        @pl.when(i == 0)
        def _():
            wait(weights(0, 0))
            wait(rope_loads)

        keys_values(xbuf[span(i * rows_per, rows_per), :], i)

        @pl.when(i == 0)
        def _():
            pl.semaphore_wait(barrier, 8)

        send_kv(i)

        @pl.when(i == 0)
        def _():
            for d in range(DIRS):
                start(z_parts(0, d))
        return carry

    lax.fori_loop(0, KV_CHUNKS, prepare, 0)
    start(weights(0, 2))
    own_rows = span(my_seq * tok_count, tok_count)

    def cache_stores(layer):
        k_ref, v_ref = ((k1_ref, v1_ref), (k2_ref, v2_ref))[layer]
        return [pltpu.make_async_copy(kv.at[own_rows, pl.ds(0, head_dim)], k_ref, cache_sem),
                pltpu.make_async_copy(kv.at[own_rows, pl.ds(head_dim, head_dim)], v_ref, cache_sem)]

    start(cache_stores(0))
    wait(weights(0, 1))

    def query(i, carry):
        queries(xbuf[span(i * rows_per, rows_per), :], i)
        return carry

    lax.fori_loop(0, KV_CHUNKS, query, 0)
    start(weights(0, 3))
    start(down_load(0))

    def residuals(n, carry):
        for h in range(HALVES):
            residual_load(n, h).start()
        return carry

    lax.fori_loop(0, CHUNKS, residuals, 0)

    def gate_half(half, tile):
        wait(weights(0, tile + 2))

        def rows_step(i, inner):
            gated(xbuf[span(i * rows_per, rows_per), :], i, tile)
            return inner

        lax.fori_loop(half * KV_CHUNKS // 2, (half + 1) * KV_CHUNKS // 2, rows_step, 0)

        @pl.when(tile < 2)
        def _():
            start(weights(0, tile + 4))

        for last in (2, 3):
            @pl.when(tile == last)
            def _():
                start(weights(1, last - 2) if half else weights(0, last))

    def first_half(tile, carry):
        gate_half(0, tile)

        @pl.when(tile < 3)
        def _():
            serve_all(tile)
        return carry

    def second_half(tile, carry):
        gate_half(1, tile)

        @pl.when(tile == 0)
        def _():
            serve_all(3)
            attend_past(0, near_count, range(KV_CHUNKS), ((0, 0), (0, 1)))
            take(part_recv.at[0], xbuf.at[pl.ds(0, depth // CHIPS), :])
            for d in range(DIRS):
                start(z_parts(1, d))
            round_start(1)
            round_start(3)
        return carry

    lax.fori_loop(0, ff_local // W_TILE, first_half, 0)
    attend_own(0)
    lax.fori_loop(0, 2, second_half, 0)
    attend_past(near_count, my_seq, range(KV_CHUNKS), ((0, 0), (0, 1)))
    finish(0, False)
    finish(1, False)

    def block_work(j, phase):
        @pl.when(phase == 0)
        def _():
            @pl.when(j == 0)
            def _():
                for n in range(3):
                    pl.semaphore_wait(ready_sem.at[n], 1)

            def few(n, inner):
                xs[0, span(n * NORM_ROWS, NORM_ROWS), :] = norm_rows(xbuf[span(j * rows_per + n * NORM_ROWS, NORM_ROWS), :], 1)
                return inner

            lax.fori_loop(0, rows_per // NORM_ROWS, few, 0)
            wait(weights(1, 0))
            keys_values(xs[0], j)
            send_kv(j)
            start(weights(1, 2))

        @pl.when(phase == 1)
        def _():
            wait(weights(1, 1))
            queries(xs[0], j)
            start(weights(1, 3))

        @pl.when(jnp.logical_and(phase >= 1, phase <= 4))
        def _():
            tile = phase - 1
            wait(weights(1, tile + 2))
            gated(xs[0], j, tile)

            @pl.when(tile < 2)
            def _():
                start(weights(1, tile + 4))

            @pl.when(jnp.logical_and(tile == 2, j < KV_CHUNKS - 1))
            def _():
                start(weights(1, 0))

            @pl.when(jnp.logical_and(tile == 3, j < KV_CHUNKS - 1))
            def _():
                start(weights(1, 1))

            @pl.when(j == KV_CHUNKS - 1)
            def _():
                send_hidden(j, tile)

    def tick(t, carry):
        for number in range(STEPS, -1, -1):
            place = t - STAGE_GAP * number
            chunk = place // START_GAP

            @pl.when(jnp.logical_and(place >= 0, jnp.logical_and(place % START_GAP == 0, chunk < CHUNKS)))
            def _():
                stage(number, chunk)

        @pl.when(jnp.logical_or(t == 1, t == 3))
        def _():
            gate_half(1, 2 + t // 2)

        @pl.when(t == OWN_TICK)
        def _():
            attend_own(1)

        @pl.when(jnp.logical_and(t > OWN_TICK, jnp.logical_and(t < DONE_TICK, t - OWN_TICK <= my_seq)))
        def _():
            visit(t - OWN_TICK - 1, ((1, 0), (1, 1)))

        @pl.when(t == EARLY_TICK)
        def _():
            attend_own(0)

        early = t - EARLY_TICK - 1

        @pl.when(jnp.logical_and(early >= 0, jnp.logical_and(early < 7, early < my_seq)))
        def _():
            arrivals(early, (0, 1))
            visit(early, ((0, 0),))

        @pl.when(t == 2)
        def _():
            take(part_recv.at[1], xbuf.at[pl.ds(0, depth // (2 * CHIPS)), :])
            round_start(2)

        @pl.when(t == DONE_TICK)
        def _():
            finish(2, False)
            finish(3, False)
            kv_sent()
            take(cache_sem, kv.at[own_rows, :])
            for n, peer in enumerate((left, right, other)):
                pl.semaphore_signal(ready_sem.at[n], inc=1, device_id={'seq': peer}, device_id_type=mesh_id)

        for when, j in NEAR_TICKS:
            @pl.when(t == when)
            def _():
                near_parts(j)

        for when, j in FAR_TICKS:
            @pl.when(t == when)
            def _():
                far_parts(j)

        @pl.when(t == GIVE_TICK)
        def _():
            for i in range(KV_CHUNKS):
                for z in range(KV_CHUNKS - 1):
                    send_hidden(z, i)

        late = t - BLOCK_TICK

        @pl.when(late >= 0)
        def _():
            block_work(late // BLOCK_GAP, late % BLOCK_GAP)

        for i, when in enumerate(SERVE_TICKS):
            @pl.when(t == when)
            def _():
                serve_all(i)
        return carry

    lax.fori_loop(0, LAST_TICK, tick, 0)

    for slot in range(PART_SLOTS):
        partials_sent(slot)
    for step in range(4, STEPS):
        take(gather_send.at[step - 4], arrived_in(step, CHUNKS))
    for d in range(DIRS):
        pl.semaphore_signal(drained_sem.at[d], inc=1, device_id={'head': y_peer(d)}, device_id_type=mesh_id)
    start(cache_stores(1))
    attend_own(1)
    attend_past(0, my_seq, (), ((1, 0),))
    take(relay_recv, relay_buf)
    for i in range(KV_CHUNKS):
        relay_hidden(i).start()
    attend_past(0, near_count, (2, 3), ((0, 1), (1, 1)))
    attend_past(near_count, my_seq, (2, 3), ((0, 1),))
    finish(0, True)
    finish(1, True)
    attend_past(near_count, my_seq, (), ((1, 1),))
    finish(2, True)
    finish(3, True)
    parts_ref = gd_ref.at[pl.ds(0, 2), pl.ds(0, 3 * depth // 4), :]
    take(side_recv, parts_ref)

    quarter_rows = rows_per // RING

    def block_cols(c):
        return span(c * LAST_COLS, LAST_COLS)

    def tile_place(c, j, first, size):
        return wtile.at[c % 2, j // 2, pl.ds((j % 2) * depth + first, size), :]

    def tile_loads(c):
        copies = []
        for j in range(RING):
            z = wrap(pos_z + j)
            down = wd_ref.at[1, :, block_cols(c)] if j == 0 else gd_ref.at[z, :, block_cols(c)]
            out = wo_ref.at[1, 0, :, block_cols(c)] if j == 0 else go_ref.at[z, :, block_cols(c)]
            copies.append(pltpu.make_async_copy(down, tile_place(c, j, 0, ff_local), tile_sem.at[c % 2]))
            copies.append(pltpu.make_async_copy(out, tile_place(c, j, ff_local, head_dim), tile_sem.at[c % 2]))
        return copies

    start(tile_loads(0))
    given = hid.at[pl.ds(0, (RING - 1) * rows_per * depth // ff_local), :]
    take(give_recv, given)
    for d in range(DIRS):
        pl.semaphore_wait(drained_sem.at[d], 1)

    def quarter_of(piece, offset, size):
        return span(piece * quarter_rows + offset, size, quarter_rows // 2)

    def landed(d, first, size):
        return pl.ds(rows_per + d * (3 * quarter_rows // 2) + first, size)

    def rows_at(z, piece, offset, size):
        return span(z * rows_per + piece * quarter_rows + offset, size, quarter_rows // 2)

    def last_messages(step, c, d, z_first):
        s, cols, half = sign[d], block_cols(c), quarter_rows // 2
        near, behind, back = wrap(pos_y + s), wrap(pos_y - s), wrap(pos_z - s)
        along_y = step < 2 or (step < 4) != z_first
        if step == 0:
            pairs = [(part.at[quarter_of(wrap(pos_y + 2), d * half, half), cols], part.at[landed(d, quarter_rows, half), cols])]
        elif step == 1:
            pairs = [(part.at[quarter_of(near, 0, quarter_rows), cols], part.at[landed(d, 0, quarter_rows), cols])]
        else:
            if step == 2:
                rows = [rows_at(pos_z, pos_y, 0, quarter_rows)]
            elif step == 3:
                rows = [rows_at(back, pos_y, d * half, half) if z_first else rows_at(pos_z, behind, d * half, half)]
            elif step == 4:
                rows = [rows_at(z, pos_y, 0, quarter_rows) for z in range(RING)] if z_first else [rows_at(pos_z, 0, 0, rows_per)]
            else:
                rows = [rows_at(z, behind, d * half, half) for z in range(RING)] if z_first else [rows_at(back, 0, d * (rows_per // 2), rows_per // 2)]
            pairs = [(xbuf.at[r, cols], xbuf.at[r, cols]) for r in rows]
        to = (y_peer if along_y else z_peer)(d)
        return [remote(src, dst, last_send.at[step], last_recv.at[c, step], head=to) for src, dst in pairs]

    def last_arrived(step, cols):
        rows = (quarter_rows, 2 * quarter_rows, 2 * quarter_rows, quarter_rows, 2 * rows_per, rows_per)[step]
        return (part if step < 2 else xbuf).at[pl.ds(0, rows), cols]

    def send_last(step, c):
        def both(z_first):
            for d in range(DIRS):
                start(last_messages(step, c, d, z_first))

        if step < 2:
            both(False)
            return
        z_first = jnp.logical_and(c >= 5, c % 2 == 1)

        @pl.when(z_first)
        def _():
            both(True)

        @pl.when(jnp.logical_not(z_first))
        def _():
            both(False)

    def out_store(c):
        return pltpu.make_async_copy(xbuf.at[:, block_cols(c)], out_ref.at[:, block_cols(c)], store_sem)

    def last_project(c):
        @pl.when(c + 1 < LAST_BLOCKS)
        def _():
            start(tile_loads(c + 1))

        take(tile_sem.at[c % 2], wtile.at[c % 2, :, pl.ds(0, 2 * depth), :])
        total = None
        for j in range(RING):
            z = wrap(pos_z + j)
            own = span(pos_z * rows_per, rows_per)
            hidden_rows = hid[own, :] if j == 0 else xs[1, :, span(z * ff_local, ff_local)]
            out_rows = att[own, :] if j == 0 else att_all[z]
            term = dot(hidden_rows, wtile[c % 2, j // 2, pl.ds((j % 2) * depth, ff_local), :])
            term = term + dot(out_rows, wtile[c % 2, j // 2, pl.ds((j % 2) * depth + ff_local, head_dim), :])
            total = term if total is None else total + term
        part[pl.ds(0, rows_per), block_cols(c)] = total

    def last_stage(number, c):
        cols, half = block_cols(c), quarter_rows // 2
        if number == 0:
            last_project(c)
        else:
            take(last_recv.at[c, number - 1], last_arrived(number - 1, cols))
        if number == 1:
            for d in range(DIRS):
                piece = quarter_of(wrap(pos_y + sign[d]), d * half, half)
                part[piece, cols] = part[piece, cols] + part[landed(d, quarter_rows, half), cols]
        if number == 2:
            own = quarter_of(pos_y, 0, quarter_rows)
            total = part[own, cols] + part[landed(0, 0, quarter_rows), cols] + part[landed(1, 0, quarter_rows), cols]
            update = total.astype(bf16).astype(f32)
            rows = rows_at(pos_z, pos_y, 0, quarter_rows)
            xbuf[rows, cols] = (xbuf[rows, cols].astype(f32) + update).astype(bf16)
        if number < LAST_STEPS:
            send_last(number, c)
        else:
            out_store(c).start()

    def last_tick(t, carry):
        for number in range(LAST_STEPS, -1, -1):
            c = t - LAST_GAP * number

            @pl.when(jnp.logical_and(c >= 0, c < LAST_BLOCKS))
            def _():
                last_stage(number, c)
        return carry

    lax.fori_loop(0, LAST_BLOCKS + LAST_GAP * LAST_STEPS, last_tick, 0)

    take(cache_sem, kv.at[own_rows, :])
    take(relay_send, relay_buf)
    kv_sent()
    take(part_send, xbuf.at[pl.ds(0, 3 * depth // 8), :])
    take(round_send, gd_ref.at[pl.ds(0, 2), pl.ds(0, 9 * depth // 16), :])
    take(side_send, parts_ref)
    take(give_send, given)
    for step in range(LAST_STEPS):
        take(last_send.at[step], last_arrived(step, pl.ds(0, d_model)))
    take(store_sem, xbuf)


def layers(x_loc, cos_t, sin_t, norm_gain, w_q, w_k, w_v, w_gate, w_up, w_down, w_o):
    tok_count, d_model = x_loc.shape
    head_dim = w_q.shape[2]
    ff_local = w_gate.shape[2]
    rows_per = tok_count // KV_CHUNKS
    chunk_rows = tok_count // CHUNKS
    landed = 3 * chunk_rows // (2 * RING)
    half_cols = d_model // HALVES
    any_spec = pl.BlockSpec(memory_space=pl.ANY)
    vmem_spec = pl.BlockSpec(memory_space=pltpu.VMEM)
    bf16, f32 = jnp.bfloat16, jnp.float32
    dma = pltpu.SemaphoreType.DMA
    shape = jax.ShapeDtypeStruct
    return pl.pallas_call(
        layers_kernel,
        out_shape=[shape((tok_count, d_model), bf16)] + [shape((tok_count, head_dim), bf16)] * 4
        + [shape((RING, ff_local, d_model), bf16), shape((RING, head_dim, d_model), bf16)],
        in_specs=[any_spec, any_spec, any_spec, vmem_spec] + [any_spec] * 7,
        out_specs=[any_spec] * 7,
        scratch_shapes=[
            pltpu.VMEM((tok_count, d_model), bf16),
            pltpu.VMEM((PART_SLOTS * chunk_rows, d_model), f32),
            pltpu.VMEM((RECV_SLOTS, HALVES, DIRS, landed, half_cols), f32),
            pltpu.VMEM((RECV_SLOTS, HALVES, DIRS, landed, half_cols // RING), f32),
            pltpu.VMEM((tok_count, ff_local), bf16),
            pltpu.VMEM((tok_count, head_dim), bf16),
            pltpu.VMEM((2, ff_local + head_dim, DOWN_TILE), bf16),
            pltpu.VMEM((2, 2, d_model, W_TILE), bf16),
            pltpu.VMEM((2 * CHIPS * tok_count, 2 * head_dim), bf16),
            pltpu.VMEM((tok_count, head_dim), bf16),
            pltpu.VMEM((2, tok_count, head_dim), f32),
            pltpu.VMEM((2, tok_count, 128), f32),
            pltpu.VMEM((2, tok_count, 128), f32),
            pltpu.VMEM((2, rows_per, d_model), bf16),
            pltpu.VMEM((CHUNKS, HALVES, chunk_rows // RING, half_cols // RING), bf16),
            dma((2,)), dma, dma((2, 2)), dma((2, 2)), dma, dma,
            dma((10,)), dma((4, KV_CHUNKS)), dma((4, KV_CHUNKS)), dma, dma((2,)),
            dma, dma((2, RING - 1)), dma, dma,
            dma, dma,
            pltpu.VMEM((KV_CHUNKS, rows_per, W_TILE), bf16), dma, dma,
            pltpu.VMEM((RING, rows_per, head_dim), bf16),
            dma((PART_SLOTS,)), dma((4,)), dma((RECV_SLOTS, STEPS)),
            dma((LAST_STEPS,)), dma((LAST_BLOCKS, LAST_STEPS)), dma((2,)),
            pltpu.VMEM((tok_count, head_dim // 2), f32), pltpu.VMEM((tok_count, head_dim // 2), f32), dma((2,)),
            pltpu.SemaphoreType.REGULAR((3,)), pltpu.SemaphoreType.REGULAR((DIRS,)),
        ],
        compiler_params=pltpu.CompilerParams(collective_id=0, has_side_effects=True, vmem_limit_bytes=67043328),
        name='layers',
    )(x_loc, cos_t, sin_t, norm_gain, w_q, w_k, w_v, w_gate, w_up, w_down, w_o)


EMIT_PARTS = 8


def emit_kernel(x_ref, k_first, k_second, v_first, v_second, x_out, k_out, v_out, xbuf, rows, load_sem, store_sem):
    size = x_ref.shape[0] // EMIT_PARTS
    loads, stores = [], []
    for n in range(EMIT_PARTS):
        part = pl.ds(n * size, size)
        loads.append(pltpu.make_async_copy(x_ref.at[part, :], xbuf.at[part, :], load_sem.at[n]))
        stores.append(pltpu.make_async_copy(xbuf.at[part, :], x_out.at[part, :], store_sem.at[n]))
    for n, (ref, out) in enumerate(((k_first, k_out.at[0]), (k_second, k_out.at[1]), (v_first, v_out.at[0]), (v_second, v_out.at[1]))):
        loads.append(pltpu.make_async_copy(ref, rows.at[n], load_sem.at[EMIT_PARTS + n]))
        stores.append(pltpu.make_async_copy(rows.at[n], out, store_sem.at[EMIT_PARTS + n]))
    for copy in loads:
        copy.start()
    for load, store in zip(loads, stores):
        load.wait()
        store.start()
    for copy in stores:
        copy.wait()


def emit(x_out, k_first, k_second, v_first, v_second):
    any_spec = pl.BlockSpec(memory_space=pl.ANY)
    cache = jax.ShapeDtypeStruct((2,) + k_first.shape, jnp.bfloat16)
    return pl.pallas_call(
        emit_kernel,
        out_shape=[jax.ShapeDtypeStruct(x_out.shape, jnp.bfloat16), cache, cache],
        in_specs=[any_spec] * 5,
        out_specs=[any_spec] * 3,
        scratch_shapes=[
            pltpu.VMEM(x_out.shape, jnp.bfloat16),
            pltpu.VMEM((4,) + k_first.shape, jnp.bfloat16),
            pltpu.SemaphoreType.DMA((EMIT_PARTS + 4,)),
            pltpu.SemaphoreType.DMA((EMIT_PARTS + 4,)),
        ],
        compiler_params=pltpu.CompilerParams(vmem_limit_bytes=63 * 1024 * 1024),
        name='emit',
    )(x_out, k_first, k_second, v_first, v_second)


def solution(mesh):
    row_spec = P(('batch', 'seq'), None)
    pos_spec = P(('batch', 'seq'))
    head_spec = P(None, None, 'head', None)
    out_proj_spec = P(None, 'head', None, None)
    col_spec = P(None, None, 'head')
    down_spec = P(None, 'head', None)
    cache_spec = P(None, ('batch', 'seq'), 'head', None)

    def local_forward(x_loc, pos_loc, w_q, w_k, w_v, w_o, w_gate, w_up, w_down, norm_gain):
        tok_count, d_model = x_loc.shape
        layer_count = w_q.shape[0]
        head_dim = w_q.shape[3]
        flat_q, flat_k, flat_v = (w.reshape(layer_count, d_model, head_dim) for w in (w_q, w_k, w_v))
        cos_t, sin_t = rope_tables(pos_loc, head_dim)
        x_out, k_first, v_first, k_second, v_second, _, _ = layers(x_loc, cos_t, sin_t, norm_gain, flat_q, flat_k, flat_v, w_gate, w_up, w_down, w_o)
        x_out, k_all, v_all = emit(x_out, k_first, k_second, v_first, v_second)
        cache_shape = (layer_count, tok_count, 1, head_dim)
        return x_out, k_all.reshape(cache_shape), v_all.reshape(cache_shape)

    return jax.shard_map(local_forward, mesh=mesh, in_specs=(row_spec, pos_spec, head_spec, head_spec, head_spec, out_proj_spec, col_spec, col_spec, down_spec, P(None, None)), out_specs=(row_spec, cache_spec, cache_spec), check_vma=False)
```

```python
import functools
import math
import jax
import jax.numpy as jnp
from jax import lax
from jax.experimental import pallas as pl
from jax.experimental.pallas import tpu as pltpu
from jax.sharding import PartitionSpec as P

ROPE_BASE = 500000.0
EPS = 1e-5


def rope_tables(positions, head_dim):
    half_dim = head_dim // 2
    inv_freq = ROPE_BASE ** (-(jnp.arange(half_dim, dtype=jnp.float32) * 2.0 / head_dim))
    angles = positions.astype(jnp.float32)[..., None] * inv_freq
    return jnp.cos(angles), jnp.sin(angles)


CHIPS = 4
RING = 4
HALVES = 2
DIRS = 2
KV_CHUNKS = 4
W_TILE = 256
NORM_ROWS = 64
CHUNKS = 8
STEPS = 8
PART_SLOTS = 4
RECV_SLOTS = 5
DOWN_TILE = 512
START_GAP = 3
STAGE_GAP = 2
BLOCK_TICK = 19
BLOCK_GAP = 6
LAST_TICK = 43
NEAR_TICKS = ((9, 1), (15, 3), (20, 2))
FAR_TICKS = ((24, 1), (26, 3), (36, 2))
SERVE_TICKS = (27, 31, 36, 42)
GIVE_TICK = 37
OWN_TICK = 3
DONE_TICK = 11
EARLY_TICK = 31
LAST_STEPS = 6
LAST_COLS = 256
LAST_BLOCKS = 16
LAST_GAP = 3


def layers_kernel(x_ref, cos_ref, sin_ref, gain_ref, wq_ref, wk_ref, wv_ref, wg_ref, wu_ref, wd_ref, wo_ref,
                 out_ref, k1_ref, v1_ref, k2_ref, v2_ref, gd_ref, go_ref,
                 xbuf, part, recv_a, recv_b, hid, att, wdo, wtile, kv, qbuf, acc, row_max, row_sum, xs, xres,
                 x_sem, res_sem, w_sem, down_sem, cache_sem, store_sem, kv_send, ici_recv, core_recv, part_send, part_recv,
                 round_send, round_recv, side_send, side_recv, give_send, give_recv, relay_buf, relay_send, relay_recv, att_all, ring_send, gather_send, ring_recv,
                 last_send, last_recv, tile_sem, cos_buf, sin_buf, rope_sem, ready_sem, drained_sem):
    tok_count, d_model = xbuf.shape
    head_dim = qbuf.shape[1]
    half_dim = head_dim // 2
    ff_local = hid.shape[1]
    depth = ff_local + head_dim
    rows_per = tok_count // KV_CHUNKS
    half_rows = tok_count // 2
    lanes = row_max.shape[2]
    chunk_rows = tok_count // CHUNKS
    quarter, eighth = chunk_rows // RING, chunk_rows // (2 * RING)
    half_cols = d_model // HALVES
    piece_cols = half_cols // RING
    bf16, f32 = jnp.bfloat16, jnp.float32
    sign = (1, -1)
    mesh_id = pl.DeviceIdType.MESH

    my_head = lax.axis_index('head')
    pos_z, pos_y = my_head // RING, my_head % RING
    my_seq = lax.axis_index('seq')
    chip, core = my_seq // 2, my_seq % 2
    other = chip * 2 + 1 - core

    def wrap(n):
        return (n + RING) % RING

    def y_peer(d):
        return pos_z * RING + wrap(pos_y + sign[d])

    def z_device(z):
        return wrap(z) * RING + pos_y

    def z_peer(d):
        return z_device(pos_z + sign[d])

    def x_device(n):
        return wrap(chip + n) * 2 + core

    right, left = x_device(1), x_device(-1)

    def span(start, size, unit=None):
        return pl.ds(pl.multiple_of(start, unit or size), size)

    def remote(src, dst, send, recv, **to):
        return pltpu.make_async_remote_copy(src_ref=src, dst_ref=dst, send_sem=send, recv_sem=recv, device_id=to, device_id_type=mesh_id)

    def take(sem, ref):
        remote(ref, ref, sem, sem, head=my_head).wait_recv()

    def x_load(i):
        return pltpu.make_async_copy(x_ref.at[span(i * rows_per, rows_per), :], xs.at[i % 2], x_sem.at[i % 2])

    def weights(layer, piece):
        slot = piece % 2
        if isinstance(piece, int) and piece < 2:
            refs = ((wk_ref, wv_ref), (wq_ref,))[piece]
            return [pltpu.make_async_copy(ref.at[layer], wtile.at[slot, n], w_sem.at[slot, n]) for n, ref in enumerate(refs)]
        cols = span((piece - 2) * W_TILE, W_TILE)
        return [pltpu.make_async_copy(ref.at[layer, :, cols], wtile.at[slot, n], w_sem.at[slot, n]) for n, ref in enumerate((wg_ref, wu_ref))]

    def start(copies):
        for copy in copies:
            copy.start()

    def wait(copies):
        for copy in copies:
            copy.wait()

    down_tiles = d_model // DOWN_TILE

    def down_load(i):
        cols = span(i * DOWN_TILE, DOWN_TILE)
        return [pltpu.make_async_copy(wd_ref.at[0, :, cols], wdo.at[i % 2, pl.ds(0, ff_local), :], down_sem.at[i % 2, 0]),
                pltpu.make_async_copy(wo_ref.at[0, 0, :, cols], wdo.at[i % 2, pl.ds(ff_local, head_dim), :], down_sem.at[i % 2, 1])]

    def kv_copy(origin_chip, origin_core, i, to, send, recv):
        rows = kv.at[span((origin_chip * 2 + origin_core) * tok_count + i * rows_per, rows_per), :]
        return remote(rows, rows, send, recv, seq=to)

    def kv_routes(i):
        def to(number, recv, origin_chip, origin_core, device):
            return lambda: kv_copy(origin_chip, origin_core, i, device, kv_send.at[number], recv)
        inner = jnp.logical_and(chip >= 1, chip < CHIPS - 1)
        return {
            'right': (chip < CHIPS - 1, 'all', to(0, ici_recv.at[0, i], chip, core, right)),
            'wrap': (chip == 0, 'all', to(1, ici_recv.at[2, i], chip, core, left)),
            'relay': (chip == 1, 'late', to(2, ici_recv.at[3, i], chip, core, left)),
            'other': (core == 0, 'all', to(3, core_recv.at[0, i], chip, core, other)),
            'on_right': (inner, 'early', to(4, ici_recv.at[1, i], chip - 1, core, right)),
            'from_relay': (chip == 0, 'late', to(5, ici_recv.at[1, i], 1, core, left)),
            'on_left': (chip == CHIPS - 1, 'late', to(6, ici_recv.at[1, i], 0, core, left)),
            'side1': (chip >= 1, 'all', to(7, core_recv.at[1, i], chip - 1, core, other)),
            'side2': (chip >= 2, 'all', to(8, core_recv.at[2, i], chip - 2, core, other)),
            'side3': (chip >= 3, 'all', to(9, core_recv.at[3, i], chip - 3, core, other)),
        }

    def start_route(i, name):
        condition, which, copy = kv_routes(i)[name]
        if which != 'all':
            late = i >= KV_CHUNKS // 2
            if isinstance(i, int):
                if late != (which == 'late'):
                    return
            else:
                condition = jnp.logical_and(condition, late if which == 'late' else jnp.logical_not(late))

        @pl.when(condition)
        def _():
            copy().start()

    def send_kv(i):
        for name in ('right', 'wrap', 'relay', 'other'):
            start_route(i, name)

    def kv_sent():
        for number, (condition, which, _) in enumerate(kv_routes(0).values()):
            @pl.when(condition)
            def _():
                take(kv_send.at[number], kv.at[pl.ds(0, tok_count if which == 'all' else half_rows), :])

    def serve(back, i):
        @pl.when(chip >= back)
        def _():
            kv_copy(chip - back, core, i, other, kv_send.at[0], ici_recv.at[back - 1, i]).wait_recv()
        start_route(i, 'side%d' % back)
        if back == 1:
            start_route(i, 'on_right')
        if back == 3:
            start_route(i, 'on_left')

    def relay(i):
        def pass_on():
            @pl.when(chip == 0)
            def _():
                kv_copy(1, core, i, left, kv_send.at[0], ici_recv.at[3, i]).wait_recv()
            start_route(i, 'from_relay')
        if not isinstance(i, int):
            pl.when(i >= KV_CHUNKS // 2)(pass_on)
        elif i >= KV_CHUNKS // 2:
            pass_on()

    def serve_all(i):
        serve(1, i)
        serve(3, i)
        relay(i)

    def taken(back, chunks):
        for i in chunks:
            kv_copy(chip - back, 1 - core, i, other, kv_send.at[0], core_recv.at[back, i]).wait_recv()

    def z_parts(step, d):
        copies = []
        for n, (own_ref, all_ref) in enumerate(((wd_ref, gd_ref), (wo_ref, go_ref))):
            size = all_ref.shape[1] // (2 * CHIPS)
            if step == 0:
                rows = span(my_seq * size, size)
                src = own_ref.at[1, rows, :] if n == 0 else own_ref.at[1, 0, rows, :]
                dst = all_ref.at[pos_z, rows, :]
            else:
                rows = span(my_seq * size + d * (size // 2), size // 2)
                src = dst = all_ref.at[wrap(pos_z - sign[d]), rows, :]
            copies.append(remote(src, dst, part_send, part_recv.at[step], head=z_peer(d)))
        return copies

    def part_copies(j, part_chip, part_core, half, send, recv, to):
        copies = []
        for n, ref in enumerate((gd_ref, go_ref)):
            size = ref.shape[1] // (2 * CHIPS)
            first = (part_chip * 2 + part_core) * size
            rows = span(first, size) if half is None else span(first + half * (size // 2), size // 2)
            place = ref.at[wrap(pos_z + j), rows, :]
            copies.append(remote(place, place, send, recv, seq=to))
        return copies

    def own_part(j, d):
        return part_copies(j, chip, core, None, round_send, round_recv.at[0, j - 1], x_device(sign[d]))

    def far_part(j, d):
        return part_copies(j, wrap(chip - sign[d]), core, d, round_send, round_recv.at[1, j - 1], x_device(sign[d]))

    def side_part(j, n, side):
        return part_copies(j, wrap(chip + n), side, None, side_send, side_recv, other)

    def round_start(j):
        for d in range(DIRS):
            start(own_part(j, d))
        start(side_part(j, 0, core))

    def near_parts(j):
        take(round_recv.at[0, j - 1], xbuf.at[pl.ds(0, depth // CHIPS), :])
        for d in range(DIRS):
            start(far_part(j, d) + side_part(j, 3 if d == 0 else 1, core))

    def far_parts(j):
        take(round_recv.at[1, j - 1], xbuf.at[pl.ds(0, depth // (2 * CHIPS)), :])
        start(side_part(j, 2, core))

    def give_hidden(z, i, source):
        cols = span(i * W_TILE, W_TILE)
        return remote(hid.at[span(z * rows_per, rows_per), cols], hidden_place(source, i), give_send, give_recv, head=z_device(z))

    def hidden_place(source, i):
        return xs.at[1, :, span(source * ff_local + i * W_TILE, W_TILE)]

    def via_neighbor(z, i):
        step = jnp.where(i < KV_CHUNKS // 2, 1, -1)
        return remote(hid.at[span(z * rows_per, rows_per), span(i * W_TILE, W_TILE)], relay_buf.at[i], give_send, relay_recv, head=z_device(pos_z + step))

    def relay_hidden(i):
        step = 1 if i < KV_CHUNKS // 2 else -1
        source = wrap(pos_z - step)
        return remote(relay_buf.at[i], hidden_place(source, i), relay_send, give_recv, head=z_device(pos_z + step))

    def send_hidden(z, i):
        away = wrap(z - pos_z)

        @pl.when(away == 2)
        def _():
            via_neighbor(z, i).start()

        @pl.when(away % 2 == 1)
        def _():
            give_hidden(z, i, pos_z).start()

    def give_rows(z, source):
        return remote(att.at[span(z * rows_per, rows_per), :], att_all.at[source], give_send, give_recv, head=z_device(z))

    def norm_rows(x_few, layer):
        x_f32 = x_few.astype(f32)
        inv_rms = lax.rsqrt(jnp.mean(x_f32 * x_f32, axis=-1, keepdims=True) + EPS)
        return (x_f32 * inv_rms * gain_ref[pl.ds(layer, 1), :].astype(f32)).astype(bf16)

    def rope(values, rows):
        cos_t, sin_t = cos_buf[rows, :], sin_buf[rows, :]
        wide = values.astype(bf16).astype(f32)
        first, second = wide[:, :half_dim], wide[:, half_dim:]
        return jnp.concatenate([first * cos_t - second * sin_t, second * cos_t + first * sin_t], axis=1).astype(bf16)

    def dot(a, b):
        return jnp.dot(a, b, preferred_element_type=f32)

    scale = 1.0 / math.sqrt(head_dim)

    def keys_values(normed, i):
        rows = span(i * rows_per, rows_per)
        own = span(my_seq * tok_count + i * rows_per, rows_per)
        kv[own, :head_dim] = rope(dot(normed, wtile[0, 0]), rows)
        kv[own, head_dim:] = dot(normed, wtile[0, 1]).astype(bf16)

    def queries(normed, i):
        rows = span(i * rows_per, rows_per)
        qbuf[rows, :] = (rope(dot(normed, wtile[1, 0]), rows).astype(f32) * scale).astype(bf16)

    def gated(normed, i, tile):
        gate = dot(normed, wtile[tile % 2, 0])
        up = dot(normed, wtile[tile % 2, 1])
        hid[span(i * rows_per, rows_per), span(tile * W_TILE, W_TILE)] = (gate * jax.nn.sigmoid(gate) * up).astype(bf16)

    def attend(key_start, q_half, side, masked, first):
        rows = pl.ds(q_half * half_rows, half_rows)
        some = span(key_start, half_rows)
        logits = lax.dot_general(qbuf[rows, :], kv[some, :head_dim], (((1,), (1,)), ((), ())), preferred_element_type=f32)
        if masked:
            seen = lax.broadcasted_iota(jnp.int32, logits.shape, 0) >= lax.broadcasted_iota(jnp.int32, logits.shape, 1)
            logits = jnp.where(seen, logits, -jnp.inf)
        block_max = jnp.max(logits, axis=-1, keepdims=True)
        if first:
            new_max = jnp.broadcast_to(block_max, (half_rows, lanes))
        else:
            new_max = jnp.maximum(row_max[side, rows, :], block_max)
        prob = jnp.exp(logits - jnp.concatenate([new_max] * (half_rows // lanes), axis=1))
        block_sum = jnp.sum(prob, axis=-1, keepdims=True)
        block_out = dot(prob.astype(bf16), kv[some, head_dim:])
        if first:
            row_sum[side, rows, :] = jnp.broadcast_to(block_sum, (half_rows, lanes))
            acc[side, rows, :] = block_out
        else:
            rescale = jnp.exp(row_max[side, rows, :] - new_max)
            row_sum[side, rows, :] = row_sum[side, rows, :] * rescale + block_sum
            acc[side, rows, :] = acc[side, rows, :] * jnp.concatenate([rescale] * (head_dim // lanes), axis=1) + block_out
        row_max[side, rows, :] = new_max

    def attend_own(layer_half):
        own_start = my_seq * tok_count
        if layer_half == 0:
            attend(own_start, 0, 0, True, True)
            top_rows = pl.ds(0, half_rows)
            row_max[1, top_rows, :] = jnp.full((half_rows, lanes), -jnp.inf, f32)
            row_sum[1, top_rows, :] = jnp.zeros((half_rows, lanes), f32)
            acc[1, top_rows, :] = jnp.zeros((half_rows, head_dim), f32)
        else:
            attend(own_start, 1, 0, False, True)
            attend(own_start + half_rows, 1, 1, True, True)

    def past_start(n):
        later = n - core
        back = jnp.where(later < 2, 1, jnp.where(chip == CHIPS - 1, jnp.where(later < 4, 3, 2), 2))
        block = (chip - back) * 2 + jnp.where(later % 2 == 0, core, 1 - core)
        return jnp.where(jnp.logical_and(core == 1, n == 0), chip * 2, block) * tok_count

    def arrivals(n, chunks):
        @pl.when(jnp.logical_and(core == 1, n == 0))
        def _():
            taken(0, chunks)

        for back in (1, 3, 2):
            place = 0 if back == 1 else 2 if back == 3 else jnp.where(chip == CHIPS - 1, 4, 2)
            if back == 2:
                @pl.when(jnp.logical_and(chip >= back, n == core + place))
                def _():
                    for i in chunks:
                        serve(2, i)

            @pl.when(jnp.logical_and(chip >= back, n == core + place + 1))
            def _():
                taken(back, chunks)

    def visit(n, visits):
        for q_half, side in visits:
            attend(past_start(n) + side * half_rows, q_half, side, False, False)

    def attend_past(first_n, last_n, chunks, visits):
        def past(n, count):
            for r in range(count if chunks else 0):
                arrivals(n + r, chunks)
            for r in range(count):
                visit(n + r, visits)

        def two(p, carry):
            past(first_n + 2 * p, 2)
            return carry

        count = last_n - first_n
        lax.fori_loop(0, count // 2, two, 0)

        @pl.when(count % 2 == 1)
        def _():
            past(last_n - 1, 1)

    near_count = my_seq - jnp.where(chip >= 2, 2, 0)

    def finish(i, spread):
        rows = pl.ds(i * rows_per, rows_per)
        top = jnp.maximum(row_max[0, rows, :], row_max[1, rows, :])
        shares = [jnp.exp(row_max[side, rows, :] - top) for side in range(2)]
        total = shares[0] * row_sum[0, rows, :] + shares[1] * row_sum[1, rows, :]
        wide = [jnp.concatenate([w] * (head_dim // lanes), axis=1) for w in shares + [total]]
        att[rows, :] = ((acc[0, rows, :] * wide[0] + acc[1, rows, :] * wide[1]) / wide[2]).astype(bf16)
        if spread:
            @pl.when(i != pos_z)
            def _():
                give_rows(i, pos_z).start()

    first_pos, second_pos = (pos_y, pos_z), (pos_z, pos_y)
    first_peer, second_peer = (y_peer, z_peer), (z_peer, y_peer)

    def part_rows(chunk, piece, offset, count):
        return span((chunk % PART_SLOTS) * chunk_rows + piece * quarter + offset, count, eighth)

    def x_rows(chunk, piece, offset, count):
        return span(chunk * chunk_rows + piece * quarter + offset, count, eighth)

    def cols_of(h, piece):
        return span(h * half_cols + piece * piece_cols, piece_cols)

    def half_of(h):
        return pl.ds(h * half_cols, half_cols)

    def message(step, chunk, h, d):
        p1, p2, s = first_pos[h], second_pos[h], sign[d]
        slot = chunk % RECV_SLOTS
        if step == 0:
            src, dst = part.at[part_rows(chunk, wrap(p1 + 2), d * eighth, eighth), half_of(h)], recv_a.at[slot, h, d, pl.ds(quarter, eighth), :]
        elif step == 1:
            src, dst = part.at[part_rows(chunk, wrap(p1 + s), 0, quarter), half_of(h)], recv_a.at[slot, h, d, pl.ds(0, quarter), :]
        elif step == 2:
            src, dst = part.at[part_rows(chunk, p1, d * eighth, eighth), cols_of(h, wrap(p2 + 2))], recv_b.at[slot, h, d, pl.ds(quarter, eighth), :]
        elif step == 3:
            src, dst = part.at[part_rows(chunk, p1, 0, quarter), cols_of(h, wrap(p2 + s))], recv_b.at[slot, h, d, pl.ds(0, quarter), :]
        elif step == 4:
            src = dst = xbuf.at[x_rows(chunk, p1, 0, quarter), cols_of(h, p2)]
        elif step == 5:
            src = dst = xbuf.at[x_rows(chunk, p1, d * eighth, eighth), cols_of(h, wrap(p2 - s))]
        elif step == 6:
            src = dst = xbuf.at[x_rows(chunk, p1, 0, quarter), half_of(h)]
        else:
            src = dst = xbuf.at[x_rows(chunk, wrap(p1 - s), d * eighth, eighth), half_of(h)]
        peer = (first_peer if step in (0, 1, 6, 7) else second_peer)[h](d)
        return remote(src, dst, ring_send.at[chunk % PART_SLOTS] if step < 4 else gather_send.at[step - 4], ring_recv.at[slot, step], head=peer)

    def arrived_in(step, count=1):
        rows = (2 * eighth, 2 * quarter, eighth // 2, quarter // 2, quarter // 2, quarter // 2, 2 * quarter, quarter)[step] * count
        return (part if step < 4 else xbuf).at[pl.ds(0, rows), pl.ds(0, half_cols if step == 5 else d_model)]

    def partials_sent(slot):
        take(ring_send.at[slot], part.at[pl.ds(0, 2 * eighth + 2 * quarter + eighth // 2 + quarter // 2), :])

    def residual_load(chunk, h):
        return pltpu.make_async_copy(x_ref.at[x_rows(chunk, first_pos[h], 0, quarter), cols_of(h, second_pos[h])], xres.at[chunk, h], res_sem)

    def project(chunk, h):
        rows = span(chunk * chunk_rows, chunk_rows)
        slot_rows = span((chunk % PART_SLOTS) * chunk_rows, chunk_rows)

        def one_tile(i, carry):
            @pl.when(jnp.logical_or(chunk < CHUNKS - 1, i < down_tiles - 1))
            def _():
                start(down_load((i + 1) % down_tiles))

            wait(down_load(i))
            total = dot(hid[rows, :], wdo[i % 2, :ff_local, :])
            part[slot_rows, span(i * DOWN_TILE, DOWN_TILE)] = total + dot(att[rows, :], wdo[i % 2, ff_local:, :])
            return carry

        per_half = down_tiles // HALVES
        lax.fori_loop(h * per_half, (h + 1) * per_half, one_tile, 0)

    def stage(number, chunk):
        slot = chunk % RECV_SLOTS
        if number == 0:
            @pl.when(chunk >= PART_SLOTS)
            def _():
                partials_sent(chunk % PART_SLOTS)
        else:
            take(ring_recv.at[slot, number - 1], arrived_in(number - 1))
        if number == 4:
            @pl.when(chunk == 0)
            def _():
                take(res_sem, xres)
        for h in range(HALVES):
            p1, p2 = first_pos[h], second_pos[h]
            if number == 0:
                project(chunk, h)
            if number in (1, 3):
                for d in range(DIRS):
                    if number == 1:
                        rows, cols, arrived = part_rows(chunk, wrap(p1 + sign[d]), d * eighth, eighth), half_of(h), recv_a
                    else:
                        rows, cols, arrived = part_rows(chunk, p1, d * eighth, eighth), cols_of(h, wrap(p2 + sign[d])), recv_b
                    part[rows, cols] = part[rows, cols] + arrived[slot, h, d, pl.ds(quarter, eighth), :]
            if number == 2:
                rows = part_rows(chunk, p1, 0, quarter)
                part[rows, half_of(h)] = part[rows, half_of(h)] + recv_a[slot, h, 0, pl.ds(0, quarter), :] + recv_a[slot, h, 1, pl.ds(0, quarter), :]
            if number == 4:
                rows, cols = part_rows(chunk, p1, 0, quarter), cols_of(h, p2)
                total = part[rows, cols] + recv_b[slot, h, 0, pl.ds(0, quarter), :] + recv_b[slot, h, 1, pl.ds(0, quarter), :]
                update = total.astype(bf16).astype(f32)
                xbuf[x_rows(chunk, p1, 0, quarter), cols] = (xres[chunk, h].astype(f32) + update).astype(bf16)
            if number < STEPS:
                for d in range(DIRS):
                    message(number, chunk, h, d).start()

    rope_loads = [pltpu.make_async_copy(ref, buf, rope_sem.at[n]) for n, (ref, buf) in enumerate(((cos_ref, cos_buf), (sin_ref, sin_buf)))]
    x_load(0).start()
    start(weights(0, 0))
    start(rope_loads)
    barrier = pltpu.get_barrier_semaphore()
    for peer in (left, right, other):
        pl.semaphore_signal(barrier, inc=1, device_id={'seq': peer}, device_id_type=mesh_id)
    for peer in [z_device(pos_z + j) for j in range(1, RING)] + [y_peer(d) for d in range(DIRS)]:
        pl.semaphore_signal(barrier, inc=1, device_id={'head': peer}, device_id_type=mesh_id)

    def prepare(i, carry):
        x_load(i).wait()

        @pl.when(i == 0)
        def _():
            x_load(1).start()
            start(weights(0, 1))

        def few(n, inner):
            xbuf[span(i * rows_per + n * NORM_ROWS, NORM_ROWS), :] = norm_rows(xs[i % 2, span(n * NORM_ROWS, NORM_ROWS), :], 0)
            return inner

        lax.fori_loop(0, rows_per // NORM_ROWS, few, 0)

        @pl.when(i + 2 < KV_CHUNKS)
        def _():
            x_load(i + 2).start()

        @pl.when(i == 0)
        def _():
            wait(weights(0, 0))
            wait(rope_loads)

        keys_values(xbuf[span(i * rows_per, rows_per), :], i)

        @pl.when(i == 0)
        def _():
            pl.semaphore_wait(barrier, 8)

        send_kv(i)

        @pl.when(i == 0)
        def _():
            for d in range(DIRS):
                start(z_parts(0, d))
        return carry

    lax.fori_loop(0, KV_CHUNKS, prepare, 0)
    start(weights(0, 2))
    own_rows = span(my_seq * tok_count, tok_count)

    def cache_stores(layer):
        k_ref, v_ref = ((k1_ref, v1_ref), (k2_ref, v2_ref))[layer]
        return [pltpu.make_async_copy(kv.at[own_rows, pl.ds(0, head_dim)], k_ref, cache_sem),
                pltpu.make_async_copy(kv.at[own_rows, pl.ds(head_dim, head_dim)], v_ref, cache_sem)]

    start(cache_stores(0))
    wait(weights(0, 1))

    def query(i, carry):
        queries(xbuf[span(i * rows_per, rows_per), :], i)
        return carry

    lax.fori_loop(0, KV_CHUNKS, query, 0)
    start(weights(0, 3))
    start(down_load(0))

    def residuals(n, carry):
        for h in range(HALVES):
            residual_load(n, h).start()
        return carry

    lax.fori_loop(0, CHUNKS, residuals, 0)

    def gate_half(half, tile):
        wait(weights(0, tile + 2))

        def rows_step(i, inner):
            gated(xbuf[span(i * rows_per, rows_per), :], i, tile)
            return inner

        lax.fori_loop(half * KV_CHUNKS // 2, (half + 1) * KV_CHUNKS // 2, rows_step, 0)

        @pl.when(tile < 2)
        def _():
            start(weights(0, tile + 4))

        for last in (2, 3):
            @pl.when(tile == last)
            def _():
                start(weights(1, last - 2) if half else weights(0, last))

    def first_half(tile, carry):
        gate_half(0, tile)

        @pl.when(tile < 3)
        def _():
            serve_all(tile)
        return carry

    def second_half(tile, carry):
        gate_half(1, tile)

        @pl.when(tile == 0)
        def _():
            serve_all(3)
            attend_past(0, near_count, range(KV_CHUNKS), ((0, 0), (0, 1)))
            take(part_recv.at[0], xbuf.at[pl.ds(0, depth // CHIPS), :])
            for d in range(DIRS):
                start(z_parts(1, d))
            round_start(1)
            round_start(3)
        return carry

    lax.fori_loop(0, ff_local // W_TILE, first_half, 0)
    attend_own(0)
    lax.fori_loop(0, 2, second_half, 0)
    attend_past(near_count, my_seq, range(KV_CHUNKS), ((0, 0), (0, 1)))
    finish(0, False)
    finish(1, False)

    def block_work(j, phase):
        @pl.when(phase == 0)
        def _():
            @pl.when(j == 0)
            def _():
                for n in range(3):
                    pl.semaphore_wait(ready_sem.at[n], 1)

            def few(n, inner):
                xs[0, span(n * NORM_ROWS, NORM_ROWS), :] = norm_rows(xbuf[span(j * rows_per + n * NORM_ROWS, NORM_ROWS), :], 1)
                return inner

            lax.fori_loop(0, rows_per // NORM_ROWS, few, 0)
            wait(weights(1, 0))
            keys_values(xs[0], j)
            send_kv(j)
            start(weights(1, 2))

        @pl.when(phase == 1)
        def _():
            wait(weights(1, 1))
            queries(xs[0], j)
            start(weights(1, 3))

        @pl.when(jnp.logical_and(phase >= 1, phase <= 4))
        def _():
            tile = phase - 1
            wait(weights(1, tile + 2))
            gated(xs[0], j, tile)

            @pl.when(tile < 2)
            def _():
                start(weights(1, tile + 4))

            @pl.when(jnp.logical_and(tile == 2, j < KV_CHUNKS - 1))
            def _():
                start(weights(1, 0))

            @pl.when(jnp.logical_and(tile == 3, j < KV_CHUNKS - 1))
            def _():
                start(weights(1, 1))

            @pl.when(j == KV_CHUNKS - 1)
            def _():
                send_hidden(j, tile)

    def tick(t, carry):
        for number in range(STEPS, -1, -1):
            place = t - STAGE_GAP * number
            chunk = place // START_GAP

            @pl.when(jnp.logical_and(place >= 0, jnp.logical_and(place % START_GAP == 0, chunk < CHUNKS)))
            def _():
                stage(number, chunk)

        @pl.when(jnp.logical_or(t == 1, t == 3))
        def _():
            gate_half(1, 2 + t // 2)

        @pl.when(t == OWN_TICK)
        def _():
            attend_own(1)

        @pl.when(jnp.logical_and(t > OWN_TICK, jnp.logical_and(t < DONE_TICK, t - OWN_TICK <= my_seq)))
        def _():
            visit(t - OWN_TICK - 1, ((1, 0), (1, 1)))

        @pl.when(t == EARLY_TICK)
        def _():
            attend_own(0)

        early = t - EARLY_TICK - 1

        @pl.when(jnp.logical_and(early >= 0, jnp.logical_and(early < 7, early < my_seq)))
        def _():
            arrivals(early, (0, 1))
            visit(early, ((0, 0),))

        @pl.when(t == 2)
        def _():
            take(part_recv.at[1], xbuf.at[pl.ds(0, depth // (2 * CHIPS)), :])
            round_start(2)

        @pl.when(t == DONE_TICK)
        def _():
            finish(2, False)
            finish(3, False)
            kv_sent()
            take(cache_sem, kv.at[own_rows, :])
            for n, peer in enumerate((left, right, other)):
                pl.semaphore_signal(ready_sem.at[n], inc=1, device_id={'seq': peer}, device_id_type=mesh_id)

        for when, j in NEAR_TICKS:
            @pl.when(t == when)
            def _():
                near_parts(j)

        for when, j in FAR_TICKS:
            @pl.when(t == when)
            def _():
                far_parts(j)

        @pl.when(t == GIVE_TICK)
        def _():
            for i in range(KV_CHUNKS):
                for z in range(KV_CHUNKS - 1):
                    send_hidden(z, i)

        late = t - BLOCK_TICK

        @pl.when(late >= 0)
        def _():
            block_work(late // BLOCK_GAP, late % BLOCK_GAP)

        for i, when in enumerate(SERVE_TICKS):
            @pl.when(t == when)
            def _():
                serve_all(i)
        return carry

    lax.fori_loop(0, LAST_TICK, tick, 0)

    for slot in range(PART_SLOTS):
        partials_sent(slot)
    for step in range(4, STEPS):
        take(gather_send.at[step - 4], arrived_in(step, CHUNKS))
    for d in range(DIRS):
        pl.semaphore_signal(drained_sem.at[d], inc=1, device_id={'head': y_peer(d)}, device_id_type=mesh_id)
    start(cache_stores(1))
    attend_own(1)
    attend_past(0, my_seq, (), ((1, 0),))
    take(relay_recv, relay_buf)
    for i in range(KV_CHUNKS):
        relay_hidden(i).start()
    attend_past(0, near_count, (2, 3), ((0, 1), (1, 1)))
    attend_past(near_count, my_seq, (2, 3), ((0, 1),))
    finish(0, True)
    finish(1, True)
    attend_past(near_count, my_seq, (), ((1, 1),))
    finish(2, True)
    finish(3, True)
    parts_ref = gd_ref.at[pl.ds(0, 2), pl.ds(0, 3 * depth // 4), :]
    take(side_recv, parts_ref)

    quarter_rows = rows_per // RING

    def block_cols(c):
        return span(c * LAST_COLS, LAST_COLS)

    def tile_place(c, j, first, size):
        return wtile.at[c % 2, j // 2, pl.ds((j % 2) * depth + first, size), :]

    def tile_loads(c):
        copies = []
        for j in range(RING):
            z = wrap(pos_z + j)
            down = wd_ref.at[1, :, block_cols(c)] if j == 0 else gd_ref.at[z, :, block_cols(c)]
            out = wo_ref.at[1, 0, :, block_cols(c)] if j == 0 else go_ref.at[z, :, block_cols(c)]
            copies.append(pltpu.make_async_copy(down, tile_place(c, j, 0, ff_local), tile_sem.at[c % 2]))
            copies.append(pltpu.make_async_copy(out, tile_place(c, j, ff_local, head_dim), tile_sem.at[c % 2]))
        return copies

    start(tile_loads(0))
    given = hid.at[pl.ds(0, (RING - 1) * rows_per * depth // ff_local), :]
    take(give_recv, given)
    for d in range(DIRS):
        pl.semaphore_wait(drained_sem.at[d], 1)

    def quarter_of(piece, offset, size):
        return span(piece * quarter_rows + offset, size, quarter_rows // 2)

    def landed(d, first, size):
        return pl.ds(rows_per + d * (3 * quarter_rows // 2) + first, size)

    def rows_at(z, piece, offset, size):
        return span(z * rows_per + piece * quarter_rows + offset, size, quarter_rows // 2)

    def last_messages(step, c, d, z_first):
        s, cols, half = sign[d], block_cols(c), quarter_rows // 2
        near, behind, back = wrap(pos_y + s), wrap(pos_y - s), wrap(pos_z - s)
        along_y = step < 2 or (step < 4) != z_first
        if step == 0:
            pairs = [(part.at[quarter_of(wrap(pos_y + 2), d * half, half), cols], part.at[landed(d, quarter_rows, half), cols])]
        elif step == 1:
            pairs = [(part.at[quarter_of(near, 0, quarter_rows), cols], part.at[landed(d, 0, quarter_rows), cols])]
        else:
            if step == 2:
                rows = [rows_at(pos_z, pos_y, 0, quarter_rows)]
            elif step == 3:
                rows = [rows_at(back, pos_y, d * half, half) if z_first else rows_at(pos_z, behind, d * half, half)]
            elif step == 4:
                rows = [rows_at(z, pos_y, 0, quarter_rows) for z in range(RING)] if z_first else [rows_at(pos_z, 0, 0, rows_per)]
            else:
                rows = [rows_at(z, behind, d * half, half) for z in range(RING)] if z_first else [rows_at(back, 0, d * (rows_per // 2), rows_per // 2)]
            pairs = [(xbuf.at[r, cols], xbuf.at[r, cols]) for r in rows]
        to = (y_peer if along_y else z_peer)(d)
        return [remote(src, dst, last_send.at[step], last_recv.at[c, step], head=to) for src, dst in pairs]

    def last_arrived(step, cols):
        rows = (quarter_rows, 2 * quarter_rows, 2 * quarter_rows, quarter_rows, 2 * rows_per, rows_per)[step]
        return (part if step < 2 else xbuf).at[pl.ds(0, rows), cols]

    def send_last(step, c):
        def both(z_first):
            for d in range(DIRS):
                start(last_messages(step, c, d, z_first))

        if step < 2:
            both(False)
            return
        z_first = jnp.logical_and(c >= 5, c % 2 == 1)

        @pl.when(z_first)
        def _():
            both(True)

        @pl.when(jnp.logical_not(z_first))
        def _():
            both(False)

    def out_store(c):
        return pltpu.make_async_copy(xbuf.at[:, block_cols(c)], out_ref.at[:, block_cols(c)], store_sem)

    def last_project(c):
        @pl.when(c + 1 < LAST_BLOCKS)
        def _():
            start(tile_loads(c + 1))

        take(tile_sem.at[c % 2], wtile.at[c % 2, :, pl.ds(0, 2 * depth), :])
        total = None
        for j in range(RING):
            z = wrap(pos_z + j)
            own = span(pos_z * rows_per, rows_per)
            hidden_rows = hid[own, :] if j == 0 else xs[1, :, span(z * ff_local, ff_local)]
            out_rows = att[own, :] if j == 0 else att_all[z]
            term = dot(hidden_rows, wtile[c % 2, j // 2, pl.ds((j % 2) * depth, ff_local), :])
            term = term + dot(out_rows, wtile[c % 2, j // 2, pl.ds((j % 2) * depth + ff_local, head_dim), :])
            total = term if total is None else total + term
        part[pl.ds(0, rows_per), block_cols(c)] = total

    def last_stage(number, c):
        cols, half = block_cols(c), quarter_rows // 2
        if number == 0:
            last_project(c)
        else:
            take(last_recv.at[c, number - 1], last_arrived(number - 1, cols))
        if number == 1:
            for d in range(DIRS):
                piece = quarter_of(wrap(pos_y + sign[d]), d * half, half)
                part[piece, cols] = part[piece, cols] + part[landed(d, quarter_rows, half), cols]
        if number == 2:
            own = quarter_of(pos_y, 0, quarter_rows)
            total = part[own, cols] + part[landed(0, 0, quarter_rows), cols] + part[landed(1, 0, quarter_rows), cols]
            update = total.astype(bf16).astype(f32)
            rows = rows_at(pos_z, pos_y, 0, quarter_rows)
            xbuf[rows, cols] = (xbuf[rows, cols].astype(f32) + update).astype(bf16)
        if number < LAST_STEPS:
            send_last(number, c)
        else:
            out_store(c).start()

    def last_tick(t, carry):
        for number in range(LAST_STEPS, -1, -1):
            c = t - LAST_GAP * number

            @pl.when(jnp.logical_and(c >= 0, c < LAST_BLOCKS))
            def _():
                last_stage(number, c)
        return carry

    lax.fori_loop(0, LAST_BLOCKS + LAST_GAP * LAST_STEPS, last_tick, 0)

    take(cache_sem, kv.at[own_rows, :])
    take(relay_send, relay_buf)
    kv_sent()
    take(part_send, xbuf.at[pl.ds(0, 3 * depth // 8), :])
    take(round_send, gd_ref.at[pl.ds(0, 2), pl.ds(0, 9 * depth // 16), :])
    take(side_send, parts_ref)
    take(give_send, given)
    for step in range(LAST_STEPS):
        take(last_send.at[step], last_arrived(step, pl.ds(0, d_model)))
    take(store_sem, xbuf)


def layers(x_loc, cos_t, sin_t, norm_gain, w_q, w_k, w_v, w_gate, w_up, w_down, w_o):
    tok_count, d_model = x_loc.shape
    head_dim = w_q.shape[2]
    ff_local = w_gate.shape[2]
    rows_per = tok_count // KV_CHUNKS
    chunk_rows = tok_count // CHUNKS
    landed = 3 * chunk_rows // (2 * RING)
    half_cols = d_model // HALVES
    any_spec = pl.BlockSpec(memory_space=pl.ANY)
    vmem_spec = pl.BlockSpec(memory_space=pltpu.VMEM)
    bf16, f32 = jnp.bfloat16, jnp.float32
    dma = pltpu.SemaphoreType.DMA
    shape = jax.ShapeDtypeStruct
    return pl.pallas_call(
        layers_kernel,
        out_shape=[shape((tok_count, d_model), bf16)] + [shape((tok_count, head_dim), bf16)] * 4
        + [shape((RING, ff_local, d_model), bf16), shape((RING, head_dim, d_model), bf16)],
        in_specs=[any_spec, any_spec, any_spec, vmem_spec] + [any_spec] * 7,
        out_specs=[any_spec] * 7,
        scratch_shapes=[
            pltpu.VMEM((tok_count, d_model), bf16),
            pltpu.VMEM((PART_SLOTS * chunk_rows, d_model), f32),
            pltpu.VMEM((RECV_SLOTS, HALVES, DIRS, landed, half_cols), f32),
            pltpu.VMEM((RECV_SLOTS, HALVES, DIRS, landed, half_cols // RING), f32),
            pltpu.VMEM((tok_count, ff_local), bf16),
            pltpu.VMEM((tok_count, head_dim), bf16),
            pltpu.VMEM((2, ff_local + head_dim, DOWN_TILE), bf16),
            pltpu.VMEM((2, 2, d_model, W_TILE), bf16),
            pltpu.VMEM((2 * CHIPS * tok_count, 2 * head_dim), bf16),
            pltpu.VMEM((tok_count, head_dim), bf16),
            pltpu.VMEM((2, tok_count, head_dim), f32),
            pltpu.VMEM((2, tok_count, 128), f32),
            pltpu.VMEM((2, tok_count, 128), f32),
            pltpu.VMEM((2, rows_per, d_model), bf16),
            pltpu.VMEM((CHUNKS, HALVES, chunk_rows // RING, half_cols // RING), bf16),
            dma((2,)), dma, dma((2, 2)), dma((2, 2)), dma, dma,
            dma((10,)), dma((4, KV_CHUNKS)), dma((4, KV_CHUNKS)), dma, dma((2,)),
            dma, dma((2, RING - 1)), dma, dma,
            dma, dma,
            pltpu.VMEM((KV_CHUNKS, rows_per, W_TILE), bf16), dma, dma,
            pltpu.VMEM((RING, rows_per, head_dim), bf16),
            dma((PART_SLOTS,)), dma((4,)), dma((RECV_SLOTS, STEPS)),
            dma((LAST_STEPS,)), dma((LAST_BLOCKS, LAST_STEPS)), dma((2,)),
            pltpu.VMEM((tok_count, head_dim // 2), f32), pltpu.VMEM((tok_count, head_dim // 2), f32), dma((2,)),
            pltpu.SemaphoreType.REGULAR((3,)), pltpu.SemaphoreType.REGULAR((DIRS,)),
        ],
        compiler_params=pltpu.CompilerParams(collective_id=0, has_side_effects=True, vmem_limit_bytes=67043328),
        name='layers',
    )(x_loc, cos_t, sin_t, norm_gain, w_q, w_k, w_v, w_gate, w_up, w_down, w_o)


EMIT_PARTS = 8


def emit_kernel(x_ref, k_first, k_second, v_first, v_second, x_out, k_out, v_out, xbuf, rows, load_sem, store_sem):
    size = x_ref.shape[0] // EMIT_PARTS
    loads, stores = [], []
    for n in range(EMIT_PARTS):
        part = pl.ds(n * size, size)
        loads.append(pltpu.make_async_copy(x_ref.at[part, :], xbuf.at[part, :], load_sem.at[n]))
        stores.append(pltpu.make_async_copy(xbuf.at[part, :], x_out.at[part, :], store_sem.at[n]))
    for n, (ref, out) in enumerate(((k_first, k_out.at[0]), (k_second, k_out.at[1]), (v_first, v_out.at[0]), (v_second, v_out.at[1]))):
        loads.append(pltpu.make_async_copy(ref, rows.at[n], load_sem.at[EMIT_PARTS + n]))
        stores.append(pltpu.make_async_copy(rows.at[n], out, store_sem.at[EMIT_PARTS + n]))
    for copy in loads:
        copy.start()
    for load, store in zip(loads, stores):
        load.wait()
        store.start()
    for copy in stores:
        copy.wait()


def emit(x_out, k_first, k_second, v_first, v_second):
    any_spec = pl.BlockSpec(memory_space=pl.ANY)
    cache = jax.ShapeDtypeStruct((2,) + k_first.shape, jnp.bfloat16)
    return pl.pallas_call(
        emit_kernel,
        out_shape=[jax.ShapeDtypeStruct(x_out.shape, jnp.bfloat16), cache, cache],
        in_specs=[any_spec] * 5,
        out_specs=[any_spec] * 3,
        scratch_shapes=[
            pltpu.VMEM(x_out.shape, jnp.bfloat16),
            pltpu.VMEM((4,) + k_first.shape, jnp.bfloat16),
            pltpu.SemaphoreType.DMA((EMIT_PARTS + 4,)),
            pltpu.SemaphoreType.DMA((EMIT_PARTS + 4,)),
        ],
        compiler_params=pltpu.CompilerParams(vmem_limit_bytes=63 * 1024 * 1024),
        name='emit',
    )(x_out, k_first, k_second, v_first, v_second)


def solution(mesh):
    row_spec = P(('batch', 'seq'), None)
    pos_spec = P(('batch', 'seq'))
    head_spec = P(None, None, 'head', None)
    out_proj_spec = P(None, 'head', None, None)
    col_spec = P(None, None, 'head')
    down_spec = P(None, 'head', None)
    cache_spec = P(None, ('batch', 'seq'), 'head', None)

    def local_forward(x_loc, pos_loc, w_q, w_k, w_v, w_o, w_gate, w_up, w_down, norm_gain):
        tok_count, d_model = x_loc.shape
        layer_count = w_q.shape[0]
        head_dim = w_q.shape[3]
        flat_q, flat_k, flat_v = (w.reshape(layer_count, d_model, head_dim) for w in (w_q, w_k, w_v))
        cos_t, sin_t = rope_tables(pos_loc, head_dim)
        x_out, k_first, v_first, k_second, v_second, _, _ = layers(x_loc, cos_t, sin_t, norm_gain, flat_q, flat_k, flat_v, w_gate, w_up, w_down, w_o)
        x_out, k_all, v_all = emit(x_out, k_first, k_second, v_first, v_second)
        cache_shape = (layer_count, tok_count, 1, head_dim)
        return x_out, k_all.reshape(cache_shape), v_all.reshape(cache_shape)

    return jax.shard_map(local_forward, mesh=mesh, in_specs=(row_spec, pos_spec, head_spec, head_spec, head_spec, out_proj_spec, col_spec, col_spec, down_spec, P(None, None)), out_specs=(row_spec, cache_spec, cache_spec), check_vma=False)
```
